128 devices in a mesh: dp: 1, row: 16 (over z, y), col: 8 (over x, core).
Axes of the slice: x: 4, y: 4, z: 4, core: 2. Of those that a mesh axis runs over, the one named last changes fastest.
Arguments:
- x_in: bfloat16 [16, 512, 4096], P('dp', None, ('row', 'col'))
- ln_gain: bfloat16 [2, 4096], P(None, ('row', 'col'))
- w_in: bfloat16 [2, 4096, 36864], P(None, 'row', 'col')
- w_kv: bfloat16 [2, 4096, 256], P(None, 'row', 'col')
- w_out: bfloat16 [2, 20480, 4096], P(None, 'col', 'row')
Outputs:
- output 1: bfloat16 [16, 512, 4096], P('dp', None, ('row', 'col'))
- output 2: bfloat16 [2, 2, 16, 512, 128], P(None, None, 'dp', ('row', 'col'))
All inputs are finite; a program needn't handle non-finite values.
Results may differ from the reference program's by a relative error of at most 0.0180243.
Values are sent between devices in bfloat16 or wider.
A program may use at most 1 GiB of HBM per device.

```python
import jax
import jax.numpy as jnp
from jax import lax

D_MODEL = 4096
HEADS = 32
HEAD_DIM = 128
FF_WIDTH = 16384
BATCH = 16
SEQ_LEN = 512
COL_SHARDS = 8
LAYERS = 2

LN_EPS = 1e-6
E_WIDTH = HEADS * HEAD_DIM + 2 * FF_WIDTH
R_WIDTH = HEADS * HEAD_DIM + FF_WIDTH
E_BLOCK = E_WIDTH // COL_SHARDS
Q_BLOCK = HEADS * HEAD_DIM // COL_SHARDS
F_BLOCK = FF_WIDTH // COL_SHARDS
HALF_DIM = HEAD_DIM // 2


def setup_inputs(seed: int = 0, part: int = 0) -> dict:
    root_key = jax.random.key(seed)
    shared_root, part_root = jax.random.split(root_key)
    part_key = jax.random.fold_in(part_root, part)
    key_x, key_off = jax.random.split(part_key)
    key_g, key_in, key_kv, key_out = jax.random.split(shared_root, 4)
    slope_part = 2.0 * (jnp.arange(D_MODEL, dtype=jnp.float32) / D_MODEL - 0.5)
    offset = slope_part + 0.5 * jax.random.normal(key_off, (D_MODEL,), jnp.float32)
    x_in = (jax.random.normal(key_x, (BATCH, SEQ_LEN, D_MODEL), jnp.float32) + offset).astype(jnp.bfloat16)
    ln_gain = (1.0 + 0.3 * jax.random.normal(key_g, (LAYERS, D_MODEL), jnp.float32)).astype(jnp.bfloat16)
    w_in = (jax.random.normal(key_in, (LAYERS, D_MODEL, E_WIDTH), jnp.float32) * D_MODEL ** -0.5).astype(jnp.bfloat16)
    w_kv = (jax.random.normal(key_kv, (LAYERS, D_MODEL, 2 * HEAD_DIM), jnp.float32) * D_MODEL ** -0.5).astype(jnp.bfloat16)
    w_out = (jax.random.normal(key_out, (LAYERS, R_WIDTH, D_MODEL), jnp.float32) * R_WIDTH ** -0.5).astype(jnp.bfloat16)
    return {"x_in": x_in, "ln_gain": ln_gain, "w_in": w_in, "w_kv": w_kv, "w_out": w_out}


def layer_norm(hidden, gain_row):
    hidden_f32 = hidden.astype(jnp.float32)
    mean_val = jnp.mean(hidden_f32, axis=-1, keepdims=True)
    centered = hidden_f32 - mean_val
    variance = jnp.mean(centered * centered, axis=-1, keepdims=True)
    return (centered * lax.rsqrt(variance + LN_EPS) * gain_row.astype(jnp.float32)).astype(jnp.bfloat16)


def rope_tables(positions):
    inv_freq = 1.0 / (10000.0 ** (jnp.arange(HALF_DIM, dtype=jnp.float32) * 2.0 / HEAD_DIM))
    angles = positions.astype(jnp.float32)[:, None] * inv_freq[None, :]
    return jnp.cos(angles), jnp.sin(angles)


def apply_rope(values, cos_tab, sin_tab):
    lower_half = values[..., :HALF_DIM]
    upper_half = values[..., HALF_DIM:]
    return jnp.concatenate([lower_half * cos_tab - upper_half * sin_tab, upper_half * cos_tab + lower_half * sin_tab], axis=-1)


def one_layer(hidden, params):
    gain_row, w_in_layer, w_kv_layer, w_out_layer = params
    normed = layer_norm(hidden, gain_row)
    projected = jnp.dot(normed, w_in_layer, preferred_element_type=jnp.float32).astype(jnp.bfloat16).reshape(SEQ_LEN, COL_SHARDS, E_BLOCK)
    kv_proj = jnp.dot(normed, w_kv_layer, preferred_element_type=jnp.float32).astype(jnp.bfloat16)
    query = projected[:, :, :Q_BLOCK].reshape(SEQ_LEN, HEADS, HEAD_DIM)
    gate_val = projected[:, :, Q_BLOCK:Q_BLOCK + F_BLOCK]
    up_val = projected[:, :, Q_BLOCK + F_BLOCK:]
    positions = jnp.arange(SEQ_LEN)
    cos_tab, sin_tab = rope_tables(positions)
    q_rot = (apply_rope(query.astype(jnp.float32), cos_tab[:, None, :], sin_tab[:, None, :]) * HEAD_DIM ** -0.5).astype(jnp.bfloat16)
    k_rot = apply_rope(kv_proj[:, :HEAD_DIM].astype(jnp.float32), cos_tab, sin_tab).astype(jnp.bfloat16)
    v_val = kv_proj[:, HEAD_DIM:]
    scores = jnp.einsum("qhd,kd->hqk", q_rot.astype(jnp.float32), k_rot.astype(jnp.float32))
    causal = positions[None, :] <= positions[:, None]
    scores = jnp.where(causal[None, :, :], scores, -1e30)
    attn_prob = jax.nn.softmax(scores, axis=-1).astype(jnp.bfloat16)
    attn_out = jnp.einsum("hqk,kd->qhd", attn_prob.astype(jnp.float32), v_val.astype(jnp.float32)).astype(jnp.bfloat16)
    mlp_out = (jax.nn.silu(gate_val.astype(jnp.float32)) * up_val.astype(jnp.float32)).astype(jnp.bfloat16)
    joined = jnp.concatenate([attn_out.reshape(SEQ_LEN, COL_SHARDS, Q_BLOCK), mlp_out], axis=2).reshape(SEQ_LEN, R_WIDTH)
    update = jnp.dot(joined, w_out_layer, preferred_element_type=jnp.float32).astype(jnp.bfloat16)
    return hidden + update, jnp.stack([k_rot, v_val])


def reference(x_in, ln_gain, w_in, w_kv, w_out):
    def one_sequence(seq_x):
        return lax.scan(one_layer, seq_x, (ln_gain, w_in, w_kv, w_out))
    y_out, kv_all = lax.map(one_sequence, x_in)
    return y_out, jnp.transpose(kv_all, (1, 2, 0, 3, 4))
```

```python
import jax
import jax.numpy as jnp
from jax import lax
from jax.sharding import Mesh
from jax.sharding import PartitionSpec as P

LN_EPS = 1e-6
NZ = 4


def rope_tables(positions, head_dim):
    half_dim = head_dim // 2
    inv_freq = 1.0 / (10000.0 ** (jnp.arange(half_dim, dtype=jnp.float32) * 2.0 / head_dim))
    angles = positions.astype(jnp.float32)[:, None] * inv_freq[None, :]
    return jnp.cos(angles), jnp.sin(angles)


def apply_rope(values, cos_tab, sin_tab):
    half_dim = values.shape[-1] // 2
    lower_half = values[..., :half_dim]
    upper_half = values[..., half_dim:]
    return jnp.concatenate([lower_half * cos_tab - upper_half * sin_tab, upper_half * cos_tab + lower_half * sin_tab], axis=-1)


def solution(mesh):
    row_size = mesh.shape["row"]
    n_col = mesh.shape["col"]
    n_z = NZ
    n_y = row_size // n_z
    n_tp = n_y * n_col
    n_dev = row_size * n_col
    mesh4 = Mesh(mesh.devices.reshape(n_z, n_y, n_col), ("z", "y", "col"))
    every = ("z", "y", "col")
    tp = ("y", "col")
    act_spec = P(None, None, every)
    w_spec = P(None, ("z", "y"), "col")

    def device_fn(x_loc, gain_loc, w_in_loc, w_kv_loc, w_out_loc):
        n_layers = w_in_loc.shape[0]
        n_batch, seq_len, d_local = x_loc.shape
        d_model = d_local * n_dev
        e_block = w_in_loc.shape[2]
        r_block = w_out_loc.shape[1]
        f_block = e_block - r_block
        q_block = r_block - f_block
        q_loc, f_loc = q_block // n_y, f_block // n_y
        head_dim = w_kv_loc.shape[2] * n_col // 2
        heads_local = q_loc // head_dim
        batch_loc = n_batch // n_z
        n_tok = n_batch * seq_len
        tok_z = n_tok // n_z
        tok_loc = n_tok // n_dev
        seq_local = seq_len // n_dev
        d_row = w_in_loc.shape[1]
        positions = jnp.arange(seq_len)
        cos_tab, sin_tab = rope_tables(positions, head_dim)
        causal = positions[None, :] <= positions[:, None]

        gain = lax.all_gather(gain_loc, every, axis=1, tiled=True)

        weights = []
        for l in range(n_layers):
            wi = w_in_loc[l]
            q_part = wi[:, :q_block].reshape(d_row, n_y, q_loc)
            g_part = wi[:, q_block:q_block + f_block].reshape(d_row, n_y, f_loc)
            u_part = wi[:, q_block + f_block:].reshape(d_row, n_y, f_loc)
            wi = jnp.concatenate([q_part, g_part, u_part], axis=2).transpose(1, 0, 2)
            wi = lax.all_to_all(wi, "y", 0, 0, tiled=True).reshape(n_y * d_row, q_loc + 2 * f_loc)
            wkv = lax.all_gather(w_kv_loc[l], "col", axis=1, tiled=True)
            wkv = lax.all_gather(wkv, "y", axis=0, tiled=True)
            wi = lax.all_gather(jnp.concatenate([wi, wkv], axis=1), "z", axis=0, tiled=True)
            wo = w_out_loc[l]
            wo = jnp.concatenate([wo[:q_block].reshape(n_y, q_loc, -1), wo[q_block:].reshape(n_y, f_loc, -1)], axis=1)
            wo = lax.all_to_all(wo, "y", 0, 0, tiled=True)
            wo = wo.transpose(1, 0, 2).reshape(q_loc + f_loc, -1)
            wo = lax.all_gather(wo, "z", axis=1, tiled=True)
            weights.append((wi, wo))

        xs = lax.all_to_all(x_loc.reshape(n_dev, tok_loc, d_local), every, 0, 0, tiled=True)
        hidden = xs.reshape(n_dev, tok_loc, d_local).transpose(1, 0, 2).reshape(tok_loc, d_model)
        kv_outs = []
        for l in range(n_layers):
            w_i, w_o = weights[l]
            hf = hidden.astype(jnp.float32)
            mean = jnp.mean(hf, axis=-1, keepdims=True)
            centered = hf - mean
            var = jnp.mean(centered * centered, axis=-1, keepdims=True)
            normed = (centered * lax.rsqrt(var + LN_EPS) * gain[l].astype(jnp.float32)).astype(jnp.bfloat16)
            h = lax.all_gather(normed, tp, axis=0, tiled=True)
            proj = jnp.dot(h, w_i, preferred_element_type=jnp.float32).astype(jnp.bfloat16)
            query = proj[:, :q_loc].reshape(batch_loc, seq_len, heads_local, head_dim)
            gate_val = proj[:, q_loc:q_loc + f_loc]
            up_val = proj[:, q_loc + f_loc:q_loc + 2 * f_loc]
            kv_proj = proj[:, q_loc + 2 * f_loc:].reshape(batch_loc, seq_len, 2 * head_dim)
            q_rot = (apply_rope(query.astype(jnp.float32), cos_tab[:, None, :], sin_tab[:, None, :]) * head_dim ** -0.5).astype(jnp.bfloat16)
            k_rot = apply_rope(kv_proj[..., :head_dim].astype(jnp.float32), cos_tab, sin_tab).astype(jnp.bfloat16)
            v_val = kv_proj[..., head_dim:]
            scores = jnp.einsum("crie,cle->cirl", q_rot, k_rot, preferred_element_type=jnp.float32)
            scores = jnp.where(causal, scores, -1e30)
            attn_prob = jax.nn.softmax(scores, axis=-1).astype(jnp.bfloat16)
            attn_out = jnp.einsum("cirl,cle->crie", attn_prob, v_val, preferred_element_type=jnp.float32).astype(jnp.bfloat16).reshape(tok_z, q_loc)
            mlp_out = (jax.nn.silu(gate_val.astype(jnp.float32)) * up_val.astype(jnp.float32)).astype(jnp.bfloat16)
            joined = jnp.concatenate([attn_out, mlp_out], axis=1)
            part = jnp.dot(joined, w_o, preferred_element_type=jnp.float32).astype(jnp.bfloat16)
            update = lax.psum_scatter(part, tp, scatter_dimension=0, tiled=True)
            hidden = hidden + update
            kv_outs.append(jnp.stack([k_rot, v_val]))

        y_parts = hidden.reshape(tok_loc, n_dev, d_local).transpose(1, 0, 2)
        y_loc = lax.all_to_all(y_parts, every, 0, 0, tiled=True).reshape(n_batch, seq_len, d_local)
        kv = jnp.stack(kv_outs).reshape(n_layers, 2, batch_loc, n_z, n_tp, seq_local, head_dim)
        me = lax.axis_index("y") * n_col + lax.axis_index("col")
        kv = lax.dynamic_index_in_dim(kv, me, axis=4, keepdims=False)
        kv = lax.all_to_all(kv, "z", 3, 2, tiled=True)
        kv = kv.reshape(n_layers, 2, n_batch, seq_local, head_dim)
        return y_loc, kv

    return jax.shard_map(device_fn, mesh=mesh4, in_specs=(act_spec, P(None, every), w_spec, w_spec, P(None, "col", ("z", "y"))), out_specs=(act_spec, P(None, None, None, every, None)), check_vma=False)
```

```python
import functools

import jax
import jax.numpy as jnp
from jax import lax
from jax.experimental import pallas as pl
from jax.experimental.pallas import tpu as pltpu
from jax.sharding import Mesh
from jax.sharding import PartitionSpec as P

LN_EPS = 1e-6
RING = 4
CORES = 2
VMEM_LIMIT = 63 * 1024 * 1024


def rope_tables(positions, head_dim):
    half_dim = head_dim // 2
    inv_freq = 1.0 / (10000.0 ** (jnp.arange(half_dim, dtype=jnp.float32) * 2.0 / head_dim))
    angles = positions.astype(jnp.float32)[:, None] * inv_freq[None, :]
    return jnp.cos(angles), jnp.sin(angles)


def apply_rope(values, cos_tab, sin_tab):
    half_dim = values.shape[-1] // 2
    lower_half = values[..., :half_dim]
    upper_half = values[..., half_dim:]
    return jnp.concatenate([lower_half * cos_tab - upper_half * sin_tab, upper_half * cos_tab + lower_half * sin_tab], axis=-1)


def _place():
    return lax.axis_index("z"), lax.axis_index("y"), lax.axis_index("x"), lax.axis_index("core")


def _enter(me):
    z, y, x, c = me
    peers = [
        (z, lax.rem(y + 1, RING), x, c),
        (z, lax.rem(y + RING - 1, RING), x, c),
        (z, y, lax.rem(x + 1, RING), c),
        (z, y, lax.rem(x + RING - 1, RING), c),
        (z, y, x, 1 - c),
    ]
    sem = pltpu.get_barrier_semaphore()
    for dev in peers:
        pl.semaphore_signal(sem, inc=1, device_id=dev, device_id_type=pl.DeviceIdType.MESH)
    return len(peers)


def _enter_wait(count):
    pl.semaphore_wait(pltpu.get_barrier_semaphore(), count)


def ag_kernel(hid_ref, gain_ref, out_ref, h_ref, send_sem, recv_sem, dsend_sem, drecv_sem, loc_sem):
    me = _place()
    z, y, x, c = me
    n_peers = _enter(me)
    rows, d_model = hid_ref.shape
    quarter = rows // 4
    gain = gain_ref[...].astype(jnp.float32)
    for r in range(4):
        blk = hid_ref[r * quarter:(r + 1) * quarter, :].astype(jnp.float32)
        mean = jnp.mean(blk, axis=-1, keepdims=True)
        cen = blk - mean
        var = jnp.mean(cen * cen, axis=-1, keepdims=True)
        h_ref[r * quarter:(r + 1) * quarter, :] = (cen * lax.rsqrt(var + LN_EPS) * gain).astype(jnp.bfloat16)
    _enter_wait(n_peers)

    def shift(q, first, second):
        if q == 0:
            return lax.rem(y + second + RING, RING), lax.rem(x + first + RING, RING)
        return lax.rem(y + first + RING, RING), lax.rem(x + second + RING, RING)

    def span(q, part):
        if part is None:
            return pl.ds(q * 2 * quarter, 2 * quarter)
        return pl.ds((q * 2 + part) * quarter, quarter)

    offs = (0, -1, 1, 2)
    copies = {}

    def ici(idx, q, first, second, part, to_first, to_second, own=False):
        sy, sx = shift(q, first, second)
        ty, tx = shift(q, to_first, to_second)
        rws = span(q, part)
        dst = out_ref.at[sy, sx, c, rws]
        cp = pltpu.make_async_remote_copy(
            src_ref=h_ref.at[rws] if own else dst,
            dst_ref=dst,
            send_sem=send_sem.at[idx],
            recv_sem=recv_sem.at[idx],
            device_id=(z, ty, tx, c),
            device_id_type=pl.DeviceIdType.MESH,
        )
        cp.start()
        copies[idx] = cp

    dies = {}

    def die(idx, q, first, second, own=False):
        sy, sx = shift(q, first, second)
        rws = span(q, None)
        dst = out_ref.at[sy, sx, c, rws]
        cp = pltpu.make_async_remote_copy(
            src_ref=h_ref.at[rws] if own else dst,
            dst_ref=dst,
            send_sem=dsend_sem.at[idx],
            recv_sem=drecv_sem.at[idx],
            device_id=(z, y, x, 1 - c),
            device_id_type=pl.DeviceIdType.MESH,
        )
        cp.start()
        dies[idx] = cp

    def p1(q, d):
        return q * 20 + d

    def p1f(q, d):
        return q * 20 + 2 + d

    def p2(q, k, d):
        return q * 20 + 4 + k * 4 + d

    def p2f(q, k, d):
        return q * 20 + 4 + k * 4 + 2 + d

    sgn = (1, -1)
    for q in range(2):
        for d in range(2):
            ici(p1(q, d), q, 0, 0, None, sgn[d], 0, own=True)
    for q in range(2):
        for d in range(2):
            ici(p2(q, 0, d), q, 0, 0, None, 0, sgn[d], own=True)
    for q in range(2):
        die(q * 16, q, 0, 0, own=True)
    own = pltpu.make_async_copy(h_ref, out_ref.at[y, x, c], loc_sem)
    own.start()

    for d in range(2):
        for q in range(2):
            copies[p1(q, d)].wait_recv()
            src = -sgn[d]
            ici(p1f(q, d), q, src, 0, d, sgn[d], 0)
            for e in range(2):
                ici(p2(q, 1 + d, e), q, src, 0, None, 0, sgn[e])
            die(q * 16 + 1 + d, q, src, 0)
    for d in range(2):
        for q in range(2):
            copies[p2(q, 0, d)].wait_recv()
            src = -sgn[d]
            ici(p2f(q, 0, d), q, 0, src, d, 0, sgn[d])
            die(q * 16 + 4 + d, q, 0, src)
    for q in range(2):
        copies[p1f(q, 0)].wait_recv()
        copies[p1f(q, 1)].wait_recv()
        for e in range(2):
            ici(p2(q, 3, e), q, 2, 0, None, 0, sgn[e])
        die(q * 16 + 3, q, 2, 0)
    for k in (1, 2, 3):
        for d in range(2):
            for q in range(2):
                copies[p2(q, k, d)].wait_recv()
                src = -sgn[d]
                ici(p2f(q, k, d), q, offs[k], src, d, 0, sgn[d])
                die(q * 16 + 4 + k * 3 + d, q, offs[k], src)
    for k in range(4):
        for q in range(2):
            copies[p2f(q, k, 0)].wait_recv()
            copies[p2f(q, k, 1)].wait_recv()
            die(q * 16 + 4 + k * 3 + 2, q, offs[k], 2)
    for idx in sorted(dies):
        dies[idx].wait_recv()
    for idx in sorted(dies):
        dies[idx].wait_send()
    for idx in sorted(copies):
        copies[idx].wait_send()
    own.wait()


def all_gather_norm(hidden, gain, layer):
    rows, d_model = hidden.shape
    group = RING * RING * CORES
    out = pl.pallas_call(
        ag_kernel,
        out_shape=jax.ShapeDtypeStruct((RING, RING, CORES, rows, d_model), jnp.bfloat16),
        in_specs=[pl.BlockSpec(memory_space=pltpu.VMEM)] * 2,
        out_specs=pl.BlockSpec(memory_space=pl.ANY),
        scratch_shapes=[
            pltpu.VMEM((rows, d_model), jnp.bfloat16),
            pltpu.SemaphoreType.DMA((40,)),
            pltpu.SemaphoreType.DMA((40,)),
            pltpu.SemaphoreType.DMA((32,)),
            pltpu.SemaphoreType.DMA((32,)),
            pltpu.SemaphoreType.DMA,
        ],
        compiler_params=pltpu.CompilerParams(collective_id=2 * layer, has_side_effects=True),
        cost_estimate=pl.CostEstimate(flops=25_000_000_000, bytes_accessed=group * rows * d_model * 2, transcendentals=0),
        name=f"gather_norm_{layer}",
    )(hidden, gain)
    return out.reshape(group * rows, d_model)


SLOT_OFF = (2, 1, 3, 0)


def rs_kernel(join_ref, w_ref, hid_ref, out_ref, lhs, away, acc, die_in, in1, in2, in3, in4,
              dsend, drecv, send1, recv1, send2, recv2, send3, recv3, send4, recv4):
    me = _place()
    z, y, x, c = me
    n_peers = _enter(me)
    rows = join_ref.shape[3]
    half = w_ref.shape[1] // 2
    depth = w_ref.shape[0]
    for s in range(RING):
        for j in range(RING):
            yy = lax.rem(y + SLOT_OFF[s], RING)
            xx = lax.rem(x + SLOT_OFF[j], RING)
            for cc in range(CORES):
                val = join_ref[yy, xx, (1 - c) if cc == 0 else c]
                lhs[0, s, cc, j] = val
                lhs[1, j, cc, s] = val
    _enter_wait(n_peers)

    def peer(q, first, second):
        dy = first * (1 - q) + second * q
        dx = first * q + second * (1 - q)
        return (z, lax.rem(y + dy + RING, RING), lax.rem(x + dx + RING, RING), c)

    def remote(src, dst, ssem, rsem, dev):
        return pltpu.make_async_remote_copy(
            src_ref=src, dst_ref=dst, send_sem=ssem, recv_sem=rsem, device_id=dev, device_id_type=pl.DeviceIdType.MESH)

    def die_copy(q, s):
        return remote(away.at[q, s], die_in.at[q, s], dsend.at[q, s], drecv.at[q, s], (z, y, x, 1 - c))

    def first_copy(q, d):
        return remote(acc.at[q, 0, pl.ds(2 * d, 2)], in1.at[q, d], send1.at[q, d], recv1.at[q, d], peer(q, 1 - 2 * d, 0))

    def second_copy(q, d, h):
        return remote(acc.at[q, 1 + d, pl.ds(2 * h, 2)], in2.at[q, d, pl.ds(2 * h, 2)], send2.at[q, d, h], recv2.at[q, d, h], peer(q, 1 - 2 * d, 0))

    def third_copy(q, d):
        rws = pl.ds(d * (rows // 2), rows // 2)
        return remote(acc.at[q, 3, 0, rws], in3.at[q, d], send3.at[q, d], recv3.at[q, d], peer(q, 0, 1 - 2 * d))

    def fourth_copy(q, d):
        return remote(acc.at[q, 3, 1 + d], in4.at[q, d], send4.at[q, d], recv4.at[q, d], peer(q, 0, 1 - 2 * d))

    n_blk = min(half, 512)

    def tile(q, s):
        left = lhs[q, s].reshape(CORES * RING * rows, depth)

        @pl.loop(0, half // n_blk)
        def _(n):
            col = pl.multiple_of(n * n_blk, n_blk)
            wcol = pl.multiple_of(q * half + n * n_blk, n_blk)
            res = jnp.dot(left, w_ref[:, pl.ds(wcol, n_blk)], preferred_element_type=jnp.float32).astype(jnp.bfloat16)
            res = res.reshape(CORES, RING, rows, n_blk)
            away[q, s, :, :, pl.ds(col, n_blk)] = res[0]
            acc[q, s, :, :, pl.ds(col, n_blk)] = res[1]

    def pair_sum(q, s):
        die_copy(q, s).wait_recv()

        @pl.loop(0, RING)
        def _(j):
            acc[q, s, j] = acc[q, s, j] + die_in[q, s, j]

    @pl.loop(0, 2 * RING)
    def _(t):
        s = t // 2
        q = t % 2
        tile(q, s)
        die_copy(q, s).start()

        @pl.when(t >= 2)
        def _():
            pair_sum(q, s - 1)

        @pl.when(s == 1)
        def _():
            first_copy(q, 0).start()
            first_copy(q, 1).start()

        @pl.when(s == 2)
        def _():
            second_copy(q, 0, 1).start()

        @pl.when(s == 3)
        def _():
            second_copy(q, 1, 0).start()

    for q in range(2):
        pair_sum(q, 3)
    for q in range(2):
        first_copy(q, 0).wait_recv()
        for j in range(2):
            acc[q, 1, j] = acc[q, 1, j] + in1[q, 0, j]
        second_copy(q, 0, 0).start()
        first_copy(q, 1).wait_recv()
        for j in range(2):
            acc[q, 2, 2 + j] = acc[q, 2, 2 + j] + in1[q, 1, j]
        second_copy(q, 1, 1).start()

    def total(q, j):
        val = acc[q, 3, j].astype(jnp.float32) + in2[q, 0, j].astype(jnp.float32) + in2[q, 1, j].astype(jnp.float32)
        acc[q, 3, j] = val.astype(jnp.bfloat16)

    for h in (1, 0):
        pass
    for q in range(2):
        second_copy(q, 0, 1).wait_recv()
        second_copy(q, 1, 0).wait_recv()
    for q in range(2):
        second_copy(q, 0, 0).wait_recv()
        second_copy(q, 1, 1).wait_recv()
        total(q, 0)
        third_copy(q, 0).start()
        third_copy(q, 1).start()
        for j in (1, 2, 3):
            total(q, j)
    hrow = rows // 2
    for q in range(2):
        third_copy(q, 0).wait_recv()
        acc[q, 3, 1, pl.ds(0, hrow)] = acc[q, 3, 1, pl.ds(0, hrow)] + in3[q, 0]
        fourth_copy(q, 0).start()
        third_copy(q, 1).wait_recv()
        acc[q, 3, 2, pl.ds(hrow, hrow)] = acc[q, 3, 2, pl.ds(hrow, hrow)] + in3[q, 1]
        fourth_copy(q, 1).start()
    for q in range(2):
        fourth_copy(q, 0).wait_recv()
        fourth_copy(q, 1).wait_recv()
        cols = pl.ds(q * half, half)
        upd = acc[q, 3, 3].astype(jnp.float32) + in4[q, 0].astype(jnp.float32) + in4[q, 1].astype(jnp.float32)
        upd = upd.astype(jnp.bfloat16)
        out_ref[:, cols] = (hid_ref[:, cols].astype(jnp.float32) + upd.astype(jnp.float32)).astype(jnp.bfloat16)
    for q in range(2):
        for s in range(RING):
            die_copy(q, s).wait_send()
        for d in range(2):
            first_copy(q, d).wait_send()
            second_copy(q, d, 0).wait_send()
            second_copy(q, d, 1).wait_send()
            third_copy(q, d).wait_send()
            fourth_copy(q, d).wait_send()


def out_reduce_scatter(joined, w_out, hidden, layer):
    rows, d_model = hidden.shape
    depth = joined.shape[1]
    half = d_model // 2
    bf = jnp.bfloat16
    dma = pltpu.SemaphoreType.DMA
    return pl.pallas_call(
        rs_kernel,
        out_shape=jax.ShapeDtypeStruct((rows, d_model), bf),
        in_specs=[pl.BlockSpec(memory_space=pltpu.VMEM)] * 3,
        out_specs=pl.BlockSpec(memory_space=pltpu.VMEM),
        scratch_shapes=[
            pltpu.VMEM((2, RING, CORES, RING, rows, depth), bf),
            pltpu.VMEM((2, RING, RING, rows, half), bf),
            pltpu.VMEM((2, RING, RING, rows, half), bf),
            pltpu.VMEM((2, RING, RING, rows, half), bf),
            pltpu.VMEM((2, 2, 2, rows, half), bf),
            pltpu.VMEM((2, 2, RING, rows, half), bf),
            pltpu.VMEM((2, 2, rows // 2, half), bf),
            pltpu.VMEM((2, 2, rows, half), bf),
            dma((2, RING)), dma((2, RING)),
            dma((2, 2)), dma((2, 2)),
            dma((2, 2, 2)), dma((2, 2, 2)),
            dma((2, 2)), dma((2, 2)),
            dma((2, 2)), dma((2, 2)),
        ],
        compiler_params=pltpu.CompilerParams(collective_id=2 * layer + 1, has_side_effects=True, vmem_limit_bytes=VMEM_LIMIT),
        cost_estimate=pl.CostEstimate(flops=35_000_000_000, bytes_accessed=(joined.size + w_out.size) * 2, transcendentals=0),
        name=f"out_scatter_{layer}",
    )(joined.reshape(RING, RING, CORES, rows, depth), w_out, hidden)


def solution(mesh):
    row_size = mesh.shape["row"]
    n_col = mesh.shape["col"]
    n_z = row_size // RING
    n_y = RING
    n_x = n_col // CORES
    n_tp = n_y * n_col
    n_dev = row_size * n_col
    mesh4 = Mesh(mesh.devices.reshape(n_z, n_y, n_x, CORES), ("z", "y", "x", "core"))
    every = ("z", "y", "x", "core")
    tp = ("y", "x", "core")
    col = ("x", "core")
    act_spec = P(None, None, every)
    w_spec = P(None, ("z", "y"), col)

    def device_fn(x_loc, gain_loc, w_in_loc, w_kv_loc, w_out_loc):
        n_layers = w_in_loc.shape[0]
        n_batch, seq_len, d_local = x_loc.shape
        d_model = d_local * n_dev
        e_block = w_in_loc.shape[2]
        r_block = w_out_loc.shape[1]
        f_block = e_block - r_block
        q_block = r_block - f_block
        q_loc, f_loc = q_block // n_y, f_block // n_y
        head_dim = w_kv_loc.shape[2] * n_col // 2
        heads_local = q_loc // head_dim
        batch_loc = n_batch // n_z
        n_tok = n_batch * seq_len
        tok_z = n_tok // n_z
        tok_loc = n_tok // n_dev
        seq_local = seq_len // n_dev
        d_row = w_in_loc.shape[1]
        positions = jnp.arange(seq_len)
        cos_tab, sin_tab = rope_tables(positions, head_dim)
        causal = positions[None, :] <= positions[:, None]

        wkv = lax.all_gather(w_kv_loc, tp, axis=0, tiled=False)
        wkv = wkv.reshape(n_y, n_col, n_layers, d_row, -1).transpose(2, 0, 3, 1, 4).reshape(n_layers, n_y * d_row, 2 * head_dim)
        weights = []
        for l in range(n_layers):
            wi = w_in_loc[l]
            q_part = wi[:, :q_block].reshape(d_row, n_y, q_loc)
            g_part = wi[:, q_block:q_block + f_block].reshape(d_row, n_y, f_loc)
            u_part = wi[:, q_block + f_block:].reshape(d_row, n_y, f_loc)
            wi = jnp.concatenate([q_part, g_part, u_part], axis=2).transpose(1, 0, 2)
            wi = lax.all_to_all(wi, "y", 0, 0, tiled=True).reshape(n_y * d_row, q_loc + 2 * f_loc)
            wi = lax.all_gather(jnp.concatenate([wi, wkv[l]], axis=1), "z", axis=0, tiled=True)
            wo = w_out_loc[l]
            wo = jnp.concatenate([wo[:q_block].reshape(n_y, q_loc, -1), wo[q_block:].reshape(n_y, f_loc, -1)], axis=1)
            wo = lax.all_to_all(wo, "y", 0, 0, tiled=True)
            wo = wo.transpose(1, 0, 2).reshape(q_loc + f_loc, -1)
            wo = lax.all_gather(wo, "z", axis=1, tiled=True)
            weights.append((wi, wo))

        send = jnp.concatenate([
            x_loc.reshape(n_dev, tok_loc, d_local),
            jnp.broadcast_to(gain_loc[None], (n_dev, n_layers, d_local)),
        ], axis=1)
        got = lax.all_to_all(send, every, 0, 0, tiled=True)
        got = got.transpose(1, 0, 2).reshape(tok_loc + n_layers, d_model)
        hidden = got[:tok_loc]
        gain = got[tok_loc:]
        kv_outs = []
        for l in range(n_layers):
            w_i, w_o = weights[l]
            h = all_gather_norm(hidden, gain[l][None], l)
            proj = jnp.dot(h, w_i, preferred_element_type=jnp.float32).astype(jnp.bfloat16)
            query = proj[:, :q_loc].reshape(batch_loc, seq_len, heads_local, head_dim)
            gate_val = proj[:, q_loc:q_loc + f_loc]
            up_val = proj[:, q_loc + f_loc:q_loc + 2 * f_loc]
            kv_proj = proj[:, q_loc + 2 * f_loc:].reshape(batch_loc, seq_len, 2 * head_dim)
            q_rot = (apply_rope(query.astype(jnp.float32), cos_tab[:, None, :], sin_tab[:, None, :]) * head_dim ** -0.5).astype(jnp.bfloat16)
            k_rot = apply_rope(kv_proj[..., :head_dim].astype(jnp.float32), cos_tab, sin_tab).astype(jnp.bfloat16)
            v_val = kv_proj[..., head_dim:]
            scores = jnp.einsum("crie,cle->cirl", q_rot, k_rot, preferred_element_type=jnp.float32)
            scores = jnp.where(causal, scores, -1e30)
            attn_prob = jax.nn.softmax(scores, axis=-1).astype(jnp.bfloat16)
            attn_out = jnp.einsum("cirl,cle->crie", attn_prob, v_val, preferred_element_type=jnp.float32).astype(jnp.bfloat16).reshape(tok_z, q_loc)
            mlp_out = (jax.nn.silu(gate_val.astype(jnp.float32)) * up_val.astype(jnp.float32)).astype(jnp.bfloat16)
            joined = jnp.concatenate([attn_out, mlp_out], axis=1)
            hidden = out_reduce_scatter(joined, w_o, hidden, l)
            kv_outs.append(jnp.stack([k_rot, v_val]))

        y_parts = hidden.reshape(tok_loc, n_dev, d_local).transpose(1, 0, 2)
        y_loc = lax.all_to_all(y_parts, every, 0, 0, tiled=True).reshape(n_batch, seq_len, d_local)
        kv = jnp.stack(kv_outs).reshape(n_layers, 2, batch_loc, n_z, n_tp, seq_local, head_dim)
        me = (lax.axis_index("y") * n_x + lax.axis_index("x")) * CORES + lax.axis_index("core")
        kv = lax.dynamic_index_in_dim(kv, me, axis=4, keepdims=False)
        kv = lax.all_to_all(kv, "z", 3, 2, tiled=True)
        kv = kv.reshape(n_layers, 2, n_batch, seq_local, head_dim)
        return y_loc, kv

    return jax.shard_map(device_fn, mesh=mesh4, in_specs=(act_spec, P(None, every), w_spec, w_spec, P(None, col, ("z", "y"))), out_specs=(act_spec, P(None, None, None, every, None)), check_vma=False)
```

```python
import jax
import jax.numpy as jnp
from jax import lax
from jax.experimental import pallas as pl
from jax.experimental.pallas import tpu as pltpu
from jax.sharding import Mesh
from jax.sharding import PartitionSpec as P

LN_EPS = 1e-6
RING = 4
CORES = 2
VMEM_LIMIT = 67_000_000
BF = jnp.bfloat16
F32 = jnp.float32
SLOT_OFF = (2, 1, 3, 0)
SIGN = (1, -1)
NAMES = (
    "hid_in", "gain", "wkv", "w_in", "w_out", "cos", "sin", "hid_out", "kv_out", "h_all", "wi", "wo", "kvh", "h_ref",
    "wv", "kvb", "wov", "hb", "joined", "qkv", "stage", "lhs", "away", "acc", "die_in", "in1", "in2", "in3", "in4",
    "ag_send", "ag_recv", "ag_dsend", "ag_drecv", "ag_loc", "h_sem", "kvo_sem", "w_load", "y_recv", "zb_recv",
    "zc_recv", "w_send", "kz_send", "kz_recv", "ky_send", "ky_recv", "kx_send", "kx_recv", "kd_send", "kd_recv",
    "k_loc", "dsend", "drecv", "send1", "recv1", "send2", "recv2", "send3", "recv3", "send4", "recv4",
)


class Refs:
    def __init__(self, refs):
        for name, ref in zip(NAMES, refs, strict=True):
            setattr(self, name, ref)


def model_kernel(*refs):
    r = Refs(refs)
    z, y, x, c = (lax.axis_index(a) for a in ("z", "y", "x", "core"))
    n_layers = r.gain.shape[0]
    rows, d_model = r.hid_in.shape
    seq_len, head_dim = r.cos.shape
    d_row = r.w_in.shape[1]
    e_loc = r.wi.shape[3]
    depth = r.wo.shape[3]
    f_loc = depth - head_dim
    quarter = rows // 4
    half = d_model // 2
    q_block = head_dim * RING
    f_block = f_loc * RING

    def turn(base, off):
        return lax.rem(base + off + RING, RING)

    def remote(src, dst, ssem, rsem, dev):
        return pltpu.make_async_remote_copy(
            src_ref=src, dst_ref=dst, send_sem=ssem, recv_sem=rsem, device_id=dev, device_id_type=pl.DeviceIdType.MESH)

    partner = (z, y, x, 1 - c)

    peers = [(turn(z, o), y, x, c) for o in (1, 2, 3)]
    peers += [(z, turn(y, o), x, c) for o in (1, 2, 3)]
    peers += [(z, y, turn(x, o), c) for o in (1, 2, 3)]
    peers.append(partner)
    gate_sem = pltpu.get_barrier_semaphore()
    for dev in peers:
        pl.semaphore_signal(gate_sem, inc=1, device_id=dev, device_id_type=pl.DeviceIdType.MESH)
    pl.semaphore_wait(gate_sem, len(peers))

    def hook(pump, i):
        with jax.named_scope(f"hook_{i}"):
            pump(i)

    def w_cols(kind):
        return pl.ds(0, head_dim + f_loc) if kind == 0 else pl.ds(head_dim + f_loc, f_loc)

    def piece(t, zz, yy):
        l, kind = t // 3, t % 3
        if kind == 2:
            return r.wo.at[l, zz, yy]
        return r.wi.at[l, zz, pl.ds(pl.multiple_of(yy * d_row, d_row), d_row), w_cols(kind)]

    def piece_half(t, zz, yy, h):
        l, kind = t // 3, t % 3
        if kind == 2:
            return r.wo.at[l, zz, yy, pl.ds(h * (depth // 2), depth // 2)]
        return r.wi.at[l, zz, pl.ds(pl.multiple_of(yy * d_row + h * (d_row // 2), d_row // 2), d_row // 2), w_cols(kind)]

    def own_parts(t, owner, zz, yy):
        l, kind = t // 3, t % 3
        hq = pl.ds(pl.multiple_of(owner * head_dim, head_dim), head_dim)
        if kind == 2:
            return [
                (r.w_out.at[l, hq], r.wo.at[l, zz, yy, pl.ds(0, head_dim)]),
                (r.w_out.at[l, pl.ds(pl.multiple_of(q_block + owner * f_loc, head_dim), f_loc)], r.wo.at[l, zz, yy, pl.ds(head_dim, f_loc)]),
            ]
        rws = pl.ds(pl.multiple_of(yy * d_row, d_row), d_row)
        if kind == 0:
            return [
                (r.w_in.at[l, :, hq], r.wi.at[l, zz, rws, pl.ds(0, head_dim)]),
                (r.w_in.at[l, :, pl.ds(pl.multiple_of(q_block + owner * f_loc, head_dim), f_loc)], r.wi.at[l, zz, rws, pl.ds(head_dim, f_loc)]),
            ]
        return [(r.w_in.at[l, :, pl.ds(pl.multiple_of(q_block + f_block + owner * f_loc, head_dim), f_loc)],
                 r.wi.at[l, zz, rws, pl.ds(head_dim + f_loc, f_loc)])]

    def y_send(t):
        for dy in (1, 3, 2):
            owner = turn(y, dy)
            for src, dst in own_parts(t, owner, z, y):
                remote(src, dst, r.w_send.at[t, 0], r.y_recv.at[t, (RING - dy) % RING], (z, owner, x, c)).start()

    def z_own(t):
        for d in range(2):
            for src, dst in own_parts(t, y, z, y):
                remote(src, dst, r.w_send.at[t, 1], r.zb_recv.at[t, 0, d], (turn(z, SIGN[d]), y, x, c)).start()

    def z_direct(t, j):
        yy = turn(y, j)
        ref = piece(t, z, yy)
        remote(ref, ref, r.w_send.at[t, 0], r.y_recv.at[t, j], (z, y, x, c)).wait_recv()
        for d in range(2):
            remote(ref, ref, r.w_send.at[t, 1], r.zb_recv.at[t, j, d], (turn(z, SIGN[d]), y, x, c)).start()

    def z_forward(t, j):
        yy = turn(y, j)
        for d in range(2):
            zz = turn(z, -SIGN[d])
            ref = piece(t, zz, yy)
            remote(ref, ref, r.w_send.at[t, 1], r.zb_recv.at[t, j, d], (z, y, x, c)).wait_recv()
            part = piece_half(t, zz, yy, d)
            remote(part, part, r.w_send.at[t, 2], r.zc_recv.at[t, j, d], (turn(z, SIGN[d]), y, x, c)).start()

    def place(t, zz):
        l, kind = t // 3, t % 3
        if kind == 2:
            return r.wo.at[l, zz], r.wov.at[zz]
        return r.wi.at[l, zz, :, w_cols(kind)], r.wv.at[zz, :, w_cols(kind)]

    def load_near(t):
        l, kind = t // 3, t % 3
        for d in range(2):
            src, dst = place(t, turn(z, SIGN[d]))
            pltpu.make_async_copy(src, dst, r.w_load.at[kind]).start()
        for j in (1, 2, 3):
            yy = turn(y, j)
            dst = r.wov.at[z, yy] if kind == 2 else r.wv.at[z, pl.ds(pl.multiple_of(yy * d_row, d_row), d_row), w_cols(kind)]
            pltpu.make_async_copy(piece(t, z, yy), dst, r.w_load.at[kind]).start()
        for src, dst in own_parts(t, y, z, y):
            if kind == 2:
                pass
            pltpu.make_async_copy(src, own_place(t, dst, src), r.w_load.at[kind]).start()

    def own_place(t, dst, src):
        kind = t % 3
        if kind == 2:
            n = src.shape[0]
            return r.wov.at[z, y, pl.ds(0 if n == head_dim and f_loc != head_dim else head_dim, n)]
        n = src.shape[1]
        rws = pl.ds(pl.multiple_of(y * d_row, d_row), d_row)
        if kind == 0:
            return r.wv.at[z, rws, pl.ds(0 if n == head_dim and f_loc != head_dim else head_dim, n)]
        return r.wv.at[z, rws, pl.ds(head_dim + f_loc, f_loc)]

    def finish(t):
        l, kind = t // 3, t % 3
        far = turn(z, 2)
        for j in range(RING):
            for d in range(2):
                part = piece_half(t, far, turn(y, j), d)
                remote(part, part, r.w_send.at[t, 2], r.zc_recv.at[t, j, d], (z, y, x, c)).wait_recv()
        load_near(t)
        src, dst = place(t, far)
        pltpu.make_async_copy(src, dst, r.w_load.at[kind]).start()

    def loaded(t):
        kind = t % 3
        dst = r.wov if kind == 2 else r.wv.at[:, :, w_cols(kind)]
        pltpu.make_async_copy(dst, dst, r.w_load.at[kind]).wait()

    def drain(t):
        l, kind = t // 3, t % 3
        if kind == 2:
            refs3 = (r.wo.at[l, 0, pl.ds(0, 3)], r.wo.at[l, pl.ds(0, 2)], r.wo.at[l, 0])
        else:
            cols = w_cols(kind)
            refs3 = (r.wi.at[l, 0, pl.ds(0, 3 * d_row), cols], r.wi.at[l, pl.ds(0, 2), :, cols], r.wi.at[l, 0, :, cols])
        for g in range(3):
            remote(refs3[g], refs3[g], r.w_send.at[t, g], r.y_recv.at[t, 0], (z, y, x, c)).wait_send()

    def kv_z():
        for i, o in enumerate((1, 3, 2)):
            remote(r.wkv, r.kvh.at[x, c, :, y, z], r.kz_send.at[i], r.kz_recv.at[i], (turn(z, o), y, x, c)).start()
        pltpu.make_async_copy(r.wkv, r.kvh.at[x, c, :, y, z], r.k_loc.at[0]).start()

    def kv_y():
        pltpu.make_async_copy(r.wkv, r.kvh.at[x, c, :, y, z], r.k_loc.at[0]).wait()
        for i, o in enumerate((1, 3, 2)):
            zz = turn(z, -o)
            remote(r.wkv, r.kvh.at[x, c, :, y, zz], r.kz_send.at[i], r.kz_recv.at[i], (turn(z, o), y, x, c)).wait()
        ref = r.kvh.at[x, c, :, y]
        for i, o in enumerate((1, 3, 2)):
            remote(ref, ref, r.ky_send.at[i], r.ky_recv.at[i], (z, turn(y, o), x, c)).start()

    def kv_x():
        for i, o in enumerate((1, 3, 2)):
            ref = r.kvh.at[x, c, :, turn(y, -o)]
            remote(ref, ref, r.ky_send.at[i], r.ky_recv.at[i], (z, turn(y, o), x, c)).wait()
        for l in range(n_layers):
            ref = r.kvh.at[x, c, l]
            for i, o in enumerate((1, 3, 2)):
                remote(ref, ref, r.kx_send.at[l, i], r.kx_recv.at[l, i], (z, y, turn(x, o), c)).start()
            remote(ref, ref, r.kd_send.at[l, 3], r.kd_recv.at[l, 3], partner).start()

    def kv_die(l):
        for i, o in enumerate((1, 3, 2)):
            ref = r.kvh.at[turn(x, -o), c, l]
            remote(ref, ref, r.kx_send.at[l, i], r.kx_recv.at[l, i], (z, y, turn(x, o), c)).wait()
            remote(ref, ref, r.kd_send.at[l, i], r.kd_recv.at[l, i], partner).start()

    def kv_load(l):
        for i, o in enumerate((1, 3, 2, 0)):
            ref = r.kvh.at[turn(x, -o), 1 - c, l]
            remote(ref, ref, r.kd_send.at[l, i], r.kd_recv.at[l, i], partner).wait()
        kc = r.wkv.shape[1]
        for xx in range(RING):
            for cc in range(CORES):
                pltpu.make_async_copy(r.kvh.at[xx, cc, l], r.kvb.at[:, :, pl.ds((xx * CORES + cc) * kc, kc)], r.k_loc.at[1]).start()

    def kv_loaded():
        pltpu.make_async_copy(r.kvb, r.kvb, r.k_loc.at[1]).wait()

    def gather_norm(l, pump):
        hid = r.hid_in if l == 0 else r.hid_out
        gain = r.gain[l:l + 1, :].astype(F32)
        for b in range(4):
            blk = hid[b * quarter:(b + 1) * quarter, :].astype(F32)
            mean = jnp.mean(blk, axis=-1, keepdims=True)
            cen = blk - mean
            var = jnp.mean(cen * cen, axis=-1, keepdims=True)
            r.h_ref[b * quarter:(b + 1) * quarter, :] = (cen * lax.rsqrt(var + LN_EPS) * gain).astype(BF)
        out = r.h_all.at[l]

        def spot(q, first, second):
            if q == 0:
                return turn(y, second), turn(x, first)
            return turn(y, first), turn(x, second)

        def span(q, part):
            if part is None:
                return pl.ds(q * 2 * quarter, 2 * quarter)
            return pl.ds((q * 2 + part) * quarter, quarter)

        copies = {}

        def ici(idx, grp, q, first, second, part, to_first, to_second, own=False):
            sy, sx = spot(q, first, second)
            ty, tx = spot(q, to_first, to_second)
            rws = span(q, part)
            dst = out.at[sy, sx, c, rws]
            cp = remote(r.h_ref.at[rws] if own else dst, dst, r.ag_send.at[l, grp], r.ag_recv.at[l, idx], (z, ty, tx, c))
            cp.start()
            copies[idx] = cp

        def die(q, first, second, own=False):
            sy, sx = spot(q, first, second)
            rws = span(q, None)
            dst = out.at[sy, sx, c, rws]
            off = (second if q == 0 else first) % RING
            remote(r.h_ref.at[rws] if own else dst, dst, r.ag_dsend.at[l], r.ag_drecv.at[l, off], partner).start()

        def p1(q, d):
            return q * 20 + d

        def p1f(q, d):
            return q * 20 + 2 + d

        def p2(q, k, d):
            return q * 20 + 4 + k * 4 + d

        def p2f(q, k, d):
            return q * 20 + 4 + k * 4 + 2 + d

        offs = (0, -1, 1, 2)
        for q in range(2):
            for d in range(2):
                ici(p1(q, d), 0, q, 0, 0, None, SIGN[d], 0, own=True)
        for q in range(2):
            for d in range(2):
                ici(p2(q, 0, d), 1, q, 0, 0, None, 0, SIGN[d], own=True)
        for q in range(2):
            die(q, 0, 0, own=True)
        own = pltpu.make_async_copy(r.h_ref, out.at[y, x, c], r.ag_loc)
        own.start()
        hook(pump, 0)
        for d in range(2):
            for q in range(2):
                copies[p1(q, d)].wait_recv()
                src = -SIGN[d]
                ici(p1f(q, d), 2, q, src, 0, d, SIGN[d], 0)
                for e in range(2):
                    ici(p2(q, 1 + d, e), 1, q, src, 0, None, 0, SIGN[e])
                die(q, src, 0)
        hook(pump, 1)
        for d in range(2):
            for q in range(2):
                copies[p2(q, 0, d)].wait_recv()
                src = -SIGN[d]
                ici(p2f(q, 0, d), 3, q, 0, src, d, 0, SIGN[d])
                die(q, 0, src)
        hook(pump, 2)
        for q in range(2):
            copies[p1f(q, 0)].wait_recv()
            copies[p1f(q, 1)].wait_recv()
            for e in range(2):
                ici(p2(q, 3, e), 1, q, 2, 0, None, 0, SIGN[e])
            die(q, 2, 0)
        hook(pump, 3)
        for k in (1, 2, 3):
            for d in range(2):
                for q in range(2):
                    copies[p2(q, k, d)].wait_recv()
                    src = -SIGN[d]
                    ici(p2f(q, k, d), 3, q, offs[k], src, d, 0, SIGN[d])
                    die(q, offs[k], src)
            hook(pump, 3 + k)
        for k in range(4):
            for q in range(2):
                copies[p2f(q, k, 0)].wait_recv()
                copies[p2f(q, k, 1)].wait_recv()
                die(q, offs[k], 2)
        hook(pump, 7)
        for off in range(RING):
            got = out.at[turn(y, off), :, 1 - c]
            remote(got, got, r.ag_dsend.at[l], r.ag_drecv.at[l, off], partner).wait_recv()
        sent = (out.at[0, 0], out.at[0], out.at[0, 0, 0], out.at[0, pl.ds(0, 2)])
        for grp in range(4):
            remote(sent[grp], sent[grp], r.ag_send.at[l, grp], r.ag_recv.at[l, 0], partner).wait_send()
        remote(out.at[pl.ds(0, 2)], out.at[pl.ds(0, 2)], r.ag_dsend.at[l], r.ag_drecv.at[l, 0], partner).wait_send()
        own.wait()

    def h_copy(l, s, slot):
        return pltpu.make_async_copy(r.h_all.at[l, s], r.hb.at[slot], r.h_sem.at[slot])

    def h_tile(slot):
        return r.hb[slot].reshape(seq_len, d_model)

    def project(h, lo, n):
        w = r.wv[:, :, lo:lo + n].reshape(d_model, n)
        return jnp.dot(h, w, preferred_element_type=F32).astype(BF)

    def rope(val):
        val = val.astype(F32)
        return val * r.cos[...] + pltpu.roll(val, head_dim // 2, 1) * r.sin[...]

    n_chunk = min(256, f_loc)

    def kv_out_copy(l, s, slot, i):
        return pltpu.make_async_copy(r.qkv.at[slot, i], r.kv_out.at[l, i, s], r.kvo_sem.at[slot, i])

    def pass_one(l, pump):
        h_copy(l, 0, 0).start()

        @pl.loop(0, RING)
        def _(s):
            slot = lax.rem(s, 2)
            h_copy(l, s, slot).wait()

            @pl.when(s + 1 < RING)
            def _():
                h_copy(l, s + 1, 1 - slot).start()

            pump(s)

            @pl.when(s >= 2)
            def _():
                for i in range(2):
                    kv_out_copy(l, s - 2, slot, i).wait()

            kv = jnp.zeros((seq_len, 2 * head_dim), F32)
            for zz in range(RING):
                for yy in range(RING):
                    col = (zz * RING + yy) * d_row
                    kv += lax.dot_general(h_cols(slot, col, d_row), r.kvb[yy, zz], (((1,), (1,)), ((), ())), preferred_element_type=F32)
            kv = kv.astype(BF)
            r.qkv[slot, 0] = rope(kv[:, :head_dim]).astype(BF)
            r.qkv[slot, 1] = kv[:, head_dim:]
            for i in range(2):
                kv_out_copy(l, s, slot, i).start()
            q = project(h_tile(slot), 0, head_dim)
            r.stage[...] = (rope(q) * head_dim ** -0.5).astype(BF)
            for lo in range(0, f_loc, n_chunk):
                r.joined[s, :, head_dim + lo:head_dim + lo + n_chunk] = project(h_tile(slot), head_dim + lo, n_chunk)
            n_tile = seq_len // 2
            for i in range(2):
                keys = (i + 1) * n_tile
                sc = lax.dot_general(r.stage[i * n_tile:(i + 1) * n_tile, :], r.qkv[slot, 0, :keys, :], (((1,), (1,)), ((), ())), preferred_element_type=F32)
                row_id = lax.broadcasted_iota(jnp.int32, sc.shape, 0) + i * n_tile
                col_id = lax.broadcasted_iota(jnp.int32, sc.shape, 1)
                sc = jnp.where(col_id <= row_id, sc, -1e30)
                top = jnp.max(sc, axis=-1, keepdims=True)
                ex = jnp.exp(sc - top)
                prob = (ex * (1.0 / jnp.sum(ex, axis=-1, keepdims=True))).astype(BF)
                att = jnp.dot(prob, r.qkv[slot, 1, :keys, :], preferred_element_type=F32)
                r.joined[s, i * n_tile:(i + 1) * n_tile, :head_dim] = att.astype(BF)

        for s in (RING - 2, RING - 1):
            for i in range(2):
                kv_out_copy(l, s, s % 2, i).wait()

    def h_cols(slot, col, n):
        return r.hb[slot, :, :, :, col:col + n].reshape(seq_len, n)

    def pass_two(l, pump):
        h_copy(l, 0, 0).start()

        @pl.loop(0, RING)
        def _(s):
            slot = lax.rem(s, 2)
            h_copy(l, s, slot).wait()

            @pl.when(s + 1 < RING)
            def _():
                h_copy(l, s + 1, 1 - slot).start()

            pump(s)
            for lo in range(0, f_loc, n_chunk):
                up = project(h_tile(slot), head_dim + f_loc + lo, n_chunk).astype(F32)
                cols = slice(head_dim + lo, head_dim + lo + n_chunk)
                g = r.joined[s, :, cols].astype(F32)
                r.joined[s, :, cols] = (g * jax.nn.sigmoid(g) * up).astype(BF)

    def out_scatter(l, pump):
        hid = r.hid_in if l == 0 else r.hid_out

        def peer(q, first, second):
            dy = first * (1 - q) + second * q
            dx = first * q + second * (1 - q)
            return (z, turn(y, dy), turn(x, dx), c)

        def die_copy(q, s):
            return remote(r.away.at[q], r.die_in.at[q, s], r.dsend.at[l, q, s], r.drecv.at[l, q, s], partner)

        def first_copy(q, d):
            return remote(r.acc.at[q, 0, pl.ds(2 * d, 2)], r.in1.at[q, d], r.send1.at[l, q, d], r.recv1.at[l, q, d], peer(q, 1 - 2 * d, 0))

        def second_copy(q, d, h):
            return remote(r.acc.at[q, 1 + d, pl.ds(2 * h, 2)], r.in2.at[q, d, pl.ds(2 * h, 2)], r.send2.at[l, q, d, h], r.recv2.at[l, q, d, h], peer(q, 1 - 2 * d, 0))

        def third_copy(q, d):
            rws = pl.ds(d * (rows // 2), rows // 2)
            return remote(r.acc.at[q, 3, 0, rws], r.in3.at[q, d], r.send3.at[l, q, d], r.recv3.at[l, q, d], peer(q, 0, 1 - 2 * d))

        def fourth_copy(q, d):
            return remote(r.acc.at[q, 3, 1 + d], r.in4.at[q, d], r.send4.at[l, q, d], r.recv4.at[l, q, d], peer(q, 0, 1 - 2 * d))

        n_blk = r.wov.shape[3]
        blk_z = RING // 2

        def tile(q, s):
            for cc in range(CORES):
                for j in range(RING):
                    oy = SLOT_OFF[s] * (1 - q) + SLOT_OFF[j] * q
                    ox = SLOT_OFF[j] * (1 - q) + SLOT_OFF[s] * q
                    core = (1 - c) if cc == 0 else c
                    at = pl.multiple_of((turn(x, ox) * CORES + core) * rows, rows)
                    r.lhs[pl.ds((cc * RING + j) * rows, rows), :] = r.joined[turn(y, oy), pl.ds(at, rows), :]
            left = r.lhs[...]

            @pl.loop(0, half // n_blk)
            def _(n):
                col = pl.multiple_of(n * n_blk, n_blk)
                w = r.wov[q * blk_z + n // RING, lax.rem(n, RING)]
                res = jnp.dot(left, w, preferred_element_type=F32).astype(BF)
                res = res.reshape(CORES, RING, rows, n_blk)
                r.away[q, :, :, pl.ds(col, n_blk)] = res[0]
                r.acc[q, s, :, :, pl.ds(col, n_blk)] = res[1]

        def pair_sum(q, s):
            die_copy(q, s).wait_recv()

            @pl.loop(0, RING)
            def _(j):
                r.acc[q, s, j] = r.acc[q, s, j] + r.die_in[q, s, j]

        for s in range(RING):
            @pl.loop(0, 2)
            def _(q, s=s):
                if s > 0:
                    die_copy(q, s - 1).wait_send()
                tile(q, s)
                die_copy(q, s).start()
                if s > 0:
                    pair_sum(q, s - 1)
                if s == 1:
                    first_copy(q, 0).start()
                    first_copy(q, 1).start()
                if s == 2:
                    second_copy(q, 0, 1).start()
                if s == 3:
                    second_copy(q, 1, 0).start()
            pump(s)

        for q in range(2):
            pair_sum(q, 3)
        for q in range(2):
            first_copy(q, 0).wait_recv()
            for j in range(2):
                r.acc[q, 1, j] = r.acc[q, 1, j] + r.in1[q, 0, j]
            second_copy(q, 0, 0).start()
            first_copy(q, 1).wait_recv()
            for j in range(2):
                r.acc[q, 2, 2 + j] = r.acc[q, 2, 2 + j] + r.in1[q, 1, j]
            second_copy(q, 1, 1).start()
        hook(pump, 4)

        def total(q, j):
            val = r.acc[q, 3, j].astype(F32) + r.in2[q, 0, j].astype(F32) + r.in2[q, 1, j].astype(F32)
            r.acc[q, 3, j] = val.astype(BF)

        for q in range(2):
            second_copy(q, 0, 1).wait_recv()
            second_copy(q, 1, 0).wait_recv()
        hook(pump, 5)
        for q in range(2):
            second_copy(q, 0, 0).wait_recv()
            second_copy(q, 1, 1).wait_recv()
            total(q, 0)
            third_copy(q, 0).start()
            third_copy(q, 1).start()
            for j in (1, 2, 3):
                total(q, j)
        hrow = rows // 2
        for q in range(2):
            third_copy(q, 0).wait_recv()
            r.acc[q, 3, 1, pl.ds(0, hrow)] = r.acc[q, 3, 1, pl.ds(0, hrow)] + r.in3[q, 0]
            fourth_copy(q, 0).start()
            third_copy(q, 1).wait_recv()
            r.acc[q, 3, 2, pl.ds(hrow, hrow)] = r.acc[q, 3, 2, pl.ds(hrow, hrow)] + r.in3[q, 1]
            fourth_copy(q, 1).start()
        hook(pump, 6)
        for q in range(2):
            fourth_copy(q, 0).wait_recv()
            fourth_copy(q, 1).wait_recv()
            cols = pl.ds(q * half, half)
            upd = r.acc[q, 3, 3].astype(F32) + r.in4[q, 0].astype(F32) + r.in4[q, 1].astype(F32)
            upd = upd.astype(BF)
            r.hid_out[:, cols] = (hid[:, cols].astype(F32) + upd.astype(F32)).astype(BF)
        for q in range(2):
            die_copy(q, 3).wait_send()
            for d in range(2):
                first_copy(q, d).wait_send()
                second_copy(q, d, 0).wait_send()
                second_copy(q, d, 1).wait_send()
                third_copy(q, d).wait_send()
                fourth_copy(q, d).wait_send()

    def z_all(t):
        for j in (1, 2, 3):
            z_direct(t, j)

    def f_all(t):
        for j in range(RING):
            z_forward(t, j)

    def when_j(s, fn):
        @pl.when(s < 3)
        def _():
            fn(s + 1)

    with jax.named_scope("start"):
        kv_z()
        y_send(0)
        z_own(0)

    def ag0(i):
        if i == 0:
            y_send(1)
        if i == 1:
            kv_y()
            z_direct(0, 3)
            z_direct(0, 1)
        if i == 2:
            z_direct(0, 2)
            z_own(1)
        if i == 3:
            z_forward(0, 0)
            kv_x()
        if i == 4:
            z_forward(0, 3)
            z_forward(0, 1)
            z_direct(1, 3)
            z_direct(1, 1)
        if i == 5:
            z_forward(0, 2)
            z_direct(1, 2)
        if i == 6:
            y_send(2)
            z_forward(1, 0)
            kv_die(0)
        if i == 7:
            finish(0)
            kv_load(0)
            z_forward(1, 3)
            z_own(2)

    with jax.named_scope("gather_0"):
        gather_norm(0, ag0)
    with jax.named_scope("wait_w0"):
        loaded(0)
        kv_loaded()
    with jax.named_scope("fwd_1"):
        z_forward(1, 1)
        z_forward(1, 2)
        y_send(3)
    with jax.named_scope("pass_one_0"):
        pass_one(0, lambda s: when_j(s, lambda j: z_direct(2, j)))
    with jax.named_scope("finish_1"):
        finish(1)
        z_own(3)
        y_send(4)
        loaded(1)
    with jax.named_scope("pass_two_0"):
        pass_two(0, lambda s: z_forward(2, s))
    with jax.named_scope("finish_2"):
        finish(2)
        z_all(3)
        loaded(2)

    def rs0(i):
        if i == 0:
            z_forward(3, 0)
            z_forward(3, 1)
        if i == 1:
            z_forward(3, 2)
            z_forward(3, 3)
        if i == 2:
            y_send(5)
            z_own(4)
            z_direct(4, 3)
            z_direct(4, 1)
            z_direct(4, 2)
        if i == 4:
            finish(3)
            z_forward(4, 0)
            kv_die(1)
        if i == 5:
            z_forward(4, 1)
            kv_load(1)
        if i == 6:
            z_forward(4, 2)
            z_forward(4, 3)

    with jax.named_scope("scatter_0"):
        out_scatter(0, rs0)

    def ag1(i):
        if i == 1:
            z_own(5)
            z_direct(5, 3)
            z_direct(5, 1)
            z_direct(5, 2)
        if i == 4:
            finish(4)
        if i == 5:
            z_forward(5, 0)
            z_forward(5, 1)
        if i == 6:
            z_forward(5, 2)
            z_forward(5, 3)

    with jax.named_scope("gather_1"):
        gather_norm(1, ag1)
    with jax.named_scope("wait_w3"):
        loaded(3)
        kv_loaded()
    with jax.named_scope("pass_one_1"):
        pass_one(1, lambda s: None)
    with jax.named_scope("finish_5"):
        loaded(4)
        finish(5)
    with jax.named_scope("pass_two_1"):
        pass_two(1, lambda s: None)
    with jax.named_scope("wait_w5"):
        loaded(5)
    with jax.named_scope("scatter_1"):
        out_scatter(1, lambda i: None)
    with jax.named_scope("drain"):
        for t in range(3 * n_layers):
            drain(t)


def run_model(hidden, gain, wkv_t, w_in, w_out, cos_full, sin_full, seqs):
    rows, d_model = hidden.shape
    n_layers, d_row, e_block = w_in.shape
    r_block, d_col = w_out.shape[1:]
    seq_len, head_dim = cos_full.shape
    e_loc, r_loc = e_block // RING, r_block // RING
    kc = wkv_t.shape[1]
    half = d_model // 2
    dma = pltpu.SemaphoreType.DMA
    any_spec = pl.BlockSpec(memory_space=pl.ANY)
    vm_spec = pl.BlockSpec(memory_space=pltpu.VMEM)
    n_t = 3 * n_layers
    out_shape = [
        jax.ShapeDtypeStruct((rows, d_model), BF),
        jax.ShapeDtypeStruct((n_layers, 2, seqs, seq_len, head_dim), BF),
        jax.ShapeDtypeStruct((n_layers, RING, RING, CORES, rows, d_model), BF),
        jax.ShapeDtypeStruct((n_layers, RING, RING * d_row, e_loc), BF),
        jax.ShapeDtypeStruct((n_layers, RING, RING, r_loc, d_col), BF),
        jax.ShapeDtypeStruct((RING, CORES, n_layers, RING, RING, kc, d_row), BF),
    ]
    scratch = [
        pltpu.VMEM((rows, d_model), BF),
        pltpu.VMEM((RING, RING * d_row, e_loc), BF),
        pltpu.VMEM((RING, RING, 2 * head_dim, d_row), BF),
        pltpu.VMEM((RING, RING, r_loc, d_col), BF),
        pltpu.VMEM((2, RING, CORES, rows, d_model), BF),
        pltpu.VMEM((RING, seq_len, r_loc), BF),
        pltpu.VMEM((2, 2, seq_len, head_dim), BF),
        pltpu.VMEM((seq_len, head_dim), BF),
        pltpu.VMEM((CORES * RING * rows, r_loc), BF),
        pltpu.VMEM((2, RING, rows, half), BF),
        pltpu.VMEM((2, RING, RING, rows, half), BF),
        pltpu.VMEM((2, RING, RING, rows, half), BF),
        pltpu.VMEM((2, 2, 2, rows, half), BF),
        pltpu.VMEM((2, 2, RING, rows, half), BF),
        pltpu.VMEM((2, 2, rows // 2, half), BF),
        pltpu.VMEM((2, 2, rows, half), BF),
        dma((n_layers, 4)), dma((n_layers, 40)), dma((n_layers,)), dma((n_layers, RING)), dma, dma((2,)), dma((2, 2)), dma((3,)),
        dma((n_t, RING)), dma((n_t, RING, 2)), dma((n_t, RING, 2)), dma((n_t, 3)),
        dma((3,)), dma((3,)), dma((3,)), dma((3,)), dma((n_layers, 3)), dma((n_layers, 3)), dma((n_layers, 4)), dma((n_layers, 4)), dma((2,)),
        dma((n_layers, 2, RING)), dma((n_layers, 2, RING)),
        dma((n_layers, 2, 2)), dma((n_layers, 2, 2)),
        dma((n_layers, 2, 2, 2)), dma((n_layers, 2, 2, 2)),
        dma((n_layers, 2, 2)), dma((n_layers, 2, 2)),
        dma((n_layers, 2, 2)), dma((n_layers, 2, 2)),
    ]
    out = pl.pallas_call(
        model_kernel,
        out_shape=out_shape,
        in_specs=[vm_spec, vm_spec, vm_spec, any_spec, any_spec, vm_spec, vm_spec],
        out_specs=[vm_spec] + [any_spec] * 5,
        scratch_shapes=scratch,
        compiler_params=pltpu.CompilerParams(collective_id=0, has_side_effects=True, vmem_limit_bytes=VMEM_LIMIT),
        name="two_layers",
    )(hidden, gain, wkv_t, w_in, w_out, cos_full, sin_full)
    return out[0], out[1]


def solution(mesh):
    row_size = mesh.shape["row"]
    n_col = mesh.shape["col"]
    n_z = row_size // RING
    n_y = RING
    n_x = n_col // CORES
    n_tp = n_y * n_col
    n_dev = row_size * n_col
    mesh4 = Mesh(mesh.devices.reshape(n_z, n_y, n_x, CORES), ("z", "y", "x", "core"))
    every = ("z", "y", "x", "core")
    col = ("x", "core")
    act_spec = P(None, None, every)
    w_spec = P(None, ("z", "y"), col)

    def device_fn(x_loc, gain_loc, w_in_loc, w_kv_loc, w_out_loc):
        n_layers = w_in_loc.shape[0]
        n_batch, seq_len, d_local = x_loc.shape
        d_model = d_local * n_dev
        head_dim = w_kv_loc.shape[2] * n_col // 2
        batch_loc = n_batch // n_z
        tok_loc = n_batch * seq_len // n_dev
        seq_local = seq_len // n_dev
        inv_freq = 1.0 / (10000.0 ** (jnp.arange(head_dim // 2, dtype=F32) * 2.0 / head_dim))
        angles = jnp.arange(seq_len).astype(F32)[:, None] * inv_freq[None, :]
        cos_tab, sin_tab = jnp.cos(angles), jnp.sin(angles)
        cos_full = jnp.concatenate([cos_tab, cos_tab], axis=1)
        sin_full = jnp.concatenate([-sin_tab, sin_tab], axis=1)

        send = jnp.concatenate([
            x_loc.reshape(n_dev, tok_loc, d_local),
            jnp.broadcast_to(gain_loc[None], (n_dev, n_layers, d_local)),
        ], axis=1)
        got = lax.all_to_all(send, every, 0, 0, tiled=True)
        got = got.transpose(1, 0, 2).reshape(tok_loc + n_layers, d_model)
        hidden, kv = run_model(got[:tok_loc], got[tok_loc:], w_kv_loc.transpose(0, 2, 1), w_in_loc, w_out_loc, cos_full, sin_full, batch_loc)

        y_parts = hidden.reshape(tok_loc, n_dev, d_local).transpose(1, 0, 2)
        y_loc = lax.all_to_all(y_parts, every, 0, 0, tiled=True).reshape(n_batch, seq_len, d_local)
        kv = kv.reshape(n_layers, 2, batch_loc, n_z, n_tp, seq_local, head_dim)
        me = (lax.axis_index("y") * n_x + lax.axis_index("x")) * CORES + lax.axis_index("core")
        kv = lax.dynamic_index_in_dim(kv, me, axis=4, keepdims=False)
        kv = lax.all_to_all(kv, "z", 3, 2, tiled=True)
        kv = kv.reshape(n_layers, 2, n_batch, seq_local, head_dim)
        return y_loc, kv

    return jax.shard_map(device_fn, mesh=mesh4, in_specs=(act_spec, P(None, every), w_spec, w_spec, P(None, col, ("z", "y"))), out_specs=(act_spec, P(None, None, None, every, None)), check_vma=False)
```

```python
import jax
import jax.numpy as jnp
from jax import lax
from jax.experimental import pallas as pl
from jax.experimental.pallas import tpu as pltpu
from jax.sharding import Mesh
from jax.sharding import PartitionSpec as P

LN_EPS = 1e-6
RING = 4
CORES = 2
VMEM_LIMIT = 67_000_000
BF = jnp.bfloat16
F32 = jnp.float32
SLOT_OFF = (2, 1, 3, 0)
SIGN = (1, -1)
NIL = None
BOTH = range(CORES)
RINGS = range(RING)
OTHERS = (1, 3, 2)
LAST = RING - 1
G_ROWS = 8
KINDS = ("first", "second", "first_on", "second_on")
NAMES = (
    "xt", "gain_in", "wkv", "w_in", "w_out", "cos", "sin", "y_out", "kv_out", "h_all", "wi", "wo", "kvh", "h_ref",
    "hid", "gain", "gbuf", "xz", "xp",
    "wv", "kvb", "wov", "hb", "joined", "qkv", "stage", "lhs", "away", "acc", "die_in", "in1", "in2", "in3", "in4",
    "xz_send", "xz_recv", "xp_send", "xp_recv", "xd_send", "xd_recv", "x_loc", "g_send", "g_recv", "gd_send", "gd_recv", "yd_send", "yd_recv", "yp_send", "yp_recv", "yz_send", "yz_recv", "y_loc",
    "ag_send", "ag_recv", "ag_dsend", "ag_drecv", "ag_loc", "h_sem", "kvo_sem", "w_load", "y_recv", "zb_recv",
    "zc_recv", "w_send", "kz_send", "kz_recv", "ky_send", "ky_recv", "kx_send", "kx_recv", "kd_send", "kd_recv",
    "k_loc", "dsend", "drecv", "send1", "recv1", "send2", "recv2", "send3", "recv3", "send4", "recv4",
)


class Refs:
    def __init__(self, refs):
        for name, ref in zip(NAMES, refs, strict=True):
            setattr(self, name, ref)


def model_kernel(*refs):
    r = Refs(refs)
    z, y, x, c = (lax.axis_index(a) for a in ("z", "y", "x", "core"))
    n_layers = r.wkv.shape[0]
    rows, d_model = r.hid.shape
    batch, d_local = r.xt.shape[:2]
    seqs = batch // RING
    seq_len, head_dim = r.cos.shape
    d_row = r.w_in.shape[1]
    e_loc = r.wi.shape[3]
    depth = r.wo.shape[3]
    f_loc = depth - head_dim
    quarter = rows // 4
    half = d_model // 2
    q_block = head_dim * RING
    f_block = f_loc * RING

    def turn(base, off):
        return lax.rem(base + off + RING, RING)

    def remote(src, dst, ssem, rsem, dev):
        return pltpu.make_async_remote_copy(
            src_ref=src, dst_ref=dst, send_sem=ssem, recv_sem=rsem, device_id=dev, device_id_type=pl.DeviceIdType.MESH)

    partner = (z, y, x, 1 - c)

    peers = [(turn(z, o), y, x, c) for o in OTHERS]
    peers += [(z, turn(y, oy), turn(x, ox), c) for oy in RINGS for ox in RINGS if oy or ox]
    peers.append(partner)
    here = (z, y, x, c)
    gate_sem = pltpu.get_barrier_semaphore()
    for dev in peers:
        pl.semaphore_signal(gate_sem, inc=1, device_id=dev, device_id_type=pl.DeviceIdType.MESH)
    pl.semaphore_wait(gate_sem, len(peers))

    def hook(pump, i):
        with jax.named_scope(f"hook_{i}"):
            pump(i)

    def w_cols(kind):
        return pl.ds(0, head_dim + f_loc) if kind == 0 else pl.ds(head_dim + f_loc, f_loc)

    def piece(t, zz, yy):
        l, kind = t // 3, t % 3
        if kind == 2:
            return r.wo.at[l, zz, yy]
        return r.wi.at[l, zz, pl.ds(pl.multiple_of(yy * d_row, d_row), d_row), w_cols(kind)]

    def piece_half(t, zz, yy, h):
        l, kind = t // 3, t % 3
        if kind == 2:
            return r.wo.at[l, zz, yy, pl.ds(h * (depth // 2), depth // 2)]
        return r.wi.at[l, zz, pl.ds(pl.multiple_of(yy * d_row + h * (d_row // 2), d_row // 2), d_row // 2), w_cols(kind)]

    def own_parts(t, owner, zz, yy):
        l, kind = t // 3, t % 3
        hq = pl.ds(pl.multiple_of(owner * head_dim, head_dim), head_dim)
        if kind == 2:
            return [
                (r.w_out.at[l, hq], r.wo.at[l, zz, yy, pl.ds(0, head_dim)]),
                (r.w_out.at[l, pl.ds(pl.multiple_of(q_block + owner * f_loc, head_dim), f_loc)], r.wo.at[l, zz, yy, pl.ds(head_dim, f_loc)]),
            ]
        rws = pl.ds(pl.multiple_of(yy * d_row, d_row), d_row)
        if kind == 0:
            return [
                (r.w_in.at[l, :, hq], r.wi.at[l, zz, rws, pl.ds(0, head_dim)]),
                (r.w_in.at[l, :, pl.ds(pl.multiple_of(q_block + owner * f_loc, head_dim), f_loc)], r.wi.at[l, zz, rws, pl.ds(head_dim, f_loc)]),
            ]
        return [(r.w_in.at[l, :, pl.ds(pl.multiple_of(q_block + f_block + owner * f_loc, head_dim), f_loc)],
                 r.wi.at[l, zz, rws, pl.ds(head_dim + f_loc, f_loc)])]

    def y_send(t):
        for dy in OTHERS:
            owner = turn(y, dy)
            for src, dst in own_parts(t, owner, z, y):
                remote(src, dst, r.w_send.at[t, 0], r.y_recv.at[t, (RING - dy) % RING], (z, owner, x, c)).start()

    def z_own(t):
        for d in BOTH:
            for src, dst in own_parts(t, y, z, y):
                remote(src, dst, r.w_send.at[t, 1], r.zb_recv.at[t, 0, d], (turn(z, SIGN[d]), y, x, c)).start()

    def z_direct(t, j):
        yy = turn(y, j)
        ref = piece(t, z, yy)
        remote(ref, ref, r.w_send.at[t, 0], r.y_recv.at[t, j], here).wait_recv()
        for d in BOTH:
            remote(ref, ref, r.w_send.at[t, 1], r.zb_recv.at[t, j, d], (turn(z, SIGN[d]), y, x, c)).start()

    def z_forward(t, j):
        yy = turn(y, j)
        for d in BOTH:
            zz = turn(z, -SIGN[d])
            ref = piece(t, zz, yy)
            remote(ref, ref, r.w_send.at[t, 1], r.zb_recv.at[t, j, d], here).wait_recv()
            part = piece_half(t, zz, yy, d)
            remote(part, part, r.w_send.at[t, 2], r.zc_recv.at[t, j, d], (turn(z, SIGN[d]), y, x, c)).start()

    def place(t, zz):
        l, kind = t // 3, t % 3
        if kind == 2:
            return r.wo.at[l, zz], r.wov.at[zz]
        return r.wi.at[l, zz, :, w_cols(kind)], r.wv.at[zz, :, w_cols(kind)]

    def load_near(t):
        l, kind = t // 3, t % 3
        for d in BOTH:
            src, dst = place(t, turn(z, SIGN[d]))
            pltpu.make_async_copy(src, dst, r.w_load.at[kind]).start()
        for j in (1, 2, 3):
            yy = turn(y, j)
            dst = r.wov.at[z, yy] if kind == 2 else r.wv.at[z, pl.ds(pl.multiple_of(yy * d_row, d_row), d_row), w_cols(kind)]
            pltpu.make_async_copy(piece(t, z, yy), dst, r.w_load.at[kind]).start()
        for src, dst in own_parts(t, y, z, y):
            pltpu.make_async_copy(src, own_place(t, dst, src), r.w_load.at[kind]).start()

    def own_place(t, dst, src):
        kind = t % 3
        if kind == 2:
            n = src.shape[0]
            return r.wov.at[z, y, pl.ds(0 if n == head_dim and f_loc != head_dim else head_dim, n)]
        n = src.shape[1]
        rws = pl.ds(pl.multiple_of(y * d_row, d_row), d_row)
        if kind == 0:
            return r.wv.at[z, rws, pl.ds(0 if n == head_dim and f_loc != head_dim else head_dim, n)]
        return r.wv.at[z, rws, pl.ds(head_dim + f_loc, f_loc)]

    def finish(t):
        l, kind = t // 3, t % 3
        far = turn(z, 2)
        for j in RINGS:
            for d in BOTH:
                part = piece_half(t, far, turn(y, j), d)
                remote(part, part, r.w_send.at[t, 2], r.zc_recv.at[t, j, d], here).wait_recv()
        load_near(t)
        src, dst = place(t, far)
        pltpu.make_async_copy(src, dst, r.w_load.at[kind]).start()

    def loaded(t):
        kind = t % 3
        dst = r.wov if kind == 2 else r.wv.at[:, :, w_cols(kind)]
        pltpu.make_async_copy(dst, dst, r.w_load.at[kind]).wait()

    def drain(t):
        l, kind = t // 3, t % 3
        if kind == 2:
            refs3 = (r.wo.at[l, 0, pl.ds(0, 3)], r.wo.at[l, pl.ds(0, 2)], r.wo.at[l, 0])
        else:
            cols = w_cols(kind)
            refs3 = (r.wi.at[l, 0, pl.ds(0, 3 * d_row), cols], r.wi.at[l, pl.ds(0, 2), :, cols], r.wi.at[l, 0, :, cols])
        for g in range(3):
            remote(refs3[g], refs3[g], r.w_send.at[t, g], r.y_recv.at[t, 0], here).wait_send()

    def kv_z():
        for i, o in enumerate(OTHERS):
            remote(r.wkv, r.kvh.at[x, c, :, y, z], r.kz_send.at[i], r.kz_recv.at[i], (turn(z, o), y, x, c)).start()
        pltpu.make_async_copy(r.wkv, r.kvh.at[x, c, :, y, z], r.k_loc.at[0]).start()

    def kv_y():
        pltpu.make_async_copy(r.wkv, r.kvh.at[x, c, :, y, z], r.k_loc.at[0]).wait()
        for i, o in enumerate(OTHERS):
            zz = turn(z, -o)
            remote(r.wkv, r.kvh.at[x, c, :, y, zz], r.kz_send.at[i], r.kz_recv.at[i], (turn(z, o), y, x, c)).wait()
        ref = r.kvh.at[x, c, :, y]
        for i, o in enumerate(OTHERS):
            remote(ref, ref, r.ky_send.at[i], r.ky_recv.at[i], (z, turn(y, o), x, c)).start()

    def kv_x():
        for i, o in enumerate(OTHERS):
            ref = r.kvh.at[x, c, :, turn(y, -o)]
            remote(ref, ref, r.ky_send.at[i], r.ky_recv.at[i], (z, turn(y, o), x, c)).wait()
        for l in range(n_layers):
            ref = r.kvh.at[x, c, l]
            for i, o in enumerate(OTHERS):
                remote(ref, ref, r.kx_send.at[l, i], r.kx_recv.at[l, i], (z, y, turn(x, o), c)).start()
            remote(ref, ref, r.kd_send.at[l, 3], r.kd_recv.at[l, 3], partner).start()

    def kv_die(l):
        for i, o in enumerate(OTHERS):
            ref = r.kvh.at[turn(x, -o), c, l]
            remote(ref, ref, r.kx_send.at[l, i], r.kx_recv.at[l, i], (z, y, turn(x, o), c)).wait()
            remote(ref, ref, r.kd_send.at[l, i], r.kd_recv.at[l, i], partner).start()

    def kv_load(l):
        for i, o in enumerate((1, 3, 2, 0)):
            ref = r.kvh.at[turn(x, -o), 1 - c, l]
            remote(ref, ref, r.kd_send.at[l, i], r.kd_recv.at[l, i], partner).wait()
        kc = r.wkv.shape[1]
        for xx in RINGS:
            for cc in BOTH:
                pltpu.make_async_copy(r.kvh.at[xx, cc, l], r.kvb.at[:, :, pl.ds((xx * CORES + cc) * kc, kc)], r.k_loc.at[1]).start()

    def kv_loaded():
        pltpu.make_async_copy(r.kvb, r.kvb, r.k_loc.at[1]).wait()

    def gain_move(i, src, dst, dev):
        return remote(src, dst, r.g_send.at[i], r.g_recv.at[i], dev)

    def gain_z(k):
        dev = (turn(z, OTHERS[k]), y, x, c)
        return gain_move(k, r.gain_in, r.gbuf.at[x, c, y, z], dev)

    def gain_y(k):
        dev = (z, turn(y, OTHERS[k]), x, c)
        return gain_move(len(OTHERS) + k, r.gbuf.at[x, c, y], r.gbuf.at[x, c, y], dev)

    def gain_x(k):
        dev = (z, y, turn(x, OTHERS[k]), c)
        return gain_move(CORES * len(OTHERS) + k, r.gbuf.at[x, c], r.gbuf.at[x, c], dev)

    def gain_die(xx, k):
        ref = r.gbuf.at[xx, c]
        return remote(ref, ref, r.gd_send.at[k], r.gd_recv.at[k], partner)

    def gain_sum():
        for zz in RINGS:
            for yy in RINGS:
                tot = jnp.zeros((n_layers, d_row), F32)
                for xx in RINGS:
                    for cc in BOTH:
                        tot += r.gbuf[xx, cc, yy, zz, :n_layers].astype(F32)
                at = (zz * RING + yy) * d_row
                r.gain[:, at:at + d_row] = tot

    tok_pair = CORES * rows

    def x_z(k):
        zz = turn(z, OTHERS[k])
        src = r.xt.at[pl.ds(zz * seqs, seqs)]
        return remote(src, r.xz.at[z], r.xz_send.at[k], r.xz_recv.at[k], (zz, y, x, c))

    def x_own():
        return pltpu.make_async_copy(r.xt.at[pl.ds(z * seqs, seqs)], r.xz.at[z], r.x_loc)

    def pos(xx):
        return pl.ds(pl.multiple_of(xx * tok_pair, tok_pair), tok_pair)

    def x_plane(oy, ox):
        yy, xx = turn(y, oy), turn(x, ox)
        return remote(r.xz.at[:, yy, :, pos(xx)], r.xp.at[c, y, x], r.xp_send.at[oy], r.xp_recv.at[(RING - oy) % RING], (z, yy, xx, c))

    def row_bytes(oy):
        return r.xp.at[c, 0] if oy else r.xp.at[c, 0, pl.ds(0, RING - 1)]

    def x_row(oy):
        yy = turn(y, oy)
        got = row_bytes(oy)
        remote(got, got, r.xp_send.at[oy], r.xp_recv.at[oy], partner).wait_recv()
        row = r.xp.at[c, yy]
        remote(row, row, r.xd_send.at[oy], r.xd_recv.at[oy], partner).start()

    def x_turn():
        for oy in RINGS:
            row = r.xp.at[1 - c, turn(y, oy)]
            remote(row, row, r.xd_send.at[oy], r.xd_recv.at[oy], partner).wait_recv()

        @pl.loop(0, RING)
        def _(zz):
            for yy in RINGS:
                for xh in BOTH:
                    blk = [r.xp[cc, yy, CORES * xh + xx, zz] for xx in BOTH for cc in BOTH]
                    blk = jnp.concatenate(blk, axis=0).astype(F32).T.astype(BF)
                    n = blk.shape[1]
                    at = pl.multiple_of(zz * RING * d_row + yy * d_row + xh * n, n)
                    r.hb[0, 0, :, :, pl.ds(at, n)] = blk.reshape(CORES, rows, n)
        r.hid[...] = r.hb[0, 0, c]
        for oy in RINGS:
            row = r.xp.at[c, turn(y, oy)]
            remote(row, row, r.xd_send.at[oy], r.xd_recv.at[oy], partner).wait_send()

    def x_sent():
        for fn in (x_z, gain_z, gain_y, gain_x):
            peers_of(fn, "wait_send")
        for k in RINGS:
            gain_die(x, k).wait_send()
        for oy in RINGS:
            got = row_bytes(oy)
            remote(got, got, r.xp_send.at[oy], r.xp_recv.at[oy], partner).wait_send()

    def y_die():
        return remote(r.hid, r.hb.at[0, 0, c], r.yd_send, r.yd_recv, partner)

    def y_plane(oy, ox):
        yy, xx = turn(y, oy), turn(x, ox)
        return remote(r.xp.at[c, yy, xx], r.xz.at[:, y, :, pos(x)], r.yp_send.at[oy], r.yp_recv.at[(RING - oy) % RING], (z, yy, xx, c))

    def y_z(s, oy, k):
        zz = turn(z, OTHERS[k])
        return remote(r.xz.at[zz, s], r.y_out.at[z * seqs + s], r.yz_send.at[oy, k], r.yz_recv.at[oy, k], (zz, y, x, c))

    def y_own(s, oy):
        return pltpu.make_async_copy(r.xz.at[z, s], r.y_out.at[z * seqs + s], r.y_loc.at[oy])

    def leave():
        y_die().start()
        r.hb[0, 0, c] = r.hid[...]
        y_die().wait()

        @pl.loop(0, RING)
        def _(zz):
            for yy in RINGS:
                for xh in BOTH:
                    n = CORES * CORES * d_local
                    at = pl.multiple_of(zz * RING * d_row + yy * d_row + xh * n, n)
                    blk = r.hb[0, 0, :, :, pl.ds(at, n)].reshape(tok_pair, n).astype(F32).T.astype(BF)
                    for xx in BOTH:
                        for cc in BOTH:
                            lo = (xx * CORES + cc) * d_local
                            r.xp[cc, yy, CORES * xh + xx, zz] = blk[lo:lo + d_local]

        for oy in OTHERS + (0,):
            for ox in RINGS:
                if oy or ox:
                    y_plane(oy, ox).start()
        for zz in RINGS:
            r.xz[zz, y, :, pos(x)] = r.xp[c, y, x, zz]
        for oy in OTHERS + (0,):
            yy = turn(y, oy)
            got = row_bytes(oy)
            remote(got, got, r.yp_send.at[oy], r.yp_recv.at[oy], partner).wait_recv()
            for k in range(len(OTHERS)):
                y_z(yy, oy, k).start()
            y_own(yy, oy).start()
        for oy in RINGS:
            got = row_bytes(oy)
            remote(got, got, r.yp_send.at[oy], r.yp_recv.at[oy], partner).wait_send()
            for k in range(len(OTHERS)):
                y_z(turn(y, oy), oy, k).wait()
            y_own(turn(y, oy), oy).wait()

    def gather_norm(l, pump):
        hid = r.hid
        gain = r.gain[l:l + 1, :]
        for b in range(4):
            blk = hid[b * quarter:(b + 1) * quarter, :].astype(F32)
            mean = jnp.mean(blk, axis=-1, keepdims=True)
            cen = blk - mean
            var = jnp.mean(cen * cen, axis=-1, keepdims=True)
            r.h_ref[b * quarter:(b + 1) * quarter, :] = (cen * lax.rsqrt(var + LN_EPS) * gain).astype(BF)
        out = r.h_all.at[l]

        def spot(q, first, second):
            if q == 0:
                return turn(y, second), turn(x, first)
            return turn(y, first), turn(x, second)

        def span(q, part):
            if part is NIL:
                return pl.ds(q * 2 * quarter, 2 * quarter)
            return pl.ds((q * 2 + part) * quarter, quarter)

        copies = {}

        def ici(key, q, first, second, part, to_first, to_second, own=False):
            sy, sx = spot(q, first, second)
            ty, tx = spot(q, to_first, to_second)
            rws = span(q, part)
            dst = out.at[sy, sx, c, rws]
            kind = KINDS.index(key[0])
            cp = remote(r.h_ref.at[rws] if own else dst, dst, r.ag_send.at[l, kind], r.ag_recv.at[l, len(copies)], (z, ty, tx, c))
            cp.start()
            copies[key] = cp

        def die(q, first, second, own=False):
            sy, sx = spot(q, first, second)
            rws = span(q, NIL)
            dst = out.at[sy, sx, c, rws]
            off = (first if q else second) % RING
            remote(r.h_ref.at[rws] if own else dst, dst, r.ag_dsend.at[l], r.ag_drecv.at[l, off], partner).start()

        offs = (0, -1, 1, 2)
        for q in BOTH:
            for d in BOTH:
                ici(("first", q, d), q, 0, 0, NIL, SIGN[d], 0, own=True)
        for q in BOTH:
            for d in BOTH:
                ici(("second", q, 0, d), q, 0, 0, NIL, 0, SIGN[d], own=True)
        for q in BOTH:
            die(q, 0, 0, own=True)
        own = pltpu.make_async_copy(r.h_ref, out.at[y, x, c], r.ag_loc)
        own.start()
        hook(pump, 0)
        for d in BOTH:
            for q in BOTH:
                copies["first", q, d].wait_recv()
                src = -SIGN[d]
                ici(("first_on", q, d), q, src, 0, d, SIGN[d], 0)
                for e in BOTH:
                    ici(("second", q, 1 + d, e), q, src, 0, NIL, 0, SIGN[e])
                die(q, src, 0)
        hook(pump, 1)
        for d in BOTH:
            for q in BOTH:
                copies["second", q, 0, d].wait_recv()
                src = -SIGN[d]
                ici(("second_on", q, 0, d), q, 0, src, d, 0, SIGN[d])
                die(q, 0, src)
        hook(pump, 2)
        for q in BOTH:
            for d in BOTH:
                copies["first_on", q, d].wait_recv()
            for e in BOTH:
                ici(("second", q, 3, e), q, 2, 0, NIL, 0, SIGN[e])
            die(q, 2, 0)
        hook(pump, 3)
        for k in (1, 2, 3):
            for d in BOTH:
                for q in BOTH:
                    copies["second", q, k, d].wait_recv()
                    src = -SIGN[d]
                    ici(("second_on", q, k, d), q, offs[k], src, d, 0, SIGN[d])
                    die(q, offs[k], src)
            hook(pump, 3 + k)
        for k in range(4):
            for q in BOTH:
                for d in BOTH:
                    copies["second_on", q, k, d].wait_recv()
                die(q, offs[k], 2)
        hook(pump, 7)
        for off in RINGS:
            got = out.at[turn(y, off), :, 1 - c]
            remote(got, got, r.ag_dsend.at[l], r.ag_drecv.at[l, off], partner).wait_recv()
        sent = (out.at[y, x], out.at[y], out.at[y, x, c], out.at[y, pl.ds(0, CORES)])
        for kind, ref in enumerate(sent):
            remote(ref, ref, r.ag_send.at[l, kind], r.ag_recv.at[l, kind], partner).wait_send()
        remote(out.at[pl.ds(0, 2)], out.at[pl.ds(0, 2)], r.ag_dsend.at[l], r.ag_drecv.at[l, 0], partner).wait_send()
        own.wait()

    def h_copy(l, s, slot):
        return pltpu.make_async_copy(r.h_all.at[l, s], r.hb.at[slot], r.h_sem.at[slot])

    def h_tile(slot):
        return r.hb[slot].reshape(seq_len, d_model)

    def project(h, lo, n):
        w = r.wv[:, :, lo:lo + n].reshape(d_model, n)
        return jnp.dot(h, w, preferred_element_type=F32).astype(BF)

    def rope(val):
        val = val.astype(F32)
        return val * r.cos[...] + pltpu.roll(val, head_dim // 2, 1) * r.sin[...]

    n_chunk = min(256, f_loc)

    def kv_out_copy(l, s, slot, i):
        return pltpu.make_async_copy(r.qkv.at[slot, i], r.kv_out.at[l, i, s], r.kvo_sem.at[slot, i])

    def pass_one(l, pump):
        h_copy(l, 0, 0).start()

        @pl.loop(0, RING)
        def _(s):
            slot = lax.rem(s, 2)
            h_copy(l, s, slot).wait()

            @pl.when(s + 1 < RING)
            def _():
                h_copy(l, s + 1, 1 - slot).start()

            pump(s)

            @pl.when(s >= 2)
            def _():
                for i in BOTH:
                    kv_out_copy(l, s - 2, slot, i).wait()

            kv = jnp.zeros((seq_len, 2 * head_dim), F32)
            for zz in RINGS:
                for yy in RINGS:
                    col = (zz * RING + yy) * d_row
                    kv += lax.dot_general(h_cols(slot, col, d_row), r.kvb[yy, zz], (((1,), (1,)), ((), ())), preferred_element_type=F32)
            kv = kv.astype(BF)
            r.qkv[slot, 0] = rope(kv[:, :head_dim]).astype(BF)
            r.qkv[slot, 1] = kv[:, head_dim:]
            for i in BOTH:
                kv_out_copy(l, s, slot, i).start()
            q = project(h_tile(slot), 0, head_dim)
            r.stage[...] = (rope(q) * head_dim ** -0.5).astype(BF)
            for lo in range(0, f_loc, n_chunk):
                r.joined[s, :, head_dim + lo:head_dim + lo + n_chunk] = project(h_tile(slot), head_dim + lo, n_chunk)
            n_tile = seq_len // 2
            for i in BOTH:
                keys = (i + 1) * n_tile
                sc = lax.dot_general(r.stage[i * n_tile:(i + 1) * n_tile, :], r.qkv[slot, 0, :keys, :], (((1,), (1,)), ((), ())), preferred_element_type=F32)
                row_id = lax.broadcasted_iota(jnp.int32, sc.shape, 0) + i * n_tile
                col_id = lax.broadcasted_iota(jnp.int32, sc.shape, 1)
                sc = jnp.where(col_id <= row_id, sc, -1e30)
                top = jnp.max(sc, axis=-1, keepdims=True)
                ex = jnp.exp(sc - top)
                prob = (ex * (1.0 / jnp.sum(ex, axis=-1, keepdims=True))).astype(BF)
                att = jnp.dot(prob, r.qkv[slot, 1, :keys, :], preferred_element_type=F32)
                r.joined[s, i * n_tile:(i + 1) * n_tile, :head_dim] = att.astype(BF)

        for s in (RING - 2, RING - 1):
            for i in BOTH:
                kv_out_copy(l, s, s % 2, i).wait()

    def h_cols(slot, col, n):
        return r.hb[slot, :, :, :, col:col + n].reshape(seq_len, n)

    def pass_two(l, pump):
        h_copy(l, 0, 0).start()

        @pl.loop(0, RING)
        def _(s):
            slot = lax.rem(s, 2)
            h_copy(l, s, slot).wait()

            @pl.when(s + 1 < RING)
            def _():
                h_copy(l, s + 1, 1 - slot).start()

            pump(s)
            for lo in range(0, f_loc, n_chunk):
                up = project(h_tile(slot), head_dim + f_loc + lo, n_chunk).astype(F32)
                cols = slice(head_dim + lo, head_dim + lo + n_chunk)
                g = r.joined[s, :, cols].astype(F32)
                r.joined[s, :, cols] = (g * jax.nn.sigmoid(g) * up).astype(BF)

    def out_scatter(l, pump):
        def peer(q, first, second):
            dy = first * (1 - q) + second * q
            dx = first * q + second * (1 - q)
            return (z, turn(y, dy), turn(x, dx), c)

        def die_copy(q, s):
            return remote(r.away.at[q], r.die_in.at[q, s], r.dsend.at[l, q, s], r.drecv.at[l, q, s], partner)

        def first_copy(q, d):
            return remote(r.acc.at[q, 0, pl.ds(2 * d, 2)], r.in1.at[q, d], r.send1.at[l, q, d], r.recv1.at[l, q, d], peer(q, 1 - 2 * d, 0))

        def second_copy(q, d, h):
            return remote(r.acc.at[q, 1 + d, pl.ds(2 * h, 2)], r.in2.at[q, d, pl.ds(2 * h, 2)], r.send2.at[l, q, d, h], r.recv2.at[l, q, d, h], peer(q, 1 - 2 * d, 0))

        def third_copy(q, d):
            rws = pl.ds(d * (rows // 2), rows // 2)
            return remote(r.acc.at[q, LAST, 0, rws], r.in3.at[q, d], r.send3.at[l, q, d], r.recv3.at[l, q, d], peer(q, 0, 1 - 2 * d))

        def fourth_copy(q, d):
            return remote(r.acc.at[q, LAST, 1 + d], r.in4.at[q, d], r.send4.at[l, q, d], r.recv4.at[l, q, d], peer(q, 0, 1 - 2 * d))

        n_blk = r.wov.shape[3]
        blk_z = RING // 2

        def tile(q, s):
            for cc in BOTH:
                for j in RINGS:
                    oy = SLOT_OFF[s] * (1 - q) + SLOT_OFF[j] * q
                    ox = SLOT_OFF[j] * (1 - q) + SLOT_OFF[s] * q
                    core = (1 - c) if cc == 0 else c
                    at = pl.multiple_of((turn(x, ox) * CORES + core) * rows, rows)
                    r.lhs[pl.ds((cc * RING + j) * rows, rows), :] = r.joined[turn(y, oy), pl.ds(at, rows), :]
            left = r.lhs[...]

            @pl.loop(0, half // n_blk)
            def _(n):
                col = pl.multiple_of(n * n_blk, n_blk)
                w = r.wov[q * blk_z + n // RING, lax.rem(n, RING)]
                res = jnp.dot(left, w, preferred_element_type=F32).astype(BF)
                res = res.reshape(CORES, RING, rows, n_blk)
                r.away[q, :, :, pl.ds(col, n_blk)] = res[0]
                r.acc[q, s, :, :, pl.ds(col, n_blk)] = res[1]

        def pair_sum(q, s):
            die_copy(q, s).wait_recv()

            @pl.loop(0, RING)
            def _(j):
                r.acc[q, s, j] = r.acc[q, s, j] + r.die_in[q, s, j]

        for s in RINGS:
            @pl.loop(0, 2)
            def _(q, s=s):
                if s > 0:
                    die_copy(q, s - 1).wait_send()
                tile(q, s)
                die_copy(q, s).start()
                if s > 0:
                    pair_sum(q, s - 1)
                if s == 1:
                    for d in BOTH:
                        first_copy(q, d).start()
                if s > 1:
                    second_copy(q, s - 2, LAST - s).start()
            pump(s)

        for q in BOTH:
            pair_sum(q, LAST)
        for q in BOTH:
            for d in BOTH:
                first_copy(q, d).wait_recv()
                for j in BOTH:
                    at = CORES * d + j
                    r.acc[q, 1 + d, at] = r.acc[q, 1 + d, at] + r.in1[q, d, j]
                second_copy(q, d, d).start()
        hook(pump, 4)

        def total(q, j):
            val = r.acc[q, LAST, j].astype(F32)
            for d in BOTH:
                val += r.in2[q, d, j].astype(F32)
            r.acc[q, LAST, j] = val.astype(BF)

        with jax.named_scope("second_a"):
            for q in BOTH:
                for d in BOTH:
                    second_copy(q, d, 1 - d).wait_recv()
        hook(pump, 5)
        for q in BOTH:
            with jax.named_scope("second_b"):
                for d in BOTH:
                    second_copy(q, d, d).wait_recv()
            total(q, 0)
            for d in BOTH:
                third_copy(q, d).start()
            for j in RINGS[1:]:
                total(q, j)
        hook(pump, 6)
        for q in BOTH:
            for d in BOTH:
                with jax.named_scope("third"):
                    third_copy(q, d).wait_recv()
                rws = pl.ds(d * (rows // 2), rows // 2)
                r.acc[q, LAST, 1 + d, rws] = r.acc[q, LAST, 1 + d, rws] + r.in3[q, d]
                fourth_copy(q, d).start()
        for q in BOTH:
            with jax.named_scope("fourth"):
                for d in BOTH:
                    fourth_copy(q, d).wait_recv()
            cols = pl.ds(q * half, half)
            upd = r.acc[q, LAST, LAST].astype(F32)
            for d in BOTH:
                upd += r.in4[q, d].astype(F32)
            upd = upd.astype(BF)
            r.hid[:, cols] = (r.hid[:, cols].astype(F32) + upd.astype(F32)).astype(BF)
        for q in BOTH:
            die_copy(q, LAST).wait_send()
            for d in BOTH:
                for cp in (first_copy, third_copy, fourth_copy):
                    cp(q, d).wait_send()
                for h in BOTH:
                    second_copy(q, d, h).wait_send()

    def near(fn, t):
        for j in (LAST, 1):
            fn(t, j)

    def far(fn, t):
        fn(t, 2)

    def z_all(t):
        near(z_direct, t)
        far(z_direct, t)

    def peers_of(fn, op="start"):
        for k in range(len(OTHERS)):
            getattr(fn(k), op)()

    def when_j(s, fn):
        @pl.when(s < 3)
        def _():
            fn(s + 1)

    def start():
        peers_of(x_z)
        x_own().start()
        peers_of(gain_z)
        r.gbuf[x, c, y, z] = r.gain_in[...]
        kv_z()
        z_own(0)
        peers_of(gain_z, "wait_recv")
        peers_of(gain_y)
        y_send(0)
        peers_of(gain_y, "wait_recv")
        peers_of(gain_x)
        gain_die(x, LAST).start()
        with jax.named_scope("x_z"):
            peers_of(x_z, "wait_recv")
            x_own().wait()
        for oy in RINGS:
            for ox in RINGS:
                if oy or ox:
                    x_plane(oy, ox).start()
        r.xp[c, y, x] = r.xz[:, y, :, pos(x)]
        with jax.named_scope("kv_y"):
            kv_y()
        y_send(1)
        for k, o in enumerate(OTHERS):
            gain_x(k).wait_recv()
            gain_die(turn(x, -o), k).start()
        with jax.named_scope("z_a"):
            near(z_direct, 0)
        with jax.named_scope("row_0"):
            x_row(0)
        with jax.named_scope("z_b"):
            z_forward(0, 0)
        with jax.named_scope("row_13"):
            near(lambda t, oy: x_row(oy), 0)
        with jax.named_scope("z_c"):
            far(z_direct, 0)
        with jax.named_scope("row_2"):
            far(lambda t, oy: x_row(oy), 0)
        for k in RINGS:
            gain_die(x, k).wait_recv()
        z_own(1)
        with jax.named_scope("gain_sum"):
            gain_sum()
        with jax.named_scope("turn"):
            x_turn()
        with jax.named_scope("z_d"):
            near(z_forward, 0)

    def ag0(i):
        if i == 1:
            far(z_forward, 0)
        if i == 2:
            near(z_direct, 1)
        if i == 3:
            far(z_direct, 1)
            kv_x()
        if i == 4:
            z_forward(1, 0)
        if i == 5:
            near(z_forward, 1)
        if i == 6:
            far(z_forward, 1)
            y_send(2)
            z_own(2)
            kv_die(0)
        if i == 7:
            finish(0)
            kv_load(0)

    def rs0(i):
        if i == 0:
            z_forward(3, 0)
            near(z_forward, 3)
        if i == 1:
            far(z_forward, 3)
            z_own(4)
        if i == 2:
            z_all(4)
        if i == 4:
            finish(3)
            z_forward(4, 0)
            kv_die(1)
        if i == 5:
            near(z_forward, 4)
            kv_load(1)
        if i == 6:
            far(z_forward, 4)

    def ag1(i):
        if i == 1:
            z_own(5)
            z_all(5)
        if i == 4:
            finish(4)
        if i == 5:
            z_forward(5, 0)
            near(z_forward, 5)
        if i == 6:
            far(z_forward, 5)

    def nothing(i):
        pass

    with jax.named_scope("start"):
        start()
    with jax.named_scope("gather_0"):
        gather_norm(0, ag0)
    with jax.named_scope("wait_w0"):
        loaded(0)
        kv_loaded()
        y_send(3)
        x_sent()
    with jax.named_scope("pass_one_0"):
        pass_one(0, lambda s: when_j(s, lambda j: z_direct(2, j)))
    with jax.named_scope("finish_1"):
        finish(1)
        z_own(3)
        y_send(4)
        y_send(5)
        loaded(1)
    with jax.named_scope("pass_two_0"):
        pass_two(0, lambda s: z_forward(2, s))
    with jax.named_scope("finish_2"):
        finish(2)
        z_all(3)
        loaded(2)
    with jax.named_scope("scatter_0"):
        out_scatter(0, rs0)
    with jax.named_scope("gather_1"):
        gather_norm(1, ag1)
    with jax.named_scope("wait_w3"):
        loaded(3)
        kv_loaded()
    with jax.named_scope("pass_one_1"):
        pass_one(1, nothing)
    with jax.named_scope("finish_5"):
        loaded(4)
        finish(5)
    with jax.named_scope("pass_two_1"):
        pass_two(1, nothing)
    with jax.named_scope("wait_w5"):
        loaded(5)
    with jax.named_scope("scatter_1"):
        out_scatter(1, nothing)
    with jax.named_scope("leave"):
        leave()
    with jax.named_scope("drain"):
        for t in range(3 * n_layers):
            drain(t)


def run_model(xt, gain, wkv_t, w_in, w_out, cos_full, sin_full):
    batch, d_local, seq_len = xt.shape
    n_layers, d_row, e_block = w_in.shape
    r_block, d_col = w_out.shape[1:]
    head_dim = cos_full.shape[1]
    d_model = d_row * RING * RING
    seqs = batch // RING
    rows = seqs * seq_len // (RING * RING * CORES)
    e_loc, r_loc = e_block // RING, r_block // RING
    kc = wkv_t.shape[1]
    half = d_model // 2
    g_rows = gain.shape[0]
    n_t = 3 * n_layers
    n_o = len(OTHERS)

    def dma(*shape):
        return pltpu.SemaphoreType.DMA(shape)

    def vm(*shape):
        return pltpu.VMEM(shape, BF)

    def out(*shape):
        return jax.ShapeDtypeStruct(shape, BF)

    any_spec = pl.BlockSpec(memory_space=pl.ANY)
    vm_spec = pl.BlockSpec(memory_space=pltpu.VMEM)
    out_shape = [
        out(batch, d_local, seq_len),
        out(n_layers, 2, seqs, seq_len, head_dim),
        out(n_layers, RING, RING, CORES, rows, d_model),
        out(n_layers, RING, RING * d_row, e_loc),
        out(n_layers, RING, RING, r_loc, d_col),
        out(RING, CORES, n_layers, RING, RING, kc, d_row),
    ]
    pair = (n_layers, 2, 2)
    scratch = [
        vm(rows, d_model), vm(rows, d_model), pltpu.VMEM((n_layers, d_model), F32),
        vm(RING, CORES, RING, RING, g_rows, d_row),
        vm(RING, seqs, d_local, seq_len),
        vm(CORES, RING, RING, RING, d_local, CORES * rows),
        vm(RING, RING * d_row, e_loc), vm(RING, RING, 2 * head_dim, d_row), vm(RING, RING, r_loc, d_col),
        vm(2, RING, CORES, rows, d_model), vm(RING, seq_len, r_loc), vm(2, 2, seq_len, head_dim), vm(seq_len, head_dim),
        vm(CORES * RING * rows, r_loc), vm(2, RING, rows, half), vm(2, RING, RING, rows, half), vm(2, RING, RING, rows, half),
        vm(2, 2, 2, rows, half), vm(2, 2, RING, rows, half), vm(2, 2, rows // 2, half), vm(2, 2, rows, half),
        dma(n_o), dma(n_o), dma(RING), dma(RING), dma(RING), dma(RING), pltpu.SemaphoreType.DMA,
        dma(3 * n_o), dma(3 * n_o), dma(RING), dma(RING),
        pltpu.SemaphoreType.DMA, pltpu.SemaphoreType.DMA, dma(RING), dma(RING), dma(RING, n_o), dma(RING, n_o), dma(RING),
        dma(n_layers, RING), dma(n_layers, 40), dma(n_layers), dma(n_layers, RING), pltpu.SemaphoreType.DMA, dma(2), dma(2, 2), dma(3),
        dma(n_t, RING), dma(n_t, RING, 2), dma(n_t, RING, 2), dma(n_t, 3),
        dma(n_o), dma(n_o), dma(n_o), dma(n_o), dma(n_layers, n_o), dma(n_layers, n_o), dma(n_layers, RING), dma(n_layers, RING), dma(2),
        dma(n_layers, 2, RING), dma(n_layers, 2, RING),
        dma(*pair), dma(*pair), dma(*pair, 2), dma(*pair, 2), dma(*pair), dma(*pair), dma(*pair), dma(*pair),
    ]
    res = pl.pallas_call(
        model_kernel,
        out_shape=out_shape,
        in_specs=[any_spec, vm_spec, vm_spec, any_spec, any_spec, vm_spec, vm_spec],
        out_specs=[any_spec] * len(out_shape),
        scratch_shapes=scratch,
        compiler_params=pltpu.CompilerParams(collective_id=0, has_side_effects=True, vmem_limit_bytes=VMEM_LIMIT),
        name="two_layers",
    )(xt, gain, wkv_t, w_in, w_out, cos_full, sin_full)
    return res[0], res[1]


def solution(mesh):
    row_size = mesh.shape["row"]
    n_col = mesh.shape["col"]
    n_z = row_size // RING
    n_y = RING
    n_x = n_col // CORES
    n_tp = n_y * n_col
    n_dev = row_size * n_col
    mesh4 = Mesh(mesh.devices.reshape(n_z, n_y, n_x, CORES), ("z", "y", "x", "core"))
    every = ("z", "y", "x", "core")
    col = ("x", "core")
    act_spec = P(NIL, NIL, every)
    w_spec = P(NIL, ("z", "y"), col)

    def device_fn(x_loc, gain_loc, w_in_loc, w_kv_loc, w_out_loc):
        n_layers = w_in_loc.shape[0]
        n_batch, seq_len, d_local = x_loc.shape
        head_dim = w_kv_loc.shape[2] * n_col // 2
        batch_loc = n_batch // n_z
        seq_local = seq_len // n_dev
        inv_freq = 1.0 / (10000.0 ** (jnp.arange(head_dim // 2, dtype=F32) * 2.0 / head_dim))
        angles = jnp.arange(seq_len).astype(F32)[:, NIL] * inv_freq[NIL, :]
        cos_tab, sin_tab = jnp.cos(angles), jnp.sin(angles)
        cos_full = jnp.concatenate([cos_tab, cos_tab], axis=1)
        sin_full = jnp.concatenate([-sin_tab, sin_tab], axis=1)

        spot = lax.axis_index("x") * CORES + lax.axis_index("core")
        own = lax.broadcasted_iota(jnp.int32, (n_layers, n_col, d_local), 1) == spot
        gains = jnp.where(own, gain_loc[:, NIL, :], 0).astype(BF).reshape(n_layers, n_col * d_local)
        gains = jnp.pad(gains, ((0, G_ROWS - n_layers), (0, 0)))
        y_loc, kv = run_model(x_loc.transpose(0, 2, 1), gains, w_kv_loc.transpose(0, 2, 1), w_in_loc, w_out_loc, cos_full, sin_full)
        y_loc = y_loc.transpose(0, 2, 1)
        kv = kv.reshape(n_layers, 2, batch_loc, n_z, n_tp, seq_local, head_dim)
        me = (lax.axis_index("y") * n_x + lax.axis_index("x")) * CORES + lax.axis_index("core")
        kv = lax.dynamic_index_in_dim(kv, me, axis=4, keepdims=False)
        kv = lax.all_to_all(kv, "z", 3, 2, tiled=True)
        kv = kv.reshape(n_layers, 2, n_batch, seq_local, head_dim)
        return y_loc, kv

    return jax.shard_map(device_fn, mesh=mesh4, in_specs=(act_spec, P(NIL, every), w_spec, w_spec, P(NIL, col, ("z", "y"))), out_specs=(act_spec, P(NIL, NIL, NIL, every, NIL)), check_vma=False)
```

```python
import jax
import jax.numpy as jnp
import numpy as np
from jax import lax
from jax.experimental import pallas as pl
from jax.experimental.pallas import tpu as pltpu
from jax.sharding import Mesh
from jax.sharding import PartitionSpec as P

LN_EPS = 1e-6
RING = 4
CORES = 2
VMEM_LIMIT = 67_000_000
BF = jnp.bfloat16
F32 = jnp.float32
SLOT_OFF = (2, 1, 3, 0)
SIGN = (1, -1)
NIL = None
BOTH = range(CORES)
RINGS = range(RING)
OTHERS = (1, 3, 2)
LAST = RING - 1
G_ROWS = 8
KINDS = ("first", "second", "first_on", "second_on")
NAMES = (
    "xt", "gain_in", "wkv", "w_in", "w_out", "cos", "sin", "y_out", "kv_out", "h_all", "wi", "wo", "kvh", "kvx", "h_ref",
    "hid", "gain", "gbuf", "xz", "xp",
    "wv", "kvb", "wov", "hb", "joined", "qkv", "stage", "lhs", "away", "acc", "die_in", "in1", "in2", "in3", "in4",
    "xz_send", "xz_recv", "xp_send", "xp_recv", "xd_send", "xd_recv", "x_loc", "g_send", "g_recv", "gd_send", "gd_recv", "yd_send", "yd_recv", "yp_send", "yp_recv", "yz_send", "yz_recv", "y_loc",
    "ag_send", "ag_recv", "ag_dsend", "ag_drecv", "ag_loc", "h_sem", "kvo_sem", "w_load", "far_load", "y_recv", "zb_recv",
    "zc_recv", "w_send", "kz_send", "kz_recv", "ky_send", "ky_recv", "kx_send", "kx_recv", "kd_send", "kd_recv",
    "k_loc", "dsend", "drecv", "send1", "recv1", "send2", "recv2", "send3", "recv3", "send4", "recv4", "kvx_send", "kvx_recv", "kvx_loc",
)


class Refs:
    def __init__(self, refs):
        for name, ref in zip(NAMES, refs, strict=True):
            setattr(self, name, ref)


def model_kernel(*refs):
    r = Refs(refs)
    z, y, x, c = (lax.axis_index(a) for a in ("z", "y", "x", "core"))
    n_layers = r.wkv.shape[0]
    rows, d_model = r.hid.shape
    batch, d_local = r.xt.shape[:2]
    seqs = batch // RING
    seq_len, head_dim = r.cos.shape
    d_row = r.w_in.shape[1]
    e_loc = r.wi.shape[3]
    depth = r.wo.shape[3]
    f_loc = depth - head_dim
    quarter = rows // 4
    width = d_model // RING
    q_block = head_dim * RING
    f_block = f_loc * RING

    def turn(base, off):
        return lax.rem(base + off + RING, RING)

    def remote(src, dst, ssem, rsem, dev):
        return pltpu.make_async_remote_copy(
            src_ref=src, dst_ref=dst, send_sem=ssem, recv_sem=rsem, device_id=dev, device_id_type=pl.DeviceIdType.MESH)

    partner = (z, y, x, 1 - c)

    peers = [(turn(z, o), y, x, c) for o in OTHERS]
    peers += [(z, turn(y, oy), turn(x, ox), c) for oy in RINGS for ox in RINGS if oy or ox]
    peers.append(partner)
    here = (z, y, x, c)
    gate_sem = pltpu.get_barrier_semaphore()
    for dev in peers:
        pl.semaphore_signal(gate_sem, inc=1, device_id=dev, device_id_type=pl.DeviceIdType.MESH)
    pl.semaphore_wait(gate_sem, len(peers))

    def hook(pump, i):
        with jax.named_scope(f"hook_{i}".replace(", ", "_")):
            pump(i)

    def w_cols(kind):
        return pl.ds(0, head_dim + f_loc) if kind == 0 else pl.ds(head_dim + f_loc, f_loc)

    def piece(t, zz, yy):
        l, kind = t // 3, t % 3
        if kind == 2:
            return r.wo.at[l, zz, yy]
        return r.wi.at[l, zz, pl.ds(pl.multiple_of(yy * d_row, d_row), d_row), w_cols(kind)]

    def piece_half(t, zz, yy, h):
        l, kind = t // 3, t % 3
        if kind == 2:
            return r.wo.at[l, zz, yy, pl.ds(h * (depth // 2), depth // 2)]
        return r.wi.at[l, zz, pl.ds(pl.multiple_of(yy * d_row + h * (d_row // 2), d_row // 2), d_row // 2), w_cols(kind)]

    def own_parts(t, owner, zz, yy):
        l, kind = t // 3, t % 3
        hq = pl.ds(pl.multiple_of(owner * head_dim, head_dim), head_dim)
        if kind == 2:
            return [
                (r.w_out.at[l, hq], r.wo.at[l, zz, yy, pl.ds(0, head_dim)]),
                (r.w_out.at[l, pl.ds(pl.multiple_of(q_block + owner * f_loc, head_dim), f_loc)], r.wo.at[l, zz, yy, pl.ds(head_dim, f_loc)]),
            ]
        rws = pl.ds(pl.multiple_of(yy * d_row, d_row), d_row)
        if kind == 0:
            return [
                (r.w_in.at[l, :, hq], r.wi.at[l, zz, rws, pl.ds(0, head_dim)]),
                (r.w_in.at[l, :, pl.ds(pl.multiple_of(q_block + owner * f_loc, head_dim), f_loc)], r.wi.at[l, zz, rws, pl.ds(head_dim, f_loc)]),
            ]
        return [(r.w_in.at[l, :, pl.ds(pl.multiple_of(q_block + f_block + owner * f_loc, head_dim), f_loc)],
                 r.wi.at[l, zz, rws, pl.ds(head_dim + f_loc, f_loc)])]

    def y_send(t):
        for dy in OTHERS:
            owner = turn(y, dy)
            for src, dst in own_parts(t, owner, z, y):
                remote(src, dst, r.w_send.at[t, 0], r.y_recv.at[t, (RING - dy) % RING], (z, owner, x, c)).start()

    def z_own(t):
        for d in BOTH:
            for src, dst in own_parts(t, y, z, y):
                remote(src, dst, r.w_send.at[t, 1], r.zb_recv.at[t, 0, d], (turn(z, SIGN[d]), y, x, c)).start()

    def z_direct(t, j):
        yy = turn(y, j)
        ref = piece(t, z, yy)
        remote(ref, ref, r.w_send.at[t, 0], r.y_recv.at[t, j], here).wait_recv()
        for d in BOTH:
            remote(ref, ref, r.w_send.at[t, 1], r.zb_recv.at[t, j, d], (turn(z, SIGN[d]), y, x, c)).start()

    def z_forward(t, j):
        yy = turn(y, j)
        for d in BOTH:
            zz = turn(z, -SIGN[d])
            ref = piece(t, zz, yy)
            remote(ref, ref, r.w_send.at[t, 1], r.zb_recv.at[t, j, d], here).wait_recv()
            part = piece_half(t, zz, yy, d)
            remote(part, part, r.w_send.at[t, 2], r.zc_recv.at[t, j, d], (turn(z, SIGN[d]), y, x, c)).start()

    def place(t, zz):
        l, kind = t // 3, t % 3
        if kind == 2:
            return r.wo.at[l, zz], r.wov.at[zz]
        return r.wi.at[l, zz, :, w_cols(kind)], r.wv.at[zz, :, w_cols(kind)]

    def load_near(t):
        kind = t % 3
        for d in BOTH:
            src, dst = place(t, turn(z, SIGN[d]))
            pltpu.make_async_copy(src, dst, r.w_load.at[kind]).start()
        for j in OTHERS:
            yy = turn(y, j)
            dst = r.wov.at[z, yy] if kind == 2 else r.wv.at[z, pl.ds(pl.multiple_of(yy * d_row, d_row), d_row), w_cols(kind)]
            pltpu.make_async_copy(piece(t, z, yy), dst, r.w_load.at[kind]).start()
        for src, dst in own_parts(t, y, z, y):
            pltpu.make_async_copy(src, own_place(t, dst, src), r.w_load.at[kind]).start()

    def load_far(t):
        far = turn(z, 2)
        for j in RINGS:
            for d in BOTH:
                part = piece_half(t, far, turn(y, j), d)
                remote(part, part, r.w_send.at[t, 2], r.zc_recv.at[t, j, d], here).wait_recv()
        src, dst = place(t, far)
        pltpu.make_async_copy(src, dst, r.far_load.at[t % 3]).start()

    def own_place(t, dst, src):
        kind = t % 3
        if kind == 2:
            n = src.shape[0]
            return r.wov.at[z, y, pl.ds(0 if n == head_dim and f_loc != head_dim else head_dim, n)]
        n = src.shape[1]
        rws = pl.ds(pl.multiple_of(y * d_row, d_row), d_row)
        if kind == 0:
            return r.wv.at[z, rws, pl.ds(0 if n == head_dim and f_loc != head_dim else head_dim, n)]
        return r.wv.at[z, rws, pl.ds(head_dim + f_loc, f_loc)]

    def finish(t):
        load_near(t)
        load_far(t)

    def near_loaded(t):
        kind = t % 3
        dst = r.wov.at[pl.ds(0, LAST)] if kind == 2 else r.wv.at[pl.ds(0, LAST), :, w_cols(kind)]
        pltpu.make_async_copy(dst, dst, r.w_load.at[kind]).wait()

    def far_loaded(t):
        kind = t % 3
        dst = r.wov.at[0] if kind == 2 else r.wv.at[0, :, w_cols(kind)]
        pltpu.make_async_copy(dst, dst, r.far_load.at[kind]).wait()

    def loaded(t):
        near_loaded(t)
        far_loaded(t)

    def drain(t):
        l, kind = t // 3, t % 3
        if kind == 2:
            refs3 = (r.wo.at[l, 0, pl.ds(0, 3)], r.wo.at[l, pl.ds(0, 2)], r.wo.at[l, 0])
        else:
            cols = w_cols(kind)
            refs3 = (r.wi.at[l, 0, pl.ds(0, 3 * d_row), cols], r.wi.at[l, pl.ds(0, 2), :, cols], r.wi.at[l, 0, :, cols])
        for g in range(3):
            remote(refs3[g], refs3[g], r.w_send.at[t, g], r.y_recv.at[t, 0], here).wait_send()

    def kv_z():
        for i, o in enumerate(OTHERS):
            remote(r.wkv, r.kvh.at[x, c, :, y, z], r.kz_send.at[i], r.kz_recv.at[i], (turn(z, o), y, x, c)).start()
        pltpu.make_async_copy(r.wkv, r.kvh.at[x, c, :, y, z], r.k_loc.at[0]).start()

    def kv_y():
        pltpu.make_async_copy(r.wkv, r.kvh.at[x, c, :, y, z], r.k_loc.at[0]).wait()
        for i, o in enumerate(OTHERS):
            zz = turn(z, -o)
            remote(r.wkv, r.kvh.at[x, c, :, y, zz], r.kz_send.at[i], r.kz_recv.at[i], (turn(z, o), y, x, c)).wait()
        ref = r.kvh.at[x, c, :, y]
        for i, o in enumerate(OTHERS):
            remote(ref, ref, r.ky_send.at[i], r.ky_recv.at[i], (z, turn(y, o), x, c)).start()

    def kv_x():
        for i, o in enumerate(OTHERS):
            ref = r.kvh.at[x, c, :, turn(y, -o)]
            remote(ref, ref, r.ky_send.at[i], r.ky_recv.at[i], (z, turn(y, o), x, c)).wait()
        for l in range(n_layers):
            ref = r.kvh.at[x, c, l]
            for i, o in enumerate(OTHERS):
                remote(ref, ref, r.kx_send.at[l, i], r.kx_recv.at[l, i], (z, y, turn(x, o), c)).start()
            remote(ref, ref, r.kd_send.at[l, 3], r.kd_recv.at[l, 3], partner).start()

    def kv_die(l):
        for i, o in enumerate(OTHERS):
            ref = r.kvh.at[turn(x, -o), c, l]
            remote(ref, ref, r.kx_send.at[l, i], r.kx_recv.at[l, i], (z, y, turn(x, o), c)).wait()
            remote(ref, ref, r.kd_send.at[l, i], r.kd_recv.at[l, i], partner).start()

    def kv_load(l):
        for i, o in enumerate((1, 3, 2, 0)):
            ref = r.kvh.at[turn(x, -o), 1 - c, l]
            remote(ref, ref, r.kd_send.at[l, i], r.kd_recv.at[l, i], partner).wait()
        kc = r.wkv.shape[1]
        for xx in RINGS:
            for cc in BOTH:
                pltpu.make_async_copy(r.kvh.at[xx, cc, l], r.kvb.at[:, :, pl.ds((xx * CORES + cc) * kc, kc)], r.k_loc.at[1]).start()

    def kv_loaded():
        pltpu.make_async_copy(r.kvb, r.kvb, r.k_loc.at[1]).wait()

    def gain_move(i, src, dst, dev):
        return remote(src, dst, r.g_send.at[i], r.g_recv.at[i], dev)

    def gain_z(k):
        dev = (turn(z, OTHERS[k]), y, x, c)
        return gain_move(k, r.gain_in, r.gbuf.at[x, c, y, z], dev)

    def gain_y(k):
        dev = (z, turn(y, OTHERS[k]), x, c)
        return gain_move(len(OTHERS) + k, r.gbuf.at[x, c, y], r.gbuf.at[x, c, y], dev)

    def gain_x(k):
        dev = (z, y, turn(x, OTHERS[k]), c)
        return gain_move(CORES * len(OTHERS) + k, r.gbuf.at[x, c], r.gbuf.at[x, c], dev)

    def gain_die(xx, k):
        ref = r.gbuf.at[xx, c]
        return remote(ref, ref, r.gd_send.at[k], r.gd_recv.at[k], partner)

    def gain_sum():
        for zz in RINGS:
            for yy in RINGS:
                tot = jnp.zeros((n_layers, d_row), F32)
                for xx in RINGS:
                    for cc in BOTH:
                        tot += r.gbuf[xx, cc, yy, zz, :n_layers].astype(F32)
                at = (zz * RING + yy) * d_row
                r.gain[:, at:at + d_row] = tot

    tok_pair = CORES * rows

    def x_z(k):
        zz = turn(z, OTHERS[k])
        src = r.xt.at[pl.ds(zz * seqs, seqs)]
        return remote(src, r.xz.at[z], r.xz_send.at[k], r.xz_recv.at[k], (zz, y, x, c))

    def x_own():
        return pltpu.make_async_copy(r.xt.at[pl.ds(z * seqs, seqs)], r.xz.at[z], r.x_loc)

    def pos(xx):
        return pl.ds(pl.multiple_of(xx * tok_pair, tok_pair), tok_pair)

    def x_plane(oy, ox):
        yy, xx = turn(y, oy), turn(x, ox)
        return remote(r.xz.at[:, yy, :, pos(xx)], r.xp.at[c, y, x], r.xp_send.at[oy], r.xp_recv.at[(RING - oy) % RING], (z, yy, xx, c))

    def row_bytes(oy):
        return r.xp.at[c, 0] if oy else r.xp.at[c, 0, pl.ds(0, RING - 1)]

    def x_row(oy):
        yy = turn(y, oy)
        got = row_bytes(oy)
        remote(got, got, r.xp_send.at[oy], r.xp_recv.at[oy], partner).wait_recv()
        row = r.xp.at[c, yy]
        remote(row, row, r.xd_send.at[oy], r.xd_recv.at[oy], partner).start()

    def x_turn():
        for oy in RINGS:
            row = r.xp.at[1 - c, turn(y, oy)]
            remote(row, row, r.xd_send.at[oy], r.xd_recv.at[oy], partner).wait_recv()

        @pl.loop(0, RING)
        def _(zz):
            for yy in RINGS:
                for xh in BOTH:
                    blk = [r.xp[cc, yy, CORES * xh + xx, zz] for xx in BOTH for cc in BOTH]
                    blk = jnp.concatenate(blk, axis=0).astype(F32).T.astype(BF)
                    n = blk.shape[1]
                    at = pl.multiple_of(zz * RING * d_row + yy * d_row + xh * n, n)
                    r.hb[0, 0, :, :, pl.ds(at, n)] = blk.reshape(CORES, rows, n)
        r.hid[...] = r.hb[0, 0, c]
        for oy in RINGS:
            row = r.xp.at[c, turn(y, oy)]
            remote(row, row, r.xd_send.at[oy], r.xd_recv.at[oy], partner).wait_send()

    def x_sent():
        for fn in (x_z, gain_z, gain_y, gain_x):
            peers_of(fn, "wait_send")
        for k in RINGS:
            gain_die(x, k).wait_send()
        for oy in RINGS:
            got = row_bytes(oy)
            remote(got, got, r.xp_send.at[oy], r.xp_recv.at[oy], partner).wait_send()

    def y_die():
        return remote(r.hid, r.hb.at[0, 0, c], r.yd_send, r.yd_recv, partner)

    def y_plane(oy, ox):
        yy, xx = turn(y, oy), turn(x, ox)
        return remote(r.xp.at[c, yy, xx], r.xz.at[:, y, :, pos(x)], r.yp_send.at[oy], r.yp_recv.at[(RING - oy) % RING], (z, yy, xx, c))

    def y_z(s, oy, k):
        zz = turn(z, OTHERS[k])
        return remote(r.xz.at[zz, s], r.y_out.at[z * seqs + s], r.yz_send.at[oy, k], r.yz_recv.at[oy, k], (zz, y, x, c))

    def y_own(s, oy):
        return pltpu.make_async_copy(r.xz.at[z, s], r.y_out.at[z * seqs + s], r.y_loc.at[oy])

    def leave():
        y_die().start()
        r.hb[0, 0, c] = r.hid[...]
        y_die().wait()

        @pl.loop(0, RING)
        def _(zz):
            for yy in RINGS:
                for xh in BOTH:
                    n = CORES * CORES * d_local
                    at = pl.multiple_of(zz * RING * d_row + yy * d_row + xh * n, n)
                    blk = r.hb[0, 0, :, :, pl.ds(at, n)].reshape(tok_pair, n).astype(F32).T.astype(BF)
                    for xx in BOTH:
                        for cc in BOTH:
                            lo = (xx * CORES + cc) * d_local
                            r.xp[cc, yy, CORES * xh + xx, zz] = blk[lo:lo + d_local]

        for oy in OTHERS + (0,):
            for ox in RINGS:
                if oy or ox:
                    y_plane(oy, ox).start()
        for zz in RINGS:
            r.xz[zz, y, :, pos(x)] = r.xp[c, y, x, zz]
        for oy in OTHERS + (0,):
            yy = turn(y, oy)
            got = row_bytes(oy)
            remote(got, got, r.yp_send.at[oy], r.yp_recv.at[oy], partner).wait_recv()
            for k in range(len(OTHERS)):
                y_z(yy, oy, k).start()
            y_own(yy, oy).start()
        for oy in RINGS:
            got = row_bytes(oy)
            remote(got, got, r.yp_send.at[oy], r.yp_recv.at[oy], partner).wait_send()
            for k in range(len(OTHERS)):
                y_z(turn(y, oy), oy, k).wait()
            y_own(turn(y, oy), oy).wait()

    def kv_rows(zz):
        n = CORES * seq_len // (RING * RING * RING * CORES)
        return pl.ds(pl.multiple_of(((zz * RING + y) * RING + x) * n, n), n)

    def kv_trade(l, k):
        zz = turn(z, OTHERS[k])
        return remote(r.kv_out.at[l, :, :, kv_rows(zz)], r.kvx.at[l, z], r.kvx_send.at[l, k], r.kvx_recv.at[l, k], (zz, y, x, c))

    def kv_keep(l):
        return pltpu.make_async_copy(r.kv_out.at[l, :, :, kv_rows(z)], r.kvx.at[l, z], r.kvx_loc.at[l])

    def kv_share(l):
        for k in range(len(OTHERS)):
            kv_trade(l, k).start()
        kv_keep(l).start()

    def kv_shared(l):
        for k in range(len(OTHERS)):
            kv_trade(l, k).wait()
        kv_keep(l).wait()

    def gather_norm(l, split, pump):
        hid = r.hid
        gain = r.gain[l:l + 1, :]
        for b in range(4):
            blk = hid[b * quarter:(b + 1) * quarter, :].astype(F32)
            mean = jnp.mean(blk, axis=-1, keepdims=True)
            cen = blk - mean
            var = jnp.mean(cen * cen, axis=-1, keepdims=True)
            r.h_ref[b * quarter:(b + 1) * quarter, :] = (cen * lax.rsqrt(var + LN_EPS) * gain).astype(BF)
        out = r.h_all.at[l]

        def spot(q, first, second):
            if q == 0:
                return turn(y, second), turn(x, first)
            return turn(y, first), turn(x, second)

        def span(q, part):
            lo, n = (split, rows - split) if q else (0, split)
            if part is NIL:
                return pl.ds(lo, n)
            return pl.ds(lo + part * (n // 2), n // 2)

        copies = {}

        def ici(key, q, first, second, part, to_first, to_second, own=False):
            sy, sx = spot(q, first, second)
            ty, tx = spot(q, to_first, to_second)
            rws = span(q, part)
            dst = out.at[sy, sx, c, rws]
            kind = KINDS.index(key[0])
            cp = remote(r.h_ref.at[rws] if own else dst, dst, r.ag_send.at[l, kind], r.ag_recv.at[l, len(copies)], (z, ty, tx, c))
            cp.start()
            copies[key] = cp

        def die(q, first, second, own=False):
            sy, sx = spot(q, first, second)
            rws = span(q, NIL)
            dst = out.at[sy, sx, c, rws]
            off = (first if q else second) % RING
            remote(r.h_ref.at[rws] if own else dst, dst, r.ag_dsend.at[l], r.ag_drecv.at[l, off], partner).start()

        offs = (0, -1, 1, 2)
        for q in BOTH:
            for d in BOTH:
                ici(("first", q, d), q, 0, 0, NIL, SIGN[d], 0, own=True)
        for q in BOTH:
            for d in BOTH:
                ici(("second", q, 0, d), q, 0, 0, NIL, 0, SIGN[d], own=True)
        for q in BOTH:
            die(q, 0, 0, own=True)
        own = pltpu.make_async_copy(r.h_ref, out.at[y, x, c], r.ag_loc)
        own.start()
        hook(pump, 0)
        for d in BOTH:
            for q in BOTH:
                copies["first", q, d].wait_recv()
                src = -SIGN[d]
                ici(("first_on", q, d), q, src, 0, d, SIGN[d], 0)
                for e in BOTH:
                    ici(("second", q, 1 + d, e), q, src, 0, NIL, 0, SIGN[e])
                die(q, src, 0)
        hook(pump, 1)
        for d in BOTH:
            for q in BOTH:
                copies["second", q, 0, d].wait_recv()
                src = -SIGN[d]
                ici(("second_on", q, 0, d), q, 0, src, d, 0, SIGN[d])
                die(q, 0, src)
        hook(pump, 2)
        for q in BOTH:
            for d in BOTH:
                copies["first_on", q, d].wait_recv()
            for e in BOTH:
                ici(("second", q, 3, e), q, 2, 0, NIL, 0, SIGN[e])
            die(q, 2, 0)
        hook(pump, 3)
        for k in (1, 2, 3):
            for d in BOTH:
                for q in BOTH:
                    copies["second", q, k, d].wait_recv()
                    src = -SIGN[d]
                    ici(("second_on", q, k, d), q, offs[k], src, d, 0, SIGN[d])
                    die(q, offs[k], src)
            hook(pump, 3 + k)
        for k in range(4):
            for q in BOTH:
                for d in BOTH:
                    copies["second_on", q, k, d].wait_recv()
                die(q, offs[k], 2)
        hook(pump, 7)
        for off in RINGS:
            got = out.at[turn(y, off), :, 1 - c]
            remote(got, got, r.ag_dsend.at[l], r.ag_drecv.at[l, off], partner).wait_recv()
        sent = (out.at[y, x], out.at[y], out.at[y, x, c], out.at[y, pl.ds(0, CORES)])
        for kind, ref in enumerate(sent):
            remote(ref, ref, r.ag_send.at[l, kind], r.ag_recv.at[l, kind], partner).wait_send()
        remote(out.at[pl.ds(0, 2)], out.at[pl.ds(0, 2)], r.ag_dsend.at[l], r.ag_drecv.at[l, 0], partner).wait_send()
        own.wait()

    def h_copy(l, s, slot):
        return pltpu.make_async_copy(r.h_all.at[l, s], r.hb.at[slot], r.h_sem.at[slot])

    def h_tile(slot):
        return r.hb[slot].reshape(seq_len, d_model)

    def project(h, lo, n):
        w = r.wv[:, :, lo:lo + n].reshape(d_model, n)
        return jnp.dot(h, w, preferred_element_type=F32).astype(BF)

    def rope(val):
        val = val.astype(F32)
        return val * r.cos[...] + pltpu.roll(val, head_dim // 2, 1) * r.sin[...]

    n_chunk = min(256, f_loc)

    def kv_out_copy(l, s, slot, i):
        return pltpu.make_async_copy(r.qkv.at[slot, i], r.kv_out.at[l, i, s], r.kvo_sem.at[slot, i])

    def pass_one(l, pump):
        h_copy(l, 0, 0).start()

        @pl.loop(0, RING)
        def _(s):
            slot = lax.rem(s, 2)
            h_copy(l, s, slot).wait()

            @pl.when(s + 1 < RING)
            def _():
                h_copy(l, s + 1, 1 - slot).start()

            pump(s)

            @pl.when(s >= 2)
            def _():
                for i in BOTH:
                    kv_out_copy(l, s - 2, slot, i).wait()

            kv = jnp.zeros((seq_len, 2 * head_dim), F32)
            for zz in RINGS:
                for yy in RINGS:
                    col = (zz * RING + yy) * d_row
                    kv += lax.dot_general(h_cols(slot, col, d_row), r.kvb[yy, zz], (((1,), (1,)), ((), ())), preferred_element_type=F32)
            kv = kv.astype(BF)
            r.qkv[slot, 0] = rope(kv[:, :head_dim]).astype(BF)
            r.qkv[slot, 1] = kv[:, head_dim:]
            for i in BOTH:
                kv_out_copy(l, s, slot, i).start()
            q = project(h_tile(slot), 0, head_dim)
            r.stage[...] = (rope(q) * head_dim ** -0.5).astype(BF)
            for lo in range(0, f_loc, n_chunk):
                r.joined[s, :, head_dim + lo:head_dim + lo + n_chunk] = project(h_tile(slot), head_dim + lo, n_chunk)
            n_tile = seq_len // 2
            for i in BOTH:
                keys = (i + 1) * n_tile
                sc = lax.dot_general(r.stage[i * n_tile:(i + 1) * n_tile, :], r.qkv[slot, 0, :keys, :], (((1,), (1,)), ((), ())), preferred_element_type=F32)
                row_id = lax.broadcasted_iota(jnp.int32, sc.shape, 0) + i * n_tile
                col_id = lax.broadcasted_iota(jnp.int32, sc.shape, 1)
                sc = jnp.where(col_id <= row_id, sc, -1e30)
                top = jnp.max(sc, axis=-1, keepdims=True)
                ex = jnp.exp(sc - top)
                prob = (ex * (1.0 / jnp.sum(ex, axis=-1, keepdims=True))).astype(BF)
                att = jnp.dot(prob, r.qkv[slot, 1, :keys, :], preferred_element_type=F32)
                r.joined[s, i * n_tile:(i + 1) * n_tile, :head_dim] = att.astype(BF)

        for s in (RING - 2, RING - 1):
            for i in BOTH:
                kv_out_copy(l, s, s % 2, i).wait()

    def h_cols(slot, col, n):
        return r.hb[slot, :, :, :, col:col + n].reshape(seq_len, n)

    def pass_two(l, pump):
        h_copy(l, 0, 0).start()

        @pl.loop(0, RING)
        def _(s):
            slot = lax.rem(s, 2)
            h_copy(l, s, slot).wait()

            @pl.when(s + 1 < RING)
            def _():
                h_copy(l, s + 1, 1 - slot).start()

            pump(s)
            for lo in range(0, f_loc, n_chunk):
                up = project(h_tile(slot), head_dim + f_loc + lo, n_chunk).astype(F32)
                cols = slice(head_dim + lo, head_dim + lo + n_chunk)
                g = r.joined[s, :, cols].astype(F32)
                r.joined[s, :, cols] = (g * jax.nn.sigmoid(g) * up).astype(BF)

    def out_scatter(l, pump):
        def peer(q, first, second):
            dy = first * (1 - q) + second * q
            dx = first * q + second * (1 - q)
            return (z, turn(y, dy), turn(x, dx), c)

        def die_copy(ch, q, s):
            return remote(r.away.at[q], r.die_in.at[ch, q, s], r.dsend.at[l, ch, q, s], r.drecv.at[l, ch, q, s], partner)

        def first_copy(ch, q, d):
            return remote(r.acc.at[ch, q, 0, pl.ds(CORES * d, CORES)], r.in1.at[ch, q, d], r.send1.at[l, ch, q, d], r.recv1.at[l, ch, q, d],
                          peer(q, SIGN[d], 0))

        def second_copy(ch, q, d, h):
            js = pl.ds(CORES * h, CORES)
            return remote(r.acc.at[ch, q, 1 + d, js], r.in2.at[ch, q, d, js], r.send2.at[l, ch, q, d, h], r.recv2.at[l, ch, q, d, h],
                          peer(q, SIGN[d], 0))

        def half_rows(d):
            return pl.ds(d * (rows // 2), rows // 2)

        def third_copy(ch, q, d):
            return remote(r.acc.at[ch, q, LAST, 0, half_rows(d)], r.in3.at[ch, q, d], r.send3.at[l, ch, q, d], r.recv3.at[l, ch, q, d],
                          peer(q, 0, SIGN[d]))

        def fourth_copy(ch, q, d):
            return remote(r.acc.at[ch, q, LAST, 1 + d], r.in4.at[ch, q, d], r.send4.at[l, ch, q, d], r.recv4.at[l, ch, q, d],
                          peer(q, 0, SIGN[d]))

        n_blk = r.wov.shape[3]

        def plane_of(ch, q):
            return turn(z, LAST - q if ch else q)

        def tile(ch, q, s):
            for cc in BOTH:
                for j in RINGS:
                    oy = SLOT_OFF[s] * (1 - q) + SLOT_OFF[j] * q
                    ox = SLOT_OFF[j] * (1 - q) + SLOT_OFF[s] * q
                    core = c if cc else 1 - c
                    at = pl.multiple_of((turn(x, ox) * CORES + core) * rows, rows)
                    r.lhs[pl.ds((cc * RING + j) * rows, rows), :] = r.joined[turn(y, oy), pl.ds(at, rows), :]
            left = r.lhs[...]
            zz = plane_of(ch, q)

            @pl.loop(0, RING)
            def _(n):
                col = pl.multiple_of(n * n_blk, n_blk)
                res = jnp.dot(left, r.wov[zz, n], preferred_element_type=F32).astype(BF)
                res = res.reshape(CORES, RING, rows, n_blk)
                r.away[q, :, :, pl.ds(col, n_blk)] = res[0]
                r.acc[ch, q, s, :, :, pl.ds(col, n_blk)] = res[1]

        def pair_sum(ch, q, s):
            die_copy(ch, q, s).wait_recv()

            @pl.loop(0, RING)
            def _(j):
                r.acc[ch, q, s, j] = r.acc[ch, q, s, j] + r.die_in[ch, q, s, j]

        def stage_a(ch):
            for s in RINGS:
                @pl.loop(0, CORES)
                def _(q, s=s):
                    if s:
                        die_copy(ch, q, s - 1).wait_send()
                    elif ch:
                        die_copy(ch - 1, q, LAST).wait_send()
                    tile(ch, q, s)
                    die_copy(ch, q, s).start()
                    if s:
                        pair_sum(ch, q, s - 1)
                    if s == 1:
                        for d in BOTH:
                            first_copy(ch, q, d).start()
                    if s > 1:
                        second_copy(ch, q, s - 2, LAST - s).start()
                if s == 1:
                    hook(pump, ("a", ch))

        def stage_b(ch):
            for q in BOTH:
                pair_sum(ch, q, LAST)
            for q in BOTH:
                for d in BOTH:
                    first_copy(ch, q, d).wait_recv()
                    for j in BOTH:
                        at = CORES * d + j
                        r.acc[ch, q, 1 + d, at] = r.acc[ch, q, 1 + d, at] + r.in1[ch, q, d, j]
                    second_copy(ch, q, d, d).start()

        def total(ch, q, j):
            val = r.acc[ch, q, LAST, j].astype(F32)
            for d in BOTH:
                val += r.in2[ch, q, d, j].astype(F32)
            r.acc[ch, q, LAST, j] = val.astype(BF)

        def stage_c(ch):
            for q in BOTH:
                for h in BOTH:
                    for d in BOTH:
                        second_copy(ch, q, d, h).wait_recv()
                total(ch, q, 0)
                for d in BOTH:
                    third_copy(ch, q, d).start()
                for j in RINGS[1:]:
                    total(ch, q, j)

        def stage_d(ch):
            for q in BOTH:
                for d in BOTH:
                    third_copy(ch, q, d).wait_recv()
                    rws = half_rows(d)
                    r.acc[ch, q, LAST, 1 + d, rws] = r.acc[ch, q, LAST, 1 + d, rws] + r.in3[ch, q, d]
                    fourth_copy(ch, q, d).start()

        def stage_e(ch):
            for q in BOTH:
                for d in BOTH:
                    fourth_copy(ch, q, d).wait_recv()
                cols = pl.ds(pl.multiple_of(plane_of(ch, q) * width, width), width)
                upd = r.acc[ch, q, LAST, LAST].astype(F32)
                for d in BOTH:
                    upd += r.in4[ch, q, d].astype(F32)
                upd = upd.astype(BF)
                r.hid[:, cols] = (r.hid[:, cols].astype(F32) + upd.astype(F32)).astype(BF)

        def sent(ch):
            for q in BOTH:
                if ch:
                    die_copy(ch, q, LAST).wait_send()
                for d in BOTH:
                    for cp in (first_copy, third_copy, fourth_copy):
                        cp(ch, q, d).wait_send()
                    for h in BOTH:
                        second_copy(ch, q, d, h).wait_send()

        for step, fn, ch in (
            ("a0", stage_a, 0), ("b0", stage_b, 0), ("a1", stage_a, 1), ("c0", stage_c, 0), ("b1", stage_b, 1),
            ("d0", stage_d, 0), ("e0", stage_e, 0), ("c1", stage_c, 1), ("d1", stage_d, 1), ("e1", stage_e, 1),
        ):
            with jax.named_scope(step):
                fn(ch)
            hook(pump, step)
        for ch in BOTH:
            sent(ch)

    def near(fn, t):
        for j in (LAST, 1):
            fn(t, j)

    def far(fn, t):
        fn(t, 2)

    def z_all(t):
        near(z_direct, t)
        far(z_direct, t)

    def peers_of(fn, op="start"):
        for k in range(len(OTHERS)):
            getattr(fn(k), op)()

    def when_j(s, fn):
        @pl.when(s < 3)
        def _():
            fn(s + 1)

    def start():
        peers_of(gain_z)
        peers_of(x_z)
        x_own().start()
        r.gbuf[x, c, y, z] = r.gain_in[...]
        z_own(0)
        z_own(1)
        with jax.named_scope("gain_a"):
            peers_of(gain_z, "wait_recv")
            peers_of(gain_y)
            peers_of(gain_y, "wait_recv")
            peers_of(gain_x)
            gain_die(x, LAST).start()
        with jax.named_scope("x_z"):
            peers_of(x_z, "wait_recv")
            x_own().wait()
        for oy in RINGS:
            for ox in RINGS:
                if oy or ox:
                    x_plane(oy, ox).start()
        r.xp[c, y, x] = r.xz[:, y, :, pos(x)]
        kv_z()
        with jax.named_scope("gain_b"):
            for k, o in enumerate(OTHERS):
                gain_x(k).wait_recv()
                gain_die(turn(x, -o), k).start()
        with jax.named_scope("z_f"):
            z_forward(0, 0)
        with jax.named_scope("rows"):
            for oy in (0, LAST, 1, 2):
                x_row(oy)
        y_send(0)
        with jax.named_scope("z_g"):
            z_forward(1, 0)
            z_own(2)
        with jax.named_scope("gain_sum"):
            for k in RINGS:
                gain_die(x, k).wait_recv()
            gain_sum()
        with jax.named_scope("turn"):
            x_turn()

    def ag0(i):
        if i == 1:
            kv_y()
        if i == 2:
            with jax.named_scope("from_before"):
                z_direct(0, LAST)
            with jax.named_scope("from_after"):
                z_direct(0, 1)
        if i == 3:
            with jax.named_scope("from_far"):
                far(z_direct, 0)
            y_send(1)
            kv_x()
        if i == 4:
            near(z_forward, 0)
        if i == 5:
            far(z_forward, 0)
            with jax.named_scope("from_before"):
                z_direct(1, LAST)
            with jax.named_scope("from_after"):
                z_direct(1, 1)
        if i == 6:
            with jax.named_scope("from_far"):
                far(z_direct, 1)
            kv_die(0)
        if i == 7:
            y_send(2)
            finish(0)
            kv_load(0)
            near(z_forward, 1)

    def rs0(i):
        if i == ("a", 0):
            load_far(2)
        if i == "b0":
            far_loaded(2)
            z_all(3)
            y_send(4)
        if i == "a1":
            z_forward(3, 0)
            near(z_forward, 3)
        if i == "c0":
            far(z_forward, 3)
            z_own(4)
        if i == "b1":
            z_all(4)
        if i == "e0":
            z_forward(4, 0)
            near(z_forward, 4)
            kv_die(1)
        if i == "c1":
            far(z_forward, 4)
            finish(3)
            kv_load(1)

    def ag1(i):
        if i == 0:
            y_send(5)
            z_own(5)
        if i == 3:
            z_all(5)
        if i == 4:
            finish(4)
        if i == 5:
            z_forward(5, 0)
            near(z_forward, 5)
        if i == 6:
            far(z_forward, 5)

    def nothing(i):
        pass

    with jax.named_scope("start"):
        start()
    with jax.named_scope("gather_0"):
        gather_norm(0, rows // RING, ag0)
    with jax.named_scope("wait_w0"):
        loaded(0)
        kv_loaded()
        far(z_forward, 1)
        x_sent()
    with jax.named_scope("pass_one_0"):
        pass_one(0, lambda s: when_j(s, lambda j: z_direct(2, j)))
    with jax.named_scope("finish_1"):
        kv_share(0)
        finish(1)
        z_own(3)
        y_send(3)
        loaded(1)
    with jax.named_scope("pass_two_0"):
        pass_two(0, lambda s: z_forward(2, s))
    with jax.named_scope("near_2"):
        load_near(2)
        near_loaded(2)
    with jax.named_scope("scatter_0"):
        out_scatter(0, rs0)
    with jax.named_scope("gather_1"):
        gather_norm(1, rows // 2, ag1)
    with jax.named_scope("wait_w3"):
        loaded(3)
        kv_loaded()
    with jax.named_scope("pass_one_1"):
        pass_one(1, nothing)
    with jax.named_scope("finish_5"):
        kv_share(1)
        loaded(4)
        finish(5)
    with jax.named_scope("pass_two_1"):
        pass_two(1, nothing)
    with jax.named_scope("wait_w5"):
        loaded(5)
    with jax.named_scope("scatter_1"):
        out_scatter(1, nothing)
    with jax.named_scope("leave"):
        leave()
    with jax.named_scope("drain"):
        for t in range(3 * n_layers):
            drain(t)
        for l in range(n_layers):
            kv_shared(l)


def run_model(xt, gain, wkv_t, w_in, w_out, cos_full, sin_full):
    batch, d_local, seq_len = xt.shape
    n_layers, d_row, e_block = w_in.shape
    r_block, d_col = w_out.shape[1:]
    head_dim = cos_full.shape[1]
    d_model = d_row * RING * RING
    seqs = batch // RING
    rows = seqs * seq_len // (RING * RING * CORES)
    e_loc, r_loc = e_block // RING, r_block // RING
    kc = wkv_t.shape[1]
    width = d_model // RING
    g_rows = gain.shape[0]
    n_t = 3 * n_layers
    n_o = len(OTHERS)

    def dma(*shape):
        return pltpu.SemaphoreType.DMA(shape)

    def vm(*shape):
        return pltpu.VMEM(shape, BF)

    def out(*shape):
        return jax.ShapeDtypeStruct(shape, BF)

    any_spec = pl.BlockSpec(memory_space=pl.ANY)
    vm_spec = pl.BlockSpec(memory_space=pltpu.VMEM)
    out_shape = [
        out(batch, d_local, seq_len),
        out(n_layers, 2, seqs, seq_len, head_dim),
        out(n_layers, RING, RING, CORES, rows, d_model),
        out(n_layers, RING, RING * d_row, e_loc),
        out(n_layers, RING, RING, r_loc, d_col),
        out(RING, CORES, n_layers, RING, RING, kc, d_row),
        out(n_layers, RING, 2, seqs, CORES * (seq_len // (CORES * RING * RING * RING)), head_dim),
    ]
    pair = (2, 2, 2)
    each = (n_layers, *pair)
    scratch = [
        vm(rows, d_model), vm(rows, d_model), pltpu.VMEM((n_layers, d_model), F32),
        vm(RING, CORES, RING, RING, g_rows, d_row),
        vm(RING, seqs, d_local, seq_len),
        vm(CORES, RING, RING, RING, d_local, CORES * rows),
        vm(RING, RING * d_row, e_loc), vm(RING, RING, 2 * head_dim, d_row), vm(RING, RING, r_loc, d_col),
        vm(2, RING, CORES, rows, d_model), vm(RING, seq_len, r_loc), vm(2, 2, seq_len, head_dim), vm(seq_len, head_dim),
        vm(CORES * RING * rows, r_loc), vm(2, RING, rows, width), vm(2, 2, RING, RING, rows, width), vm(2, 2, RING, RING, rows, width),
        vm(*pair, 2, rows, width), vm(*pair, RING, rows, width), vm(*pair, rows // 2, width), vm(*pair, rows, width),
        dma(n_o), dma(n_o), dma(RING), dma(RING), dma(RING), dma(RING), pltpu.SemaphoreType.DMA,
        dma(3 * n_o), dma(3 * n_o), dma(RING), dma(RING),
        pltpu.SemaphoreType.DMA, pltpu.SemaphoreType.DMA, dma(RING), dma(RING), dma(RING, n_o), dma(RING, n_o), dma(RING),
        dma(n_layers, RING), dma(n_layers, 40), dma(n_layers), dma(n_layers, RING), pltpu.SemaphoreType.DMA, dma(2), dma(2, 2), dma(3), dma(3),
        dma(n_t, RING), dma(n_t, RING, 2), dma(n_t, RING, 2), dma(n_t, 3),
        dma(n_o), dma(n_o), dma(n_o), dma(n_o), dma(n_layers, n_o), dma(n_layers, n_o), dma(n_layers, RING), dma(n_layers, RING), dma(2),
        dma(n_layers, 2, 2, RING), dma(n_layers, 2, 2, RING),
        dma(*each), dma(*each), dma(*each, 2), dma(*each, 2), dma(*each), dma(*each), dma(*each), dma(*each),
        dma(n_layers, n_o), dma(n_layers, n_o), dma(n_layers),
    ]
    res = pl.pallas_call(
        model_kernel,
        out_shape=out_shape,
        in_specs=[any_spec, vm_spec, vm_spec, any_spec, any_spec, vm_spec, vm_spec],
        out_specs=[any_spec] * len(out_shape),
        scratch_shapes=scratch,
        compiler_params=pltpu.CompilerParams(collective_id=0, has_side_effects=True, vmem_limit_bytes=VMEM_LIMIT),
        name="two_layers",
    )(xt, gain, wkv_t, w_in, w_out, cos_full, sin_full)
    return res[0], res[-1]


def solution(mesh):
    row_size = mesh.shape["row"]
    n_col = mesh.shape["col"]
    n_z = row_size // RING
    n_y = RING
    n_x = n_col // CORES
    n_tp = n_y * n_col
    n_dev = row_size * n_col
    mesh4 = Mesh(mesh.devices.reshape(n_z, n_y, n_x, CORES), ("z", "y", "x", "core"))
    every = ("z", "y", "x", "core")
    col = ("x", "core")
    act_spec = P(NIL, NIL, every)
    w_spec = P(NIL, ("z", "y"), col)

    def device_fn(x_loc, gain_loc, w_in_loc, w_kv_loc, w_out_loc):
        n_layers = w_in_loc.shape[0]
        n_batch, seq_len, d_local = x_loc.shape
        head_dim = w_kv_loc.shape[2] * n_col // 2
        batch_loc = n_batch // n_z
        seq_local = seq_len // n_dev
        steps = np.arange(head_dim // 2, dtype=np.float32)
        inv_freq = (1.0 / 10000.0 ** (steps * 2 / head_dim)).astype(np.float32)
        angles = np.arange(seq_len, dtype=np.float32)[:, NIL] * inv_freq[NIL, :]
        cos_tab, sin_tab = np.cos(angles), np.sin(angles)
        cos_full = jnp.asarray(np.concatenate([cos_tab, cos_tab], axis=1))
        sin_full = jnp.asarray(np.concatenate([-sin_tab, sin_tab], axis=1))
        spot = lax.axis_index("x") * CORES + lax.axis_index("core")
        own = lax.broadcasted_iota(jnp.int32, (n_layers, n_col, d_local), 1) == spot
        gains = jnp.where(own, gain_loc[:, NIL, :], 0).astype(BF).reshape(n_layers, n_col * d_local)
        gains = jnp.pad(gains, ((0, G_ROWS - n_layers), (0, 0)))
        y_loc, kv = run_model(x_loc.transpose(0, 2, 1), gains, w_kv_loc.transpose(0, 2, 1), w_in_loc, w_out_loc, cos_full, sin_full)
        y_loc = y_loc.transpose(0, 2, 1)
        kv = kv.reshape(n_layers, n_z, 2, batch_loc, CORES, seq_local, head_dim)
        kv = lax.dynamic_index_in_dim(kv, lax.axis_index("core"), axis=4, keepdims=False)
        kv = kv.transpose(0, 2, 1, 3, 4, 5).reshape(n_layers, 2, n_batch, seq_local, head_dim)
        return y_loc, kv

    return jax.shard_map(device_fn, mesh=mesh4, in_specs=(act_spec, P(NIL, every), w_spec, w_spec, P(NIL, col, ("z", "y"))), out_specs=(act_spec, P(NIL, NIL, NIL, every, NIL)), check_vma=False)
```

```python
import jax
import jax.numpy as jnp
import numpy as np
from jax import lax
from jax.experimental import pallas as pl
from jax.experimental.pallas import tpu as pltpu
from jax.sharding import Mesh
from jax.sharding import PartitionSpec as P

LN_EPS = 1e-6
RING = 4
CORES = 2
VMEM_LIMIT = 67_000_000
BF = jnp.bfloat16
F32 = jnp.float32
SLOT_OFF = (2, 1, 3, 0)
SIGN = (1, -1)
NIL = None
BOTH = range(CORES)
RINGS = range(RING)
OTHERS = (1, 3, 2)
LAST = RING - 1
G_ROWS = 8
KINDS = ("first", "second", "first_on", "second_on")
NAMES = (
    "xt", "gain_in", "wkv", "w_in", "w_out", "cos", "sin", "y_out", "kv_out", "h_all", "wi", "wo", "kvh", "kvx", "rwi", "rwo", "h_ref",
    "hid", "gain", "gbuf", "xz", "xp",
    "wv", "kvb", "wov", "hb", "joined", "qkv", "stage", "lhs", "away", "acc", "die_in", "in1", "in2", "in3", "in4",
    "xz_send", "xz_recv", "xp_send", "xp_recv", "xd_send", "xd_recv", "x_loc", "g_send", "g_recv", "gd_send", "gd_recv", "yd_send", "yd_recv", "yp_send", "yp_recv", "yz_send", "yz_recv", "y_loc",
    "ag_send", "ag_recv", "ag_dsend", "ag_drecv", "ag_loc", "h_sem", "kvo_sem", "w_load", "far_load", "y_recv", "ry_recv", "zb_recv",
    "zc_recv", "w_send", "kz_send", "kz_recv", "ky_send", "ky_recv", "kx_send", "kx_recv", "kd_send", "kd_recv",
    "k_loc", "dsend", "drecv", "send1", "recv1", "send2", "recv2", "send3", "recv3", "send4", "recv4", "kvx_send", "kvx_recv", "kvx_loc",
)


class Refs:
    def __init__(self, refs):
        for name, ref in zip(NAMES, refs, strict=True):
            setattr(self, name, ref)


def model_kernel(*refs):
    r = Refs(refs)
    z, y, x, c = (lax.axis_index(a) for a in ("z", "y", "x", "core"))
    n_layers = r.wkv.shape[0]
    rows, d_model = r.hid.shape
    batch, d_local = r.xt.shape[:2]
    seqs = batch // RING
    seq_len, head_dim = r.cos.shape
    d_row = r.w_in.shape[1]
    e_loc = r.wi.shape[3]
    depth = r.wo.shape[3]
    f_loc = depth - head_dim
    quarter = rows // 4
    width = d_model // RING
    q_block = head_dim * RING
    f_block = f_loc * RING

    def turn(base, off):
        return lax.rem(base + off + RING, RING)

    def remote(src, dst, ssem, rsem, dev):
        return pltpu.make_async_remote_copy(
            src_ref=src, dst_ref=dst, send_sem=ssem, recv_sem=rsem, device_id=dev, device_id_type=pl.DeviceIdType.MESH)

    partner = (z, y, x, 1 - c)

    peers = [(turn(z, o), y, x, c) for o in OTHERS]
    peers += [(z, turn(y, oy), turn(x, ox), c) for oy in RINGS for ox in RINGS if oy or ox]
    peers.append(partner)
    here = (z, y, x, c)
    gate_sem = pltpu.get_barrier_semaphore()
    for dev in peers:
        pl.semaphore_signal(gate_sem, inc=1, device_id=dev, device_id_type=pl.DeviceIdType.MESH)
    pl.semaphore_wait(gate_sem, len(peers))

    def hook(pump, i):
        with jax.named_scope(f"hook_{i}".replace(", ", "_")):
            pump(i)

    def w_cols(kind):
        return pl.ds(0, head_dim + f_loc) if kind == 0 else pl.ds(head_dim + f_loc, f_loc)

    def piece(t, zz, yy):
        l, kind = t // 3, t % 3
        if kind == 2:
            return r.wo.at[l, zz, yy]
        return r.wi.at[l, zz, pl.ds(pl.multiple_of(yy * d_row, d_row), d_row), w_cols(kind)]

    def piece_half(t, zz, yy, h):
        l, kind = t // 3, t % 3
        if kind == 2:
            return r.wo.at[l, zz, yy, pl.ds(h * (depth // 2), depth // 2)]
        return r.wi.at[l, zz, pl.ds(pl.multiple_of(yy * d_row + h * (d_row // 2), d_row // 2), d_row // 2), w_cols(kind)]

    def own_parts(t, owner, zz, yy):
        l, kind = t // 3, t % 3
        hq = pl.ds(pl.multiple_of(owner * head_dim, head_dim), head_dim)
        if kind == 2:
            return [
                (r.w_out.at[l, hq], r.wo.at[l, zz, yy, pl.ds(0, head_dim)]),
                (r.w_out.at[l, pl.ds(pl.multiple_of(q_block + owner * f_loc, head_dim), f_loc)], r.wo.at[l, zz, yy, pl.ds(head_dim, f_loc)]),
            ]
        rws = pl.ds(pl.multiple_of(yy * d_row, d_row), d_row)
        if kind == 0:
            return [
                (r.w_in.at[l, :, hq], r.wi.at[l, zz, rws, pl.ds(0, head_dim)]),
                (r.w_in.at[l, :, pl.ds(pl.multiple_of(q_block + owner * f_loc, head_dim), f_loc)], r.wi.at[l, zz, rws, pl.ds(head_dim, f_loc)]),
            ]
        return [(r.w_in.at[l, :, pl.ds(pl.multiple_of(q_block + f_block + owner * f_loc, head_dim), f_loc)],
                 r.wi.at[l, zz, rws, pl.ds(head_dim + f_loc, f_loc)])]

    def relay_ref(t, d):
        l, kind = t // 3, t % 3
        return r.rwo.at[l, d] if kind == 2 else r.rwi.at[l, d, :, w_cols(kind)]

    def far_parts(t, d):
        l, kind = t // 3, t % 3
        owner = turn(y, 2)
        hq = pl.ds(pl.multiple_of(owner * head_dim, head_dim), head_dim)
        if kind == 2:
            n = depth // 2
            base = q_block + owner * f_loc
            if d:
                return [(r.w_out.at[l, pl.ds(pl.multiple_of(base + n - head_dim, G_ROWS), n)], r.rwo.at[l, d])]
            return [
                (r.w_out.at[l, hq], r.rwo.at[l, d, pl.ds(0, head_dim)]),
                (r.w_out.at[l, pl.ds(pl.multiple_of(base, head_dim), n - head_dim)], r.rwo.at[l, d, pl.ds(head_dim, n - head_dim)]),
            ]
        rws = pl.ds(d * (d_row // 2), d_row // 2)
        if kind == 0:
            return [
                (r.w_in.at[l, rws, hq], r.rwi.at[l, d, :, pl.ds(0, head_dim)]),
                (r.w_in.at[l, rws, pl.ds(pl.multiple_of(q_block + owner * f_loc, head_dim), f_loc)], r.rwi.at[l, d, :, pl.ds(head_dim, f_loc)]),
            ]
        return [(r.w_in.at[l, rws, pl.ds(pl.multiple_of(q_block + f_block + owner * f_loc, head_dim), f_loc)], relay_ref(t, d))]

    def y_send(t):
        for d in BOTH:
            owner = turn(y, SIGN[d])
            dev = (z, owner, x, c)
            for src, dst in far_parts(t, d):
                remote(src, dst, r.w_send.at[t, 0], r.ry_recv.at[t, d], dev).start()
            for src, dst in own_parts(t, owner, z, y):
                remote(src, dst, r.w_send.at[t, 0], r.y_recv.at[t, -SIGN[d] % RING], dev).start()

    def y_relay(t):
        for d in BOTH:
            ref = relay_ref(t, d)
            remote(ref, ref, r.w_send.at[t, 3], r.ry_recv.at[t, d], here).wait_recv()
            dst = piece_half(t, z, turn(y, -SIGN[d]), d)
            remote(ref, dst, r.w_send.at[t, 3], r.y_recv.at[t, 2], (z, turn(y, SIGN[d]), x, c)).start()

    def z_own(t):
        for d in BOTH:
            for src, dst in own_parts(t, y, z, y):
                remote(src, dst, r.w_send.at[t, 1], r.zb_recv.at[t, 0, d], (turn(z, SIGN[d]), y, x, c)).start()

    def z_direct(t, j):
        yy = turn(y, j)
        ref = piece(t, z, yy)
        remote(ref, ref, r.w_send.at[t, 0], r.y_recv.at[t, j], here).wait_recv()
        for d in BOTH:
            remote(ref, ref, r.w_send.at[t, 1], r.zb_recv.at[t, j, d], (turn(z, SIGN[d]), y, x, c)).start()

    def z_forward(t, j):
        yy = turn(y, j)
        for d in BOTH:
            zz = turn(z, -SIGN[d])
            ref = piece(t, zz, yy)
            remote(ref, ref, r.w_send.at[t, 1], r.zb_recv.at[t, j, d], here).wait_recv()
            part = piece_half(t, zz, yy, d)
            remote(part, part, r.w_send.at[t, 2], r.zc_recv.at[t, j, d], (turn(z, SIGN[d]), y, x, c)).start()

    def place(t, zz):
        l, kind = t // 3, t % 3
        if kind == 2:
            return r.wo.at[l, zz], r.wov.at[zz]
        return r.wi.at[l, zz, :, w_cols(kind)], r.wv.at[zz, :, w_cols(kind)]

    def load_near(t):
        kind = t % 3
        for d in BOTH:
            src, dst = place(t, turn(z, SIGN[d]))
            pltpu.make_async_copy(src, dst, r.w_load.at[kind]).start()
        for j in OTHERS:
            yy = turn(y, j)
            dst = r.wov.at[z, yy] if kind == 2 else r.wv.at[z, pl.ds(pl.multiple_of(yy * d_row, d_row), d_row), w_cols(kind)]
            pltpu.make_async_copy(piece(t, z, yy), dst, r.w_load.at[kind]).start()
        for src, dst in own_parts(t, y, z, y):
            pltpu.make_async_copy(src, own_place(t, dst, src), r.w_load.at[kind]).start()

    def load_far(t):
        far = turn(z, 2)
        for j in RINGS:
            for d in BOTH:
                part = piece_half(t, far, turn(y, j), d)
                remote(part, part, r.w_send.at[t, 2], r.zc_recv.at[t, j, d], here).wait_recv()
        src, dst = place(t, far)
        pltpu.make_async_copy(src, dst, r.far_load.at[t % 3]).start()

    def own_place(t, dst, src):
        kind = t % 3
        if kind == 2:
            n = src.shape[0]
            return r.wov.at[z, y, pl.ds(0 if n == head_dim and f_loc != head_dim else head_dim, n)]
        n = src.shape[1]
        rws = pl.ds(pl.multiple_of(y * d_row, d_row), d_row)
        if kind == 0:
            return r.wv.at[z, rws, pl.ds(0 if n == head_dim and f_loc != head_dim else head_dim, n)]
        return r.wv.at[z, rws, pl.ds(head_dim + f_loc, f_loc)]

    def finish(t):
        load_near(t)
        load_far(t)

    def near_loaded(t):
        kind = t % 3
        dst = r.wov.at[pl.ds(0, LAST)] if kind == 2 else r.wv.at[pl.ds(0, LAST), :, w_cols(kind)]
        pltpu.make_async_copy(dst, dst, r.w_load.at[kind]).wait()

    def far_loaded(t):
        kind = t % 3
        dst = r.wov.at[0] if kind == 2 else r.wv.at[0, :, w_cols(kind)]
        pltpu.make_async_copy(dst, dst, r.far_load.at[kind]).wait()

    def loaded(t):
        near_loaded(t)
        far_loaded(t)

    def drain(t):
        l, kind = t // 3, t % 3
        if kind == 2:
            done = (r.wo.at[l, 0, pl.ds(0, LAST)], r.wo.at[l, pl.ds(0, 2)], r.wo.at[l, 0], r.wo.at[l, 0, 0])
        else:
            cols = w_cols(kind)
            done = (r.wi.at[l, 0, pl.ds(0, LAST * d_row), cols], r.wi.at[l, pl.ds(0, 2), :, cols], r.wi.at[l, 0, :, cols],
                    r.wi.at[l, 0, pl.ds(0, d_row), cols])
        for g, ref in enumerate(done):
            remote(ref, ref, r.w_send.at[t, g], r.y_recv.at[t, 0], here).wait_send()

    def kv_z_copy(k):
        return remote(r.wkv, r.kvh.at[x, c, :, y, z], r.kz_send.at[k], r.kz_recv.at[k], (turn(z, OTHERS[k]), y, x, c))

    def kv_own():
        return pltpu.make_async_copy(r.wkv, r.kvh.at[x, c, :, y, z], r.k_loc.at[0])

    def kv_z():
        for k in range(len(OTHERS)):
            kv_z_copy(k).start()
        kv_own().start()

    def kv_y_copy(ref, k, d):
        return remote(ref, ref, r.ky_send, r.ky_recv.at[k], (z, turn(y, SIGN[d]), x, c))

    def kv_y1():
        kv_own().wait()
        for k in range(len(OTHERS)):
            kv_z_copy(k).wait()
        for d in BOTH:
            kv_y_copy(r.kvh.at[x, c, :, y], d, d).start()

    def kv_y2():
        for d in BOTH:
            yy = turn(y, -SIGN[d])
            kv_y_copy(r.kvh.at[x, c, :, yy], d, d).wait_recv()
            kv_y_copy(r.kvh.at[x, c, :, yy, pl.ds(2 * d, 2)], 2, d).start()

    def kv_y3():
        kv_y_copy(r.kvh.at[x, c, :, turn(y, 2)], 2, 0).wait_recv()
        kv_y_copy(r.kvh.at[x, c, :, pl.ds(0, LAST)], 0, 0).wait_send()

    def kv_x_copy(l, ref, k, d):
        return remote(ref, ref, r.kx_send.at[l], r.kx_recv.at[l, k], (z, y, turn(x, SIGN[d]), c))

    def kv_die(l, ref):
        return remote(ref, ref, r.kd_send.at[l], r.kd_recv.at[l], partner)

    def kv_x1(l):
        ref = r.kvh.at[x, c, l]
        for d in BOTH:
            kv_x_copy(l, ref, d, d).start()
        kv_die(l, ref).start()

    def kv_x2(l):
        for d in BOTH:
            xx = turn(x, -SIGN[d])
            ref = r.kvh.at[xx, c, l]
            kv_x_copy(l, ref, d, d).wait_recv()
            kv_x_copy(l, r.kvh.at[xx, c, l, pl.ds(2 * d, 2)], 2, d).start()
            kv_die(l, ref).start()

    def kv_x3(l):
        ref = r.kvh.at[turn(x, 2), c, l]
        kv_x_copy(l, ref, 2, 0).wait_recv()
        kv_die(l, ref).start()

    def kv_load(l):
        kv_die(l, r.kvh.at[:, 1 - c, l]).wait_recv()
        kc = r.wkv.shape[1]
        for xx in RINGS:
            for cc in BOTH:
                pltpu.make_async_copy(r.kvh.at[xx, cc, l], r.kvb.at[:, :, pl.ds((xx * CORES + cc) * kc, kc)], r.k_loc.at[1]).start()

    def kv_sent(l):
        kv_x_copy(l, r.kvh.at[pl.ds(0, LAST), c, l], 0, 0).wait_send()
        kv_die(l, r.kvh.at[:, c, l]).wait_send()

    def kv_loaded():
        pltpu.make_async_copy(r.kvb, r.kvb, r.k_loc.at[1]).wait()

    def gain_move(i, src, dst, dev):
        return remote(src, dst, r.g_send.at[i], r.g_recv.at[i], dev)

    def gain_z(k):
        dev = (turn(z, OTHERS[k]), y, x, c)
        return gain_move(k, r.gain_in, r.gbuf.at[x, c, y, z], dev)

    def gain_y(k):
        dev = (z, turn(y, OTHERS[k]), x, c)
        return gain_move(len(OTHERS) + k, r.gbuf.at[x, c, y], r.gbuf.at[x, c, y], dev)

    def gain_x(k):
        dev = (z, y, turn(x, OTHERS[k]), c)
        return gain_move(CORES * len(OTHERS) + k, r.gbuf.at[x, c], r.gbuf.at[x, c], dev)

    def gain_die(xx, k):
        ref = r.gbuf.at[xx, c]
        return remote(ref, ref, r.gd_send.at[k], r.gd_recv.at[k], partner)

    def gain_sum():
        for zz in RINGS:
            for yy in RINGS:
                tot = jnp.zeros((n_layers, d_row), F32)
                for xx in RINGS:
                    for cc in BOTH:
                        tot += r.gbuf[xx, cc, yy, zz, :n_layers].astype(F32)
                at = (zz * RING + yy) * d_row
                r.gain[:, at:at + d_row] = tot

    tok_pair = CORES * rows

    def x_z(k):
        zz = turn(z, OTHERS[k])
        src = r.xt.at[pl.ds(zz * seqs, seqs)]
        return remote(src, r.xz.at[z], r.xz_send.at[k], r.xz_recv.at[k], (zz, y, x, c))

    def x_own():
        return pltpu.make_async_copy(r.xt.at[pl.ds(z * seqs, seqs)], r.xz.at[z], r.x_loc)

    def pos(xx):
        return pl.ds(pl.multiple_of(xx * tok_pair, tok_pair), tok_pair)

    def x_plane(oy, ox):
        yy, xx = turn(y, oy), turn(x, ox)
        return remote(r.xz.at[:, yy, :, pos(xx)], r.xp.at[c, y, x], r.xp_send.at[oy], r.xp_recv.at[(RING - oy) % RING], (z, yy, xx, c))

    def row_bytes(oy):
        return r.xp.at[c, 0] if oy else r.xp.at[c, 0, pl.ds(0, RING - 1)]

    def x_row(oy):
        yy = turn(y, oy)
        got = row_bytes(oy)
        remote(got, got, r.xp_send.at[oy], r.xp_recv.at[oy], partner).wait_recv()
        row = r.xp.at[c, yy]
        remote(row, row, r.xd_send.at[oy], r.xd_recv.at[oy], partner).start()

    def x_turn():
        for oy in RINGS:
            row = r.xp.at[1 - c, turn(y, oy)]
            remote(row, row, r.xd_send.at[oy], r.xd_recv.at[oy], partner).wait_recv()

        @pl.loop(0, RING)
        def _(zz):
            for yy in RINGS:
                for xh in BOTH:
                    blk = [r.xp[cc, yy, CORES * xh + xx, zz] for xx in BOTH for cc in BOTH]
                    blk = jnp.concatenate(blk, axis=0).astype(F32).T.astype(BF)
                    n = blk.shape[1]
                    at = pl.multiple_of(zz * RING * d_row + yy * d_row + xh * n, n)
                    r.hb[0, 0, :, :, pl.ds(at, n)] = blk.reshape(CORES, rows, n)
        r.hid[...] = r.hb[0, 0, c]
        for oy in RINGS:
            row = r.xp.at[c, turn(y, oy)]
            remote(row, row, r.xd_send.at[oy], r.xd_recv.at[oy], partner).wait_send()

    def x_sent():
        for fn in (x_z, gain_z, gain_y, gain_x):
            peers_of(fn, "wait_send")
        for k in RINGS:
            gain_die(x, k).wait_send()
        for oy in RINGS:
            got = row_bytes(oy)
            remote(got, got, r.xp_send.at[oy], r.xp_recv.at[oy], partner).wait_send()

    def y_die():
        return remote(r.hid, r.hb.at[0, 0, c], r.yd_send, r.yd_recv, partner)

    def y_plane(oy, ox):
        yy, xx = turn(y, oy), turn(x, ox)
        return remote(r.xp.at[c, yy, xx], r.xz.at[:, y, :, pos(x)], r.yp_send.at[oy], r.yp_recv.at[(RING - oy) % RING], (z, yy, xx, c))

    def y_z(s, oy, k):
        zz = turn(z, OTHERS[k])
        return remote(r.xz.at[zz, s], r.y_out.at[z * seqs + s], r.yz_send.at[oy, k], r.yz_recv.at[oy, k], (zz, y, x, c))

    def y_own(s, oy):
        return pltpu.make_async_copy(r.xz.at[z, s], r.y_out.at[z * seqs + s], r.y_loc.at[oy])

    def leave():
        y_die().start()
        r.hb[0, 0, c] = r.hid[...]
        y_die().wait()

        @pl.loop(0, RING)
        def _(zz):
            for yy in RINGS:
                for xh in BOTH:
                    n = CORES * CORES * d_local
                    at = pl.multiple_of(zz * RING * d_row + yy * d_row + xh * n, n)
                    blk = r.hb[0, 0, :, :, pl.ds(at, n)].reshape(tok_pair, n).astype(F32).T.astype(BF)
                    for xx in BOTH:
                        for cc in BOTH:
                            lo = (xx * CORES + cc) * d_local
                            r.xp[cc, yy, CORES * xh + xx, zz] = blk[lo:lo + d_local]

        for oy in OTHERS + (0,):
            for ox in RINGS:
                if oy or ox:
                    y_plane(oy, ox).start()
        for zz in RINGS:
            r.xz[zz, y, :, pos(x)] = r.xp[c, y, x, zz]
        for oy in OTHERS + (0,):
            yy = turn(y, oy)
            got = row_bytes(oy)
            remote(got, got, r.yp_send.at[oy], r.yp_recv.at[oy], partner).wait_recv()
            for k in range(len(OTHERS)):
                y_z(yy, oy, k).start()
            y_own(yy, oy).start()
        for oy in RINGS:
            got = row_bytes(oy)
            remote(got, got, r.yp_send.at[oy], r.yp_recv.at[oy], partner).wait_send()
            for k in range(len(OTHERS)):
                y_z(turn(y, oy), oy, k).wait()
            y_own(turn(y, oy), oy).wait()

    def kv_rows(zz):
        n = CORES * seq_len // (RING * RING * RING * CORES)
        return pl.ds(pl.multiple_of(((zz * RING + y) * RING + x) * n, n), n)

    def kv_trade(l, k):
        zz = turn(z, OTHERS[k])
        return remote(r.kv_out.at[l, :, :, kv_rows(zz)], r.kvx.at[l, z], r.kvx_send.at[l, k], r.kvx_recv.at[l, k], (zz, y, x, c))

    def kv_keep(l):
        return pltpu.make_async_copy(r.kv_out.at[l, :, :, kv_rows(z)], r.kvx.at[l, z], r.kvx_loc.at[l])

    def kv_share(l):
        for k in range(len(OTHERS)):
            kv_trade(l, k).start()
        kv_keep(l).start()

    def kv_shared(l):
        for k in range(len(OTHERS)):
            kv_trade(l, k).wait()
        kv_keep(l).wait()

    def gather_norm(l, split, pump):
        hid = r.hid
        gain = r.gain[l:l + 1, :]
        for b in range(4):
            blk = hid[b * quarter:(b + 1) * quarter, :].astype(F32)
            mean = jnp.mean(blk, axis=-1, keepdims=True)
            cen = blk - mean
            var = jnp.mean(cen * cen, axis=-1, keepdims=True)
            r.h_ref[b * quarter:(b + 1) * quarter, :] = (cen * lax.rsqrt(var + LN_EPS) * gain).astype(BF)
        out = r.h_all.at[l]

        def spot(q, first, second):
            if q == 0:
                return turn(y, second), turn(x, first)
            return turn(y, first), turn(x, second)

        def span(q, part):
            lo, n = (split, rows - split) if q else (0, split)
            if part is NIL:
                return pl.ds(lo, n)
            return pl.ds(lo + part * (n // 2), n // 2)

        copies = {}

        def ici(key, q, first, second, part, to_first, to_second, own=False):
            sy, sx = spot(q, first, second)
            ty, tx = spot(q, to_first, to_second)
            rws = span(q, part)
            dst = out.at[sy, sx, c, rws]
            kind = KINDS.index(key[0])
            cp = remote(r.h_ref.at[rws] if own else dst, dst, r.ag_send.at[l, kind], r.ag_recv.at[l, len(copies)], (z, ty, tx, c))
            cp.start()
            copies[key] = cp

        def die(q, first, second, own=False):
            sy, sx = spot(q, first, second)
            rws = span(q, NIL)
            dst = out.at[sy, sx, c, rws]
            off = (first if q else second) % RING
            remote(r.h_ref.at[rws] if own else dst, dst, r.ag_dsend.at[l], r.ag_drecv.at[l, off], partner).start()

        offs = (0, -1, 1, 2)
        for q in BOTH:
            for d in BOTH:
                ici(("first", q, d), q, 0, 0, NIL, SIGN[d], 0, own=True)
        for q in BOTH:
            for d in BOTH:
                ici(("second", q, 0, d), q, 0, 0, NIL, 0, SIGN[d], own=True)
        for q in BOTH:
            die(q, 0, 0, own=True)
        own = pltpu.make_async_copy(r.h_ref, out.at[y, x, c], r.ag_loc)
        own.start()
        hook(pump, 0)
        for d in BOTH:
            for q in BOTH:
                copies["first", q, d].wait_recv()
                src = -SIGN[d]
                ici(("first_on", q, d), q, src, 0, d, SIGN[d], 0)
                for e in BOTH:
                    ici(("second", q, 1 + d, e), q, src, 0, NIL, 0, SIGN[e])
                die(q, src, 0)
        hook(pump, 1)
        for d in BOTH:
            for q in BOTH:
                copies["second", q, 0, d].wait_recv()
                src = -SIGN[d]
                ici(("second_on", q, 0, d), q, 0, src, d, 0, SIGN[d])
                die(q, 0, src)
        hook(pump, 2)
        for q in BOTH:
            for d in BOTH:
                copies["first_on", q, d].wait_recv()
            for e in BOTH:
                ici(("second", q, 3, e), q, 2, 0, NIL, 0, SIGN[e])
            die(q, 2, 0)
        hook(pump, 3)
        for k in (1, 2, 3):
            for d in BOTH:
                for q in BOTH:
                    copies["second", q, k, d].wait_recv()
                    src = -SIGN[d]
                    ici(("second_on", q, k, d), q, offs[k], src, d, 0, SIGN[d])
                    die(q, offs[k], src)
            hook(pump, 3 + k)
        for k in range(4):
            for q in BOTH:
                for d in BOTH:
                    copies["second_on", q, k, d].wait_recv()
                die(q, offs[k], 2)
        hook(pump, 7)
        for off in RINGS:
            got = out.at[turn(y, off), :, 1 - c]
            remote(got, got, r.ag_dsend.at[l], r.ag_drecv.at[l, off], partner).wait_recv()
        sent = (out.at[y, x], out.at[y], out.at[y, x, c], out.at[y, pl.ds(0, CORES)])
        for kind, ref in enumerate(sent):
            remote(ref, ref, r.ag_send.at[l, kind], r.ag_recv.at[l, kind], partner).wait_send()
        remote(out.at[pl.ds(0, 2)], out.at[pl.ds(0, 2)], r.ag_dsend.at[l], r.ag_drecv.at[l, 0], partner).wait_send()
        own.wait()

    def h_copy(l, s, slot):
        return pltpu.make_async_copy(r.h_all.at[l, s], r.hb.at[slot], r.h_sem.at[slot])

    def h_tile(slot):
        return r.hb[slot].reshape(seq_len, d_model)

    def project(h, lo, n):
        w = r.wv[:, :, lo:lo + n].reshape(d_model, n)
        return jnp.dot(h, w, preferred_element_type=F32).astype(BF)

    def rope(val):
        val = val.astype(F32)
        return val * r.cos[...] + pltpu.roll(val, head_dim // 2, 1) * r.sin[...]

    n_chunk = min(256, f_loc)

    def kv_out_copy(l, s, slot, i):
        return pltpu.make_async_copy(r.qkv.at[slot, i], r.kv_out.at[l, i, s], r.kvo_sem.at[slot, i])

    def pass_one(l, pump):
        h_copy(l, 0, 0).start()

        @pl.loop(0, RING)
        def _(s):
            slot = lax.rem(s, 2)
            h_copy(l, s, slot).wait()

            @pl.when(s + 1 < RING)
            def _():
                h_copy(l, s + 1, 1 - slot).start()

            pump(s)

            @pl.when(s >= 2)
            def _():
                for i in BOTH:
                    kv_out_copy(l, s - 2, slot, i).wait()

            kv = jnp.zeros((seq_len, 2 * head_dim), F32)
            for zz in RINGS:
                for yy in RINGS:
                    col = (zz * RING + yy) * d_row
                    kv += lax.dot_general(h_cols(slot, col, d_row), r.kvb[yy, zz], (((1,), (1,)), ((), ())), preferred_element_type=F32)
            kv = kv.astype(BF)
            r.qkv[slot, 0] = rope(kv[:, :head_dim]).astype(BF)
            r.qkv[slot, 1] = kv[:, head_dim:]
            for i in BOTH:
                kv_out_copy(l, s, slot, i).start()
            q = project(h_tile(slot), 0, head_dim)
            r.stage[...] = (rope(q) * head_dim ** -0.5).astype(BF)
            for lo in range(0, f_loc, n_chunk):
                r.joined[s, :, head_dim + lo:head_dim + lo + n_chunk] = project(h_tile(slot), head_dim + lo, n_chunk)
            n_tile = seq_len // 2
            for i in BOTH:
                keys = (i + 1) * n_tile
                sc = lax.dot_general(r.stage[i * n_tile:(i + 1) * n_tile, :], r.qkv[slot, 0, :keys, :], (((1,), (1,)), ((), ())), preferred_element_type=F32)
                row_id = lax.broadcasted_iota(jnp.int32, sc.shape, 0) + i * n_tile
                col_id = lax.broadcasted_iota(jnp.int32, sc.shape, 1)
                sc = jnp.where(col_id <= row_id, sc, -1e30)
                top = jnp.max(sc, axis=-1, keepdims=True)
                ex = jnp.exp(sc - top)
                prob = (ex * (1.0 / jnp.sum(ex, axis=-1, keepdims=True))).astype(BF)
                att = jnp.dot(prob, r.qkv[slot, 1, :keys, :], preferred_element_type=F32)
                r.joined[s, i * n_tile:(i + 1) * n_tile, :head_dim] = att.astype(BF)

        for s in (RING - 2, RING - 1):
            for i in BOTH:
                kv_out_copy(l, s, s % 2, i).wait()

    def h_cols(slot, col, n):
        return r.hb[slot, :, :, :, col:col + n].reshape(seq_len, n)

    def pass_two(l, pump):
        h_copy(l, 0, 0).start()

        @pl.loop(0, RING)
        def _(s):
            slot = lax.rem(s, 2)
            h_copy(l, s, slot).wait()

            @pl.when(s + 1 < RING)
            def _():
                h_copy(l, s + 1, 1 - slot).start()

            pump(s)
            for lo in range(0, f_loc, n_chunk):
                up = project(h_tile(slot), head_dim + f_loc + lo, n_chunk).astype(F32)
                cols = slice(head_dim + lo, head_dim + lo + n_chunk)
                g = r.joined[s, :, cols].astype(F32)
                r.joined[s, :, cols] = (g * jax.nn.sigmoid(g) * up).astype(BF)

    def out_scatter(l, pump):
        def peer(q, first, second):
            dy = first * (1 - q) + second * q
            dx = first * q + second * (1 - q)
            return (z, turn(y, dy), turn(x, dx), c)

        def die_copy(ch, q, s):
            return remote(r.away.at[q], r.die_in.at[ch, q, s], r.dsend.at[l, ch, q, s], r.drecv.at[l, ch, q, s], partner)

        def first_copy(ch, q, d):
            return remote(r.acc.at[ch, q, 0, pl.ds(CORES * d, CORES)], r.in1.at[ch, q, d], r.send1.at[l, ch, q, d], r.recv1.at[l, ch, q, d],
                          peer(q, SIGN[d], 0))

        def second_copy(ch, q, d, h):
            js = pl.ds(CORES * h, CORES)
            return remote(r.acc.at[ch, q, 1 + d, js], r.in2.at[ch, q, d, js], r.send2.at[l, ch, q, d, h], r.recv2.at[l, ch, q, d, h],
                          peer(q, SIGN[d], 0))

        def half_rows(d):
            return pl.ds(d * (rows // 2), rows // 2)

        def third_copy(ch, q, d):
            return remote(r.acc.at[ch, q, LAST, 0, half_rows(d)], r.in3.at[ch, q, d], r.send3.at[l, ch, q, d], r.recv3.at[l, ch, q, d],
                          peer(q, 0, SIGN[d]))

        def fourth_copy(ch, q, d):
            return remote(r.acc.at[ch, q, LAST, 1 + d], r.in4.at[ch, q, d], r.send4.at[l, ch, q, d], r.recv4.at[l, ch, q, d],
                          peer(q, 0, SIGN[d]))

        n_blk = r.wov.shape[3]

        def plane_of(ch, q):
            return turn(z, LAST - q if ch else q)

        def tile(ch, q, s):
            for cc in BOTH:
                for j in RINGS:
                    oy = SLOT_OFF[s] * (1 - q) + SLOT_OFF[j] * q
                    ox = SLOT_OFF[j] * (1 - q) + SLOT_OFF[s] * q
                    core = c if cc else 1 - c
                    at = pl.multiple_of((turn(x, ox) * CORES + core) * rows, rows)
                    r.lhs[pl.ds((cc * RING + j) * rows, rows), :] = r.joined[turn(y, oy), pl.ds(at, rows), :]
            left = r.lhs[...]
            zz = plane_of(ch, q)

            @pl.loop(0, RING)
            def _(n):
                col = pl.multiple_of(n * n_blk, n_blk)
                res = jnp.dot(left, r.wov[zz, n], preferred_element_type=F32).astype(BF)
                res = res.reshape(CORES, RING, rows, n_blk)
                r.away[q, :, :, pl.ds(col, n_blk)] = res[0]
                r.acc[ch, q, s, :, :, pl.ds(col, n_blk)] = res[1]

        def pair_sum(ch, q, s):
            die_copy(ch, q, s).wait_recv()

            @pl.loop(0, RING)
            def _(j):
                r.acc[ch, q, s, j] = r.acc[ch, q, s, j] + r.die_in[ch, q, s, j]

        def stage_a(ch):
            for s in RINGS:
                @pl.loop(0, CORES)
                def _(q, s=s):
                    if s:
                        die_copy(ch, q, s - 1).wait_send()
                    elif ch:
                        die_copy(ch - 1, q, LAST).wait_send()
                    tile(ch, q, s)
                    die_copy(ch, q, s).start()
                    if s:
                        pair_sum(ch, q, s - 1)
                    if s == 1:
                        for d in BOTH:
                            first_copy(ch, q, d).start()
                    if s > 1:
                        second_copy(ch, q, s - 2, LAST - s).start()
                if s == 1:
                    hook(pump, ("a", ch))

        def stage_b(ch):
            for q in BOTH:
                pair_sum(ch, q, LAST)
            for q in BOTH:
                for d in BOTH:
                    first_copy(ch, q, d).wait_recv()
                    for j in BOTH:
                        at = CORES * d + j
                        r.acc[ch, q, 1 + d, at] = r.acc[ch, q, 1 + d, at] + r.in1[ch, q, d, j]
                    second_copy(ch, q, d, d).start()

        def total(ch, q, j):
            val = r.acc[ch, q, LAST, j].astype(F32)
            for d in BOTH:
                val += r.in2[ch, q, d, j].astype(F32)
            r.acc[ch, q, LAST, j] = val.astype(BF)

        def stage_c(ch):
            for q in BOTH:
                for h in BOTH:
                    for d in BOTH:
                        second_copy(ch, q, d, h).wait_recv()
                total(ch, q, 0)
                for d in BOTH:
                    third_copy(ch, q, d).start()
                for j in RINGS[1:]:
                    total(ch, q, j)

        def stage_d(ch):
            for q in BOTH:
                for d in BOTH:
                    third_copy(ch, q, d).wait_recv()
                    rws = half_rows(d)
                    r.acc[ch, q, LAST, 1 + d, rws] = r.acc[ch, q, LAST, 1 + d, rws] + r.in3[ch, q, d]
                    fourth_copy(ch, q, d).start()

        def stage_e(ch):
            for q in BOTH:
                for d in BOTH:
                    fourth_copy(ch, q, d).wait_recv()
                cols = pl.ds(pl.multiple_of(plane_of(ch, q) * width, width), width)
                upd = r.acc[ch, q, LAST, LAST].astype(F32)
                for d in BOTH:
                    upd += r.in4[ch, q, d].astype(F32)
                upd = upd.astype(BF)
                r.hid[:, cols] = (r.hid[:, cols].astype(F32) + upd.astype(F32)).astype(BF)

        def sent(ch):
            for q in BOTH:
                if ch:
                    die_copy(ch, q, LAST).wait_send()
                for d in BOTH:
                    for cp in (first_copy, third_copy, fourth_copy):
                        cp(ch, q, d).wait_send()
                    for h in BOTH:
                        second_copy(ch, q, d, h).wait_send()

        for step, fn, ch in (
            ("a0", stage_a, 0), ("b0", stage_b, 0), ("a1", stage_a, 1), ("c0", stage_c, 0), ("b1", stage_b, 1),
            ("d0", stage_d, 0), ("e0", stage_e, 0), ("c1", stage_c, 1), ("d1", stage_d, 1), ("e1", stage_e, 1),
        ):
            with jax.named_scope(step):
                fn(ch)
            hook(pump, step)
        for ch in BOTH:
            sent(ch)

    def near(fn, t):
        for j in (LAST, 1):
            fn(t, j)

    def far(fn, t):
        fn(t, 2)

    def z_all(t):
        near(z_direct, t)
        far(z_direct, t)

    def peers_of(fn, op="start"):
        for k in range(len(OTHERS)):
            getattr(fn(k), op)()

    def when_j(s, fn):
        @pl.when(s < 3)
        def _():
            fn(s + 1)

    def start():
        peers_of(gain_z)
        peers_of(x_z)
        x_own().start()
        r.gbuf[x, c, y, z] = r.gain_in[...]
        z_own(0)
        z_own(1)
        with jax.named_scope("gain_a"):
            peers_of(gain_z, "wait_recv")
            peers_of(gain_y)
            peers_of(gain_y, "wait_recv")
            peers_of(gain_x)
            gain_die(x, LAST).start()
        with jax.named_scope("x_z"):
            peers_of(x_z, "wait_recv")
            x_own().wait()
        for oy in RINGS:
            for ox in RINGS:
                if oy or ox:
                    x_plane(oy, ox).start()
        r.xp[c, y, x] = r.xz[:, y, :, pos(x)]
        kv_z()
        with jax.named_scope("gain_b"):
            for k, o in enumerate(OTHERS):
                gain_x(k).wait_recv()
                gain_die(turn(x, -o), k).start()
        with jax.named_scope("z_f"):
            z_forward(0, 0)
        with jax.named_scope("rows"):
            for oy in (0, LAST, 1, 2):
                x_row(oy)
        y_send(0)
        with jax.named_scope("z_g"):
            z_forward(1, 0)
            z_own(2)
        with jax.named_scope("gain_sum"):
            for k in RINGS:
                gain_die(x, k).wait_recv()
            gain_sum()
        with jax.named_scope("turn"):
            x_turn()

    def ag0(i):
        if i == 1:
            kv_y1()
            near(z_direct, 0)
            y_relay(0)
        if i == 2:
            kv_y2()
            y_send(1)
            z_forward(2, 0)
        if i == 3:
            far(z_direct, 0)
            kv_y3()
            kv_x1(0)
        if i == 4:
            near(z_forward, 0)
            y_relay(1)
        if i == 5:
            kv_x2(0)
            far(z_forward, 0)
            near(z_direct, 1)
        if i == 6:
            far(z_direct, 1)
            y_send(2)
            kv_x3(0)
        if i == 7:
            near(z_forward, 1)
            finish(0)
            kv_load(0)

    def rs0(i):
        if i == ("a", 0):
            load_far(2)
        if i == "b0":
            far_loaded(2)
            z_forward(3, 0)
        if i == "a1":
            near(z_forward, 3)
            y_relay(5)
        if i == "c0":
            far(z_forward, 3)
            z_own(4)
        if i == "b1":
            z_all(4)
        if i == "c1":
            finish(3)
            kv_load(1)

    def ag1(i):
        if i == 1:
            z_forward(4, 0)
        if i == 2:
            near(z_forward, 4)
        if i == 3:
            far(z_forward, 4)
            z_own(5)
        if i == 5:
            z_all(5)
        if i == 7:
            finish(4)

    def nothing(i):
        pass

    with jax.named_scope("start"):
        start()
    with jax.named_scope("gather_0"):
        gather_norm(0, rows // RING, ag0)
    with jax.named_scope("wait_w0"):
        loaded(0)
        kv_loaded()
        y_relay(2)
        far(z_forward, 1)
        y_send(3)
        kv_x1(1)
        x_sent()
    with jax.named_scope("pass_one_0"):
        pass_one(0, lambda s: when_j(s, lambda j: z_direct(2, j)))
    with jax.named_scope("finish_1"):
        kv_share(0)
        finish(1)
        z_own(3)
        y_relay(3)
        y_send(4)
        y_send(5)
        kv_x2(1)
        loaded(1)
    with jax.named_scope("pass_two_0"):
        pass_two(0, lambda s: when_j(s, lambda j: z_forward(2, j)))
    with jax.named_scope("near_2"):
        load_near(2)
        y_relay(4)
        kv_x3(1)
        z_all(3)
        near_loaded(2)
    with jax.named_scope("scatter_0"):
        out_scatter(0, rs0)
    with jax.named_scope("gather_1"):
        gather_norm(1, rows // 2, ag1)
    with jax.named_scope("wait_w3"):
        loaded(3)
        kv_loaded()
    with jax.named_scope("pass_one_1"):
        pass_one(1, lambda s: z_forward(5, s))
    with jax.named_scope("finish_5"):
        kv_share(1)
        loaded(4)
        finish(5)
    with jax.named_scope("pass_two_1"):
        pass_two(1, nothing)
    with jax.named_scope("wait_w5"):
        loaded(5)
    with jax.named_scope("scatter_1"):
        out_scatter(1, nothing)
    with jax.named_scope("leave"):
        leave()
    with jax.named_scope("drain"):
        for t in range(3 * n_layers):
            drain(t)
        for l in range(n_layers):
            kv_shared(l)
            kv_sent(l)


def run_model(xt, gain, wkv_t, w_in, w_out, cos_full, sin_full):
    batch, d_local, seq_len = xt.shape
    n_layers, d_row, e_block = w_in.shape
    r_block, d_col = w_out.shape[1:]
    head_dim = cos_full.shape[1]
    d_model = d_row * RING * RING
    seqs = batch // RING
    rows = seqs * seq_len // (RING * RING * CORES)
    e_loc, r_loc = e_block // RING, r_block // RING
    kc = wkv_t.shape[1]
    width = d_model // RING
    g_rows = gain.shape[0]
    n_t = 3 * n_layers
    n_o = len(OTHERS)

    def dma(*shape):
        return pltpu.SemaphoreType.DMA(shape)

    def vm(*shape):
        return pltpu.VMEM(shape, BF)

    def out(*shape):
        return jax.ShapeDtypeStruct(shape, BF)

    any_spec = pl.BlockSpec(memory_space=pl.ANY)
    vm_spec = pl.BlockSpec(memory_space=pltpu.VMEM)
    out_shape = [
        out(batch, d_local, seq_len),
        out(n_layers, 2, seqs, seq_len, head_dim),
        out(n_layers, RING, RING, CORES, rows, d_model),
        out(n_layers, RING, RING * d_row, e_loc),
        out(n_layers, RING, RING, r_loc, d_col),
        out(RING, CORES, n_layers, RING, RING, kc, d_row),
        out(n_layers, RING, 2, seqs, CORES * (seq_len // (CORES * RING * RING * RING)), head_dim),
        out(n_layers, 2, d_row // 2, e_loc),
        out(n_layers, 2, r_loc // 2, d_col),
    ]
    pair = (2, 2, 2)
    each = (n_layers, *pair)
    scratch = [
        vm(rows, d_model), vm(rows, d_model), pltpu.VMEM((n_layers, d_model), F32),
        vm(RING, CORES, RING, RING, g_rows, d_row),
        vm(RING, seqs, d_local, seq_len),
        vm(CORES, RING, RING, RING, d_local, CORES * rows),
        vm(RING, RING * d_row, e_loc), vm(RING, RING, 2 * head_dim, d_row), vm(RING, RING, r_loc, d_col),
        vm(2, RING, CORES, rows, d_model), vm(RING, seq_len, r_loc), vm(2, 2, seq_len, head_dim), vm(seq_len, head_dim),
        vm(CORES * RING * rows, r_loc), vm(2, RING, rows, width), vm(2, 2, RING, RING, rows, width), vm(2, 2, RING, RING, rows, width),
        vm(*pair, 2, rows, width), vm(*pair, RING, rows, width), vm(*pair, rows // 2, width), vm(*pair, rows, width),
        dma(n_o), dma(n_o), dma(RING), dma(RING), dma(RING), dma(RING), pltpu.SemaphoreType.DMA,
        dma(3 * n_o), dma(3 * n_o), dma(RING), dma(RING),
        pltpu.SemaphoreType.DMA, pltpu.SemaphoreType.DMA, dma(RING), dma(RING), dma(RING, n_o), dma(RING, n_o), dma(RING),
        dma(n_layers, RING), dma(n_layers, 40), dma(n_layers), dma(n_layers, RING), pltpu.SemaphoreType.DMA, dma(2), dma(2, 2), dma(3), dma(3),
        dma(n_t, RING), dma(n_t, 2), dma(n_t, RING, 2), dma(n_t, RING, 2), dma(n_t, RING),
        dma(n_o), dma(n_o), pltpu.SemaphoreType.DMA, dma(n_o), dma(n_layers), dma(n_layers, n_o), dma(n_layers), dma(n_layers), dma(2),
        dma(n_layers, 2, 2, RING), dma(n_layers, 2, 2, RING),
        dma(*each), dma(*each), dma(*each, 2), dma(*each, 2), dma(*each), dma(*each), dma(*each), dma(*each),
        dma(n_layers, n_o), dma(n_layers, n_o), dma(n_layers),
    ]
    res = pl.pallas_call(
        model_kernel,
        out_shape=out_shape,
        in_specs=[any_spec, vm_spec, vm_spec, any_spec, any_spec, vm_spec, vm_spec],
        out_specs=[any_spec] * len(out_shape),
        scratch_shapes=scratch,
        compiler_params=pltpu.CompilerParams(collective_id=0, has_side_effects=True, vmem_limit_bytes=VMEM_LIMIT),
        name="two_layers",
    )(xt, gain, wkv_t, w_in, w_out, cos_full, sin_full)
    return res[0], res[6]


def solution(mesh):
    row_size = mesh.shape["row"]
    n_col = mesh.shape["col"]
    n_z = row_size // RING
    n_y = RING
    n_x = n_col // CORES
    n_tp = n_y * n_col
    n_dev = row_size * n_col
    mesh4 = Mesh(mesh.devices.reshape(n_z, n_y, n_x, CORES), ("z", "y", "x", "core"))
    every = ("z", "y", "x", "core")
    col = ("x", "core")
    act_spec = P(NIL, NIL, every)
    w_spec = P(NIL, ("z", "y"), col)

    def device_fn(x_loc, gain_loc, w_in_loc, w_kv_loc, w_out_loc):
        n_layers = w_in_loc.shape[0]
        n_batch, seq_len, d_local = x_loc.shape
        head_dim = w_kv_loc.shape[2] * n_col // 2
        batch_loc = n_batch // n_z
        seq_local = seq_len // n_dev
        steps = np.arange(head_dim // 2, dtype=np.float32)
        inv_freq = (1.0 / 10000.0 ** (steps * 2 / head_dim)).astype(np.float32)
        angles = np.arange(seq_len, dtype=np.float32)[:, NIL] * inv_freq[NIL, :]
        cos_tab, sin_tab = np.cos(angles), np.sin(angles)
        cos_full = jnp.asarray(np.concatenate([cos_tab, cos_tab], axis=1))
        sin_full = jnp.asarray(np.concatenate([-sin_tab, sin_tab], axis=1))
        spot = lax.axis_index("x") * CORES + lax.axis_index("core")
        own = lax.broadcasted_iota(jnp.int32, (n_layers, n_col, d_local), 1) == spot
        gains = jnp.where(own, gain_loc[:, NIL, :], 0).astype(BF).reshape(n_layers, n_col * d_local)
        gains = jnp.pad(gains, ((0, G_ROWS - n_layers), (0, 0)))
        y_loc, kv = run_model(x_loc.transpose(0, 2, 1), gains, w_kv_loc.transpose(0, 2, 1), w_in_loc, w_out_loc, cos_full, sin_full)
        y_loc = y_loc.transpose(0, 2, 1)
        kv = kv.reshape(n_layers, n_z, 2, batch_loc, CORES, seq_local, head_dim)
        kv = lax.dynamic_index_in_dim(kv, lax.axis_index("core"), axis=4, keepdims=False)
        kv = kv.transpose(0, 2, 1, 3, 4, 5).reshape(n_layers, 2, n_batch, seq_local, head_dim)
        return y_loc, kv

    return jax.shard_map(device_fn, mesh=mesh4, in_specs=(act_spec, P(NIL, every), w_spec, w_spec, P(NIL, col, ("z", "y"))), out_specs=(act_spec, P(NIL, NIL, NIL, every, NIL)), check_vma=False)
```

```python
import jax
import jax.numpy as jnp
import numpy as np
from jax import lax
from jax.experimental import pallas as pl
from jax.experimental.pallas import tpu as pltpu
from jax.sharding import Mesh
from jax.sharding import PartitionSpec as P

LN_EPS = 1e-6
RING = 4
CORES = 2
VMEM_LIMIT = 67_000_000
BF = jnp.bfloat16
F32 = jnp.float32
SLOT_OFF = (2, 1, 3, 0)
SIGN = (1, -1)
NIL = None
BOTH = range(CORES)
RINGS = range(RING)
OTHERS = (1, 3, 2)
LAST = RING - 1
G_ROWS = 8
QG0, UP0, WO0, QG1, UP1, WO1 = range(6)
KINDS = ("first", "second", "first_on", "second_on")
NAMES = (
    "xt", "gain_in", "wkv", "w_in", "w_out", "cos", "sin", "y_out", "kv_out", "h_all", "wi", "wo", "kvh", "kvx", "rwi", "rwo", "h_ref",
    "hid", "gain", "gbuf", "xz", "xp",
    "wv", "kvb", "wov", "hb", "joined", "qkv", "stage", "lhs", "away", "acc", "die_in", "in1", "in2", "in3", "in4",
    "xz_send", "xz_recv", "xp_send", "xp_recv", "xd_send", "xd_recv", "x_loc", "g_send", "g_recv", "gd_send", "gd_recv", "yd_send", "yd_recv", "yp_send", "yp_recv", "yz_send", "yz_recv", "y_loc",
    "ag_send", "ag_recv", "ag_dsend", "ag_drecv", "ag_loc", "h_sem", "kvo_sem", "w_load", "far_load", "y_recv", "ry_recv", "zb_recv",
    "zc_recv", "w_send", "kz_send", "kz_recv", "ky_send", "ky_recv", "kx_send", "kx_recv", "kd_send", "kd_recv",
    "k_loc", "dsend", "drecv", "send1", "recv1", "send2", "recv2", "send3", "recv3", "send4", "recv4", "kvx_send", "kvx_recv", "kvx_loc",
)


class Refs:
    def __init__(self, refs):
        for name, ref in zip(NAMES, refs, strict=True):
            setattr(self, name, ref)


def model_kernel(*refs):
    r = Refs(refs)
    z, y, x, c = (lax.axis_index(a) for a in ("z", "y", "x", "core"))
    n_layers = r.wkv.shape[0]
    rows, d_model = r.hid.shape
    batch, d_local = r.xt.shape[:2]
    seqs = batch // RING
    seq_len, head_dim = r.cos.shape
    d_row = r.w_in.shape[1]
    e_loc = r.wi.shape[3]
    depth = r.wo.shape[3]
    f_loc = depth - head_dim
    quarter = rows // 4
    width = d_model // RING
    q_block = head_dim * RING
    f_block = f_loc * RING

    def turn(base, off):
        return lax.rem(base + off + RING, RING)

    def remote(src, dst, ssem, rsem, dev):
        return pltpu.make_async_remote_copy(
            src_ref=src, dst_ref=dst, send_sem=ssem, recv_sem=rsem, device_id=dev, device_id_type=pl.DeviceIdType.MESH)

    partner = (z, y, x, 1 - c)

    peers = [(turn(z, o), y, x, c) for o in OTHERS]
    peers += [(z, turn(y, oy), turn(x, ox), c) for oy in RINGS for ox in RINGS if oy or ox]
    peers.append(partner)
    here = (z, y, x, c)
    gate_sem = pltpu.get_barrier_semaphore()
    for dev in peers:
        pl.semaphore_signal(gate_sem, inc=1, device_id=dev, device_id_type=pl.DeviceIdType.MESH)
    src_id = lax.broadcasted_iota(jnp.int32, (d_local, d_row), 0) + (x * CORES + c) * d_local
    dst_id = lax.broadcasted_iota(jnp.int32, (d_local, d_row), 1)
    spread = jnp.where(src_id == dst_id, 1.0, 0.0).astype(BF)
    r.gbuf[x, c, y, z] = jnp.zeros((G_ROWS, d_row), BF)
    r.gbuf[x, c, y, z, :n_layers] = jnp.dot(r.gain_in[...], spread, preferred_element_type=F32).astype(BF)
    pl.semaphore_wait(gate_sem, len(peers))

    def hook(pump, i):
        with jax.named_scope(f"hook_{i}"):
            pump(i)

    def w_cols(kind):
        return pl.ds(0, head_dim + f_loc) if kind == 0 else pl.ds(head_dim + f_loc, f_loc)

    def piece(t, zz, yy):
        l, kind = t // 3, t % 3
        if kind == 2:
            return r.wo.at[l, zz, yy]
        return r.wi.at[l, zz, pl.ds(pl.multiple_of(yy * d_row, d_row), d_row), w_cols(kind)]

    def piece_half(t, zz, yy, h):
        l, kind = t // 3, t % 3
        if kind == 2:
            return r.wo.at[l, zz, yy, pl.ds(h * (depth // 2), depth // 2)]
        return r.wi.at[l, zz, pl.ds(pl.multiple_of(yy * d_row + h * (d_row // 2), d_row // 2), d_row // 2), w_cols(kind)]

    def own_parts(t, owner, zz, yy):
        l, kind = t // 3, t % 3
        hq = pl.ds(pl.multiple_of(owner * head_dim, head_dim), head_dim)
        if kind == 2:
            return [
                (r.w_out.at[l, hq], r.wo.at[l, zz, yy, pl.ds(0, head_dim)]),
                (r.w_out.at[l, pl.ds(pl.multiple_of(q_block + owner * f_loc, head_dim), f_loc)], r.wo.at[l, zz, yy, pl.ds(head_dim, f_loc)]),
            ]
        rws = pl.ds(pl.multiple_of(yy * d_row, d_row), d_row)
        if kind == 0:
            return [
                (r.w_in.at[l, :, hq], r.wi.at[l, zz, rws, pl.ds(0, head_dim)]),
                (r.w_in.at[l, :, pl.ds(pl.multiple_of(q_block + owner * f_loc, head_dim), f_loc)], r.wi.at[l, zz, rws, pl.ds(head_dim, f_loc)]),
            ]
        return [(r.w_in.at[l, :, pl.ds(pl.multiple_of(q_block + f_block + owner * f_loc, head_dim), f_loc)],
                 r.wi.at[l, zz, rws, pl.ds(head_dim + f_loc, f_loc)])]

    def relay_ref(t, d):
        l, kind = t // 3, t % 3
        return r.rwo.at[l, d] if kind == 2 else r.rwi.at[l, d, :, w_cols(kind)]

    def far_parts(t, d):
        l, kind = t // 3, t % 3
        owner = turn(y, 2)
        hq = pl.ds(pl.multiple_of(owner * head_dim, head_dim), head_dim)
        if kind == 2:
            n = depth // 2
            base = q_block + owner * f_loc
            if d:
                return [(r.w_out.at[l, pl.ds(pl.multiple_of(base + n - head_dim, G_ROWS), n)], r.rwo.at[l, d])]
            return [
                (r.w_out.at[l, hq], r.rwo.at[l, d, pl.ds(0, head_dim)]),
                (r.w_out.at[l, pl.ds(pl.multiple_of(base, head_dim), n - head_dim)], r.rwo.at[l, d, pl.ds(head_dim, n - head_dim)]),
            ]
        rws = pl.ds(d * (d_row // 2), d_row // 2)
        if kind == 0:
            return [
                (r.w_in.at[l, rws, hq], r.rwi.at[l, d, :, pl.ds(0, head_dim)]),
                (r.w_in.at[l, rws, pl.ds(pl.multiple_of(q_block + owner * f_loc, head_dim), f_loc)], r.rwi.at[l, d, :, pl.ds(head_dim, f_loc)]),
            ]
        return [(r.w_in.at[l, rws, pl.ds(pl.multiple_of(q_block + f_block + owner * f_loc, head_dim), f_loc)], relay_ref(t, d))]

    def y_send(t):
        for d in BOTH:
            owner = turn(y, SIGN[d])
            dev = (z, owner, x, c)
            for src, dst in far_parts(t, d):
                remote(src, dst, r.w_send.at[t, 0], r.ry_recv.at[t, d], dev).start()
            for src, dst in own_parts(t, owner, z, y):
                remote(src, dst, r.w_send.at[t, 0], r.y_recv.at[t, -SIGN[d] % RING], dev).start()

    def y_relay(t):
        for d in BOTH:
            ref = relay_ref(t, d)
            remote(ref, ref, r.w_send.at[t, 3], r.ry_recv.at[t, d], here).wait_recv()
            dst = piece_half(t, z, turn(y, -SIGN[d]), d)
            remote(ref, dst, r.w_send.at[t, 3], r.y_recv.at[t, 2], (z, turn(y, SIGN[d]), x, c)).start()

    def z_own(t):
        for d in BOTH:
            for src, dst in own_parts(t, y, z, y):
                remote(src, dst, r.w_send.at[t, 1], r.zb_recv.at[t, 0, d], (turn(z, SIGN[d]), y, x, c)).start()

    def z_direct(t, j):
        yy = turn(y, j)
        ref = piece(t, z, yy)
        remote(ref, ref, r.w_send.at[t, 0], r.y_recv.at[t, j], here).wait_recv()
        for d in BOTH:
            remote(ref, ref, r.w_send.at[t, 1], r.zb_recv.at[t, j, d], (turn(z, SIGN[d]), y, x, c)).start()

    def z_forward(t, j):
        yy = turn(y, j)
        for d in BOTH:
            zz = turn(z, -SIGN[d])
            ref = piece(t, zz, yy)
            remote(ref, ref, r.w_send.at[t, 1], r.zb_recv.at[t, j, d], here).wait_recv()
            part = piece_half(t, zz, yy, d)
            remote(part, part, r.w_send.at[t, 2], r.zc_recv.at[t, j, d], (turn(z, SIGN[d]), y, x, c)).start()

    def place(t, zz):
        l, kind = t // 3, t % 3
        if kind == 2:
            return r.wo.at[l, zz], r.wov.at[zz]
        return r.wi.at[l, zz, :, w_cols(kind)], r.wv.at[zz, :, w_cols(kind)]

    def load_near(t):
        kind = t % 3
        for d in BOTH:
            src, dst = place(t, turn(z, SIGN[d]))
            pltpu.make_async_copy(src, dst, r.w_load.at[kind]).start()
        for j in OTHERS:
            yy = turn(y, j)
            dst = r.wov.at[z, yy] if kind == 2 else r.wv.at[z, pl.ds(pl.multiple_of(yy * d_row, d_row), d_row), w_cols(kind)]
            pltpu.make_async_copy(piece(t, z, yy), dst, r.w_load.at[kind]).start()
        for src, dst in own_parts(t, y, z, y):
            pltpu.make_async_copy(src, own_place(t, dst, src), r.w_load.at[kind]).start()

    def load_far(t):
        far = turn(z, 2)
        for j in RINGS:
            for d in BOTH:
                part = piece_half(t, far, turn(y, j), d)
                remote(part, part, r.w_send.at[t, 2], r.zc_recv.at[t, j, d], here).wait_recv()
        src, dst = place(t, far)
        pltpu.make_async_copy(src, dst, r.far_load.at[t % 3]).start()

    def own_place(t, dst, src):
        kind = t % 3
        if kind == 2:
            n = src.shape[0]
            return r.wov.at[z, y, pl.ds(0 if n == head_dim and f_loc != head_dim else head_dim, n)]
        n = src.shape[1]
        rws = pl.ds(pl.multiple_of(y * d_row, d_row), d_row)
        if kind == 0:
            return r.wv.at[z, rws, pl.ds(0 if n == head_dim and f_loc != head_dim else head_dim, n)]
        return r.wv.at[z, rws, pl.ds(head_dim + f_loc, f_loc)]

    def finish(t):
        load_near(t)
        load_far(t)

    def near_loaded(t):
        kind = t % 3
        dst = r.wov.at[pl.ds(0, LAST)] if kind == 2 else r.wv.at[pl.ds(0, LAST), :, w_cols(kind)]
        pltpu.make_async_copy(dst, dst, r.w_load.at[kind]).wait()

    def far_loaded(t):
        kind = t % 3
        dst = r.wov.at[0] if kind == 2 else r.wv.at[0, :, w_cols(kind)]
        pltpu.make_async_copy(dst, dst, r.far_load.at[kind]).wait()

    def loaded(t):
        near_loaded(t)
        far_loaded(t)

    def drain(t):
        l, kind = t // 3, t % 3
        if kind == 2:
            done = (r.wo.at[l, 0, pl.ds(0, LAST)], r.wo.at[l, pl.ds(0, 2)], r.wo.at[l, 0], r.wo.at[l, 0, 0])
        else:
            cols = w_cols(kind)
            done = (r.wi.at[l, 0, pl.ds(0, LAST * d_row), cols], r.wi.at[l, pl.ds(0, 2), :, cols], r.wi.at[l, 0, :, cols],
                    r.wi.at[l, 0, pl.ds(0, d_row), cols])
        for g, ref in enumerate(done):
            remote(ref, ref, r.w_send.at[t, g], r.y_recv.at[t, 0], here).wait_send()

    def kv_z_copy(k):
        return remote(r.wkv, r.kvh.at[x, c, :, y, z], r.kz_send.at[k], r.kz_recv.at[k], (turn(z, OTHERS[k]), y, x, c))

    def kv_own():
        return pltpu.make_async_copy(r.wkv, r.kvh.at[x, c, :, y, z], r.k_loc.at[0])

    def kv_z():
        for k in range(len(OTHERS)):
            kv_z_copy(k).start()
        kv_own().start()

    def kv_y_copy(ref, k, d):
        return remote(ref, ref, r.ky_send, r.ky_recv.at[k], (z, turn(y, SIGN[d]), x, c))

    def kv_y1():
        kv_own().wait()
        for k in range(len(OTHERS)):
            kv_z_copy(k).wait()
        for d in BOTH:
            kv_y_copy(r.kvh.at[x, c, :, y], d, d).start()

    def kv_y2():
        for d in BOTH:
            yy = turn(y, -SIGN[d])
            kv_y_copy(r.kvh.at[x, c, :, yy], d, d).wait_recv()
            kv_y_copy(r.kvh.at[x, c, :, yy, pl.ds(2 * d, 2)], 2, d).start()

    def kv_y3():
        kv_y_copy(r.kvh.at[x, c, :, turn(y, 2)], 2, 0).wait_recv()
        kv_y_copy(r.kvh.at[x, c, :, pl.ds(0, LAST)], 0, 0).wait_send()

    def kv_x_copy(l, ref, k, d):
        return remote(ref, ref, r.kx_send.at[l], r.kx_recv.at[l, k], (z, y, turn(x, SIGN[d]), c))

    def kv_die(l, ref):
        return remote(ref, ref, r.kd_send.at[l], r.kd_recv.at[l], partner)

    def kv_x1(l):
        ref = r.kvh.at[x, c, l]
        for d in BOTH:
            kv_x_copy(l, ref, d, d).start()
        kv_die(l, ref).start()

    def kv_x2(l):
        for d in BOTH:
            xx = turn(x, -SIGN[d])
            ref = r.kvh.at[xx, c, l]
            kv_x_copy(l, ref, d, d).wait_recv()
            kv_x_copy(l, r.kvh.at[xx, c, l, pl.ds(2 * d, 2)], 2, d).start()
            kv_die(l, ref).start()

    def kv_x3(l):
        ref = r.kvh.at[turn(x, 2), c, l]
        kv_x_copy(l, ref, 2, 0).wait_recv()
        kv_die(l, ref).start()

    def kv_load(l):
        kv_die(l, r.kvh.at[:, 1 - c, l]).wait_recv()
        kc = r.wkv.shape[1]
        for xx in RINGS:
            for cc in BOTH:
                pltpu.make_async_copy(r.kvh.at[xx, cc, l], r.kvb.at[:, :, pl.ds((xx * CORES + cc) * kc, kc)], r.k_loc.at[1]).start()

    def kv_sent(l):
        kv_x_copy(l, r.kvh.at[pl.ds(0, LAST), c, l], 0, 0).wait_send()
        kv_die(l, r.kvh.at[:, c, l]).wait_send()

    def kv_loaded():
        pltpu.make_async_copy(r.kvb, r.kvb, r.k_loc.at[1]).wait()

    def gain_move(i, src, dst, dev):
        return remote(src, dst, r.g_send.at[i], r.g_recv.at[i], dev)

    def gain_z(k):
        dev = (turn(z, OTHERS[k]), y, x, c)
        return gain_move(k, r.gbuf.at[x, c, y, z], r.gbuf.at[x, c, y, z], dev)

    def gain_y(k):
        dev = (z, turn(y, OTHERS[k]), x, c)
        return gain_move(len(OTHERS) + k, r.gbuf.at[x, c, y], r.gbuf.at[x, c, y], dev)

    def gain_x(k):
        dev = (z, y, turn(x, OTHERS[k]), c)
        return gain_move(CORES * len(OTHERS) + k, r.gbuf.at[x, c], r.gbuf.at[x, c], dev)

    def gain_die(xx, k):
        ref = r.gbuf.at[xx, c]
        return remote(ref, ref, r.gd_send.at[k], r.gd_recv.at[k], partner)

    def gain_sum():
        for zz in RINGS:
            for yy in RINGS:
                tot = jnp.zeros((n_layers, d_row), F32)
                for xx in RINGS:
                    for cc in BOTH:
                        tot += r.gbuf[xx, cc, yy, zz, :n_layers].astype(F32)
                at = (zz * RING + yy) * d_row
                r.gain[:, at:at + d_row] = tot

    tok_pair = CORES * rows

    def x_z(k):
        zz = turn(z, OTHERS[k])
        src = r.xt.at[pl.ds(zz * seqs, seqs)]
        return remote(src, r.xz.at[z], r.xz_send.at[k], r.xz_recv.at[k], (zz, y, x, c))

    def x_own():
        return pltpu.make_async_copy(r.xt.at[pl.ds(z * seqs, seqs)], r.xz.at[z], r.x_loc)

    def pos(xx):
        return pl.ds(pl.multiple_of(xx * tok_pair, tok_pair), tok_pair)

    def x_plane(oy, ox):
        yy, xx = turn(y, oy), turn(x, ox)
        return remote(r.xz.at[:, yy, :, pos(xx)], r.xp.at[c, y, x], r.xp_send.at[oy], r.xp_recv.at[(RING - oy) % RING], (z, yy, xx, c))

    def row_bytes(oy):
        return r.xp.at[c, 0] if oy else r.xp.at[c, 0, pl.ds(0, RING - 1)]

    def x_row(oy):
        yy = turn(y, oy)
        got = row_bytes(oy)
        remote(got, got, r.xp_send.at[oy], r.xp_recv.at[oy], partner).wait_recv()
        row = r.xp.at[c, yy]
        remote(row, row, r.xd_send.at[oy], r.xd_recv.at[oy], partner).start()

    def x_turn():
        for oy in RINGS:
            row = r.xp.at[1 - c, turn(y, oy)]
            remote(row, row, r.xd_send.at[oy], r.xd_recv.at[oy], partner).wait_recv()

        @pl.loop(0, RING)
        def _(zz):
            for yy in RINGS:
                for xh in BOTH:
                    blk = [r.xp[cc, yy, CORES * xh + xx, zz] for xx in BOTH for cc in BOTH]
                    blk = jnp.concatenate(blk, axis=0).astype(F32).T.astype(BF)
                    n = blk.shape[1]
                    at = pl.multiple_of(zz * RING * d_row + yy * d_row + xh * n, n)
                    r.hb[0, 0, :, :, pl.ds(at, n)] = blk.reshape(CORES, rows, n)
        r.hid[...] = r.hb[0, 0, c]
        for oy in RINGS:
            row = r.xp.at[c, turn(y, oy)]
            remote(row, row, r.xd_send.at[oy], r.xd_recv.at[oy], partner).wait_send()

    def x_sent():
        for fn in (x_z, gain_z, gain_y, gain_x):
            peers_of(fn, "wait_send")
        for k in RINGS:
            gain_die(x, k).wait_send()
        for oy in RINGS:
            got = row_bytes(oy)
            remote(got, got, r.xp_send.at[oy], r.xp_recv.at[oy], partner).wait_send()

    def y_die(p):
        cols = pl.ds(pl.multiple_of(turn(z, p) * width, width), width)
        return remote(r.hid.at[:, cols], r.hb.at[0, 0, c, :, cols], r.yd_send.at[p], r.yd_recv.at[p], partner)

    def planes(h):
        return pl.ds(2 * h, 2)

    def y_plane(h, oy, ox):
        yy, xx = turn(y, oy), turn(x, ox)
        return remote(r.xp.at[c, yy, xx, planes(h)], r.xz.at[planes(h), y, :, pos(x)], r.yp_send.at[h, oy], r.yp_recv.at[h, (RING - oy) % RING],
                      (z, yy, xx, c))

    def y_z(p, oy):
        s = turn(y, oy)
        return remote(r.xz.at[p, s], r.y_out.at[z * seqs + s], r.yz_send.at[p, oy], r.yz_recv.at[p, oy], (turn(z, p), y, x, c))

    def y_own(oy):
        s = turn(y, oy)
        return pltpu.make_async_copy(r.xz.at[0, s], r.y_out.at[z * seqs + s], r.y_loc.at[oy])

    def leave_a(h):
        for p in BOTH:
            p = 2 * h + p
            y_die(p).start()
            cols = pl.ds(pl.multiple_of(turn(z, p) * width, width), width)
            r.hb[0, 0, c, :, cols] = r.hid[:, cols]

    def leave_b(h):
        n = CORES * CORES * d_local
        for p in BOTH:
            p = 2 * h + p
            y_die(p).wait()

            @pl.loop(0, RING)
            def _(yy, p=p):
                for xh in BOTH:
                    at = pl.multiple_of(turn(z, p) * width + yy * d_row + xh * n, n)
                    blk = r.hb[0, 0, :, :, pl.ds(at, n)].reshape(tok_pair, n).astype(F32).T.astype(BF)
                    for xx in BOTH:
                        for cc in BOTH:
                            lo = (xx * CORES + cc) * d_local
                            r.xp[cc, yy, CORES * xh + xx, p] = blk[lo:lo + d_local]

        for oy in OTHERS + (0,):
            for ox in RINGS:
                if oy or ox:
                    y_plane(h, oy, ox).start()
        for p in BOTH:
            p = 2 * h + p
            r.xz[p, y, :, pos(x)] = r.xp[c, y, x, p]

    def plane_bytes(h, oy):
        return r.xp.at[c, 0, :, planes(h)] if oy else r.xp.at[c, 0, pl.ds(0, LAST), planes(h)]

    def leave_c(h):
        for oy in OTHERS + (0,):
            got = plane_bytes(h, oy)
            remote(got, got, r.yp_send.at[h, oy], r.yp_recv.at[h, oy], partner).wait_recv()
            for p in BOTH:
                p = 2 * h + p
                (y_z(p, oy) if p else y_own(oy)).start()

    def left():
        for oy in RINGS:
            for h in BOTH:
                got = plane_bytes(h, oy)
                remote(got, got, r.yp_send.at[h, oy], r.yp_recv.at[h, oy], partner).wait_send()
            for p in RINGS:
                (y_z(p, oy) if p else y_own(oy)).wait()

    def kv_rows(zz):
        n = CORES * seq_len // (RING * RING * RING * CORES)
        return pl.ds(pl.multiple_of(((zz * RING + y) * RING + x) * n, n), n)

    def kv_trade(l, k):
        zz = turn(z, OTHERS[k])
        return remote(r.kv_out.at[l, :, :, kv_rows(zz)], r.kvx.at[l, z], r.kvx_send.at[l, k], r.kvx_recv.at[l, k], (zz, y, x, c))

    def kv_keep(l):
        return pltpu.make_async_copy(r.kv_out.at[l, :, :, kv_rows(z)], r.kvx.at[l, z], r.kvx_loc.at[l])

    def kv_share(l):
        for k in range(len(OTHERS)):
            kv_trade(l, k).start()
        kv_keep(l).start()

    def kv_shared(l):
        for k in range(len(OTHERS)):
            kv_trade(l, k).wait()
        kv_keep(l).wait()

    def gather_norm(l, split, both, pump):
        hid = r.hid
        gain = r.gain[l:l + 1, :]
        for b in range(4):
            blk = hid[b * quarter:(b + 1) * quarter, :].astype(F32)
            mean = jnp.mean(blk, axis=-1, keepdims=True)
            cen = blk - mean
            var = jnp.mean(cen * cen, axis=-1, keepdims=True)
            r.h_ref[b * quarter:(b + 1) * quarter, :] = (cen * lax.rsqrt(var + LN_EPS) * gain).astype(BF)
        out = r.h_all.at[l]

        def spot(q, first, second):
            if q == 0:
                return turn(y, second), turn(x, first)
            return turn(y, first), turn(x, second)

        def span(q, part):
            lo, n = (split, rows - split) if q else (0, split)
            if part is NIL:
                return pl.ds(lo, n)
            return pl.ds(lo + part * (n // 2), n // 2)

        table = {}

        def link(key, *args, own=False):
            idx, (q, first, second, part, to_first, to_second) = table.setdefault(key, (len(table), args))
            sy, sx = spot(q, first, second)
            ty, tx = spot(q, to_first, to_second)
            rws = span(q, part)
            dst = out.at[sy, sx, c, rws]
            return remote(r.h_ref.at[rws] if own else dst, dst, r.ag_send.at[l, KINDS.index(key[0])], r.ag_recv.at[l, idx], (z, ty, tx, c))

        def arrived(*key):
            for d in BOTH:
                link((*key, d)).wait_recv()

        def die(q, first, second, own=False):
            sy, sx = spot(q, first, second)
            rws = span(q, NIL)
            dst = out.at[sy, sx, c, rws]
            off = (first if q else second) % RING
            remote(r.h_ref.at[rws] if own else dst, dst, r.ag_dsend.at[l], r.ag_drecv.at[l, off], partner).start()

        offs = (0, -1, 1, 2)

        def second_step(k):
            for d in BOTH:
                for q in BOTH:
                    link(("second", q, k, d)).wait_recv()
                    src = -SIGN[d]
                    link(("second_on", q, k, d), q, offs[k], src, d, 0, SIGN[d]).start()
                    die(q, offs[k], src)

        def last_step(q, k):
            arrived("second_on", q, k)
            die(q, offs[k], 2)

        def tail_a():
            for k in (2, LAST):
                second_step(k)
                hook(pump, f"k{k}")
            for k in (1, 2):
                last_step(1, k)

        def tail_b():
            for k in RINGS:
                last_step(0, k)
            last_step(1, LAST)

        for q in BOTH:
            for d in BOTH:
                link(("first", q, d), q, 0, 0, NIL, SIGN[d], 0, own=True).start()
        for q in BOTH:
            for d in BOTH:
                link(("second", q, 0, d), q, 0, 0, NIL, 0, SIGN[d], own=True).start()
        for q in BOTH:
            die(q, 0, 0, own=True)
        own = pltpu.make_async_copy(r.h_ref, out.at[y, x, c], r.ag_loc)
        own.start()
        hook(pump, "begin")
        for d in BOTH:
            for q in BOTH:
                link(("first", q, d)).wait_recv()
                src = -SIGN[d]
                link(("first_on", q, d), q, src, 0, d, SIGN[d], 0).start()
                for e in BOTH:
                    link(("second", q, 1 + d, e), q, src, 0, NIL, 0, SIGN[e]).start()
                die(q, src, 0)
        hook(pump, "first")
        second_step(0)
        hook(pump, "k0")
        for q in BOTH:
            arrived("first_on", q)
            for e in BOTH:
                link(("second", q, LAST, e), q, 2, 0, NIL, 0, SIGN[e]).start()
            die(q, 2, 0)
        hook(pump, "first_on")
        second_step(1)
        hook(pump, "k1")
        last_step(1, 0)
        own.wait()
        if not both:
            tail_a()
        hook(pump, "ready")

        def crossed(off):
            got = out.at[turn(y, off), :, 1 - c]
            remote(got, got, r.ag_dsend.at[l], r.ag_drecv.at[l, off], partner).wait_recv()

        def order(i):
            return lax.rem(3 * i + 3 * (i // 2) + 2 * (i // 3), RING)

        crossed(0)
        h_copy(l, y, 0).start()

        @pl.loop(0, RING)
        def _(i):
            slot = lax.rem(i, 2)
            s = turn(y, order(i))
            h_copy(l, s, slot).wait()
            pump(("seq", i))
            one(l, s, slot, i)

            @pl.when(i == 0)
            def _():
                (tail_a if both else tail_b)()

            if both:
                @pl.when(i == 1)
                def _():
                    tail_b()

            @pl.when(i < LAST)
            def _():
                crossed(order(i + 1))
                h_copy(l, turn(y, order(i + 1)), 1 - slot).start()

            if both:
                two(s, slot)

        for slot in BOTH:
            for i in BOTH:
                kv_out_copy(l, 0, slot, i).wait()
        sent = (out.at[y, x], out.at[y], out.at[y, x, c], out.at[y, pl.ds(0, CORES)])
        for kind, ref in enumerate(sent):
            remote(ref, ref, r.ag_send.at[l, kind], r.ag_recv.at[l, kind], partner).wait_send()
        remote(out.at[pl.ds(0, 2)], out.at[pl.ds(0, 2)], r.ag_dsend.at[l], r.ag_drecv.at[l, 0], partner).wait_send()

    def h_copy(l, s, slot):
        return pltpu.make_async_copy(r.h_all.at[l, s], r.hb.at[slot], r.h_sem.at[slot])

    def h_tile(slot):
        return r.hb[slot].reshape(seq_len, d_model)

    def project(h, lo, n):
        w = r.wv[:, :, lo:lo + n].reshape(d_model, n)
        return jnp.dot(h, w, preferred_element_type=F32).astype(BF)

    def rope(val):
        val = val.astype(F32)
        return val * r.cos[...] + pltpu.roll(val, head_dim // 2, 1) * r.sin[...]

    n_chunk = min(256, f_loc)

    def kv_out_copy(l, s, slot, i):
        return pltpu.make_async_copy(r.qkv.at[slot, i], r.kv_out.at[l, i, s], r.kvo_sem.at[slot, i])

    def one(l, s, slot, i):
        @pl.when(i >= 2)
        def _():
            for k in BOTH:
                kv_out_copy(l, s, slot, k).wait()

        kv = jnp.zeros((seq_len, 2 * head_dim), F32)
        for zz in RINGS:
            for yy in RINGS:
                col = (zz * RING + yy) * d_row
                kv += lax.dot_general(h_cols(slot, col, d_row), r.kvb[yy, zz], (((1,), (1,)), ((), ())), preferred_element_type=F32)
        kv = kv.astype(BF)
        r.qkv[slot, 0] = rope(kv[:, :head_dim]).astype(BF)
        r.qkv[slot, 1] = kv[:, head_dim:]
        for i in BOTH:
            kv_out_copy(l, s, slot, i).start()
        q = project(h_tile(slot), 0, head_dim)
        r.stage[...] = (rope(q) * head_dim ** -0.5).astype(BF)
        for lo in range(0, f_loc, n_chunk):
            r.joined[s, :, head_dim + lo:head_dim + lo + n_chunk] = project(h_tile(slot), head_dim + lo, n_chunk)
        n_tile = seq_len // 2
        for i in BOTH:
            keys = (i + 1) * n_tile
            sc = lax.dot_general(r.stage[i * n_tile:(i + 1) * n_tile, :], r.qkv[slot, 0, :keys, :], (((1,), (1,)), ((), ())), preferred_element_type=F32)
            row_id = lax.broadcasted_iota(jnp.int32, sc.shape, 0) + i * n_tile
            col_id = lax.broadcasted_iota(jnp.int32, sc.shape, 1)
            sc = jnp.where(col_id <= row_id, sc, -1e30)
            top = jnp.max(sc, axis=-1, keepdims=True)
            ex = jnp.exp(sc - top)
            prob = (ex * (1.0 / jnp.sum(ex, axis=-1, keepdims=True))).astype(BF)
            att = jnp.dot(prob, r.qkv[slot, 1, :keys, :], preferred_element_type=F32)
            r.joined[s, i * n_tile:(i + 1) * n_tile, :head_dim] = att.astype(BF)

    def h_cols(slot, col, n):
        return r.hb[slot, :, :, :, col:col + n].reshape(seq_len, n)

    def two(s, slot):
        for lo in range(0, f_loc, n_chunk):
            up = project(h_tile(slot), head_dim + f_loc + lo, n_chunk).astype(F32)
            cols = slice(head_dim + lo, head_dim + lo + n_chunk)
            g = r.joined[s, :, cols].astype(F32)
            r.joined[s, :, cols] = (g * jax.nn.sigmoid(g) * up).astype(BF)

    def pass_two(l, pump):
        h_copy(l, 0, 0).start()

        @pl.loop(0, RING)
        def _(s):
            slot = lax.rem(s, 2)
            h_copy(l, s, slot).wait()

            @pl.when(s + 1 < RING)
            def _():
                h_copy(l, s + 1, 1 - slot).start()

            pump(s)
            two(s, slot)

    def out_scatter(l, pump):
        def peer(q, first, second):
            dy = first * (1 - q) + second * q
            dx = first * q + second * (1 - q)
            return (z, turn(y, dy), turn(x, dx), c)

        def die_copy(ch, q, s):
            return remote(r.away.at[q], r.die_in.at[ch, q, s], r.dsend.at[l, ch, q, s], r.drecv.at[l, ch, q, s], partner)

        def first_copy(ch, q, d):
            return remote(r.acc.at[ch, q, 0, pl.ds(CORES * d, CORES)], r.in1.at[ch, q, d], r.send1.at[l, ch, q, d], r.recv1.at[l, ch, q, d],
                          peer(q, SIGN[d], 0))

        def second_copy(ch, q, d, h):
            js = pl.ds(CORES * h, CORES)
            return remote(r.acc.at[ch, q, 1 + d, js], r.in2.at[ch, q, d, js], r.send2.at[l, ch, q, d, h], r.recv2.at[l, ch, q, d, h],
                          peer(q, SIGN[d], 0))

        def half_rows(d):
            return pl.ds(d * (rows // 2), rows // 2)

        def third_copy(ch, q, d):
            return remote(r.acc.at[ch, q, LAST, 0, half_rows(d)], r.in3.at[ch, q, d], r.send3.at[l, ch, q, d], r.recv3.at[l, ch, q, d],
                          peer(q, 0, SIGN[d]))

        def fourth_copy(ch, q, d):
            return remote(r.acc.at[ch, q, LAST, 1 + d], r.in4.at[ch, q, d], r.send4.at[l, ch, q, d], r.recv4.at[l, ch, q, d],
                          peer(q, 0, SIGN[d]))

        n_blk = r.wov.shape[3]

        def plane_of(ch, q):
            if l:
                return turn(z, q if ch else 2 + q)
            return turn(z, LAST - q if ch else q)

        def tile(ch, q, s):
            for cc in BOTH:
                for j in RINGS:
                    oy = SLOT_OFF[s] * (1 - q) + SLOT_OFF[j] * q
                    ox = SLOT_OFF[j] * (1 - q) + SLOT_OFF[s] * q
                    core = c if cc else 1 - c
                    at = pl.multiple_of((turn(x, ox) * CORES + core) * rows, rows)
                    r.lhs[pl.ds((cc * RING + j) * rows, rows), :] = r.joined[turn(y, oy), pl.ds(at, rows), :]
            left = r.lhs[...]
            zz = plane_of(ch, q)

            @pl.loop(0, RING)
            def _(n):
                col = pl.multiple_of(n * n_blk, n_blk)
                res = jnp.dot(left, r.wov[zz, n], preferred_element_type=F32).astype(BF)
                res = res.reshape(CORES, RING, rows, n_blk)
                r.away[q, :, :, pl.ds(col, n_blk)] = res[0]
                r.acc[ch, q, s, :, :, pl.ds(col, n_blk)] = res[1]

        def pair_sum(ch, q, s):
            die_copy(ch, q, s).wait_recv()

            @pl.loop(0, RING)
            def _(j):
                r.acc[ch, q, s, j] = r.acc[ch, q, s, j] + r.die_in[ch, q, s, j]

        def stage_a(ch):
            for s in RINGS:
                @pl.loop(0, CORES)
                def _(q, s=s):
                    if s:
                        die_copy(ch, q, s - 1).wait_send()
                    elif ch:
                        die_copy(ch - 1, q, LAST).wait_send()
                    tile(ch, q, s)
                    die_copy(ch, q, s).start()
                    if s:
                        pair_sum(ch, q, s - 1)
                    if s == 1:
                        for d in BOTH:
                            first_copy(ch, q, d).start()
                    if s > 1:
                        second_copy(ch, q, s - 2, LAST - s).start()
                if s == 1:
                    hook(pump, f"mid{ch}")

        def stage_b(ch):
            for q in BOTH:
                pair_sum(ch, q, LAST)
            for q in BOTH:
                for d in BOTH:
                    first_copy(ch, q, d).wait_recv()
                    for j in BOTH:
                        at = CORES * d + j
                        r.acc[ch, q, 1 + d, at] = r.acc[ch, q, 1 + d, at] + r.in1[ch, q, d, j]
                    second_copy(ch, q, d, d).start()

        def total(ch, q, j):
            val = r.acc[ch, q, LAST, j].astype(F32)
            for d in BOTH:
                val += r.in2[ch, q, d, j].astype(F32)
            r.acc[ch, q, LAST, j] = val.astype(BF)

        def stage_c(ch):
            for q in BOTH:
                for h in BOTH:
                    for d in BOTH:
                        second_copy(ch, q, d, h).wait_recv()
                total(ch, q, 0)
                for d in BOTH:
                    third_copy(ch, q, d).start()
                for j in RINGS[1:]:
                    total(ch, q, j)

        def stage_d(ch):
            for q in BOTH:
                for d in BOTH:
                    third_copy(ch, q, d).wait_recv()
                    rws = half_rows(d)
                    r.acc[ch, q, LAST, 1 + d, rws] = r.acc[ch, q, LAST, 1 + d, rws] + r.in3[ch, q, d]
                    fourth_copy(ch, q, d).start()

        def stage_e(ch):
            for q in BOTH:
                for d in BOTH:
                    fourth_copy(ch, q, d).wait_recv()
                cols = pl.ds(pl.multiple_of(plane_of(ch, q) * width, width), width)
                upd = r.acc[ch, q, LAST, LAST].astype(F32)
                for d in BOTH:
                    upd += r.in4[ch, q, d].astype(F32)
                upd = upd.astype(BF)
                r.hid[:, cols] = (r.hid[:, cols].astype(F32) + upd.astype(F32)).astype(BF)

        def sent(ch):
            for q in BOTH:
                if ch:
                    die_copy(ch, q, LAST).wait_send()
                for d in BOTH:
                    for cp in (first_copy, third_copy, fourth_copy):
                        cp(ch, q, d).wait_send()
                    for h in BOTH:
                        second_copy(ch, q, d, h).wait_send()

        for step, fn, ch in (
            ("a0", stage_a, 0), ("b0", stage_b, 0), ("a1", stage_a, 1), ("c0", stage_c, 0), ("b1", stage_b, 1),
            ("d0", stage_d, 0), ("e0", stage_e, 0), ("c1", stage_c, 1), ("d1", stage_d, 1), ("e1", stage_e, 1),
        ):
            with jax.named_scope(step):
                fn(ch)
            hook(pump, step)
        for ch in BOTH:
            sent(ch)

    def near(fn, t):
        for j in (LAST, 1):
            fn(t, j)

    def far(fn, t):
        fn(t, 2)

    def z_all(t):
        near(z_direct, t)
        far(z_direct, t)

    def peers_of(fn, op="start"):
        for k in range(len(OTHERS)):
            getattr(fn(k), op)()

    def start():
        peers_of(x_z)
        peers_of(gain_z)
        x_own().start()
        z_own(QG0)
        z_own(UP0)
        with jax.named_scope("gain_a"):
            peers_of(gain_z, "wait_recv")
            peers_of(gain_y)
            peers_of(gain_y, "wait_recv")
            peers_of(gain_x)
            gain_die(x, LAST).start()
        with jax.named_scope("x_z"):
            peers_of(x_z, "wait_recv")
            x_own().wait()
        for oy in RINGS:
            for ox in RINGS:
                if oy or ox:
                    x_plane(oy, ox).start()
        r.xp[c, y, x] = r.xz[:, y, :, pos(x)]
        kv_z()
        with jax.named_scope("gain_b"):
            for k, o in enumerate(OTHERS):
                gain_x(k).wait_recv()
                gain_die(turn(x, -o), k).start()
        y_send(QG0)
        with jax.named_scope("rows"):
            for oy in (0, LAST, 1, 2):
                x_row(oy)
        with jax.named_scope("gain_sum"):
            for k in RINGS:
                gain_die(x, k).wait_recv()
            gain_sum()
        with jax.named_scope("turn"):
            x_turn()

    def when(i, n, *fns):
        @pl.when(i == n)
        def _():
            for fn in fns:
                fn()

    def plan(steps):
        def pump(step):
            for fn, *args in steps.get(step, ()):
                fn(*args)
        return pump

    def both_loaded(t):
        loaded(t)
        kv_loaded()

    first_gather = plan({
        "begin": [(z_forward, QG0, 0)],
        "first": [(kv_y1,), (near, z_direct, QG0), (y_relay, QG0), (z_forward, UP0, 0)],
        "k0": [(kv_y2,), (y_send, UP0)],
        "first_on": [(far, z_direct, QG0), (kv_y3,), (kv_x1, 0)],
        "k1": [(near, z_forward, QG0)],
        "k2": [(kv_x2, 0), (y_relay, UP0), (far, z_forward, QG0), (near, z_direct, UP0)],
        "k3": [(far, z_direct, UP0), (z_own, WO0), (y_send, WO0), (kv_x3, 0)],
        "ready": [(finish, QG0), (kv_load, 0), (both_loaded, QG0)],
    })

    def first_front(step):
        if isinstance(step, str):
            first_gather(step)
            return
        i = step[1]
        when(i, 0, lambda: z_forward(UP0, LAST), lambda: z_forward(UP0, 1), lambda: y_relay(WO0))
        when(i, 1, lambda: z_forward(UP0, 2), lambda: z_direct(WO0, LAST), lambda: z_direct(WO0, 1), x_sent)
        when(i, 2, lambda: y_send(QG1), lambda: z_direct(WO0, 2), lambda: kv_x1(1))
        when(i, LAST, lambda: z_forward(WO0, 0))

    def first_two(s):
        when(s, 0, lambda: z_forward(WO0, LAST), lambda: z_own(QG1), lambda: y_send(WO1))
        when(s, 1, lambda: z_forward(WO0, 1), lambda: y_relay(QG1))
        when(s, 2, lambda: z_forward(WO0, 2), lambda: kv_x2(1))
        when(s, LAST, lambda: near(z_direct, QG1))

    first_scatter = plan({
        "mid0": [(load_far, WO0)],
        "b0": [(far_loaded, WO0), (z_forward, QG1, 0)],
        "a1": [(near, z_forward, QG1), (y_relay, WO1)],
        "c0": [(far, z_forward, QG1), (z_own, UP1)],
        "b1": [(z_all, UP1)],
        "c1": [(finish, QG1), (kv_load, 1)],
    })
    second_gather = plan({
        "first": [(z_forward, UP1, 0)],
        "k0": [(near, z_forward, UP1)],
        "first_on": [(far, z_forward, UP1), (z_own, WO1)],
        "k1": [(z_all, WO1), (finish, UP1)],
        "ready": [(both_loaded, QG1), (loaded, UP1)],
    })

    def second_front(step):
        if isinstance(step, str):
            second_gather(step)
        else:
            z_forward(WO1, step[1])

    second_scatter = plan({
        "e0": [(leave_a, 1)],
        "c1": [(leave_b, 1)],
        "d1": [(leave_c, 1)],
    })

    with jax.named_scope("start"):
        start()
    with jax.named_scope("front_0"):
        gather_norm(0, rows // RING, False, first_front)
    with jax.named_scope("finish_1"):
        kv_share(0)
        finish(UP0)
        y_send(UP1)
        loaded(UP0)
    with jax.named_scope("pass_two_0"):
        pass_two(0, first_two)
    with jax.named_scope("near_2"):
        load_near(WO0)
        y_relay(UP1)
        kv_x3(1)
        far(z_direct, QG1)
        near_loaded(WO0)
    with jax.named_scope("scatter_0"):
        out_scatter(0, first_scatter)
    with jax.named_scope("front_1"):
        gather_norm(1, rows // 2, True, second_front)
    with jax.named_scope("finish_5"):
        kv_share(1)
        finish(WO1)
        loaded(WO1)
    with jax.named_scope("scatter_1"):
        out_scatter(1, second_scatter)
    with jax.named_scope("leave"):
        leave_a(0)
        leave_b(0)
        leave_c(0)
        left()
    with jax.named_scope("drain"):
        for t in range(WO1 + 1):
            drain(t)
        for l in range(n_layers):
            kv_shared(l)
            kv_sent(l)


def run_model(xt, gain, wkv_t, w_in, w_out, cos_full, sin_full):
    batch, d_local, seq_len = xt.shape
    n_layers, d_row, e_block = w_in.shape
    r_block, d_col = w_out.shape[1:]
    head_dim = cos_full.shape[1]
    d_model = d_row * RING * RING
    seqs = batch // RING
    rows = seqs * seq_len // (RING * RING * CORES)
    e_loc, r_loc = e_block // RING, r_block // RING
    kc = wkv_t.shape[1]
    width = d_model // RING
    n_t = 3 * n_layers
    n_o = len(OTHERS)

    def dma(*shape):
        return pltpu.SemaphoreType.DMA(shape)

    def vm(*shape):
        return pltpu.VMEM(shape, BF)

    def out(*shape):
        return jax.ShapeDtypeStruct(shape, BF)

    any_spec = pl.BlockSpec(memory_space=pl.ANY)
    vm_spec = pl.BlockSpec(memory_space=pltpu.VMEM)
    out_shape = [
        out(batch, d_local, seq_len),
        out(n_layers, 2, seqs, seq_len, head_dim),
        out(n_layers, RING, RING, CORES, rows, d_model),
        out(n_layers, RING, RING * d_row, e_loc),
        out(n_layers, RING, RING, r_loc, d_col),
        out(RING, CORES, n_layers, RING, RING, kc, d_row),
        out(n_layers, RING, 2, seqs, CORES * (seq_len // (CORES * RING * RING * RING)), head_dim),
        out(n_layers, 2, d_row // 2, e_loc),
        out(n_layers, 2, r_loc // 2, d_col),
    ]
    pair = (2, 2, 2)
    each = (n_layers, *pair)
    scratch = [
        vm(rows, d_model), vm(rows, d_model), pltpu.VMEM((n_layers, d_model), F32),
        vm(RING, CORES, RING, RING, G_ROWS, d_row),
        vm(RING, seqs, d_local, seq_len),
        vm(CORES, RING, RING, RING, d_local, CORES * rows),
        vm(RING, RING * d_row, e_loc), vm(RING, RING, 2 * head_dim, d_row), vm(RING, RING, r_loc, d_col),
        vm(2, RING, CORES, rows, d_model), vm(RING, seq_len, r_loc), vm(2, 2, seq_len, head_dim), vm(seq_len, head_dim),
        vm(CORES * RING * rows, r_loc), vm(2, RING, rows, width), vm(2, 2, RING, RING, rows, width), vm(2, 2, RING, RING, rows, width),
        vm(*pair, 2, rows, width), vm(*pair, RING, rows, width), vm(*pair, rows // 2, width), vm(*pair, rows, width),
        dma(n_o), dma(n_o), dma(RING), dma(RING), dma(RING), dma(RING), pltpu.SemaphoreType.DMA,
        dma(3 * n_o), dma(3 * n_o), dma(RING), dma(RING),
        dma(RING), dma(RING), dma(2, RING), dma(2, RING), dma(RING, RING), dma(RING, RING), dma(RING),
        dma(n_layers, RING), dma(n_layers, 40), dma(n_layers), dma(n_layers, RING), pltpu.SemaphoreType.DMA, dma(2), dma(2, 2), dma(3), dma(3),
        dma(n_t, RING), dma(n_t, 2), dma(n_t, RING, 2), dma(n_t, RING, 2), dma(n_t, RING),
        dma(n_o), dma(n_o), pltpu.SemaphoreType.DMA, dma(n_o), dma(n_layers), dma(n_layers, n_o), dma(n_layers), dma(n_layers), dma(2),
        dma(n_layers, 2, 2, RING), dma(n_layers, 2, 2, RING),
        dma(*each), dma(*each), dma(*each, 2), dma(*each, 2), dma(*each), dma(*each), dma(*each), dma(*each),
        dma(n_layers, n_o), dma(n_layers, n_o), dma(n_layers),
    ]
    res = pl.pallas_call(
        model_kernel,
        out_shape=out_shape,
        in_specs=[any_spec, vm_spec, vm_spec, any_spec, any_spec, vm_spec, vm_spec],
        out_specs=[any_spec] * len(out_shape),
        scratch_shapes=scratch,
        compiler_params=pltpu.CompilerParams(collective_id=0, has_side_effects=True, vmem_limit_bytes=VMEM_LIMIT),
        name="two_layers",
    )(xt, gain, wkv_t, w_in, w_out, cos_full, sin_full)
    return res[0], res[6]


def solution(mesh):
    row_size = mesh.shape["row"]
    n_col = mesh.shape["col"]
    n_z = row_size // RING
    n_y = RING
    n_x = n_col // CORES
    n_tp = n_y * n_col
    n_dev = row_size * n_col
    mesh4 = Mesh(mesh.devices.reshape(n_z, n_y, n_x, CORES), ("z", "y", "x", "core"))
    every = ("z", "y", "x", "core")
    col = ("x", "core")
    act_spec = P(NIL, NIL, every)
    w_spec = P(NIL, ("z", "y"), col)

    def device_fn(x_loc, gain_loc, w_in_loc, w_kv_loc, w_out_loc):
        n_layers = w_in_loc.shape[0]
        n_batch, seq_len, d_local = x_loc.shape
        head_dim = w_kv_loc.shape[2] * n_col // 2
        batch_loc = n_batch // n_z
        seq_local = seq_len // n_dev
        steps = np.arange(head_dim // 2, dtype=np.float32)
        inv_freq = (1.0 / 10000.0 ** (steps * 2 / head_dim)).astype(np.float32)
        angles = np.arange(seq_len, dtype=np.float32)[:, NIL] * inv_freq[NIL, :]
        cos_tab, sin_tab = np.cos(angles), np.sin(angles)
        cos_full = jnp.asarray(np.concatenate([cos_tab, cos_tab], axis=1))
        sin_full = jnp.asarray(np.concatenate([-sin_tab, sin_tab], axis=1))
        y_loc, kv = run_model(x_loc.transpose(0, 2, 1), gain_loc, w_kv_loc.transpose(0, 2, 1), w_in_loc, w_out_loc, cos_full, sin_full)
        y_loc = y_loc.transpose(0, 2, 1)
        kv = kv.reshape(n_layers, n_z, 2, batch_loc, CORES, seq_local, head_dim)
        kv = lax.dynamic_index_in_dim(kv, lax.axis_index("core"), axis=4, keepdims=False)
        kv = kv.transpose(0, 2, 1, 3, 4, 5).reshape(n_layers, 2, n_batch, seq_local, head_dim)
        return y_loc, kv

    return jax.shard_map(device_fn, mesh=mesh4, in_specs=(act_spec, P(NIL, every), w_spec, w_spec, P(NIL, col, ("z", "y"))), out_specs=(act_spec, P(NIL, NIL, NIL, every, NIL)), check_vma=False)
```

```python
import jax
import jax.numpy as jnp
import numpy as np
from jax import lax
from jax.experimental import pallas as pl
from jax.experimental.pallas import tpu as pltpu
from jax.sharding import Mesh
from jax.sharding import PartitionSpec as P

LN_EPS = 1e-6
RING = 4
CORES = 2
VMEM_LIMIT = 67_000_000
BF = jnp.bfloat16
F32 = jnp.float32
SLOT_OFF = (2, 1, 3, 0)
SIGN = (1, -1)
NIL = None
BOTH = range(CORES)
RINGS = range(RING)
OTHERS = (1, 3, 2)
LAST = RING - 1
G_ROWS = 8
QG0, UP0, WO0, QG1, UP1, WO1 = range(6)
KINDS = ("first", "second", "first_on", "second_on")
NAMES = (
    "xt", "gain_in", "wkv", "w_in", "w_out", "cos", "sin", "y_out", "kv_out", "h_all", "wi", "wo", "kvh", "kvx", "rwi", "rwo", "h_ref",
    "hid", "gain", "gbuf", "xz", "xp",
    "wv", "kvb", "wov", "hb", "joined", "qkv", "stage", "lhs", "away", "acc", "die_in", "in1", "in2", "in3", "in4",
    "xz_send", "xz_recv", "xp_send", "xp_recv", "xd_send", "xd_recv", "x_loc", "g_send", "g_recv", "gd_send", "gd_recv", "yd_send", "yd_recv", "yp_send", "yp_recv", "yz_send", "yz_recv", "y_loc",
    "ag_send", "ag_recv", "ag_dsend", "ag_drecv", "ag_loc", "h_sem", "kvo_sem", "w_load", "far_load", "y_recv", "ry_recv", "zb_recv",
    "zc_recv", "w_send", "kz_send", "kz_recv", "ky_send", "ky_recv", "kx_send", "kx_recv", "kd_send", "kd_recv",
    "k_loc", "dsend", "drecv", "send1", "recv1", "send2", "recv2", "send3", "recv3", "send4", "recv4", "kvx_send", "kvx_recv", "kvx_loc",
)


class Refs:
    def __init__(self, refs):
        for name, ref in zip(NAMES, refs, strict=True):
            setattr(self, name, ref)


def model_kernel(*refs):
    r = Refs(refs)
    z, y, x, c = (lax.axis_index(a) for a in ("z", "y", "x", "core"))
    n_layers = r.wkv.shape[0]
    rows, d_model = r.hid.shape
    batch, d_local = r.xt.shape[:2]
    seqs = batch // RING
    seq_len, head_dim = r.cos.shape
    d_row = r.w_in.shape[1]
    e_loc = r.wi.shape[3]
    depth = r.wo.shape[3]
    f_loc = depth - head_dim
    quarter = rows // 4
    width = d_model // RING
    q_block = head_dim * RING
    f_block = f_loc * RING

    def turn(base, off):
        return lax.rem(base + off + RING, RING)

    def remote(src, dst, ssem, rsem, dev):
        return pltpu.make_async_remote_copy(
            src_ref=src, dst_ref=dst, send_sem=ssem, recv_sem=rsem, device_id=dev, device_id_type=pl.DeviceIdType.MESH)

    partner = (z, y, x, 1 - c)

    peers = [(turn(z, o), y, x, c) for o in OTHERS]
    peers += [(z, turn(y, oy), turn(x, ox), c) for oy in RINGS for ox in RINGS if oy or ox]
    peers.append(partner)
    here = (z, y, x, c)
    gate_sem = pltpu.get_barrier_semaphore()
    for dev in peers:
        pl.semaphore_signal(gate_sem, inc=1, device_id=dev, device_id_type=pl.DeviceIdType.MESH)
    src_id = lax.broadcasted_iota(jnp.int32, (d_local, d_row), 0) + (x * CORES + c) * d_local
    dst_id = lax.broadcasted_iota(jnp.int32, (d_local, d_row), 1)
    spread = jnp.where(src_id == dst_id, 1.0, 0.0).astype(BF)
    r.gbuf[x, c, y, z] = jnp.zeros((G_ROWS, d_row), BF)
    r.gbuf[x, c, y, z, :n_layers] = jnp.dot(r.gain_in[...], spread, preferred_element_type=F32).astype(BF)
    pl.semaphore_wait(gate_sem, len(peers))

    def hook(pump, i):
        with jax.named_scope(f"hook_{i}"):
            pump(i)

    def w_cols(kind):
        return pl.ds(0, head_dim + f_loc) if kind == 0 else pl.ds(head_dim + f_loc, f_loc)

    def piece(t, zz, yy):
        l, kind = t // 3, t % 3
        if kind == 2:
            return r.wo.at[l, zz, yy]
        return r.wi.at[l, zz, pl.ds(pl.multiple_of(yy * d_row, d_row), d_row), w_cols(kind)]

    def piece_half(t, zz, yy, h):
        l, kind = t // 3, t % 3
        if kind == 2:
            return r.wo.at[l, zz, yy, pl.ds(h * (depth // 2), depth // 2)]
        return r.wi.at[l, zz, pl.ds(pl.multiple_of(yy * d_row + h * (d_row // 2), d_row // 2), d_row // 2), w_cols(kind)]

    def own_parts(t, owner, zz, yy):
        l, kind = t // 3, t % 3
        hq = pl.ds(pl.multiple_of(owner * head_dim, head_dim), head_dim)
        if kind == 2:
            return [
                (r.w_out.at[l, hq], r.wo.at[l, zz, yy, pl.ds(0, head_dim)]),
                (r.w_out.at[l, pl.ds(pl.multiple_of(q_block + owner * f_loc, head_dim), f_loc)], r.wo.at[l, zz, yy, pl.ds(head_dim, f_loc)]),
            ]
        rws = pl.ds(pl.multiple_of(yy * d_row, d_row), d_row)
        if kind == 0:
            return [
                (r.w_in.at[l, :, hq], r.wi.at[l, zz, rws, pl.ds(0, head_dim)]),
                (r.w_in.at[l, :, pl.ds(pl.multiple_of(q_block + owner * f_loc, head_dim), f_loc)], r.wi.at[l, zz, rws, pl.ds(head_dim, f_loc)]),
            ]
        return [(r.w_in.at[l, :, pl.ds(pl.multiple_of(q_block + f_block + owner * f_loc, head_dim), f_loc)],
                 r.wi.at[l, zz, rws, pl.ds(head_dim + f_loc, f_loc)])]

    def relay_ref(t, d):
        l, kind = t // 3, t % 3
        return r.rwo.at[l, d] if kind == 2 else r.rwi.at[l, d, :, w_cols(kind)]

    def far_parts(t, d):
        l, kind = t // 3, t % 3
        owner = turn(y, 2)
        hq = pl.ds(pl.multiple_of(owner * head_dim, head_dim), head_dim)
        if kind == 2:
            n = depth // 2
            base = q_block + owner * f_loc
            if d:
                return [(r.w_out.at[l, pl.ds(pl.multiple_of(base + n - head_dim, G_ROWS), n)], r.rwo.at[l, d])]
            return [
                (r.w_out.at[l, hq], r.rwo.at[l, d, pl.ds(0, head_dim)]),
                (r.w_out.at[l, pl.ds(pl.multiple_of(base, head_dim), n - head_dim)], r.rwo.at[l, d, pl.ds(head_dim, n - head_dim)]),
            ]
        rws = pl.ds(d * (d_row // 2), d_row // 2)
        if kind == 0:
            return [
                (r.w_in.at[l, rws, hq], r.rwi.at[l, d, :, pl.ds(0, head_dim)]),
                (r.w_in.at[l, rws, pl.ds(pl.multiple_of(q_block + owner * f_loc, head_dim), f_loc)], r.rwi.at[l, d, :, pl.ds(head_dim, f_loc)]),
            ]
        return [(r.w_in.at[l, rws, pl.ds(pl.multiple_of(q_block + f_block + owner * f_loc, head_dim), f_loc)], relay_ref(t, d))]

    def y_send(t):
        for d in BOTH:
            owner = turn(y, SIGN[d])
            dev = (z, owner, x, c)
            for src, dst in far_parts(t, d):
                remote(src, dst, r.w_send.at[t, 0], r.ry_recv.at[t, d], dev).start()
            for src, dst in own_parts(t, owner, z, y):
                remote(src, dst, r.w_send.at[t, 0], r.y_recv.at[t, -SIGN[d] % RING], dev).start()

    def y_relay(t):
        for d in BOTH:
            ref = relay_ref(t, d)
            remote(ref, ref, r.w_send.at[t, 3], r.ry_recv.at[t, d], here).wait_recv()
            dst = piece_half(t, z, turn(y, -SIGN[d]), d)
            remote(ref, dst, r.w_send.at[t, 3], r.y_recv.at[t, 2], (z, turn(y, SIGN[d]), x, c)).start()

    def z_own(t):
        for d in BOTH:
            for src, dst in own_parts(t, y, z, y):
                remote(src, dst, r.w_send.at[t, 1], r.zb_recv.at[t, 0, d], (turn(z, SIGN[d]), y, x, c)).start()

    def z_direct(t, j):
        yy = turn(y, j)
        ref = piece(t, z, yy)
        remote(ref, ref, r.w_send.at[t, 0], r.y_recv.at[t, j], here).wait_recv()
        for d in BOTH:
            remote(ref, ref, r.w_send.at[t, 1], r.zb_recv.at[t, j, d], (turn(z, SIGN[d]), y, x, c)).start()

    def z_forward(t, j):
        yy = turn(y, j)
        for d in BOTH:
            zz = turn(z, -SIGN[d])
            ref = piece(t, zz, yy)
            remote(ref, ref, r.w_send.at[t, 1], r.zb_recv.at[t, j, d], here).wait_recv()
            part = piece_half(t, zz, yy, d)
            remote(part, part, r.w_send.at[t, 2], r.zc_recv.at[t, j, d], (turn(z, SIGN[d]), y, x, c)).start()

    def place(t, zz):
        l, kind = t // 3, t % 3
        if kind == 2:
            return r.wo.at[l, zz], r.wov.at[zz]
        return r.wi.at[l, zz, :, w_cols(kind)], r.wv.at[zz, :, w_cols(kind)]

    def load_near(t):
        kind = t % 3
        for d in BOTH:
            src, dst = place(t, turn(z, SIGN[d]))
            pltpu.make_async_copy(src, dst, r.w_load.at[kind]).start()
        for j in OTHERS:
            yy = turn(y, j)
            dst = r.wov.at[z, yy] if kind == 2 else r.wv.at[z, pl.ds(pl.multiple_of(yy * d_row, d_row), d_row), w_cols(kind)]
            pltpu.make_async_copy(piece(t, z, yy), dst, r.w_load.at[kind]).start()
        for src, dst in own_parts(t, y, z, y):
            pltpu.make_async_copy(src, own_place(t, dst, src), r.w_load.at[kind]).start()

    def load_far(t):
        far = turn(z, 2)
        for j in RINGS:
            for d in BOTH:
                part = piece_half(t, far, turn(y, j), d)
                remote(part, part, r.w_send.at[t, 2], r.zc_recv.at[t, j, d], here).wait_recv()
        src, dst = place(t, far)
        pltpu.make_async_copy(src, dst, r.far_load.at[t % 3]).start()

    def own_place(t, dst, src):
        kind = t % 3
        if kind == 2:
            n = src.shape[0]
            return r.wov.at[z, y, pl.ds(0 if n == head_dim and f_loc != head_dim else head_dim, n)]
        n = src.shape[1]
        rws = pl.ds(pl.multiple_of(y * d_row, d_row), d_row)
        if kind == 0:
            return r.wv.at[z, rws, pl.ds(0 if n == head_dim and f_loc != head_dim else head_dim, n)]
        return r.wv.at[z, rws, pl.ds(head_dim + f_loc, f_loc)]

    def finish(t):
        load_near(t)
        load_far(t)

    def near_loaded(t):
        kind = t % 3
        dst = r.wov.at[pl.ds(0, LAST)] if kind == 2 else r.wv.at[pl.ds(0, LAST), :, w_cols(kind)]
        pltpu.make_async_copy(dst, dst, r.w_load.at[kind]).wait()

    def far_loaded(t):
        kind = t % 3
        dst = r.wov.at[0] if kind == 2 else r.wv.at[0, :, w_cols(kind)]
        pltpu.make_async_copy(dst, dst, r.far_load.at[kind]).wait()

    def loaded(t):
        near_loaded(t)
        far_loaded(t)

    def drain(t):
        l, kind = t // 3, t % 3
        if kind == 2:
            done = (r.wo.at[l, 0, pl.ds(0, LAST)], r.wo.at[l, pl.ds(0, 2)], r.wo.at[l, 0], r.wo.at[l, 0, 0])
        else:
            cols = w_cols(kind)
            done = (r.wi.at[l, 0, pl.ds(0, LAST * d_row), cols], r.wi.at[l, pl.ds(0, 2), :, cols], r.wi.at[l, 0, :, cols],
                    r.wi.at[l, 0, pl.ds(0, d_row), cols])
        for g, ref in enumerate(done):
            remote(ref, ref, r.w_send.at[t, g], r.y_recv.at[t, 0], here).wait_send()

    def kv_z_copy(k):
        return remote(r.wkv, r.kvh.at[x, c, :, y, z], r.kz_send.at[k], r.kz_recv.at[k], (turn(z, OTHERS[k]), y, x, c))

    def kv_own():
        return pltpu.make_async_copy(r.wkv, r.kvh.at[x, c, :, y, z], r.k_loc.at[0])

    def kv_z():
        for k in range(len(OTHERS)):
            kv_z_copy(k).start()
        kv_own().start()

    def kv_y_copy(ref, k, d):
        return remote(ref, ref, r.ky_send, r.ky_recv.at[k], (z, turn(y, SIGN[d]), x, c))

    def kv_y1():
        kv_own().wait()
        for k in range(len(OTHERS)):
            kv_z_copy(k).wait()
        for d in BOTH:
            kv_y_copy(r.kvh.at[x, c, :, y], d, d).start()

    def kv_y2():
        for d in BOTH:
            yy = turn(y, -SIGN[d])
            kv_y_copy(r.kvh.at[x, c, :, yy], d, d).wait_recv()
            kv_y_copy(r.kvh.at[x, c, :, yy, pl.ds(2 * d, 2)], 2, d).start()

    def kv_y3():
        kv_y_copy(r.kvh.at[x, c, :, turn(y, 2)], 2, 0).wait_recv()
        kv_y_copy(r.kvh.at[x, c, :, pl.ds(0, LAST)], 0, 0).wait_send()

    def kv_x_copy(l, ref, k, d):
        return remote(ref, ref, r.kx_send.at[l], r.kx_recv.at[l, k], (z, y, turn(x, SIGN[d]), c))

    def kv_die(l, ref):
        return remote(ref, ref, r.kd_send.at[l], r.kd_recv.at[l], partner)

    def kv_x1(l):
        ref = r.kvh.at[x, c, l]
        for d in BOTH:
            kv_x_copy(l, ref, d, d).start()
        kv_die(l, ref).start()

    def kv_x2(l):
        for d in BOTH:
            xx = turn(x, -SIGN[d])
            ref = r.kvh.at[xx, c, l]
            kv_x_copy(l, ref, d, d).wait_recv()
            kv_x_copy(l, r.kvh.at[xx, c, l, pl.ds(2 * d, 2)], 2, d).start()
            kv_die(l, ref).start()

    def kv_x3(l):
        ref = r.kvh.at[turn(x, 2), c, l]
        kv_x_copy(l, ref, 2, 0).wait_recv()
        kv_die(l, ref).start()

    def kv_load(l):
        kv_die(l, r.kvh.at[:, 1 - c, l]).wait_recv()
        kc = r.wkv.shape[1]
        for xx in RINGS:
            for cc in BOTH:
                pltpu.make_async_copy(r.kvh.at[xx, cc, l], r.kvb.at[:, :, pl.ds((xx * CORES + cc) * kc, kc)], r.k_loc.at[1]).start()

    def kv_sent(l):
        kv_x_copy(l, r.kvh.at[pl.ds(0, LAST), c, l], 0, 0).wait_send()
        kv_die(l, r.kvh.at[:, c, l]).wait_send()

    def kv_loaded():
        pltpu.make_async_copy(r.kvb, r.kvb, r.k_loc.at[1]).wait()

    def gain_move(i, src, dst, dev):
        return remote(src, dst, r.g_send.at[i], r.g_recv.at[i], dev)

    def gain_z(k):
        dev = (turn(z, OTHERS[k]), y, x, c)
        return gain_move(k, r.gbuf.at[x, c, y, z], r.gbuf.at[x, c, y, z], dev)

    def gain_y(k):
        dev = (z, turn(y, OTHERS[k]), x, c)
        return gain_move(len(OTHERS) + k, r.gbuf.at[x, c, y], r.gbuf.at[x, c, y], dev)

    def gain_x(k):
        dev = (z, y, turn(x, OTHERS[k]), c)
        return gain_move(CORES * len(OTHERS) + k, r.gbuf.at[x, c], r.gbuf.at[x, c], dev)

    def gain_die(xx, k):
        ref = r.gbuf.at[xx, c]
        return remote(ref, ref, r.gd_send.at[k], r.gd_recv.at[k], partner)

    def gain_sum():
        for zz in RINGS:
            for yy in RINGS:
                tot = jnp.zeros((n_layers, d_row), F32)
                for xx in RINGS:
                    for cc in BOTH:
                        tot += r.gbuf[xx, cc, yy, zz, :n_layers].astype(F32)
                at = (zz * RING + yy) * d_row
                r.gain[:, at:at + d_row] = tot

    tok_pair = CORES * rows

    def x_z(k):
        zz = turn(z, OTHERS[k])
        src = r.xt.at[pl.ds(zz * seqs, seqs)]
        return remote(src, r.xz.at[z], r.xz_send.at[k], r.xz_recv.at[k], (zz, y, x, c))

    def x_own():
        return pltpu.make_async_copy(r.xt.at[pl.ds(z * seqs, seqs)], r.xz.at[z], r.x_loc)

    def pos(xx):
        return pl.ds(pl.multiple_of(xx * tok_pair, tok_pair), tok_pair)

    def x_plane(oy, ox):
        yy, xx = turn(y, oy), turn(x, ox)
        return remote(r.xz.at[:, yy, :, pos(xx)], r.xp.at[c, y, x], r.xp_send.at[oy], r.xp_recv.at[(RING - oy) % RING], (z, yy, xx, c))

    def row_bytes(oy):
        return r.xp.at[c, 0] if oy else r.xp.at[c, 0, pl.ds(0, RING - 1)]

    def x_row(oy):
        yy = turn(y, oy)
        got = row_bytes(oy)
        remote(got, got, r.xp_send.at[oy], r.xp_recv.at[oy], partner).wait_recv()
        row = r.xp.at[c, yy]
        remote(row, row, r.xd_send.at[oy], r.xd_recv.at[oy], partner).start()

    def x_turn():
        for oy in RINGS:
            row = r.xp.at[1 - c, turn(y, oy)]
            remote(row, row, r.xd_send.at[oy], r.xd_recv.at[oy], partner).wait_recv()

        @pl.loop(0, RING)
        def _(zz):
            for yy in RINGS:
                for xh in BOTH:
                    blk = [r.xp[cc, yy, CORES * xh + xx, zz] for xx in BOTH for cc in BOTH]
                    blk = jnp.concatenate(blk, axis=0).astype(F32).T.astype(BF)
                    n = blk.shape[1]
                    at = pl.multiple_of(zz * RING * d_row + yy * d_row + xh * n, n)
                    r.hb[0, 0, :, :, pl.ds(at, n)] = blk.reshape(CORES, rows, n)
        r.hid[...] = r.hb[0, 0, c]
        for oy in RINGS:
            row = r.xp.at[c, turn(y, oy)]
            remote(row, row, r.xd_send.at[oy], r.xd_recv.at[oy], partner).wait_send()

    def x_sent():
        for fn in (x_z, gain_z, gain_y, gain_x):
            peers_of(fn, "wait_send")
        for k in RINGS:
            gain_die(x, k).wait_send()
        for oy in RINGS:
            got = row_bytes(oy)
            remote(got, got, r.xp_send.at[oy], r.xp_recv.at[oy], partner).wait_send()

    def y_die(p):
        cols = pl.ds(pl.multiple_of(turn(z, p) * width, width), width)
        return remote(r.hid.at[:, cols], r.hb.at[0, 0, c, :, cols], r.yd_send.at[p], r.yd_recv.at[p], partner)

    def planes(h):
        return pl.ds(2 * h, 2)

    def y_plane(h, oy, ox):
        yy, xx = turn(y, oy), turn(x, ox)
        return remote(r.xp.at[c, yy, xx, planes(h)], r.xz.at[planes(h), y, :, pos(x)], r.yp_send.at[h, oy], r.yp_recv.at[h, (RING - oy) % RING],
                      (z, yy, xx, c))

    def y_z(p, oy):
        s = turn(y, oy)
        return remote(r.xz.at[p, s], r.y_out.at[z * seqs + s], r.yz_send.at[p, oy], r.yz_recv.at[p, oy], (turn(z, p), y, x, c))

    def y_own(oy):
        s = turn(y, oy)
        return pltpu.make_async_copy(r.xz.at[0, s], r.y_out.at[z * seqs + s], r.y_loc.at[oy])

    def leave_a(h):
        for p in BOTH:
            p = 2 * h + p
            y_die(p).start()
            cols = pl.ds(pl.multiple_of(turn(z, p) * width, width), width)
            r.hb[0, 0, c, :, cols] = r.hid[:, cols]

    def leave_b(h):
        n = CORES * CORES * d_local
        for p in BOTH:
            p = 2 * h + p
            y_die(p).wait()

            @pl.loop(0, RING)
            def _(yy, p=p):
                for xh in BOTH:
                    at = pl.multiple_of(turn(z, p) * width + yy * d_row + xh * n, n)
                    blk = r.hb[0, 0, :, :, pl.ds(at, n)].reshape(tok_pair, n).astype(F32).T.astype(BF)
                    for xx in BOTH:
                        for cc in BOTH:
                            lo = (xx * CORES + cc) * d_local
                            r.xp[cc, yy, CORES * xh + xx, p] = blk[lo:lo + d_local]

        for oy in OTHERS + (0,):
            for ox in RINGS:
                if oy or ox:
                    y_plane(h, oy, ox).start()
        for p in BOTH:
            p = 2 * h + p
            r.xz[p, y, :, pos(x)] = r.xp[c, y, x, p]

    def plane_bytes(h, oy):
        return r.xp.at[c, 0, :, planes(h)] if oy else r.xp.at[c, 0, pl.ds(0, LAST), planes(h)]

    def leave_c(h):
        for oy in OTHERS + (0,):
            got = plane_bytes(h, oy)
            remote(got, got, r.yp_send.at[h, oy], r.yp_recv.at[h, oy], partner).wait_recv()
            for p in BOTH:
                p = 2 * h + p
                (y_z(p, oy) if p else y_own(oy)).start()

    def left():
        for oy in RINGS:
            for h in BOTH:
                got = plane_bytes(h, oy)
                remote(got, got, r.yp_send.at[h, oy], r.yp_recv.at[h, oy], partner).wait_send()
            for p in RINGS:
                (y_z(p, oy) if p else y_own(oy)).wait()

    def kv_rows(zz):
        n = CORES * seq_len // (RING * RING * RING * CORES)
        return pl.ds(pl.multiple_of(((zz * RING + y) * RING + x) * n, n), n)

    def kv_trade(l, k):
        zz = turn(z, OTHERS[k])
        return remote(r.kv_out.at[l, :, :, kv_rows(zz)], r.kvx.at[l, z], r.kvx_send.at[l, k], r.kvx_recv.at[l, k], (zz, y, x, c))

    def kv_keep(l):
        return pltpu.make_async_copy(r.kv_out.at[l, :, :, kv_rows(z)], r.kvx.at[l, z], r.kvx_loc.at[l])

    def kv_share(l):
        for k in range(len(OTHERS)):
            kv_trade(l, k).start()
        kv_keep(l).start()

    def kv_shared(l):
        for k in range(len(OTHERS)):
            kv_trade(l, k).wait()
        kv_keep(l).wait()

    def gather_norm(l, split, pump):
        hid = r.hid
        gain = r.gain[l:l + 1, :]
        for b in range(4):
            blk = hid[b * quarter:(b + 1) * quarter, :].astype(F32)
            mean = jnp.mean(blk, axis=-1, keepdims=True)
            cen = blk - mean
            var = jnp.mean(cen * cen, axis=-1, keepdims=True)
            r.h_ref[b * quarter:(b + 1) * quarter, :] = (cen * lax.rsqrt(var + LN_EPS) * gain).astype(BF)
        out = r.h_all.at[l]

        def spot(q, first, second):
            if q == 0:
                return turn(y, second), turn(x, first)
            return turn(y, first), turn(x, second)

        def span(q, part):
            lo, n = (split, rows - split) if q else (0, split)
            if part is NIL:
                return pl.ds(lo, n)
            return pl.ds(lo + part * (n // 2), n // 2)

        table = {}

        def link(key, *args, own=False):
            idx, (q, first, second, part, to_first, to_second) = table.setdefault(key, (len(table), args))
            sy, sx = spot(q, first, second)
            ty, tx = spot(q, to_first, to_second)
            rws = span(q, part)
            dst = out.at[sy, sx, c, rws]
            return remote(r.h_ref.at[rws] if own else dst, dst, r.ag_send.at[l, KINDS.index(key[0])], r.ag_recv.at[l, idx], (z, ty, tx, c))

        def arrived(*key):
            for d in BOTH:
                link((*key, d)).wait_recv()

        def die(q, first, second, own=False):
            sy, sx = spot(q, first, second)
            rws = span(q, NIL)
            dst = out.at[sy, sx, c, rws]
            off = (first if q else second) % RING
            remote(r.h_ref.at[rws] if own else dst, dst, r.ag_dsend.at[l], r.ag_drecv.at[l, off], partner).start()

        offs = (0, -1, 1, 2)

        def second_step(k):
            for d in BOTH:
                for q in BOTH:
                    link(("second", q, k, d)).wait_recv()
                    src = -SIGN[d]
                    link(("second_on", q, k, d), q, offs[k], src, d, 0, SIGN[d]).start()
                    die(q, offs[k], src)

        def last_step(q, k):
            arrived("second_on", q, k)
            die(q, offs[k], 2)

        def tail_a():
            for k in RINGS[1:]:
                second_step(k)
                hook(pump, f"k{k}")
            for k in (1, 2):
                last_step(1, k)

        def tail_b():
            for k in RINGS:
                last_step(0, k)
            last_step(1, LAST)

        for q in BOTH:
            for d in BOTH:
                link(("first", q, d), q, 0, 0, NIL, SIGN[d], 0, own=True).start()
        for q in BOTH:
            for d in BOTH:
                link(("second", q, 0, d), q, 0, 0, NIL, 0, SIGN[d], own=True).start()
        for q in BOTH:
            die(q, 0, 0, own=True)
        own = pltpu.make_async_copy(r.h_ref, out.at[y, x, c], r.ag_loc)
        own.start()
        hook(pump, "begin")
        for d in BOTH:
            for q in BOTH:
                link(("first", q, d)).wait_recv()
                src = -SIGN[d]
                link(("first_on", q, d), q, src, 0, d, SIGN[d], 0).start()
                for e in BOTH:
                    link(("second", q, 1 + d, e), q, src, 0, NIL, 0, SIGN[e]).start()
                die(q, src, 0)
        hook(pump, "first")
        second_step(0)
        hook(pump, "k0")
        for q in BOTH:
            arrived("first_on", q)
            for e in BOTH:
                link(("second", q, LAST, e), q, 2, 0, NIL, 0, SIGN[e]).start()
            die(q, 2, 0)
        hook(pump, "first_on")
        last_step(1, 0)
        own.wait()
        hook(pump, "ready")

        def crossed(off):
            got = out.at[turn(y, off), :, 1 - c]
            remote(got, got, r.ag_dsend.at[l], r.ag_drecv.at[l, off], partner).wait_recv()

        def order(i):
            return lax.rem(3 * i + 3 * (i // 2) + 2 * (i // 3), RING)

        crossed(0)
        h_copy(l, y, 0).start()

        @pl.loop(0, RING)
        def _(i):
            slot = lax.rem(i, 2)
            s = turn(y, order(i))
            h_copy(l, s, slot).wait()
            pump(("seq", i))
            one(l, s, slot, i)

            @pl.when(i == 0)
            def _():
                tail_a()

            @pl.when(i == 1)
            def _():
                tail_b()

            @pl.when(i < LAST)
            def _():
                crossed(order(i + 1))
                h_copy(l, turn(y, order(i + 1)), 1 - slot).start()

        for slot in BOTH:
            for i in BOTH:
                kv_out_copy(l, 0, slot, i).wait()
        sent = (out.at[y, x], out.at[y], out.at[y, x, c], out.at[y, pl.ds(0, CORES)])
        for kind, ref in enumerate(sent):
            remote(ref, ref, r.ag_send.at[l, kind], r.ag_recv.at[l, kind], partner).wait_send()
        remote(out.at[pl.ds(0, 2)], out.at[pl.ds(0, 2)], r.ag_dsend.at[l], r.ag_drecv.at[l, 0], partner).wait_send()

    def h_copy(l, s, slot):
        return pltpu.make_async_copy(r.h_all.at[l, s], r.hb.at[slot], r.h_sem.at[slot])

    def h_tile(slot):
        return r.hb[slot].reshape(seq_len, d_model)

    def project(h, lo, n):
        w = r.wv[:, :, lo:lo + n].reshape(d_model, n)
        return jnp.dot(h, w, preferred_element_type=F32).astype(BF)

    def rope(val):
        val = val.astype(F32)
        return val * r.cos[...] + pltpu.roll(val, head_dim // 2, 1) * r.sin[...]

    n_chunk = min(256, f_loc)

    def kv_out_copy(l, s, slot, i):
        return pltpu.make_async_copy(r.qkv.at[slot, i], r.kv_out.at[l, i, s], r.kvo_sem.at[slot, i])

    def one(l, s, slot, i):
        @pl.when(i >= 2)
        def _():
            for k in BOTH:
                kv_out_copy(l, s, slot, k).wait()

        kv = jnp.zeros((seq_len, 2 * head_dim), F32)
        for zz in RINGS:
            for yy in RINGS:
                col = (zz * RING + yy) * d_row
                kv += lax.dot_general(h_cols(slot, col, d_row), r.kvb[yy, zz], (((1,), (1,)), ((), ())), preferred_element_type=F32)
        kv = kv.astype(BF)
        r.qkv[slot, 0] = rope(kv[:, :head_dim]).astype(BF)
        r.qkv[slot, 1] = kv[:, head_dim:]
        for i in BOTH:
            kv_out_copy(l, s, slot, i).start()
        q = project(h_tile(slot), 0, head_dim)
        r.stage[...] = (rope(q) * head_dim ** -0.5).astype(BF)
        for lo in range(0, f_loc, n_chunk):
            r.joined[s, :, head_dim + lo:head_dim + lo + n_chunk] = project(h_tile(slot), head_dim + lo, n_chunk)
        n_tile = seq_len // 2
        for i in BOTH:
            keys = (i + 1) * n_tile
            sc = lax.dot_general(r.stage[i * n_tile:(i + 1) * n_tile, :], r.qkv[slot, 0, :keys, :], (((1,), (1,)), ((), ())), preferred_element_type=F32)
            row_id = lax.broadcasted_iota(jnp.int32, sc.shape, 0) + i * n_tile
            col_id = lax.broadcasted_iota(jnp.int32, sc.shape, 1)
            sc = jnp.where(col_id <= row_id, sc, -1e30)
            top = jnp.max(sc, axis=-1, keepdims=True)
            ex = jnp.exp(sc - top)
            prob = (ex * (1.0 / jnp.sum(ex, axis=-1, keepdims=True))).astype(BF)
            att = jnp.dot(prob, r.qkv[slot, 1, :keys, :], preferred_element_type=F32)
            r.joined[s, i * n_tile:(i + 1) * n_tile, :head_dim] = att.astype(BF)

    def h_cols(slot, col, n):
        return r.hb[slot, :, :, :, col:col + n].reshape(seq_len, n)

    def two(s, slot):
        for lo in range(0, f_loc, n_chunk):
            up = project(h_tile(slot), head_dim + f_loc + lo, n_chunk).astype(F32)
            cols = slice(head_dim + lo, head_dim + lo + n_chunk)
            g = r.joined[s, :, cols].astype(F32)
            r.joined[s, :, cols] = (g * jax.nn.sigmoid(g) * up).astype(BF)

    def pass_two(l, pump):
        h_copy(l, 0, 0).start()

        @pl.loop(0, RING)
        def _(s):
            slot = lax.rem(s, 2)
            h_copy(l, s, slot).wait()

            @pl.when(s + 1 < RING)
            def _():
                h_copy(l, s + 1, 1 - slot).start()

            pump(("two", s))
            two(s, slot)

    def out_scatter(l, pump):
        def peer(q, first, second):
            dy = first * (1 - q) + second * q
            dx = first * q + second * (1 - q)
            return (z, turn(y, dy), turn(x, dx), c)

        def die_copy(ch, q, s):
            return remote(r.away.at[q], r.die_in.at[ch, q, s], r.dsend.at[l, ch, q, s], r.drecv.at[l, ch, q, s], partner)

        def first_copy(ch, q, d):
            return remote(r.acc.at[ch, q, 0, pl.ds(CORES * d, CORES)], r.in1.at[ch, q, d], r.send1.at[l, ch, q, d], r.recv1.at[l, ch, q, d],
                          peer(q, SIGN[d], 0))

        def second_copy(ch, q, d, h):
            js = pl.ds(CORES * h, CORES)
            return remote(r.acc.at[ch, q, 1 + d, js], r.in2.at[ch, q, d, js], r.send2.at[l, ch, q, d, h], r.recv2.at[l, ch, q, d, h],
                          peer(q, SIGN[d], 0))

        def half_rows(d):
            return pl.ds(d * (rows // 2), rows // 2)

        def third_copy(ch, q, d):
            return remote(r.acc.at[ch, q, LAST, 0, half_rows(d)], r.in3.at[ch, q, d], r.send3.at[l, ch, q, d], r.recv3.at[l, ch, q, d],
                          peer(q, 0, SIGN[d]))

        def fourth_copy(ch, q, d):
            return remote(r.acc.at[ch, q, LAST, 1 + d], r.in4.at[ch, q, d], r.send4.at[l, ch, q, d], r.recv4.at[l, ch, q, d],
                          peer(q, 0, SIGN[d]))

        n_blk = r.wov.shape[3]

        def plane_of(ch, q):
            return turn(z, LAST - q if ch else q)

        def tile(ch, q, s):
            for cc in BOTH:
                for j in RINGS:
                    oy = SLOT_OFF[s] * (1 - q) + SLOT_OFF[j] * q
                    ox = SLOT_OFF[j] * (1 - q) + SLOT_OFF[s] * q
                    core = c if cc else 1 - c
                    at = pl.multiple_of((turn(x, ox) * CORES + core) * rows, rows)
                    r.lhs[pl.ds((cc * RING + j) * rows, rows), :] = r.joined[turn(y, oy), pl.ds(at, rows), :]
            left = r.lhs[...]
            zz = plane_of(ch, q)

            @pl.loop(0, RING)
            def _(n):
                col = pl.multiple_of(n * n_blk, n_blk)
                res = jnp.dot(left, r.wov[zz, n], preferred_element_type=F32).astype(BF)
                res = res.reshape(CORES, RING, rows, n_blk)
                r.away[q, :, :, pl.ds(col, n_blk)] = res[0]
                r.acc[ch, q, s, :, :, pl.ds(col, n_blk)] = res[1]

        def pair_sum(ch, q, s):
            die_copy(ch, q, s).wait_recv()

            @pl.loop(0, RING)
            def _(j):
                r.acc[ch, q, s, j] = r.acc[ch, q, s, j] + r.die_in[ch, q, s, j]

        def stage_a(ch):
            for s in RINGS:
                @pl.loop(0, CORES)
                def _(q, s=s):
                    if s:
                        die_copy(ch, q, s - 1).wait_send()
                    elif ch:
                        die_copy(ch - 1, q, LAST).wait_send()
                    tile(ch, q, s)
                    die_copy(ch, q, s).start()
                    if s:
                        pair_sum(ch, q, s - 1)
                    if s == 1:
                        for d in BOTH:
                            first_copy(ch, q, d).start()
                    if s > 1:
                        second_copy(ch, q, s - 2, LAST - s).start()
                if s == 1:
                    hook(pump, f"mid{ch}")

        def stage_b(ch):
            for q in BOTH:
                pair_sum(ch, q, LAST)
            for q in BOTH:
                for d in BOTH:
                    first_copy(ch, q, d).wait_recv()
                    for j in BOTH:
                        at = CORES * d + j
                        r.acc[ch, q, 1 + d, at] = r.acc[ch, q, 1 + d, at] + r.in1[ch, q, d, j]
                    second_copy(ch, q, d, d).start()

        def total(ch, q, j):
            val = r.acc[ch, q, LAST, j].astype(F32)
            for d in BOTH:
                val += r.in2[ch, q, d, j].astype(F32)
            r.acc[ch, q, LAST, j] = val.astype(BF)

        def stage_c(ch):
            for q in BOTH:
                for h in BOTH:
                    for d in BOTH:
                        second_copy(ch, q, d, h).wait_recv()
                total(ch, q, 0)
                for d in BOTH:
                    third_copy(ch, q, d).start()
                for j in RINGS[1:]:
                    total(ch, q, j)

        def stage_d(ch):
            for q in BOTH:
                for d in BOTH:
                    third_copy(ch, q, d).wait_recv()
                    rws = half_rows(d)
                    r.acc[ch, q, LAST, 1 + d, rws] = r.acc[ch, q, LAST, 1 + d, rws] + r.in3[ch, q, d]
                    fourth_copy(ch, q, d).start()

        def stage_e(ch):
            for q in BOTH:
                for d in BOTH:
                    fourth_copy(ch, q, d).wait_recv()
                cols = pl.ds(pl.multiple_of(plane_of(ch, q) * width, width), width)
                upd = r.acc[ch, q, LAST, LAST].astype(F32)
                for d in BOTH:
                    upd += r.in4[ch, q, d].astype(F32)
                upd = upd.astype(BF)
                r.hid[:, cols] = (r.hid[:, cols].astype(F32) + upd.astype(F32)).astype(BF)

        def sent(ch):
            for q in BOTH:
                if ch:
                    die_copy(ch, q, LAST).wait_send()
                for d in BOTH:
                    for cp in (first_copy, third_copy, fourth_copy):
                        cp(ch, q, d).wait_send()
                    for h in BOTH:
                        second_copy(ch, q, d, h).wait_send()

        for step, fn, ch in (
            ("a0", stage_a, 0), ("b0", stage_b, 0), ("a1", stage_a, 1), ("c0", stage_c, 0), ("b1", stage_b, 1),
            ("d0", stage_d, 0), ("e0", stage_e, 0), ("c1", stage_c, 1), ("d1", stage_d, 1), ("e1", stage_e, 1),
        ):
            with jax.named_scope(step):
                fn(ch)
            hook(pump, step)
        for ch in BOTH:
            sent(ch)

    def near(fn, t):
        for j in (LAST, 1):
            fn(t, j)

    def far(fn, t):
        fn(t, 2)

    def z_all(t):
        near(z_direct, t)
        far(z_direct, t)

    def peers_of(fn, op="start"):
        for k in range(len(OTHERS)):
            getattr(fn(k), op)()

    def start():
        peers_of(gain_z)
        kv_z()
        peers_of(x_z)
        x_own().start()
        z_own(QG0)
        with jax.named_scope("gain_a"):
            peers_of(gain_z, "wait_recv")
            peers_of(gain_y)
        with jax.named_scope("kv_a"):
            kv_y1()
        y_send(QG0)
        with jax.named_scope("gain_b"):
            peers_of(gain_y, "wait_recv")
            peers_of(gain_x)
            gain_die(x, LAST).start()
        with jax.named_scope("x_z"):
            peers_of(x_z, "wait_recv")
            x_own().wait()
        for oy in RINGS:
            for ox in RINGS:
                if oy or ox:
                    x_plane(oy, ox).start()
        r.xp[c, y, x] = r.xz[:, y, :, pos(x)]
        with jax.named_scope("kv_b"):
            kv_y2()
        with jax.named_scope("gain_c"):
            for k, o in enumerate(OTHERS):
                gain_x(k).wait_recv()
                gain_die(turn(x, -o), k).start()
        with jax.named_scope("own_on"):
            z_forward(QG0, 0)
        with jax.named_scope("rows"):
            for oy in (0, LAST, 1, 2):
                x_row(oy)
        with jax.named_scope("near_direct"):
            near(z_direct, QG0)
        with jax.named_scope("relay"):
            y_relay(QG0)
        with jax.named_scope("kv_c"):
            kv_y3()
            kv_x1(0)
        with jax.named_scope("gain_sum"):
            for k in RINGS:
                gain_die(x, k).wait_recv()
            gain_sum()
        with jax.named_scope("turn"):
            x_turn()

    def when(i, n, *fns):
        @pl.when(i == n)
        def _():
            for fn in fns:
                fn()

    def plan(steps):
        def pump(step):
            for fn, *args in steps.get(step, ()):
                with jax.named_scope(f"{fn.__name__}_{args[-1] if args else 0}"):
                    fn(*args)

        def front(step):
            if isinstance(step, str):
                pump(step)
                return
            for n in RINGS:
                if (step[0], n) in steps:
                    when(step[1], n, lambda n=n: pump((step[0], n)))
        return front

    def both_loaded(t):
        loaded(t)
        kv_loaded()

    first_front = plan({
        "begin": [(kv_x2, 0), (far, z_direct, QG0)],
        "first": [(near, z_forward, QG0)],
        "k0": [(kv_x3, 0), (far, z_forward, QG0), (y_send, UP0)],
        "first_on": [(z_own, UP0)],
        "ready": [(finish, QG0), (kv_load, 0), (both_loaded, QG0)],
        "k1": [(near, z_direct, UP0), (y_relay, UP0)],
        "k2": [(z_forward, UP0, 0), (y_send, WO0)],
        "k3": [(far, z_direct, UP0)],
        ("seq", 1): [(near, z_forward, UP0), (z_own, WO0), (x_sent,)],
        ("seq", 2): [(far, z_forward, UP0), (near, z_direct, WO0), (y_relay, WO0)],
        ("seq", LAST): [(far, z_direct, WO0), (z_forward, WO0, 0), (y_send, QG1)],
    })
    first_two = plan({
        ("two", 0): [(near, z_forward, WO0), (kv_x1, 1)],
        ("two", 1): [(z_own, QG1), (y_relay, QG1)],
        ("two", 2): [(far, z_forward, WO0), (near, z_direct, QG1), (kv_x2, 1)],
        ("two", LAST): [(y_send, UP1)],
    })
    first_scatter = plan({
        "mid0": [(far, z_direct, QG1)],
        "b0": [(load_far, WO0), (far_loaded, WO0), (z_forward, QG1, 0)],
        "a1": [(near, z_forward, QG1), (y_relay, UP1), (z_own, UP1)],
        "c0": [(far, z_forward, QG1), (near, z_direct, UP1)],
        "b1": [(far, z_direct, UP1), (kv_x3, 1)],
        "e0": [(z_forward, UP1, 0), (kv_load, 1)],
        "c1": [(near, z_forward, UP1), (y_send, WO1)],
        "d1": [(far, z_forward, UP1)],
    })
    second_front = plan({
        "begin": [(z_own, WO1)],
        "first": [(y_relay, WO1), (near, z_direct, WO1)],
        "first_on": [(finish, QG1), (far, z_direct, WO1)],
        "ready": [(both_loaded, QG1)],
        "k1": [(z_forward, WO1, 0)],
        ("seq", 1): [(near, z_forward, WO1)],
        ("seq", 2): [(far, z_forward, WO1)],
    })
    second_two = plan({})
    second_scatter = plan({
        "b0": [(load_far, WO1), (far_loaded, WO1)],
        "e0": [(leave_a, 0)],
        "c1": [(leave_b, 0)],
        "d1": [(leave_c, 0)],
    })

    with jax.named_scope("start"):
        start()
    with jax.named_scope("front_0"):
        gather_norm(0, rows // RING, first_front)
    with jax.named_scope("finish_0"):
        kv_share(0)
        finish(UP0)
        loaded(UP0)
    with jax.named_scope("two_0"):
        pass_two(0, first_two)
    with jax.named_scope("near_0"):
        load_near(WO0)
        near_loaded(WO0)
    with jax.named_scope("scatter_0"):
        out_scatter(0, first_scatter)
    with jax.named_scope("front_1"):
        gather_norm(1, rows // 2, second_front)
    with jax.named_scope("finish_1"):
        kv_share(1)
        finish(UP1)
        loaded(UP1)
    with jax.named_scope("two_1"):
        pass_two(1, second_two)
    with jax.named_scope("near_1"):
        load_near(WO1)
        near_loaded(WO1)
    with jax.named_scope("scatter_1"):
        out_scatter(1, second_scatter)
    with jax.named_scope("leave"):
        leave_a(1)
        leave_b(1)
        leave_c(1)
        left()
    with jax.named_scope("drain"):
        for t in range(WO1 + 1):
            drain(t)
        for l in range(n_layers):
            kv_shared(l)
            kv_sent(l)


def run_model(xt, gain, wkv_t, w_in, w_out, cos_full, sin_full):
    batch, d_local, seq_len = xt.shape
    n_layers, d_row, e_block = w_in.shape
    r_block, d_col = w_out.shape[1:]
    head_dim = cos_full.shape[1]
    d_model = d_row * RING * RING
    seqs = batch // RING
    rows = seqs * seq_len // (RING * RING * CORES)
    e_loc, r_loc = e_block // RING, r_block // RING
    kc = wkv_t.shape[1]
    width = d_model // RING
    n_t = 3 * n_layers
    n_o = len(OTHERS)

    def dma(*shape):
        return pltpu.SemaphoreType.DMA(shape)

    def vm(*shape):
        return pltpu.VMEM(shape, BF)

    def out(*shape):
        return jax.ShapeDtypeStruct(shape, BF)

    any_spec = pl.BlockSpec(memory_space=pl.ANY)
    vm_spec = pl.BlockSpec(memory_space=pltpu.VMEM)
    out_shape = [
        out(batch, d_local, seq_len),
        out(n_layers, 2, seqs, seq_len, head_dim),
        out(n_layers, RING, RING, CORES, rows, d_model),
        out(n_layers, RING, RING * d_row, e_loc),
        out(n_layers, RING, RING, r_loc, d_col),
        out(RING, CORES, n_layers, RING, RING, kc, d_row),
        out(n_layers, RING, 2, seqs, CORES * (seq_len // (CORES * RING * RING * RING)), head_dim),
        out(n_layers, 2, d_row // 2, e_loc),
        out(n_layers, 2, r_loc // 2, d_col),
    ]
    pair = (2, 2, 2)
    each = (n_layers, *pair)
    scratch = [
        vm(rows, d_model), vm(rows, d_model), pltpu.VMEM((n_layers, d_model), F32),
        vm(RING, CORES, RING, RING, G_ROWS, d_row),
        vm(RING, seqs, d_local, seq_len),
        vm(CORES, RING, RING, RING, d_local, CORES * rows),
        vm(RING, RING * d_row, e_loc), vm(RING, RING, 2 * head_dim, d_row), vm(RING, RING, r_loc, d_col),
        vm(2, RING, CORES, rows, d_model), vm(RING, seq_len, r_loc), vm(2, 2, seq_len, head_dim), vm(seq_len, head_dim),
        vm(CORES * RING * rows, r_loc), vm(2, RING, rows, width), vm(2, 2, RING, RING, rows, width), vm(2, 2, RING, RING, rows, width),
        vm(*pair, 2, rows, width), vm(*pair, RING, rows, width), vm(*pair, rows // 2, width), vm(*pair, rows, width),
        dma(n_o), dma(n_o), dma(RING), dma(RING), dma(RING), dma(RING), pltpu.SemaphoreType.DMA,
        dma(3 * n_o), dma(3 * n_o), dma(RING), dma(RING),
        dma(RING), dma(RING), dma(2, RING), dma(2, RING), dma(RING, RING), dma(RING, RING), dma(RING),
        dma(n_layers, RING), dma(n_layers, 40), dma(n_layers), dma(n_layers, RING), pltpu.SemaphoreType.DMA, dma(2), dma(2, 2), dma(3), dma(3),
        dma(n_t, RING), dma(n_t, 2), dma(n_t, RING, 2), dma(n_t, RING, 2), dma(n_t, RING),
        dma(n_o), dma(n_o), pltpu.SemaphoreType.DMA, dma(n_o), dma(n_layers), dma(n_layers, n_o), dma(n_layers), dma(n_layers), dma(2),
        dma(n_layers, 2, 2, RING), dma(n_layers, 2, 2, RING),
        dma(*each), dma(*each), dma(*each, 2), dma(*each, 2), dma(*each), dma(*each), dma(*each), dma(*each),
        dma(n_layers, n_o), dma(n_layers, n_o), dma(n_layers),
    ]
    res = pl.pallas_call(
        model_kernel,
        out_shape=out_shape,
        in_specs=[any_spec, vm_spec, vm_spec, any_spec, any_spec, vm_spec, vm_spec],
        out_specs=[any_spec] * len(out_shape),
        scratch_shapes=scratch,
        compiler_params=pltpu.CompilerParams(collective_id=0, has_side_effects=True, vmem_limit_bytes=VMEM_LIMIT),
        name="two_layers",
    )(xt, gain, wkv_t, w_in, w_out, cos_full, sin_full)
    return res[0], res[6]


def solution(mesh):
    row_size = mesh.shape["row"]
    n_col = mesh.shape["col"]
    n_z = row_size // RING
    n_y = RING
    n_x = n_col // CORES
    n_tp = n_y * n_col
    n_dev = row_size * n_col
    mesh4 = Mesh(mesh.devices.reshape(n_z, n_y, n_x, CORES), ("z", "y", "x", "core"))
    every = ("z", "y", "x", "core")
    col = ("x", "core")
    act_spec = P(NIL, NIL, every)
    w_spec = P(NIL, ("z", "y"), col)

    def device_fn(x_loc, gain_loc, w_in_loc, w_kv_loc, w_out_loc):
        n_layers = w_in_loc.shape[0]
        n_batch, seq_len, d_local = x_loc.shape
        head_dim = w_kv_loc.shape[2] * n_col // 2
        batch_loc = n_batch // n_z
        seq_local = seq_len // n_dev
        steps = np.arange(head_dim // 2, dtype=np.float32)
        inv_freq = (1.0 / 10000.0 ** (steps * 2 / head_dim)).astype(np.float32)
        angles = np.arange(seq_len, dtype=np.float32)[:, NIL] * inv_freq[NIL, :]
        cos_tab, sin_tab = np.cos(angles), np.sin(angles)
        cos_full = jnp.asarray(np.concatenate([cos_tab, cos_tab], axis=1))
        sin_full = jnp.asarray(np.concatenate([-sin_tab, sin_tab], axis=1))
        y_loc, kv = run_model(x_loc.transpose(0, 2, 1), gain_loc, w_kv_loc.transpose(0, 2, 1), w_in_loc, w_out_loc, cos_full, sin_full)
        y_loc = y_loc.transpose(0, 2, 1)
        kv = kv.reshape(n_layers, n_z, 2, batch_loc, CORES, seq_local, head_dim)
        kv = lax.dynamic_index_in_dim(kv, lax.axis_index("core"), axis=4, keepdims=False)
        kv = kv.transpose(0, 2, 1, 3, 4, 5).reshape(n_layers, 2, n_batch, seq_local, head_dim)
        return y_loc, kv

    return jax.shard_map(device_fn, mesh=mesh4, in_specs=(act_spec, P(NIL, every), w_spec, w_spec, P(NIL, col, ("z", "y"))), out_specs=(act_spec, P(NIL, NIL, NIL, every, NIL)), check_vma=False)
```

```python
import jax
import jax.numpy as jnp
import numpy as np
from jax import lax
from jax.experimental import pallas as pl
from jax.experimental.pallas import tpu as pltpu
from jax.sharding import Mesh
from jax.sharding import PartitionSpec as P

LN_EPS = 1e-6
RING = 4
CORES = 2
VMEM_LIMIT = 67_000_000
BF = jnp.bfloat16
F32 = jnp.float32
SLOT_OFF = (2, 1, 3, 0)
SIGN = (1, -1)
NIL = None
BOTH = range(CORES)
RINGS = range(RING)
OTHERS = (1, 3, 2)
LAST = RING - 1
G_ROWS = 8
QG0, UP0, WO0, QG1, UP1, WO1 = range(6)
KINDS = ("first", "second", "first_on", "second_on")
NAMES = (
    "xt", "gain_in", "wkv", "w_in", "w_out", "cos", "sin", "y_out", "kv_out", "h_all", "wi", "wo", "kvh", "kvx", "rwi", "rwo", "h_ref",
    "hid", "gain", "gbuf", "xz", "xp",
    "wv", "kvb", "wov", "hb", "joined", "qkv", "stage", "lhs", "away", "acc", "die_in", "in1", "in2", "in3", "in4",
    "xz_send", "xz_recv", "xp_send", "xp_recv", "xd_send", "xd_recv", "x_loc", "g_send", "g_recv", "gd_send", "gd_recv", "yd_send", "yd_recv", "yp_send", "yp_recv", "yz_send", "yz_recv", "y_loc",
    "ag_send", "ag_recv", "ag_dsend", "ag_drecv", "ag_loc", "h_sem", "kvo_sem", "w_load", "far_load", "y_recv", "ry_recv", "zb_recv",
    "zc_recv", "w_send", "kz_send", "kz_recv", "ky_send", "ky_recv", "kx_send", "kx_recv", "kd_send", "kd_recv",
    "k_loc", "dsend", "drecv", "send1", "recv1", "send2", "recv2", "send3", "recv3", "send4", "recv4", "kvx_send", "kvx_recv", "kvx_loc",
)


class Refs:
    def __init__(self, refs):
        for name, ref in zip(NAMES, refs, strict=True):
            setattr(self, name, ref)


def model_kernel(*refs):
    r = Refs(refs)
    z, y, x, c = (lax.axis_index(a) for a in ("z", "y", "x", "core"))
    n_layers = r.wkv.shape[0]
    rows, d_model = r.hid.shape
    batch, d_local = r.xt.shape[:2]
    seqs = batch // RING
    seq_len, head_dim = r.cos.shape
    d_row = r.w_in.shape[1]
    e_loc = r.wi.shape[3]
    depth = r.wo.shape[3]
    f_loc = depth - head_dim
    quarter = rows // 4
    width = d_model // RING
    q_block = head_dim * RING
    f_block = f_loc * RING

    def turn(base, off):
        return lax.rem(base + off + RING, RING)

    def remote(src, dst, ssem, rsem, dev):
        return pltpu.make_async_remote_copy(
            src_ref=src, dst_ref=dst, send_sem=ssem, recv_sem=rsem, device_id=dev, device_id_type=pl.DeviceIdType.MESH)

    partner = (z, y, x, 1 - c)

    peers = [(turn(z, o), y, x, c) for o in OTHERS]
    peers += [(z, turn(y, oy), turn(x, ox), c) for oy in RINGS for ox in RINGS if oy or ox]
    peers.append(partner)
    here = (z, y, x, c)
    gate_sem = pltpu.get_barrier_semaphore()
    for dev in peers:
        pl.semaphore_signal(gate_sem, inc=1, device_id=dev, device_id_type=pl.DeviceIdType.MESH)
    src_id = lax.broadcasted_iota(jnp.int32, (d_local, d_row), 0) + (x * CORES + c) * d_local
    dst_id = lax.broadcasted_iota(jnp.int32, (d_local, d_row), 1)
    spread = jnp.where(src_id == dst_id, 1.0, 0.0).astype(BF)
    r.gbuf[x, c, y, z] = jnp.zeros((G_ROWS, d_row), BF)
    r.gbuf[x, c, y, z, :n_layers] = jnp.dot(r.gain_in[...], spread, preferred_element_type=F32).astype(BF)
    pl.semaphore_wait(gate_sem, len(peers))

    def hook(pump, i):
        with jax.named_scope(f"hook_{i}"):
            pump(i)

    def w_cols(kind):
        return pl.ds(0, head_dim + f_loc) if kind == 0 else pl.ds(head_dim + f_loc, f_loc)

    def piece(t, zz, yy):
        l, kind = t // 3, t % 3
        if kind == 2:
            return r.wo.at[l, zz, yy]
        return r.wi.at[l, zz, pl.ds(pl.multiple_of(yy * d_row, d_row), d_row), w_cols(kind)]

    def piece_half(t, zz, yy, h):
        l, kind = t // 3, t % 3
        if kind == 2:
            return r.wo.at[l, zz, yy, pl.ds(h * (depth // 2), depth // 2)]
        return r.wi.at[l, zz, pl.ds(pl.multiple_of(yy * d_row + h * (d_row // 2), d_row // 2), d_row // 2), w_cols(kind)]

    def own_parts(t, owner, zz, yy):
        l, kind = t // 3, t % 3
        hq = pl.ds(pl.multiple_of(owner * head_dim, head_dim), head_dim)
        if kind == 2:
            return [
                (r.w_out.at[l, hq], r.wo.at[l, zz, yy, pl.ds(0, head_dim)]),
                (r.w_out.at[l, pl.ds(pl.multiple_of(q_block + owner * f_loc, head_dim), f_loc)], r.wo.at[l, zz, yy, pl.ds(head_dim, f_loc)]),
            ]
        rws = pl.ds(pl.multiple_of(yy * d_row, d_row), d_row)
        if kind == 0:
            return [
                (r.w_in.at[l, :, hq], r.wi.at[l, zz, rws, pl.ds(0, head_dim)]),
                (r.w_in.at[l, :, pl.ds(pl.multiple_of(q_block + owner * f_loc, head_dim), f_loc)], r.wi.at[l, zz, rws, pl.ds(head_dim, f_loc)]),
            ]
        return [(r.w_in.at[l, :, pl.ds(pl.multiple_of(q_block + f_block + owner * f_loc, head_dim), f_loc)],
                 r.wi.at[l, zz, rws, pl.ds(head_dim + f_loc, f_loc)])]

    def relay_ref(t, d):
        l, kind = t // 3, t % 3
        return r.rwo.at[l, d] if kind == 2 else r.rwi.at[l, d, :, w_cols(kind)]

    def far_parts(t, d):
        l, kind = t // 3, t % 3
        owner = turn(y, 2)
        hq = pl.ds(pl.multiple_of(owner * head_dim, head_dim), head_dim)
        if kind == 2:
            n = depth // 2
            base = q_block + owner * f_loc
            if d:
                return [(r.w_out.at[l, pl.ds(pl.multiple_of(base + n - head_dim, G_ROWS), n)], r.rwo.at[l, d])]
            return [
                (r.w_out.at[l, hq], r.rwo.at[l, d, pl.ds(0, head_dim)]),
                (r.w_out.at[l, pl.ds(pl.multiple_of(base, head_dim), n - head_dim)], r.rwo.at[l, d, pl.ds(head_dim, n - head_dim)]),
            ]
        rws = pl.ds(d * (d_row // 2), d_row // 2)
        if kind == 0:
            return [
                (r.w_in.at[l, rws, hq], r.rwi.at[l, d, :, pl.ds(0, head_dim)]),
                (r.w_in.at[l, rws, pl.ds(pl.multiple_of(q_block + owner * f_loc, head_dim), f_loc)], r.rwi.at[l, d, :, pl.ds(head_dim, f_loc)]),
            ]
        return [(r.w_in.at[l, rws, pl.ds(pl.multiple_of(q_block + f_block + owner * f_loc, head_dim), f_loc)], relay_ref(t, d))]

    def y_send(t):
        for d in BOTH:
            owner = turn(y, SIGN[d])
            dev = (z, owner, x, c)
            for src, dst in far_parts(t, d):
                remote(src, dst, r.w_send.at[t, 0], r.ry_recv.at[t, d], dev).start()
            for src, dst in own_parts(t, owner, z, y):
                remote(src, dst, r.w_send.at[t, 0], r.y_recv.at[t, -SIGN[d] % RING], dev).start()

    def y_relay(t):
        for d in BOTH:
            ref = relay_ref(t, d)
            remote(ref, ref, r.w_send.at[t, 3], r.ry_recv.at[t, d], here).wait_recv()
            dst = piece_half(t, z, turn(y, -SIGN[d]), d)
            remote(ref, dst, r.w_send.at[t, 3], r.y_recv.at[t, 2], (z, turn(y, SIGN[d]), x, c)).start()

    def z_own(t):
        for d in BOTH:
            for src, dst in own_parts(t, y, z, y):
                remote(src, dst, r.w_send.at[t, 1], r.zb_recv.at[t, 0, d], (turn(z, SIGN[d]), y, x, c)).start()

    def z_direct(t, j):
        yy = turn(y, j)
        ref = piece(t, z, yy)
        remote(ref, ref, r.w_send.at[t, 0], r.y_recv.at[t, j], here).wait_recv()
        for d in BOTH:
            remote(ref, ref, r.w_send.at[t, 1], r.zb_recv.at[t, j, d], (turn(z, SIGN[d]), y, x, c)).start()

    def z_forward(t, j):
        yy = turn(y, j)
        for d in BOTH:
            zz = turn(z, -SIGN[d])
            ref = piece(t, zz, yy)
            remote(ref, ref, r.w_send.at[t, 1], r.zb_recv.at[t, j, d], here).wait_recv()
            part = piece_half(t, zz, yy, d)
            remote(part, part, r.w_send.at[t, 2], r.zc_recv.at[t, j, d], (turn(z, SIGN[d]), y, x, c)).start()

    def place(t, zz):
        l, kind = t // 3, t % 3
        if kind == 2:
            return r.wo.at[l, zz], r.wov.at[zz]
        return r.wi.at[l, zz, :, w_cols(kind)], r.wv.at[zz, :, w_cols(kind)]

    def load_near(t):
        kind = t % 3
        for d in BOTH:
            src, dst = place(t, turn(z, SIGN[d]))
            pltpu.make_async_copy(src, dst, r.w_load.at[kind]).start()
        for j in OTHERS:
            yy = turn(y, j)
            dst = r.wov.at[z, yy] if kind == 2 else r.wv.at[z, pl.ds(pl.multiple_of(yy * d_row, d_row), d_row), w_cols(kind)]
            pltpu.make_async_copy(piece(t, z, yy), dst, r.w_load.at[kind]).start()
        for src, dst in own_parts(t, y, z, y):
            pltpu.make_async_copy(src, own_place(t, dst, src), r.w_load.at[kind]).start()

    def load_far(t):
        far = turn(z, 2)
        for j in RINGS:
            for d in BOTH:
                part = piece_half(t, far, turn(y, j), d)
                remote(part, part, r.w_send.at[t, 2], r.zc_recv.at[t, j, d], here).wait_recv()
        src, dst = place(t, far)
        pltpu.make_async_copy(src, dst, r.far_load.at[t % 3]).start()

    def own_place(t, dst, src):
        kind = t % 3
        if kind == 2:
            n = src.shape[0]
            return r.wov.at[z, y, pl.ds(0 if n == head_dim and f_loc != head_dim else head_dim, n)]
        n = src.shape[1]
        rws = pl.ds(pl.multiple_of(y * d_row, d_row), d_row)
        if kind == 0:
            return r.wv.at[z, rws, pl.ds(0 if n == head_dim and f_loc != head_dim else head_dim, n)]
        return r.wv.at[z, rws, pl.ds(head_dim + f_loc, f_loc)]

    def finish(t):
        load_near(t)
        load_far(t)

    def near_loaded(t):
        kind = t % 3
        dst = r.wov.at[pl.ds(0, LAST)] if kind == 2 else r.wv.at[pl.ds(0, LAST), :, w_cols(kind)]
        pltpu.make_async_copy(dst, dst, r.w_load.at[kind]).wait()

    def far_loaded(t):
        kind = t % 3
        dst = r.wov.at[0] if kind == 2 else r.wv.at[0, :, w_cols(kind)]
        pltpu.make_async_copy(dst, dst, r.far_load.at[kind]).wait()

    def loaded(t):
        near_loaded(t)
        far_loaded(t)

    def drain(t):
        l, kind = t // 3, t % 3
        if kind == 2:
            done = (r.wo.at[l, 0, pl.ds(0, LAST)], r.wo.at[l, pl.ds(0, 2)], r.wo.at[l, 0], r.wo.at[l, 0, 0])
        else:
            cols = w_cols(kind)
            done = (r.wi.at[l, 0, pl.ds(0, LAST * d_row), cols], r.wi.at[l, pl.ds(0, 2), :, cols], r.wi.at[l, 0, :, cols],
                    r.wi.at[l, 0, pl.ds(0, d_row), cols])
        for g, ref in enumerate(done):
            remote(ref, ref, r.w_send.at[t, g], r.y_recv.at[t, 0], here).wait_send()

    def kv_z_copy(k):
        return remote(r.wkv, r.kvh.at[x, c, :, y, z], r.kz_send.at[k], r.kz_recv.at[k], (turn(z, OTHERS[k]), y, x, c))

    def kv_own():
        return pltpu.make_async_copy(r.wkv, r.kvh.at[x, c, :, y, z], r.k_loc.at[0])

    def kv_z():
        for k in range(len(OTHERS)):
            kv_z_copy(k).start()
        kv_own().start()

    def kv_y_copy(ref, k, d):
        return remote(ref, ref, r.ky_send, r.ky_recv.at[k], (z, turn(y, SIGN[d]), x, c))

    def kv_y1():
        kv_own().wait()
        for k in range(len(OTHERS)):
            kv_z_copy(k).wait()
        for d in BOTH:
            kv_y_copy(r.kvh.at[x, c, :, y], d, d).start()

    def kv_y2():
        for d in BOTH:
            yy = turn(y, -SIGN[d])
            kv_y_copy(r.kvh.at[x, c, :, yy], d, d).wait_recv()
            kv_y_copy(r.kvh.at[x, c, :, yy, pl.ds(2 * d, 2)], 2, d).start()

    def kv_y3():
        kv_y_copy(r.kvh.at[x, c, :, turn(y, 2)], 2, 0).wait_recv()
        kv_y_copy(r.kvh.at[x, c, :, pl.ds(0, LAST)], 0, 0).wait_send()

    def kv_x_copy(l, ref, k, d):
        return remote(ref, ref, r.kx_send.at[l], r.kx_recv.at[l, k], (z, y, turn(x, SIGN[d]), c))

    def kv_die(l, ref):
        return remote(ref, ref, r.kd_send.at[l], r.kd_recv.at[l], partner)

    def kv_x1(l):
        ref = r.kvh.at[x, c, l]
        for d in BOTH:
            kv_x_copy(l, ref, d, d).start()
        kv_die(l, ref).start()

    def kv_x2(l):
        for d in BOTH:
            xx = turn(x, -SIGN[d])
            ref = r.kvh.at[xx, c, l]
            kv_x_copy(l, ref, d, d).wait_recv()
            kv_x_copy(l, r.kvh.at[xx, c, l, pl.ds(2 * d, 2)], 2, d).start()
            kv_die(l, ref).start()

    def kv_x3(l):
        ref = r.kvh.at[turn(x, 2), c, l]
        kv_x_copy(l, ref, 2, 0).wait_recv()
        kv_die(l, ref).start()

    def kv_load(l):
        kv_die(l, r.kvh.at[:, 1 - c, l]).wait_recv()
        kc = r.wkv.shape[1]
        for xx in RINGS:
            for cc in BOTH:
                pltpu.make_async_copy(r.kvh.at[xx, cc, l], r.kvb.at[:, :, pl.ds((xx * CORES + cc) * kc, kc)], r.k_loc.at[1]).start()

    def kv_sent(l):
        kv_x_copy(l, r.kvh.at[pl.ds(0, LAST), c, l], 0, 0).wait_send()
        kv_die(l, r.kvh.at[:, c, l]).wait_send()

    def kv_loaded():
        pltpu.make_async_copy(r.kvb, r.kvb, r.k_loc.at[1]).wait()

    def gain_move(i, src, dst, dev):
        return remote(src, dst, r.g_send.at[i], r.g_recv.at[i], dev)

    def gain_z(k):
        dev = (turn(z, OTHERS[k]), y, x, c)
        return gain_move(k, r.gbuf.at[x, c, y, z], r.gbuf.at[x, c, y, z], dev)

    def gain_y(k):
        dev = (z, turn(y, OTHERS[k]), x, c)
        return gain_move(len(OTHERS) + k, r.gbuf.at[x, c, y], r.gbuf.at[x, c, y], dev)

    def gain_x(k):
        dev = (z, y, turn(x, OTHERS[k]), c)
        return gain_move(CORES * len(OTHERS) + k, r.gbuf.at[x, c], r.gbuf.at[x, c], dev)

    def gain_die(xx, k):
        ref = r.gbuf.at[xx, c]
        return remote(ref, ref, r.gd_send.at[k], r.gd_recv.at[k], partner)

    def gain_sum():
        for zz in RINGS:
            for yy in RINGS:
                tot = jnp.zeros((n_layers, d_row), F32)
                for xx in RINGS:
                    for cc in BOTH:
                        tot += r.gbuf[xx, cc, yy, zz, :n_layers].astype(F32)
                at = (zz * RING + yy) * d_row
                r.gain[:, at:at + d_row] = tot

    tok_pair = CORES * rows

    def x_z(k):
        zz = turn(z, OTHERS[k])
        src = r.xt.at[pl.ds(zz * seqs, seqs)]
        return remote(src, r.xz.at[z], r.xz_send.at[k], r.xz_recv.at[k], (zz, y, x, c))

    def x_own():
        return pltpu.make_async_copy(r.xt.at[pl.ds(z * seqs, seqs)], r.xz.at[z], r.x_loc)

    def pos(xx):
        return pl.ds(pl.multiple_of(xx * tok_pair, tok_pair), tok_pair)

    def x_plane(oy, ox):
        yy, xx = turn(y, oy), turn(x, ox)
        return remote(r.xz.at[:, yy, :, pos(xx)], r.xp.at[c, y, x], r.xp_send.at[oy], r.xp_recv.at[(RING - oy) % RING], (z, yy, xx, c))

    def row_bytes(oy):
        return r.xp.at[c, 0] if oy else r.xp.at[c, 0, pl.ds(0, RING - 1)]

    def x_row(oy):
        yy = turn(y, oy)
        got = row_bytes(oy)
        remote(got, got, r.xp_send.at[oy], r.xp_recv.at[oy], partner).wait_recv()
        row = r.xp.at[c, yy]
        remote(row, row, r.xd_send.at[oy], r.xd_recv.at[oy], partner).start()

    def x_turn():
        for oy in RINGS:
            row = r.xp.at[1 - c, turn(y, oy)]
            remote(row, row, r.xd_send.at[oy], r.xd_recv.at[oy], partner).wait_recv()

        @pl.loop(0, RING)
        def _(zz):
            for yy in RINGS:
                for xh in BOTH:
                    blk = [r.xp[cc, yy, CORES * xh + xx, zz] for xx in BOTH for cc in BOTH]
                    blk = jnp.concatenate(blk, axis=0).astype(F32).T.astype(BF)
                    n = blk.shape[1]
                    at = pl.multiple_of(zz * RING * d_row + yy * d_row + xh * n, n)
                    r.hb[0, 0, :, :, pl.ds(at, n)] = blk.reshape(CORES, rows, n)
        r.hid[...] = r.hb[0, 0, c]
        for oy in RINGS:
            row = r.xp.at[c, turn(y, oy)]
            remote(row, row, r.xd_send.at[oy], r.xd_recv.at[oy], partner).wait_send()

    def x_sent():
        for fn in (x_z, gain_z, gain_y, gain_x):
            peers_of(fn, "wait_send")
        for k in RINGS:
            gain_die(x, k).wait_send()
        for oy in RINGS:
            got = row_bytes(oy)
            remote(got, got, r.xp_send.at[oy], r.xp_recv.at[oy], partner).wait_send()

    def y_die(p):
        cols = pl.ds(pl.multiple_of(turn(z, p) * width, width), width)
        return remote(r.hid.at[:, cols], r.hb.at[0, 0, c, :, cols], r.yd_send.at[p], r.yd_recv.at[p], partner)

    def planes(h):
        return pl.ds(2 * h, 2)

    def y_plane(h, oy, ox):
        yy, xx = turn(y, oy), turn(x, ox)
        return remote(r.xp.at[c, yy, xx, planes(h)], r.xz.at[planes(h), y, :, pos(x)], r.yp_send.at[h, oy], r.yp_recv.at[h, (RING - oy) % RING],
                      (z, yy, xx, c))

    def y_z(p, oy):
        s = turn(y, oy)
        return remote(r.xz.at[p, s], r.y_out.at[z * seqs + s], r.yz_send.at[p, oy], r.yz_recv.at[p, oy], (turn(z, p), y, x, c))

    def y_own(oy):
        s = turn(y, oy)
        return pltpu.make_async_copy(r.xz.at[0, s], r.y_out.at[z * seqs + s], r.y_loc.at[oy])

    def leave_a(h):
        for p in BOTH:
            p = 2 * h + p
            y_die(p).start()
            cols = pl.ds(pl.multiple_of(turn(z, p) * width, width), width)
            r.hb[0, 0, c, :, cols] = r.hid[:, cols]

    def leave_b(h):
        n = CORES * CORES * d_local
        for p in BOTH:
            p = 2 * h + p
            y_die(p).wait()

            @pl.loop(0, RING)
            def _(yy, p=p):
                for xh in BOTH:
                    at = pl.multiple_of(turn(z, p) * width + yy * d_row + xh * n, n)
                    blk = r.hb[0, 0, :, :, pl.ds(at, n)].reshape(tok_pair, n).astype(F32).T.astype(BF)
                    for xx in BOTH:
                        for cc in BOTH:
                            lo = (xx * CORES + cc) * d_local
                            r.xp[cc, yy, CORES * xh + xx, p] = blk[lo:lo + d_local]

        for oy in OTHERS + (0,):
            for ox in RINGS:
                if oy or ox:
                    y_plane(h, oy, ox).start()
        for p in BOTH:
            p = 2 * h + p
            r.xz[p, y, :, pos(x)] = r.xp[c, y, x, p]

    def plane_bytes(h, oy):
        return r.xp.at[c, 0, :, planes(h)] if oy else r.xp.at[c, 0, pl.ds(0, LAST), planes(h)]

    def leave_c(h):
        for oy in OTHERS + (0,):
            got = plane_bytes(h, oy)
            remote(got, got, r.yp_send.at[h, oy], r.yp_recv.at[h, oy], partner).wait_recv()
            for p in BOTH:
                p = 2 * h + p
                (y_z(p, oy) if p else y_own(oy)).start()

    def left():
        for oy in RINGS:
            for h in BOTH:
                got = plane_bytes(h, oy)
                remote(got, got, r.yp_send.at[h, oy], r.yp_recv.at[h, oy], partner).wait_send()
            for p in RINGS:
                (y_z(p, oy) if p else y_own(oy)).wait()

    def kv_rows(zz):
        n = CORES * seq_len // (RING * RING * RING * CORES)
        return pl.ds(pl.multiple_of(((zz * RING + y) * RING + x) * n, n), n)

    def kv_trade(l, k):
        zz = turn(z, OTHERS[k])
        return remote(r.kv_out.at[l, :, :, kv_rows(zz)], r.kvx.at[l, z], r.kvx_send.at[l, k], r.kvx_recv.at[l, k], (zz, y, x, c))

    def kv_keep(l):
        return pltpu.make_async_copy(r.kv_out.at[l, :, :, kv_rows(z)], r.kvx.at[l, z], r.kvx_loc.at[l])

    def kv_share(l):
        for k in range(len(OTHERS)):
            kv_trade(l, k).start()
        kv_keep(l).start()

    def kv_shared(l):
        for k in range(len(OTHERS)):
            kv_trade(l, k).wait()
        kv_keep(l).wait()

    def gather_norm(l, split, pump):
        hid = r.hid
        gain = r.gain[l:l + 1, :]
        for b in range(4):
            blk = hid[b * quarter:(b + 1) * quarter, :].astype(F32)
            mean = jnp.mean(blk, axis=-1, keepdims=True)
            cen = blk - mean
            var = jnp.mean(cen * cen, axis=-1, keepdims=True)
            r.h_ref[b * quarter:(b + 1) * quarter, :] = (cen * lax.rsqrt(var + LN_EPS) * gain).astype(BF)
        out = r.h_all.at[l]

        def spot(q, first, second):
            if q == 0:
                return turn(y, second), turn(x, first)
            return turn(y, first), turn(x, second)

        def span(q, part):
            lo, n = (split, rows - split) if q else (0, split)
            if part is NIL:
                return pl.ds(lo, n)
            return pl.ds(lo + part * (n // 2), n // 2)

        table = {}

        def link(key, *args, own=False):
            idx, (q, first, second, part, to_first, to_second) = table.setdefault(key, (len(table), args))
            sy, sx = spot(q, first, second)
            ty, tx = spot(q, to_first, to_second)
            rws = span(q, part)
            dst = out.at[sy, sx, c, rws]
            return remote(r.h_ref.at[rws] if own else dst, dst, r.ag_send.at[l, KINDS.index(key[0])], r.ag_recv.at[l, idx], (z, ty, tx, c))

        def arrived(*key):
            for d in BOTH:
                link((*key, d)).wait_recv()

        def die(q, first, second, own=False):
            sy, sx = spot(q, first, second)
            rws = span(q, NIL)
            dst = out.at[sy, sx, c, rws]
            off = (first if q else second) % RING
            remote(r.h_ref.at[rws] if own else dst, dst, r.ag_dsend.at[l], r.ag_drecv.at[l, off], partner).start()

        offs = (0, -1, 1, 2)

        def second_step(k):
            for d in BOTH:
                for q in BOTH:
                    link(("second", q, k, d)).wait_recv()
                    src = -SIGN[d]
                    link(("second_on", q, k, d), q, offs[k], src, d, 0, SIGN[d]).start()
                    die(q, offs[k], src)

        def last_step(q, k):
            arrived("second_on", q, k)
            die(q, offs[k], 2)

        def tail_a():
            for k in RINGS[1:]:
                second_step(k)
                hook(pump, f"k{k}")
            for k in (1, 2):
                last_step(1, k)

        def tail_b():
            for k in RINGS:
                last_step(0, k)
            last_step(1, LAST)

        for q in BOTH:
            for d in BOTH:
                link(("first", q, d), q, 0, 0, NIL, SIGN[d], 0, own=True).start()
        for q in BOTH:
            for d in BOTH:
                link(("second", q, 0, d), q, 0, 0, NIL, 0, SIGN[d], own=True).start()
        for q in BOTH:
            die(q, 0, 0, own=True)
        own = pltpu.make_async_copy(r.h_ref, out.at[y, x, c], r.ag_loc)
        own.start()
        hook(pump, "begin")
        for d in BOTH:
            for q in BOTH:
                link(("first", q, d)).wait_recv()
                src = -SIGN[d]
                link(("first_on", q, d), q, src, 0, d, SIGN[d], 0).start()
                die(q, src, 0)
        hook(pump, "first")
        second_step(0)
        for q in reversed(BOTH):
            for d in BOTH:
                for e in BOTH:
                    link(("second", q, 1 + d, e), q, -SIGN[d], 0, NIL, 0, SIGN[e]).start()
        hook(pump, "k0")
        for q in BOTH:
            arrived("first_on", q)
            for e in BOTH:
                link(("second", q, LAST, e), q, 2, 0, NIL, 0, SIGN[e]).start()
            die(q, 2, 0)
        hook(pump, "first_on")
        last_step(1, 0)
        own.wait()
        hook(pump, "ready")

        def crossed(off):
            got = out.at[turn(y, off), :, 1 - c]
            remote(got, got, r.ag_dsend.at[l], r.ag_drecv.at[l, off], partner).wait_recv()

        def order(i):
            return lax.rem(3 * i + 3 * (i // 2) + 2 * (i // 3), RING)

        crossed(0)
        h_copy(l, y, 0).start()

        @pl.loop(0, RING)
        def _(i):
            slot = lax.rem(i, 2)
            s = turn(y, order(i))
            h_copy(l, s, slot).wait()
            pump(("seq", i))
            one(l, s, slot, i)

            @pl.when(i == 0)
            def _():
                tail_a()

            @pl.when(i == 1)
            def _():
                tail_b()

            @pl.when(i < LAST)
            def _():
                crossed(order(i + 1))
                h_copy(l, turn(y, order(i + 1)), 1 - slot).start()

        for slot in BOTH:
            for i in BOTH:
                kv_out_copy(l, 0, slot, i).wait()
        sent = (out.at[y, x], out.at[y], out.at[y, x, c], out.at[y, pl.ds(0, CORES)])
        for kind, ref in enumerate(sent):
            remote(ref, ref, r.ag_send.at[l, kind], r.ag_recv.at[l, kind], partner).wait_send()
        remote(out.at[pl.ds(0, 2)], out.at[pl.ds(0, 2)], r.ag_dsend.at[l], r.ag_drecv.at[l, 0], partner).wait_send()

    def h_copy(l, s, slot):
        return pltpu.make_async_copy(r.h_all.at[l, s], r.hb.at[slot], r.h_sem.at[slot])

    def h_tile(slot):
        return r.hb[slot].reshape(seq_len, d_model)

    def project(h, lo, n):
        w = r.wv[:, :, lo:lo + n].reshape(d_model, n)
        return jnp.dot(h, w, preferred_element_type=F32).astype(BF)

    def rope(val):
        val = val.astype(F32)
        return val * r.cos[...] + pltpu.roll(val, head_dim // 2, 1) * r.sin[...]

    n_chunk = min(256, f_loc)

    def kv_out_copy(l, s, slot, i):
        return pltpu.make_async_copy(r.qkv.at[slot, i], r.kv_out.at[l, i, s], r.kvo_sem.at[slot, i])

    def one(l, s, slot, i):
        @pl.when(i >= 2)
        def _():
            for k in BOTH:
                kv_out_copy(l, s, slot, k).wait()

        kv = jnp.zeros((seq_len, 2 * head_dim), F32)
        for zz in RINGS:
            for yy in RINGS:
                col = (zz * RING + yy) * d_row
                kv += lax.dot_general(h_cols(slot, col, d_row), r.kvb[yy, zz], (((1,), (1,)), ((), ())), preferred_element_type=F32)
        kv = kv.astype(BF)
        r.qkv[slot, 0] = rope(kv[:, :head_dim]).astype(BF)
        r.qkv[slot, 1] = kv[:, head_dim:]
        for i in BOTH:
            kv_out_copy(l, s, slot, i).start()
        q = project(h_tile(slot), 0, head_dim)
        r.stage[...] = (rope(q) * head_dim ** -0.5).astype(BF)
        for lo in range(0, f_loc, n_chunk):
            r.joined[s, :, head_dim + lo:head_dim + lo + n_chunk] = project(h_tile(slot), head_dim + lo, n_chunk)
        n_tile = seq_len // 2
        for i in BOTH:
            keys = (i + 1) * n_tile
            sc = lax.dot_general(r.stage[i * n_tile:(i + 1) * n_tile, :], r.qkv[slot, 0, :keys, :], (((1,), (1,)), ((), ())), preferred_element_type=F32)
            row_id = lax.broadcasted_iota(jnp.int32, sc.shape, 0) + i * n_tile
            col_id = lax.broadcasted_iota(jnp.int32, sc.shape, 1)
            sc = jnp.where(col_id <= row_id, sc, -1e30)
            top = jnp.max(sc, axis=-1, keepdims=True)
            ex = jnp.exp(sc - top)
            prob = (ex * (1.0 / jnp.sum(ex, axis=-1, keepdims=True))).astype(BF)
            att = jnp.dot(prob, r.qkv[slot, 1, :keys, :], preferred_element_type=F32)
            r.joined[s, i * n_tile:(i + 1) * n_tile, :head_dim] = att.astype(BF)

    def h_cols(slot, col, n):
        return r.hb[slot, :, :, :, col:col + n].reshape(seq_len, n)

    def two(s, slot):
        for lo in range(0, f_loc, n_chunk):
            up = project(h_tile(slot), head_dim + f_loc + lo, n_chunk).astype(F32)
            cols = slice(head_dim + lo, head_dim + lo + n_chunk)
            g = r.joined[s, :, cols].astype(F32)
            r.joined[s, :, cols] = (g * jax.nn.sigmoid(g) * up).astype(BF)

    def pass_two(l, pump):
        h_copy(l, 0, 0).start()

        @pl.loop(0, RING)
        def _(s):
            slot = lax.rem(s, 2)
            h_copy(l, s, slot).wait()

            @pl.when(s + 1 < RING)
            def _():
                h_copy(l, s + 1, 1 - slot).start()

            pump(("two", s))
            two(s, slot)

    def out_scatter(l, pump):
        def peer(q, first, second):
            dy = first * (1 - q) + second * q
            dx = first * q + second * (1 - q)
            return (z, turn(y, dy), turn(x, dx), c)

        def die_copy(ch, q, s):
            return remote(r.away.at[q], r.die_in.at[ch, q, s], r.dsend.at[l, ch, q, s], r.drecv.at[l, ch, q, s], partner)

        def first_copy(ch, q, d):
            return remote(r.acc.at[ch, q, 0, pl.ds(CORES * d, CORES)], r.in1.at[ch, q, d], r.send1.at[l, ch, q, d], r.recv1.at[l, ch, q, d],
                          peer(q, SIGN[d], 0))

        def second_copy(ch, q, d, h):
            js = pl.ds(CORES * h, CORES)
            return remote(r.acc.at[ch, q, 1 + d, js], r.in2.at[ch, q, d, js], r.send2.at[l, ch, q, d, h], r.recv2.at[l, ch, q, d, h],
                          peer(q, SIGN[d], 0))

        def half_rows(d):
            return pl.ds(d * (rows // 2), rows // 2)

        def third_copy(ch, q, d):
            return remote(r.acc.at[ch, q, LAST, 0, half_rows(d)], r.in3.at[ch, q, d], r.send3.at[l, ch, q, d], r.recv3.at[l, ch, q, d],
                          peer(q, 0, SIGN[d]))

        def fourth_copy(ch, q, d):
            return remote(r.acc.at[ch, q, LAST, 1 + d], r.in4.at[ch, q, d], r.send4.at[l, ch, q, d], r.recv4.at[l, ch, q, d],
                          peer(q, 0, SIGN[d]))

        n_blk = r.wov.shape[3]

        def plane_of(ch, q):
            return turn(z, LAST - q if ch else q)

        def tile(ch, q, s):
            for cc in BOTH:
                for j in RINGS:
                    oy = SLOT_OFF[s] * (1 - q) + SLOT_OFF[j] * q
                    ox = SLOT_OFF[j] * (1 - q) + SLOT_OFF[s] * q
                    core = c if cc else 1 - c
                    at = pl.multiple_of((turn(x, ox) * CORES + core) * rows, rows)
                    r.lhs[pl.ds((cc * RING + j) * rows, rows), :] = r.joined[turn(y, oy), pl.ds(at, rows), :]
            left = r.lhs[...]
            zz = plane_of(ch, q)

            @pl.loop(0, RING)
            def _(n):
                col = pl.multiple_of(n * n_blk, n_blk)
                res = jnp.dot(left, r.wov[zz, n], preferred_element_type=F32).astype(BF)
                res = res.reshape(CORES, RING, rows, n_blk)
                r.away[q, :, :, pl.ds(col, n_blk)] = res[0]
                r.acc[ch, q, s, :, :, pl.ds(col, n_blk)] = res[1]

        def pair_sum(ch, q, s):
            die_copy(ch, q, s).wait_recv()

            @pl.loop(0, RING)
            def _(j):
                r.acc[ch, q, s, j] = r.acc[ch, q, s, j] + r.die_in[ch, q, s, j]

        def stage_a(ch):
            for s in RINGS:
                @pl.loop(0, CORES)
                def _(q, s=s):
                    if s:
                        die_copy(ch, q, s - 1).wait_send()
                    elif ch:
                        die_copy(ch - 1, q, LAST).wait_send()
                    tile(ch, q, s)
                    die_copy(ch, q, s).start()
                    if s:
                        pair_sum(ch, q, s - 1)
                    if s == 1:
                        for d in BOTH:
                            first_copy(ch, q, d).start()
                    if s > 1:
                        second_copy(ch, q, s - 2, LAST - s).start()
                if s == 1:
                    hook(pump, f"mid{ch}")

        def stage_b(ch):
            for q in BOTH:
                pair_sum(ch, q, LAST)
            for q in BOTH:
                for d in BOTH:
                    first_copy(ch, q, d).wait_recv()
                    for j in BOTH:
                        at = CORES * d + j
                        r.acc[ch, q, 1 + d, at] = r.acc[ch, q, 1 + d, at] + r.in1[ch, q, d, j]
                    second_copy(ch, q, d, d).start()

        def total(ch, q, j):
            val = r.acc[ch, q, LAST, j].astype(F32)
            for d in BOTH:
                val += r.in2[ch, q, d, j].astype(F32)
            r.acc[ch, q, LAST, j] = val.astype(BF)

        def stage_c(ch):
            for q in BOTH:
                for h in BOTH:
                    for d in BOTH:
                        second_copy(ch, q, d, h).wait_recv()
                total(ch, q, 0)
                for d in BOTH:
                    third_copy(ch, q, d).start()
                for j in RINGS[1:]:
                    total(ch, q, j)

        def stage_d(ch):
            for q in BOTH:
                for d in BOTH:
                    third_copy(ch, q, d).wait_recv()
                    rws = half_rows(d)
                    r.acc[ch, q, LAST, 1 + d, rws] = r.acc[ch, q, LAST, 1 + d, rws] + r.in3[ch, q, d]
                    fourth_copy(ch, q, d).start()

        def stage_e(ch):
            for q in BOTH:
                for d in BOTH:
                    fourth_copy(ch, q, d).wait_recv()
                cols = pl.ds(pl.multiple_of(plane_of(ch, q) * width, width), width)
                upd = r.acc[ch, q, LAST, LAST].astype(F32)
                for d in BOTH:
                    upd += r.in4[ch, q, d].astype(F32)
                upd = upd.astype(BF)
                r.hid[:, cols] = (r.hid[:, cols].astype(F32) + upd.astype(F32)).astype(BF)

        def sent(ch):
            for q in BOTH:
                if ch:
                    die_copy(ch, q, LAST).wait_send()
                for d in BOTH:
                    for cp in (first_copy, third_copy, fourth_copy):
                        cp(ch, q, d).wait_send()
                    for h in BOTH:
                        second_copy(ch, q, d, h).wait_send()

        for step, fn, ch in (
            ("a0", stage_a, 0), ("b0", stage_b, 0), ("a1", stage_a, 1), ("b1", stage_b, 1), ("c0", stage_c, 0), ("c1", stage_c, 1),
            ("d0", stage_d, 0), ("d1", stage_d, 1), ("e0", stage_e, 0), ("e1", stage_e, 1),
        ):
            with jax.named_scope(step):
                fn(ch)
            hook(pump, step)
        for ch in BOTH:
            sent(ch)

    def near(fn, t):
        for j in (LAST, 1):
            fn(t, j)

    def far(fn, t):
        fn(t, 2)

    def z_all(t):
        near(z_direct, t)
        far(z_direct, t)

    def peers_of(fn, op="start"):
        for k in range(len(OTHERS)):
            getattr(fn(k), op)()

    def start():
        peers_of(gain_z)
        kv_z()
        peers_of(x_z)
        x_own().start()
        z_own(QG0)
        z_own(UP0)
        with jax.named_scope("gain_a"):
            peers_of(gain_z, "wait_recv")
            peers_of(gain_y)
        with jax.named_scope("kv_a"):
            kv_y1()
        y_send(QG0)
        with jax.named_scope("gain_b"):
            peers_of(gain_y, "wait_recv")
            peers_of(gain_x)
            gain_die(x, LAST).start()
        with jax.named_scope("x_z"):
            peers_of(x_z, "wait_recv")
            x_own().wait()
        for oy in RINGS:
            for ox in RINGS:
                if oy or ox:
                    x_plane(oy, ox).start()
        r.xp[c, y, x] = r.xz[:, y, :, pos(x)]
        with jax.named_scope("kv_b"):
            kv_y2()
        with jax.named_scope("gain_c"):
            for k, o in enumerate(OTHERS):
                gain_x(k).wait_recv()
                gain_die(turn(x, -o), k).start()
        with jax.named_scope("rows"):
            for oy in (0, LAST, 1, 2):
                x_row(oy)
        with jax.named_scope("relay"):
            y_relay(QG0)
            z_forward(QG0, 0)
            near(z_direct, QG0)
            z_forward(UP0, 0)
        with jax.named_scope("kv_c"):
            kv_y3()
            kv_x1(0)
        with jax.named_scope("gain_sum"):
            for k in RINGS:
                gain_die(x, k).wait_recv()
            gain_sum()
        with jax.named_scope("turn"):
            x_turn()

    def when(i, n, *fns):
        @pl.when(i == n)
        def _():
            for fn in fns:
                fn()

    def plan(steps):
        def pump(step):
            for fn, *args in steps.get(step, ()):
                with jax.named_scope(f"{fn.__name__}_{args[-1] if args else 0}"):
                    fn(*args)

        def front(step):
            if isinstance(step, str):
                pump(step)
                return
            for n in RINGS:
                if (step[0], n) in steps:
                    when(step[1], n, lambda n=n: pump((step[0], n)))
        return front

    def both_loaded(t):
        loaded(t)
        kv_loaded()

    first_front = plan({
        "begin": [(z_direct, QG0, 2), (y_send, UP0)],
        "first": [(kv_x2, 0), (z_forward, QG0, LAST)],
        "k0": [(z_forward, QG0, 1)],
        "first_on": [(kv_x3, 0), (z_forward, QG0, 2), (y_relay, UP0), (z_direct, UP0, LAST), (z_direct, UP0, 1), (y_send, WO0)],
        "ready": [(load_near, QG0), (load_far, QG0), (kv_load, 0), (loaded, QG0), (kv_loaded,)],
        ("seq", 0): [(y_send, UP1)],
        "k1": [(z_forward, UP0, LAST), (z_direct, UP0, 2), (y_relay, WO0)],
        "k3": [(z_forward, UP0, 1), (z_own, WO0)],
        ("seq", 1): [(z_forward, UP0, 2), (z_direct, WO0, LAST), (z_direct, WO0, 1), (y_relay, UP1), (x_sent,)],
        ("seq", 3): [(z_forward, WO0, 1), (kv_x1, 1)],
    })
    first_two = plan({
        ("two", 0): [(z_own, QG1)],
        ("two", 1): [(z_forward, WO0, LAST), (y_relay, QG1)],
        ("two", 2): [(z_forward, WO0, 2), (y_relay, WO1)],
        ("two", 3): [(kv_x2, 1)],
    })
    first_scatter = plan({
        "mid0": [(z_forward, QG1, 0), (kv_x3, 1), (z_direct, QG1, 1)],
        "a0": [(z_direct, QG1, 2)],
        "b0": [(load_far, WO0), (far_loaded, WO0)],
        "mid1": [(z_forward, QG1, LAST)],
        "a1": [(z_direct, UP1, LAST), (z_direct, UP1, 1)],
        "b1": [(z_forward, QG1, 1)],
        "c1": [(z_forward, QG1, 2), (z_direct, UP1, 2), (z_own, UP1)],
        "d1": [(z_forward, UP1, LAST)],
        "e1": [(z_forward, UP1, 1)],
    })
    second_front = plan({
        "begin": [(kv_load, 1)],
        "first": [(z_direct, WO1, LAST)],
        "k0": [(z_forward, UP1, 2)],
        "first_on": [(z_forward, UP1, 0)],
        "ready": [(z_direct, WO1, 1), (load_near, QG1), (load_far, QG1), (loaded, QG1), (kv_loaded,)],
        "k1": [(z_direct, WO1, 2), (z_forward, WO1, LAST)],
        "k2": [(z_own, WO1)],
        ("seq", 1): [(z_forward, WO1, 1)],
    })
    second_two = plan({
        ("two", 1): [(z_forward, WO1, 2)],
        ("two", 2): [(z_forward, WO1, 0)],
    })
    second_scatter = plan({
        "b0": [(load_far, WO1), (far_loaded, WO1)],
        "e0": [(leave_a, 0)],
    })

    with jax.named_scope("start"):
        start()
    with jax.named_scope("front_0"):
        gather_norm(0, rows // RING, first_front)
    with jax.named_scope("finish_0"):
        kv_share(0)
        z_direct(WO0, 2)
        z_forward(WO0, 0)
        y_send(QG1)
        y_send(WO1)
        finish(UP0)
        loaded(UP0)
    with jax.named_scope("two_0"):
        pass_two(0, first_two)
    with jax.named_scope("near_0"):
        z_direct(QG1, LAST)
        load_near(WO0)
        near_loaded(WO0)
    with jax.named_scope("scatter_0"):
        out_scatter(0, first_scatter)
    with jax.named_scope("front_1"):
        gather_norm(1, rows // 2, second_front)
    with jax.named_scope("finish_1"):
        kv_share(1)
        finish(UP1)
        loaded(UP1)
    with jax.named_scope("two_1"):
        pass_two(1, second_two)
    with jax.named_scope("near_1"):
        load_near(WO1)
        near_loaded(WO1)
    with jax.named_scope("scatter_1"):
        out_scatter(1, second_scatter)
    with jax.named_scope("leave"):
        leave_a(1)
        leave_b(1)
        leave_b(0)
        leave_c(1)
        leave_c(0)
        left()
    with jax.named_scope("drain"):
        for t in range(WO1 + 1):
            drain(t)
        for l in range(n_layers):
            kv_shared(l)
            kv_sent(l)


def run_model(xt, gain, wkv_t, w_in, w_out, cos_full, sin_full):
    batch, d_local, seq_len = xt.shape
    n_layers, d_row, e_block = w_in.shape
    r_block, d_col = w_out.shape[1:]
    head_dim = cos_full.shape[1]
    d_model = d_row * RING * RING
    seqs = batch // RING
    rows = seqs * seq_len // (RING * RING * CORES)
    e_loc, r_loc = e_block // RING, r_block // RING
    kc = wkv_t.shape[1]
    width = d_model // RING
    n_t = 3 * n_layers
    n_o = len(OTHERS)

    def dma(*shape):
        return pltpu.SemaphoreType.DMA(shape)

    def vm(*shape):
        return pltpu.VMEM(shape, BF)

    def out(*shape):
        return jax.ShapeDtypeStruct(shape, BF)

    any_spec = pl.BlockSpec(memory_space=pl.ANY)
    vm_spec = pl.BlockSpec(memory_space=pltpu.VMEM)
    out_shape = [
        out(batch, d_local, seq_len),
        out(n_layers, 2, seqs, seq_len, head_dim),
        out(n_layers, RING, RING, CORES, rows, d_model),
        out(n_layers, RING, RING * d_row, e_loc),
        out(n_layers, RING, RING, r_loc, d_col),
        out(RING, CORES, n_layers, RING, RING, kc, d_row),
        out(n_layers, RING, 2, seqs, CORES * (seq_len // (CORES * RING * RING * RING)), head_dim),
        out(n_layers, 2, d_row // 2, e_loc),
        out(n_layers, 2, r_loc // 2, d_col),
    ]
    pair = (2, 2, 2)
    each = (n_layers, *pair)
    scratch = [
        vm(rows, d_model), vm(rows, d_model), pltpu.VMEM((n_layers, d_model), F32),
        vm(RING, CORES, RING, RING, G_ROWS, d_row),
        vm(RING, seqs, d_local, seq_len),
        vm(CORES, RING, RING, RING, d_local, CORES * rows),
        vm(RING, RING * d_row, e_loc), vm(RING, RING, 2 * head_dim, d_row), vm(RING, RING, r_loc, d_col),
        vm(2, RING, CORES, rows, d_model), vm(RING, seq_len, r_loc), vm(2, 2, seq_len, head_dim), vm(seq_len, head_dim),
        vm(CORES * RING * rows, r_loc), vm(2, RING, rows, width), vm(2, 2, RING, RING, rows, width), vm(2, 2, RING, RING, rows, width),
        vm(*pair, 2, rows, width), vm(*pair, RING, rows, width), vm(*pair, rows // 2, width), vm(*pair, rows, width),
        dma(n_o), dma(n_o), dma(RING), dma(RING), dma(RING), dma(RING), pltpu.SemaphoreType.DMA,
        dma(3 * n_o), dma(3 * n_o), dma(RING), dma(RING),
        dma(RING), dma(RING), dma(2, RING), dma(2, RING), dma(RING, RING), dma(RING, RING), dma(RING),
        dma(n_layers, RING), dma(n_layers, 40), dma(n_layers), dma(n_layers, RING), pltpu.SemaphoreType.DMA, dma(2), dma(2, 2), dma(3), dma(3),
        dma(n_t, RING), dma(n_t, 2), dma(n_t, RING, 2), dma(n_t, RING, 2), dma(n_t, RING),
        dma(n_o), dma(n_o), pltpu.SemaphoreType.DMA, dma(n_o), dma(n_layers), dma(n_layers, n_o), dma(n_layers), dma(n_layers), dma(2),
        dma(n_layers, 2, 2, RING), dma(n_layers, 2, 2, RING),
        dma(*each), dma(*each), dma(*each, 2), dma(*each, 2), dma(*each), dma(*each), dma(*each), dma(*each),
        dma(n_layers, n_o), dma(n_layers, n_o), dma(n_layers),
    ]
    res = pl.pallas_call(
        model_kernel,
        out_shape=out_shape,
        in_specs=[any_spec, vm_spec, vm_spec, any_spec, any_spec, vm_spec, vm_spec],
        out_specs=[any_spec] * len(out_shape),
        scratch_shapes=scratch,
        compiler_params=pltpu.CompilerParams(collective_id=0, has_side_effects=True, vmem_limit_bytes=VMEM_LIMIT),
        name="two_layers",
    )(xt, gain, wkv_t, w_in, w_out, cos_full, sin_full)
    return res[0], res[6]


def solution(mesh):
    row_size = mesh.shape["row"]
    n_col = mesh.shape["col"]
    n_z = row_size // RING
    n_y = RING
    n_x = n_col // CORES
    n_tp = n_y * n_col
    n_dev = row_size * n_col
    mesh4 = Mesh(mesh.devices.reshape(n_z, n_y, n_x, CORES), ("z", "y", "x", "core"))
    every = ("z", "y", "x", "core")
    col = ("x", "core")
    act_spec = P(NIL, NIL, every)
    w_spec = P(NIL, ("z", "y"), col)

    def device_fn(x_loc, gain_loc, w_in_loc, w_kv_loc, w_out_loc):
        n_layers = w_in_loc.shape[0]
        n_batch, seq_len, d_local = x_loc.shape
        head_dim = w_kv_loc.shape[2] * n_col // 2
        batch_loc = n_batch // n_z
        seq_local = seq_len // n_dev
        steps = np.arange(head_dim // 2, dtype=np.float32)
        inv_freq = (1.0 / 10000.0 ** (steps * 2 / head_dim)).astype(np.float32)
        angles = np.arange(seq_len, dtype=np.float32)[:, NIL] * inv_freq[NIL, :]
        cos_tab, sin_tab = np.cos(angles), np.sin(angles)
        cos_full = jnp.asarray(np.concatenate([cos_tab, cos_tab], axis=1))
        sin_full = jnp.asarray(np.concatenate([-sin_tab, sin_tab], axis=1))
        y_loc, kv = run_model(x_loc.transpose(0, 2, 1), gain_loc, w_kv_loc.transpose(0, 2, 1), w_in_loc, w_out_loc, cos_full, sin_full)
        y_loc = y_loc.transpose(0, 2, 1)
        kv = kv.reshape(n_layers, n_z, 2, batch_loc, CORES, seq_local, head_dim)
        kv = lax.dynamic_index_in_dim(kv, lax.axis_index("core"), axis=4, keepdims=False)
        kv = kv.transpose(0, 2, 1, 3, 4, 5).reshape(n_layers, 2, n_batch, seq_local, head_dim)
        return y_loc, kv

    return jax.shard_map(device_fn, mesh=mesh4, in_specs=(act_spec, P(NIL, every), w_spec, w_spec, P(NIL, col, ("z", "y"))), out_specs=(act_spec, P(NIL, NIL, NIL, every, NIL)), check_vma=False)
```

```python
import jax
import jax.numpy as jnp
import numpy as np
from jax import lax
from jax.experimental import pallas as pl
from jax.experimental.pallas import tpu as pltpu
from jax.sharding import Mesh
from jax.sharding import PartitionSpec as P

LN_EPS = 1e-6
RING = 4
CORES = 2
VMEM_LIMIT = 67_000_000
BF = jnp.bfloat16
F32 = jnp.float32
SLOT_OFF = (2, 1, 3, 0)
SIGN = (1, -1)
NIL = None
BOTH = range(CORES)
RINGS = range(RING)
OTHERS = (1, 3, 2)
LAST = RING - 1
G_ROWS = 8
QG0, UP0, WO0, QG1, UP1, WO1 = range(6)
KINDS = ("first", "second", "first_on", "second_on")
NAMES = (
    "xt", "gain_in", "wkv", "w_in", "w_out", "cos", "sin", "y_out", "kv_out", "h_all", "wi", "wo", "kvh", "kvx", "rwi", "rwo", "h_ref",
    "hid", "gain", "gbuf", "xz", "xp",
    "wv", "kvb", "wov", "hb", "joined", "qkv", "stage", "lhs", "away", "acc", "die_in", "in1", "in2", "in3", "in4",
    "xz_send", "xz_recv", "xp_send", "xp_recv", "xd_send", "xd_recv", "x_loc", "g_send", "g_recv", "gd_send", "gd_recv", "yd_send", "yd_recv", "yp_send", "yp_recv", "yz_send", "yz_recv", "y_loc",
    "ag_send", "ag_recv", "ag_dsend", "ag_drecv", "ag_loc", "h_sem", "kvo_sem", "w_load", "far_load", "y_recv", "ry_recv", "zb_recv",
    "zc_recv", "w_send", "kz_send", "kz_recv", "ky_send", "ky_recv", "kx_send", "kx_recv", "kd_send", "kd_recv",
    "k_loc", "dsend", "drecv", "send1", "recv1", "send2", "recv2", "send3", "recv3", "send4", "recv4", "kvx_send", "kvx_recv", "kvx_loc",
)


class Refs:
    def __init__(self, refs):
        for name, ref in zip(NAMES, refs, strict=True):
            setattr(self, name, ref)


def model_kernel(*refs):
    r = Refs(refs)
    z, y, x, c = (lax.axis_index(a) for a in ("z", "y", "x", "core"))
    n_layers = r.wkv.shape[0]
    rows, d_model = r.hid.shape
    batch, d_local = r.xt.shape[:2]
    seqs = batch // RING
    seq_len, head_dim = r.cos.shape
    d_row = r.w_in.shape[1]
    e_loc = r.wi.shape[3]
    depth = r.wo.shape[3]
    f_loc = depth - head_dim
    quarter = rows // 4
    width = d_model // RING
    q_block = head_dim * RING
    f_block = f_loc * RING

    turned = {id(v): [lax.rem(v + o, RING) for o in RINGS] for v in (z, y, x)}

    def turn(base, off):
        if isinstance(off, int):
            return turned[id(base)][off % RING]
        return lax.rem(base + off + RING, RING)

    def remote(src, dst, ssem, rsem, dev):
        return pltpu.make_async_remote_copy(
            src_ref=src, dst_ref=dst, send_sem=ssem, recv_sem=rsem, device_id=dev, device_id_type=pl.DeviceIdType.MESH)

    partner = (z, y, x, 1 - c)

    peers = [(turn(z, o), y, x, c) for o in OTHERS]
    peers += [(z, turn(y, oy), turn(x, ox), c) for oy in RINGS for ox in RINGS if oy or ox]
    peers.append(partner)
    here = (z, y, x, c)
    gate_sem = pltpu.get_barrier_semaphore()
    for dev in peers:
        pl.semaphore_signal(gate_sem, inc=1, device_id=dev, device_id_type=pl.DeviceIdType.MESH)
    src_id = lax.broadcasted_iota(jnp.int32, (d_local, d_row), 0) + (x * CORES + c) * d_local
    dst_id = lax.broadcasted_iota(jnp.int32, (d_local, d_row), 1)
    spread = jnp.where(src_id == dst_id, 1.0, 0.0).astype(BF)
    r.gbuf[x, c, y, z] = jnp.zeros((G_ROWS, d_row), BF)
    r.gbuf[x, c, y, z, :n_layers] = jnp.dot(r.gain_in[...], spread, preferred_element_type=F32).astype(BF)
    pl.semaphore_wait(gate_sem, len(peers))

    def hook(pump, i):
        with jax.named_scope(f"hook_{i}"):
            pump(i)

    def w_cols(kind):
        return pl.ds(0, head_dim + f_loc) if kind == 0 else pl.ds(head_dim + f_loc, f_loc)

    def piece(t, zz, yy):
        l, kind = t // 3, t % 3
        if kind == 2:
            return r.wo.at[l, zz, yy]
        return r.wi.at[l, zz, pl.ds(pl.multiple_of(yy * d_row, d_row), d_row), w_cols(kind)]

    def piece_half(t, zz, yy, h):
        l, kind = t // 3, t % 3
        if kind == 2:
            return r.wo.at[l, zz, yy, pl.ds(h * (depth // 2), depth // 2)]
        return r.wi.at[l, zz, pl.ds(pl.multiple_of(yy * d_row + h * (d_row // 2), d_row // 2), d_row // 2), w_cols(kind)]

    def own_parts(t, owner, zz, yy):
        l, kind = t // 3, t % 3
        hq = pl.ds(pl.multiple_of(owner * head_dim, head_dim), head_dim)
        if kind == 2:
            return [
                (r.w_out.at[l, hq], r.wo.at[l, zz, yy, pl.ds(0, head_dim)]),
                (r.w_out.at[l, pl.ds(pl.multiple_of(q_block + owner * f_loc, head_dim), f_loc)], r.wo.at[l, zz, yy, pl.ds(head_dim, f_loc)]),
            ]
        rws = pl.ds(pl.multiple_of(yy * d_row, d_row), d_row)
        if kind == 0:
            return [
                (r.w_in.at[l, :, hq], r.wi.at[l, zz, rws, pl.ds(0, head_dim)]),
                (r.w_in.at[l, :, pl.ds(pl.multiple_of(q_block + owner * f_loc, head_dim), f_loc)], r.wi.at[l, zz, rws, pl.ds(head_dim, f_loc)]),
            ]
        return [(r.w_in.at[l, :, pl.ds(pl.multiple_of(q_block + f_block + owner * f_loc, head_dim), f_loc)],
                 r.wi.at[l, zz, rws, pl.ds(head_dim + f_loc, f_loc)])]

    def relay_ref(t, d):
        l, kind = t // 3, t % 3
        return r.rwo.at[l, d] if kind == 2 else r.rwi.at[l, d, :, w_cols(kind)]

    def far_parts(t, d):
        l, kind = t // 3, t % 3
        owner = turn(y, 2)
        hq = pl.ds(pl.multiple_of(owner * head_dim, head_dim), head_dim)
        if kind == 2:
            n = depth // 2
            base = q_block + owner * f_loc
            if d:
                return [(r.w_out.at[l, pl.ds(pl.multiple_of(base + n - head_dim, G_ROWS), n)], r.rwo.at[l, d])]
            return [
                (r.w_out.at[l, hq], r.rwo.at[l, d, pl.ds(0, head_dim)]),
                (r.w_out.at[l, pl.ds(pl.multiple_of(base, head_dim), n - head_dim)], r.rwo.at[l, d, pl.ds(head_dim, n - head_dim)]),
            ]
        rws = pl.ds(d * (d_row // 2), d_row // 2)
        if kind == 0:
            return [
                (r.w_in.at[l, rws, hq], r.rwi.at[l, d, :, pl.ds(0, head_dim)]),
                (r.w_in.at[l, rws, pl.ds(pl.multiple_of(q_block + owner * f_loc, head_dim), f_loc)], r.rwi.at[l, d, :, pl.ds(head_dim, f_loc)]),
            ]
        return [(r.w_in.at[l, rws, pl.ds(pl.multiple_of(q_block + f_block + owner * f_loc, head_dim), f_loc)], relay_ref(t, d))]

    def y_send(t):
        for d in BOTH:
            owner = turn(y, SIGN[d])
            dev = (z, owner, x, c)
            for src, dst in far_parts(t, d):
                remote(src, dst, r.w_send.at[t, 0], r.ry_recv.at[t, d], dev).start()
            for src, dst in own_parts(t, owner, z, y):
                remote(src, dst, r.w_send.at[t, 0], r.y_recv.at[t, -SIGN[d] % RING], dev).start()

    def y_relay(t):
        for d in BOTH:
            ref = relay_ref(t, d)
            remote(ref, ref, r.w_send.at[t, 3], r.ry_recv.at[t, d], here).wait_recv()
            dst = piece_half(t, z, turn(y, -SIGN[d]), d)
            remote(ref, dst, r.w_send.at[t, 3], r.y_recv.at[t, 2], (z, turn(y, SIGN[d]), x, c)).start()

    def z_own(t):
        for d in BOTH:
            for src, dst in own_parts(t, y, z, y):
                remote(src, dst, r.w_send.at[t, 1], r.zb_recv.at[t, 0, d], (turn(z, SIGN[d]), y, x, c)).start()

    def z_direct(t, j):
        yy = turn(y, j)
        ref = piece(t, z, yy)
        remote(ref, ref, r.w_send.at[t, 0], r.y_recv.at[t, j], here).wait_recv()
        for d in BOTH:
            remote(ref, ref, r.w_send.at[t, 1], r.zb_recv.at[t, j, d], (turn(z, SIGN[d]), y, x, c)).start()

    def z_forward(t, j):
        yy = turn(y, j)
        for d in BOTH:
            zz = turn(z, -SIGN[d])
            ref = piece(t, zz, yy)
            remote(ref, ref, r.w_send.at[t, 1], r.zb_recv.at[t, j, d], here).wait_recv()
            part = piece_half(t, zz, yy, d)
            remote(part, part, r.w_send.at[t, 2], r.zc_recv.at[t, j, d], (turn(z, SIGN[d]), y, x, c)).start()

    def place(t, zz):
        l, kind = t // 3, t % 3
        if kind == 2:
            return r.wo.at[l, zz], r.wov.at[zz]
        return r.wi.at[l, zz, :, w_cols(kind)], r.wv.at[zz, :, w_cols(kind)]

    def load_near(t):
        kind = t % 3
        for d in BOTH:
            src, dst = place(t, turn(z, SIGN[d]))
            pltpu.make_async_copy(src, dst, r.w_load.at[kind]).start()
        for j in OTHERS:
            yy = turn(y, j)
            dst = r.wov.at[z, yy] if kind == 2 else r.wv.at[z, pl.ds(pl.multiple_of(yy * d_row, d_row), d_row), w_cols(kind)]
            pltpu.make_async_copy(piece(t, z, yy), dst, r.w_load.at[kind]).start()
        for src, dst in own_parts(t, y, z, y):
            pltpu.make_async_copy(src, own_place(t, dst, src), r.w_load.at[kind]).start()

    def load_far(t):
        far = turn(z, 2)
        for j in RINGS:
            for d in BOTH:
                part = piece_half(t, far, turn(y, j), d)
                remote(part, part, r.w_send.at[t, 2], r.zc_recv.at[t, j, d], here).wait_recv()
        src, dst = place(t, far)
        pltpu.make_async_copy(src, dst, r.far_load.at[t % 3]).start()

    def own_place(t, dst, src):
        kind = t % 3
        if kind == 2:
            n = src.shape[0]
            return r.wov.at[z, y, pl.ds(0 if n == head_dim and f_loc != head_dim else head_dim, n)]
        n = src.shape[1]
        rws = pl.ds(pl.multiple_of(y * d_row, d_row), d_row)
        if kind == 0:
            return r.wv.at[z, rws, pl.ds(0 if n == head_dim and f_loc != head_dim else head_dim, n)]
        return r.wv.at[z, rws, pl.ds(head_dim + f_loc, f_loc)]

    def finish(t):
        load_near(t)
        load_far(t)

    def near_loaded(t):
        kind = t % 3
        dst = r.wov.at[pl.ds(0, LAST)] if kind == 2 else r.wv.at[pl.ds(0, LAST), :, w_cols(kind)]
        pltpu.make_async_copy(dst, dst, r.w_load.at[kind]).wait()

    def far_loaded(t):
        kind = t % 3
        dst = r.wov.at[0] if kind == 2 else r.wv.at[0, :, w_cols(kind)]
        pltpu.make_async_copy(dst, dst, r.far_load.at[kind]).wait()

    def loaded(t):
        near_loaded(t)
        far_loaded(t)

    def drain(t):
        l, kind = t // 3, t % 3
        if kind == 2:
            done = (r.wo.at[l, 0, pl.ds(0, LAST)], r.wo.at[l, pl.ds(0, 2)], r.wo.at[l, 0], r.wo.at[l, 0, 0])
        else:
            cols = w_cols(kind)
            done = (r.wi.at[l, 0, pl.ds(0, LAST * d_row), cols], r.wi.at[l, pl.ds(0, 2), :, cols], r.wi.at[l, 0, :, cols],
                    r.wi.at[l, 0, pl.ds(0, d_row), cols])
        for g, ref in enumerate(done):
            remote(ref, ref, r.w_send.at[t, g], r.y_recv.at[t, 0], here).wait_send()

    def kv_z_copy(k):
        return remote(r.wkv, r.kvh.at[x, c, :, y, z], r.kz_send.at[k], r.kz_recv.at[k], (turn(z, OTHERS[k]), y, x, c))

    def kv_own():
        return pltpu.make_async_copy(r.wkv, r.kvh.at[x, c, :, y, z], r.k_loc.at[0])

    def kv_z():
        for k in range(len(OTHERS)):
            kv_z_copy(k).start()
        kv_own().start()

    def kv_y_copy(ref, k, d):
        return remote(ref, ref, r.ky_send, r.ky_recv.at[k], (z, turn(y, SIGN[d]), x, c))

    def kv_y1():
        kv_own().wait()
        for k in range(len(OTHERS)):
            kv_z_copy(k).wait()
        for d in BOTH:
            kv_y_copy(r.kvh.at[x, c, :, y], d, d).start()

    def kv_y2():
        for d in BOTH:
            yy = turn(y, -SIGN[d])
            kv_y_copy(r.kvh.at[x, c, :, yy], d, d).wait_recv()
            kv_y_copy(r.kvh.at[x, c, :, yy, pl.ds(2 * d, 2)], 2, d).start()

    def kv_y3():
        kv_y_copy(r.kvh.at[x, c, :, turn(y, 2)], 2, 0).wait_recv()
        kv_y_copy(r.kvh.at[x, c, :, pl.ds(0, LAST)], 0, 0).wait_send()

    def kv_x_copy(l, ref, k, d):
        return remote(ref, ref, r.kx_send.at[l], r.kx_recv.at[l, k], (z, y, turn(x, SIGN[d]), c))

    def kv_die(l, ref):
        return remote(ref, ref, r.kd_send.at[l], r.kd_recv.at[l], partner)

    def kv_x1(l):
        ref = r.kvh.at[x, c, l]
        for d in BOTH:
            kv_x_copy(l, ref, d, d).start()
        kv_die(l, ref).start()

    def kv_x2(l):
        for d in BOTH:
            xx = turn(x, -SIGN[d])
            ref = r.kvh.at[xx, c, l]
            kv_x_copy(l, ref, d, d).wait_recv()
            kv_x_copy(l, r.kvh.at[xx, c, l, pl.ds(2 * d, 2)], 2, d).start()
            kv_die(l, ref).start()

    def kv_x3(l):
        ref = r.kvh.at[turn(x, 2), c, l]
        kv_x_copy(l, ref, 2, 0).wait_recv()
        kv_die(l, ref).start()

    def kv_load(l):
        kv_die(l, r.kvh.at[:, 1 - c, l]).wait_recv()
        kc = r.wkv.shape[1]
        for xx in RINGS:
            for cc in BOTH:
                pltpu.make_async_copy(r.kvh.at[xx, cc, l], r.kvb.at[:, :, pl.ds((xx * CORES + cc) * kc, kc)], r.k_loc.at[1]).start()

    def kv_sent(l):
        kv_x_copy(l, r.kvh.at[pl.ds(0, LAST), c, l], 0, 0).wait_send()
        kv_die(l, r.kvh.at[:, c, l]).wait_send()

    def kv_loaded():
        pltpu.make_async_copy(r.kvb, r.kvb, r.k_loc.at[1]).wait()

    def gain_move(i, src, dst, dev):
        return remote(src, dst, r.g_send.at[i], r.g_recv.at[i], dev)

    def gain_z(k):
        dev = (turn(z, OTHERS[k]), y, x, c)
        return gain_move(k, r.gbuf.at[x, c, y, z], r.gbuf.at[x, c, y, z], dev)

    def gain_y(k):
        dev = (z, turn(y, OTHERS[k]), x, c)
        return gain_move(len(OTHERS) + k, r.gbuf.at[x, c, y], r.gbuf.at[x, c, y], dev)

    def gain_x(k):
        dev = (z, y, turn(x, OTHERS[k]), c)
        return gain_move(CORES * len(OTHERS) + k, r.gbuf.at[x, c], r.gbuf.at[x, c], dev)

    def gain_die(xx, k):
        ref = r.gbuf.at[xx, c]
        return remote(ref, ref, r.gd_send.at[k], r.gd_recv.at[k], partner)

    def gain_sum():
        for zz in RINGS:
            for yy in RINGS:
                tot = jnp.zeros((n_layers, d_row), F32)
                for xx in RINGS:
                    for cc in BOTH:
                        tot += r.gbuf[xx, cc, yy, zz, :n_layers].astype(F32)
                at = (zz * RING + yy) * d_row
                r.gain[:, at:at + d_row] = tot

    tok_pair = CORES * rows

    def x_z(k):
        zz = turn(z, OTHERS[k])
        src = r.xt.at[pl.ds(zz * seqs, seqs)]
        return remote(src, r.xz.at[z], r.xz_send.at[k], r.xz_recv.at[k], (zz, y, x, c))

    def x_own():
        return pltpu.make_async_copy(r.xt.at[pl.ds(z * seqs, seqs)], r.xz.at[z], r.x_loc)

    def pos(xx):
        return pl.ds(pl.multiple_of(xx * tok_pair, tok_pair), tok_pair)

    def x_plane(oy, ox):
        yy, xx = turn(y, oy), turn(x, ox)
        return remote(r.xz.at[:, yy, :, pos(xx)], r.xp.at[c, y, x], r.xp_send.at[oy], r.xp_recv.at[(RING - oy) % RING], (z, yy, xx, c))

    def row_bytes(oy):
        return r.xp.at[c, 0] if oy else r.xp.at[c, 0, pl.ds(0, RING - 1)]

    def x_row(oy):
        yy = turn(y, oy)
        got = row_bytes(oy)
        remote(got, got, r.xp_send.at[oy], r.xp_recv.at[oy], partner).wait_recv()
        row = r.xp.at[c, yy]
        remote(row, row, r.xd_send.at[oy], r.xd_recv.at[oy], partner).start()

    def x_turn():
        for oy in RINGS:
            row = r.xp.at[1 - c, turn(y, oy)]
            remote(row, row, r.xd_send.at[oy], r.xd_recv.at[oy], partner).wait_recv()

        @pl.loop(0, RING)
        def _(zz):
            for yy in RINGS:
                for xh in BOTH:
                    blk = [r.xp[cc, yy, CORES * xh + xx, zz] for xx in BOTH for cc in BOTH]
                    blk = jnp.concatenate(blk, axis=0).astype(F32).T.astype(BF)
                    n = blk.shape[1]
                    at = pl.multiple_of(zz * RING * d_row + yy * d_row + xh * n, n)
                    r.hb[0, 0, :, :, pl.ds(at, n)] = blk.reshape(CORES, rows, n)
        r.hid[...] = r.hb[0, 0, c]
        for oy in RINGS:
            row = r.xp.at[c, turn(y, oy)]
            remote(row, row, r.xd_send.at[oy], r.xd_recv.at[oy], partner).wait_send()

    def x_sent():
        for fn in (x_z, gain_z, gain_y, gain_x):
            peers_of(fn, "wait_send")
        for k in RINGS:
            gain_die(x, k).wait_send()
        for oy in RINGS:
            got = row_bytes(oy)
            remote(got, got, r.xp_send.at[oy], r.xp_recv.at[oy], partner).wait_send()

    def y_die(p):
        cols = pl.ds(pl.multiple_of(turn(z, p) * width, width), width)
        return remote(r.hid.at[:, cols], r.hb.at[0, 0, c, :, cols], r.yd_send.at[p], r.yd_recv.at[p], partner)

    def planes(h):
        return pl.ds(2 * h, 2)

    def y_plane(h, oy, ox):
        yy, xx = turn(y, oy), turn(x, ox)
        return remote(r.xp.at[c, yy, xx, planes(h)], r.xz.at[planes(h), y, :, pos(x)], r.yp_send.at[h, oy], r.yp_recv.at[h, (RING - oy) % RING],
                      (z, yy, xx, c))

    def y_z(p, oy):
        s = turn(y, oy)
        return remote(r.xz.at[p, s], r.y_out.at[z * seqs + s], r.yz_send.at[p, oy], r.yz_recv.at[p, oy], (turn(z, p), y, x, c))

    def y_own(oy):
        s = turn(y, oy)
        return pltpu.make_async_copy(r.xz.at[0, s], r.y_out.at[z * seqs + s], r.y_loc.at[oy])

    def leave_a(h):
        for p in BOTH:
            p = 2 * h + p
            y_die(p).start()
            cols = pl.ds(pl.multiple_of(turn(z, p) * width, width), width)
            r.hb[0, 0, c, :, cols] = r.hid[:, cols]

    def leave_b(h):
        n = CORES * CORES * d_local
        for p in BOTH:
            p = 2 * h + p
            y_die(p).wait()

            @pl.loop(0, RING)
            def _(yy, p=p):
                for xh in BOTH:
                    at = pl.multiple_of(turn(z, p) * width + yy * d_row + xh * n, n)
                    blk = r.hb[0, 0, :, :, pl.ds(at, n)].reshape(tok_pair, n).astype(F32).T.astype(BF)
                    for xx in BOTH:
                        for cc in BOTH:
                            lo = (xx * CORES + cc) * d_local
                            r.xp[cc, yy, CORES * xh + xx, p] = blk[lo:lo + d_local]

        for oy in OTHERS + (0,):
            for ox in RINGS:
                if oy or ox:
                    y_plane(h, oy, ox).start()
        for p in BOTH:
            p = 2 * h + p
            r.xz[p, y, :, pos(x)] = r.xp[c, y, x, p]

    def plane_bytes(h, oy):
        return r.xp.at[c, 0, :, planes(h)] if oy else r.xp.at[c, 0, pl.ds(0, LAST), planes(h)]

    def leave_c(h):
        for oy in OTHERS + (0,):
            got = plane_bytes(h, oy)
            remote(got, got, r.yp_send.at[h, oy], r.yp_recv.at[h, oy], partner).wait_recv()
            for p in BOTH:
                p = 2 * h + p
                (y_z(p, oy) if p else y_own(oy)).start()

    def left():
        for oy in RINGS:
            for h in BOTH:
                got = plane_bytes(h, oy)
                remote(got, got, r.yp_send.at[h, oy], r.yp_recv.at[h, oy], partner).wait_send()
            for p in RINGS:
                (y_z(p, oy) if p else y_own(oy)).wait()

    def kv_rows(zz):
        n = CORES * seq_len // (RING * RING * RING * CORES)
        return pl.ds(pl.multiple_of(((zz * RING + y) * RING + x) * n, n), n)

    def kv_trade(l, k):
        zz = turn(z, OTHERS[k])
        return remote(r.kv_out.at[l, :, :, kv_rows(zz)], r.kvx.at[l, z], r.kvx_send.at[l, k], r.kvx_recv.at[l, k], (zz, y, x, c))

    def kv_keep(l):
        return pltpu.make_async_copy(r.kv_out.at[l, :, :, kv_rows(z)], r.kvx.at[l, z], r.kvx_loc.at[l])

    def kv_share(l):
        for k in range(len(OTHERS)):
            kv_trade(l, k).start()
        kv_keep(l).start()

    def kv_shared(l):
        for k in range(len(OTHERS)):
            kv_trade(l, k).wait()
        kv_keep(l).wait()

    def gather_norm(l, split, pump):
        hid = r.hid
        gain = r.gain[l:l + 1, :]
        for b in range(4):
            blk = hid[b * quarter:(b + 1) * quarter, :].astype(F32)
            mean = jnp.mean(blk, axis=-1, keepdims=True)
            cen = blk - mean
            var = jnp.mean(cen * cen, axis=-1, keepdims=True)
            r.h_ref[b * quarter:(b + 1) * quarter, :] = (cen * lax.rsqrt(var + LN_EPS) * gain).astype(BF)
        out = r.h_all.at[l]

        def spot(q, first, second):
            if q == 0:
                return turn(y, second), turn(x, first)
            return turn(y, first), turn(x, second)

        def span(q, part):
            lo, n = (split, rows - split) if q else (0, split)
            if part is NIL:
                return pl.ds(lo, n)
            return pl.ds(lo + part * (n // 2), n // 2)

        table = {}

        def link(key, *args, own=False):
            idx, (q, first, second, part, to_first, to_second) = table.setdefault(key, (len(table), args))
            sy, sx = spot(q, first, second)
            ty, tx = spot(q, to_first, to_second)
            rws = span(q, part)
            dst = out.at[sy, sx, c, rws]
            return remote(r.h_ref.at[rws] if own else dst, dst, r.ag_send.at[l, KINDS.index(key[0])], r.ag_recv.at[l, idx], (z, ty, tx, c))

        def arrived(*key):
            for d in BOTH:
                link((*key, d)).wait_recv()

        def die(q, first, second, own=False):
            sy, sx = spot(q, first, second)
            rws = span(q, NIL)
            dst = out.at[sy, sx, c, rws]
            off = (first if q else second) % RING
            remote(r.h_ref.at[rws] if own else dst, dst, r.ag_dsend.at[l], r.ag_drecv.at[l, off], partner).start()

        offs = (0, -1, 1, 2)

        def second_step(k):
            for d in BOTH:
                for q in BOTH:
                    link(("second", q, k, d)).wait_recv()
                    src = -SIGN[d]
                    link(("second_on", q, k, d), q, offs[k], src, d, 0, SIGN[d]).start()
                    die(q, offs[k], src)

        def last_step(q, k):
            arrived("second_on", q, k)
            die(q, offs[k], 2)

        def tail_a():
            for k in RINGS[2:]:
                second_step(k)
                hook(pump, f"k{k}")
            for k in (1, 2):
                last_step(1, k)

        def tail_b():
            for k in RINGS:
                last_step(0, k)
            last_step(1, LAST)

        for q in BOTH:
            for d in BOTH:
                link(("first", q, d), q, 0, 0, NIL, SIGN[d], 0, own=True).start()
        for q in BOTH:
            for d in BOTH:
                link(("second", q, 0, d), q, 0, 0, NIL, 0, SIGN[d], own=True).start()
        for q in BOTH:
            die(q, 0, 0, own=True)
        own = pltpu.make_async_copy(r.h_ref, out.at[y, x, c], r.ag_loc)
        own.start()
        hook(pump, "begin")
        for d in BOTH:
            for q in BOTH:
                link(("first", q, d)).wait_recv()
                src = -SIGN[d]
                link(("first_on", q, d), q, src, 0, d, SIGN[d], 0).start()
                die(q, src, 0)
        hook(pump, "first")
        second_step(0)
        for q in reversed(BOTH):
            for d in BOTH:
                for e in BOTH:
                    link(("second", q, 1 + d, e), q, -SIGN[d], 0, NIL, 0, SIGN[e]).start()
        hook(pump, "k0")
        for q in BOTH:
            arrived("first_on", q)
            for e in BOTH:
                link(("second", q, LAST, e), q, 2, 0, NIL, 0, SIGN[e]).start()
            die(q, 2, 0)
        hook(pump, "first_on")
        last_step(1, 0)
        own.wait()
        hook(pump, "ready")

        def crossed(off):
            got = out.at[turn(y, off), :, 1 - c]
            remote(got, got, r.ag_dsend.at[l], r.ag_drecv.at[l, off], partner).wait_recv()

        def order(i):
            return lax.rem(3 * i + 3 * (i // 2) + 2 * (i // 3), RING)

        def fetch(i, slot):
            off = order(i)
            crossed(off)
            h_copy(l, turn(y, off), slot).start()

        def up_ready():
            hook(pump, "up")
            loaded(UP1 if l else UP0)

        crossed(0)
        h_copy(l, y, 0).start()

        def opening():
            second_step(1)
            hook(pump, "k1")

        if l:
            @pl.loop(0, RING)
            def _(i):
                slot = lax.rem(i, 2)
                s = turn(y, order(i))
                h_copy(l, s, slot).wait()
                pump(("seq", i))
                one(l, s, slot, i)

                @pl.when(i == 0)
                def _():
                    opening()
                    up_ready()

                pump(("two", i))
                two(s, slot)

                @pl.when(i == 0)
                def _():
                    tail_a()
                    fetch(i + 1, 1 - slot)
                    fetch(i + 2, slot)

                @pl.when(i == 1)
                def _():
                    tail_b()
                    fetch(i + 2, slot)
        else:
            h_copy(l, y, 0).wait()
            hook(pump, "own")
            one(l, y, 0, 0)
            opening()
            tail_a()
            crossed(LAST)
            h_copy(l, turn(y, LAST), 1).start()

            @pl.loop(1, RING)
            def _(i):
                slot = lax.rem(i, 2)
                s = turn(y, order(i))
                h_copy(l, s, slot).wait()
                pump(("seq", i))
                one(l, s, slot, i)

                @pl.when(i == 1)
                def _():
                    up_ready()

                pump(("two", i - 1))
                two(turn(y, order(i - 1)), 1 - slot)

                @pl.when(i == 1)
                def _():
                    tail_b()

                @pl.when(i < LAST)
                def _():
                    fetch(i + 1, 1 - slot)

            hook(pump, "two3")
            two(turn(y, 2), 1)

        for slot in BOTH:
            for i in BOTH:
                kv_out_copy(l, 0, slot, i).wait()
        sent = (out.at[y, x], out.at[y], out.at[y, x, c], out.at[y, pl.ds(0, CORES)])
        for kind, ref in enumerate(sent):
            remote(ref, ref, r.ag_send.at[l, kind], r.ag_recv.at[l, kind], partner).wait_send()
        remote(out.at[pl.ds(0, 2)], out.at[pl.ds(0, 2)], r.ag_dsend.at[l], r.ag_drecv.at[l, 0], partner).wait_send()

    def h_copy(l, s, slot):
        return pltpu.make_async_copy(r.h_all.at[l, s], r.hb.at[slot], r.h_sem.at[slot])

    def h_tile(slot):
        return r.hb[slot].reshape(seq_len, d_model)

    def project(h, lo, n):
        w = r.wv[:, :, lo:lo + n].reshape(d_model, n)
        return jnp.dot(h, w, preferred_element_type=F32).astype(BF)

    def rope(val):
        val = val.astype(F32)
        return val * r.cos[...] + pltpu.roll(val, head_dim // 2, 1) * r.sin[...]

    n_chunk = min(256, f_loc)

    def kv_out_copy(l, s, slot, i):
        return pltpu.make_async_copy(r.qkv.at[slot, i], r.kv_out.at[l, i, s], r.kvo_sem.at[slot, i])

    def one(l, s, slot, i):
        @pl.when(i >= 2)
        def _():
            for k in BOTH:
                kv_out_copy(l, s, slot, k).wait()

        kv = jnp.zeros((seq_len, 2 * head_dim), F32)
        for zz in RINGS:
            for yy in RINGS:
                col = (zz * RING + yy) * d_row
                kv += lax.dot_general(h_cols(slot, col, d_row), r.kvb[yy, zz], (((1,), (1,)), ((), ())), preferred_element_type=F32)
        kv = kv.astype(BF)
        r.qkv[slot, 0] = rope(kv[:, :head_dim]).astype(BF)
        r.qkv[slot, 1] = kv[:, head_dim:]
        for i in BOTH:
            kv_out_copy(l, s, slot, i).start()
        q = project(h_tile(slot), 0, head_dim)
        r.stage[...] = (rope(q) * head_dim ** -0.5).astype(BF)
        for lo in range(0, f_loc, n_chunk):
            r.joined[s, :, head_dim + lo:head_dim + lo + n_chunk] = project(h_tile(slot), head_dim + lo, n_chunk)
        n_tile = seq_len // 2
        for i in BOTH:
            keys = (i + 1) * n_tile
            sc = lax.dot_general(r.stage[i * n_tile:(i + 1) * n_tile, :], r.qkv[slot, 0, :keys, :], (((1,), (1,)), ((), ())), preferred_element_type=F32)
            row_id = lax.broadcasted_iota(jnp.int32, sc.shape, 0) + i * n_tile
            col_id = lax.broadcasted_iota(jnp.int32, sc.shape, 1)
            sc = jnp.where(col_id <= row_id, sc, -1e30)
            top = jnp.max(sc, axis=-1, keepdims=True)
            ex = jnp.exp(sc - top)
            prob = (ex * (1.0 / jnp.sum(ex, axis=-1, keepdims=True))).astype(BF)
            att = jnp.dot(prob, r.qkv[slot, 1, :keys, :], preferred_element_type=F32)
            r.joined[s, i * n_tile:(i + 1) * n_tile, :head_dim] = att.astype(BF)

    def h_cols(slot, col, n):
        return r.hb[slot, :, :, :, col:col + n].reshape(seq_len, n)

    def two(s, slot):
        for lo in range(0, f_loc, n_chunk):
            up = project(h_tile(slot), head_dim + f_loc + lo, n_chunk).astype(F32)
            cols = slice(head_dim + lo, head_dim + lo + n_chunk)
            g = r.joined[s, :, cols].astype(F32)
            r.joined[s, :, cols] = (g * jax.nn.sigmoid(g) * up).astype(BF)

    def out_scatter(l, pump):
        def peer(q, first, second):
            dy = first * (1 - q) + second * q
            dx = first * q + second * (1 - q)
            return (z, turn(y, dy), turn(x, dx), c)

        def die_copy(ch, q, s):
            return remote(r.away.at[q], r.die_in.at[ch, q, s], r.dsend.at[l, ch, q, s], r.drecv.at[l, ch, q, s], partner)

        def first_copy(ch, q, d):
            return remote(r.acc.at[ch, q, 0, pl.ds(CORES * d, CORES)], r.in1.at[ch, q, d], r.send1.at[l, ch, q, d], r.recv1.at[l, ch, q, d],
                          peer(q, SIGN[d], 0))

        def second_copy(ch, q, d, h):
            js = pl.ds(CORES * h, CORES)
            return remote(r.acc.at[ch, q, 1 + d, js], r.in2.at[ch, q, d, js], r.send2.at[l, ch, q, d, h], r.recv2.at[l, ch, q, d, h],
                          peer(q, SIGN[d], 0))

        def half_rows(d):
            return pl.ds(d * (rows // 2), rows // 2)

        def third_copy(ch, q, d):
            return remote(r.acc.at[ch, q, LAST, 0, half_rows(d)], r.in3.at[ch, q, d], r.send3.at[l, ch, q, d], r.recv3.at[l, ch, q, d],
                          peer(q, 0, SIGN[d]))

        def fourth_copy(ch, q, d):
            return remote(r.acc.at[ch, q, LAST, 1 + d], r.in4.at[ch, q, d], r.send4.at[l, ch, q, d], r.recv4.at[l, ch, q, d],
                          peer(q, 0, SIGN[d]))

        n_blk = r.wov.shape[3]

        def plane_of(ch, q):
            return turn(z, LAST - q if ch else q)

        def tile(ch, q, s):
            for cc in BOTH:
                for j in RINGS:
                    oy = SLOT_OFF[s] * (1 - q) + SLOT_OFF[j] * q
                    ox = SLOT_OFF[j] * (1 - q) + SLOT_OFF[s] * q
                    core = c if cc else 1 - c
                    at = pl.multiple_of((turn(x, ox) * CORES + core) * rows, rows)
                    r.lhs[pl.ds((cc * RING + j) * rows, rows), :] = r.joined[turn(y, oy), pl.ds(at, rows), :]
            left = r.lhs[...]
            zz = plane_of(ch, q)

            @pl.loop(0, RING)
            def _(n):
                col = pl.multiple_of(n * n_blk, n_blk)
                res = jnp.dot(left, r.wov[zz, n], preferred_element_type=F32).astype(BF)
                res = res.reshape(CORES, RING, rows, n_blk)
                r.away[q, :, :, pl.ds(col, n_blk)] = res[0]
                r.acc[ch, q, s, :, :, pl.ds(col, n_blk)] = res[1]

        def pair_sum(ch, q, s):
            die_copy(ch, q, s).wait_recv()

            @pl.loop(0, RING)
            def _(j):
                r.acc[ch, q, s, j] = r.acc[ch, q, s, j] + r.die_in[ch, q, s, j]

        def stage_a(ch):
            for s in RINGS:
                @pl.loop(0, CORES)
                def _(q, s=s):
                    if s:
                        die_copy(ch, q, s - 1).wait_send()
                    elif ch:
                        die_copy(ch - 1, q, LAST).wait_send()
                    tile(ch, q, s)
                    die_copy(ch, q, s).start()
                    if s:
                        pair_sum(ch, q, s - 1)
                    if s == 1:
                        for d in BOTH:
                            first_copy(ch, q, d).start()
                    if s > 1:
                        second_copy(ch, q, s - 2, LAST - s).start()
                hook(pump, f"a{ch}s{s}")

        def stage_b(ch):
            for q in BOTH:
                pair_sum(ch, q, LAST)
            for q in BOTH:
                for d in BOTH:
                    first_copy(ch, q, d).wait_recv()
                    for j in BOTH:
                        at = CORES * d + j
                        r.acc[ch, q, 1 + d, at] = r.acc[ch, q, 1 + d, at] + r.in1[ch, q, d, j]
                    second_copy(ch, q, d, d).start()

        def total(ch, q, j):
            val = r.acc[ch, q, LAST, j].astype(F32)
            for d in BOTH:
                val += r.in2[ch, q, d, j].astype(F32)
            r.acc[ch, q, LAST, j] = val.astype(BF)

        def stage_c(ch):
            for q in BOTH:
                for h in BOTH:
                    for d in BOTH:
                        second_copy(ch, q, d, h).wait_recv()
                total(ch, q, 0)
                for d in BOTH:
                    third_copy(ch, q, d).start()
                for j in RINGS[1:]:
                    total(ch, q, j)

        def stage_d(ch):
            for q in BOTH:
                for d in BOTH:
                    third_copy(ch, q, d).wait_recv()
                    rws = half_rows(d)
                    r.acc[ch, q, LAST, 1 + d, rws] = r.acc[ch, q, LAST, 1 + d, rws] + r.in3[ch, q, d]
                    fourth_copy(ch, q, d).start()

        def stage_e(ch):
            for q in BOTH:
                for d in BOTH:
                    fourth_copy(ch, q, d).wait_recv()
                cols = pl.ds(pl.multiple_of(plane_of(ch, q) * width, width), width)
                upd = r.acc[ch, q, LAST, LAST].astype(F32)
                for d in BOTH:
                    upd += r.in4[ch, q, d].astype(F32)
                upd = upd.astype(BF)
                r.hid[:, cols] = (r.hid[:, cols].astype(F32) + upd.astype(F32)).astype(BF)

        def sent(ch):
            for q in BOTH:
                if ch:
                    die_copy(ch, q, LAST).wait_send()
                for d in BOTH:
                    for cp in (first_copy, third_copy, fourth_copy):
                        cp(ch, q, d).wait_send()
                    for h in BOTH:
                        second_copy(ch, q, d, h).wait_send()

        for step, fn, ch in (
            ("a0", stage_a, 0), ("b0", stage_b, 0), ("a1", stage_a, 1), ("b1", stage_b, 1), ("c0", stage_c, 0), ("c1", stage_c, 1),
            ("d0", stage_d, 0), ("d1", stage_d, 1), ("e0", stage_e, 0), ("e1", stage_e, 1),
        ):
            with jax.named_scope(step):
                fn(ch)
            hook(pump, step)
        for ch in BOTH:
            sent(ch)

    def near(fn, t):
        for j in (LAST, 1):
            fn(t, j)

    def far(fn, t):
        fn(t, 2)

    def z_all(t):
        near(z_direct, t)
        far(z_direct, t)

    def peers_of(fn, op="start"):
        for k in range(len(OTHERS)):
            getattr(fn(k), op)()

    def start():
        peers_of(gain_z)
        kv_z()
        peers_of(x_z)
        x_own().start()
        z_own(QG0)
        z_own(UP0)
        with jax.named_scope("gain_a"):
            peers_of(gain_z, "wait_recv")
            peers_of(gain_y)
        with jax.named_scope("kv_a"):
            kv_y1()
        y_send(QG0)
        with jax.named_scope("gain_b"):
            peers_of(gain_y, "wait_recv")
            peers_of(gain_x)
            gain_die(x, LAST).start()
        with jax.named_scope("x_z"):
            peers_of(x_z, "wait_recv")
            x_own().wait()
        for oy in RINGS:
            for ox in RINGS:
                if oy or ox:
                    x_plane(oy, ox).start()
        r.xp[c, y, x] = r.xz[:, y, :, pos(x)]
        with jax.named_scope("kv_b"):
            kv_y2()
        with jax.named_scope("gain_c"):
            for k, o in enumerate(OTHERS):
                gain_x(k).wait_recv()
                gain_die(turn(x, -o), k).start()
        with jax.named_scope("rows"):
            for oy in (0, LAST, 1, 2):
                x_row(oy)
        with jax.named_scope("relay"):
            y_relay(QG0)
            z_forward(QG0, 0)
            near(z_direct, QG0)
            z_forward(UP0, 0)
        with jax.named_scope("kv_c"):
            kv_y3()
            kv_x1(0)
        with jax.named_scope("gain_sum"):
            for k in RINGS:
                gain_die(x, k).wait_recv()
            gain_sum()
        with jax.named_scope("turn"):
            x_turn()

    def when(i, n, *fns):
        @pl.when(i == n)
        def _():
            for fn in fns:
                fn()

    def plan(steps):
        def pump(step):
            for fn, *args in steps.get(step, ()):
                with jax.named_scope(f"{fn.__name__}_{args[-1] if args else 0}"):
                    fn(*args)

        def front(step):
            if isinstance(step, str):
                pump(step)
                return
            for n in RINGS:
                if (step[0], n) in steps:
                    when(step[1], n, lambda n=n: pump((step[0], n)))
        return front

    def both_loaded(t):
        loaded(t)
        kv_loaded()

    first_front = plan({
        "begin": [(z_direct, QG0, 2), (y_send, UP0)],
        "first": [(kv_x2, 0), (z_forward, QG0, LAST)],
        "k0": [(z_forward, QG0, 1)],
        "first_on": [(kv_x3, 0), (z_forward, QG0, 2), (y_relay, UP0), (z_direct, UP0, LAST), (z_direct, UP0, 1), (y_send, WO0)],
        "ready": [(load_near, QG0), (load_far, QG0), (kv_load, 0), (loaded, QG0), (kv_loaded,)],
        "own": [(y_send, UP1)],
        "k1": [(z_forward, UP0, LAST), (z_direct, UP0, 2), (y_relay, WO0)],
        "k3": [(z_forward, UP0, 1), (z_own, WO0)],
        ("seq", 1): [(z_forward, UP0, 2), (z_direct, WO0, LAST), (z_direct, WO0, 1), (y_relay, UP1), (x_sent,)],
        "up": [(z_direct, WO0, 2), (z_forward, WO0, 0), (y_send, QG1), (y_send, WO1), (load_near, UP0), (load_far, UP0)],
        ("two", 0): [(z_own, QG1)],
        ("two", 1): [(z_forward, WO0, LAST), (y_relay, QG1)],
        ("seq", 3): [(z_forward, WO0, 1), (kv_x1, 1)],
        ("two", 2): [(z_forward, WO0, 2), (y_relay, WO1)],
        "two3": [(kv_x2, 1)],
    })
    first_scatter = plan({
        "a0s0": [(z_forward, QG1, 0), (kv_x3, 1)],
        "a0s1": [(z_direct, QG1, 1)],
        "a0": [(z_direct, QG1, 2)],
        "b0": [(load_far, WO0), (far_loaded, WO0)],
        "a1s1": [(z_forward, QG1, LAST)],
        "a1s2": [(z_direct, UP1, LAST)],
        "a1": [(z_direct, UP1, 1)],
        "b1": [(z_forward, QG1, 1)],
        "c1": [(z_forward, QG1, 2), (z_direct, UP1, 2), (z_own, UP1)],
        "d1": [(z_forward, UP1, LAST)],
        "e1": [(z_forward, UP1, 1)],
    })
    second_front = plan({
        "begin": [(kv_load, 1)],
        "first": [(z_direct, WO1, LAST)],
        "k0": [(z_forward, UP1, 2)],
        "first_on": [(z_forward, UP1, 0)],
        "ready": [(z_direct, WO1, 1), (load_near, QG1), (load_far, QG1), (loaded, QG1), (kv_loaded,)],
        "k1": [(z_direct, WO1, 2), (z_forward, WO1, LAST)],
        "up": [(load_near, UP1), (load_far, UP1)],
        "k2": [(z_own, WO1)],
        ("seq", 1): [(z_forward, WO1, 1)],
        ("two", 1): [(z_forward, WO1, 2)],
        ("two", 2): [(z_forward, WO1, 0)],
    })
    second_scatter = plan({
        "b0": [(load_far, WO1), (far_loaded, WO1)],
        "e0": [(leave_a, 0)],
    })

    with jax.named_scope("start"):
        start()
    with jax.named_scope("front_0"):
        gather_norm(0, rows // RING, first_front)
    with jax.named_scope("near_0"):
        kv_share(0)
        z_direct(QG1, LAST)
        load_near(WO0)
        near_loaded(WO0)
    with jax.named_scope("scatter_0"):
        out_scatter(0, first_scatter)
    with jax.named_scope("front_1"):
        gather_norm(1, rows // 2, second_front)
    with jax.named_scope("near_1"):
        kv_share(1)
        load_near(WO1)
        near_loaded(WO1)
    with jax.named_scope("scatter_1"):
        out_scatter(1, second_scatter)
    with jax.named_scope("leave"):
        leave_a(1)
        leave_b(1)
        leave_b(0)
        leave_c(1)
        leave_c(0)
        left()
    with jax.named_scope("drain"):
        for t in range(WO1 + 1):
            drain(t)
        for l in range(n_layers):
            kv_shared(l)
            kv_sent(l)


def run_model(xt, gain, wkv_t, w_in, w_out, cos_full, sin_full):
    batch, d_local, seq_len = xt.shape
    n_layers, d_row, e_block = w_in.shape
    r_block, d_col = w_out.shape[1:]
    head_dim = cos_full.shape[1]
    d_model = d_row * RING * RING
    seqs = batch // RING
    rows = seqs * seq_len // (RING * RING * CORES)
    e_loc, r_loc = e_block // RING, r_block // RING
    kc = wkv_t.shape[1]
    width = d_model // RING
    n_t = 3 * n_layers
    n_o = len(OTHERS)

    def dma(*shape):
        return pltpu.SemaphoreType.DMA(shape)

    def vm(*shape):
        return pltpu.VMEM(shape, BF)

    def out(*shape):
        return jax.ShapeDtypeStruct(shape, BF)

    any_spec = pl.BlockSpec(memory_space=pl.ANY)
    vm_spec = pl.BlockSpec(memory_space=pltpu.VMEM)
    out_shape = [
        out(batch, d_local, seq_len),
        out(n_layers, 2, seqs, seq_len, head_dim),
        out(n_layers, RING, RING, CORES, rows, d_model),
        out(n_layers, RING, RING * d_row, e_loc),
        out(n_layers, RING, RING, r_loc, d_col),
        out(RING, CORES, n_layers, RING, RING, kc, d_row),
        out(n_layers, RING, 2, seqs, CORES * (seq_len // (CORES * RING * RING * RING)), head_dim),
        out(n_layers, 2, d_row // 2, e_loc),
        out(n_layers, 2, r_loc // 2, d_col),
    ]
    pair = (2, 2, 2)
    each = (n_layers, *pair)
    scratch = [
        vm(rows, d_model), vm(rows, d_model), pltpu.VMEM((n_layers, d_model), F32),
        vm(RING, CORES, RING, RING, G_ROWS, d_row),
        vm(RING, seqs, d_local, seq_len),
        vm(CORES, RING, RING, RING, d_local, CORES * rows),
        vm(RING, RING * d_row, e_loc), vm(RING, RING, 2 * head_dim, d_row), vm(RING, RING, r_loc, d_col),
        vm(2, RING, CORES, rows, d_model), vm(RING, seq_len, r_loc), vm(2, 2, seq_len, head_dim), vm(seq_len, head_dim),
        vm(CORES * RING * rows, r_loc), vm(2, RING, rows, width), vm(2, 2, RING, RING, rows, width), vm(2, 2, RING, RING, rows, width),
        vm(*pair, 2, rows, width), vm(*pair, RING, rows, width), vm(*pair, rows // 2, width), vm(*pair, rows, width),
        dma(n_o), dma(n_o), dma(RING), dma(RING), dma(RING), dma(RING), pltpu.SemaphoreType.DMA,
        dma(3 * n_o), dma(3 * n_o), dma(RING), dma(RING),
        dma(RING), dma(RING), dma(2, RING), dma(2, RING), dma(RING, RING), dma(RING, RING), dma(RING),
        dma(n_layers, RING), dma(n_layers, 40), dma(n_layers), dma(n_layers, RING), pltpu.SemaphoreType.DMA, dma(2), dma(2, 2), dma(3), dma(3),
        dma(n_t, RING), dma(n_t, 2), dma(n_t, RING, 2), dma(n_t, RING, 2), dma(n_t, RING),
        dma(n_o), dma(n_o), pltpu.SemaphoreType.DMA, dma(n_o), dma(n_layers), dma(n_layers, n_o), dma(n_layers), dma(n_layers), dma(2),
        dma(n_layers, 2, 2, RING), dma(n_layers, 2, 2, RING),
        dma(*each), dma(*each), dma(*each, 2), dma(*each, 2), dma(*each), dma(*each), dma(*each), dma(*each),
        dma(n_layers, n_o), dma(n_layers, n_o), dma(n_layers),
    ]
    res = pl.pallas_call(
        model_kernel,
        out_shape=out_shape,
        in_specs=[any_spec, vm_spec, vm_spec, any_spec, any_spec, vm_spec, vm_spec],
        out_specs=[any_spec] * len(out_shape),
        scratch_shapes=scratch,
        compiler_params=pltpu.CompilerParams(collective_id=0, has_side_effects=True, vmem_limit_bytes=VMEM_LIMIT),
        name="two_layers",
    )(xt, gain, wkv_t, w_in, w_out, cos_full, sin_full)
    return res[0], res[6]


def solution(mesh):
    row_size = mesh.shape["row"]
    n_col = mesh.shape["col"]
    n_z = row_size // RING
    n_y = RING
    n_x = n_col // CORES
    n_tp = n_y * n_col
    n_dev = row_size * n_col
    mesh4 = Mesh(mesh.devices.reshape(n_z, n_y, n_x, CORES), ("z", "y", "x", "core"))
    every = ("z", "y", "x", "core")
    col = ("x", "core")
    act_spec = P(NIL, NIL, every)
    w_spec = P(NIL, ("z", "y"), col)

    def device_fn(x_loc, gain_loc, w_in_loc, w_kv_loc, w_out_loc):
        n_layers = w_in_loc.shape[0]
        n_batch, seq_len, d_local = x_loc.shape
        head_dim = w_kv_loc.shape[2] * n_col // 2
        batch_loc = n_batch // n_z
        seq_local = seq_len // n_dev
        steps = np.arange(head_dim // 2, dtype=np.float32)
        inv_freq = (1.0 / 10000.0 ** (steps * 2 / head_dim)).astype(np.float32)
        angles = np.arange(seq_len, dtype=np.float32)[:, NIL] * inv_freq[NIL, :]
        cos_tab, sin_tab = np.cos(angles), np.sin(angles)
        cos_full = jnp.asarray(np.concatenate([cos_tab, cos_tab], axis=1))
        sin_full = jnp.asarray(np.concatenate([-sin_tab, sin_tab], axis=1))
        y_loc, kv = run_model(x_loc.transpose(0, 2, 1), gain_loc, w_kv_loc.transpose(0, 2, 1), w_in_loc, w_out_loc, cos_full, sin_full)
        y_loc = y_loc.transpose(0, 2, 1)
        kv = kv.reshape(n_layers, n_z, 2, batch_loc, CORES, seq_local, head_dim)
        kv = lax.dynamic_index_in_dim(kv, lax.axis_index("core"), axis=4, keepdims=False)
        kv = kv.transpose(0, 2, 1, 3, 4, 5).reshape(n_layers, 2, n_batch, seq_local, head_dim)
        return y_loc, kv

    return jax.shard_map(device_fn, mesh=mesh4, in_specs=(act_spec, P(NIL, every), w_spec, w_spec, P(NIL, col, ("z", "y"))), out_specs=(act_spec, P(NIL, NIL, NIL, every, NIL)), check_vma=False)
```

```python
import jax
import jax.numpy as jnp
import numpy as np
from jax import lax
from jax.experimental import pallas as pl
from jax.experimental.pallas import tpu as pltpu
from jax.sharding import Mesh
from jax.sharding import PartitionSpec as P

LN_EPS = 1e-6
RING = 4
CORES = 2
VMEM_LIMIT = 67_000_000
BF = jnp.bfloat16
F32 = jnp.float32
SLOT_OFF = (2, 1, 3, 0)
SIGN = (1, -1)
NIL = None
BOTH = range(CORES)
RINGS = range(RING)
OTHERS = (1, 3, 2)
LAST = RING - 1
G_ROWS = 8
QG0, UP0, WO0, QG1, UP1, WO1 = range(6)
OWN, AFTER, FAR, BEFORE = RINGS
FIRST_ORDER = ("a0", "b0", "a1", "b1", "c0", "c1", "d0", "d1", "e0", "e1")
LAST_ORDER = FIRST_ORDER[:-1] + ("f1", "e1", "g1", "f0", "g0", "h1", "h0")
KINDS = ("first", "second", "first_on", "second_on")
NAMES = (
    "xt", "gain_in", "wkv", "w_in", "w_out", "cos", "sin", "y_out", "kv_out", "h_all", "wi", "wo", "kvh", "kvx", "rwi", "rwo", "h_ref",
    "hid", "gain", "gbuf", "xz", "xp",
    "wv", "kvb", "wov", "hb", "joined", "qkv", "stage", "lhs", "away", "acc", "die_in", "in1", "in2", "in3", "in4",
    "xz_send", "xz_recv", "xp_send", "xp_recv", "xd_send", "xd_recv", "x_loc", "g_send", "g_recv", "gd_send", "gd_recv", "yd_send", "yd_recv", "yp_send", "yp_recv", "yz_send", "yz_recv", "y_loc",
    "ag_send", "ag_recv", "ag_dsend", "ag_drecv", "ag_loc", "h_sem", "kvo_sem", "w_load", "far_load", "y_recv", "ry_recv", "zb_recv",
    "zc_recv", "w_send", "kz_send", "kz_recv", "ky_send", "ky_recv", "kx_send", "kx_recv", "kd_send", "kd_recv",
    "k_loc", "dsend", "drecv", "send1", "recv1", "send2", "recv2", "send3", "recv3", "send4", "recv4", "kvx_send", "kvx_recv", "kvx_loc",
)


class Refs:
    def __init__(self, refs):
        for name, ref in zip(NAMES, refs, strict=True):
            setattr(self, name, ref)


def model_kernel(*refs):
    r = Refs(refs)
    z, y, x, c = (lax.axis_index(a) for a in ("z", "y", "x", "core"))
    n_layers = r.wkv.shape[0]
    rows, d_model = r.hid.shape
    batch, d_local = r.xt.shape[:2]
    seqs = batch // RING
    seq_len, head_dim = r.cos.shape
    d_row = r.w_in.shape[1]
    e_loc = r.wi.shape[3]
    depth = r.wo.shape[3]
    f_loc = depth - head_dim
    quarter = rows // 4
    width = d_model // RING
    q_block = head_dim * RING
    f_block = f_loc * RING

    turned = {id(v): [lax.rem(v + o, RING) for o in RINGS] for v in (z, y, x)}

    def turn(base, off):
        if isinstance(off, int):
            return turned[id(base)][off % RING]
        return lax.rem(base + off + RING, RING)

    def remote(src, dst, ssem, rsem, dev):
        return pltpu.make_async_remote_copy(
            src_ref=src, dst_ref=dst, send_sem=ssem, recv_sem=rsem, device_id=dev, device_id_type=pl.DeviceIdType.MESH)

    partner = (z, y, x, 1 - c)

    peers = [(turn(z, o), y, x, c) for o in OTHERS]
    peers += [(z, turn(y, oy), turn(x, ox), c) for oy in RINGS for ox in RINGS if oy or ox]
    peers.append(partner)
    here = (z, y, x, c)
    gate_sem = pltpu.get_barrier_semaphore()
    for dev in peers:
        pl.semaphore_signal(gate_sem, inc=1, device_id=dev, device_id_type=pl.DeviceIdType.MESH)
    src_id = lax.broadcasted_iota(jnp.int32, (d_local, d_row), 0) + (x * CORES + c) * d_local
    dst_id = lax.broadcasted_iota(jnp.int32, (d_local, d_row), 1)
    spread = jnp.where(src_id == dst_id, 1.0, 0.0).astype(BF)
    r.gbuf[x, c, y, z] = jnp.zeros((G_ROWS, d_row), BF)
    r.gbuf[x, c, y, z, :n_layers] = jnp.dot(r.gain_in[...], spread, preferred_element_type=F32).astype(BF)
    pl.semaphore_wait(gate_sem, len(peers))

    def hook(pump, i):
        with jax.named_scope(f"hook_{i}"):
            pump(i)

    def w_cols(kind):
        return pl.ds(0, head_dim + f_loc) if kind == 0 else pl.ds(head_dim + f_loc, f_loc)

    def piece(t, zz, yy):
        l, kind = t // 3, t % 3
        if kind == 2:
            return r.wo.at[l, zz, yy]
        return r.wi.at[l, zz, pl.ds(pl.multiple_of(yy * d_row, d_row), d_row), w_cols(kind)]

    def piece_half(t, zz, yy, h):
        l, kind = t // 3, t % 3
        if kind == 2:
            return r.wo.at[l, zz, yy, pl.ds(h * (depth // 2), depth // 2)]
        return r.wi.at[l, zz, pl.ds(pl.multiple_of(yy * d_row + h * (d_row // 2), d_row // 2), d_row // 2), w_cols(kind)]

    def own_parts(t, owner, zz, yy):
        l, kind = t // 3, t % 3
        hq = pl.ds(pl.multiple_of(owner * head_dim, head_dim), head_dim)
        if kind == 2:
            return [
                (r.w_out.at[l, hq], r.wo.at[l, zz, yy, pl.ds(0, head_dim)]),
                (r.w_out.at[l, pl.ds(pl.multiple_of(q_block + owner * f_loc, head_dim), f_loc)], r.wo.at[l, zz, yy, pl.ds(head_dim, f_loc)]),
            ]
        rws = pl.ds(pl.multiple_of(yy * d_row, d_row), d_row)
        if kind == 0:
            return [
                (r.w_in.at[l, :, hq], r.wi.at[l, zz, rws, pl.ds(0, head_dim)]),
                (r.w_in.at[l, :, pl.ds(pl.multiple_of(q_block + owner * f_loc, head_dim), f_loc)], r.wi.at[l, zz, rws, pl.ds(head_dim, f_loc)]),
            ]
        return [(r.w_in.at[l, :, pl.ds(pl.multiple_of(q_block + f_block + owner * f_loc, head_dim), f_loc)],
                 r.wi.at[l, zz, rws, pl.ds(head_dim + f_loc, f_loc)])]

    def relay_ref(t, d):
        l, kind = t // 3, t % 3
        return r.rwo.at[l, d] if kind == 2 else r.rwi.at[l, d, :, w_cols(kind)]

    def far_parts(t, d):
        l, kind = t // 3, t % 3
        owner = turn(y, 2)
        hq = pl.ds(pl.multiple_of(owner * head_dim, head_dim), head_dim)
        if kind == 2:
            n = depth // 2
            base = q_block + owner * f_loc
            if d:
                return [(r.w_out.at[l, pl.ds(pl.multiple_of(base + n - head_dim, G_ROWS), n)], r.rwo.at[l, d])]
            return [
                (r.w_out.at[l, hq], r.rwo.at[l, d, pl.ds(0, head_dim)]),
                (r.w_out.at[l, pl.ds(pl.multiple_of(base, head_dim), n - head_dim)], r.rwo.at[l, d, pl.ds(head_dim, n - head_dim)]),
            ]
        rws = pl.ds(d * (d_row // 2), d_row // 2)
        if kind == 0:
            return [
                (r.w_in.at[l, rws, hq], r.rwi.at[l, d, :, pl.ds(0, head_dim)]),
                (r.w_in.at[l, rws, pl.ds(pl.multiple_of(q_block + owner * f_loc, head_dim), f_loc)], r.rwi.at[l, d, :, pl.ds(head_dim, f_loc)]),
            ]
        return [(r.w_in.at[l, rws, pl.ds(pl.multiple_of(q_block + f_block + owner * f_loc, head_dim), f_loc)], relay_ref(t, d))]

    def y_send(t):
        for d in BOTH:
            owner = turn(y, SIGN[d])
            dev = (z, owner, x, c)
            for src, dst in far_parts(t, d):
                remote(src, dst, r.w_send.at[t, 0], r.ry_recv.at[t, d], dev).start()
            for src, dst in own_parts(t, owner, z, y):
                remote(src, dst, r.w_send.at[t, 0], r.y_recv.at[t, -SIGN[d] % RING], dev).start()

    def y_relay(t):
        for d in BOTH:
            ref = relay_ref(t, d)
            remote(ref, ref, r.w_send.at[t, 3], r.ry_recv.at[t, d], here).wait_recv()
            dst = piece_half(t, z, turn(y, -SIGN[d]), d)
            remote(ref, dst, r.w_send.at[t, 3], r.y_recv.at[t, 2], (z, turn(y, SIGN[d]), x, c)).start()

    def z_own(t):
        for d in BOTH:
            for src, dst in own_parts(t, y, z, y):
                remote(src, dst, r.w_send.at[t, 1], r.zb_recv.at[t, 0, d], (turn(z, SIGN[d]), y, x, c)).start()

    def z_direct(t, j):
        yy = turn(y, j)
        ref = piece(t, z, yy)
        remote(ref, ref, r.w_send.at[t, 0], r.y_recv.at[t, j], here).wait_recv()
        for d in BOTH:
            remote(ref, ref, r.w_send.at[t, 1], r.zb_recv.at[t, j, d], (turn(z, SIGN[d]), y, x, c)).start()

    def z_forward(t, j):
        yy = turn(y, j)
        for d in BOTH:
            zz = turn(z, -SIGN[d])
            ref = piece(t, zz, yy)
            remote(ref, ref, r.w_send.at[t, 1], r.zb_recv.at[t, j, d], here).wait_recv()
            part = piece_half(t, zz, yy, d)
            remote(part, part, r.w_send.at[t, 2], r.zc_recv.at[t, j, d], (turn(z, SIGN[d]), y, x, c)).start()

    def place(t, zz):
        l, kind = t // 3, t % 3
        if kind == 2:
            return r.wo.at[l, zz], r.wov.at[zz]
        return r.wi.at[l, zz, :, w_cols(kind)], r.wv.at[zz, :, w_cols(kind)]

    def load_near(t):
        kind = t % 3
        for d in BOTH:
            src, dst = place(t, turn(z, SIGN[d]))
            pltpu.make_async_copy(src, dst, r.w_load.at[kind]).start()
        for j in OTHERS:
            yy = turn(y, j)
            dst = r.wov.at[z, yy] if kind == 2 else r.wv.at[z, pl.ds(pl.multiple_of(yy * d_row, d_row), d_row), w_cols(kind)]
            pltpu.make_async_copy(piece(t, z, yy), dst, r.w_load.at[kind]).start()
        for src, dst in own_parts(t, y, z, y):
            pltpu.make_async_copy(src, own_place(t, dst, src), r.w_load.at[kind]).start()

    def load_far(t):
        far = turn(z, 2)
        for j in RINGS:
            for d in BOTH:
                part = piece_half(t, far, turn(y, j), d)
                remote(part, part, r.w_send.at[t, 2], r.zc_recv.at[t, j, d], here).wait_recv()
        src, dst = place(t, far)
        pltpu.make_async_copy(src, dst, r.far_load.at[t % 3]).start()

    def own_place(t, dst, src):
        kind = t % 3
        if kind == 2:
            n = src.shape[0]
            return r.wov.at[z, y, pl.ds(0 if n == head_dim and f_loc != head_dim else head_dim, n)]
        n = src.shape[1]
        rws = pl.ds(pl.multiple_of(y * d_row, d_row), d_row)
        if kind == 0:
            return r.wv.at[z, rws, pl.ds(0 if n == head_dim and f_loc != head_dim else head_dim, n)]
        return r.wv.at[z, rws, pl.ds(head_dim + f_loc, f_loc)]

    def finish(t):
        load_near(t)
        load_far(t)

    def near_loaded(t):
        kind = t % 3
        dst = r.wov.at[pl.ds(0, LAST)] if kind == 2 else r.wv.at[pl.ds(0, LAST), :, w_cols(kind)]
        pltpu.make_async_copy(dst, dst, r.w_load.at[kind]).wait()

    def far_loaded(t):
        kind = t % 3
        dst = r.wov.at[0] if kind == 2 else r.wv.at[0, :, w_cols(kind)]
        pltpu.make_async_copy(dst, dst, r.far_load.at[kind]).wait()

    def loaded(t):
        near_loaded(t)
        far_loaded(t)

    def drain(t):
        l, kind = t // 3, t % 3
        if kind == 2:
            done = (r.wo.at[l, 0, pl.ds(0, LAST)], r.wo.at[l, pl.ds(0, 2)], r.wo.at[l, 0], r.wo.at[l, 0, 0])
        else:
            cols = w_cols(kind)
            done = (r.wi.at[l, 0, pl.ds(0, LAST * d_row), cols], r.wi.at[l, pl.ds(0, 2), :, cols], r.wi.at[l, 0, :, cols],
                    r.wi.at[l, 0, pl.ds(0, d_row), cols])
        for g, ref in enumerate(done):
            remote(ref, ref, r.w_send.at[t, g], r.y_recv.at[t, 0], here).wait_send()

    def kv_z_copy(k):
        return remote(r.wkv, r.kvh.at[x, c, :, y, z], r.kz_send.at[k], r.kz_recv.at[k], (turn(z, OTHERS[k]), y, x, c))

    def kv_own():
        return pltpu.make_async_copy(r.wkv, r.kvh.at[x, c, :, y, z], r.k_loc.at[0])

    def kv_z():
        for k in range(len(OTHERS)):
            kv_z_copy(k).start()
        kv_own().start()

    def kv_y_copy(ref, k, d):
        return remote(ref, ref, r.ky_send, r.ky_recv.at[k], (z, turn(y, SIGN[d]), x, c))

    def kv_y1():
        kv_own().wait()
        for k in range(len(OTHERS)):
            kv_z_copy(k).wait()
        for d in BOTH:
            kv_y_copy(r.kvh.at[x, c, :, y], d, d).start()

    def kv_y2():
        for d in BOTH:
            yy = turn(y, -SIGN[d])
            kv_y_copy(r.kvh.at[x, c, :, yy], d, d).wait_recv()
            kv_y_copy(r.kvh.at[x, c, :, yy, pl.ds(2 * d, 2)], 2, d).start()

    def kv_y3():
        kv_y_copy(r.kvh.at[x, c, :, turn(y, 2)], 2, 0).wait_recv()
        kv_y_copy(r.kvh.at[x, c, :, pl.ds(0, LAST)], 0, 0).wait_send()

    def kv_x_copy(l, ref, k, d):
        return remote(ref, ref, r.kx_send.at[l], r.kx_recv.at[l, k], (z, y, turn(x, SIGN[d]), c))

    def kv_die(l, ref):
        return remote(ref, ref, r.kd_send.at[l], r.kd_recv.at[l], partner)

    def kv_x1(l):
        ref = r.kvh.at[x, c, l]
        for d in BOTH:
            kv_x_copy(l, ref, d, d).start()
        kv_die(l, ref).start()

    def kv_x2(l):
        for d in BOTH:
            xx = turn(x, -SIGN[d])
            ref = r.kvh.at[xx, c, l]
            kv_x_copy(l, ref, d, d).wait_recv()
            kv_x_copy(l, r.kvh.at[xx, c, l, pl.ds(2 * d, 2)], 2, d).start()
            kv_die(l, ref).start()

    def kv_x3(l):
        ref = r.kvh.at[turn(x, 2), c, l]
        kv_x_copy(l, ref, 2, 0).wait_recv()
        kv_die(l, ref).start()

    def kv_load(l):
        kv_die(l, r.kvh.at[:, 1 - c, l]).wait_recv()
        kc = r.wkv.shape[1]
        for xx in RINGS:
            for cc in BOTH:
                pltpu.make_async_copy(r.kvh.at[xx, cc, l], r.kvb.at[:, :, pl.ds((xx * CORES + cc) * kc, kc)], r.k_loc.at[1]).start()

    def kv_sent(l):
        kv_x_copy(l, r.kvh.at[pl.ds(0, LAST), c, l], 0, 0).wait_send()
        kv_die(l, r.kvh.at[:, c, l]).wait_send()

    def kv_loaded():
        pltpu.make_async_copy(r.kvb, r.kvb, r.k_loc.at[1]).wait()

    def gain_move(i, src, dst, dev):
        return remote(src, dst, r.g_send.at[i], r.g_recv.at[i], dev)

    def gain_z(k):
        dev = (turn(z, OTHERS[k]), y, x, c)
        return gain_move(k, r.gbuf.at[x, c, y, z], r.gbuf.at[x, c, y, z], dev)

    def gain_y(k):
        dev = (z, turn(y, OTHERS[k]), x, c)
        return gain_move(len(OTHERS) + k, r.gbuf.at[x, c, y], r.gbuf.at[x, c, y], dev)

    def gain_x(k):
        dev = (z, y, turn(x, OTHERS[k]), c)
        return gain_move(CORES * len(OTHERS) + k, r.gbuf.at[x, c], r.gbuf.at[x, c], dev)

    def gain_die(xx, k):
        ref = r.gbuf.at[xx, c]
        return remote(ref, ref, r.gd_send.at[k], r.gd_recv.at[k], partner)

    def gain_sum():
        for zz in RINGS:
            for yy in RINGS:
                tot = jnp.zeros((n_layers, d_row), F32)
                for xx in RINGS:
                    for cc in BOTH:
                        tot += r.gbuf[xx, cc, yy, zz, :n_layers].astype(F32)
                at = (zz * RING + yy) * d_row
                r.gain[:, at:at + d_row] = tot

    tok_pair = CORES * rows

    def x_z(k):
        zz = turn(z, OTHERS[k])
        src = r.xt.at[pl.ds(zz * seqs, seqs)]
        return remote(src, r.xz.at[z], r.xz_send.at[k], r.xz_recv.at[k], (zz, y, x, c))

    def x_own():
        return pltpu.make_async_copy(r.xt.at[pl.ds(z * seqs, seqs)], r.xz.at[z], r.x_loc)

    def pos(xx):
        return pl.ds(pl.multiple_of(xx * tok_pair, tok_pair), tok_pair)

    def x_plane(oy, ox):
        yy, xx = turn(y, oy), turn(x, ox)
        return remote(r.xz.at[:, yy, :, pos(xx)], r.xp.at[c, y, x], r.xp_send.at[oy], r.xp_recv.at[(RING - oy) % RING], (z, yy, xx, c))

    def row_bytes(oy):
        return r.xp.at[c, 0] if oy else r.xp.at[c, 0, pl.ds(0, RING - 1)]

    def x_row(oy):
        yy = turn(y, oy)
        got = row_bytes(oy)
        remote(got, got, r.xp_send.at[oy], r.xp_recv.at[oy], partner).wait_recv()
        row = r.xp.at[c, yy]
        remote(row, row, r.xd_send.at[oy], r.xd_recv.at[oy], partner).start()

    def x_turn():
        for oy in RINGS:
            row = r.xp.at[1 - c, turn(y, oy)]
            remote(row, row, r.xd_send.at[oy], r.xd_recv.at[oy], partner).wait_recv()

        @pl.loop(0, RING)
        def _(zz):
            for yy in RINGS:
                for xh in BOTH:
                    blk = [r.xp[cc, yy, CORES * xh + xx, zz] for xx in BOTH for cc in BOTH]
                    blk = jnp.concatenate(blk, axis=0).astype(F32).T.astype(BF)
                    n = blk.shape[1]
                    at = pl.multiple_of(zz * RING * d_row + yy * d_row + xh * n, n)
                    r.hb[0, 0, :, :, pl.ds(at, n)] = blk.reshape(CORES, rows, n)
        r.hid[...] = r.hb[0, 0, c]
        for oy in RINGS:
            row = r.xp.at[c, turn(y, oy)]
            remote(row, row, r.xd_send.at[oy], r.xd_recv.at[oy], partner).wait_send()

    def x_sent():
        for fn in (x_z, gain_z, gain_y, gain_x):
            peers_of(fn, "wait_send")
        for k in RINGS:
            gain_die(x, k).wait_send()
        for oy in RINGS:
            got = row_bytes(oy)
            remote(got, got, r.xp_send.at[oy], r.xp_recv.at[oy], partner).wait_send()

    def y_die(p):
        cols = pl.ds(pl.multiple_of(turn(z, p) * width, width), width)
        return remote(r.hid.at[:, cols], r.hb.at[0, 0, c, :, cols], r.yd_send.at[p], r.yd_recv.at[p], partner)

    def planes(h):
        return pl.ds(2 * h, 2)

    def y_plane(h, oy, ox):
        yy, xx = turn(y, oy), turn(x, ox)
        return remote(r.xp.at[c, yy, xx, planes(h)], r.xz.at[planes(h), y, :, pos(x)], r.yp_send.at[h, oy], r.yp_recv.at[h, (RING - oy) % RING],
                      (z, yy, xx, c))

    def y_z(p, oy):
        s = turn(y, oy)
        return remote(r.xz.at[p, s], r.y_out.at[z * seqs + s], r.yz_send.at[p, oy], r.yz_recv.at[p, oy], (turn(z, p), y, x, c))

    def y_own(oy):
        s = turn(y, oy)
        return pltpu.make_async_copy(r.xz.at[0, s], r.y_out.at[z * seqs + s], r.y_loc.at[oy])

    def leave_a(h):
        for p in BOTH:
            p = 2 * h + p
            y_die(p).start()
            cols = pl.ds(pl.multiple_of(turn(z, p) * width, width), width)
            r.hb[0, 0, c, :, cols] = r.hid[:, cols]

    def leave_b(h):
        n = CORES * CORES * d_local
        for p in BOTH:
            p = 2 * h + p
            y_die(p).wait()

            @pl.loop(0, RING)
            def _(yy, p=p):
                for xh in BOTH:
                    at = pl.multiple_of(turn(z, p) * width + yy * d_row + xh * n, n)
                    blk = r.hb[0, 0, :, :, pl.ds(at, n)].reshape(tok_pair, n).astype(F32).T.astype(BF)
                    for xx in BOTH:
                        for cc in BOTH:
                            lo = (xx * CORES + cc) * d_local
                            r.xp[cc, yy, CORES * xh + xx, p] = blk[lo:lo + d_local]

        for oy in OTHERS + (0,):
            for ox in RINGS:
                if oy or ox:
                    y_plane(h, oy, ox).start()
        for p in BOTH:
            p = 2 * h + p
            r.xz[p, y, :, pos(x)] = r.xp[c, y, x, p]

    def plane_bytes(h, oy):
        return r.xp.at[c, 0, :, planes(h)] if oy else r.xp.at[c, 0, pl.ds(0, LAST), planes(h)]

    def leave_c(h):
        for oy in OTHERS + (0,):
            got = plane_bytes(h, oy)
            remote(got, got, r.yp_send.at[h, oy], r.yp_recv.at[h, oy], partner).wait_recv()
            for p in BOTH:
                p = 2 * h + p
                (y_z(p, oy) if p else y_own(oy)).start()

    def left():
        for oy in RINGS:
            for h in BOTH:
                got = plane_bytes(h, oy)
                remote(got, got, r.yp_send.at[h, oy], r.yp_recv.at[h, oy], partner).wait_send()
            for p in RINGS:
                (y_z(p, oy) if p else y_own(oy)).wait()

    def kv_rows(zz):
        n = CORES * seq_len // (RING * RING * RING * CORES)
        return pl.ds(pl.multiple_of(((zz * RING + y) * RING + x) * n, n), n)

    def kv_trade(l, k):
        zz = turn(z, OTHERS[k])
        return remote(r.kv_out.at[l, :, :, kv_rows(zz)], r.kvx.at[l, z], r.kvx_send.at[l, k], r.kvx_recv.at[l, k], (zz, y, x, c))

    def kv_keep(l):
        return pltpu.make_async_copy(r.kv_out.at[l, :, :, kv_rows(z)], r.kvx.at[l, z], r.kvx_loc.at[l])

    def kv_share(l):
        for k in range(len(OTHERS)):
            kv_trade(l, k).start()
        kv_keep(l).start()

    def kv_shared(l):
        for k in range(len(OTHERS)):
            kv_trade(l, k).wait()
        kv_keep(l).wait()

    def gather_norm(l, split, pump):
        hid = r.hid
        gain = r.gain[l:l + 1, :]
        for b in range(4):
            blk = hid[b * quarter:(b + 1) * quarter, :].astype(F32)
            mean = jnp.mean(blk, axis=-1, keepdims=True)
            cen = blk - mean
            var = jnp.mean(cen * cen, axis=-1, keepdims=True)
            r.h_ref[b * quarter:(b + 1) * quarter, :] = (cen * lax.rsqrt(var + LN_EPS) * gain).astype(BF)
        out = r.h_all.at[l]

        def spot(q, first, second):
            if q == 0:
                return turn(y, second), turn(x, first)
            return turn(y, first), turn(x, second)

        def span(q, part):
            lo, n = (split, rows - split) if q else (0, split)
            if part is NIL:
                return pl.ds(lo, n)
            return pl.ds(lo + part * (n // 2), n // 2)

        table = {}

        def link(key, *args, own=False):
            idx, (q, first, second, part, to_first, to_second) = table.setdefault(key, (len(table), args))
            sy, sx = spot(q, first, second)
            ty, tx = spot(q, to_first, to_second)
            rws = span(q, part)
            dst = out.at[sy, sx, c, rws]
            return remote(r.h_ref.at[rws] if own else dst, dst, r.ag_send.at[l, KINDS.index(key[0])], r.ag_recv.at[l, idx], (z, ty, tx, c))

        def arrived(*key):
            for d in BOTH:
                link((*key, d)).wait_recv()

        def die(q, first, second, own=False):
            sy, sx = spot(q, first, second)
            rws = span(q, NIL)
            dst = out.at[sy, sx, c, rws]
            off = (first if q else second) % RING
            remote(r.h_ref.at[rws] if own else dst, dst, r.ag_dsend.at[l], r.ag_drecv.at[l, off], partner).start()

        offs = (0, -1, 1, 2)

        def second_step(k):
            for d in BOTH:
                for q in BOTH:
                    link(("second", q, k, d)).wait_recv()
                    src = -SIGN[d]
                    link(("second_on", q, k, d), q, offs[k], src, d, 0, SIGN[d]).start()
                    die(q, offs[k], src)

        def last_step(q, k):
            arrived("second_on", q, k)
            die(q, offs[k], 2)

        def tail_a():
            for k in RINGS[2:]:
                second_step(k)
                hook(pump, f"k{k}")
            for k in (1, 2):
                last_step(1, k)

        def tail_b():
            for k in RINGS:
                last_step(0, k)
            last_step(1, LAST)

        for q in BOTH:
            for d in BOTH:
                link(("first", q, d), q, 0, 0, NIL, SIGN[d], 0, own=True).start()
        for q in BOTH:
            for d in BOTH:
                link(("second", q, 0, d), q, 0, 0, NIL, 0, SIGN[d], own=True).start()
        for q in BOTH:
            die(q, 0, 0, own=True)
        own = pltpu.make_async_copy(r.h_ref, out.at[y, x, c], r.ag_loc)
        own.start()
        hook(pump, "begin")
        for d in BOTH:
            for q in BOTH:
                link(("first", q, d)).wait_recv()
                src = -SIGN[d]
                link(("first_on", q, d), q, src, 0, d, SIGN[d], 0).start()
                die(q, src, 0)
        hook(pump, "first")
        second_step(0)
        for q in reversed(BOTH):
            for d in BOTH:
                for e in BOTH:
                    link(("second", q, 1 + d, e), q, -SIGN[d], 0, NIL, 0, SIGN[e]).start()
        hook(pump, "k0")
        for q in BOTH:
            arrived("first_on", q)
            for e in BOTH:
                link(("second", q, LAST, e), q, 2, 0, NIL, 0, SIGN[e]).start()
            die(q, 2, 0)
        hook(pump, "first_on")
        last_step(1, 0)
        own.wait()
        hook(pump, "ready")

        def crossed(off):
            got = out.at[turn(y, off), :, 1 - c]
            remote(got, got, r.ag_dsend.at[l], r.ag_drecv.at[l, off], partner).wait_recv()

        def order(i):
            return lax.rem(3 * i + 3 * (i // 2) + 2 * (i // 3), RING)

        def fetch(i, slot):
            off = order(i)
            crossed(off)
            h_copy(l, turn(y, off), slot).start()

        def up_ready():
            hook(pump, "up")
            loaded(UP1 if l else UP0)

        crossed(0)
        h_copy(l, y, 0).start()

        def opening():
            second_step(1)
            hook(pump, "k1")

        if l:
            @pl.loop(0, RING)
            def _(i):
                slot = lax.rem(i, 2)
                s = turn(y, order(i))
                h_copy(l, s, slot).wait()
                pump(("seq", i))
                one(l, s, slot, i)

                @pl.when(i == 0)
                def _():
                    opening()
                    up_ready()

                pump(("two", i))
                two(s, slot)

                @pl.when(i == 0)
                def _():
                    tail_a()
                    fetch(i + 1, 1 - slot)
                    fetch(i + 2, slot)

                @pl.when(i == 1)
                def _():
                    tail_b()
                    fetch(i + 2, slot)
        else:
            h_copy(l, y, 0).wait()
            hook(pump, "own")
            one(l, y, 0, 0)
            opening()
            tail_a()
            crossed(LAST)
            h_copy(l, turn(y, LAST), 1).start()

            @pl.loop(1, RING)
            def _(i):
                slot = lax.rem(i, 2)
                s = turn(y, order(i))
                h_copy(l, s, slot).wait()
                pump(("seq", i))
                one(l, s, slot, i)

                @pl.when(i == 1)
                def _():
                    up_ready()

                pump(("two", i - 1))
                two(turn(y, order(i - 1)), 1 - slot)

                @pl.when(i == 1)
                def _():
                    tail_b()

                @pl.when(i < LAST)
                def _():
                    fetch(i + 1, 1 - slot)

            hook(pump, "two3")
            two(turn(y, 2), 1)

        for slot in BOTH:
            for i in BOTH:
                kv_out_copy(l, 0, slot, i).wait()
        sent = (out.at[y, x], out.at[y], out.at[y, x, c], out.at[y, pl.ds(0, CORES)])
        for kind, ref in enumerate(sent):
            remote(ref, ref, r.ag_send.at[l, kind], r.ag_recv.at[l, kind], partner).wait_send()
        remote(out.at[pl.ds(0, 2)], out.at[pl.ds(0, 2)], r.ag_dsend.at[l], r.ag_drecv.at[l, 0], partner).wait_send()

    def h_copy(l, s, slot):
        return pltpu.make_async_copy(r.h_all.at[l, s], r.hb.at[slot], r.h_sem.at[slot])

    def h_tile(slot):
        return r.hb[slot].reshape(seq_len, d_model)

    def project(h, lo, n):
        w = r.wv[:, :, lo:lo + n].reshape(d_model, n)
        return jnp.dot(h, w, preferred_element_type=F32).astype(BF)

    def rope(val):
        val = val.astype(F32)
        return val * r.cos[...] + pltpu.roll(val, head_dim // 2, 1) * r.sin[...]

    n_chunk = min(256, f_loc)

    def kv_out_copy(l, s, slot, i):
        return pltpu.make_async_copy(r.qkv.at[slot, i], r.kv_out.at[l, i, s], r.kvo_sem.at[slot, i])

    def one(l, s, slot, i):
        @pl.when(i >= 2)
        def _():
            for k in BOTH:
                kv_out_copy(l, s, slot, k).wait()

        kv = jnp.zeros((seq_len, 2 * head_dim), F32)
        for zz in RINGS:
            for yy in RINGS:
                col = (zz * RING + yy) * d_row
                kv += lax.dot_general(h_cols(slot, col, d_row), r.kvb[yy, zz], (((1,), (1,)), ((), ())), preferred_element_type=F32)
        kv = kv.astype(BF)
        r.qkv[slot, 0] = rope(kv[:, :head_dim]).astype(BF)
        r.qkv[slot, 1] = kv[:, head_dim:]
        for i in BOTH:
            kv_out_copy(l, s, slot, i).start()
        q = project(h_tile(slot), 0, head_dim)
        r.stage[...] = (rope(q) * head_dim ** -0.5).astype(BF)
        for lo in range(0, f_loc, n_chunk):
            r.joined[s, :, head_dim + lo:head_dim + lo + n_chunk] = project(h_tile(slot), head_dim + lo, n_chunk)
        n_tile = seq_len // 2
        for i in BOTH:
            keys = (i + 1) * n_tile
            sc = lax.dot_general(r.stage[i * n_tile:(i + 1) * n_tile, :], r.qkv[slot, 0, :keys, :], (((1,), (1,)), ((), ())), preferred_element_type=F32)
            row_id = lax.broadcasted_iota(jnp.int32, sc.shape, 0) + i * n_tile
            col_id = lax.broadcasted_iota(jnp.int32, sc.shape, 1)
            sc = jnp.where(col_id <= row_id, sc, -1e30)
            top = jnp.max(sc, axis=-1, keepdims=True)
            ex = jnp.exp(sc - top)
            prob = (ex * (1.0 / jnp.sum(ex, axis=-1, keepdims=True))).astype(BF)
            att = jnp.dot(prob, r.qkv[slot, 1, :keys, :], preferred_element_type=F32)
            r.joined[s, i * n_tile:(i + 1) * n_tile, :head_dim] = att.astype(BF)

    def h_cols(slot, col, n):
        return r.hb[slot, :, :, :, col:col + n].reshape(seq_len, n)

    def two(s, slot):
        for lo in range(0, f_loc, n_chunk):
            up = project(h_tile(slot), head_dim + f_loc + lo, n_chunk).astype(F32)
            cols = slice(head_dim + lo, head_dim + lo + n_chunk)
            g = r.joined[s, :, cols].astype(F32)
            r.joined[s, :, cols] = (g * jax.nn.sigmoid(g) * up).astype(BF)

    def out_scatter(l, pump):
        def peer(q, first, second):
            dy = first * (1 - q) + second * q
            dx = first * q + second * (1 - q)
            return (z, turn(y, dy), turn(x, dx), c)

        def die_copy(ch, q, s):
            return remote(r.away.at[q], r.die_in.at[ch, q, s], r.dsend.at[l, ch, q, s], r.drecv.at[l, ch, q, s], partner)

        def first_copy(ch, q, d):
            return remote(r.acc.at[ch, q, 0, pl.ds(CORES * d, CORES)], r.in1.at[ch, q, d], r.send1.at[l, ch, q, d], r.recv1.at[l, ch, q, d],
                          peer(q, SIGN[d], 0))

        def second_copy(ch, q, d, h):
            js = pl.ds(CORES * h, CORES)
            return remote(r.acc.at[ch, q, 1 + d, js], r.in2.at[ch, q, d, js], r.send2.at[l, ch, q, d, h], r.recv2.at[l, ch, q, d, h],
                          peer(q, SIGN[d], 0))

        def half_rows(d):
            return pl.ds(d * (rows // 2), rows // 2)

        def third_copy(ch, q, d):
            return remote(r.acc.at[ch, q, LAST, 0, half_rows(d)], r.in3.at[ch, q, d], r.send3.at[l, ch, q, d], r.recv3.at[l, ch, q, d],
                          peer(q, 0, SIGN[d]))

        def fourth_copy(ch, q, d):
            return remote(r.acc.at[ch, q, LAST, 1 + d], r.in4.at[ch, q, d], r.send4.at[l, ch, q, d], r.recv4.at[l, ch, q, d],
                          peer(q, 0, SIGN[d]))

        n_blk = r.wov.shape[3]

        def plane_of(ch, q):
            if l:
                return turn(z, q if ch else 2 + q)
            return turn(z, LAST - q if ch else q)

        def slot_off(s):
            return lax.rem(2 + 3 * s + 3 * (s // 2) + 2 * (s // 3), RING)

        def tile(ch, q, s):
            off = slot_off(s)
            for cc in BOTH:
                for j in RINGS:
                    oy = off * (1 - q) + SLOT_OFF[j] * q
                    ox = SLOT_OFF[j] * (1 - q) + off * q
                    core = c if cc else 1 - c
                    at = pl.multiple_of((turn(x, ox) * CORES + core) * rows, rows)
                    r.lhs[pl.ds((cc * RING + j) * rows, rows), :] = r.joined[turn(y, oy), pl.ds(at, rows), :]
            left = r.lhs[...]
            zz = plane_of(ch, q)
            for n in RINGS:
                res = jnp.dot(left, r.wov[zz, n], preferred_element_type=F32).astype(BF)
                res = res.reshape(CORES, RING, rows, n_blk)
                r.away[q, :, :, n * n_blk:(n + 1) * n_blk] = res[0]
                r.acc[ch, q, s, :, :, n * n_blk:(n + 1) * n_blk] = res[1]

        def pair_sum(ch, q, s):
            die_copy(ch, q, s).wait_recv()

            @pl.loop(0, RING)
            def _(j):
                r.acc[ch, q, s, j] = r.acc[ch, q, s, j] + r.die_in[ch, q, s, j]

        def stage_a(ch):
            @pl.loop(0, CORES * RING)
            def _(t):
                s = t // CORES
                q = lax.rem(t, CORES)

                @pl.when(s >= 1)
                def _():
                    die_copy(ch, q, s - 1).wait_send()

                if ch:
                    @pl.when(s == 0)
                    def _():
                        die_copy(ch - 1, q, LAST).wait_send()

                tile(ch, q, s)
                die_copy(ch, q, s).start()

                @pl.when(s >= 1)
                def _():
                    pair_sum(ch, q, s - 1)

                @pl.when(s == 1)
                def _():
                    for d in BOTH:
                        first_copy(ch, q, d).start()

                for d in BOTH:
                    @pl.when(s == 2 + d)
                    def _(d=d):
                        second_copy(ch, q, d, 1 - d).start()

                for n in RINGS:
                    name = f"a{ch}s{n}"
                    if pump(name, False):
                        @pl.when(t == CORES * n + 1)
                        def _(name=name):
                            hook(pump, name)

        def stage_b(ch):
            for q in BOTH:
                pair_sum(ch, q, LAST)
            for q in BOTH:
                for d in BOTH:
                    first_copy(ch, q, d).wait_recv()
                    for j in BOTH:
                        at = CORES * d + j
                        r.acc[ch, q, 1 + d, at] = r.acc[ch, q, 1 + d, at] + r.in1[ch, q, d, j]
                    second_copy(ch, q, d, d).start()

        def total(ch, q, j):
            val = r.acc[ch, q, LAST, j].astype(F32)
            for d in BOTH:
                val += r.in2[ch, q, d, j].astype(F32)
            r.acc[ch, q, LAST, j] = val.astype(BF)

        def stage_c(ch):
            for q in BOTH:
                for h in BOTH:
                    for d in BOTH:
                        second_copy(ch, q, d, h).wait_recv()
                total(ch, q, 0)
                for d in BOTH:
                    third_copy(ch, q, d).start()
                for j in RINGS[1:]:
                    total(ch, q, j)

        def stage_d(ch):
            for q in BOTH:
                for d in BOTH:
                    third_copy(ch, q, d).wait_recv()
                    rws = half_rows(d)
                    r.acc[ch, q, LAST, 1 + d, rws] = r.acc[ch, q, LAST, 1 + d, rws] + r.in3[ch, q, d]
                    fourth_copy(ch, q, d).start()

        def stage_e(ch):
            for q in BOTH:
                for d in BOTH:
                    fourth_copy(ch, q, d).wait_recv()
                cols = pl.ds(pl.multiple_of(plane_of(ch, q) * width, width), width)
                upd = r.acc[ch, q, LAST, LAST].astype(F32)
                for d in BOTH:
                    upd += r.in4[ch, q, d].astype(F32)
                upd = upd.astype(BF)
                r.hid[:, cols] = (r.hid[:, cols].astype(F32) + upd.astype(F32)).astype(BF)

        def sent(ch):
            for q in BOTH:
                if ch:
                    die_copy(ch, q, LAST).wait_send()
                for d in BOTH:
                    for cp in (first_copy, third_copy, fourth_copy):
                        cp(ch, q, d).wait_send()
                    for h in BOTH:
                        second_copy(ch, q, d, h).wait_send()

        stages = {"a": stage_a, "b": stage_b, "c": stage_c, "d": stage_d, "e": stage_e, "f": leave_a, "g": leave_b, "h": leave_c}
        for step in LAST_ORDER if l else FIRST_ORDER:
            with jax.named_scope(step):
                stages[step[0]](int(step[1]))
            hook(pump, step)
        for ch in BOTH:
            sent(ch)

    def near(fn, t):
        for j in (LAST, 1):
            fn(t, j)

    def far(fn, t):
        fn(t, 2)

    def z_all(t):
        near(z_direct, t)
        far(z_direct, t)

    def peers_of(fn, op="start"):
        for k in range(len(OTHERS)):
            getattr(fn(k), op)()

    def start(pump):
        peers_of(gain_z)
        kv_z()
        peers_of(x_z)
        x_own().start()
        pump("s0")
        with jax.named_scope("gain_a"):
            peers_of(gain_z, "wait_recv")
            peers_of(gain_y)
            kv_y1()
        pump("s1")
        with jax.named_scope("gain_b"):
            peers_of(gain_y, "wait_recv")
            peers_of(gain_x)
            gain_die(x, LAST).start()
        pump("s2")
        with jax.named_scope("x_z"):
            peers_of(x_z, "wait_recv")
            x_own().wait()
        for oy in RINGS:
            for ox in RINGS:
                if oy or ox:
                    x_plane(oy, ox).start()
        r.xp[c, y, x] = r.xz[:, y, :, pos(x)]
        pump("s3")
        with jax.named_scope("kv_b"):
            kv_y2()
        with jax.named_scope("gain_c"):
            for k, o in enumerate(OTHERS):
                gain_x(k).wait_recv()
                gain_die(turn(x, -o), k).start()
        pump("s4")
        for oy in (OWN, BEFORE, AFTER, FAR):
            with jax.named_scope(f"row_{oy}"):
                x_row(oy)
            pump(f"r{oy}")
        pump("s5")
        kv_y3()
        pump("s6")
        with jax.named_scope("gain_sum"):
            for k in RINGS:
                gain_die(x, k).wait_recv()
            gain_sum()
        with jax.named_scope("turn"):
            x_turn()
        pump("s7")

    def when(i, n, *fns):
        @pl.when(i == n)
        def _():
            for fn in fns:
                fn()

    def plan(steps):
        def pump(step, run=True):
            if not isinstance(step, str):
                for n in RINGS:
                    if (step[0], n) in steps:
                        when(step[1], n, lambda n=n: run_steps(steps[step[0], n]))
                return True
            found = steps.get(step, ())
            if run:
                run_steps(found)
            return found
        return pump

    def run_steps(steps):
        for fn, *args in steps:
            with jax.named_scope(f"{fn.__name__}_{args[-1] if args else 0}"):
                fn(*args)

    first_entry = plan({
        "s0": [(z_own, QG0), (z_own, UP0)],
        "r0": [(y_send, QG0)],
        "r3": [(z_forward, QG0, OWN)],
        "s5": [(z_forward, UP0, OWN), (y_relay, QG0)],
        "s6": [(kv_x1, 0)],
    })
    first_front = plan({
        "begin": [(kv_x2, 0), (z_direct, QG0, BEFORE), (z_direct, QG0, AFTER)],
        "first": [(z_direct, QG0, FAR), (y_send, UP0), (z_forward, QG0, BEFORE)],
        "k0": [(kv_x3, 0)],
        "first_on": [(z_forward, QG0, AFTER)],
        "ready": [
            (y_relay, UP0), (z_forward, QG0, FAR), (z_direct, UP0, BEFORE), (load_near, QG0), (load_far, QG0), (kv_load, 0), (loaded, QG0),
            (kv_loaded,),
        ],
        "own": [(z_direct, UP0, AFTER), (y_send, WO0)],
        "k1": [(z_forward, UP0, BEFORE), (z_direct, UP0, FAR), (y_relay, WO0)],
        "k3": [(z_forward, UP0, AFTER)],
        ("seq", 1): [(z_forward, UP0, FAR), (z_direct, WO0, BEFORE), (y_send, QG1), (x_sent,)],
        "up": [(z_direct, WO0, AFTER), (y_relay, QG1), (load_near, UP0), (load_far, UP0)],
        ("two", 0): [(y_send, UP1), (z_direct, WO0, FAR)],
        ("seq", 2): [(z_forward, WO0, BEFORE)],
        ("two", 1): [(z_own, WO0), (y_send, WO1)],
        ("seq", 3): [(z_forward, WO0, AFTER), (y_relay, UP1)],
        ("two", 2): [(z_forward, WO0, FAR), (kv_x1, 1)],
        "two3": [(z_own, QG1), (y_relay, WO1)],
        "near": [(z_forward, WO0, OWN), (load_near, WO0)],
    })
    first_scatter = plan({
        "a0s0": [(kv_x2, 1)],
        "a0s2": [(z_direct, QG1, BEFORE)],
        "a0": [(z_own, UP1), (kv_x3, 1)],
        "b0": [(z_forward, QG1, OWN), (load_far, WO0), (far_loaded, WO0)],
        "a1s1": [(z_direct, QG1, AFTER)],
        "a1s2": [(z_forward, QG1, BEFORE)],
        "a1": [(z_forward, UP1, OWN)],
        "c1": [(z_forward, QG1, AFTER), (z_direct, QG1, FAR)],
        "e0": [(z_direct, UP1, BEFORE)],
    })
    second_front = plan({
        "begin": [(z_direct, UP1, AFTER), (kv_load, 1)],
        "first": [(z_forward, QG1, FAR), (z_direct, UP1, FAR)],
        "k0": [(z_forward, UP1, BEFORE), (z_forward, UP1, AFTER)],
        "ready": [(load_near, QG1), (load_far, QG1), (loaded, QG1), (kv_loaded,)],
        ("seq", 0): [(z_forward, UP1, FAR), (z_direct, WO1, BEFORE)],
        "k1": [(z_direct, WO1, AFTER)],
        "up": [(load_near, UP1), (load_far, UP1)],
        "k2": [(z_direct, WO1, FAR)],
        "k3": [(z_forward, WO1, BEFORE), (z_own, WO1)],
        ("two", 1): [(z_forward, WO1, AFTER)],
        ("seq", 2): [(z_forward, WO1, FAR)],
        ("seq", 3): [(z_forward, WO1, OWN)],
        "near": [(load_near, WO1), (load_far, WO1)],
    })
    second_scatter = plan({
    })

    with jax.named_scope("start"):
        start(first_entry)
    with jax.named_scope("front_0"):
        gather_norm(0, rows // RING, first_front)
    with jax.named_scope("near_0"):
        kv_share(0)
        first_front("near")
        near_loaded(WO0)
    with jax.named_scope("scatter_0"):
        out_scatter(0, first_scatter)
    with jax.named_scope("front_1"):
        gather_norm(1, rows // 2, second_front)
    with jax.named_scope("near_1"):
        kv_share(1)
        second_front("near")
        loaded(WO1)
    with jax.named_scope("scatter_1"):
        out_scatter(1, second_scatter)
    with jax.named_scope("drain"):
        left()
        for t in range(WO1 + 1):
            drain(t)
        for l in range(n_layers):
            kv_shared(l)
            kv_sent(l)


def run_model(xt, gain, wkv_t, w_in, w_out, cos_full, sin_full):
    batch, d_local, seq_len = xt.shape
    n_layers, d_row, e_block = w_in.shape
    r_block, d_col = w_out.shape[1:]
    head_dim = cos_full.shape[1]
    d_model = d_row * RING * RING
    seqs = batch // RING
    rows = seqs * seq_len // (RING * RING * CORES)
    e_loc, r_loc = e_block // RING, r_block // RING
    kc = wkv_t.shape[1]
    width = d_model // RING
    n_t = 3 * n_layers
    n_o = len(OTHERS)

    def dma(*shape):
        return pltpu.SemaphoreType.DMA(shape)

    def vm(*shape):
        return pltpu.VMEM(shape, BF)

    def out(*shape):
        return jax.ShapeDtypeStruct(shape, BF)

    any_spec = pl.BlockSpec(memory_space=pl.ANY)
    vm_spec = pl.BlockSpec(memory_space=pltpu.VMEM)
    out_shape = [
        out(batch, d_local, seq_len),
        out(n_layers, 2, seqs, seq_len, head_dim),
        out(n_layers, RING, RING, CORES, rows, d_model),
        out(n_layers, RING, RING * d_row, e_loc),
        out(n_layers, RING, RING, r_loc, d_col),
        out(RING, CORES, n_layers, RING, RING, kc, d_row),
        out(n_layers, RING, 2, seqs, CORES * (seq_len // (CORES * RING * RING * RING)), head_dim),
        out(n_layers, 2, d_row // 2, e_loc),
        out(n_layers, 2, r_loc // 2, d_col),
    ]
    pair = (2, 2, 2)
    each = (n_layers, *pair)
    scratch = [
        vm(rows, d_model), vm(rows, d_model), pltpu.VMEM((n_layers, d_model), F32),
        vm(RING, CORES, RING, RING, G_ROWS, d_row),
        vm(RING, seqs, d_local, seq_len),
        vm(CORES, RING, RING, RING, d_local, CORES * rows),
        vm(RING, RING * d_row, e_loc), vm(RING, RING, 2 * head_dim, d_row), vm(RING, RING, r_loc, d_col),
        vm(2, RING, CORES, rows, d_model), vm(RING, seq_len, r_loc), vm(2, 2, seq_len, head_dim), vm(seq_len, head_dim),
        vm(CORES * RING * rows, r_loc), vm(2, RING, rows, width), vm(2, 2, RING, RING, rows, width), vm(2, 2, RING, RING, rows, width),
        vm(*pair, 2, rows, width), vm(*pair, RING, rows, width), vm(*pair, rows // 2, width), vm(*pair, rows, width),
        dma(n_o), dma(n_o), dma(RING), dma(RING), dma(RING), dma(RING), pltpu.SemaphoreType.DMA,
        dma(3 * n_o), dma(3 * n_o), dma(RING), dma(RING),
        dma(RING), dma(RING), dma(2, RING), dma(2, RING), dma(RING, RING), dma(RING, RING), dma(RING),
        dma(n_layers, RING), dma(n_layers, 40), dma(n_layers), dma(n_layers, RING), pltpu.SemaphoreType.DMA, dma(2), dma(2, 2), dma(3), dma(3),
        dma(n_t, RING), dma(n_t, 2), dma(n_t, RING, 2), dma(n_t, RING, 2), dma(n_t, RING),
        dma(n_o), dma(n_o), pltpu.SemaphoreType.DMA, dma(n_o), dma(n_layers), dma(n_layers, n_o), dma(n_layers), dma(n_layers), dma(2),
        dma(n_layers, 2, 2, RING), dma(n_layers, 2, 2, RING),
        dma(*each), dma(*each), dma(*each, 2), dma(*each, 2), dma(*each), dma(*each), dma(*each), dma(*each),
        dma(n_layers, n_o), dma(n_layers, n_o), dma(n_layers),
    ]
    res = pl.pallas_call(
        model_kernel,
        out_shape=out_shape,
        in_specs=[any_spec, vm_spec, vm_spec, any_spec, any_spec, vm_spec, vm_spec],
        out_specs=[any_spec] * len(out_shape),
        scratch_shapes=scratch,
        compiler_params=pltpu.CompilerParams(collective_id=0, has_side_effects=True, vmem_limit_bytes=VMEM_LIMIT),
        name="two_layers",
    )(xt, gain, wkv_t, w_in, w_out, cos_full, sin_full)
    return res[0], res[6]


def solution(mesh):
    row_size = mesh.shape["row"]
    n_col = mesh.shape["col"]
    n_z = row_size // RING
    n_y = RING
    n_x = n_col // CORES
    n_tp = n_y * n_col
    n_dev = row_size * n_col
    mesh4 = Mesh(mesh.devices.reshape(n_z, n_y, n_x, CORES), ("z", "y", "x", "core"))
    every = ("z", "y", "x", "core")
    col = ("x", "core")
    act_spec = P(NIL, NIL, every)
    w_spec = P(NIL, ("z", "y"), col)

    def device_fn(x_loc, gain_loc, w_in_loc, w_kv_loc, w_out_loc):
        n_layers = w_in_loc.shape[0]
        n_batch, seq_len, d_local = x_loc.shape
        head_dim = w_kv_loc.shape[2] * n_col // 2
        batch_loc = n_batch // n_z
        seq_local = seq_len // n_dev
        steps = np.arange(head_dim // 2, dtype=np.float32)
        inv_freq = (1.0 / 10000.0 ** (steps * 2 / head_dim)).astype(np.float32)
        angles = np.arange(seq_len, dtype=np.float32)[:, NIL] * inv_freq[NIL, :]
        cos_tab, sin_tab = np.cos(angles), np.sin(angles)
        cos_full = jnp.asarray(np.concatenate([cos_tab, cos_tab], axis=1))
        sin_full = jnp.asarray(np.concatenate([-sin_tab, sin_tab], axis=1))
        y_loc, kv = run_model(x_loc.transpose(0, 2, 1), gain_loc, w_kv_loc.transpose(0, 2, 1), w_in_loc, w_out_loc, cos_full, sin_full)
        y_loc = y_loc.transpose(0, 2, 1)
        kv = kv.reshape(n_layers, n_z, 2, batch_loc, CORES, seq_local, head_dim)
        kv = lax.dynamic_index_in_dim(kv, lax.axis_index("core"), axis=4, keepdims=False)
        kv = kv.transpose(0, 2, 1, 3, 4, 5).reshape(n_layers, 2, n_batch, seq_local, head_dim)
        return y_loc, kv

    return jax.shard_map(device_fn, mesh=mesh4, in_specs=(act_spec, P(NIL, every), w_spec, w_spec, P(NIL, col, ("z", "y"))), out_specs=(act_spec, P(NIL, NIL, NIL, every, NIL)), check_vma=False)
```

```python
import typing

import jax
import jax.numpy as jnp
import numpy as np
from jax import lax
from jax.experimental import pallas as pl
from jax.experimental.pallas import tpu as pltpu
from jax.sharding import Mesh
from jax.sharding import PartitionSpec as P

LN_EPS = 1e-6
RING = 4
CORES = 2
VMEM_LIMIT = 67_000_000
BF = jnp.bfloat16
F32 = jnp.float32
SLOT_OFF = (2, 1, 3, 0)
SIGN = (1, -1)
NIL = None
BOTH = range(CORES)
RINGS = range(RING)
OTHERS = (1, 3, 2)
LAST = RING - 1
G_ROWS = 8
H_SLOTS = 3
QG0, UP0, WO0, QG1, UP1, WO1 = range(6)
OWN, AFTER, FAR, BEFORE = RINGS
FIRST_ORDER = ("a0", "b0", "a1", "b1", "c0", "c1", "d0", "d1", "e0", "e1")
LAST_ORDER = FIRST_ORDER[:-1] + ("f1", "e1", "g1", "f0", "g0", "h1", "h0")
KINDS = ("first", "second", "first_on", "second_on")


class Refs(typing.NamedTuple):
    xt: typing.Any
    gain_in: typing.Any
    wkv: typing.Any
    w_in: typing.Any
    w_out: typing.Any
    cos: typing.Any
    sin: typing.Any
    y_out: typing.Any
    kv_out: typing.Any
    h_all: typing.Any
    wi: typing.Any
    wo: typing.Any
    kvh: typing.Any
    kvx: typing.Any
    rwi: typing.Any
    rwo: typing.Any
    h_ref: typing.Any
    hid: typing.Any
    gain: typing.Any
    gbuf: typing.Any
    xz: typing.Any
    xp: typing.Any
    wv: typing.Any
    kvb: typing.Any
    wov: typing.Any
    hb: typing.Any
    joined: typing.Any
    qkv: typing.Any
    stage: typing.Any
    lhs: typing.Any
    away: typing.Any
    acc: typing.Any
    die_in: typing.Any
    in1: typing.Any
    in2: typing.Any
    in3: typing.Any
    in4: typing.Any
    xz_send: typing.Any
    xz_recv: typing.Any
    xp_send: typing.Any
    xp_recv: typing.Any
    xd_send: typing.Any
    xd_recv: typing.Any
    x_loc: typing.Any
    g_send: typing.Any
    g_recv: typing.Any
    gd_send: typing.Any
    gd_recv: typing.Any
    yd_send: typing.Any
    yd_recv: typing.Any
    yp_send: typing.Any
    yp_recv: typing.Any
    yz_send: typing.Any
    yz_recv: typing.Any
    y_loc: typing.Any
    ag_send: typing.Any
    ag_recv: typing.Any
    ag_dsend: typing.Any
    ag_drecv: typing.Any
    ag_loc: typing.Any
    h_sem: typing.Any
    kvo_sem: typing.Any
    w_load: typing.Any
    far_load: typing.Any
    y_recv: typing.Any
    ry_recv: typing.Any
    zb_recv: typing.Any
    zc_recv: typing.Any
    w_send: typing.Any
    kz_send: typing.Any
    kz_recv: typing.Any
    ky_send: typing.Any
    ky_recv: typing.Any
    kx_send: typing.Any
    kx_recv: typing.Any
    kd_send: typing.Any
    kd_recv: typing.Any
    k_loc: typing.Any
    dsend: typing.Any
    drecv: typing.Any
    send1: typing.Any
    recv1: typing.Any
    send2: typing.Any
    recv2: typing.Any
    send3: typing.Any
    recv3: typing.Any
    send4: typing.Any
    recv4: typing.Any
    kvx_send: typing.Any
    kvx_recv: typing.Any
    kvx_loc: typing.Any


def model_kernel(*refs):
    r = Refs(*refs)
    z, y, x, c = (lax.axis_index(a) for a in ("z", "y", "x", "core"))
    n_layers = r.wkv.shape[0]
    rows, d_model = r.hid.shape
    batch, d_local = r.xt.shape[:2]
    seqs = batch // RING
    seq_len, head_dim = r.cos.shape
    d_row = r.w_in.shape[1]
    e_loc = r.wi.shape[3]
    depth = r.wo.shape[3]
    f_loc = depth - head_dim
    quarter = rows // 4
    width = d_model // RING
    q_block = head_dim * RING
    f_block = f_loc * RING

    turned = {id(v): [lax.rem(v + o, RING) for o in RINGS] for v in (z, y, x)}

    def turn(base, off):
        if isinstance(off, int):
            return turned[id(base)][off % RING]
        return lax.rem(base + off + RING, RING)

    def remote(src, dst, ssem, rsem, dev):
        return pltpu.make_async_remote_copy(
            src_ref=src, dst_ref=dst, send_sem=ssem, recv_sem=rsem, device_id=dev, device_id_type=pl.DeviceIdType.MESH)

    partner = (z, y, x, 1 - c)

    peers = [(turn(z, o), y, x, c) for o in OTHERS]
    peers += [(z, turn(y, oy), turn(x, ox), c) for oy in RINGS for ox in RINGS if oy or ox]
    peers.append(partner)
    here = (z, y, x, c)
    gate_sem = pltpu.get_barrier_semaphore()
    for dev in peers:
        pl.semaphore_signal(gate_sem, inc=1, device_id=dev, device_id_type=pl.DeviceIdType.MESH)
    src_id = lax.broadcasted_iota(jnp.int32, (d_local, d_row), 0) + (x * CORES + c) * d_local
    dst_id = lax.broadcasted_iota(jnp.int32, (d_local, d_row), 1)
    spread = jnp.where(src_id == dst_id, 1.0, 0.0).astype(BF)
    r.gbuf[x, c, y, z] = jnp.zeros((G_ROWS, d_row), BF)
    r.gbuf[x, c, y, z, :n_layers] = jnp.dot(r.gain_in[...], spread, preferred_element_type=F32).astype(BF)
    pl.semaphore_wait(gate_sem, len(peers))

    def hook(pump, i):
        with jax.named_scope(f"hook_{i}"):
            pump(i)

    def w_cols(kind):
        return pl.ds(0, head_dim + f_loc) if kind == 0 else pl.ds(head_dim + f_loc, f_loc)

    def piece(t, zz, yy):
        l, kind = t // 3, t % 3
        if kind == 2:
            return r.wo.at[l, zz, yy]
        return r.wi.at[l, zz, pl.ds(pl.multiple_of(yy * d_row, d_row), d_row), w_cols(kind)]

    def piece_half(t, zz, yy, h):
        l, kind = t // 3, t % 3
        if kind == 2:
            return r.wo.at[l, zz, yy, pl.ds(h * (depth // 2), depth // 2)]
        return r.wi.at[l, zz, pl.ds(pl.multiple_of(yy * d_row + h * (d_row // 2), d_row // 2), d_row // 2), w_cols(kind)]

    def own_parts(t, owner, zz, yy):
        l, kind = t // 3, t % 3
        hq = pl.ds(pl.multiple_of(owner * head_dim, head_dim), head_dim)
        if kind == 2:
            return [
                (r.w_out.at[l, hq], r.wo.at[l, zz, yy, pl.ds(0, head_dim)]),
                (r.w_out.at[l, pl.ds(pl.multiple_of(q_block + owner * f_loc, head_dim), f_loc)], r.wo.at[l, zz, yy, pl.ds(head_dim, f_loc)]),
            ]
        rws = pl.ds(pl.multiple_of(yy * d_row, d_row), d_row)
        if kind == 0:
            return [
                (r.w_in.at[l, :, hq], r.wi.at[l, zz, rws, pl.ds(0, head_dim)]),
                (r.w_in.at[l, :, pl.ds(pl.multiple_of(q_block + owner * f_loc, head_dim), f_loc)], r.wi.at[l, zz, rws, pl.ds(head_dim, f_loc)]),
            ]
        return [(r.w_in.at[l, :, pl.ds(pl.multiple_of(q_block + f_block + owner * f_loc, head_dim), f_loc)],
                 r.wi.at[l, zz, rws, pl.ds(head_dim + f_loc, f_loc)])]

    def relay_ref(t, d):
        l, kind = t // 3, t % 3
        return r.rwo.at[l, d] if kind == 2 else r.rwi.at[l, d, :, w_cols(kind)]

    def far_parts(t, d):
        l, kind = t // 3, t % 3
        owner = turn(y, 2)
        hq = pl.ds(pl.multiple_of(owner * head_dim, head_dim), head_dim)
        if kind == 2:
            n = depth // 2
            base = q_block + owner * f_loc
            if d:
                return [(r.w_out.at[l, pl.ds(pl.multiple_of(base + n - head_dim, G_ROWS), n)], r.rwo.at[l, d])]
            return [
                (r.w_out.at[l, hq], r.rwo.at[l, d, pl.ds(0, head_dim)]),
                (r.w_out.at[l, pl.ds(pl.multiple_of(base, head_dim), n - head_dim)], r.rwo.at[l, d, pl.ds(head_dim, n - head_dim)]),
            ]
        rws = pl.ds(d * (d_row // 2), d_row // 2)
        if kind == 0:
            return [
                (r.w_in.at[l, rws, hq], r.rwi.at[l, d, :, pl.ds(0, head_dim)]),
                (r.w_in.at[l, rws, pl.ds(pl.multiple_of(q_block + owner * f_loc, head_dim), f_loc)], r.rwi.at[l, d, :, pl.ds(head_dim, f_loc)]),
            ]
        return [(r.w_in.at[l, rws, pl.ds(pl.multiple_of(q_block + f_block + owner * f_loc, head_dim), f_loc)], relay_ref(t, d))]

    def y_send(t):
        for d in BOTH:
            owner = turn(y, SIGN[d])
            dev = (z, owner, x, c)
            for src, dst in far_parts(t, d):
                remote(src, dst, r.w_send.at[t, 0], r.ry_recv.at[t, d], dev).start()
            for src, dst in own_parts(t, owner, z, y):
                remote(src, dst, r.w_send.at[t, 0], r.y_recv.at[t, -SIGN[d] % RING], dev).start()

    def y_relay(t):
        for d in BOTH:
            ref = relay_ref(t, d)
            remote(ref, ref, r.w_send.at[t, 3], r.ry_recv.at[t, d], here).wait_recv()
            dst = piece_half(t, z, turn(y, -SIGN[d]), d)
            remote(ref, dst, r.w_send.at[t, 3], r.y_recv.at[t, 2], (z, turn(y, SIGN[d]), x, c)).start()

    def z_own(t):
        for d in BOTH:
            for src, dst in own_parts(t, y, z, y):
                remote(src, dst, r.w_send.at[t, 1], r.zb_recv.at[t, 0, d], (turn(z, SIGN[d]), y, x, c)).start()

    def z_direct(t, j):
        yy = turn(y, j)
        ref = piece(t, z, yy)
        remote(ref, ref, r.w_send.at[t, 0], r.y_recv.at[t, j], here).wait_recv()
        for d in BOTH:
            remote(ref, ref, r.w_send.at[t, 1], r.zb_recv.at[t, j, d], (turn(z, SIGN[d]), y, x, c)).start()

    def z_forward(t, j):
        yy = turn(y, j)
        for d in BOTH:
            zz = turn(z, -SIGN[d])
            ref = piece(t, zz, yy)
            remote(ref, ref, r.w_send.at[t, 1], r.zb_recv.at[t, j, d], here).wait_recv()
            part = piece_half(t, zz, yy, d)
            remote(part, part, r.w_send.at[t, 2], r.zc_recv.at[t, j, d], (turn(z, SIGN[d]), y, x, c)).start()

    def place(t, zz):
        l, kind = t // 3, t % 3
        if kind == 2:
            return r.wo.at[l, zz], r.wov.at[zz]
        return r.wi.at[l, zz, :, w_cols(kind)], r.wv.at[zz, :, w_cols(kind)]

    def load_near(t):
        kind = t % 3
        for d in BOTH:
            src, dst = place(t, turn(z, SIGN[d]))
            pltpu.make_async_copy(src, dst, r.w_load.at[kind]).start()
        for j in OTHERS:
            yy = turn(y, j)
            dst = r.wov.at[z, yy] if kind == 2 else r.wv.at[z, pl.ds(pl.multiple_of(yy * d_row, d_row), d_row), w_cols(kind)]
            pltpu.make_async_copy(piece(t, z, yy), dst, r.w_load.at[kind]).start()
        for src, dst in own_parts(t, y, z, y):
            pltpu.make_async_copy(src, own_place(t, dst, src), r.w_load.at[kind]).start()

    def load_far(t):
        far = turn(z, 2)
        for j in RINGS:
            for d in BOTH:
                part = piece_half(t, far, turn(y, j), d)
                remote(part, part, r.w_send.at[t, 2], r.zc_recv.at[t, j, d], here).wait_recv()
        src, dst = place(t, far)
        pltpu.make_async_copy(src, dst, r.far_load.at[t % 3]).start()

    def own_place(t, dst, src):
        kind = t % 3
        if kind == 2:
            n = src.shape[0]
            return r.wov.at[z, y, pl.ds(0 if n == head_dim and f_loc != head_dim else head_dim, n)]
        n = src.shape[1]
        rws = pl.ds(pl.multiple_of(y * d_row, d_row), d_row)
        if kind == 0:
            return r.wv.at[z, rws, pl.ds(0 if n == head_dim and f_loc != head_dim else head_dim, n)]
        return r.wv.at[z, rws, pl.ds(head_dim + f_loc, f_loc)]

    def finish(t):
        load_near(t)
        load_far(t)

    def near_loaded(t):
        kind = t % 3
        dst = r.wov.at[pl.ds(0, LAST)] if kind == 2 else r.wv.at[pl.ds(0, LAST), :, w_cols(kind)]
        pltpu.make_async_copy(dst, dst, r.w_load.at[kind]).wait()

    def far_loaded(t):
        kind = t % 3
        dst = r.wov.at[0] if kind == 2 else r.wv.at[0, :, w_cols(kind)]
        pltpu.make_async_copy(dst, dst, r.far_load.at[kind]).wait()

    def loaded(t):
        near_loaded(t)
        far_loaded(t)

    def drain(t):
        l, kind = t // 3, t % 3
        if kind == 2:
            done = (r.wo.at[l, 0, pl.ds(0, LAST)], r.wo.at[l, pl.ds(0, 2)], r.wo.at[l, 0], r.wo.at[l, 0, 0])
        else:
            cols = w_cols(kind)
            done = (r.wi.at[l, 0, pl.ds(0, LAST * d_row), cols], r.wi.at[l, pl.ds(0, 2), :, cols], r.wi.at[l, 0, :, cols],
                    r.wi.at[l, 0, pl.ds(0, d_row), cols])
        for g, ref in enumerate(done):
            remote(ref, ref, r.w_send.at[t, g], r.y_recv.at[t, 0], here).wait_send()

    def kv_z_copy(k):
        return remote(r.wkv, r.kvh.at[x, c, :, y, z], r.kz_send.at[k], r.kz_recv.at[k], (turn(z, OTHERS[k]), y, x, c))

    def kv_own():
        return pltpu.make_async_copy(r.wkv, r.kvh.at[x, c, :, y, z], r.k_loc.at[0])

    def kv_z():
        for k in range(len(OTHERS)):
            kv_z_copy(k).start()
        kv_own().start()

    def kv_y_copy(ref, k, d):
        return remote(ref, ref, r.ky_send, r.ky_recv.at[k], (z, turn(y, SIGN[d]), x, c))

    def kv_y1():
        kv_own().wait()
        for k in range(len(OTHERS)):
            kv_z_copy(k).wait()
        for d in BOTH:
            kv_y_copy(r.kvh.at[x, c, :, y], d, d).start()

    def kv_y2():
        for d in BOTH:
            yy = turn(y, -SIGN[d])
            kv_y_copy(r.kvh.at[x, c, :, yy], d, d).wait_recv()
            kv_y_copy(r.kvh.at[x, c, :, yy, pl.ds(2 * d, 2)], 2, d).start()

    def kv_y3():
        kv_y_copy(r.kvh.at[x, c, :, turn(y, 2)], 2, 0).wait_recv()
        kv_y_copy(r.kvh.at[x, c, :, pl.ds(0, LAST)], 0, 0).wait_send()

    def kv_x_copy(l, ref, k, d):
        return remote(ref, ref, r.kx_send.at[l], r.kx_recv.at[l, k], (z, y, turn(x, SIGN[d]), c))

    def kv_die(l, ref):
        return remote(ref, ref, r.kd_send.at[l], r.kd_recv.at[l], partner)

    def kv_x1(l):
        ref = r.kvh.at[x, c, l]
        for d in BOTH:
            kv_x_copy(l, ref, d, d).start()
        kv_die(l, ref).start()

    def kv_x2(l):
        for d in BOTH:
            xx = turn(x, -SIGN[d])
            ref = r.kvh.at[xx, c, l]
            kv_x_copy(l, ref, d, d).wait_recv()
            kv_x_copy(l, r.kvh.at[xx, c, l, pl.ds(2 * d, 2)], 2, d).start()
            kv_die(l, ref).start()

    def kv_x3(l):
        ref = r.kvh.at[turn(x, 2), c, l]
        kv_x_copy(l, ref, 2, 0).wait_recv()
        kv_die(l, ref).start()

    def kv_load(l):
        kv_die(l, r.kvh.at[:, 1 - c, l]).wait_recv()
        kc = r.wkv.shape[1]
        for xx in RINGS:
            for cc in BOTH:
                pltpu.make_async_copy(r.kvh.at[xx, cc, l], r.kvb.at[:, :, pl.ds((xx * CORES + cc) * kc, kc)], r.k_loc.at[1]).start()

    def kv_sent(l):
        kv_x_copy(l, r.kvh.at[pl.ds(0, LAST), c, l], 0, 0).wait_send()
        kv_die(l, r.kvh.at[:, c, l]).wait_send()

    def kv_loaded():
        pltpu.make_async_copy(r.kvb, r.kvb, r.k_loc.at[1]).wait()

    def gain_move(i, src, dst, dev):
        return remote(src, dst, r.g_send.at[i], r.g_recv.at[i], dev)

    def gain_z(k):
        dev = (turn(z, OTHERS[k]), y, x, c)
        return gain_move(k, r.gbuf.at[x, c, y, z], r.gbuf.at[x, c, y, z], dev)

    def gain_y(k):
        dev = (z, turn(y, OTHERS[k]), x, c)
        return gain_move(len(OTHERS) + k, r.gbuf.at[x, c, y], r.gbuf.at[x, c, y], dev)

    def gain_x(k):
        dev = (z, y, turn(x, OTHERS[k]), c)
        return gain_move(CORES * len(OTHERS) + k, r.gbuf.at[x, c], r.gbuf.at[x, c], dev)

    def gain_die(xx, k):
        ref = r.gbuf.at[xx, c]
        return remote(ref, ref, r.gd_send.at[k], r.gd_recv.at[k], partner)

    def gain_sum():
        for zz in RINGS:
            for yy in RINGS:
                tot = jnp.zeros((n_layers, d_row), F32)
                for xx in RINGS:
                    for cc in BOTH:
                        tot += r.gbuf[xx, cc, yy, zz, :n_layers].astype(F32)
                at = (zz * RING + yy) * d_row
                r.gain[:, at:at + d_row] = tot

    tok_pair = CORES * rows

    def x_z(k):
        zz = turn(z, OTHERS[k])
        src = r.xt.at[pl.ds(zz * seqs, seqs)]
        return remote(src, r.xz.at[z], r.xz_send.at[k], r.xz_recv.at[k], (zz, y, x, c))

    def x_own():
        return pltpu.make_async_copy(r.xt.at[pl.ds(z * seqs, seqs)], r.xz.at[z], r.x_loc)

    def pos(xx):
        return pl.ds(pl.multiple_of(xx * tok_pair, tok_pair), tok_pair)

    def x_plane(oy, ox):
        yy, xx = turn(y, oy), turn(x, ox)
        return remote(r.xz.at[:, yy, :, pos(xx)], r.xp.at[c, y, x], r.xp_send.at[oy], r.xp_recv.at[(RING - oy) % RING], (z, yy, xx, c))

    def row_bytes(oy):
        return r.xp.at[c, 0] if oy else r.xp.at[c, 0, pl.ds(0, RING - 1)]

    def x_row(oy):
        yy = turn(y, oy)
        got = row_bytes(oy)
        remote(got, got, r.xp_send.at[oy], r.xp_recv.at[oy], partner).wait_recv()
        row = r.xp.at[c, yy]
        remote(row, row, r.xd_send.at[oy], r.xd_recv.at[oy], partner).start()

    def x_turn():
        for oy in RINGS:
            row = r.xp.at[1 - c, turn(y, oy)]
            remote(row, row, r.xd_send.at[oy], r.xd_recv.at[oy], partner).wait_recv()

        @pl.loop(0, RING)
        def _(zz):
            for yy in RINGS:
                for xh in BOTH:
                    blk = [r.xp[cc, yy, CORES * xh + xx, zz] for xx in BOTH for cc in BOTH]
                    blk = jnp.concatenate(blk, axis=0).astype(F32).T.astype(BF)
                    n = blk.shape[1]
                    at = pl.multiple_of(zz * RING * d_row + yy * d_row + xh * n, n)
                    r.hb[0, 0, :, :, pl.ds(at, n)] = blk.reshape(CORES, rows, n)
        r.hid[...] = r.hb[0, 0, c]
        for oy in RINGS:
            row = r.xp.at[c, turn(y, oy)]
            remote(row, row, r.xd_send.at[oy], r.xd_recv.at[oy], partner).wait_send()

    def x_sent():
        for fn in (x_z, gain_z, gain_y, gain_x):
            peers_of(fn, "wait_send")
        for k in RINGS:
            gain_die(x, k).wait_send()
        for oy in RINGS:
            got = row_bytes(oy)
            remote(got, got, r.xp_send.at[oy], r.xp_recv.at[oy], partner).wait_send()

    def y_die(p):
        cols = pl.ds(pl.multiple_of(turn(z, p) * width, width), width)
        return remote(r.hid.at[:, cols], r.hb.at[0, 0, c, :, cols], r.yd_send.at[p], r.yd_recv.at[p], partner)

    def planes(h):
        return pl.ds(2 * h, 2)

    def y_plane(h, oy, ox):
        yy, xx = turn(y, oy), turn(x, ox)
        return remote(r.xp.at[c, yy, xx, planes(h)], r.xz.at[planes(h), y, :, pos(x)], r.yp_send.at[h, oy], r.yp_recv.at[h, (RING - oy) % RING],
                      (z, yy, xx, c))

    def y_z(p, oy):
        s = turn(y, oy)
        return remote(r.xz.at[p, s], r.y_out.at[z * seqs + s], r.yz_send.at[p, oy], r.yz_recv.at[p, oy], (turn(z, p), y, x, c))

    def y_own(oy):
        s = turn(y, oy)
        return pltpu.make_async_copy(r.xz.at[0, s], r.y_out.at[z * seqs + s], r.y_loc.at[oy])

    def leave_a(h):
        for p in BOTH:
            p = 2 * h + p
            y_die(p).start()
            cols = pl.ds(pl.multiple_of(turn(z, p) * width, width), width)
            r.hb[0, 0, c, :, cols] = r.hid[:, cols]

    def leave_b(h):
        n = CORES * CORES * d_local
        for p in BOTH:
            p = 2 * h + p
            y_die(p).wait()

            @pl.loop(0, RING)
            def _(yy, p=p):
                for xh in BOTH:
                    at = pl.multiple_of(turn(z, p) * width + yy * d_row + xh * n, n)
                    blk = r.hb[0, 0, :, :, pl.ds(at, n)].reshape(tok_pair, n).astype(F32).T.astype(BF)
                    for xx in BOTH:
                        for cc in BOTH:
                            lo = (xx * CORES + cc) * d_local
                            r.xp[cc, yy, CORES * xh + xx, p] = blk[lo:lo + d_local]

        for oy in OTHERS + (0,):
            for ox in RINGS:
                if oy or ox:
                    y_plane(h, oy, ox).start()
        for p in BOTH:
            p = 2 * h + p
            r.xz[p, y, :, pos(x)] = r.xp[c, y, x, p]

    def plane_bytes(h, oy):
        return r.xp.at[c, 0, :, planes(h)] if oy else r.xp.at[c, 0, pl.ds(0, LAST), planes(h)]

    def leave_c(h):
        for oy in OTHERS + (0,):
            got = plane_bytes(h, oy)
            remote(got, got, r.yp_send.at[h, oy], r.yp_recv.at[h, oy], partner).wait_recv()
            for p in BOTH:
                p = 2 * h + p
                (y_z(p, oy) if p else y_own(oy)).start()

    def left():
        for oy in RINGS:
            for h in BOTH:
                got = plane_bytes(h, oy)
                remote(got, got, r.yp_send.at[h, oy], r.yp_recv.at[h, oy], partner).wait_send()
            for p in RINGS:
                (y_z(p, oy) if p else y_own(oy)).wait()

    def kv_rows(zz):
        n = CORES * seq_len // (RING * RING * RING * CORES)
        return pl.ds(pl.multiple_of(((zz * RING + y) * RING + x) * n, n), n)

    def kv_trade(l, k):
        zz = turn(z, OTHERS[k])
        return remote(r.kv_out.at[l, :, :, kv_rows(zz)], r.kvx.at[l, z], r.kvx_send.at[l, k], r.kvx_recv.at[l, k], (zz, y, x, c))

    def kv_keep(l):
        return pltpu.make_async_copy(r.kv_out.at[l, :, :, kv_rows(z)], r.kvx.at[l, z], r.kvx_loc.at[l])

    def kv_share(l):
        for k in range(len(OTHERS)):
            kv_trade(l, k).start()
        kv_keep(l).start()

    def kv_shared(l):
        for k in range(len(OTHERS)):
            kv_trade(l, k).wait()
        kv_keep(l).wait()

    def gather_norm(l, split, pump):
        hid = r.hid
        gain = r.gain[l:l + 1, :]
        for b in range(4):
            blk = hid[b * quarter:(b + 1) * quarter, :].astype(F32)
            mean = jnp.mean(blk, axis=-1, keepdims=True)
            cen = blk - mean
            var = jnp.mean(cen * cen, axis=-1, keepdims=True)
            r.h_ref[b * quarter:(b + 1) * quarter, :] = (cen * lax.rsqrt(var + LN_EPS) * gain).astype(BF)
        out = r.h_all.at[l]

        def spot(q, first, second):
            if q == 0:
                return turn(y, second), turn(x, first)
            return turn(y, first), turn(x, second)

        def span(q, part):
            lo, n = (split, rows - split) if q else (0, split)
            if part is NIL:
                return pl.ds(lo, n)
            return pl.ds(lo + part * (n // 2), n // 2)

        offs = (0, -1, 1, 2)
        plans = {}
        for q in BOTH:
            for d in BOTH:
                plans["first", q, d] = (q, 0, 0, NIL, SIGN[d], 0)
                plans["first_on", q, d] = (q, -SIGN[d], 0, d, SIGN[d], 0)
                for k in RINGS:
                    plans["second", q, k, d] = (q, offs[k], 0, NIL, 0, SIGN[d])
                    plans["second_on", q, k, d] = (q, offs[k], -SIGN[d], d, 0, SIGN[d])
        index = {key: n for n, key in enumerate(plans)}

        def link(*key, own=False):
            idx, (q, first, second, part, to_first, to_second) = index[key], plans[key]
            sy, sx = spot(q, first, second)
            ty, tx = spot(q, to_first, to_second)
            rws = span(q, part)
            dst = out.at[sy, sx, c, rws]
            return remote(r.h_ref.at[rws] if own else dst, dst, r.ag_send.at[l, KINDS.index(key[0])], r.ag_recv.at[l, idx], (z, ty, tx, c))

        def arrived(*key):
            for d in BOTH:
                link(*key, d).wait_recv()

        def die(q, first, second, own=False):
            sy, sx = spot(q, first, second)
            rws = span(q, NIL)
            dst = out.at[sy, sx, c, rws]
            off = (first if q else second) % RING
            remote(r.h_ref.at[rws] if own else dst, dst, r.ag_dsend.at[l], r.ag_drecv.at[l, off], partner).start()

        def take(k, q):
            for d in BOTH:
                link("second", q, k, d).wait_recv()
                die(q, offs[k], -SIGN[d])

        def pass_on(k, q):
            for d in BOTH:
                link("second_on", q, k, d).start()

        def second_step(k):
            take(k, 1)
            pass_on(k, 1)
            take(k, 0)

        def far_first(q):
            for e in BOTH:
                link("second", q, LAST, e).start()

        def last_step(q, k):
            arrived("second_on", q, k)
            die(q, offs[k], 2)

        def tail_a():
            second_step(2)
            far_first(1)
            for k in RINGS[:-1]:
                pass_on(k, 0)
            hook(pump, "k2")
            take(LAST, 0)
            pass_on(LAST, 0)
            hook(pump, "k3")
            for k in (1, 2):
                last_step(1, k)

        def tail_b():
            take(LAST, 1)
            pass_on(LAST, 1)

        def tail_c():
            for k in RINGS:
                last_step(0, k)
            last_step(1, LAST)

        for q in BOTH:
            for d in BOTH:
                link("first", q, d, own=True).start()
        for q in BOTH:
            for d in BOTH:
                link("second", q, 0, d, own=True).start()
        for q in BOTH:
            die(q, 0, 0, own=True)
        own = pltpu.make_async_copy(r.h_ref, out.at[y, x, c], r.ag_loc)
        own.start()
        hook(pump, "begin")
        for d in BOTH:
            for q in BOTH:
                link("first", q, d).wait_recv()
                src = -SIGN[d]
                link("first_on", q, d).start()
                die(q, src, 0)
        hook(pump, "first")
        second_step(0)
        for q in reversed(BOTH):
            for d in BOTH:
                for e in BOTH:
                    link("second", q, 1 + d, e).start()
        hook(pump, "k0")
        for q in BOTH:
            arrived("first_on", q)
            die(q, 2, 0)
        far_first(0)
        hook(pump, "first_on")
        last_step(1, 0)
        own.wait()
        hook(pump, "ready")

        def crossed(off):
            got = out.at[turn(y, off), :, 1 - c]
            remote(got, got, r.ag_dsend.at[l], r.ag_drecv.at[l, off], partner).wait_recv()

        def order(i):
            if isinstance(i, int):
                return (OWN, BEFORE, AFTER, FAR)[i]
            return lax.rem(3 * i + 3 * (i // 2) + 2 * (i // 3), RING)

        def fetch(i, slot):
            off = order(i)
            crossed(off)
            h_copy(l, turn(y, off), slot).start()

        def up_ready():
            hook(pump, "up")
            loaded(UP1 if l else UP0)

        crossed(0)
        h_copy(l, y, 0).start()

        def opening():
            second_step(1)
            hook(pump, "k1")

        def turn_of(i):
            slot = lax.rem(i, H_SLOTS)
            s = turn(y, order(i))
            h_copy(l, s, slot).wait()
            pump(("seq", i))
            one(l, s, slot, i)

            @pl.when(i == 1)
            def _():
                tail_b()

            @pl.when(i == 2)
            def _():
                tail_c()
                fetch(LAST, 0)

            return s, slot

        def neighbours():
            tail_a()
            for n in (1, 2):
                fetch(n, n)

        if l:
            @pl.loop(0, RING)
            def _(i):
                s, slot = turn_of(i)

                @pl.when(i == 0)
                def _():
                    opening()
                    up_ready()

                pump(("two", i))
                two(s, slot)

                @pl.when(i == 0)
                def _():
                    neighbours()
        else:
            h_copy(l, y, 0).wait()
            hook(pump, "own")
            one(l, y, 0, 0)
            opening()
            neighbours()

            @pl.loop(1, RING)
            def _(i):
                turn_of(i)

                @pl.when(i == 1)
                def _():
                    up_ready()

                pump(("two", i - 1))
                two(turn(y, order(i - 1)), lax.rem(i - 1, H_SLOTS))

            hook(pump, "two3")
            two(turn(y, FAR), 0)

        for slot in BOTH:
            for i in BOTH:
                kv_out_copy(l, 0, slot, i).wait()
        sent = (out.at[y, x], out.at[y], out.at[y, x, c], out.at[y, pl.ds(0, CORES)])
        for kind, ref in enumerate(sent):
            remote(ref, ref, r.ag_send.at[l, kind], r.ag_recv.at[l, kind], partner).wait_send()
        remote(out.at[pl.ds(0, 2)], out.at[pl.ds(0, 2)], r.ag_dsend.at[l], r.ag_drecv.at[l, 0], partner).wait_send()

    def h_copy(l, s, slot):
        return pltpu.make_async_copy(r.h_all.at[l, s], r.hb.at[slot], r.h_sem.at[slot])

    def h_tile(slot):
        return r.hb[slot].reshape(seq_len, d_model)

    def project(h, lo, n):
        w = r.wv[:, :, lo:lo + n].reshape(d_model, n)
        return jnp.dot(h, w, preferred_element_type=F32).astype(BF)

    def rope(val):
        val = val.astype(F32)
        return val * r.cos[...] + pltpu.roll(val, head_dim // 2, 1) * r.sin[...]

    n_chunk = min(256, f_loc)

    def kv_out_copy(l, s, slot, i):
        return pltpu.make_async_copy(r.qkv.at[slot, i], r.kv_out.at[l, i, s], r.kvo_sem.at[slot, i])

    def one(l, s, slot, i):
        pair = i % 2 if isinstance(i, int) else lax.rem(i, 2)

        @pl.when(i >= 2)
        def _():
            for k in BOTH:
                kv_out_copy(l, s, pair, k).wait()

        kv = jnp.zeros((seq_len, 2 * head_dim), F32)
        for zz in RINGS:
            for yy in RINGS:
                col = (zz * RING + yy) * d_row
                kv += lax.dot_general(h_cols(slot, col, d_row), r.kvb[yy, zz], (((1,), (1,)), ((), ())), preferred_element_type=F32)
        kv = kv.astype(BF)
        r.qkv[pair, 0] = rope(kv[:, :head_dim]).astype(BF)
        r.qkv[pair, 1] = kv[:, head_dim:]
        for i in BOTH:
            kv_out_copy(l, s, pair, i).start()
        q = project(h_tile(slot), 0, head_dim)
        r.stage[...] = (rope(q) * head_dim ** -0.5).astype(BF)
        for lo in range(0, f_loc, n_chunk):
            r.joined[s, :, head_dim + lo:head_dim + lo + n_chunk] = project(h_tile(slot), head_dim + lo, n_chunk)
        n_tile = seq_len // 2
        for i in BOTH:
            keys = (i + 1) * n_tile
            sc = lax.dot_general(r.stage[i * n_tile:(i + 1) * n_tile, :], r.qkv[pair, 0, :keys, :], (((1,), (1,)), ((), ())), preferred_element_type=F32)
            row_id = lax.broadcasted_iota(jnp.int32, sc.shape, 0) + i * n_tile
            col_id = lax.broadcasted_iota(jnp.int32, sc.shape, 1)
            sc = jnp.where(col_id <= row_id, sc, -1e30)
            top = jnp.max(sc, axis=-1, keepdims=True)
            ex = jnp.exp(sc - top)
            prob = (ex * (1.0 / jnp.sum(ex, axis=-1, keepdims=True))).astype(BF)
            att = jnp.dot(prob, r.qkv[pair, 1, :keys, :], preferred_element_type=F32)
            r.joined[s, i * n_tile:(i + 1) * n_tile, :head_dim] = att.astype(BF)

    def h_cols(slot, col, n):
        return r.hb[slot, :, :, :, col:col + n].reshape(seq_len, n)

    def two(s, slot):
        for lo in range(0, f_loc, n_chunk):
            up = project(h_tile(slot), head_dim + f_loc + lo, n_chunk).astype(F32)
            cols = slice(head_dim + lo, head_dim + lo + n_chunk)
            g = r.joined[s, :, cols].astype(F32)
            r.joined[s, :, cols] = (g * jax.nn.sigmoid(g) * up).astype(BF)

    def out_scatter(l, pump):
        def peer(q, first, second):
            dy = first * (1 - q) + second * q
            dx = first * q + second * (1 - q)
            return (z, turn(y, dy), turn(x, dx), c)

        def die_copy(ch, q, s):
            return remote(r.away.at[q], r.die_in.at[ch, q, s], r.dsend.at[l, ch, q, s], r.drecv.at[l, ch, q, s], partner)

        def first_copy(ch, q, d):
            return remote(r.acc.at[ch, q, 0, pl.ds(CORES * d, CORES)], r.in1.at[ch, q, d], r.send1.at[l, ch, q, d], r.recv1.at[l, ch, q, d],
                          peer(q, SIGN[d], 0))

        def second_copy(ch, q, d, h):
            js = pl.ds(CORES * h, CORES)
            return remote(r.acc.at[ch, q, 1 + d, js], r.in2.at[ch, q, d, js], r.send2.at[l, ch, q, d, h], r.recv2.at[l, ch, q, d, h],
                          peer(q, SIGN[d], 0))

        def half_rows(d):
            return pl.ds(d * (rows // 2), rows // 2)

        def third_copy(ch, q, d):
            return remote(r.acc.at[ch, q, LAST, 0, half_rows(d)], r.in3.at[ch, q, d], r.send3.at[l, ch, q, d], r.recv3.at[l, ch, q, d],
                          peer(q, 0, SIGN[d]))

        def fourth_copy(ch, q, d):
            return remote(r.acc.at[ch, q, LAST, 1 + d], r.in4.at[ch, q, d], r.send4.at[l, ch, q, d], r.recv4.at[l, ch, q, d],
                          peer(q, 0, SIGN[d]))

        n_blk = r.wov.shape[3]

        def plane_of(ch, q):
            if l:
                return turn(z, q if ch else 2 + q)
            return turn(z, LAST - q if ch else q)

        def slot_off(s):
            return lax.rem(2 + 3 * s + 3 * (s // 2) + 2 * (s // 3), RING)

        def tile(ch, q, s):
            off = slot_off(s)
            for cc in BOTH:
                for j in RINGS:
                    oy = off * (1 - q) + SLOT_OFF[j] * q
                    ox = SLOT_OFF[j] * (1 - q) + off * q
                    core = c if cc else 1 - c
                    at = pl.multiple_of((turn(x, ox) * CORES + core) * rows, rows)
                    r.lhs[pl.ds((cc * RING + j) * rows, rows), :] = r.joined[turn(y, oy), pl.ds(at, rows), :]
            left = r.lhs[...]
            zz = plane_of(ch, q)
            for n in RINGS:
                res = jnp.dot(left, r.wov[zz, n], preferred_element_type=F32).astype(BF)
                res = res.reshape(CORES, RING, rows, n_blk)
                r.away[q, :, :, n * n_blk:(n + 1) * n_blk] = res[0]
                r.acc[ch, q, s, :, :, n * n_blk:(n + 1) * n_blk] = res[1]

        def pair_sum(ch, q, s):
            die_copy(ch, q, s).wait_recv()

            @pl.loop(0, RING)
            def _(j):
                r.acc[ch, q, s, j] = r.acc[ch, q, s, j] + r.die_in[ch, q, s, j]

        def stage_a(ch):
            @pl.loop(0, CORES * RING)
            def _(t):
                s = t // CORES
                q = lax.rem(t, CORES)

                @pl.when(s >= 1)
                def _():
                    die_copy(ch, q, s - 1).wait_send()

                if ch:
                    @pl.when(s == 0)
                    def _():
                        die_copy(ch - 1, q, LAST).wait_send()

                tile(ch, q, s)
                die_copy(ch, q, s).start()

                @pl.when(s >= 1)
                def _():
                    pair_sum(ch, q, s - 1)

                @pl.when(s == 1)
                def _():
                    for d in BOTH:
                        first_copy(ch, q, d).start()

                for d in BOTH:
                    @pl.when(s == 2 + d)
                    def _(d=d):
                        second_copy(ch, q, d, 1 - d).start()

                for n in RINGS:
                    name = f"a{ch}s{n}"
                    if pump(name, False):
                        @pl.when(t == CORES * n + 1)
                        def _(name=name):
                            hook(pump, name)

        def stage_b(ch):
            for q in BOTH:
                pair_sum(ch, q, LAST)
            for q in BOTH:
                for d in BOTH:
                    first_copy(ch, q, d).wait_recv()
                    for j in BOTH:
                        at = CORES * d + j
                        r.acc[ch, q, 1 + d, at] = r.acc[ch, q, 1 + d, at] + r.in1[ch, q, d, j]
                    second_copy(ch, q, d, d).start()

        def total(ch, q, j):
            val = r.acc[ch, q, LAST, j].astype(F32)
            for d in BOTH:
                val += r.in2[ch, q, d, j].astype(F32)
            r.acc[ch, q, LAST, j] = val.astype(BF)

        def stage_c(ch):
            for q in BOTH:
                for h in BOTH:
                    for d in BOTH:
                        second_copy(ch, q, d, h).wait_recv()
                total(ch, q, 0)
                for d in BOTH:
                    third_copy(ch, q, d).start()
                for j in RINGS[1:]:
                    total(ch, q, j)

        def stage_d(ch):
            for q in BOTH:
                for d in BOTH:
                    third_copy(ch, q, d).wait_recv()
                    rws = half_rows(d)
                    r.acc[ch, q, LAST, 1 + d, rws] = r.acc[ch, q, LAST, 1 + d, rws] + r.in3[ch, q, d]
                    fourth_copy(ch, q, d).start()

        def stage_e(ch):
            for q in BOTH:
                for d in BOTH:
                    fourth_copy(ch, q, d).wait_recv()
                cols = pl.ds(pl.multiple_of(plane_of(ch, q) * width, width), width)
                upd = r.acc[ch, q, LAST, LAST].astype(F32)
                for d in BOTH:
                    upd += r.in4[ch, q, d].astype(F32)
                upd = upd.astype(BF)
                r.hid[:, cols] = (r.hid[:, cols].astype(F32) + upd.astype(F32)).astype(BF)

        def sent(ch):
            for q in BOTH:
                if ch:
                    die_copy(ch, q, LAST).wait_send()
                for d in BOTH:
                    for cp in (first_copy, third_copy, fourth_copy):
                        cp(ch, q, d).wait_send()
                    for h in BOTH:
                        second_copy(ch, q, d, h).wait_send()

        stages = {"a": stage_a, "b": stage_b, "c": stage_c, "d": stage_d, "e": stage_e, "f": leave_a, "g": leave_b, "h": leave_c}
        for step in LAST_ORDER if l else FIRST_ORDER:
            with jax.named_scope(step):
                stages[step[0]](int(step[1]))
            hook(pump, step)
        for ch in BOTH:
            sent(ch)

    def near(fn, t):
        for j in (LAST, 1):
            fn(t, j)

    def far(fn, t):
        fn(t, 2)

    def z_all(t):
        near(z_direct, t)
        far(z_direct, t)

    def peers_of(fn, op="start"):
        for k in range(len(OTHERS)):
            getattr(fn(k), op)()

    def start(pump):
        peers_of(gain_z)
        kv_z()
        peers_of(x_z)
        x_own().start()
        pump("s0")
        with jax.named_scope("gain_a"):
            peers_of(gain_z, "wait_recv")
            peers_of(gain_y)
            kv_y1()
        pump("s1")
        with jax.named_scope("gain_b"):
            peers_of(gain_y, "wait_recv")
            peers_of(gain_x)
            gain_die(x, LAST).start()
        pump("s2")
        with jax.named_scope("x_z"):
            peers_of(x_z, "wait_recv")
            x_own().wait()
        for oy in RINGS:
            for ox in RINGS:
                if oy or ox:
                    x_plane(oy, ox).start()
        r.xp[c, y, x] = r.xz[:, y, :, pos(x)]
        pump("s3")
        with jax.named_scope("kv_b"):
            kv_y2()
        with jax.named_scope("gain_c"):
            for k, o in enumerate(OTHERS):
                gain_x(k).wait_recv()
                gain_die(turn(x, -o), k).start()
        pump("s4")
        for oy in (OWN, BEFORE, AFTER, FAR):
            with jax.named_scope(f"row_{oy}"):
                x_row(oy)
            pump(f"r{oy}")
        pump("s5")
        kv_y3()
        pump("s6")
        with jax.named_scope("gain_sum"):
            for k in RINGS:
                gain_die(x, k).wait_recv()
            gain_sum()
        with jax.named_scope("turn"):
            x_turn()
        pump("s7")

    def when(i, n, *fns):
        @pl.when(i == n)
        def _():
            for fn in fns:
                fn()

    def plan(steps):
        def pump(step, run=True):
            if not isinstance(step, str):
                for n in RINGS:
                    if (step[0], n) in steps:
                        when(step[1], n, lambda n=n: run_steps(steps[step[0], n]))
                return True
            found = steps.get(step, ())
            if run:
                run_steps(found)
            return found
        return pump

    def run_steps(steps):
        for fn, *args in steps:
            with jax.named_scope(f"{fn.__name__}_{args[-1] if args else 0}"):
                fn(*args)

    first_entry = plan({
        "s0": [(z_own, UP0)],
        "s1": [(y_send, QG0)],
        "s3": [(z_own, QG0)],
        "r0": [(y_relay, QG0), (z_forward, UP0, OWN), (z_direct, QG0, AFTER), (z_forward, QG0, OWN), (z_direct, QG0, BEFORE)],
        "s6": [(kv_x1, 0)],
    })
    first_front = plan({
        "begin": [(kv_x2, 0), (y_send, UP0), (z_forward, QG0, AFTER), (z_direct, QG0, FAR)],
        "k0": [(y_relay, UP0), (kv_x3, 0), (z_forward, QG0, BEFORE), (z_forward, QG0, FAR), (z_direct, UP0, AFTER), (z_direct, UP0, BEFORE)],
        "first_on": [(y_send, WO0)],
        "ready": [(load_near, QG0), (load_far, QG0), (kv_load, 0), (loaded, QG0), (kv_loaded,)],
        "k1": [(z_direct, UP0, FAR), (z_forward, UP0, AFTER)],
        "k2": [
            (z_forward, UP0, BEFORE), (y_relay, WO0), (z_forward, UP0, FAR), (y_send, QG1), (z_own, WO0), (z_direct, WO0, BEFORE),
            (kv_x1, 1),
        ],
        ("seq", 1): [(y_send, WO1), (z_direct, WO0, AFTER), (x_sent,)],
        "up": [(y_send, UP1), (z_direct, WO0, FAR), (load_near, UP0), (load_far, UP0)],
        ("two", 0): [(y_relay, QG1), (z_forward, WO0, OWN)],
        ("seq", 2): [(kv_x2, 1)],
        ("two", 1): [(kv_x3, 1), (z_direct, QG1, AFTER), (z_forward, WO0, BEFORE)],
        ("seq", 3): [(y_relay, WO1), (z_forward, WO0, AFTER)],
        ("two", 2): [(z_forward, WO0, FAR), (z_own, QG1), (y_relay, UP1)],
        "near": [(load_near, WO0)],
    })
    first_scatter = plan({
        "a0s0": [(z_forward, QG1, AFTER)],
        "a0s2": [(z_direct, QG1, BEFORE)],
        "b0": [(load_far, WO0), (far_loaded, WO0)],
        "a1s0": [(z_direct, QG1, FAR)],
        "a1s1": [(z_forward, QG1, OWN)],
        "a1": [(z_direct, UP1, FAR)],
        "b1": [(z_direct, UP1, BEFORE)],
        "c1": [(z_forward, QG1, FAR), (z_direct, UP1, AFTER), (z_own, UP1), (z_forward, QG1, BEFORE)],
        "e0": [(z_forward, UP1, FAR)],
    })
    second_front = plan({
        "begin": [(z_forward, UP1, BEFORE), (kv_load, 1)],
        "first": [(z_forward, UP1, AFTER)],
        "k0": [(z_forward, UP1, OWN), (z_direct, WO1, FAR)],
        "ready": [(load_near, QG1), (load_far, QG1), (loaded, QG1), (kv_loaded,)],
        ("seq", 0): [(z_own, WO1)],
        "k1": [(z_direct, WO1, BEFORE)],
        "up": [(load_near, UP1), (load_far, UP1)],
        "k2": [(z_direct, WO1, AFTER)],
        ("seq", 1): [(z_forward, WO1, FAR)],
        ("two", 1): [(z_forward, WO1, OWN)],
        ("two", 2): [(z_forward, WO1, BEFORE), (z_forward, WO1, AFTER)],
        "near": [(load_near, WO1), (load_far, WO1)],
    })
    second_scatter = plan({
    })

    with jax.named_scope("start"):
        start(first_entry)
    with jax.named_scope("front_0"):
        gather_norm(0, rows // RING, first_front)
    with jax.named_scope("near_0"):
        kv_share(0)
        first_front("near")
        near_loaded(WO0)
    with jax.named_scope("scatter_0"):
        out_scatter(0, first_scatter)
    with jax.named_scope("front_1"):
        gather_norm(1, rows // 2, second_front)
    with jax.named_scope("near_1"):
        kv_share(1)
        second_front("near")
        loaded(WO1)
    with jax.named_scope("scatter_1"):
        out_scatter(1, second_scatter)
    with jax.named_scope("drain"):
        left()
        for t in range(WO1 + 1):
            drain(t)
        for l in range(n_layers):
            kv_shared(l)
            kv_sent(l)


def run_model(xt, gain, wkv_t, w_in, w_out, cos_full, sin_full):
    batch, d_local, seq_len = xt.shape
    n_layers, d_row, e_block = w_in.shape
    r_block, d_col = w_out.shape[1:]
    head_dim = cos_full.shape[1]
    d_model = d_row * RING * RING
    seqs = batch // RING
    rows = seqs * seq_len // (RING * RING * CORES)
    e_loc, r_loc = e_block // RING, r_block // RING
    kc = wkv_t.shape[1]
    width = d_model // RING
    n_t = 3 * n_layers
    n_o = len(OTHERS)

    def dma(*shape):
        return pltpu.SemaphoreType.DMA(shape)

    def vm(*shape):
        return pltpu.VMEM(shape, BF)

    def out(*shape):
        return jax.ShapeDtypeStruct(shape, BF)

    any_spec = pl.BlockSpec(memory_space=pl.ANY)
    vm_spec = pl.BlockSpec(memory_space=pltpu.VMEM)
    out_shape = [
        out(batch, d_local, seq_len),
        out(n_layers, 2, seqs, seq_len, head_dim),
        out(n_layers, RING, RING, CORES, rows, d_model),
        out(n_layers, RING, RING * d_row, e_loc),
        out(n_layers, RING, RING, r_loc, d_col),
        out(RING, CORES, n_layers, RING, RING, kc, d_row),
        out(n_layers, RING, 2, seqs, CORES * (seq_len // (CORES * RING * RING * RING)), head_dim),
        out(n_layers, 2, d_row // 2, e_loc),
        out(n_layers, 2, r_loc // 2, d_col),
    ]
    pair = (2, 2, 2)
    each = (n_layers, *pair)
    scratch = [
        vm(rows, d_model), vm(rows, d_model), pltpu.VMEM((n_layers, d_model), F32),
        vm(RING, CORES, RING, RING, G_ROWS, d_row),
        vm(RING, seqs, d_local, seq_len),
        vm(CORES, RING, RING, RING, d_local, CORES * rows),
        vm(RING, RING * d_row, e_loc), vm(RING, RING, 2 * head_dim, d_row), vm(RING, RING, r_loc, d_col),
        vm(H_SLOTS, RING, CORES, rows, d_model), vm(RING, seq_len, r_loc), vm(2, 2, seq_len, head_dim), vm(seq_len, head_dim),
        vm(CORES * RING * rows, r_loc), vm(2, RING, rows, width), vm(2, 2, RING, RING, rows, width), vm(2, 2, RING, RING, rows, width),
        vm(*pair, 2, rows, width), vm(*pair, RING, rows, width), vm(*pair, rows // 2, width), vm(*pair, rows, width),
        dma(n_o), dma(n_o), dma(RING), dma(RING), dma(RING), dma(RING), pltpu.SemaphoreType.DMA,
        dma(3 * n_o), dma(3 * n_o), dma(RING), dma(RING),
        dma(RING), dma(RING), dma(2, RING), dma(2, RING), dma(RING, RING), dma(RING, RING), dma(RING),
        dma(n_layers, RING), dma(n_layers, 40), dma(n_layers), dma(n_layers, RING), pltpu.SemaphoreType.DMA, dma(H_SLOTS), dma(2, 2), dma(3), dma(3),
        dma(n_t, RING), dma(n_t, 2), dma(n_t, RING, 2), dma(n_t, RING, 2), dma(n_t, RING),
        dma(n_o), dma(n_o), pltpu.SemaphoreType.DMA, dma(n_o), dma(n_layers), dma(n_layers, n_o), dma(n_layers), dma(n_layers), dma(2),
        dma(n_layers, 2, 2, RING), dma(n_layers, 2, 2, RING),
        dma(*each), dma(*each), dma(*each, 2), dma(*each, 2), dma(*each), dma(*each), dma(*each), dma(*each),
        dma(n_layers, n_o), dma(n_layers, n_o), dma(n_layers),
    ]
    res = pl.pallas_call(
        model_kernel,
        out_shape=out_shape,
        in_specs=[any_spec, vm_spec, vm_spec, any_spec, any_spec, vm_spec, vm_spec],
        out_specs=[any_spec] * len(out_shape),
        scratch_shapes=scratch,
        compiler_params=pltpu.CompilerParams(collective_id=0, has_side_effects=True, vmem_limit_bytes=VMEM_LIMIT),
        name="two_layers",
    )(xt, gain, wkv_t, w_in, w_out, cos_full, sin_full)
    return res[0], res[6]


def solution(mesh):
    row_size = mesh.shape["row"]
    n_col = mesh.shape["col"]
    n_z = row_size // RING
    n_y = RING
    n_x = n_col // CORES
    n_tp = n_y * n_col
    n_dev = row_size * n_col
    mesh4 = Mesh(mesh.devices.reshape(n_z, n_y, n_x, CORES), ("z", "y", "x", "core"))
    every = ("z", "y", "x", "core")
    col = ("x", "core")
    act_spec = P(NIL, NIL, every)
    w_spec = P(NIL, ("z", "y"), col)

    def device_fn(x_loc, gain_loc, w_in_loc, w_kv_loc, w_out_loc):
        n_layers = w_in_loc.shape[0]
        n_batch, seq_len, d_local = x_loc.shape
        head_dim = w_kv_loc.shape[2] * n_col // 2
        batch_loc = n_batch // n_z
        seq_local = seq_len // n_dev
        steps = np.arange(head_dim // 2, dtype=np.float32)
        inv_freq = (1.0 / 10000.0 ** (steps * 2 / head_dim)).astype(np.float32)
        angles = np.arange(seq_len, dtype=np.float32)[:, NIL] * inv_freq[NIL, :]
        cos_tab, sin_tab = np.cos(angles), np.sin(angles)
        cos_full = jnp.asarray(np.concatenate([cos_tab, cos_tab], axis=1))
        sin_full = jnp.asarray(np.concatenate([-sin_tab, sin_tab], axis=1))
        y_loc, kv = run_model(x_loc.transpose(0, 2, 1), gain_loc, w_kv_loc.transpose(0, 2, 1), w_in_loc, w_out_loc, cos_full, sin_full)
        y_loc = y_loc.transpose(0, 2, 1)
        kv = kv.reshape(n_layers, n_z, 2, batch_loc, CORES, seq_local, head_dim)
        kv = lax.dynamic_index_in_dim(kv, lax.axis_index("core"), axis=4, keepdims=False)
        kv = kv.transpose(0, 2, 1, 3, 4, 5).reshape(n_layers, 2, n_batch, seq_local, head_dim)
        return y_loc, kv

    return jax.shard_map(device_fn, mesh=mesh4, in_specs=(act_spec, P(NIL, every), w_spec, w_spec, P(NIL, col, ("z", "y"))), out_specs=(act_spec, P(NIL, NIL, NIL, every, NIL)), check_vma=False)
```

```python
import typing

import jax
import jax.numpy as jnp
import numpy as np
from jax import lax
from jax.experimental import pallas as pl
from jax.experimental.pallas import tpu as pltpu
from jax.sharding import Mesh
from jax.sharding import PartitionSpec as P

LN_EPS = 1e-6
RING = 4
CORES = 2
VMEM_LIMIT = 67_000_000
BF = jnp.bfloat16
F32 = jnp.float32
SLOT_OFF = (2, 1, 3, 0)
SIGN = (1, -1)
NIL = None
BOTH = range(CORES)
RINGS = range(RING)
OTHERS = (1, 3, 2)
LAST = RING - 1
G_ROWS = 8
H_SLOTS = 3
QG0, UP0, WO0, QG1, UP1, WO1 = range(6)
OWN, AFTER, FAR, BEFORE = RINGS
FIRST_ORDER = ("a0", "b0", "a1", "b1", "c0", "c1", "d0", "d1", "e0", "e1")
LAST_ORDER = FIRST_ORDER[:-1] + ("f1", "e1", "g1", "f0", "g0", "h1", "h0")
KINDS = ("first", "second", "first_on", "second_on")


class Refs(typing.NamedTuple):
    xt: typing.Any
    gain_in: typing.Any
    wkv: typing.Any
    w_in: typing.Any
    w_out: typing.Any
    cos: typing.Any
    sin: typing.Any
    y_out: typing.Any
    kv_out: typing.Any
    h_all: typing.Any
    wi: typing.Any
    wo: typing.Any
    kvh: typing.Any
    kvx: typing.Any
    rwi: typing.Any
    rwo: typing.Any
    h_ref: typing.Any
    hid: typing.Any
    gain: typing.Any
    gbuf: typing.Any
    xz: typing.Any
    xp: typing.Any
    wv: typing.Any
    kvb: typing.Any
    wov: typing.Any
    hb: typing.Any
    joined: typing.Any
    qkv: typing.Any
    stage: typing.Any
    lhs: typing.Any
    away: typing.Any
    acc: typing.Any
    die_in: typing.Any
    in1: typing.Any
    in2: typing.Any
    in3: typing.Any
    in4: typing.Any
    xz_send: typing.Any
    xz_recv: typing.Any
    xp_send: typing.Any
    xp_recv: typing.Any
    xd_send: typing.Any
    xd_recv: typing.Any
    x_loc: typing.Any
    g_send: typing.Any
    g_recv: typing.Any
    gd_send: typing.Any
    gd_recv: typing.Any
    yd_send: typing.Any
    yd_recv: typing.Any
    yp_send: typing.Any
    yp_recv: typing.Any
    yz_send: typing.Any
    yz_recv: typing.Any
    y_loc: typing.Any
    ag_send: typing.Any
    ag_recv: typing.Any
    ag_dsend: typing.Any
    ag_drecv: typing.Any
    ag_loc: typing.Any
    h_sem: typing.Any
    kvo_sem: typing.Any
    w_load: typing.Any
    far_load: typing.Any
    y_recv: typing.Any
    ry_recv: typing.Any
    zb_recv: typing.Any
    zc_recv: typing.Any
    w_send: typing.Any
    kz_send: typing.Any
    kz_recv: typing.Any
    ky_send: typing.Any
    ky_recv: typing.Any
    kx_send: typing.Any
    kx_recv: typing.Any
    kd_send: typing.Any
    kd_recv: typing.Any
    k_loc: typing.Any
    dsend: typing.Any
    drecv: typing.Any
    rs_send: typing.Any
    recv1: typing.Any
    recv2: typing.Any
    recv3: typing.Any
    recv4: typing.Any
    kvx_send: typing.Any
    kvx_recv: typing.Any
    kvx_loc: typing.Any


def model_kernel(*refs):
    r = Refs(*refs)
    z, y, x, c = (lax.axis_index(a) for a in ("z", "y", "x", "core"))
    n_layers = r.wkv.shape[0]
    rows, d_model = r.hid.shape
    batch, d_local = r.xt.shape[:2]
    seqs = batch // RING
    seq_len, head_dim = r.cos.shape
    d_row = r.w_in.shape[1]
    e_loc = r.wi.shape[3]
    depth = r.wo.shape[3]
    f_loc = depth - head_dim
    quarter = rows // 4
    width = d_model // RING
    q_block = head_dim * RING
    f_block = f_loc * RING

    turned = {id(v): [lax.rem(v + o, RING) for o in RINGS] for v in (z, y, x)}

    def turn(base, off):
        if isinstance(off, int):
            return turned[id(base)][off % RING]
        return lax.rem(base + off + RING, RING)

    def remote(src, dst, ssem, rsem, dev):
        return pltpu.make_async_remote_copy(
            src_ref=src, dst_ref=dst, send_sem=ssem, recv_sem=rsem, device_id=dev, device_id_type=pl.DeviceIdType.MESH)

    partner = (z, y, x, 1 - c)

    peers = [(turn(z, o), y, x, c) for o in OTHERS]
    peers += [(z, turn(y, oy), turn(x, ox), c) for oy in RINGS for ox in RINGS if oy or ox]
    peers.append(partner)
    here = (z, y, x, c)
    gate_sem = pltpu.get_barrier_semaphore()
    for dev in peers:
        pl.semaphore_signal(gate_sem, inc=1, device_id=dev, device_id_type=pl.DeviceIdType.MESH)
    src_id = lax.broadcasted_iota(jnp.int32, (d_local, d_row), 0) + (x * CORES + c) * d_local
    dst_id = lax.broadcasted_iota(jnp.int32, (d_local, d_row), 1)
    spread = jnp.where(src_id == dst_id, 1.0, 0.0).astype(BF)
    r.gbuf[x, c, y, z] = jnp.zeros((G_ROWS, d_row), BF)
    r.gbuf[x, c, y, z, :n_layers] = jnp.dot(r.gain_in[...], spread, preferred_element_type=F32).astype(BF)
    pl.semaphore_wait(gate_sem, len(peers))

    def hook(pump, i):
        with jax.named_scope(f"hook_{i}"):
            pump(i)

    def w_cols(kind):
        return pl.ds(0, head_dim + f_loc) if kind == 0 else pl.ds(head_dim + f_loc, f_loc)

    def piece(t, zz, yy):
        l, kind = t // 3, t % 3
        if kind == 2:
            return r.wo.at[l, zz, yy]
        return r.wi.at[l, zz, pl.ds(pl.multiple_of(yy * d_row, d_row), d_row), w_cols(kind)]

    def piece_half(t, zz, yy, h):
        l, kind = t // 3, t % 3
        if kind == 2:
            return r.wo.at[l, zz, yy, pl.ds(h * (depth // 2), depth // 2)]
        return r.wi.at[l, zz, pl.ds(pl.multiple_of(yy * d_row + h * (d_row // 2), d_row // 2), d_row // 2), w_cols(kind)]

    def own_parts(t, owner, zz, yy):
        l, kind = t // 3, t % 3
        hq = pl.ds(pl.multiple_of(owner * head_dim, head_dim), head_dim)
        if kind == 2:
            return [
                (r.w_out.at[l, hq], r.wo.at[l, zz, yy, pl.ds(0, head_dim)]),
                (r.w_out.at[l, pl.ds(pl.multiple_of(q_block + owner * f_loc, head_dim), f_loc)], r.wo.at[l, zz, yy, pl.ds(head_dim, f_loc)]),
            ]
        rws = pl.ds(pl.multiple_of(yy * d_row, d_row), d_row)
        if kind == 0:
            return [
                (r.w_in.at[l, :, hq], r.wi.at[l, zz, rws, pl.ds(0, head_dim)]),
                (r.w_in.at[l, :, pl.ds(pl.multiple_of(q_block + owner * f_loc, head_dim), f_loc)], r.wi.at[l, zz, rws, pl.ds(head_dim, f_loc)]),
            ]
        return [(r.w_in.at[l, :, pl.ds(pl.multiple_of(q_block + f_block + owner * f_loc, head_dim), f_loc)],
                 r.wi.at[l, zz, rws, pl.ds(head_dim + f_loc, f_loc)])]

    def relay_ref(t, d):
        l, kind = t // 3, t % 3
        return r.rwo.at[l, d] if kind == 2 else r.rwi.at[l, d, :, w_cols(kind)]

    def far_parts(t, d):
        l, kind = t // 3, t % 3
        owner = turn(y, 2)
        hq = pl.ds(pl.multiple_of(owner * head_dim, head_dim), head_dim)
        if kind == 2:
            n = depth // 2
            base = q_block + owner * f_loc
            if d:
                return [(r.w_out.at[l, pl.ds(pl.multiple_of(base + n - head_dim, G_ROWS), n)], r.rwo.at[l, d])]
            return [
                (r.w_out.at[l, hq], r.rwo.at[l, d, pl.ds(0, head_dim)]),
                (r.w_out.at[l, pl.ds(pl.multiple_of(base, head_dim), n - head_dim)], r.rwo.at[l, d, pl.ds(head_dim, n - head_dim)]),
            ]
        rws = pl.ds(d * (d_row // 2), d_row // 2)
        if kind == 0:
            return [
                (r.w_in.at[l, rws, hq], r.rwi.at[l, d, :, pl.ds(0, head_dim)]),
                (r.w_in.at[l, rws, pl.ds(pl.multiple_of(q_block + owner * f_loc, head_dim), f_loc)], r.rwi.at[l, d, :, pl.ds(head_dim, f_loc)]),
            ]
        return [(r.w_in.at[l, rws, pl.ds(pl.multiple_of(q_block + f_block + owner * f_loc, head_dim), f_loc)], relay_ref(t, d))]

    def y_send(t):
        for d in BOTH:
            owner = turn(y, SIGN[d])
            dev = (z, owner, x, c)
            for src, dst in far_parts(t, d):
                remote(src, dst, r.w_send.at[t, 0], r.ry_recv.at[t, d], dev).start()
            for src, dst in own_parts(t, owner, z, y):
                remote(src, dst, r.w_send.at[t, 0], r.y_recv.at[t, -SIGN[d] % RING], dev).start()

    def y_relay(t):
        for d in BOTH:
            ref = relay_ref(t, d)
            remote(ref, ref, r.w_send.at[t, 3], r.ry_recv.at[t, d], here).wait_recv()
            dst = piece_half(t, z, turn(y, -SIGN[d]), d)
            remote(ref, dst, r.w_send.at[t, 3], r.y_recv.at[t, 2], (z, turn(y, SIGN[d]), x, c)).start()

    def z_own(t):
        for d in BOTH:
            for src, dst in own_parts(t, y, z, y):
                remote(src, dst, r.w_send.at[t, 1], r.zb_recv.at[t % 3, 0, d], (turn(z, SIGN[d]), y, x, c)).start()

    def z_direct(t, j):
        yy = turn(y, j)
        ref = piece(t, z, yy)
        remote(ref, ref, r.w_send.at[t, 0], r.y_recv.at[t, j], here).wait_recv()
        for d in BOTH:
            remote(ref, ref, r.w_send.at[t, 1], r.zb_recv.at[t % 3, j, d], (turn(z, SIGN[d]), y, x, c)).start()

    def z_forward(t, j):
        yy = turn(y, j)
        for d in BOTH:
            zz = turn(z, -SIGN[d])
            ref = piece(t, zz, yy)
            remote(ref, ref, r.w_send.at[t, 1], r.zb_recv.at[t % 3, j, d], here).wait_recv()
            part = piece_half(t, zz, yy, d)
            remote(part, part, r.w_send.at[t, 2], r.zc_recv.at[t % 3, j, d], (turn(z, SIGN[d]), y, x, c)).start()

    def place(t, zz):
        l, kind = t // 3, t % 3
        if kind == 2:
            return r.wo.at[l, zz], r.wov.at[zz]
        return r.wi.at[l, zz, :, w_cols(kind)], r.wv.at[zz, :, w_cols(kind)]

    def load_near(t):
        kind = t % 3
        for d in BOTH:
            src, dst = place(t, turn(z, SIGN[d]))
            pltpu.make_async_copy(src, dst, r.w_load.at[kind]).start()
        for j in OTHERS:
            yy = turn(y, j)
            dst = r.wov.at[z, yy] if kind == 2 else r.wv.at[z, pl.ds(pl.multiple_of(yy * d_row, d_row), d_row), w_cols(kind)]
            pltpu.make_async_copy(piece(t, z, yy), dst, r.w_load.at[kind]).start()
        for src, dst in own_parts(t, y, z, y):
            pltpu.make_async_copy(src, own_place(t, dst, src), r.w_load.at[kind]).start()

    def load_far(t):
        far = turn(z, 2)
        for j in RINGS:
            for d in BOTH:
                part = piece_half(t, far, turn(y, j), d)
                remote(part, part, r.w_send.at[t, 2], r.zc_recv.at[t % 3, j, d], here).wait_recv()
        src, dst = place(t, far)
        pltpu.make_async_copy(src, dst, r.far_load.at[t % 3]).start()

    def own_place(t, dst, src):
        kind = t % 3
        if kind == 2:
            n = src.shape[0]
            return r.wov.at[z, y, pl.ds(0 if n == head_dim and f_loc != head_dim else head_dim, n)]
        n = src.shape[1]
        rws = pl.ds(pl.multiple_of(y * d_row, d_row), d_row)
        if kind == 0:
            return r.wv.at[z, rws, pl.ds(0 if n == head_dim and f_loc != head_dim else head_dim, n)]
        return r.wv.at[z, rws, pl.ds(head_dim + f_loc, f_loc)]

    def finish(t):
        load_near(t)
        load_far(t)

    def near_loaded(t):
        kind = t % 3
        dst = r.wov.at[pl.ds(0, LAST)] if kind == 2 else r.wv.at[pl.ds(0, LAST), :, w_cols(kind)]
        pltpu.make_async_copy(dst, dst, r.w_load.at[kind]).wait()

    def far_loaded(t):
        kind = t % 3
        dst = r.wov.at[0] if kind == 2 else r.wv.at[0, :, w_cols(kind)]
        pltpu.make_async_copy(dst, dst, r.far_load.at[kind]).wait()

    def loaded(t):
        near_loaded(t)
        far_loaded(t)

    def drain(t):
        l, kind = t // 3, t % 3
        if kind == 2:
            done = (r.wo.at[l, 0, pl.ds(0, LAST)], r.wo.at[l, pl.ds(0, 2)], r.wo.at[l, 0], r.wo.at[l, 0, 0])
        else:
            cols = w_cols(kind)
            done = (r.wi.at[l, 0, pl.ds(0, LAST * d_row), cols], r.wi.at[l, pl.ds(0, 2), :, cols], r.wi.at[l, 0, :, cols],
                    r.wi.at[l, 0, pl.ds(0, d_row), cols])
        for g, ref in enumerate(done):
            remote(ref, ref, r.w_send.at[t, g], r.y_recv.at[t, 0], here).wait_send()

    def kv_z_copy(k):
        return remote(r.wkv, r.kvh.at[x, c, :, y, z], r.kz_send.at[k], r.kz_recv.at[k], (turn(z, OTHERS[k]), y, x, c))

    def kv_own():
        return pltpu.make_async_copy(r.wkv, r.kvh.at[x, c, :, y, z], r.k_loc.at[0])

    def kv_z():
        for k in range(len(OTHERS)):
            kv_z_copy(k).start()
        kv_own().start()

    def kv_y_copy(ref, k, d):
        return remote(ref, ref, r.ky_send, r.ky_recv.at[k], (z, turn(y, SIGN[d]), x, c))

    def kv_y1():
        kv_own().wait()
        for k in range(len(OTHERS)):
            kv_z_copy(k).wait()
        for d in BOTH:
            kv_y_copy(r.kvh.at[x, c, :, y], d, d).start()

    def kv_y2():
        for d in BOTH:
            yy = turn(y, -SIGN[d])
            kv_y_copy(r.kvh.at[x, c, :, yy], d, d).wait_recv()
            kv_y_copy(r.kvh.at[x, c, :, yy, pl.ds(2 * d, 2)], 2, d).start()

    def kv_y3():
        kv_y_copy(r.kvh.at[x, c, :, turn(y, 2)], 2, 0).wait_recv()
        kv_y_copy(r.kvh.at[x, c, :, pl.ds(0, LAST)], 0, 0).wait_send()

    def kv_x_copy(l, ref, k, d):
        return remote(ref, ref, r.kx_send.at[l], r.kx_recv.at[l, k], (z, y, turn(x, SIGN[d]), c))

    def kv_die(l, ref):
        return remote(ref, ref, r.kd_send.at[l], r.kd_recv.at[l], partner)

    def kv_x1(l):
        ref = r.kvh.at[x, c, l]
        for d in BOTH:
            kv_x_copy(l, ref, d, d).start()
        kv_die(l, ref).start()

    def kv_x2(l):
        for d in BOTH:
            xx = turn(x, -SIGN[d])
            ref = r.kvh.at[xx, c, l]
            kv_x_copy(l, ref, d, d).wait_recv()
            kv_x_copy(l, r.kvh.at[xx, c, l, pl.ds(2 * d, 2)], 2, d).start()
            kv_die(l, ref).start()

    def kv_x3(l):
        ref = r.kvh.at[turn(x, 2), c, l]
        kv_x_copy(l, ref, 2, 0).wait_recv()
        kv_die(l, ref).start()

    def kv_load(l):
        kv_die(l, r.kvh.at[:, 1 - c, l]).wait_recv()
        kc = r.wkv.shape[1]
        for xx in RINGS:
            for cc in BOTH:
                pltpu.make_async_copy(r.kvh.at[xx, cc, l], r.kvb.at[:, :, pl.ds((xx * CORES + cc) * kc, kc)], r.k_loc.at[1]).start()

    def kv_sent(l):
        kv_x_copy(l, r.kvh.at[pl.ds(0, LAST), c, l], 0, 0).wait_send()
        kv_die(l, r.kvh.at[:, c, l]).wait_send()

    def kv_loaded():
        pltpu.make_async_copy(r.kvb, r.kvb, r.k_loc.at[1]).wait()

    def gain_move(i, src, dst, dev):
        return remote(src, dst, r.g_send.at[i], r.g_recv.at[i], dev)

    def gain_z(k):
        dev = (turn(z, OTHERS[k]), y, x, c)
        return gain_move(k, r.gbuf.at[x, c, y, z], r.gbuf.at[x, c, y, z], dev)

    def gain_y(k):
        dev = (z, turn(y, OTHERS[k]), x, c)
        return gain_move(len(OTHERS) + k, r.gbuf.at[x, c, y], r.gbuf.at[x, c, y], dev)

    def gain_x(k):
        dev = (z, y, turn(x, OTHERS[k]), c)
        return gain_move(CORES * len(OTHERS) + k, r.gbuf.at[x, c], r.gbuf.at[x, c], dev)

    def gain_die(xx, k):
        ref = r.gbuf.at[xx, c]
        return remote(ref, ref, r.gd_send.at[k], r.gd_recv.at[k], partner)

    def gain_sum():
        for zz in RINGS:
            for yy in RINGS:
                tot = jnp.zeros((n_layers, d_row), F32)
                for xx in RINGS:
                    for cc in BOTH:
                        tot += r.gbuf[xx, cc, yy, zz, :n_layers].astype(F32)
                at = (zz * RING + yy) * d_row
                r.gain[:, at:at + d_row] = tot

    tok_pair = CORES * rows

    def x_z(k):
        zz = turn(z, OTHERS[k])
        src = r.xt.at[pl.ds(zz * seqs, seqs)]
        return remote(src, r.xz.at[z], r.xz_send.at[k], r.xz_recv.at[k], (zz, y, x, c))

    def x_own():
        return pltpu.make_async_copy(r.xt.at[pl.ds(z * seqs, seqs)], r.xz.at[z], r.x_loc)

    def pos(xx):
        return pl.ds(pl.multiple_of(xx * tok_pair, tok_pair), tok_pair)

    def x_plane(oy, ox):
        yy, xx = turn(y, oy), turn(x, ox)
        return remote(r.xz.at[:, yy, :, pos(xx)], r.xp.at[c, y, x], r.xp_send.at[oy], r.xp_recv.at[(RING - oy) % RING], (z, yy, xx, c))

    def row_bytes(oy):
        return r.xp.at[c, 0] if oy else r.xp.at[c, 0, pl.ds(0, RING - 1)]

    def x_row(oy):
        yy = turn(y, oy)
        got = row_bytes(oy)
        remote(got, got, r.xp_send.at[oy], r.xp_recv.at[oy], partner).wait_recv()
        row = r.xp.at[c, yy]
        remote(row, row, r.xd_send.at[oy], r.xd_recv.at[oy], partner).start()

    def x_turn():
        for oy in RINGS:
            row = r.xp.at[1 - c, turn(y, oy)]
            remote(row, row, r.xd_send.at[oy], r.xd_recv.at[oy], partner).wait_recv()

        @pl.loop(0, RING)
        def _(zz):
            for yy in RINGS:
                for xh in BOTH:
                    blk = [r.xp[cc, yy, CORES * xh + xx, zz] for xx in BOTH for cc in BOTH]
                    blk = jnp.concatenate(blk, axis=0).astype(F32).T.astype(BF)
                    n = blk.shape[1]
                    at = pl.multiple_of(zz * RING * d_row + yy * d_row + xh * n, n)
                    r.hb[0, 0, :, :, pl.ds(at, n)] = blk.reshape(CORES, rows, n)
        r.hid[...] = r.hb[0, 0, c]
        for oy in RINGS:
            row = r.xp.at[c, turn(y, oy)]
            remote(row, row, r.xd_send.at[oy], r.xd_recv.at[oy], partner).wait_send()

    def x_sent():
        for fn in (x_z, gain_z, gain_y, gain_x):
            peers_of(fn, "wait_send")
        for k in RINGS:
            gain_die(x, k).wait_send()
        for oy in RINGS:
            got = row_bytes(oy)
            remote(got, got, r.xp_send.at[oy], r.xp_recv.at[oy], partner).wait_send()

    def y_die(p):
        cols = pl.ds(pl.multiple_of(turn(z, p) * width, width), width)
        return remote(r.hid.at[:, cols], r.hb.at[0, 0, c, :, cols], r.yd_send.at[p], r.yd_recv.at[p], partner)

    def planes(h):
        return pl.ds(2 * h, 2)

    def y_plane(h, oy, ox):
        yy, xx = turn(y, oy), turn(x, ox)
        return remote(r.xp.at[c, yy, xx, planes(h)], r.xz.at[planes(h), y, :, pos(x)], r.yp_send.at[h, oy], r.yp_recv.at[h, (RING - oy) % RING],
                      (z, yy, xx, c))

    def y_z(p, oy):
        s = turn(y, oy)
        return remote(r.xz.at[p, s], r.y_out.at[z * seqs + s], r.yz_send.at[p], r.yz_recv.at[p], (turn(z, p), y, x, c))

    def y_own(oy):
        s = turn(y, oy)
        return pltpu.make_async_copy(r.xz.at[0, s], r.y_out.at[z * seqs + s], r.y_loc)

    def leave_a(h):
        for p in BOTH:
            p = 2 * h + p
            y_die(p).start()
            cols = pl.ds(pl.multiple_of(turn(z, p) * width, width), width)
            r.hb[0, 0, c, :, cols] = r.hid[:, cols]

    def leave_b(h):
        n = CORES * CORES * d_local
        for p in BOTH:
            p = 2 * h + p
            y_die(p).wait()

            @pl.loop(0, RING)
            def _(yy, p=p):
                for xh in BOTH:
                    at = pl.multiple_of(turn(z, p) * width + yy * d_row + xh * n, n)
                    blk = r.hb[0, 0, :, :, pl.ds(at, n)].reshape(tok_pair, n).astype(F32).T.astype(BF)
                    for xx in BOTH:
                        for cc in BOTH:
                            lo = (xx * CORES + cc) * d_local
                            r.xp[cc, yy, CORES * xh + xx, p] = blk[lo:lo + d_local]

        for oy in OTHERS + (0,):
            for ox in RINGS:
                if oy or ox:
                    y_plane(h, oy, ox).start()
        for p in BOTH:
            p = 2 * h + p
            r.xz[p, y, :, pos(x)] = r.xp[c, y, x, p]

    def plane_bytes(h, oy):
        return r.xp.at[c, 0, :, planes(h)] if oy else r.xp.at[c, 0, pl.ds(0, LAST), planes(h)]

    def leave_c(h):
        for oy in OTHERS + (0,):
            got = plane_bytes(h, oy)
            remote(got, got, r.yp_send.at[h, oy], r.yp_recv.at[h, oy], partner).wait_recv()
            for p in BOTH:
                p = 2 * h + p
                (y_z(p, oy) if p else y_own(oy)).start()

    def left():
        for oy in RINGS:
            for h in BOTH:
                got = plane_bytes(h, oy)
                remote(got, got, r.yp_send.at[h, oy], r.yp_recv.at[h, oy], partner).wait_send()
        for p in OTHERS:
            ref = r.xz.at[p]
            remote(ref, ref, r.yz_send.at[p], r.yz_recv.at[p], here).wait()
        pltpu.make_async_copy(r.xz.at[0], r.xz.at[0], r.y_loc).wait()

    def kv_rows(zz):
        n = CORES * seq_len // (RING * RING * RING * CORES)
        return pl.ds(pl.multiple_of(((zz * RING + y) * RING + x) * n, n), n)

    def kv_trade(l, k):
        zz = turn(z, OTHERS[k])
        return remote(r.kv_out.at[l, :, :, kv_rows(zz)], r.kvx.at[l, z], r.kvx_send.at[l, k], r.kvx_recv.at[l, k], (zz, y, x, c))

    def kv_keep(l):
        return pltpu.make_async_copy(r.kv_out.at[l, :, :, kv_rows(z)], r.kvx.at[l, z], r.kvx_loc.at[l])

    def kv_share(l):
        for k in range(len(OTHERS)):
            kv_trade(l, k).start()
        kv_keep(l).start()

    def kv_shared(l):
        for k in range(len(OTHERS)):
            kv_trade(l, k).wait()
        kv_keep(l).wait()

    def gather_norm(l, split, pump):
        hid = r.hid
        gain = r.gain[l:l + 1, :]
        for b in range(4):
            blk = hid[b * quarter:(b + 1) * quarter, :].astype(F32)
            mean = jnp.mean(blk, axis=-1, keepdims=True)
            cen = blk - mean
            var = jnp.mean(cen * cen, axis=-1, keepdims=True)
            r.h_ref[b * quarter:(b + 1) * quarter, :] = (cen * lax.rsqrt(var + LN_EPS) * gain).astype(BF)
        out = r.h_all.at[l]

        def spot(q, first, second):
            if q == 0:
                return turn(y, second), turn(x, first)
            return turn(y, first), turn(x, second)

        def span(q, part):
            lo, n = (split, rows - split) if q else (0, split)
            if part is NIL:
                return pl.ds(lo, n)
            return pl.ds(lo + part * (n // 2), n // 2)

        offs = (0, -1, 1, 2)
        plans = {}
        for q in BOTH:
            for d in BOTH:
                plans["first", q, d] = (q, 0, 0, NIL, SIGN[d], 0)
                plans["first_on", q, d] = (q, -SIGN[d], 0, d, SIGN[d], 0)
                for k in RINGS:
                    plans["second", q, k, d] = (q, offs[k], 0, NIL, 0, SIGN[d])
                    plans["second_on", q, k, d] = (q, offs[k], -SIGN[d], d, 0, SIGN[d])
        index = {key: n for n, key in enumerate(plans)}

        def link(*key, own=False):
            idx, (q, first, second, part, to_first, to_second) = index[key], plans[key]
            sy, sx = spot(q, first, second)
            ty, tx = spot(q, to_first, to_second)
            rws = span(q, part)
            dst = out.at[sy, sx, c, rws]
            return remote(r.h_ref.at[rws] if own else dst, dst, r.ag_send.at[KINDS.index(key[0])], r.ag_recv.at[idx], (z, ty, tx, c))

        def arrived(*key):
            for d in BOTH:
                link(*key, d).wait_recv()

        def die(q, first, second, own=False):
            sy, sx = spot(q, first, second)
            rws = span(q, NIL)
            dst = out.at[sy, sx, c, rws]
            off = (first if q else second) % RING
            remote(r.h_ref.at[rws] if own else dst, dst, r.ag_dsend, r.ag_drecv.at[off], partner).start()

        def take(k, q):
            for d in BOTH:
                link("second", q, k, d).wait_recv()
                die(q, offs[k], -SIGN[d])

        def pass_on(k, q):
            for d in BOTH:
                link("second_on", q, k, d).start()

        def second_step(k):
            take(k, 1)
            pass_on(k, 1)
            take(k, 0)

        def far_first(q):
            for e in BOTH:
                link("second", q, LAST, e).start()

        def last_step(q, k):
            arrived("second_on", q, k)
            die(q, offs[k], 2)

        def tail_a():
            second_step(2)
            far_first(1)
            for k in RINGS[:-1]:
                pass_on(k, 0)
            hook(pump, "k2")
            take(LAST, 0)
            pass_on(LAST, 0)
            hook(pump, "k3")
            for k in (1, 2):
                last_step(1, k)

        def tail_b():
            take(LAST, 1)
            pass_on(LAST, 1)

        def tail_c():
            for k in RINGS:
                last_step(0, k)
            last_step(1, LAST)

        for q in BOTH:
            for d in BOTH:
                link("first", q, d, own=True).start()
        for q in BOTH:
            for d in BOTH:
                link("second", q, 0, d, own=True).start()
        for q in BOTH:
            die(q, 0, 0, own=True)
        own = pltpu.make_async_copy(r.h_ref, out.at[y, x, c], r.ag_loc)
        own.start()
        hook(pump, "begin")
        for d in BOTH:
            for q in BOTH:
                link("first", q, d).wait_recv()
                src = -SIGN[d]
                link("first_on", q, d).start()
                die(q, src, 0)
        hook(pump, "first")
        second_step(0)
        for q in reversed(BOTH):
            for d in BOTH:
                for e in BOTH:
                    link("second", q, 1 + d, e).start()
        hook(pump, "k0")
        for q in BOTH:
            arrived("first_on", q)
            die(q, 2, 0)
        far_first(0)
        hook(pump, "first_on")
        last_step(1, 0)
        own.wait()
        hook(pump, "ready")

        def crossed(off):
            got = out.at[turn(y, off), :, 1 - c]
            remote(got, got, r.ag_dsend, r.ag_drecv.at[off], partner).wait_recv()

        def order(i):
            if isinstance(i, int):
                return (OWN, BEFORE, AFTER, FAR)[i]
            return lax.rem(3 * i + 3 * (i // 2) + 2 * (i // 3), RING)

        def fetch(i, slot):
            off = order(i)
            crossed(off)
            h_copy(l, turn(y, off), slot).start()

        def up_ready():
            hook(pump, "up")
            loaded(UP1 if l else UP0)

        crossed(0)
        h_copy(l, y, 0).start()

        def opening():
            second_step(1)
            hook(pump, "k1")

        def turn_of(i):
            slot = lax.rem(i, H_SLOTS)
            s = turn(y, order(i))
            h_copy(l, s, slot).wait()
            pump(("seq", i))
            one(l, s, slot, i)

            @pl.when(i == 1)
            def _():
                tail_b()

            @pl.when(i == 2)
            def _():
                tail_c()
                fetch(LAST, 0)

            return s, slot

        def neighbours():
            tail_a()
            for n in (1, 2):
                fetch(n, n)

        if l:
            @pl.loop(0, RING)
            def _(i):
                s, slot = turn_of(i)

                @pl.when(i == 0)
                def _():
                    opening()
                    up_ready()

                pump(("two", i))
                two(s, slot)

                @pl.when(i == 0)
                def _():
                    neighbours()
        else:
            h_copy(l, y, 0).wait()
            hook(pump, "own")
            one(l, y, 0, 0)
            opening()
            neighbours()

            @pl.loop(1, RING)
            def _(i):
                turn_of(i)

                @pl.when(i == 1)
                def _():
                    up_ready()

                pump(("two", i - 1))
                two(turn(y, order(i - 1)), lax.rem(i - 1, H_SLOTS))

            hook(pump, "two3")
            two(turn(y, FAR), 0)

        for slot in BOTH:
            for i in BOTH:
                kv_out_copy(l, 0, slot, i).wait()
        sent = (out.at[y, x], out.at[y], out.at[y, x, c], out.at[y, pl.ds(0, CORES)])
        for kind, ref in enumerate(sent):
            remote(ref, ref, r.ag_send.at[kind], r.ag_recv.at[kind], partner).wait_send()
        remote(out.at[pl.ds(0, 2)], out.at[pl.ds(0, 2)], r.ag_dsend, r.ag_drecv.at[0], partner).wait_send()

    def h_copy(l, s, slot):
        return pltpu.make_async_copy(r.h_all.at[l, s], r.hb.at[slot], r.h_sem.at[slot])

    def h_tile(slot):
        return r.hb[slot].reshape(seq_len, d_model)

    def project(h, lo, n):
        w = r.wv[:, :, lo:lo + n].reshape(d_model, n)
        return jnp.dot(h, w, preferred_element_type=F32).astype(BF)

    def rope(val):
        val = val.astype(F32)
        return val * r.cos[...] + pltpu.roll(val, head_dim // 2, 1) * r.sin[...]

    n_chunk = min(256, f_loc)

    def kv_out_copy(l, s, slot, i):
        return pltpu.make_async_copy(r.qkv.at[slot, i], r.kv_out.at[l, i, s], r.kvo_sem.at[slot, i])

    def one(l, s, slot, i):
        pair = i % 2 if isinstance(i, int) else lax.rem(i, 2)

        @pl.when(i >= 2)
        def _():
            for k in BOTH:
                kv_out_copy(l, s, pair, k).wait()

        kv = jnp.zeros((seq_len, 2 * head_dim), F32)
        for zz in RINGS:
            for yy in RINGS:
                col = (zz * RING + yy) * d_row
                kv += lax.dot_general(h_cols(slot, col, d_row), r.kvb[yy, zz], (((1,), (1,)), ((), ())), preferred_element_type=F32)
        kv = kv.astype(BF)
        r.qkv[pair, 0] = rope(kv[:, :head_dim]).astype(BF)
        r.qkv[pair, 1] = kv[:, head_dim:]
        for i in BOTH:
            kv_out_copy(l, s, pair, i).start()
        q = project(h_tile(slot), 0, head_dim)
        r.stage[...] = (rope(q) * head_dim ** -0.5).astype(BF)
        for lo in range(0, f_loc, n_chunk):
            r.joined[s, :, head_dim + lo:head_dim + lo + n_chunk] = project(h_tile(slot), head_dim + lo, n_chunk)
        n_tile = seq_len // 2
        for i in BOTH:
            keys = (i + 1) * n_tile
            sc = lax.dot_general(r.stage[i * n_tile:(i + 1) * n_tile, :], r.qkv[pair, 0, :keys, :], (((1,), (1,)), ((), ())), preferred_element_type=F32)
            row_id = lax.broadcasted_iota(jnp.int32, sc.shape, 0) + i * n_tile
            col_id = lax.broadcasted_iota(jnp.int32, sc.shape, 1)
            sc = jnp.where(col_id <= row_id, sc, -1e30)
            top = jnp.max(sc, axis=-1, keepdims=True)
            ex = jnp.exp(sc - top)
            prob = (ex * (1.0 / jnp.sum(ex, axis=-1, keepdims=True))).astype(BF)
            att = jnp.dot(prob, r.qkv[pair, 1, :keys, :], preferred_element_type=F32)
            r.joined[s, i * n_tile:(i + 1) * n_tile, :head_dim] = att.astype(BF)

    def h_cols(slot, col, n):
        return r.hb[slot, :, :, :, col:col + n].reshape(seq_len, n)

    def two(s, slot):
        for lo in range(0, f_loc, n_chunk):
            up = project(h_tile(slot), head_dim + f_loc + lo, n_chunk).astype(F32)
            cols = slice(head_dim + lo, head_dim + lo + n_chunk)
            g = r.joined[s, :, cols].astype(F32)
            r.joined[s, :, cols] = (g * jax.nn.sigmoid(g) * up).astype(BF)

    def out_scatter(l, pump):
        def peer(q, first, second):
            dy = first * (1 - q) + second * q
            dx = first * q + second * (1 - q)
            return (z, turn(y, dy), turn(x, dx), c)

        def die_copy(ch, q, s):
            return remote(r.away.at[q], r.die_in.at[ch, q, s], r.dsend.at[q], r.drecv.at[ch, q, s], partner)

        def first_copy(ch, q, d):
            return remote(r.acc.at[ch, q, 0, pl.ds(CORES * d, CORES)], r.in1.at[ch, q, d], r.rs_send.at[0], r.recv1.at[ch, q, d],
                          peer(q, SIGN[d], 0))

        def second_copy(ch, q, d, h):
            js = pl.ds(CORES * h, CORES)
            return remote(r.acc.at[ch, q, 1 + d, js], r.in2.at[ch, q, d, js], r.rs_send.at[1], r.recv2.at[ch, q, d, h],
                          peer(q, SIGN[d], 0))

        def half_rows(d):
            return pl.ds(d * (rows // 2), rows // 2)

        def third_copy(ch, q, d):
            return remote(r.acc.at[ch, q, LAST, 0, half_rows(d)], r.in3.at[ch, q, d], r.rs_send.at[2], r.recv3.at[ch, q, d],
                          peer(q, 0, SIGN[d]))

        def fourth_copy(ch, q, d):
            return remote(r.acc.at[ch, q, LAST, 1 + d], r.in4.at[ch, q, d], r.rs_send.at[LAST], r.recv4.at[ch, q, d],
                          peer(q, 0, SIGN[d]))

        n_blk = r.wov.shape[3]

        def plane_of(ch, q):
            if l:
                return turn(z, q if ch else 2 + q)
            return turn(z, LAST - q if ch else q)

        def slot_off(s):
            return lax.rem(2 + 3 * s + 3 * (s // 2) + 2 * (s // 3), RING)

        def tile(ch, q, s):
            off = slot_off(s)
            for cc in BOTH:
                for j in RINGS:
                    oy = off * (1 - q) + SLOT_OFF[j] * q
                    ox = SLOT_OFF[j] * (1 - q) + off * q
                    core = c if cc else 1 - c
                    at = pl.multiple_of((turn(x, ox) * CORES + core) * rows, rows)
                    r.lhs[pl.ds((cc * RING + j) * rows, rows), :] = r.joined[turn(y, oy), pl.ds(at, rows), :]
            left = r.lhs[...]
            zz = plane_of(ch, q)
            for n in RINGS:
                res = jnp.dot(left, r.wov[zz, n], preferred_element_type=F32).astype(BF)
                res = res.reshape(CORES, RING, rows, n_blk)
                r.away[q, :, :, n * n_blk:(n + 1) * n_blk] = res[0]
                r.acc[ch, q, s, :, :, n * n_blk:(n + 1) * n_blk] = res[1]

        def pair_sum(ch, q, s):
            die_copy(ch, q, s).wait_recv()

            @pl.loop(0, RING)
            def _(j):
                r.acc[ch, q, s, j] = r.acc[ch, q, s, j] + r.die_in[ch, q, s, j]

        def stage_a(ch):
            @pl.loop(0, CORES * RING)
            def _(t):
                s = t // CORES
                q = lax.rem(t, CORES)

                @pl.when(s >= 1)
                def _():
                    die_copy(ch, q, s - 1).wait_send()

                if ch:
                    @pl.when(s == 0)
                    def _():
                        die_copy(ch - 1, q, LAST).wait_send()

                tile(ch, q, s)
                die_copy(ch, q, s).start()

                @pl.when(s >= 1)
                def _():
                    pair_sum(ch, q, s - 1)

                @pl.when(s == 1)
                def _():
                    for d in BOTH:
                        first_copy(ch, q, d).start()

                for d in BOTH:
                    @pl.when(s == 2 + d)
                    def _(d=d):
                        second_copy(ch, q, d, 1 - d).start()

                for n in RINGS:
                    name = f"a{ch}s{n}"
                    if pump(name, False):
                        @pl.when(t == CORES * n + 1)
                        def _(name=name):
                            hook(pump, name)

        def stage_b(ch):
            for q in BOTH:
                pair_sum(ch, q, LAST)
            for q in BOTH:
                for d in BOTH:
                    first_copy(ch, q, d).wait_recv()
                    for j in BOTH:
                        at = CORES * d + j
                        r.acc[ch, q, 1 + d, at] = r.acc[ch, q, 1 + d, at] + r.in1[ch, q, d, j]
                    second_copy(ch, q, d, d).start()

        def total(ch, q, j):
            val = r.acc[ch, q, LAST, j].astype(F32)
            for d in BOTH:
                val += r.in2[ch, q, d, j].astype(F32)
            r.acc[ch, q, LAST, j] = val.astype(BF)

        def stage_c(ch):
            for q in BOTH:
                for h in BOTH:
                    for d in BOTH:
                        second_copy(ch, q, d, h).wait_recv()
                total(ch, q, 0)
                for d in BOTH:
                    third_copy(ch, q, d).start()
                for j in RINGS[1:]:
                    total(ch, q, j)

        def stage_d(ch):
            for q in BOTH:
                for d in BOTH:
                    third_copy(ch, q, d).wait_recv()
                    rws = half_rows(d)
                    r.acc[ch, q, LAST, 1 + d, rws] = r.acc[ch, q, LAST, 1 + d, rws] + r.in3[ch, q, d]
                    fourth_copy(ch, q, d).start()

        def stage_e(ch):
            for q in BOTH:
                for d in BOTH:
                    fourth_copy(ch, q, d).wait_recv()
                cols = pl.ds(pl.multiple_of(plane_of(ch, q) * width, width), width)
                upd = r.acc[ch, q, LAST, LAST].astype(F32)
                for d in BOTH:
                    upd += r.in4[ch, q, d].astype(F32)
                upd = upd.astype(BF)
                r.hid[:, cols] = (r.hid[:, cols].astype(F32) + upd.astype(F32)).astype(BF)

        stages = {"a": stage_a, "b": stage_b, "c": stage_c, "d": stage_d, "e": stage_e, "f": leave_a, "g": leave_b, "h": leave_c}
        for step in LAST_ORDER if l else FIRST_ORDER:
            with jax.named_scope(step):
                stages[step[0]](int(step[1]))
            hook(pump, step)
        for q in BOTH:
            die_copy(1, q, LAST).wait_send()
        for n, ref in enumerate((r.in1, r.in2, r.in3, r.in4)):
            remote(ref, ref, r.rs_send.at[n], r.drecv.at[0, 0, 0], here).wait_send()

    def near(fn, t):
        for j in (LAST, 1):
            fn(t, j)

    def far(fn, t):
        fn(t, 2)

    def z_all(t):
        near(z_direct, t)
        far(z_direct, t)

    def peers_of(fn, op="start"):
        for k in range(len(OTHERS)):
            getattr(fn(k), op)()

    def start(pump):
        peers_of(gain_z)
        kv_z()
        peers_of(x_z)
        x_own().start()
        pump("s0")
        with jax.named_scope("gain_a"):
            peers_of(gain_z, "wait_recv")
            peers_of(gain_y)
            kv_y1()
        pump("s1")
        with jax.named_scope("gain_b"):
            peers_of(gain_y, "wait_recv")
            peers_of(gain_x)
            gain_die(x, LAST).start()
        pump("s2")
        with jax.named_scope("x_z"):
            peers_of(x_z, "wait_recv")
            x_own().wait()
        for oy in RINGS:
            for ox in RINGS:
                if oy or ox:
                    x_plane(oy, ox).start()
        r.xp[c, y, x] = r.xz[:, y, :, pos(x)]
        pump("s3")
        with jax.named_scope("kv_b"):
            kv_y2()
        with jax.named_scope("gain_c"):
            for k, o in enumerate(OTHERS):
                gain_x(k).wait_recv()
                gain_die(turn(x, -o), k).start()
        pump("s4")
        for oy in (OWN, BEFORE, AFTER, FAR):
            with jax.named_scope(f"row_{oy}"):
                x_row(oy)
            pump(f"r{oy}")
        pump("s5")
        kv_y3()
        pump("s6")
        with jax.named_scope("gain_sum"):
            for k in RINGS:
                gain_die(x, k).wait_recv()
            gain_sum()
        with jax.named_scope("turn"):
            x_turn()
        pump("s7")

    def when(i, n, *fns):
        @pl.when(i == n)
        def _():
            for fn in fns:
                fn()

    def plan(steps):
        def pump(step, run=True):
            if not isinstance(step, str):
                for n in RINGS:
                    if (step[0], n) in steps:
                        when(step[1], n, lambda n=n: run_steps(steps[step[0], n]))
                return True
            found = steps.get(step, ())
            if run:
                run_steps(found)
            return found
        return pump

    def run_steps(steps):
        for fn, *args in steps:
            with jax.named_scope(f"{fn.__name__}_{args[-1] if args else 0}"):
                fn(*args)

    first_entry = plan({
        "s0": [(z_own, UP0)],
        "s1": [(y_send, QG0)],
        "s3": [(z_own, QG0)],
        "r0": [(y_relay, QG0), (z_forward, UP0, OWN), (z_direct, QG0, AFTER), (z_forward, QG0, OWN), (z_direct, QG0, BEFORE)],
        "s6": [(kv_x1, 0)],
    })
    first_front = plan({
        "begin": [(kv_x2, 0), (y_send, UP0), (z_forward, QG0, AFTER), (z_direct, QG0, FAR)],
        "k0": [(y_relay, UP0), (kv_x3, 0), (z_forward, QG0, BEFORE), (z_forward, QG0, FAR), (z_direct, UP0, AFTER), (z_direct, UP0, BEFORE)],
        "first_on": [(y_send, WO0)],
        "ready": [(load_near, QG0), (load_far, QG0), (kv_load, 0), (loaded, QG0), (kv_loaded,)],
        "k1": [(z_direct, UP0, FAR), (z_forward, UP0, AFTER)],
        "k2": [
            (z_forward, UP0, BEFORE), (y_relay, WO0), (z_forward, UP0, FAR), (y_send, QG1), (z_own, WO0), (z_direct, WO0, BEFORE),
            (kv_x1, 1),
        ],
        ("seq", 1): [(y_send, WO1), (z_direct, WO0, AFTER), (x_sent,)],
        "up": [(y_send, UP1), (z_direct, WO0, FAR), (load_near, UP0), (load_far, UP0)],
        ("two", 0): [(y_relay, QG1), (z_forward, WO0, OWN)],
        ("seq", 2): [(kv_x2, 1)],
        ("two", 1): [(kv_x3, 1), (z_direct, QG1, AFTER), (z_forward, WO0, BEFORE)],
        ("seq", 3): [(y_relay, WO1), (z_forward, WO0, AFTER)],
        ("two", 2): [(z_forward, WO0, FAR), (z_own, QG1), (y_relay, UP1)],
        "near": [(load_near, WO0)],
    })
    first_scatter = plan({
        "a0s0": [(z_forward, QG1, AFTER)],
        "a0s2": [(z_direct, QG1, BEFORE)],
        "b0": [(load_far, WO0), (far_loaded, WO0)],
        "a1s0": [(z_direct, QG1, FAR)],
        "a1s1": [(z_forward, QG1, OWN)],
        "a1": [(z_direct, UP1, FAR)],
        "b1": [(z_direct, UP1, BEFORE)],
        "c1": [(z_forward, QG1, FAR), (z_direct, UP1, AFTER), (z_own, UP1), (z_forward, QG1, BEFORE)],
        "e0": [(z_forward, UP1, FAR)],
    })
    second_front = plan({
        "begin": [(z_forward, UP1, BEFORE), (kv_load, 1)],
        "first": [(z_forward, UP1, AFTER)],
        "k0": [(z_forward, UP1, OWN), (z_direct, WO1, FAR)],
        "ready": [(load_near, QG1), (load_far, QG1), (loaded, QG1), (kv_loaded,)],
        ("seq", 0): [(z_own, WO1)],
        "k1": [(z_direct, WO1, BEFORE)],
        "up": [(load_near, UP1), (load_far, UP1)],
        "k2": [(z_direct, WO1, AFTER)],
        ("seq", 1): [(z_forward, WO1, FAR)],
        ("two", 1): [(z_forward, WO1, OWN)],
        ("two", 2): [(z_forward, WO1, BEFORE), (z_forward, WO1, AFTER)],
        "near": [(load_near, WO1), (load_far, WO1)],
    })
    second_scatter = plan({
    })

    with jax.named_scope("start"):
        start(first_entry)
    with jax.named_scope("front_0"):
        gather_norm(0, rows // RING, first_front)
    with jax.named_scope("near_0"):
        kv_share(0)
        first_front("near")
        near_loaded(WO0)
    with jax.named_scope("scatter_0"):
        out_scatter(0, first_scatter)
    with jax.named_scope("front_1"):
        gather_norm(1, rows // 2, second_front)
    with jax.named_scope("near_1"):
        kv_share(1)
        second_front("near")
        loaded(WO1)
    with jax.named_scope("scatter_1"):
        out_scatter(1, second_scatter)
    with jax.named_scope("drain"):
        left()
        for t in range(WO1 + 1):
            drain(t)
        for l in range(n_layers):
            kv_shared(l)
            kv_sent(l)


def run_model(xt, gain, wkv_t, w_in, w_out, cos_full, sin_full):
    batch, d_local, seq_len = xt.shape
    n_layers, d_row, e_block = w_in.shape
    r_block, d_col = w_out.shape[1:]
    head_dim = cos_full.shape[1]
    d_model = d_row * RING * RING
    seqs = batch // RING
    rows = seqs * seq_len // (RING * RING * CORES)
    e_loc, r_loc = e_block // RING, r_block // RING
    kc = wkv_t.shape[1]
    width = d_model // RING
    n_t = 3 * n_layers
    n_o = len(OTHERS)

    def dma(*shape):
        return pltpu.SemaphoreType.DMA(shape)

    def vm(*shape):
        return pltpu.VMEM(shape, BF)

    def out(*shape):
        return jax.ShapeDtypeStruct(shape, BF)

    any_spec = pl.BlockSpec(memory_space=pl.ANY)
    vm_spec = pl.BlockSpec(memory_space=pltpu.VMEM)
    out_shape = [
        out(batch, d_local, seq_len),
        out(n_layers, 2, seqs, seq_len, head_dim),
        out(n_layers, RING, RING, CORES, rows, d_model),
        out(n_layers, RING, RING * d_row, e_loc),
        out(n_layers, RING, RING, r_loc, d_col),
        out(RING, CORES, n_layers, RING, RING, kc, d_row),
        out(n_layers, RING, 2, seqs, CORES * (seq_len // (CORES * RING * RING * RING)), head_dim),
        out(n_layers, 2, d_row // 2, e_loc),
        out(n_layers, 2, r_loc // 2, d_col),
    ]
    pair = (2, 2, 2)
    scratch = [
        vm(rows, d_model), vm(rows, d_model), pltpu.VMEM((n_layers, d_model), F32),
        vm(RING, CORES, RING, RING, G_ROWS, d_row),
        vm(RING, seqs, d_local, seq_len),
        vm(CORES, RING, RING, RING, d_local, CORES * rows),
        vm(RING, RING * d_row, e_loc), vm(RING, RING, 2 * head_dim, d_row), vm(RING, RING, r_loc, d_col),
        vm(H_SLOTS, RING, CORES, rows, d_model), vm(RING, seq_len, r_loc), vm(2, 2, seq_len, head_dim), vm(seq_len, head_dim),
        vm(CORES * RING * rows, r_loc), vm(2, RING, rows, width), vm(2, 2, RING, RING, rows, width), vm(2, 2, RING, RING, rows, width),
        vm(*pair, 2, rows, width), vm(*pair, RING, rows, width), vm(*pair, rows // 2, width), vm(*pair, rows, width),
        dma(n_o), dma(n_o), dma(RING), dma(RING), dma(RING), dma(RING), pltpu.SemaphoreType.DMA,
        dma(3 * n_o), dma(3 * n_o), dma(RING), dma(RING),
        dma(RING), dma(RING), dma(2, RING), dma(2, RING), dma(RING), dma(RING), pltpu.SemaphoreType.DMA,
        dma(RING), dma(40), pltpu.SemaphoreType.DMA, dma(RING), pltpu.SemaphoreType.DMA, dma(H_SLOTS), dma(2, 2), dma(3), dma(3),
        dma(n_t, RING), dma(n_t, 2), dma(3, RING, 2), dma(3, RING, 2), dma(n_t, RING),
        dma(n_o), dma(n_o), pltpu.SemaphoreType.DMA, dma(n_o), dma(n_layers), dma(n_layers, n_o), dma(n_layers), dma(n_layers), dma(2),
        dma(2), dma(2, 2, RING), dma(RING), dma(*pair), dma(*pair, 2), dma(*pair), dma(*pair),
        dma(n_layers, n_o), dma(n_layers, n_o), dma(n_layers),
    ]
    res = pl.pallas_call(
        model_kernel,
        out_shape=out_shape,
        in_specs=[any_spec, vm_spec, vm_spec, any_spec, any_spec, vm_spec, vm_spec],
        out_specs=[any_spec] * len(out_shape),
        scratch_shapes=scratch,
        compiler_params=pltpu.CompilerParams(collective_id=0, has_side_effects=True, vmem_limit_bytes=VMEM_LIMIT),
        name="two_layers",
    )(xt, gain, wkv_t, w_in, w_out, cos_full, sin_full)
    return res[0], res[6]


def solution(mesh):
    row_size = mesh.shape["row"]
    n_col = mesh.shape["col"]
    n_z = row_size // RING
    n_y = RING
    n_x = n_col // CORES
    n_tp = n_y * n_col
    n_dev = row_size * n_col
    mesh4 = Mesh(mesh.devices.reshape(n_z, n_y, n_x, CORES), ("z", "y", "x", "core"))
    every = ("z", "y", "x", "core")
    col = ("x", "core")
    act_spec = P(NIL, NIL, every)
    w_spec = P(NIL, ("z", "y"), col)

    def device_fn(x_loc, gain_loc, w_in_loc, w_kv_loc, w_out_loc):
        n_layers = w_in_loc.shape[0]
        n_batch, seq_len, d_local = x_loc.shape
        head_dim = w_kv_loc.shape[2] * n_col // 2
        batch_loc = n_batch // n_z
        seq_local = seq_len // n_dev
        steps = np.arange(head_dim // 2, dtype=np.float32)
        inv_freq = (1.0 / 10000.0 ** (steps * 2 / head_dim)).astype(np.float32)
        angles = np.arange(seq_len, dtype=np.float32)[:, NIL] * inv_freq[NIL, :]
        cos_tab, sin_tab = np.cos(angles), np.sin(angles)
        cos_full = jnp.asarray(np.concatenate([cos_tab, cos_tab], axis=1))
        sin_full = jnp.asarray(np.concatenate([-sin_tab, sin_tab], axis=1))
        y_loc, kv = run_model(x_loc.transpose(0, 2, 1), gain_loc, w_kv_loc.transpose(0, 2, 1), w_in_loc, w_out_loc, cos_full, sin_full)
        y_loc = y_loc.transpose(0, 2, 1)
        kv = kv.reshape(n_layers, n_z, 2, batch_loc, CORES, seq_local, head_dim)
        kv = lax.dynamic_index_in_dim(kv, lax.axis_index("core"), axis=4, keepdims=False)
        kv = kv.transpose(0, 2, 1, 3, 4, 5).reshape(n_layers, 2, n_batch, seq_local, head_dim)
        return y_loc, kv

    return jax.shard_map(device_fn, mesh=mesh4, in_specs=(act_spec, P(NIL, every), w_spec, w_spec, P(NIL, col, ("z", "y"))), out_specs=(act_spec, P(NIL, NIL, NIL, every, NIL)), check_vma=False)
```

```python
import typing

import jax
import jax.numpy as jnp
import numpy as np
from jax import lax
from jax.experimental import pallas as pl
from jax.experimental.pallas import tpu as pltpu
from jax.sharding import Mesh
from jax.sharding import PartitionSpec as P

LN_EPS = 1e-6
RING = 4
CORES = 2
VMEM_LIMIT = 67_000_000
BF = jnp.bfloat16
F32 = jnp.float32
SLOT_OFF = (2, 1, 3, 0)
SIGN = (1, -1)
NIL = None
BOTH = range(CORES)
RINGS = range(RING)
OTHERS = (1, 3, 2)
LAST = RING - 1
G_ROWS = 8
H_SLOTS = 3
QG0, UP0, WO0, QG1, UP1, WO1 = range(6)
OWN, AFTER, FAR, BEFORE = RINGS
FIRST_ORDER = ("a0", "b0", "a1", "b1", "c0", "c1", "d0", "d1", "e0", "e1")
LAST_ORDER = FIRST_ORDER[:-1] + ("f1", "e1", "g1", "f0", "g0", "h1", "h0")
KINDS = ("first", "second", "first_on", "second_on")


class Refs(typing.NamedTuple):
    xt: typing.Any
    gain_in: typing.Any
    wkv: typing.Any
    w_in: typing.Any
    w_out: typing.Any
    cos: typing.Any
    sin: typing.Any
    y_out: typing.Any
    kv_out: typing.Any
    h_all: typing.Any
    wi: typing.Any
    wo: typing.Any
    kvh: typing.Any
    kvx: typing.Any
    rwi: typing.Any
    rwo: typing.Any
    h_ref: typing.Any
    hid: typing.Any
    gain: typing.Any
    gbuf: typing.Any
    xz: typing.Any
    xp: typing.Any
    wv: typing.Any
    kvb: typing.Any
    wov: typing.Any
    hb: typing.Any
    joined: typing.Any
    qkv: typing.Any
    stage: typing.Any
    lhs: typing.Any
    away: typing.Any
    acc: typing.Any
    die_in: typing.Any
    in1: typing.Any
    in2: typing.Any
    in3: typing.Any
    in4: typing.Any
    xz_send: typing.Any
    xz_recv: typing.Any
    xp_send: typing.Any
    xp_recv: typing.Any
    xd_send: typing.Any
    xd_recv: typing.Any
    x_loc: typing.Any
    g_send: typing.Any
    g_recv: typing.Any
    gd_send: typing.Any
    gd_recv: typing.Any
    yd_send: typing.Any
    yd_recv: typing.Any
    yp_send: typing.Any
    yp_recv: typing.Any
    yz_send: typing.Any
    yz_recv: typing.Any
    y_loc: typing.Any
    ag_send: typing.Any
    ag_recv: typing.Any
    ag_dsend: typing.Any
    ag_drecv: typing.Any
    ag_loc: typing.Any
    h_sem: typing.Any
    kvo_sem: typing.Any
    w_load: typing.Any
    far_load: typing.Any
    y_recv: typing.Any
    ry_recv: typing.Any
    zb_recv: typing.Any
    zc_recv: typing.Any
    w_send: typing.Any
    kz_send: typing.Any
    kz_recv: typing.Any
    ky_send: typing.Any
    ky_recv: typing.Any
    kx_send: typing.Any
    kx_recv: typing.Any
    kd_send: typing.Any
    kd_recv: typing.Any
    k_loc: typing.Any
    dsend: typing.Any
    drecv: typing.Any
    rs_send: typing.Any
    recv1: typing.Any
    recv2: typing.Any
    recv3: typing.Any
    recv4: typing.Any
    kvx_send: typing.Any
    kvx_recv: typing.Any
    kvx_loc: typing.Any


def model_kernel(*refs):
    r = Refs(*refs)
    z, y, x, c = (lax.axis_index(a) for a in ("z", "y", "x", "core"))
    n_layers = r.wkv.shape[0]
    rows, d_model = r.hid.shape
    batch, d_local = r.xt.shape[:2]
    seqs = batch // RING
    seq_len, head_dim = r.cos.shape
    d_row = r.w_in.shape[1]
    e_loc = r.wi.shape[3]
    depth = r.wo.shape[3]
    f_loc = depth - head_dim
    quarter = rows // 4
    width = d_model // RING
    q_block = head_dim * RING
    f_block = f_loc * RING

    turned = {id(v): [lax.rem(v + o, RING) for o in RINGS] for v in (z, y, x)}

    def turn(base, off):
        if isinstance(off, int):
            return turned[id(base)][off % RING]
        return lax.rem(base + off + RING, RING)

    def remote(src, dst, ssem, rsem, dev):
        return pltpu.make_async_remote_copy(
            src_ref=src, dst_ref=dst, send_sem=ssem, recv_sem=rsem, device_id=dev, device_id_type=pl.DeviceIdType.MESH)

    partner = (z, y, x, 1 - c)

    peers = [(turn(z, o), y, x, c) for o in OTHERS]
    peers += [(z, turn(y, oy), turn(x, ox), c) for oy in RINGS for ox in RINGS if oy or ox]
    peers.append(partner)
    here = (z, y, x, c)
    gate_sem = pltpu.get_barrier_semaphore()
    for dev in peers:
        pl.semaphore_signal(gate_sem, inc=1, device_id=dev, device_id_type=pl.DeviceIdType.MESH)
    src_id = lax.broadcasted_iota(jnp.int32, (d_local, d_row), 0) + (x * CORES + c) * d_local
    dst_id = lax.broadcasted_iota(jnp.int32, (d_local, d_row), 1)
    spread = jnp.where(src_id == dst_id, 1.0, 0.0).astype(BF)
    r.gbuf[x, c, y, z] = jnp.zeros((G_ROWS, d_row), BF)
    r.gbuf[x, c, y, z, :n_layers] = jnp.dot(r.gain_in[...], spread, preferred_element_type=F32).astype(BF)
    pl.semaphore_wait(gate_sem, len(peers))

    def hook(pump, i):
        with jax.named_scope(f"hook_{i}"):
            pump(i)

    def w_cols(kind):
        return pl.ds(0, head_dim + f_loc) if kind == 0 else pl.ds(head_dim + f_loc, f_loc)

    def piece(t, zz, yy):
        l, kind = t // 3, t % 3
        if kind == 2:
            return r.wo.at[l, zz, yy]
        return r.wi.at[l, zz, pl.ds(pl.multiple_of(yy * d_row, d_row), d_row), w_cols(kind)]

    def piece_half(t, zz, yy, h):
        l, kind = t // 3, t % 3
        if kind == 2:
            return r.wo.at[l, zz, yy, pl.ds(h * (depth // 2), depth // 2)]
        return r.wi.at[l, zz, pl.ds(pl.multiple_of(yy * d_row + h * (d_row // 2), d_row // 2), d_row // 2), w_cols(kind)]

    def own_parts(t, owner, zz, yy):
        l, kind = t // 3, t % 3
        hq = pl.ds(pl.multiple_of(owner * head_dim, head_dim), head_dim)
        if kind == 2:
            return [
                (r.w_out.at[l, hq], r.wo.at[l, zz, yy, pl.ds(0, head_dim)]),
                (r.w_out.at[l, pl.ds(pl.multiple_of(q_block + owner * f_loc, head_dim), f_loc)], r.wo.at[l, zz, yy, pl.ds(head_dim, f_loc)]),
            ]
        rws = pl.ds(pl.multiple_of(yy * d_row, d_row), d_row)
        if kind == 0:
            return [
                (r.w_in.at[l, :, hq], r.wi.at[l, zz, rws, pl.ds(0, head_dim)]),
                (r.w_in.at[l, :, pl.ds(pl.multiple_of(q_block + owner * f_loc, head_dim), f_loc)], r.wi.at[l, zz, rws, pl.ds(head_dim, f_loc)]),
            ]
        return [(r.w_in.at[l, :, pl.ds(pl.multiple_of(q_block + f_block + owner * f_loc, head_dim), f_loc)],
                 r.wi.at[l, zz, rws, pl.ds(head_dim + f_loc, f_loc)])]

    def relay_ref(t, d):
        l, kind = t // 3, t % 3
        return r.rwo.at[l, d] if kind == 2 else r.rwi.at[l, d, :, w_cols(kind)]

    def far_parts(t, d):
        l, kind = t // 3, t % 3
        owner = turn(y, 2)
        hq = pl.ds(pl.multiple_of(owner * head_dim, head_dim), head_dim)
        if kind == 2:
            n = depth // 2
            base = q_block + owner * f_loc
            if d:
                return [(r.w_out.at[l, pl.ds(pl.multiple_of(base + n - head_dim, G_ROWS), n)], r.rwo.at[l, d])]
            return [
                (r.w_out.at[l, hq], r.rwo.at[l, d, pl.ds(0, head_dim)]),
                (r.w_out.at[l, pl.ds(pl.multiple_of(base, head_dim), n - head_dim)], r.rwo.at[l, d, pl.ds(head_dim, n - head_dim)]),
            ]
        rws = pl.ds(d * (d_row // 2), d_row // 2)
        if kind == 0:
            return [
                (r.w_in.at[l, rws, hq], r.rwi.at[l, d, :, pl.ds(0, head_dim)]),
                (r.w_in.at[l, rws, pl.ds(pl.multiple_of(q_block + owner * f_loc, head_dim), f_loc)], r.rwi.at[l, d, :, pl.ds(head_dim, f_loc)]),
            ]
        return [(r.w_in.at[l, rws, pl.ds(pl.multiple_of(q_block + f_block + owner * f_loc, head_dim), f_loc)], relay_ref(t, d))]

    def y_send(t):
        for d in BOTH:
            owner = turn(y, SIGN[d])
            dev = (z, owner, x, c)
            for src, dst in far_parts(t, d):
                remote(src, dst, r.w_send.at[t], r.ry_recv.at[t, d], dev).start()
            for src, dst in own_parts(t, owner, z, y):
                remote(src, dst, r.w_send.at[t], r.y_recv.at[t, -SIGN[d] % RING], dev).start()

    def y_relay(t):
        for d in BOTH:
            ref = relay_ref(t, d)
            remote(ref, ref, r.w_send.at[t], r.ry_recv.at[t, d], here).wait_recv()
            dst = piece_half(t, z, turn(y, -SIGN[d]), d)
            remote(ref, dst, r.w_send.at[t], r.y_recv.at[t, 2], (z, turn(y, SIGN[d]), x, c)).start()

    def z_own(t):
        for d in BOTH:
            for src, dst in own_parts(t, y, z, y):
                remote(src, dst, r.w_send.at[t], r.zb_recv.at[t % 3, 0, d], (turn(z, SIGN[d]), y, x, c)).start()

    def z_direct(t, j):
        yy = turn(y, j)
        ref = piece(t, z, yy)
        remote(ref, ref, r.w_send.at[t], r.y_recv.at[t, j], here).wait_recv()
        for d in BOTH:
            remote(ref, ref, r.w_send.at[t], r.zb_recv.at[t % 3, j, d], (turn(z, SIGN[d]), y, x, c)).start()

    def z_forward(t, j):
        yy = turn(y, j)
        for d in BOTH:
            zz = turn(z, -SIGN[d])
            ref = piece(t, zz, yy)
            remote(ref, ref, r.w_send.at[t], r.zb_recv.at[t % 3, j, d], here).wait_recv()
            part = piece_half(t, zz, yy, d)
            remote(part, part, r.w_send.at[t], r.zc_recv.at[t % 3], (turn(z, SIGN[d]), y, x, c)).start()

    def place(t, zz):
        l, kind = t // 3, t % 3
        if kind == 2:
            return r.wo.at[l, zz], r.wov.at[zz]
        return r.wi.at[l, zz, :, w_cols(kind)], r.wv.at[zz, :, w_cols(kind)]

    def load_near(t):
        kind = t % 3
        for d in BOTH:
            src, dst = place(t, turn(z, SIGN[d]))
            pltpu.make_async_copy(src, dst, r.w_load.at[kind]).start()
        for j in OTHERS:
            yy = turn(y, j)
            dst = r.wov.at[z, yy] if kind == 2 else r.wv.at[z, pl.ds(pl.multiple_of(yy * d_row, d_row), d_row), w_cols(kind)]
            pltpu.make_async_copy(piece(t, z, yy), dst, r.w_load.at[kind]).start()
        for src, dst in own_parts(t, y, z, y):
            pltpu.make_async_copy(src, own_place(t, dst, src), r.w_load.at[kind]).start()

    def load_far(t):
        src, dst = place(t, turn(z, 2))
        remote(src, src, r.w_send.at[t], r.zc_recv.at[t % 3], here).wait_recv()
        pltpu.make_async_copy(src, dst, r.far_load.at[t % 3]).start()

    def own_place(t, dst, src):
        kind = t % 3
        if kind == 2:
            n = src.shape[0]
            return r.wov.at[z, y, pl.ds(0 if n == head_dim and f_loc != head_dim else head_dim, n)]
        n = src.shape[1]
        rws = pl.ds(pl.multiple_of(y * d_row, d_row), d_row)
        if kind == 0:
            return r.wv.at[z, rws, pl.ds(0 if n == head_dim and f_loc != head_dim else head_dim, n)]
        return r.wv.at[z, rws, pl.ds(head_dim + f_loc, f_loc)]

    def near_loaded(t):
        kind = t % 3
        dst = r.wov.at[pl.ds(0, LAST)] if kind == 2 else r.wv.at[pl.ds(0, LAST), :, w_cols(kind)]
        pltpu.make_async_copy(dst, dst, r.w_load.at[kind]).wait()

    def far_loaded(t):
        kind = t % 3
        dst = r.wov.at[0] if kind == 2 else r.wv.at[0, :, w_cols(kind)]
        pltpu.make_async_copy(dst, dst, r.far_load.at[kind]).wait()

    def loaded(t):
        near_loaded(t)
        far_loaded(t)

    def drain(t):
        l, kind = t // 3, t % 3
        ref = r.wo.at[l] if kind == 2 else r.wi.at[l, :, :, w_cols(kind)]
        remote(ref, ref, r.w_send.at[t], r.y_recv.at[t, 0], here).wait_send()

    def kv_z_copy(k):
        return remote(r.wkv, r.kvh.at[x, c, :, y, z], r.kz_send.at[k], r.kz_recv.at[k], (turn(z, OTHERS[k]), y, x, c))

    def kv_own():
        return pltpu.make_async_copy(r.wkv, r.kvh.at[x, c, :, y, z], r.k_loc.at[0])

    def kv_z():
        for k in range(len(OTHERS)):
            kv_z_copy(k).start()
        kv_own().start()

    def kv_y_copy(ref, k, d):
        return remote(ref, ref, r.ky_send, r.ky_recv.at[k], (z, turn(y, SIGN[d]), x, c))

    def kv_y1():
        kv_own().wait()
        for k in range(len(OTHERS)):
            kv_z_copy(k).wait()
        for d in BOTH:
            kv_y_copy(r.kvh.at[x, c, :, y], d, d).start()

    def kv_y2():
        for d in BOTH:
            yy = turn(y, -SIGN[d])
            kv_y_copy(r.kvh.at[x, c, :, yy], d, d).wait_recv()
            kv_y_copy(r.kvh.at[x, c, :, yy, pl.ds(2 * d, 2)], 2, d).start()

    def kv_y3():
        kv_y_copy(r.kvh.at[x, c, :, turn(y, 2)], 2, 0).wait_recv()
        kv_y_copy(r.kvh.at[x, c, :, pl.ds(0, LAST)], 0, 0).wait_send()

    def kv_x_copy(l, ref, k, d):
        return remote(ref, ref, r.kx_send.at[l], r.kx_recv.at[l, k], (z, y, turn(x, SIGN[d]), c))

    def kv_die(l, ref):
        return remote(ref, ref, r.kd_send.at[l], r.kd_recv.at[l], partner)

    def kv_x1(l):
        ref = r.kvh.at[x, c, l]
        for d in BOTH:
            kv_x_copy(l, ref, d, d).start()
        kv_die(l, ref).start()

    def kv_x2(l):
        for d in BOTH:
            xx = turn(x, -SIGN[d])
            ref = r.kvh.at[xx, c, l]
            kv_x_copy(l, ref, d, d).wait_recv()
            kv_x_copy(l, r.kvh.at[xx, c, l, pl.ds(2 * d, 2)], 2, d).start()
            kv_die(l, ref).start()

    def kv_x3(l):
        ref = r.kvh.at[turn(x, 2), c, l]
        kv_x_copy(l, ref, 2, 0).wait_recv()
        kv_die(l, ref).start()

    def kv_load(l):
        kv_die(l, r.kvh.at[:, 1 - c, l]).wait_recv()
        kc = r.wkv.shape[1]
        for xx in RINGS:
            for cc in BOTH:
                pltpu.make_async_copy(r.kvh.at[xx, cc, l], r.kvb.at[:, :, pl.ds((xx * CORES + cc) * kc, kc)], r.k_loc.at[1]).start()

    def kv_sent(l):
        kv_x_copy(l, r.kvh.at[pl.ds(0, LAST), c, l], 0, 0).wait_send()
        kv_die(l, r.kvh.at[:, c, l]).wait_send()

    def kv_loaded():
        pltpu.make_async_copy(r.kvb, r.kvb, r.k_loc.at[1]).wait()

    def gain_move(i, src, dst, dev):
        return remote(src, dst, r.g_send.at[i], r.g_recv.at[i], dev)

    def gain_z(k):
        dev = (turn(z, OTHERS[k]), y, x, c)
        return gain_move(k, r.gbuf.at[x, c, y, z], r.gbuf.at[x, c, y, z], dev)

    def gain_y(k):
        dev = (z, turn(y, OTHERS[k]), x, c)
        return gain_move(len(OTHERS) + k, r.gbuf.at[x, c, y], r.gbuf.at[x, c, y], dev)

    def gain_x(k):
        dev = (z, y, turn(x, OTHERS[k]), c)
        return gain_move(CORES * len(OTHERS) + k, r.gbuf.at[x, c], r.gbuf.at[x, c], dev)

    def gain_die(xx, k):
        ref = r.gbuf.at[xx, c]
        return remote(ref, ref, r.gd_send.at[k], r.gd_recv.at[k], partner)

    def gain_sum():
        for zz in RINGS:
            for yy in RINGS:
                tot = jnp.zeros((n_layers, d_row), F32)
                for xx in RINGS:
                    for cc in BOTH:
                        tot += r.gbuf[xx, cc, yy, zz, :n_layers].astype(F32)
                at = (zz * RING + yy) * d_row
                r.gain[:, at:at + d_row] = tot

    tok_pair = CORES * rows

    def x_z(k):
        zz = turn(z, OTHERS[k])
        src = r.xt.at[pl.ds(zz * seqs, seqs)]
        return remote(src, r.xz.at[z], r.xz_send, r.xz_recv, (zz, y, x, c))

    def three_planes():
        ref = r.xz.at[pl.ds(0, LAST)]
        return remote(ref, ref, r.xz_send, r.xz_recv, here)

    def x_own():
        return pltpu.make_async_copy(r.xt.at[pl.ds(z * seqs, seqs)], r.xz.at[z], r.x_loc)

    def pos(xx):
        return pl.ds(pl.multiple_of(xx * tok_pair, tok_pair), tok_pair)

    def x_plane(oy, ox):
        yy, xx = turn(y, oy), turn(x, ox)
        return remote(r.xz.at[:, yy, :, pos(xx)], r.xp.at[c, y, x], r.xp_send.at[oy], r.xp_recv.at[(RING - oy) % RING], (z, yy, xx, c))

    def row_bytes(oy):
        return r.xp.at[c, 0] if oy else r.xp.at[c, 0, pl.ds(0, RING - 1)]

    def x_row(oy):
        yy = turn(y, oy)
        got = row_bytes(oy)
        remote(got, got, r.xp_send.at[oy], r.xp_recv.at[oy], partner).wait_recv()
        row = r.xp.at[c, yy]
        remote(row, row, r.xd_send, r.xd_recv, partner).start()

    def x_turn():
        got = r.xp.at[1 - c]
        remote(got, got, r.xd_send, r.xd_recv, partner).wait_recv()

        @pl.loop(0, RING)
        def _(zz):
            for yy in RINGS:
                for xh in BOTH:
                    blk = [r.xp[cc, yy, CORES * xh + xx, zz] for xx in BOTH for cc in BOTH]
                    blk = jnp.concatenate(blk, axis=0).astype(F32).T.astype(BF)
                    n = blk.shape[1]
                    at = pl.multiple_of(zz * RING * d_row + yy * d_row + xh * n, n)
                    r.hb[0, 0, :, :, pl.ds(at, n)] = blk.reshape(CORES, rows, n)
        r.hid[...] = r.hb[0, 0, c]
        remote(got, got, r.xd_send, r.xd_recv, partner).wait_send()

    def x_sent():
        three_planes().wait_send()
        for fn in (gain_z, gain_y, gain_x):
            peers_of(fn, "wait_send")
        for k in RINGS:
            gain_die(x, k).wait_send()
        for oy in RINGS:
            got = row_bytes(oy)
            remote(got, got, r.xp_send.at[oy], r.xp_recv.at[oy], partner).wait_send()

    def y_die(p):
        cols = pl.ds(pl.multiple_of(turn(z, p) * width, width), width)
        return remote(r.hid.at[:, cols], r.hb.at[0, 0, c, :, cols], r.yd_send.at[p], r.yd_recv.at[p], partner)

    def planes(h):
        return pl.ds(2 * h, 2)

    def y_plane(h, oy, ox):
        yy, xx = turn(y, oy), turn(x, ox)
        return remote(r.xp.at[c, yy, xx, planes(h)], r.xz.at[planes(h), y, :, pos(x)], r.yp_send.at[h, oy], r.yp_recv.at[h, (RING - oy) % RING],
                      (z, yy, xx, c))

    def y_z(p, oy):
        s = turn(y, oy)
        return remote(r.xz.at[p, s], r.y_out.at[z * seqs + s], r.yz_send.at[p], r.yz_recv.at[p], (turn(z, p), y, x, c))

    def y_own(oy):
        s = turn(y, oy)
        return pltpu.make_async_copy(r.xz.at[0, s], r.y_out.at[z * seqs + s], r.y_loc)

    def leave_a(h):
        for p in BOTH:
            p = 2 * h + p
            y_die(p).start()
            cols = pl.ds(pl.multiple_of(turn(z, p) * width, width), width)
            r.hb[0, 0, c, :, cols] = r.hid[:, cols]

    def leave_b(h):
        n = CORES * CORES * d_local
        for p in BOTH:
            p = 2 * h + p
            y_die(p).wait()

            @pl.loop(0, RING)
            def _(yy, p=p):
                for xh in BOTH:
                    at = pl.multiple_of(turn(z, p) * width + yy * d_row + xh * n, n)
                    blk = r.hb[0, 0, :, :, pl.ds(at, n)].reshape(tok_pair, n).astype(F32).T.astype(BF)
                    for xx in BOTH:
                        for cc in BOTH:
                            lo = (xx * CORES + cc) * d_local
                            r.xp[cc, yy, CORES * xh + xx, p] = blk[lo:lo + d_local]

        for oy in OTHERS + (0,):
            for ox in RINGS:
                if oy or ox:
                    y_plane(h, oy, ox).start()
        for p in BOTH:
            p = 2 * h + p
            r.xz[p, y, :, pos(x)] = r.xp[c, y, x, p]

    def plane_bytes(h, oy):
        return r.xp.at[c, 0, :, planes(h)] if oy else r.xp.at[c, 0, pl.ds(0, LAST), planes(h)]

    def leave_c(h):
        for oy in OTHERS + (0,):
            got = plane_bytes(h, oy)
            remote(got, got, r.yp_send.at[h, oy], r.yp_recv.at[h, oy], partner).wait_recv()
            for p in BOTH:
                p = 2 * h + p
                (y_z(p, oy) if p else y_own(oy)).start()

    def left():
        for oy in RINGS:
            for h in BOTH:
                got = plane_bytes(h, oy)
                remote(got, got, r.yp_send.at[h, oy], r.yp_recv.at[h, oy], partner).wait_send()
        for p in OTHERS:
            ref = r.xz.at[p]
            remote(ref, ref, r.yz_send.at[p], r.yz_recv.at[p], here).wait()
        pltpu.make_async_copy(r.xz.at[0], r.xz.at[0], r.y_loc).wait()

    def kv_rows(zz):
        n = CORES * seq_len // (RING * RING * RING * CORES)
        return pl.ds(pl.multiple_of(((zz * RING + y) * RING + x) * n, n), n)

    def kv_trade(l, k):
        zz = turn(z, OTHERS[k])
        return remote(r.kv_out.at[l, :, :, kv_rows(zz)], r.kvx.at[l, z], r.kvx_send.at[l, k], r.kvx_recv.at[l, k], (zz, y, x, c))

    def kv_keep(l):
        return pltpu.make_async_copy(r.kv_out.at[l, :, :, kv_rows(z)], r.kvx.at[l, z], r.kvx_loc.at[l])

    def kv_share(l):
        for k in range(len(OTHERS)):
            kv_trade(l, k).start()
        kv_keep(l).start()

    def kv_shared(l):
        for k in range(len(OTHERS)):
            kv_trade(l, k).wait()
        kv_keep(l).wait()

    def gather_norm(l, split, pump):
        hid = r.hid
        gain = r.gain[l:l + 1, :]
        for b in range(4):
            blk = hid[b * quarter:(b + 1) * quarter, :].astype(F32)
            mean = jnp.mean(blk, axis=-1, keepdims=True)
            cen = blk - mean
            var = jnp.mean(cen * cen, axis=-1, keepdims=True)
            r.h_ref[b * quarter:(b + 1) * quarter, :] = (cen * lax.rsqrt(var + LN_EPS) * gain).astype(BF)
        out = r.h_all.at[l]

        def spot(q, first, second):
            if q == 0:
                return turn(y, second), turn(x, first)
            return turn(y, first), turn(x, second)

        def span(q, part):
            lo, n = (split, rows - split) if q else (0, split)
            if part is NIL:
                return pl.ds(lo, n)
            return pl.ds(lo + part * (n // 2), n // 2)

        offs = (0, -1, 1, 2)
        plans = {}
        for q in BOTH:
            for d in BOTH:
                plans["first", q, d] = (q, 0, 0, NIL, SIGN[d], 0)
                plans["first_on", q, d] = (q, -SIGN[d], 0, d, SIGN[d], 0)
                for k in RINGS:
                    plans["second", q, k, d] = (q, offs[k], 0, NIL, 0, SIGN[d])
                    plans["second_on", q, k, d] = (q, offs[k], -SIGN[d], d, 0, SIGN[d])
        index = {key: n for n, key in enumerate(plans)}

        def link(*key, own=False):
            idx, (q, first, second, part, to_first, to_second) = index[key], plans[key]
            sy, sx = spot(q, first, second)
            ty, tx = spot(q, to_first, to_second)
            rws = span(q, part)
            dst = out.at[sy, sx, c, rws]
            return remote(r.h_ref.at[rws] if own else dst, dst, r.ag_send.at[KINDS.index(key[0])], r.ag_recv.at[idx], (z, ty, tx, c))

        def arrived(*key):
            for d in BOTH:
                link(*key, d).wait_recv()

        def die(q, first, second, own=False):
            sy, sx = spot(q, first, second)
            rws = span(q, NIL)
            dst = out.at[sy, sx, c, rws]
            off = (first if q else second) % RING
            remote(r.h_ref.at[rws] if own else dst, dst, r.ag_dsend, r.ag_drecv.at[off], partner).start()

        def take(k, q):
            for d in BOTH:
                link("second", q, k, d).wait_recv()
                die(q, offs[k], -SIGN[d])

        def pass_on(k, q):
            for d in BOTH:
                link("second_on", q, k, d).start()

        def second_step(k):
            take(k, 1)
            pass_on(k, 1)
            take(k, 0)

        def far_first(q):
            for e in BOTH:
                link("second", q, LAST, e).start()

        def last_step(q, k):
            arrived("second_on", q, k)
            die(q, offs[k], 2)

        def tail_a():
            second_step(2)
            far_first(1)
            for k in RINGS[:-1]:
                pass_on(k, 0)
            hook(pump, "k2")
            take(LAST, 0)
            pass_on(LAST, 0)
            hook(pump, "k3")
            for k in (1, 2):
                last_step(1, k)

        def tail_b():
            take(LAST, 1)
            pass_on(LAST, 1)

        def tail_c():
            for k in RINGS:
                last_step(0, k)
            last_step(1, LAST)

        for q in BOTH:
            for d in BOTH:
                link("first", q, d, own=True).start()
        for q in BOTH:
            for d in BOTH:
                link("second", q, 0, d, own=True).start()
        for q in BOTH:
            die(q, 0, 0, own=True)
        own = pltpu.make_async_copy(r.h_ref, out.at[y, x, c], r.ag_loc)
        own.start()
        hook(pump, "begin")
        for d in BOTH:
            for q in BOTH:
                link("first", q, d).wait_recv()
                src = -SIGN[d]
                link("first_on", q, d).start()
                die(q, src, 0)
        hook(pump, "first")
        second_step(0)
        for q in reversed(BOTH):
            for d in BOTH:
                for e in BOTH:
                    link("second", q, 1 + d, e).start()
        hook(pump, "k0")
        for q in BOTH:
            arrived("first_on", q)
            die(q, 2, 0)
        far_first(0)
        hook(pump, "first_on")
        last_step(1, 0)
        own.wait()
        hook(pump, "ready")

        def crossed(off):
            got = out.at[turn(y, off), :, 1 - c]
            remote(got, got, r.ag_dsend, r.ag_drecv.at[off], partner).wait_recv()

        def order(i):
            if isinstance(i, int):
                return (OWN, BEFORE, AFTER, FAR)[i]
            return lax.rem(3 * i + 3 * (i // 2) + 2 * (i // 3), RING)

        def fetch(i, slot):
            off = order(i)
            crossed(off)
            h_copy(l, turn(y, off), slot).start()

        def up_ready():
            hook(pump, "up")
            loaded(UP1 if l else UP0)

        crossed(0)
        h_copy(l, y, 0).start()

        def opening():
            second_step(1)
            hook(pump, "k1")

        def turn_of(i):
            slot = lax.rem(i, H_SLOTS)
            s = turn(y, order(i))
            h_copy(l, s, slot).wait()
            pump(("seq", i))
            one(l, s, slot, i)

            @pl.when(i == 1)
            def _():
                tail_b()

            @pl.when(i == 2)
            def _():
                tail_c()
                fetch(LAST, 0)

            return s, slot

        def neighbours():
            tail_a()
            for n in (1, 2):
                fetch(n, n)

        if l:
            @pl.loop(0, RING)
            def _(i):
                s, slot = turn_of(i)

                @pl.when(i == 0)
                def _():
                    opening()
                    up_ready()

                pump(("two", i))
                two(s, slot)

                @pl.when(i == 0)
                def _():
                    neighbours()
        else:
            h_copy(l, y, 0).wait()
            hook(pump, "own")
            one(l, y, 0, 0)
            opening()
            neighbours()

            @pl.loop(1, RING)
            def _(i):
                turn_of(i)

                @pl.when(i == 1)
                def _():
                    up_ready()

                pump(("two", i - 1))
                two(turn(y, order(i - 1)), lax.rem(i - 1, H_SLOTS))

            hook(pump, "two3")
            two(turn(y, FAR), 0)

        for slot in BOTH:
            for i in BOTH:
                kv_out_copy(l, 0, slot, i).wait()
        sent = (out.at[y, x], out.at[y], out.at[y, x, c], out.at[y, pl.ds(0, CORES)])
        for kind, ref in enumerate(sent):
            remote(ref, ref, r.ag_send.at[kind], r.ag_recv.at[kind], partner).wait_send()
        remote(out.at[pl.ds(0, 2)], out.at[pl.ds(0, 2)], r.ag_dsend, r.ag_drecv.at[0], partner).wait_send()

    def h_copy(l, s, slot):
        return pltpu.make_async_copy(r.h_all.at[l, s], r.hb.at[slot], r.h_sem.at[slot])

    def h_tile(slot):
        return r.hb[slot].reshape(seq_len, d_model)

    def project(h, lo, n):
        w = r.wv[:, :, lo:lo + n].reshape(d_model, n)
        return jnp.dot(h, w, preferred_element_type=F32).astype(BF)

    def rope(val):
        val = val.astype(F32)
        return val * r.cos[...] + pltpu.roll(val, head_dim // 2, 1) * r.sin[...]

    n_chunk = min(256, f_loc)

    def kv_out_copy(l, s, slot, i):
        return pltpu.make_async_copy(r.qkv.at[slot, i], r.kv_out.at[l, i, s], r.kvo_sem.at[slot, i])

    def one(l, s, slot, i):
        pair = i % 2 if isinstance(i, int) else lax.rem(i, 2)

        @pl.when(i >= 2)
        def _():
            for k in BOTH:
                kv_out_copy(l, s, pair, k).wait()

        kv = jnp.zeros((seq_len, 2 * head_dim), F32)
        for zz in RINGS:
            for yy in RINGS:
                col = (zz * RING + yy) * d_row
                kv += lax.dot_general(h_cols(slot, col, d_row), r.kvb[yy, zz], (((1,), (1,)), ((), ())), preferred_element_type=F32)
        kv = kv.astype(BF)
        r.qkv[pair, 0] = rope(kv[:, :head_dim]).astype(BF)
        r.qkv[pair, 1] = kv[:, head_dim:]
        for i in BOTH:
            kv_out_copy(l, s, pair, i).start()
        q = project(h_tile(slot), 0, head_dim)
        r.stage[...] = (rope(q) * head_dim ** -0.5).astype(BF)
        for lo in range(0, f_loc, n_chunk):
            r.joined[s, :, head_dim + lo:head_dim + lo + n_chunk] = project(h_tile(slot), head_dim + lo, n_chunk)
        n_tile = seq_len // 2
        for i in BOTH:
            keys = (i + 1) * n_tile
            sc = lax.dot_general(r.stage[i * n_tile:(i + 1) * n_tile, :], r.qkv[pair, 0, :keys, :], (((1,), (1,)), ((), ())), preferred_element_type=F32)
            row_id = lax.broadcasted_iota(jnp.int32, sc.shape, 0) + i * n_tile
            col_id = lax.broadcasted_iota(jnp.int32, sc.shape, 1)
            sc = jnp.where(col_id <= row_id, sc, -1e30)
            top = jnp.max(sc, axis=-1, keepdims=True)
            ex = jnp.exp(sc - top)
            prob = (ex * (1.0 / jnp.sum(ex, axis=-1, keepdims=True))).astype(BF)
            att = jnp.dot(prob, r.qkv[pair, 1, :keys, :], preferred_element_type=F32)
            r.joined[s, i * n_tile:(i + 1) * n_tile, :head_dim] = att.astype(BF)

    def h_cols(slot, col, n):
        return r.hb[slot, :, :, :, col:col + n].reshape(seq_len, n)

    def two(s, slot):
        for lo in range(0, f_loc, n_chunk):
            up = project(h_tile(slot), head_dim + f_loc + lo, n_chunk).astype(F32)
            cols = slice(head_dim + lo, head_dim + lo + n_chunk)
            g = r.joined[s, :, cols].astype(F32)
            r.joined[s, :, cols] = (g * jax.nn.sigmoid(g) * up).astype(BF)

    def out_scatter(l, pump):
        def peer(q, first, second):
            dy = first * (1 - q) + second * q
            dx = first * q + second * (1 - q)
            return (z, turn(y, dy), turn(x, dx), c)

        def die_copy(ch, q, s):
            return remote(r.away.at[q], r.die_in.at[ch, q, s], r.dsend.at[q], r.drecv.at[ch, q, s], partner)

        def first_copy(ch, q, d):
            return remote(r.acc.at[ch, q, 0, pl.ds(CORES * d, CORES)], r.in1.at[ch, q, d], r.rs_send.at[0], r.recv1.at[ch, q, d],
                          peer(q, SIGN[d], 0))

        def second_copy(ch, q, d, h):
            js = pl.ds(CORES * h, CORES)
            return remote(r.acc.at[ch, q, 1 + d, js], r.in2.at[ch, q, d, js], r.rs_send.at[1], r.recv2.at[ch, q],
                          peer(q, SIGN[d], 0))

        def half_rows(d):
            return pl.ds(d * (rows // 2), rows // 2)

        def third_copy(ch, q, d):
            return remote(r.acc.at[ch, q, LAST, 0, half_rows(d)], r.in3.at[ch, q, d], r.rs_send.at[2], r.recv3.at[ch, q, d],
                          peer(q, 0, SIGN[d]))

        def fourth_copy(ch, q, d):
            return remote(r.acc.at[ch, q, LAST, 1 + d], r.in4.at[ch, q, d], r.rs_send.at[LAST], r.recv4.at[ch, q],
                          peer(q, 0, SIGN[d]))

        n_blk = r.wov.shape[3]

        def plane_of(ch, q):
            if l:
                return turn(z, q if ch else 2 + q)
            return turn(z, LAST - q if ch else q)

        def slot_off(s):
            return lax.rem(2 + 3 * s + 3 * (s // 2) + 2 * (s // 3), RING)

        def tile(ch, q, s):
            off = slot_off(s)
            for cc in BOTH:
                for j in RINGS:
                    oy = off * (1 - q) + SLOT_OFF[j] * q
                    ox = SLOT_OFF[j] * (1 - q) + off * q
                    core = c if cc else 1 - c
                    at = pl.multiple_of((turn(x, ox) * CORES + core) * rows, rows)
                    r.lhs[pl.ds((cc * RING + j) * rows, rows), :] = r.joined[turn(y, oy), pl.ds(at, rows), :]
            left = r.lhs[...]
            zz = plane_of(ch, q)
            for n in RINGS:
                res = jnp.dot(left, r.wov[zz, n], preferred_element_type=F32).astype(BF)
                res = res.reshape(CORES, RING, rows, n_blk)
                r.away[q, :, :, n * n_blk:(n + 1) * n_blk] = res[0]
                r.acc[ch, q, s, :, :, n * n_blk:(n + 1) * n_blk] = res[1]

        def pair_sum(ch, q, s):
            die_copy(ch, q, s).wait_recv()

            @pl.loop(0, RING)
            def _(j):
                r.acc[ch, q, s, j] = r.acc[ch, q, s, j] + r.die_in[ch, q, s, j]

        def stage_a(ch):
            @pl.loop(0, CORES * RING)
            def _(t):
                s = t // CORES
                q = lax.rem(t, CORES)

                @pl.when(s >= 1)
                def _():
                    die_copy(ch, q, s - 1).wait_send()

                if ch:
                    @pl.when(s == 0)
                    def _():
                        die_copy(ch - 1, q, LAST).wait_send()

                tile(ch, q, s)
                die_copy(ch, q, s).start()

                @pl.when(s >= 1)
                def _():
                    pair_sum(ch, q, s - 1)

                @pl.when(s == 1)
                def _():
                    for d in BOTH:
                        first_copy(ch, q, d).start()

                for d in BOTH:
                    @pl.when(s == 2 + d)
                    def _(d=d):
                        second_copy(ch, q, d, 1 - d).start()

                for n in RINGS:
                    name = f"a{ch}s{n}"
                    if pump(name, False):
                        @pl.when(t == CORES * n + 1)
                        def _(name=name):
                            hook(pump, name)

        def stage_b(ch):
            for q in BOTH:
                pair_sum(ch, q, LAST)
            for q in BOTH:
                for d in BOTH:
                    first_copy(ch, q, d).wait_recv()
                    for j in BOTH:
                        at = CORES * d + j
                        r.acc[ch, q, 1 + d, at] = r.acc[ch, q, 1 + d, at] + r.in1[ch, q, d, j]
                    second_copy(ch, q, d, d).start()

        def total(ch, q, j):
            val = r.acc[ch, q, LAST, j].astype(F32)
            for d in BOTH:
                val += r.in2[ch, q, d, j].astype(F32)
            r.acc[ch, q, LAST, j] = val.astype(BF)

        def stage_c(ch):
            for q in BOTH:
                ref = r.in2.at[ch, q]
                remote(ref, ref, r.rs_send.at[1], r.recv2.at[ch, q], here).wait_recv()
                total(ch, q, 0)
                for d in BOTH:
                    third_copy(ch, q, d).start()
                for j in RINGS[1:]:
                    total(ch, q, j)

        def stage_d(ch):
            for q in BOTH:
                for d in BOTH:
                    third_copy(ch, q, d).wait_recv()
                    rws = half_rows(d)
                    r.acc[ch, q, LAST, 1 + d, rws] = r.acc[ch, q, LAST, 1 + d, rws] + r.in3[ch, q, d]
                    fourth_copy(ch, q, d).start()

        def stage_e(ch):
            for q in BOTH:
                ref = r.in4.at[ch, q]
                remote(ref, ref, r.rs_send.at[LAST], r.recv4.at[ch, q], here).wait_recv()
                cols = pl.ds(pl.multiple_of(plane_of(ch, q) * width, width), width)
                upd = r.acc[ch, q, LAST, LAST].astype(F32)
                for d in BOTH:
                    upd += r.in4[ch, q, d].astype(F32)
                upd = upd.astype(BF)
                r.hid[:, cols] = (r.hid[:, cols].astype(F32) + upd.astype(F32)).astype(BF)

        stages = {"a": stage_a, "b": stage_b, "c": stage_c, "d": stage_d, "e": stage_e, "f": leave_a, "g": leave_b, "h": leave_c}
        for step in LAST_ORDER if l else FIRST_ORDER:
            with jax.named_scope(step):
                stages[step[0]](int(step[1]))
            hook(pump, step)
        for q in BOTH:
            die_copy(1, q, LAST).wait_send()
        for n, ref in enumerate((r.in1, r.in2, r.in3, r.in4)):
            remote(ref, ref, r.rs_send.at[n], r.drecv.at[0, 0, 0], here).wait_send()

    def near(fn, t):
        for j in (LAST, 1):
            fn(t, j)

    def far(fn, t):
        fn(t, 2)

    def z_all(t):
        near(z_direct, t)
        far(z_direct, t)

    def peers_of(fn, op="start"):
        for k in range(len(OTHERS)):
            getattr(fn(k), op)()

    def start(pump):
        peers_of(gain_z)
        kv_z()
        peers_of(x_z)
        x_own().start()
        pump("s0")
        with jax.named_scope("gain_a"):
            peers_of(gain_z, "wait_recv")
            peers_of(gain_y)
            kv_y1()
        pump("s1")
        with jax.named_scope("gain_b"):
            peers_of(gain_y, "wait_recv")
            peers_of(gain_x)
            gain_die(x, LAST).start()
        pump("s2")
        with jax.named_scope("x_z"):
            three_planes().wait_recv()
            x_own().wait()
        for oy in RINGS:
            for ox in RINGS:
                if oy or ox:
                    x_plane(oy, ox).start()
        r.xp[c, y, x] = r.xz[:, y, :, pos(x)]
        pump("s3")
        with jax.named_scope("kv_b"):
            kv_y2()
        with jax.named_scope("gain_c"):
            for k, o in enumerate(OTHERS):
                gain_x(k).wait_recv()
                gain_die(turn(x, -o), k).start()
        pump("s4")
        for oy in (OWN, BEFORE, AFTER, FAR):
            with jax.named_scope(f"row_{oy}"):
                x_row(oy)
            pump(f"r{oy}")
        pump("s5")
        kv_y3()
        pump("s6")
        with jax.named_scope("gain_sum"):
            for k in RINGS:
                gain_die(x, k).wait_recv()
            gain_sum()
        with jax.named_scope("turn"):
            x_turn()
        pump("s7")

    def when(i, n, *fns):
        @pl.when(i == n)
        def _():
            for fn in fns:
                fn()

    def plan(steps):
        def pump(step, run=True):
            if not isinstance(step, str):
                for n in RINGS:
                    if (step[0], n) in steps:
                        when(step[1], n, lambda n=n: run_steps(steps[step[0], n]))
                return True
            found = steps.get(step, ())
            if run:
                run_steps(found)
            return found
        return pump

    def run_steps(steps):
        for fn, *args in steps:
            with jax.named_scope(f"{fn.__name__}_{args[-1] if args else 0}"):
                fn(*args)

    first_entry = plan({
        "s0": [(z_own, UP0)],
        "s1": [(y_send, QG0)],
        "s3": [(z_own, QG0)],
        "r0": [(y_relay, QG0), (z_forward, UP0, OWN), (z_direct, QG0, AFTER), (z_forward, QG0, OWN), (z_direct, QG0, BEFORE)],
        "s6": [(kv_x1, 0)],
    })
    first_front = plan({
        "begin": [(kv_x2, 0), (y_send, UP0), (z_forward, QG0, AFTER), (z_direct, QG0, FAR)],
        "k0": [(y_relay, UP0), (kv_x3, 0), (z_forward, QG0, BEFORE), (z_forward, QG0, FAR), (z_direct, UP0, AFTER), (z_direct, UP0, BEFORE)],
        "first_on": [(y_send, WO0)],
        "ready": [(load_near, QG0), (load_far, QG0), (kv_load, 0), (loaded, QG0), (kv_loaded,)],
        "k1": [(z_direct, UP0, FAR), (z_forward, UP0, AFTER)],
        "k2": [
            (z_forward, UP0, BEFORE), (y_relay, WO0), (z_forward, UP0, FAR), (y_send, QG1), (z_own, WO0), (z_direct, WO0, BEFORE),
            (kv_x1, 1),
        ],
        ("seq", 1): [(y_send, WO1), (z_direct, WO0, AFTER), (x_sent,)],
        "up": [(y_send, UP1), (z_direct, WO0, FAR), (load_near, UP0), (load_far, UP0)],
        ("two", 0): [(y_relay, QG1), (z_forward, WO0, OWN)],
        ("seq", 2): [(kv_x2, 1)],
        ("two", 1): [(kv_x3, 1), (z_direct, QG1, AFTER), (z_forward, WO0, BEFORE)],
        ("seq", 3): [(y_relay, WO1), (z_forward, WO0, AFTER)],
        ("two", 2): [(z_forward, WO0, FAR), (z_own, QG1), (y_relay, UP1)],
        "near": [(load_near, WO0)],
    })
    first_scatter = plan({
        "a0s0": [(z_forward, QG1, AFTER)],
        "a0s2": [(z_direct, QG1, BEFORE)],
        "b0": [(load_far, WO0), (far_loaded, WO0)],
        "a1s0": [(z_direct, QG1, FAR)],
        "a1s1": [(z_forward, QG1, OWN)],
        "a1": [(z_direct, UP1, FAR)],
        "b1": [(z_direct, UP1, BEFORE)],
        "c1": [(z_forward, QG1, FAR), (z_direct, UP1, AFTER), (z_own, UP1), (z_forward, QG1, BEFORE)],
        "e0": [(z_forward, UP1, FAR)],
    })
    second_front = plan({
        "begin": [(z_forward, UP1, BEFORE), (kv_load, 1)],
        "first": [(z_forward, UP1, AFTER)],
        "k0": [(z_forward, UP1, OWN), (z_direct, WO1, FAR)],
        "ready": [(load_near, QG1), (load_far, QG1), (loaded, QG1), (kv_loaded,)],
        ("seq", 0): [(z_own, WO1)],
        "k1": [(z_direct, WO1, BEFORE)],
        "up": [(load_near, UP1), (load_far, UP1)],
        "k2": [(z_direct, WO1, AFTER)],
        ("seq", 1): [(z_forward, WO1, FAR)],
        ("two", 1): [(z_forward, WO1, OWN)],
        ("two", 2): [(z_forward, WO1, BEFORE), (z_forward, WO1, AFTER)],
        "near": [(load_near, WO1), (load_far, WO1)],
    })
    second_scatter = plan({
    })

    with jax.named_scope("start"):
        start(first_entry)
    with jax.named_scope("front_0"):
        gather_norm(0, rows // RING, first_front)
    with jax.named_scope("near_0"):
        kv_share(0)
        first_front("near")
        near_loaded(WO0)
    with jax.named_scope("scatter_0"):
        out_scatter(0, first_scatter)
    with jax.named_scope("front_1"):
        gather_norm(1, rows // 2, second_front)
    with jax.named_scope("near_1"):
        kv_share(1)
        second_front("near")
        loaded(WO1)
    with jax.named_scope("scatter_1"):
        out_scatter(1, second_scatter)
    with jax.named_scope("drain"):
        left()
        for t in range(WO1 + 1):
            drain(t)
        for l in range(n_layers):
            kv_shared(l)
            kv_sent(l)


def run_model(xt, gain, wkv_t, w_in, w_out, cos_full, sin_full):
    batch, d_local, seq_len = xt.shape
    n_layers, d_row, e_block = w_in.shape
    r_block, d_col = w_out.shape[1:]
    head_dim = cos_full.shape[1]
    d_model = d_row * RING * RING
    seqs = batch // RING
    rows = seqs * seq_len // (RING * RING * CORES)
    e_loc, r_loc = e_block // RING, r_block // RING
    kc = wkv_t.shape[1]
    width = d_model // RING
    n_t = 3 * n_layers
    n_o = len(OTHERS)

    def dma(*shape):
        return pltpu.SemaphoreType.DMA(shape)

    def vm(*shape):
        return pltpu.VMEM(shape, BF)

    def out(*shape):
        return jax.ShapeDtypeStruct(shape, BF)

    any_spec = pl.BlockSpec(memory_space=pl.ANY)
    vm_spec = pl.BlockSpec(memory_space=pltpu.VMEM)
    out_shape = [
        out(batch, d_local, seq_len),
        out(n_layers, 2, seqs, seq_len, head_dim),
        out(n_layers, RING, RING, CORES, rows, d_model),
        out(n_layers, RING, RING * d_row, e_loc),
        out(n_layers, RING, RING, r_loc, d_col),
        out(RING, CORES, n_layers, RING, RING, kc, d_row),
        out(n_layers, RING, 2, seqs, CORES * (seq_len // (CORES * RING * RING * RING)), head_dim),
        out(n_layers, 2, d_row // 2, e_loc),
        out(n_layers, 2, r_loc // 2, d_col),
    ]
    pair = (2, 2, 2)
    scratch = [
        vm(rows, d_model), vm(rows, d_model), pltpu.VMEM((n_layers, d_model), F32),
        vm(RING, CORES, RING, RING, G_ROWS, d_row),
        vm(RING, seqs, d_local, seq_len),
        vm(CORES, RING, RING, RING, d_local, CORES * rows),
        vm(RING, RING * d_row, e_loc), vm(RING, RING, 2 * head_dim, d_row), vm(RING, RING, r_loc, d_col),
        vm(H_SLOTS, RING, CORES, rows, d_model), vm(RING, seq_len, r_loc), vm(2, 2, seq_len, head_dim), vm(seq_len, head_dim),
        vm(CORES * RING * rows, r_loc), vm(2, RING, rows, width), vm(2, 2, RING, RING, rows, width), vm(2, 2, RING, RING, rows, width),
        vm(*pair, 2, rows, width), vm(*pair, RING, rows, width), vm(*pair, rows // 2, width), vm(*pair, rows, width),
        pltpu.SemaphoreType.DMA, pltpu.SemaphoreType.DMA, dma(RING), dma(RING), pltpu.SemaphoreType.DMA, pltpu.SemaphoreType.DMA,
        pltpu.SemaphoreType.DMA,
        dma(3 * n_o), dma(3 * n_o), dma(RING), dma(RING),
        dma(RING), dma(RING), dma(2, RING), dma(2, RING), dma(RING), dma(RING), pltpu.SemaphoreType.DMA,
        dma(RING), dma(40), pltpu.SemaphoreType.DMA, dma(RING), pltpu.SemaphoreType.DMA, dma(H_SLOTS), dma(2, 2), dma(3), dma(3),
        dma(n_t, RING), dma(n_t, 2), dma(3, RING, 2), dma(3), dma(n_t),
        dma(n_o), dma(n_o), pltpu.SemaphoreType.DMA, dma(n_o), dma(n_layers), dma(n_layers, n_o), dma(n_layers), dma(n_layers), dma(2),
        dma(2), dma(2, 2, RING), dma(RING), dma(*pair), dma(2, 2), dma(*pair), dma(2, 2),
        dma(n_layers, n_o), dma(n_layers, n_o), dma(n_layers),
    ]
    res = pl.pallas_call(
        model_kernel,
        out_shape=out_shape,
        in_specs=[any_spec, vm_spec, vm_spec, any_spec, any_spec, vm_spec, vm_spec],
        out_specs=[any_spec] * len(out_shape),
        scratch_shapes=scratch,
        compiler_params=pltpu.CompilerParams(collective_id=0, has_side_effects=True, vmem_limit_bytes=VMEM_LIMIT),
        name="two_layers",
    )(xt, gain, wkv_t, w_in, w_out, cos_full, sin_full)
    return res[0], res[6]


def solution(mesh):
    row_size = mesh.shape["row"]
    n_col = mesh.shape["col"]
    n_z = row_size // RING
    n_y = RING
    n_x = n_col // CORES
    n_tp = n_y * n_col
    n_dev = row_size * n_col
    mesh4 = Mesh(mesh.devices.reshape(n_z, n_y, n_x, CORES), ("z", "y", "x", "core"))
    every = ("z", "y", "x", "core")
    col = ("x", "core")
    act_spec = P(NIL, NIL, every)
    w_spec = P(NIL, ("z", "y"), col)

    def device_fn(x_loc, gain_loc, w_in_loc, w_kv_loc, w_out_loc):
        n_layers = w_in_loc.shape[0]
        n_batch, seq_len, d_local = x_loc.shape
        head_dim = w_kv_loc.shape[2] * n_col // 2
        batch_loc = n_batch // n_z
        seq_local = seq_len // n_dev
        steps = np.arange(head_dim // 2, dtype=np.float32)
        inv_freq = (1.0 / 10000.0 ** (steps * 2 / head_dim)).astype(np.float32)
        angles = np.arange(seq_len, dtype=np.float32)[:, NIL] * inv_freq[NIL, :]
        cos_tab, sin_tab = np.cos(angles), np.sin(angles)
        cos_full = jnp.asarray(np.concatenate([cos_tab, cos_tab], axis=1))
        sin_full = jnp.asarray(np.concatenate([-sin_tab, sin_tab], axis=1))
        y_loc, kv = run_model(x_loc.transpose(0, 2, 1), gain_loc, w_kv_loc.transpose(0, 2, 1), w_in_loc, w_out_loc, cos_full, sin_full)
        y_loc = y_loc.transpose(0, 2, 1)
        kv = kv.reshape(n_layers, n_z, 2, batch_loc, CORES, seq_local, head_dim)
        kv = lax.dynamic_index_in_dim(kv, lax.axis_index("core"), axis=4, keepdims=False)
        kv = kv.transpose(0, 2, 1, 3, 4, 5).reshape(n_layers, 2, n_batch, seq_local, head_dim)
        return y_loc, kv

    return jax.shard_map(device_fn, mesh=mesh4, in_specs=(act_spec, P(NIL, every), w_spec, w_spec, P(NIL, col, ("z", "y"))), out_specs=(act_spec, P(NIL, NIL, NIL, every, NIL)), check_vma=False)
```

```python
import typing

import jax
import jax.numpy as jnp
import numpy as np
from jax import lax
from jax.experimental import pallas as pl
from jax.experimental.pallas import tpu as pltpu
from jax.sharding import Mesh
from jax.sharding import PartitionSpec as P

LN_EPS = 1e-6
RING = 4
CORES = 2
VMEM_LIMIT = 67_000_000
BF = jnp.bfloat16
F32 = jnp.float32
SLOT_OFF = (2, 1, 3, 0)
SIGN = (1, -1)
NIL = None
BOTH = range(CORES)
RINGS = range(RING)
OTHERS = (1, 3, 2)
LAST = RING - 1
G_ROWS = 8
H_SLOTS = 3
QG0, UP0, WO0, QG1, UP1, WO1 = range(6)
OWN, AFTER, FAR, BEFORE = RINGS
FIRST_ORDER = ("a0", "b0", "a1", "b1", "c0", "c1", "d0", "d1", "e0", "e1")
LAST_ORDER = FIRST_ORDER[:-1] + ("f1", "e1", "g1", "f0", "g0", "h1", "h0")
KINDS = ("first", "second", "first_on", "second_on")


class Refs(typing.NamedTuple):
    xt: typing.Any
    gain_in: typing.Any
    wkv: typing.Any
    w_in: typing.Any
    w_out: typing.Any
    cos_in: typing.Any
    sin_in: typing.Any
    y_out: typing.Any
    kv_out: typing.Any
    h_all: typing.Any
    wi: typing.Any
    wo: typing.Any
    kvh: typing.Any
    kvx: typing.Any
    rwi: typing.Any
    rwo: typing.Any
    cos: typing.Any
    sin: typing.Any
    gain_own: typing.Any
    h_ref: typing.Any
    hid: typing.Any
    gain: typing.Any
    gbuf: typing.Any
    xz: typing.Any
    xp: typing.Any
    wv: typing.Any
    kvb: typing.Any
    wov: typing.Any
    hb: typing.Any
    joined: typing.Any
    qkv: typing.Any
    stage: typing.Any
    lhs: typing.Any
    away: typing.Any
    acc: typing.Any
    die_in: typing.Any
    in1: typing.Any
    in2: typing.Any
    in3: typing.Any
    in4: typing.Any
    xz_send: typing.Any
    xz_recv: typing.Any
    xp_send: typing.Any
    xp_recv: typing.Any
    xd_send: typing.Any
    xd_recv: typing.Any
    x_loc: typing.Any
    g_send: typing.Any
    g_recv: typing.Any
    gd_send: typing.Any
    gd_recv: typing.Any
    yd_send: typing.Any
    yd_recv: typing.Any
    yp_send: typing.Any
    yp_recv: typing.Any
    yz_send: typing.Any
    yz_recv: typing.Any
    y_loc: typing.Any
    ag_send: typing.Any
    ag_recv: typing.Any
    ag_dsend: typing.Any
    ag_drecv: typing.Any
    ag_loc: typing.Any
    h_sem: typing.Any
    kvo_sem: typing.Any
    w_load: typing.Any
    far_load: typing.Any
    y_recv: typing.Any
    ry_recv: typing.Any
    zb_recv: typing.Any
    zc_recv: typing.Any
    w_send: typing.Any
    kz_send: typing.Any
    kz_recv: typing.Any
    ky_send: typing.Any
    ky_recv: typing.Any
    kx_send: typing.Any
    kx_recv: typing.Any
    kd_send: typing.Any
    kd_recv: typing.Any
    k_loc: typing.Any
    dsend: typing.Any
    drecv: typing.Any
    rs_send: typing.Any
    recv1: typing.Any
    recv2: typing.Any
    recv3: typing.Any
    recv4: typing.Any
    small: typing.Any
    kvx_send: typing.Any
    kvx_recv: typing.Any
    kvx_loc: typing.Any


def model_kernel(*refs):
    r = Refs(*refs)
    z, y, x, c = (lax.axis_index(a) for a in ("z", "y", "x", "core"))
    n_layers = r.wkv.shape[0]
    rows, d_model = r.hid.shape
    batch, d_local = r.xt.shape[:2]
    seqs = batch // RING
    seq_len, head_dim = r.cos.shape
    d_row = r.w_in.shape[1]
    e_loc = r.wi.shape[3]
    depth = r.wo.shape[3]
    f_loc = depth - head_dim
    quarter = rows // 4
    width = d_model // RING
    q_block = head_dim * RING
    f_block = f_loc * RING

    turned = {id(v): [lax.rem(v + o, RING) for o in RINGS] for v in (z, y, x)}

    def turn(base, off):
        if isinstance(off, int):
            return turned[id(base)][off % RING]
        return lax.rem(base + off + RING, RING)

    def remote(src, dst, ssem, rsem, dev):
        return pltpu.make_async_remote_copy(
            src_ref=src, dst_ref=dst, send_sem=ssem, recv_sem=rsem, device_id=dev, device_id_type=pl.DeviceIdType.MESH)

    partner = (z, y, x, 1 - c)

    peers = [(turn(z, o), y, x, c) for o in OTHERS]
    peers += [(z, turn(y, oy), turn(x, ox), c) for oy in RINGS for ox in RINGS if oy or ox]
    peers.append(partner)
    here = (z, y, x, c)
    gate_sem = pltpu.get_barrier_semaphore()
    for dev in peers:
        pl.semaphore_signal(gate_sem, inc=1, device_id=dev, device_id_type=pl.DeviceIdType.MESH)
    fills = [pltpu.make_async_copy(src, dst, r.small.at[n]) for n, (src, dst) in enumerate(
        ((r.gain_in, r.gain_own), (r.cos_in, r.cos), (r.sin_in, r.sin)))]
    for fill in fills:
        fill.start()
    fills[0].wait()

    src_id = lax.broadcasted_iota(jnp.int32, (d_local, d_row), 0) + (x * CORES + c) * d_local
    dst_id = lax.broadcasted_iota(jnp.int32, (d_local, d_row), 1)
    spread = jnp.where(src_id == dst_id, 1.0, 0.0).astype(BF)
    r.gbuf[x, c, y, z] = jnp.zeros((G_ROWS, d_row), BF)
    r.gbuf[x, c, y, z, :n_layers] = jnp.dot(r.gain_own[...], spread, preferred_element_type=F32).astype(BF)
    pl.semaphore_wait(gate_sem, len(peers))

    def hook(pump, i):
        with jax.named_scope(f"hook_{i}"):
            pump(i)

    def w_cols(kind):
        return pl.ds(0, head_dim + f_loc) if kind == 0 else pl.ds(head_dim + f_loc, f_loc)

    def piece(t, zz, yy):
        l, kind = t // 3, t % 3
        if kind == 2:
            return r.wo.at[l, zz, yy]
        return r.wi.at[l, zz, pl.ds(pl.multiple_of(yy * d_row, d_row), d_row), w_cols(kind)]

    def piece_half(t, zz, yy, h):
        l, kind = t // 3, t % 3
        if kind == 2:
            return r.wo.at[l, zz, yy, pl.ds(h * (depth // 2), depth // 2)]
        return r.wi.at[l, zz, pl.ds(pl.multiple_of(yy * d_row + h * (d_row // 2), d_row // 2), d_row // 2), w_cols(kind)]

    def own_parts(t, owner, zz, yy):
        l, kind = t // 3, t % 3
        hq = pl.ds(pl.multiple_of(owner * head_dim, head_dim), head_dim)
        if kind == 2:
            return [
                (r.w_out.at[l, hq], r.wo.at[l, zz, yy, pl.ds(0, head_dim)]),
                (r.w_out.at[l, pl.ds(pl.multiple_of(q_block + owner * f_loc, head_dim), f_loc)], r.wo.at[l, zz, yy, pl.ds(head_dim, f_loc)]),
            ]
        rws = pl.ds(pl.multiple_of(yy * d_row, d_row), d_row)
        if kind == 0:
            return [
                (r.w_in.at[l, :, hq], r.wi.at[l, zz, rws, pl.ds(0, head_dim)]),
                (r.w_in.at[l, :, pl.ds(pl.multiple_of(q_block + owner * f_loc, head_dim), f_loc)], r.wi.at[l, zz, rws, pl.ds(head_dim, f_loc)]),
            ]
        return [(r.w_in.at[l, :, pl.ds(pl.multiple_of(q_block + f_block + owner * f_loc, head_dim), f_loc)],
                 r.wi.at[l, zz, rws, pl.ds(head_dim + f_loc, f_loc)])]

    def relay_ref(t, d):
        l, kind = t // 3, t % 3
        return r.rwo.at[l, d] if kind == 2 else r.rwi.at[l, d, :, w_cols(kind)]

    def far_parts(t, d):
        l, kind = t // 3, t % 3
        owner = turn(y, 2)
        hq = pl.ds(pl.multiple_of(owner * head_dim, head_dim), head_dim)
        if kind == 2:
            n = depth // 2
            base = q_block + owner * f_loc
            if d:
                return [(r.w_out.at[l, pl.ds(pl.multiple_of(base + n - head_dim, G_ROWS), n)], r.rwo.at[l, d])]
            return [
                (r.w_out.at[l, hq], r.rwo.at[l, d, pl.ds(0, head_dim)]),
                (r.w_out.at[l, pl.ds(pl.multiple_of(base, head_dim), n - head_dim)], r.rwo.at[l, d, pl.ds(head_dim, n - head_dim)]),
            ]
        rws = pl.ds(d * (d_row // 2), d_row // 2)
        if kind == 0:
            return [
                (r.w_in.at[l, rws, hq], r.rwi.at[l, d, :, pl.ds(0, head_dim)]),
                (r.w_in.at[l, rws, pl.ds(pl.multiple_of(q_block + owner * f_loc, head_dim), f_loc)], r.rwi.at[l, d, :, pl.ds(head_dim, f_loc)]),
            ]
        return [(r.w_in.at[l, rws, pl.ds(pl.multiple_of(q_block + f_block + owner * f_loc, head_dim), f_loc)], relay_ref(t, d))]

    def y_send(t):
        for d in BOTH:
            owner = turn(y, SIGN[d])
            dev = (z, owner, x, c)
            for src, dst in far_parts(t, d):
                remote(src, dst, r.w_send.at[t], r.ry_recv.at[t, d], dev).start()
            for src, dst in own_parts(t, owner, z, y):
                remote(src, dst, r.w_send.at[t], r.y_recv.at[t, -SIGN[d] % RING], dev).start()

    def y_relay(t):
        for d in BOTH:
            ref = relay_ref(t, d)
            remote(ref, ref, r.w_send.at[t], r.ry_recv.at[t, d], here).wait_recv()
            dst = piece_half(t, z, turn(y, -SIGN[d]), d)
            remote(ref, dst, r.w_send.at[t], r.y_recv.at[t, 2], (z, turn(y, SIGN[d]), x, c)).start()

    def z_own(t):
        for d in BOTH:
            for src, dst in own_parts(t, y, z, y):
                remote(src, dst, r.w_send.at[t], r.zb_recv.at[t % 3, 0, d], (turn(z, SIGN[d]), y, x, c)).start()

    def z_direct(t, j):
        yy = turn(y, j)
        ref = piece(t, z, yy)
        remote(ref, ref, r.w_send.at[t], r.y_recv.at[t, j], here).wait_recv()
        for d in BOTH:
            remote(ref, ref, r.w_send.at[t], r.zb_recv.at[t % 3, j, d], (turn(z, SIGN[d]), y, x, c)).start()

    def z_forward(t, j):
        yy = turn(y, j)
        for d in BOTH:
            zz = turn(z, -SIGN[d])
            ref = piece(t, zz, yy)
            remote(ref, ref, r.w_send.at[t], r.zb_recv.at[t % 3, j, d], here).wait_recv()
            part = piece_half(t, zz, yy, d)
            remote(part, part, r.w_send.at[t], r.zc_recv.at[t % 3], (turn(z, SIGN[d]), y, x, c)).start()

    def place(t, zz):
        l, kind = t // 3, t % 3
        if kind == 2:
            return r.wo.at[l, zz], r.wov.at[zz]
        return r.wi.at[l, zz, :, w_cols(kind)], r.wv.at[zz, :, w_cols(kind)]

    def load_near(t):
        kind = t % 3
        for d in BOTH:
            src, dst = place(t, turn(z, SIGN[d]))
            pltpu.make_async_copy(src, dst, r.w_load.at[kind]).start()
        for j in OTHERS:
            yy = turn(y, j)
            dst = r.wov.at[z, yy] if kind == 2 else r.wv.at[z, pl.ds(pl.multiple_of(yy * d_row, d_row), d_row), w_cols(kind)]
            pltpu.make_async_copy(piece(t, z, yy), dst, r.w_load.at[kind]).start()
        for src, dst in own_parts(t, y, z, y):
            pltpu.make_async_copy(src, own_place(t, dst, src), r.w_load.at[kind]).start()

    def load_far(t):
        src, dst = place(t, turn(z, 2))
        remote(src, src, r.w_send.at[t], r.zc_recv.at[t % 3], here).wait_recv()
        pltpu.make_async_copy(src, dst, r.far_load.at[t % 3]).start()

    def own_place(t, dst, src):
        kind = t % 3
        if kind == 2:
            n = src.shape[0]
            return r.wov.at[z, y, pl.ds(0 if n == head_dim and f_loc != head_dim else head_dim, n)]
        n = src.shape[1]
        rws = pl.ds(pl.multiple_of(y * d_row, d_row), d_row)
        if kind == 0:
            return r.wv.at[z, rws, pl.ds(0 if n == head_dim and f_loc != head_dim else head_dim, n)]
        return r.wv.at[z, rws, pl.ds(head_dim + f_loc, f_loc)]

    def near_loaded(t):
        kind = t % 3
        dst = r.wov.at[pl.ds(0, LAST)] if kind == 2 else r.wv.at[pl.ds(0, LAST), :, w_cols(kind)]
        pltpu.make_async_copy(dst, dst, r.w_load.at[kind]).wait()

    def far_loaded(t):
        kind = t % 3
        dst = r.wov.at[0] if kind == 2 else r.wv.at[0, :, w_cols(kind)]
        pltpu.make_async_copy(dst, dst, r.far_load.at[kind]).wait()

    def loaded(t):
        near_loaded(t)
        far_loaded(t)

    def drain(t):
        l, kind = t // 3, t % 3
        ref = r.wo.at[l] if kind == 2 else r.wi.at[l, :, :, w_cols(kind)]
        remote(ref, ref, r.w_send.at[t], r.y_recv.at[t, 0], here).wait_send()

    def kv_z_copy(k):
        return remote(r.wkv, r.kvh.at[x, c, :, y, z], r.kz_send.at[k], r.kz_recv.at[k], (turn(z, OTHERS[k]), y, x, c))

    def kv_own():
        return pltpu.make_async_copy(r.wkv, r.kvh.at[x, c, :, y, z], r.k_loc.at[0])

    def kv_z():
        for k in range(len(OTHERS)):
            kv_z_copy(k).start()
        kv_own().start()

    def kv_y_copy(ref, k, d):
        return remote(ref, ref, r.ky_send, r.ky_recv.at[k], (z, turn(y, SIGN[d]), x, c))

    def kv_y1():
        kv_own().wait()
        for k in range(len(OTHERS)):
            kv_z_copy(k).wait()
        for d in BOTH:
            kv_y_copy(r.kvh.at[x, c, :, y], d, d).start()

    def kv_y2():
        for d in BOTH:
            yy = turn(y, -SIGN[d])
            kv_y_copy(r.kvh.at[x, c, :, yy], d, d).wait_recv()
            kv_y_copy(r.kvh.at[x, c, :, yy, pl.ds(2 * d, 2)], 2, d).start()

    def kv_y3():
        kv_y_copy(r.kvh.at[x, c, :, turn(y, 2)], 2, 0).wait_recv()
        kv_y_copy(r.kvh.at[x, c, :, pl.ds(0, LAST)], 0, 0).wait_send()

    def kv_x_copy(l, ref, k, d):
        return remote(ref, ref, r.kx_send.at[l], r.kx_recv.at[l, k], (z, y, turn(x, SIGN[d]), c))

    def kv_die(l, ref):
        return remote(ref, ref, r.kd_send.at[l], r.kd_recv.at[l], partner)

    def kv_x1(l):
        ref = r.kvh.at[x, c, l]
        for d in BOTH:
            kv_x_copy(l, ref, d, d).start()
        kv_die(l, ref).start()

    def kv_x2(l):
        for d in BOTH:
            xx = turn(x, -SIGN[d])
            ref = r.kvh.at[xx, c, l]
            kv_x_copy(l, ref, d, d).wait_recv()
            kv_x_copy(l, r.kvh.at[xx, c, l, pl.ds(2 * d, 2)], 2, d).start()
            kv_die(l, ref).start()

    def kv_x3(l):
        ref = r.kvh.at[turn(x, 2), c, l]
        kv_x_copy(l, ref, 2, 0).wait_recv()
        kv_die(l, ref).start()

    def kv_load(l):
        kv_die(l, r.kvh.at[:, 1 - c, l]).wait_recv()
        kc = r.wkv.shape[1]
        for xx in RINGS:
            for cc in BOTH:
                pltpu.make_async_copy(r.kvh.at[xx, cc, l], r.kvb.at[:, :, pl.ds((xx * CORES + cc) * kc, kc)], r.k_loc.at[1]).start()

    def kv_sent(l):
        kv_x_copy(l, r.kvh.at[pl.ds(0, LAST), c, l], 0, 0).wait_send()
        kv_die(l, r.kvh.at[:, c, l]).wait_send()

    def kv_loaded():
        pltpu.make_async_copy(r.kvb, r.kvb, r.k_loc.at[1]).wait()

    def gain_move(i, src, dst, dev):
        return remote(src, dst, r.g_send.at[i], r.g_recv.at[i], dev)

    def gain_z(k):
        dev = (turn(z, OTHERS[k]), y, x, c)
        return gain_move(k, r.gbuf.at[x, c, y, z], r.gbuf.at[x, c, y, z], dev)

    def gain_y(k):
        dev = (z, turn(y, OTHERS[k]), x, c)
        return gain_move(len(OTHERS) + k, r.gbuf.at[x, c, y], r.gbuf.at[x, c, y], dev)

    def gain_x(k):
        dev = (z, y, turn(x, OTHERS[k]), c)
        return gain_move(CORES * len(OTHERS) + k, r.gbuf.at[x, c], r.gbuf.at[x, c], dev)

    def gain_die(xx, k):
        ref = r.gbuf.at[xx, c]
        return remote(ref, ref, r.gd_send.at[k], r.gd_recv.at[k], partner)

    def gain_sum():
        for zz in RINGS:
            for yy in RINGS:
                tot = jnp.zeros((n_layers, d_row), F32)
                for xx in RINGS:
                    for cc in BOTH:
                        tot += r.gbuf[xx, cc, yy, zz, :n_layers].astype(F32)
                at = (zz * RING + yy) * d_row
                r.gain[:, at:at + d_row] = tot

    tok_pair = CORES * rows

    def x_z(k):
        zz = turn(z, OTHERS[k])
        src = r.xt.at[pl.ds(zz * seqs, seqs)]
        return remote(src, r.xz.at[z], r.xz_send, r.xz_recv, (zz, y, x, c))

    def three_planes():
        ref = r.xz.at[pl.ds(0, LAST)]
        return remote(ref, ref, r.xz_send, r.xz_recv, here)

    def x_own():
        return pltpu.make_async_copy(r.xt.at[pl.ds(z * seqs, seqs)], r.xz.at[z], r.x_loc)

    def pos(xx):
        return pl.ds(pl.multiple_of(xx * tok_pair, tok_pair), tok_pair)

    def x_plane(oy, ox):
        yy, xx = turn(y, oy), turn(x, ox)
        return remote(r.xz.at[:, yy, :, pos(xx)], r.xp.at[c, y, x], r.xp_send.at[oy], r.xp_recv.at[(RING - oy) % RING], (z, yy, xx, c))

    def row_bytes(oy):
        return r.xp.at[c, 0] if oy else r.xp.at[c, 0, pl.ds(0, RING - 1)]

    def x_row(oy):
        yy = turn(y, oy)
        got = row_bytes(oy)
        remote(got, got, r.xp_send.at[oy], r.xp_recv.at[oy], partner).wait_recv()
        row = r.xp.at[c, yy]
        remote(row, row, r.xd_send, r.xd_recv, partner).start()

    def x_turn():
        got = r.xp.at[1 - c]
        remote(got, got, r.xd_send, r.xd_recv, partner).wait_recv()

        @pl.loop(0, RING)
        def _(zz):
            for yy in RINGS:
                for xh in BOTH:
                    blk = [r.xp[cc, yy, CORES * xh + xx, zz] for xx in BOTH for cc in BOTH]
                    blk = jnp.concatenate(blk, axis=0).astype(F32).T.astype(BF)
                    n = blk.shape[1]
                    at = pl.multiple_of(zz * RING * d_row + yy * d_row + xh * n, n)
                    r.hb[0, 0, :, :, pl.ds(at, n)] = blk.reshape(CORES, rows, n)
        r.hid[...] = r.hb[0, 0, c]
        remote(got, got, r.xd_send, r.xd_recv, partner).wait_send()

    def x_sent():
        three_planes().wait_send()
        for fn in (gain_z, gain_y, gain_x):
            peers_of(fn, "wait_send")
        for k in RINGS:
            gain_die(x, k).wait_send()
        for oy in RINGS:
            got = row_bytes(oy)
            remote(got, got, r.xp_send.at[oy], r.xp_recv.at[oy], partner).wait_send()

    def y_die(p):
        cols = pl.ds(pl.multiple_of(turn(z, p) * width, width), width)
        return remote(r.hid.at[:, cols], r.hb.at[0, 0, c, :, cols], r.yd_send.at[p], r.yd_recv.at[p], partner)

    def planes(h):
        return pl.ds(2 * h, 2)

    def y_plane(h, oy, ox):
        yy, xx = turn(y, oy), turn(x, ox)
        return remote(r.xp.at[c, yy, xx, planes(h)], r.xz.at[planes(h), y, :, pos(x)], r.yp_send.at[h, oy], r.yp_recv.at[h, (RING - oy) % RING],
                      (z, yy, xx, c))

    def y_z(p, oy):
        s = turn(y, oy)
        return remote(r.xz.at[p, s], r.y_out.at[z * seqs + s], r.yz_send.at[p], r.yz_recv.at[p], (turn(z, p), y, x, c))

    def y_own(oy):
        s = turn(y, oy)
        return pltpu.make_async_copy(r.xz.at[0, s], r.y_out.at[z * seqs + s], r.y_loc)

    def leave_a(h):
        for p in BOTH:
            p = 2 * h + p
            y_die(p).start()
            cols = pl.ds(pl.multiple_of(turn(z, p) * width, width), width)
            r.hb[0, 0, c, :, cols] = r.hid[:, cols]

    def leave_b(h):
        n = CORES * CORES * d_local
        for p in BOTH:
            p = 2 * h + p
            y_die(p).wait()

            @pl.loop(0, RING)
            def _(yy, p=p):
                for xh in BOTH:
                    at = pl.multiple_of(turn(z, p) * width + yy * d_row + xh * n, n)
                    blk = r.hb[0, 0, :, :, pl.ds(at, n)].reshape(tok_pair, n).astype(F32).T.astype(BF)
                    for xx in BOTH:
                        for cc in BOTH:
                            lo = (xx * CORES + cc) * d_local
                            r.xp[cc, yy, CORES * xh + xx, p] = blk[lo:lo + d_local]

        for oy in OTHERS + (0,):
            for ox in RINGS:
                if oy or ox:
                    y_plane(h, oy, ox).start()
        for p in BOTH:
            p = 2 * h + p
            r.xz[p, y, :, pos(x)] = r.xp[c, y, x, p]

    def plane_bytes(h, oy):
        return r.xp.at[c, 0, :, planes(h)] if oy else r.xp.at[c, 0, pl.ds(0, LAST), planes(h)]

    def leave_c(h):
        for oy in OTHERS + (0,):
            got = plane_bytes(h, oy)
            remote(got, got, r.yp_send.at[h, oy], r.yp_recv.at[h, oy], partner).wait_recv()
            for p in BOTH:
                p = 2 * h + p
                (y_z(p, oy) if p else y_own(oy)).start()

    def left():
        for oy in RINGS:
            for h in BOTH:
                got = plane_bytes(h, oy)
                remote(got, got, r.yp_send.at[h, oy], r.yp_recv.at[h, oy], partner).wait_send()
        for p in OTHERS:
            ref = r.xz.at[p]
            remote(ref, ref, r.yz_send.at[p], r.yz_recv.at[p], here).wait()
        pltpu.make_async_copy(r.xz.at[0], r.xz.at[0], r.y_loc).wait()

    def kv_rows(zz):
        n = CORES * seq_len // (RING * RING * RING * CORES)
        return pl.ds(pl.multiple_of(((zz * RING + y) * RING + x) * n, n), n)

    def kv_trade(l, k):
        zz = turn(z, OTHERS[k])
        return remote(r.kv_out.at[l, :, :, kv_rows(zz)], r.kvx.at[l, z], r.kvx_send.at[l, k], r.kvx_recv.at[l, k], (zz, y, x, c))

    def kv_keep(l):
        return pltpu.make_async_copy(r.kv_out.at[l, :, :, kv_rows(z)], r.kvx.at[l, z], r.kvx_loc.at[l])

    def kv_share(l):
        for k in range(len(OTHERS)):
            kv_trade(l, k).start()
        kv_keep(l).start()

    def kv_shared(l):
        for k in range(len(OTHERS)):
            kv_trade(l, k).wait()
        kv_keep(l).wait()

    def gather_norm(l, split, pump):
        hid = r.hid
        gain = r.gain[l:l + 1, :]
        for b in range(4):
            blk = hid[b * quarter:(b + 1) * quarter, :].astype(F32)
            mean = jnp.mean(blk, axis=-1, keepdims=True)
            cen = blk - mean
            var = jnp.mean(cen * cen, axis=-1, keepdims=True)
            r.h_ref[b * quarter:(b + 1) * quarter, :] = (cen * lax.rsqrt(var + LN_EPS) * gain).astype(BF)
        out = r.h_all.at[l]

        def spot(q, first, second):
            if q == 0:
                return turn(y, second), turn(x, first)
            return turn(y, first), turn(x, second)

        def span(q, part):
            lo, n = (split, rows - split) if q else (0, split)
            if part is NIL:
                return pl.ds(lo, n)
            return pl.ds(lo + part * (n // 2), n // 2)

        offs = (0, -1, 1, 2)
        plans = {}
        for q in BOTH:
            for d in BOTH:
                plans["first", q, d] = (q, 0, 0, NIL, SIGN[d], 0)
                plans["first_on", q, d] = (q, -SIGN[d], 0, d, SIGN[d], 0)
                for k in RINGS:
                    plans["second", q, k, d] = (q, offs[k], 0, NIL, 0, SIGN[d])
                    plans["second_on", q, k, d] = (q, offs[k], -SIGN[d], d, 0, SIGN[d])
        index = {key: n for n, key in enumerate(plans)}

        def link(*key, own=False):
            idx, (q, first, second, part, to_first, to_second) = index[key], plans[key]
            sy, sx = spot(q, first, second)
            ty, tx = spot(q, to_first, to_second)
            rws = span(q, part)
            dst = out.at[sy, sx, c, rws]
            return remote(r.h_ref.at[rws] if own else dst, dst, r.ag_send.at[KINDS.index(key[0])], r.ag_recv.at[idx], (z, ty, tx, c))

        def arrived(*key):
            for d in BOTH:
                link(*key, d).wait_recv()

        def die(q, first, second, own=False):
            sy, sx = spot(q, first, second)
            rws = span(q, NIL)
            dst = out.at[sy, sx, c, rws]
            off = (first if q else second) % RING
            remote(r.h_ref.at[rws] if own else dst, dst, r.ag_dsend, r.ag_drecv.at[off], partner).start()

        def take(k, q):
            for d in BOTH:
                link("second", q, k, d).wait_recv()
                die(q, offs[k], -SIGN[d])

        def pass_on(k, q):
            for d in BOTH:
                link("second_on", q, k, d).start()

        def second_step(k):
            take(k, 1)
            pass_on(k, 1)
            take(k, 0)

        def far_first(q):
            for e in BOTH:
                link("second", q, LAST, e).start()

        def last_step(q, k):
            arrived("second_on", q, k)
            die(q, offs[k], 2)

        def tail_a():
            second_step(2)
            far_first(1)
            for k in RINGS[:-1]:
                pass_on(k, 0)
            hook(pump, "k2")
            take(LAST, 0)
            pass_on(LAST, 0)
            hook(pump, "k3")
            for k in (1, 2):
                last_step(1, k)

        def tail_b():
            take(LAST, 1)
            pass_on(LAST, 1)

        def tail_c():
            for k in RINGS:
                last_step(0, k)
            last_step(1, LAST)

        for q in BOTH:
            for d in BOTH:
                link("first", q, d, own=True).start()
        for q in BOTH:
            for d in BOTH:
                link("second", q, 0, d, own=True).start()
        for q in BOTH:
            die(q, 0, 0, own=True)
        own = pltpu.make_async_copy(r.h_ref, out.at[y, x, c], r.ag_loc)
        own.start()
        hook(pump, "begin")
        for d in BOTH:
            for q in BOTH:
                link("first", q, d).wait_recv()
                src = -SIGN[d]
                link("first_on", q, d).start()
                die(q, src, 0)
        hook(pump, "first")
        second_step(0)
        for q in reversed(BOTH):
            for d in BOTH:
                for e in BOTH:
                    link("second", q, 1 + d, e).start()
        hook(pump, "k0")
        for q in BOTH:
            arrived("first_on", q)
            die(q, 2, 0)
        far_first(0)
        hook(pump, "first_on")
        last_step(1, 0)
        own.wait()
        hook(pump, "ready")

        def crossed(off):
            got = out.at[turn(y, off), :, 1 - c]
            remote(got, got, r.ag_dsend, r.ag_drecv.at[off], partner).wait_recv()

        def order(i):
            if isinstance(i, int):
                return (OWN, BEFORE, AFTER, FAR)[i]
            return lax.rem(3 * i + 3 * (i // 2) + 2 * (i // 3), RING)

        def fetch(i, slot):
            off = order(i)
            crossed(off)
            h_copy(l, turn(y, off), slot).start()

        def up_ready():
            hook(pump, "up")
            loaded(UP1 if l else UP0)

        crossed(0)
        h_copy(l, y, 0).start()

        def opening():
            second_step(1)
            hook(pump, "k1")

        def turn_of(i):
            slot = lax.rem(i, H_SLOTS)
            s = turn(y, order(i))
            h_copy(l, s, slot).wait()
            pump(("seq", i))
            one(l, s, slot, i)

            @pl.when(i == 1)
            def _():
                tail_b()

            @pl.when(i == 2)
            def _():
                tail_c()
                fetch(LAST, 0)

            return s, slot

        def neighbours():
            tail_a()
            for n in (1, 2):
                fetch(n, n)

        if l:
            @pl.loop(0, RING)
            def _(i):
                s, slot = turn_of(i)

                @pl.when(i == 0)
                def _():
                    opening()
                    up_ready()

                pump(("two", i))
                two(s, slot)

                @pl.when(i == 0)
                def _():
                    neighbours()
        else:
            h_copy(l, y, 0).wait()
            hook(pump, "own")
            one(l, y, 0, 0)
            opening()
            neighbours()

            @pl.loop(1, RING)
            def _(i):
                turn_of(i)

                @pl.when(i == 1)
                def _():
                    up_ready()

                pump(("two", i - 1))
                two(turn(y, order(i - 1)), lax.rem(i - 1, H_SLOTS))

            hook(pump, "two3")
            two(turn(y, FAR), 0)

        for slot in BOTH:
            for i in BOTH:
                kv_out_copy(l, 0, slot, i).wait()
        sent = (out.at[y, x], out.at[y], out.at[y, x, c], out.at[y, pl.ds(0, CORES)])
        for kind, ref in enumerate(sent):
            remote(ref, ref, r.ag_send.at[kind], r.ag_recv.at[kind], partner).wait_send()
        remote(out.at[pl.ds(0, 2)], out.at[pl.ds(0, 2)], r.ag_dsend, r.ag_drecv.at[0], partner).wait_send()

    def h_copy(l, s, slot):
        return pltpu.make_async_copy(r.h_all.at[l, s], r.hb.at[slot], r.h_sem.at[slot])

    def h_tile(slot):
        return r.hb[slot].reshape(seq_len, d_model)

    def project(h, lo, n):
        w = r.wv[:, :, lo:lo + n].reshape(d_model, n)
        return jnp.dot(h, w, preferred_element_type=F32).astype(BF)

    def rope(val):
        val = val.astype(F32)
        return val * r.cos[...] + pltpu.roll(val, head_dim // 2, 1) * r.sin[...]

    n_chunk = min(256, f_loc)

    def kv_out_copy(l, s, slot, i):
        return pltpu.make_async_copy(r.qkv.at[slot, i], r.kv_out.at[l, i, s], r.kvo_sem.at[slot, i])

    def one(l, s, slot, i):
        pair = i % 2 if isinstance(i, int) else lax.rem(i, 2)

        @pl.when(i >= 2)
        def _():
            for k in BOTH:
                kv_out_copy(l, s, pair, k).wait()

        kv = jnp.zeros((seq_len, 2 * head_dim), F32)
        for zz in RINGS:
            for yy in RINGS:
                col = (zz * RING + yy) * d_row
                kv += lax.dot_general(h_cols(slot, col, d_row), r.kvb[yy, zz], (((1,), (1,)), ((), ())), preferred_element_type=F32)
        kv = kv.astype(BF)
        r.qkv[pair, 0] = rope(kv[:, :head_dim]).astype(BF)
        r.qkv[pair, 1] = kv[:, head_dim:]
        for i in BOTH:
            kv_out_copy(l, s, pair, i).start()
        q = project(h_tile(slot), 0, head_dim)
        r.stage[...] = (rope(q) * head_dim ** -0.5).astype(BF)
        for lo in range(0, f_loc, n_chunk):
            r.joined[s, :, head_dim + lo:head_dim + lo + n_chunk] = project(h_tile(slot), head_dim + lo, n_chunk)
        n_tile = seq_len // 2
        for i in BOTH:
            keys = (i + 1) * n_tile
            sc = lax.dot_general(r.stage[i * n_tile:(i + 1) * n_tile, :], r.qkv[pair, 0, :keys, :], (((1,), (1,)), ((), ())), preferred_element_type=F32)
            row_id = lax.broadcasted_iota(jnp.int32, sc.shape, 0) + i * n_tile
            col_id = lax.broadcasted_iota(jnp.int32, sc.shape, 1)
            sc = jnp.where(col_id <= row_id, sc, -1e30)
            top = jnp.max(sc, axis=-1, keepdims=True)
            ex = jnp.exp(sc - top)
            prob = (ex * (1.0 / jnp.sum(ex, axis=-1, keepdims=True))).astype(BF)
            att = jnp.dot(prob, r.qkv[pair, 1, :keys, :], preferred_element_type=F32)
            r.joined[s, i * n_tile:(i + 1) * n_tile, :head_dim] = att.astype(BF)

    def h_cols(slot, col, n):
        return r.hb[slot, :, :, :, col:col + n].reshape(seq_len, n)

    def two(s, slot):
        for lo in range(0, f_loc, n_chunk):
            up = project(h_tile(slot), head_dim + f_loc + lo, n_chunk).astype(F32)
            cols = slice(head_dim + lo, head_dim + lo + n_chunk)
            g = r.joined[s, :, cols].astype(F32)
            r.joined[s, :, cols] = (g * jax.nn.sigmoid(g) * up).astype(BF)

    def out_scatter(l, pump):
        def peer(q, first, second):
            dy = first * (1 - q) + second * q
            dx = first * q + second * (1 - q)
            return (z, turn(y, dy), turn(x, dx), c)

        def die_copy(ch, q, s):
            return remote(r.away.at[q], r.die_in.at[ch, q, s], r.dsend.at[q], r.drecv.at[ch, q, s], partner)

        def first_copy(ch, q, d):
            return remote(r.acc.at[ch, q, 0, pl.ds(CORES * d, CORES)], r.in1.at[ch, q, d], r.rs_send.at[0], r.recv1.at[ch, q, d],
                          peer(q, SIGN[d], 0))

        def second_copy(ch, q, d, h):
            js = pl.ds(CORES * h, CORES)
            return remote(r.acc.at[ch, q, 1 + d, js], r.in2.at[ch, q, d, js], r.rs_send.at[1], r.recv2.at[ch, q],
                          peer(q, SIGN[d], 0))

        def half_rows(d):
            return pl.ds(d * (rows // 2), rows // 2)

        def third_copy(ch, q, d):
            return remote(r.acc.at[ch, q, LAST, 0, half_rows(d)], r.in3.at[ch, q, d], r.rs_send.at[2], r.recv3.at[ch, q, d],
                          peer(q, 0, SIGN[d]))

        def fourth_copy(ch, q, d):
            return remote(r.acc.at[ch, q, LAST, 1 + d], r.in4.at[ch, q, d], r.rs_send.at[LAST], r.recv4.at[ch, q],
                          peer(q, 0, SIGN[d]))

        n_blk = r.wov.shape[3]

        def plane_of(ch, q):
            if l:
                return turn(z, q if ch else 2 + q)
            return turn(z, LAST - q if ch else q)

        def slot_off(s):
            return lax.rem(2 + 3 * s + 3 * (s // 2) + 2 * (s // 3), RING)

        def tile(ch, q, s):
            off = slot_off(s)
            for cc in BOTH:
                for j in RINGS:
                    oy = off * (1 - q) + SLOT_OFF[j] * q
                    ox = SLOT_OFF[j] * (1 - q) + off * q
                    core = c if cc else 1 - c
                    at = pl.multiple_of((turn(x, ox) * CORES + core) * rows, rows)
                    r.lhs[pl.ds((cc * RING + j) * rows, rows), :] = r.joined[turn(y, oy), pl.ds(at, rows), :]
            left = r.lhs[...]
            zz = plane_of(ch, q)
            for n in RINGS:
                res = jnp.dot(left, r.wov[zz, n], preferred_element_type=F32).astype(BF)
                res = res.reshape(CORES, RING, rows, n_blk)
                r.away[q, :, :, n * n_blk:(n + 1) * n_blk] = res[0]
                r.acc[ch, q, s, :, :, n * n_blk:(n + 1) * n_blk] = res[1]

        def pair_sum(ch, q, s):
            die_copy(ch, q, s).wait_recv()

            @pl.loop(0, RING)
            def _(j):
                r.acc[ch, q, s, j] = r.acc[ch, q, s, j] + r.die_in[ch, q, s, j]

        def stage_a(ch):
            @pl.loop(0, CORES * RING)
            def _(t):
                s = t // CORES
                q = lax.rem(t, CORES)

                @pl.when(s >= 1)
                def _():
                    die_copy(ch, q, s - 1).wait_send()

                if ch:
                    @pl.when(s == 0)
                    def _():
                        die_copy(ch - 1, q, LAST).wait_send()

                tile(ch, q, s)
                die_copy(ch, q, s).start()

                @pl.when(s >= 1)
                def _():
                    pair_sum(ch, q, s - 1)

                @pl.when(s == 1)
                def _():
                    for d in BOTH:
                        first_copy(ch, q, d).start()

                for d in BOTH:
                    @pl.when(s == 2 + d)
                    def _(d=d):
                        second_copy(ch, q, d, 1 - d).start()

                for n in RINGS:
                    name = f"a{ch}s{n}"
                    if pump(name, False):
                        @pl.when(t == CORES * n + 1)
                        def _(name=name):
                            hook(pump, name)

        def stage_b(ch):
            for q in BOTH:
                pair_sum(ch, q, LAST)
            for q in BOTH:
                for d in BOTH:
                    first_copy(ch, q, d).wait_recv()
                    for j in BOTH:
                        at = CORES * d + j
                        r.acc[ch, q, 1 + d, at] = r.acc[ch, q, 1 + d, at] + r.in1[ch, q, d, j]
                    second_copy(ch, q, d, d).start()

        def total(ch, q, j):
            val = r.acc[ch, q, LAST, j].astype(F32)
            for d in BOTH:
                val += r.in2[ch, q, d, j].astype(F32)
            r.acc[ch, q, LAST, j] = val.astype(BF)

        def stage_c(ch):
            for q in BOTH:
                ref = r.in2.at[ch, q]
                remote(ref, ref, r.rs_send.at[1], r.recv2.at[ch, q], here).wait_recv()
                total(ch, q, 0)
                for d in BOTH:
                    third_copy(ch, q, d).start()
                for j in RINGS[1:]:
                    total(ch, q, j)

        def stage_d(ch):
            for q in BOTH:
                for d in BOTH:
                    third_copy(ch, q, d).wait_recv()
                    rws = half_rows(d)
                    r.acc[ch, q, LAST, 1 + d, rws] = r.acc[ch, q, LAST, 1 + d, rws] + r.in3[ch, q, d]
                    fourth_copy(ch, q, d).start()

        def stage_e(ch):
            for q in BOTH:
                ref = r.in4.at[ch, q]
                remote(ref, ref, r.rs_send.at[LAST], r.recv4.at[ch, q], here).wait_recv()
                cols = pl.ds(pl.multiple_of(plane_of(ch, q) * width, width), width)
                upd = r.acc[ch, q, LAST, LAST].astype(F32)
                for d in BOTH:
                    upd += r.in4[ch, q, d].astype(F32)
                upd = upd.astype(BF)
                r.hid[:, cols] = (r.hid[:, cols].astype(F32) + upd.astype(F32)).astype(BF)

        stages = {"a": stage_a, "b": stage_b, "c": stage_c, "d": stage_d, "e": stage_e, "f": leave_a, "g": leave_b, "h": leave_c}
        for step in LAST_ORDER if l else FIRST_ORDER:
            with jax.named_scope(step):
                stages[step[0]](int(step[1]))
            hook(pump, step)
        for q in BOTH:
            die_copy(1, q, LAST).wait_send()
        for n, ref in enumerate((r.in1, r.in2, r.in3, r.in4)):
            remote(ref, ref, r.rs_send.at[n], r.drecv.at[0, 0, 0], here).wait_send()

    def near(fn, t):
        for j in (LAST, 1):
            fn(t, j)

    def far(fn, t):
        fn(t, 2)

    def z_all(t):
        near(z_direct, t)
        far(z_direct, t)

    def peers_of(fn, op="start"):
        for k in range(len(OTHERS)):
            getattr(fn(k), op)()

    def start(pump):
        peers_of(gain_z)
        kv_z()
        peers_of(x_z)
        x_own().start()
        pump("s0")
        with jax.named_scope("gain_a"):
            peers_of(gain_z, "wait_recv")
            peers_of(gain_y)
            kv_y1()
        pump("s1")
        with jax.named_scope("gain_b"):
            peers_of(gain_y, "wait_recv")
            peers_of(gain_x)
            gain_die(x, LAST).start()
        pump("s2")
        with jax.named_scope("x_z"):
            three_planes().wait_recv()
            x_own().wait()
        for oy in RINGS:
            for ox in RINGS:
                if oy or ox:
                    x_plane(oy, ox).start()
        r.xp[c, y, x] = r.xz[:, y, :, pos(x)]
        pump("s3")
        with jax.named_scope("kv_b"):
            kv_y2()
        with jax.named_scope("gain_c"):
            for k, o in enumerate(OTHERS):
                gain_x(k).wait_recv()
                gain_die(turn(x, -o), k).start()
        pump("s4")
        for oy in (OWN, BEFORE, AFTER, FAR):
            with jax.named_scope(f"row_{oy}"):
                x_row(oy)
            pump(f"r{oy}")
        pump("s5")
        kv_y3()
        pump("s6")
        with jax.named_scope("gain_sum"):
            for k in RINGS:
                gain_die(x, k).wait_recv()
            gain_sum()
            for fill in fills[1:]:
                fill.wait()
        with jax.named_scope("turn"):
            x_turn()
        pump("s7")

    def when(i, n, *fns):
        @pl.when(i == n)
        def _():
            for fn in fns:
                fn()

    def plan(steps):
        def pump(step, run=True):
            if not isinstance(step, str):
                for n in RINGS:
                    if (step[0], n) in steps:
                        when(step[1], n, lambda n=n: run_steps(steps[step[0], n]))
                return True
            found = steps.get(step, ())
            if run:
                run_steps(found)
            return found
        return pump

    def run_steps(steps):
        for fn, *args in steps:
            with jax.named_scope(f"{fn.__name__}_{args[-1] if args else 0}"):
                fn(*args)

    first_entry = plan({
        "s0": [(z_own, UP0)],
        "s1": [(y_send, QG0)],
        "s3": [(z_own, QG0)],
        "r0": [(y_relay, QG0), (z_forward, UP0, OWN), (z_direct, QG0, AFTER), (z_forward, QG0, OWN), (z_direct, QG0, BEFORE)],
        "s6": [(kv_x1, 0)],
    })
    first_front = plan({
        "begin": [(kv_x2, 0), (y_send, UP0), (z_forward, QG0, AFTER), (z_direct, QG0, FAR)],
        "k0": [(y_relay, UP0), (kv_x3, 0), (z_forward, QG0, BEFORE), (z_forward, QG0, FAR), (z_direct, UP0, AFTER), (z_direct, UP0, BEFORE)],
        "first_on": [(y_send, WO0)],
        "ready": [(load_near, QG0), (load_far, QG0), (kv_load, 0), (loaded, QG0), (kv_loaded,)],
        "k1": [(z_direct, UP0, FAR), (z_forward, UP0, AFTER)],
        "k2": [
            (z_forward, UP0, BEFORE), (y_relay, WO0), (z_forward, UP0, FAR), (y_send, QG1), (z_own, WO0), (z_direct, WO0, BEFORE),
            (kv_x1, 1),
        ],
        ("seq", 1): [(y_send, WO1), (z_direct, WO0, AFTER), (x_sent,)],
        "up": [(y_send, UP1), (z_direct, WO0, FAR), (load_near, UP0), (load_far, UP0)],
        ("two", 0): [(y_relay, QG1), (z_forward, WO0, OWN)],
        ("seq", 2): [(kv_x2, 1)],
        ("two", 1): [(kv_x3, 1), (z_direct, QG1, AFTER), (z_forward, WO0, BEFORE)],
        ("seq", 3): [(y_relay, WO1), (z_forward, WO0, AFTER)],
        ("two", 2): [(z_forward, WO0, FAR), (z_own, QG1), (y_relay, UP1)],
        "near": [(load_near, WO0)],
    })
    first_scatter = plan({
        "a0s0": [(z_forward, QG1, AFTER)],
        "a0s2": [(z_direct, QG1, BEFORE)],
        "b0": [(load_far, WO0), (far_loaded, WO0)],
        "a1s0": [(z_direct, QG1, FAR)],
        "a1s1": [(z_forward, QG1, OWN)],
        "a1": [(z_direct, UP1, FAR)],
        "b1": [(z_direct, UP1, BEFORE)],
        "c1": [(z_forward, QG1, FAR), (z_direct, UP1, AFTER), (z_own, UP1), (z_forward, QG1, BEFORE)],
        "e0": [(z_forward, UP1, FAR)],
    })
    second_front = plan({
        "begin": [(z_forward, UP1, BEFORE), (kv_load, 1)],
        "first": [(z_forward, UP1, AFTER)],
        "k0": [(z_forward, UP1, OWN), (z_direct, WO1, FAR)],
        "ready": [(load_near, QG1), (load_far, QG1), (loaded, QG1), (kv_loaded,)],
        ("seq", 0): [(z_own, WO1)],
        "k1": [(z_direct, WO1, BEFORE)],
        "up": [(load_near, UP1), (load_far, UP1)],
        "k2": [(z_direct, WO1, AFTER)],
        ("seq", 1): [(z_forward, WO1, FAR)],
        ("two", 1): [(z_forward, WO1, OWN)],
        ("two", 2): [(z_forward, WO1, BEFORE), (z_forward, WO1, AFTER)],
        "near": [(load_near, WO1), (load_far, WO1)],
    })
    second_scatter = plan({
    })

    with jax.named_scope("start"):
        start(first_entry)
    with jax.named_scope("front_0"):
        gather_norm(0, rows // RING, first_front)
    with jax.named_scope("near_0"):
        kv_share(0)
        first_front("near")
        near_loaded(WO0)
    with jax.named_scope("scatter_0"):
        out_scatter(0, first_scatter)
    with jax.named_scope("front_1"):
        gather_norm(1, rows // 2, second_front)
    with jax.named_scope("near_1"):
        kv_share(1)
        second_front("near")
        loaded(WO1)
    with jax.named_scope("scatter_1"):
        out_scatter(1, second_scatter)
    with jax.named_scope("drain"):
        left()
        for t in range(WO1 + 1):
            drain(t)
        for l in range(n_layers):
            kv_shared(l)
            kv_sent(l)


def run_model(xt, gain, wkv_t, w_in, w_out, cos_full, sin_full):
    batch, d_local, seq_len = xt.shape
    n_layers, d_row, e_block = w_in.shape
    r_block, d_col = w_out.shape[1:]
    head_dim = cos_full.shape[1]
    d_model = d_row * RING * RING
    seqs = batch // RING
    rows = seqs * seq_len // (RING * RING * CORES)
    e_loc, r_loc = e_block // RING, r_block // RING
    kc = wkv_t.shape[1]
    width = d_model // RING
    n_t = 3 * n_layers
    n_o = len(OTHERS)

    def dma(*shape):
        return pltpu.SemaphoreType.DMA(shape)

    def vm(*shape):
        return pltpu.VMEM(shape, BF)

    def out(*shape):
        return jax.ShapeDtypeStruct(shape, BF)

    any_spec = pl.BlockSpec(memory_space=pl.ANY)
    out_shape = [
        out(batch, d_local, seq_len),
        out(n_layers, 2, seqs, seq_len, head_dim),
        out(n_layers, RING, RING, CORES, rows, d_model),
        out(n_layers, RING, RING * d_row, e_loc),
        out(n_layers, RING, RING, r_loc, d_col),
        out(RING, CORES, n_layers, RING, RING, kc, d_row),
        out(n_layers, RING, 2, seqs, CORES * (seq_len // (CORES * RING * RING * RING)), head_dim),
        out(n_layers, 2, d_row // 2, e_loc),
        out(n_layers, 2, r_loc // 2, d_col),
    ]
    pair = (2, 2, 2)
    scratch = [
        pltpu.VMEM(cos_full.shape, F32), pltpu.VMEM(cos_full.shape, F32), vm(n_layers, d_local),
        vm(rows, d_model), vm(rows, d_model), pltpu.VMEM((n_layers, d_model), F32),
        vm(RING, CORES, RING, RING, G_ROWS, d_row),
        vm(RING, seqs, d_local, seq_len),
        vm(CORES, RING, RING, RING, d_local, CORES * rows),
        vm(RING, RING * d_row, e_loc), vm(RING, RING, 2 * head_dim, d_row), vm(RING, RING, r_loc, d_col),
        vm(H_SLOTS, RING, CORES, rows, d_model), vm(RING, seq_len, r_loc), vm(2, 2, seq_len, head_dim), vm(seq_len, head_dim),
        vm(CORES * RING * rows, r_loc), vm(2, RING, rows, width), vm(2, 2, RING, RING, rows, width), vm(2, 2, RING, RING, rows, width),
        vm(*pair, 2, rows, width), vm(*pair, RING, rows, width), vm(*pair, rows // 2, width), vm(*pair, rows, width),
        pltpu.SemaphoreType.DMA, pltpu.SemaphoreType.DMA, dma(RING), dma(RING), pltpu.SemaphoreType.DMA, pltpu.SemaphoreType.DMA,
        pltpu.SemaphoreType.DMA,
        dma(3 * n_o), dma(3 * n_o), dma(RING), dma(RING),
        dma(RING), dma(RING), dma(2, RING), dma(2, RING), dma(RING), dma(RING), pltpu.SemaphoreType.DMA,
        dma(RING), dma(40), pltpu.SemaphoreType.DMA, dma(RING), pltpu.SemaphoreType.DMA, dma(H_SLOTS), dma(2, 2), dma(3), dma(3),
        dma(n_t, RING), dma(n_t, 2), dma(3, RING, 2), dma(3), dma(n_t),
        dma(n_o), dma(n_o), pltpu.SemaphoreType.DMA, dma(n_o), dma(n_layers), dma(n_layers, n_o), dma(n_layers), dma(n_layers), dma(2),
        dma(2), dma(2, 2, RING), dma(RING), dma(*pair), dma(2, 2), dma(*pair), dma(2, 2),
        dma(3), dma(n_layers, n_o), dma(n_layers, n_o), dma(n_layers),
    ]
    res = pl.pallas_call(
        model_kernel,
        out_shape=out_shape,
        in_specs=[any_spec] * 7,
        out_specs=[any_spec] * len(out_shape),
        scratch_shapes=scratch,
        compiler_params=pltpu.CompilerParams(collective_id=0, has_side_effects=True, vmem_limit_bytes=VMEM_LIMIT),
        name="two_layers",
    )(xt, gain, wkv_t, w_in, w_out, cos_full, sin_full)
    return res[0], res[6]


def solution(mesh):
    row_size = mesh.shape["row"]
    n_col = mesh.shape["col"]
    n_z = row_size // RING
    n_y = RING
    n_x = n_col // CORES
    n_tp = n_y * n_col
    n_dev = row_size * n_col
    mesh4 = Mesh(mesh.devices.reshape(n_z, n_y, n_x, CORES), ("z", "y", "x", "core"))
    every = ("z", "y", "x", "core")
    col = ("x", "core")
    act_spec = P(NIL, NIL, every)
    w_spec = P(NIL, ("z", "y"), col)

    def device_fn(x_loc, gain_loc, w_in_loc, w_kv_loc, w_out_loc):
        n_layers = w_in_loc.shape[0]
        n_batch, seq_len, d_local = x_loc.shape
        head_dim = w_kv_loc.shape[2] * n_col // 2
        batch_loc = n_batch // n_z
        seq_local = seq_len // n_dev
        steps = np.arange(head_dim // 2, dtype=np.float32)
        inv_freq = (1.0 / 10000.0 ** (steps * 2 / head_dim)).astype(np.float32)
        angles = np.arange(seq_len, dtype=np.float32)[:, NIL] * inv_freq[NIL, :]
        cos_tab, sin_tab = np.cos(angles), np.sin(angles)
        cos_full = jnp.asarray(np.concatenate([cos_tab, cos_tab], axis=1))
        sin_full = jnp.asarray(np.concatenate([-sin_tab, sin_tab], axis=1))
        y_loc, kv = run_model(x_loc.transpose(0, 2, 1), gain_loc, w_kv_loc.transpose(0, 2, 1), w_in_loc, w_out_loc, cos_full, sin_full)
        y_loc = y_loc.transpose(0, 2, 1)
        kv = kv.reshape(n_layers, n_z, 2, batch_loc, CORES, seq_local, head_dim)
        kv = lax.dynamic_index_in_dim(kv, lax.axis_index("core"), axis=4, keepdims=False)
        kv = kv.transpose(0, 2, 1, 3, 4, 5).reshape(n_layers, 2, n_batch, seq_local, head_dim)
        return y_loc, kv

    return jax.shard_map(device_fn, mesh=mesh4, in_specs=(act_spec, P(NIL, every), w_spec, w_spec, P(NIL, col, ("z", "y"))), out_specs=(act_spec, P(NIL, NIL, NIL, every, NIL)), check_vma=False)
```

```python
import typing

import jax
import jax.numpy as jnp
import numpy as np
from jax import lax
from jax.experimental import pallas as pl
from jax.experimental.pallas import tpu as pltpu
from jax.sharding import Mesh
from jax.sharding import PartitionSpec as P

LN_EPS = 1e-6
RING = 4
CORES = 2
VMEM_LIMIT = 67_000_000
BF = jnp.bfloat16
F32 = jnp.float32
SLOT_OFF = (2, 1, 3, 0)
SIGN = (1, -1)
NIL = None
BOTH = range(CORES)
RINGS = range(RING)
OTHERS = (1, 3, 2)
LAST = RING - 1
G_ROWS = 8
H_SLOTS = 3
QG0, UP0, WO0, QG1, UP1, WO1 = range(6)
OWN, AFTER, FAR, BEFORE = RINGS
FIRST_ORDER = ("a0", "b0", "a1", "b1", "c0", "c1", "d0", "d1", "e0", "e1")
LAST_ORDER = FIRST_ORDER[:-1] + ("f1", "e1", "g1", "f0", "g0", "h1", "h0")
KINDS = ("first", "second", "first_on", "second_on")


class Refs(typing.NamedTuple):
    xt: typing.Any
    gain_in: typing.Any
    wkv: typing.Any
    w_in: typing.Any
    w_out: typing.Any
    cos_in: typing.Any
    sin_in: typing.Any
    y_out: typing.Any
    kv_out: typing.Any
    h_all: typing.Any
    wi: typing.Any
    wo: typing.Any
    kvh: typing.Any
    kvx: typing.Any
    rwi: typing.Any
    rwo: typing.Any
    cos: typing.Any
    sin: typing.Any
    gain_own: typing.Any
    h_ref: typing.Any
    hid: typing.Any
    gain: typing.Any
    gbuf: typing.Any
    xz: typing.Any
    xp: typing.Any
    wv: typing.Any
    kvb: typing.Any
    wov: typing.Any
    hb: typing.Any
    joined: typing.Any
    qkv: typing.Any
    stage: typing.Any
    lhs: typing.Any
    away: typing.Any
    acc: typing.Any
    die_in: typing.Any
    in1: typing.Any
    in2: typing.Any
    in3: typing.Any
    in4: typing.Any
    xz_send: typing.Any
    xz_recv: typing.Any
    xp_send: typing.Any
    xp_recv: typing.Any
    xd_send: typing.Any
    xd_recv: typing.Any
    x_loc: typing.Any
    g_send: typing.Any
    g_recv: typing.Any
    gd_send: typing.Any
    gd_recv: typing.Any
    yd_send: typing.Any
    yd_recv: typing.Any
    yp_send: typing.Any
    yp_recv: typing.Any
    yz_send: typing.Any
    yz_recv: typing.Any
    y_loc: typing.Any
    ag_send: typing.Any
    ag_recv: typing.Any
    ag_dsend: typing.Any
    ag_drecv: typing.Any
    ag_loc: typing.Any
    h_sem: typing.Any
    kvo_sem: typing.Any
    w_load: typing.Any
    far_load: typing.Any
    y_recv: typing.Any
    ry_recv: typing.Any
    zb_recv: typing.Any
    zc_recv: typing.Any
    w_send: typing.Any
    kz_send: typing.Any
    kz_recv: typing.Any
    ky_send: typing.Any
    ky_recv: typing.Any
    kx_send: typing.Any
    kx_recv: typing.Any
    kd_send: typing.Any
    kd_recv: typing.Any
    k_loc: typing.Any
    dsend: typing.Any
    drecv: typing.Any
    rs_send: typing.Any
    recv1: typing.Any
    recv2: typing.Any
    recv3: typing.Any
    recv4: typing.Any
    small: typing.Any
    kvx_send: typing.Any
    kvx_recv: typing.Any
    kvx_loc: typing.Any


def model_kernel(*refs):
    r = Refs(*refs)
    z, y, x, c = (lax.axis_index(a) for a in ("z", "y", "x", "core"))
    n_layers = r.wkv.shape[0]
    rows, d_model = r.hid.shape
    batch, d_local = r.xt.shape[:2]
    seqs = batch // RING
    seq_len, head_dim = r.cos.shape
    d_row = r.w_in.shape[1]
    e_loc = r.wi.shape[3]
    depth = r.wo.shape[3]
    f_loc = depth - head_dim
    quarter = rows // 4
    width = d_model // RING
    q_block = head_dim * RING
    f_block = f_loc * RING

    turned = {id(v): [lax.rem(v + o, RING) for o in RINGS] for v in (z, y, x)}

    def turn(base, off):
        if isinstance(off, int):
            return turned[id(base)][off % RING]
        return lax.rem(base + off + RING, RING)

    def remote(src, dst, ssem, rsem, dev):
        return pltpu.make_async_remote_copy(
            src_ref=src, dst_ref=dst, send_sem=ssem, recv_sem=rsem, device_id=dev, device_id_type=pl.DeviceIdType.MESH)

    partner = (z, y, x, 1 - c)

    peers = [(turn(z, o), y, x, c) for o in OTHERS]
    peers += [(z, turn(y, oy), turn(x, ox), c) for oy in RINGS for ox in RINGS if oy or ox]
    peers.append(partner)
    here = (z, y, x, c)
    gate_sem = pltpu.get_barrier_semaphore()
    for dev in peers:
        pl.semaphore_signal(gate_sem, inc=1, device_id=dev, device_id_type=pl.DeviceIdType.MESH)
    fills = [pltpu.make_async_copy(src, dst, r.small.at[n]) for n, (src, dst) in enumerate(
        ((r.gain_in, r.gain_own), (r.cos_in, r.cos), (r.sin_in, r.sin)))]
    for fill in fills:
        fill.start()
    fills[0].wait()

    src_id = lax.broadcasted_iota(jnp.int32, (d_local, d_row), 0) + (x * CORES + c) * d_local
    dst_id = lax.broadcasted_iota(jnp.int32, (d_local, d_row), 1)
    spread = jnp.where(src_id == dst_id, 1.0, 0.0).astype(BF)
    r.gbuf[x, c, y, z] = jnp.zeros((G_ROWS, d_row), BF)
    r.gbuf[x, c, y, z, :n_layers] = jnp.dot(r.gain_own[...], spread, preferred_element_type=F32).astype(BF)
    pl.semaphore_wait(gate_sem, len(peers))

    def hook(pump, i):
        with jax.named_scope(f"hook_{i}"):
            pump(i)

    def w_cols(kind):
        return pl.ds(0, head_dim + f_loc) if kind == 0 else pl.ds(head_dim + f_loc, f_loc)

    def piece(t, zz, yy):
        l, kind = t // 3, t % 3
        if kind == 2:
            return r.wo.at[l, zz, yy]
        return r.wi.at[l, zz, pl.ds(pl.multiple_of(yy * d_row, d_row), d_row), w_cols(kind)]

    def piece_half(t, zz, yy, h):
        l, kind = t // 3, t % 3
        if kind == 2:
            return r.wo.at[l, zz, yy, pl.ds(h * (depth // 2), depth // 2)]
        return r.wi.at[l, zz, pl.ds(pl.multiple_of(yy * d_row + h * (d_row // 2), d_row // 2), d_row // 2), w_cols(kind)]

    def own_parts(t, owner, zz, yy):
        l, kind = t // 3, t % 3
        hq = pl.ds(pl.multiple_of(owner * head_dim, head_dim), head_dim)
        if kind == 2:
            return [
                (r.w_out.at[l, hq], r.wo.at[l, zz, yy, pl.ds(0, head_dim)]),
                (r.w_out.at[l, pl.ds(pl.multiple_of(q_block + owner * f_loc, head_dim), f_loc)], r.wo.at[l, zz, yy, pl.ds(head_dim, f_loc)]),
            ]
        rws = pl.ds(pl.multiple_of(yy * d_row, d_row), d_row)
        if kind == 0:
            return [
                (r.w_in.at[l, :, hq], r.wi.at[l, zz, rws, pl.ds(0, head_dim)]),
                (r.w_in.at[l, :, pl.ds(pl.multiple_of(q_block + owner * f_loc, head_dim), f_loc)], r.wi.at[l, zz, rws, pl.ds(head_dim, f_loc)]),
            ]
        return [(r.w_in.at[l, :, pl.ds(pl.multiple_of(q_block + f_block + owner * f_loc, head_dim), f_loc)],
                 r.wi.at[l, zz, rws, pl.ds(head_dim + f_loc, f_loc)])]

    def relay_ref(t, d):
        l, kind = t // 3, t % 3
        return r.rwo.at[l, d] if kind == 2 else r.rwi.at[l, d, :, w_cols(kind)]

    def far_parts(t, d):
        l, kind = t // 3, t % 3
        owner = turn(y, 2)
        hq = pl.ds(pl.multiple_of(owner * head_dim, head_dim), head_dim)
        if kind == 2:
            n = depth // 2
            base = q_block + owner * f_loc
            if d:
                return [(r.w_out.at[l, pl.ds(pl.multiple_of(base + n - head_dim, G_ROWS), n)], r.rwo.at[l, d])]
            return [
                (r.w_out.at[l, hq], r.rwo.at[l, d, pl.ds(0, head_dim)]),
                (r.w_out.at[l, pl.ds(pl.multiple_of(base, head_dim), n - head_dim)], r.rwo.at[l, d, pl.ds(head_dim, n - head_dim)]),
            ]
        rws = pl.ds(d * (d_row // 2), d_row // 2)
        if kind == 0:
            return [
                (r.w_in.at[l, rws, hq], r.rwi.at[l, d, :, pl.ds(0, head_dim)]),
                (r.w_in.at[l, rws, pl.ds(pl.multiple_of(q_block + owner * f_loc, head_dim), f_loc)], r.rwi.at[l, d, :, pl.ds(head_dim, f_loc)]),
            ]
        return [(r.w_in.at[l, rws, pl.ds(pl.multiple_of(q_block + f_block + owner * f_loc, head_dim), f_loc)], relay_ref(t, d))]

    def y_send(t):
        for d in BOTH:
            owner = turn(y, SIGN[d])
            dev = (z, owner, x, c)
            for src, dst in far_parts(t, d):
                remote(src, dst, r.w_send.at[t], r.ry_recv.at[t, d], dev).start()
            for src, dst in own_parts(t, owner, z, y):
                remote(src, dst, r.w_send.at[t], r.y_recv.at[t, -SIGN[d] % RING], dev).start()

    def y_relay(t):
        for d in BOTH:
            ref = relay_ref(t, d)
            remote(ref, ref, r.w_send.at[t], r.ry_recv.at[t, d], here).wait_recv()
            dst = piece_half(t, z, turn(y, -SIGN[d]), d)
            remote(ref, dst, r.w_send.at[t], r.y_recv.at[t, 2], (z, turn(y, SIGN[d]), x, c)).start()

    def z_own(t):
        for d in BOTH:
            for src, dst in own_parts(t, y, z, y):
                remote(src, dst, r.w_send.at[t], r.zb_recv.at[t % 3, 0, d], (turn(z, SIGN[d]), y, x, c)).start()

    def z_direct(t, j):
        yy = turn(y, j)
        ref = piece(t, z, yy)
        remote(ref, ref, r.w_send.at[t], r.y_recv.at[t, j], here).wait_recv()
        for d in BOTH:
            remote(ref, ref, r.w_send.at[t], r.zb_recv.at[t % 3, j, d], (turn(z, SIGN[d]), y, x, c)).start()

    def z_forward(t, j):
        yy = turn(y, j)
        for d in BOTH:
            zz = turn(z, -SIGN[d])
            ref = piece(t, zz, yy)
            remote(ref, ref, r.w_send.at[t], r.zb_recv.at[t % 3, j, d], here).wait_recv()
            part = piece_half(t, zz, yy, d)
            remote(part, part, r.w_send.at[t], r.zc_recv.at[t % 3], (turn(z, SIGN[d]), y, x, c)).start()

    def place(t, zz):
        l, kind = t // 3, t % 3
        if kind == 2:
            return r.wo.at[l, zz], r.wov.at[zz]
        return r.wi.at[l, zz, :, w_cols(kind)], r.wv.at[zz, :, w_cols(kind)]

    def load_near(t):
        kind = t % 3
        for d in BOTH:
            src, dst = place(t, turn(z, SIGN[d]))
            pltpu.make_async_copy(src, dst, r.w_load.at[kind]).start()
        for j in OTHERS:
            yy = turn(y, j)
            dst = r.wov.at[z, yy] if kind == 2 else r.wv.at[z, pl.ds(pl.multiple_of(yy * d_row, d_row), d_row), w_cols(kind)]
            pltpu.make_async_copy(piece(t, z, yy), dst, r.w_load.at[kind]).start()
        for src, dst in own_parts(t, y, z, y):
            pltpu.make_async_copy(src, own_place(t, dst, src), r.w_load.at[kind]).start()

    def load_far(t):
        src, dst = place(t, turn(z, 2))
        remote(src, src, r.w_send.at[t], r.zc_recv.at[t % 3], here).wait_recv()
        pltpu.make_async_copy(src, dst, r.far_load.at[t % 3]).start()

    def own_place(t, dst, src):
        kind = t % 3
        if kind == 2:
            n = src.shape[0]
            return r.wov.at[z, y, pl.ds(0 if n == head_dim and f_loc != head_dim else head_dim, n)]
        n = src.shape[1]
        rws = pl.ds(pl.multiple_of(y * d_row, d_row), d_row)
        if kind == 0:
            return r.wv.at[z, rws, pl.ds(0 if n == head_dim and f_loc != head_dim else head_dim, n)]
        return r.wv.at[z, rws, pl.ds(head_dim + f_loc, f_loc)]

    def near_loaded(t):
        kind = t % 3
        dst = r.wov.at[pl.ds(0, LAST)] if kind == 2 else r.wv.at[pl.ds(0, LAST), :, w_cols(kind)]
        pltpu.make_async_copy(dst, dst, r.w_load.at[kind]).wait()

    def far_loaded(t):
        kind = t % 3
        dst = r.wov.at[0] if kind == 2 else r.wv.at[0, :, w_cols(kind)]
        pltpu.make_async_copy(dst, dst, r.far_load.at[kind]).wait()

    def loaded(t):
        near_loaded(t)
        far_loaded(t)

    def drain(t):
        l, kind = t // 3, t % 3
        ref = r.wo.at[l] if kind == 2 else r.wi.at[l, :, :, w_cols(kind)]
        remote(ref, ref, r.w_send.at[t], r.y_recv.at[t, 0], here).wait_send()

    def kv_z_copy(k):
        return remote(r.wkv, r.kvh.at[x, c, :, y, z], r.kz_send.at[k], r.kz_recv.at[k], (turn(z, OTHERS[k]), y, x, c))

    def kv_own():
        return pltpu.make_async_copy(r.wkv, r.kvh.at[x, c, :, y, z], r.k_loc.at[0])

    def kv_z():
        for k in range(len(OTHERS)):
            kv_z_copy(k).start()
        kv_own().start()

    def kv_y_copy(ref, k, d):
        return remote(ref, ref, r.ky_send, r.ky_recv.at[k], (z, turn(y, SIGN[d]), x, c))

    def kv_y1():
        kv_own().wait()
        for k in range(len(OTHERS)):
            kv_z_copy(k).wait()
        for d in BOTH:
            kv_y_copy(r.kvh.at[x, c, :, y], d, d).start()

    def kv_y2():
        for d in BOTH:
            yy = turn(y, -SIGN[d])
            kv_y_copy(r.kvh.at[x, c, :, yy], d, d).wait_recv()
            kv_y_copy(r.kvh.at[x, c, :, yy, pl.ds(2 * d, 2)], 2, d).start()

    def kv_y3():
        kv_y_copy(r.kvh.at[x, c, :, turn(y, 2)], 2, 0).wait_recv()
        kv_y_copy(r.kvh.at[x, c, :, pl.ds(0, LAST)], 0, 0).wait_send()

    def kv_x_copy(l, ref, k, d):
        return remote(ref, ref, r.kx_send.at[l], r.kx_recv.at[l, k], (z, y, turn(x, SIGN[d]), c))

    def kv_die(l, ref):
        return remote(ref, ref, r.kd_send.at[l], r.kd_recv.at[l], partner)

    def kv_x1(l):
        ref = r.kvh.at[x, c, l]
        for d in BOTH:
            kv_x_copy(l, ref, d, d).start()
        kv_die(l, ref).start()

    def kv_x2(l):
        for d in BOTH:
            xx = turn(x, -SIGN[d])
            ref = r.kvh.at[xx, c, l]
            kv_x_copy(l, ref, d, d).wait_recv()
            kv_x_copy(l, r.kvh.at[xx, c, l, pl.ds(2 * d, 2)], 2, d).start()
            kv_die(l, ref).start()

    def kv_x3(l):
        ref = r.kvh.at[turn(x, 2), c, l]
        kv_x_copy(l, ref, 2, 0).wait_recv()
        kv_die(l, ref).start()

    def kv_load(l):
        kv_die(l, r.kvh.at[:, 1 - c, l]).wait_recv()
        kc = r.wkv.shape[1]
        for xx in RINGS:
            for cc in BOTH:
                pltpu.make_async_copy(r.kvh.at[xx, cc, l], r.kvb.at[:, :, pl.ds((xx * CORES + cc) * kc, kc)], r.k_loc.at[1]).start()

    def kv_sent(l):
        kv_x_copy(l, r.kvh.at[pl.ds(0, LAST), c, l], 0, 0).wait_send()
        kv_die(l, r.kvh.at[:, c, l]).wait_send()

    def kv_loaded():
        pltpu.make_async_copy(r.kvb, r.kvb, r.k_loc.at[1]).wait()

    def gain_move(i, src, dst, dev):
        return remote(src, dst, r.g_send.at[i], r.g_recv.at[i], dev)

    def gain_z(k):
        dev = (turn(z, OTHERS[k]), y, x, c)
        return gain_move(k, r.gbuf.at[x, c, y, z], r.gbuf.at[x, c, y, z], dev)

    def gain_y(k):
        dev = (z, turn(y, OTHERS[k]), x, c)
        return gain_move(len(OTHERS) + k, r.gbuf.at[x, c, y], r.gbuf.at[x, c, y], dev)

    def gain_x(k):
        dev = (z, y, turn(x, OTHERS[k]), c)
        return gain_move(CORES * len(OTHERS) + k, r.gbuf.at[x, c], r.gbuf.at[x, c], dev)

    def gain_die(xx, k):
        ref = r.gbuf.at[xx, c]
        return remote(ref, ref, r.gd_send.at[k], r.gd_recv.at[k], partner)

    def gain_sum():
        for zz in RINGS:
            for yy in RINGS:
                tot = jnp.zeros((n_layers, d_row), F32)
                for xx in RINGS:
                    for cc in BOTH:
                        tot += r.gbuf[xx, cc, yy, zz, :n_layers].astype(F32)
                at = (zz * RING + yy) * d_row
                r.gain[:, at:at + d_row] = tot

    tok_pair = CORES * rows

    def x_z(k):
        zz = turn(z, OTHERS[k])
        src = r.xt.at[pl.ds(zz * seqs, seqs)]
        return remote(src, r.xz.at[z], r.xz_send, r.xz_recv, (zz, y, x, c))

    def three_planes():
        ref = r.xz.at[pl.ds(0, LAST)]
        return remote(ref, ref, r.xz_send, r.xz_recv, here)

    def x_own():
        return pltpu.make_async_copy(r.xt.at[pl.ds(z * seqs, seqs)], r.xz.at[z], r.x_loc)

    def pos(xx):
        return pl.ds(pl.multiple_of(xx * tok_pair, tok_pair), tok_pair)

    def x_plane(oy, ox):
        yy, xx = turn(y, oy), turn(x, ox)
        return remote(r.xz.at[:, yy, :, pos(xx)], r.xp.at[c, y, x], r.xp_send.at[oy], r.xp_recv.at[(RING - oy) % RING], (z, yy, xx, c))

    def row_bytes(oy):
        return r.xp.at[c, 0] if oy else r.xp.at[c, 0, pl.ds(0, RING - 1)]

    def x_row(oy):
        yy = turn(y, oy)
        got = row_bytes(oy)
        remote(got, got, r.xp_send.at[oy], r.xp_recv.at[oy], partner).wait_recv()
        row = r.xp.at[c, yy]
        remote(row, row, r.xd_send, r.xd_recv, partner).start()

    def x_turn():
        got = r.xp.at[1 - c]
        remote(got, got, r.xd_send, r.xd_recv, partner).wait_recv()

        @pl.loop(0, RING)
        def _(zz):
            for yy in RINGS:
                for xh in BOTH:
                    blk = [r.xp[cc, yy, CORES * xh + xx, zz] for xx in BOTH for cc in BOTH]
                    blk = jnp.concatenate(blk, axis=0).astype(F32).T.astype(BF)
                    n = blk.shape[1]
                    at = pl.multiple_of(zz * RING * d_row + yy * d_row + xh * n, n)
                    r.hb[0, 0, :, :, pl.ds(at, n)] = blk.reshape(CORES, rows, n)
        r.hid[...] = r.hb[0, 0, c]
        remote(got, got, r.xd_send, r.xd_recv, partner).wait_send()

    def x_sent():
        three_planes().wait_send()
        for fn in (gain_z, gain_y, gain_x):
            peers_of(fn, "wait_send")
        for k in RINGS:
            gain_die(x, k).wait_send()
        for oy in RINGS:
            got = row_bytes(oy)
            remote(got, got, r.xp_send.at[oy], r.xp_recv.at[oy], partner).wait_send()

    def y_die(p):
        cols = pl.ds(pl.multiple_of(turn(z, p) * width, width), width)
        return remote(r.hid.at[:, cols], r.hb.at[0, 0, c, :, cols], r.yd_send.at[p], r.yd_recv.at[p], partner)

    def planes(h):
        return pl.ds(2 * h, 2)

    def y_plane(h, oy, ox):
        yy, xx = turn(y, oy), turn(x, ox)
        return remote(r.xp.at[c, yy, xx, planes(h)], r.xz.at[planes(h), y, :, pos(x)], r.yp_send.at[h, oy], r.yp_recv.at[h, (RING - oy) % RING],
                      (z, yy, xx, c))

    def y_z(p, oy):
        s = turn(y, oy)
        return remote(r.xz.at[p, s], r.y_out.at[z * seqs + s], r.yz_send.at[p], r.yz_recv.at[p], (turn(z, p), y, x, c))

    def y_own(oy):
        s = turn(y, oy)
        return pltpu.make_async_copy(r.xz.at[0, s], r.y_out.at[z * seqs + s], r.y_loc)

    def leave_a(h):
        for p in BOTH:
            p = 2 * h + p
            y_die(p).start()
            cols = pl.ds(pl.multiple_of(turn(z, p) * width, width), width)
            r.hb[0, 0, c, :, cols] = r.hid[:, cols]

    def leave_b(h):
        n = CORES * CORES * d_local
        for p in BOTH:
            p = 2 * h + p
            y_die(p).wait()

            @pl.loop(0, RING)
            def _(yy, p=p):
                for xh in BOTH:
                    at = pl.multiple_of(turn(z, p) * width + yy * d_row + xh * n, n)
                    blk = r.hb[0, 0, :, :, pl.ds(at, n)].reshape(tok_pair, n).astype(F32).T.astype(BF)
                    for xx in BOTH:
                        for cc in BOTH:
                            lo = (xx * CORES + cc) * d_local
                            r.xp[cc, yy, CORES * xh + xx, p] = blk[lo:lo + d_local]

        for oy in OTHERS + (0,):
            for ox in RINGS:
                if oy or ox:
                    y_plane(h, oy, ox).start()
        for p in BOTH:
            p = 2 * h + p
            r.xz[p, y, :, pos(x)] = r.xp[c, y, x, p]

    def plane_bytes(h, oy):
        return r.xp.at[c, 0, :, planes(h)] if oy else r.xp.at[c, 0, pl.ds(0, LAST), planes(h)]

    def leave_c(h):
        for oy in OTHERS + (0,):
            got = plane_bytes(h, oy)
            remote(got, got, r.yp_send.at[h, oy], r.yp_recv.at[h, oy], partner).wait_recv()
            for p in BOTH:
                p = 2 * h + p
                (y_z(p, oy) if p else y_own(oy)).start()

    def left():
        for oy in RINGS:
            for h in BOTH:
                got = plane_bytes(h, oy)
                remote(got, got, r.yp_send.at[h, oy], r.yp_recv.at[h, oy], partner).wait_send()
        for p in OTHERS:
            ref = r.xz.at[p]
            remote(ref, ref, r.yz_send.at[p], r.yz_recv.at[p], here).wait()
        pltpu.make_async_copy(r.xz.at[0], r.xz.at[0], r.y_loc).wait()

    def kv_rows(zz):
        n = CORES * seq_len // (RING * RING * RING * CORES)
        return pl.ds(pl.multiple_of(((zz * RING + y) * RING + x) * n, n), n)

    def kv_trade(l, k):
        zz = turn(z, OTHERS[k])
        return remote(r.kv_out.at[l, :, :, kv_rows(zz)], r.kvx.at[l, z], r.kvx_send.at[l, k], r.kvx_recv.at[l, k], (zz, y, x, c))

    def kv_keep(l):
        return pltpu.make_async_copy(r.kv_out.at[l, :, :, kv_rows(z)], r.kvx.at[l, z], r.kvx_loc.at[l])

    def kv_share(l):
        for k in range(len(OTHERS)):
            kv_trade(l, k).start()
        kv_keep(l).start()

    def kv_shared(l):
        for k in range(len(OTHERS)):
            kv_trade(l, k).wait()
        kv_keep(l).wait()

    def gather_norm(l, split, pump):
        hid = r.hid
        gain = r.gain[l:l + 1, :]
        for b in range(4):
            blk = hid[b * quarter:(b + 1) * quarter, :].astype(F32)
            mean = jnp.mean(blk, axis=-1, keepdims=True)
            cen = blk - mean
            var = jnp.mean(cen * cen, axis=-1, keepdims=True)
            r.h_ref[b * quarter:(b + 1) * quarter, :] = (cen * lax.rsqrt(var + LN_EPS) * gain).astype(BF)
        out = r.h_all.at[l]

        def spot(q, first, second):
            if q == 0:
                return turn(y, second), turn(x, first)
            return turn(y, first), turn(x, second)

        def span(q, part):
            lo, n = (split, rows - split) if q else (0, split)
            if part is NIL:
                return pl.ds(lo, n)
            return pl.ds(lo + part * (n // 2), n // 2)

        offs = (0, -1, 1, 2)
        plans = {}
        for q in BOTH:
            for d in BOTH:
                plans["first", q, d] = (q, 0, 0, NIL, SIGN[d], 0)
                plans["first_on", q, d] = (q, -SIGN[d], 0, d, SIGN[d], 0)
                for k in RINGS:
                    plans["second", q, k, d] = (q, offs[k], 0, NIL, 0, SIGN[d])
                    plans["second_on", q, k, d] = (q, offs[k], -SIGN[d], d, 0, SIGN[d])
        index = {key: n for n, key in enumerate(plans)}

        def link(*key, own=False):
            idx, (q, first, second, part, to_first, to_second) = index[key], plans[key]
            sy, sx = spot(q, first, second)
            ty, tx = spot(q, to_first, to_second)
            rws = span(q, part)
            dst = out.at[sy, sx, c, rws]
            return remote(r.h_ref.at[rws] if own else dst, dst, r.ag_send.at[KINDS.index(key[0])], r.ag_recv.at[idx], (z, ty, tx, c))

        def arrived(*key):
            for d in BOTH:
                link(*key, d).wait_recv()

        def die(q, first, second, own=False):
            sy, sx = spot(q, first, second)
            rws = span(q, NIL)
            dst = out.at[sy, sx, c, rws]
            off = (first if q else second) % RING
            remote(r.h_ref.at[rws] if own else dst, dst, r.ag_dsend, r.ag_drecv.at[off], partner).start()

        def take(k, q):
            for d in BOTH:
                link("second", q, k, d).wait_recv()
                die(q, offs[k], -SIGN[d])

        def pass_on(k, q):
            for d in BOTH:
                link("second_on", q, k, d).start()

        def second_step(k):
            take(k, 1)
            pass_on(k, 1)
            take(k, 0)

        def far_first(q):
            for e in BOTH:
                link("second", q, LAST, e).start()

        def last_step(q, k):
            arrived("second_on", q, k)
            die(q, offs[k], 2)

        def tail_a():
            second_step(2)
            far_first(1)
            for k in RINGS[:-1]:
                pass_on(k, 0)
            hook(pump, "k2")
            take(LAST, 0)
            pass_on(LAST, 0)
            hook(pump, "k3")
            for k in (1, 2):
                last_step(1, k)

        def tail_b():
            take(LAST, 1)
            pass_on(LAST, 1)

        def tail_c():
            for k in RINGS:
                last_step(0, k)
            last_step(1, LAST)

        for q in BOTH:
            for d in BOTH:
                link("first", q, d, own=True).start()
        for q in BOTH:
            for d in BOTH:
                link("second", q, 0, d, own=True).start()
        for q in BOTH:
            die(q, 0, 0, own=True)
        own = pltpu.make_async_copy(r.h_ref, out.at[y, x, c], r.ag_loc)
        own.start()
        hook(pump, "begin")
        for d in BOTH:
            for q in BOTH:
                link("first", q, d).wait_recv()
                src = -SIGN[d]
                link("first_on", q, d).start()
                die(q, src, 0)
        hook(pump, "first")
        second_step(0)
        for q in reversed(BOTH):
            for d in BOTH:
                for e in BOTH:
                    link("second", q, 1 + d, e).start()
        hook(pump, "k0")
        for q in BOTH:
            arrived("first_on", q)
            die(q, 2, 0)
        far_first(0)
        hook(pump, "first_on")
        last_step(1, 0)
        own.wait()
        hook(pump, "ready")

        def crossed(off):
            got = out.at[turn(y, off), :, 1 - c]
            remote(got, got, r.ag_dsend, r.ag_drecv.at[off], partner).wait_recv()

        def order(i):
            if isinstance(i, int):
                return (OWN, BEFORE, AFTER, FAR)[i]
            return lax.rem(3 * i + 3 * (i // 2) + 2 * (i // 3), RING)

        def fetch(i, slot):
            off = order(i)
            crossed(off)
            h_copy(l, turn(y, off), slot).start()

        def up_ready():
            hook(pump, "up")
            loaded(UP1 if l else UP0)

        crossed(0)
        h_copy(l, y, 0).start()

        def opening():
            second_step(1)
            hook(pump, "k1")

        def turn_of(i):
            slot = lax.rem(i, H_SLOTS)
            s = turn(y, order(i))
            h_copy(l, s, slot).wait()
            pump(("seq", i))
            one(l, s, slot, i)

            @pl.when(i == 1)
            def _():
                tail_b()

            @pl.when(i == 2)
            def _():
                tail_c()
                fetch(LAST, 0)

            return s, slot

        def neighbours():
            tail_a()
            for n in (1, 2):
                fetch(n, n)

        if l:
            @pl.loop(0, RING)
            def _(i):
                s, slot = turn_of(i)

                @pl.when(i == 0)
                def _():
                    opening()
                    up_ready()

                pump(("two", i))
                two(s, slot)

                @pl.when(i == 0)
                def _():
                    neighbours()
        else:
            h_copy(l, y, 0).wait()
            hook(pump, "own")
            one(l, y, 0, 0)
            opening()
            neighbours()

            @pl.loop(1, RING)
            def _(i):
                turn_of(i)

                @pl.when(i == 1)
                def _():
                    up_ready()

                pump(("two", i - 1))
                two(turn(y, order(i - 1)), lax.rem(i - 1, H_SLOTS))

            hook(pump, "two3")
            two(turn(y, FAR), 0)

        for slot in BOTH:
            for i in BOTH:
                kv_out_copy(l, 0, slot, i).wait()
        sent = (out.at[y, x], out.at[y], out.at[y, x, c], out.at[y, pl.ds(0, CORES)])
        for kind, ref in enumerate(sent):
            remote(ref, ref, r.ag_send.at[kind], r.ag_recv.at[kind], partner).wait_send()
        remote(out.at[pl.ds(0, 2)], out.at[pl.ds(0, 2)], r.ag_dsend, r.ag_drecv.at[0], partner).wait_send()

    def h_copy(l, s, slot):
        return pltpu.make_async_copy(r.h_all.at[l, s], r.hb.at[slot], r.h_sem.at[slot])

    def h_tile(slot):
        return r.hb[slot].reshape(seq_len, d_model)

    def project(h, lo, n):
        w = r.wv[:, :, lo:lo + n].reshape(d_model, n)
        return jnp.dot(h, w, preferred_element_type=F32).astype(BF)

    def rope(val):
        val = val.astype(F32)
        return val * r.cos[...] + pltpu.roll(val, head_dim // 2, 1) * r.sin[...]

    n_chunk = min(256, f_loc)

    def kv_out_copy(l, s, slot, i):
        return pltpu.make_async_copy(r.qkv.at[slot, i], r.kv_out.at[l, i, s], r.kvo_sem.at[slot, i])

    def one(l, s, slot, i):
        pair = i % 2 if isinstance(i, int) else lax.rem(i, 2)

        @pl.when(i >= 2)
        def _():
            for k in BOTH:
                kv_out_copy(l, s, pair, k).wait()

        kv = jnp.zeros((seq_len, 2 * head_dim), F32)
        for zz in RINGS:
            for yy in RINGS:
                col = (zz * RING + yy) * d_row
                kv += lax.dot_general(h_cols(slot, col, d_row), r.kvb[yy, zz], (((1,), (1,)), ((), ())), preferred_element_type=F32)
        kv = kv.astype(BF)
        r.qkv[pair, 0] = rope(kv[:, :head_dim]).astype(BF)
        r.qkv[pair, 1] = kv[:, head_dim:]
        for i in BOTH:
            kv_out_copy(l, s, pair, i).start()
        q = project(h_tile(slot), 0, head_dim)
        r.stage[...] = (rope(q) * head_dim ** -0.5).astype(BF)
        n_tile = seq_len // 2
        for i in BOTH:
            keys = (i + 1) * n_tile
            sc = lax.dot_general(r.stage[i * n_tile:(i + 1) * n_tile, :], r.qkv[pair, 0, :keys, :], (((1,), (1,)), ((), ())), preferred_element_type=F32)
            row_id = lax.broadcasted_iota(jnp.int32, sc.shape, 0) + i * n_tile
            col_id = lax.broadcasted_iota(jnp.int32, sc.shape, 1)
            sc = jnp.where(col_id <= row_id, sc, -1e30)
            top = jnp.max(sc, axis=-1, keepdims=True)
            ex = jnp.exp(sc - top)
            prob = (ex * (1.0 / jnp.sum(ex, axis=-1, keepdims=True))).astype(BF)
            att = jnp.dot(prob, r.qkv[pair, 1, :keys, :], preferred_element_type=F32)
            r.joined[s, i * n_tile:(i + 1) * n_tile, :head_dim] = att.astype(BF)
        for lo in range(0, f_loc, n_chunk):
            r.joined[s, :, head_dim + lo:head_dim + lo + n_chunk] = project(h_tile(slot), head_dim + lo, n_chunk)

    def h_cols(slot, col, n):
        return r.hb[slot, :, :, :, col:col + n].reshape(seq_len, n)

    def two(s, slot):
        for lo in range(0, f_loc, n_chunk):
            up = project(h_tile(slot), head_dim + f_loc + lo, n_chunk).astype(F32)
            cols = slice(head_dim + lo, head_dim + lo + n_chunk)
            g = r.joined[s, :, cols].astype(F32)
            r.joined[s, :, cols] = (g * jax.nn.sigmoid(g) * up).astype(BF)

    def out_scatter(l, pump):
        def peer(q, first, second):
            dy = first * (1 - q) + second * q
            dx = first * q + second * (1 - q)
            return (z, turn(y, dy), turn(x, dx), c)

        def die_copy(ch, q, s):
            return remote(r.away.at[q], r.die_in.at[ch, q, s], r.dsend.at[q], r.drecv.at[ch, q, s], partner)

        def first_copy(ch, q, d):
            return remote(r.acc.at[ch, q, 0, pl.ds(CORES * d, CORES)], r.in1.at[ch, q, d], r.rs_send.at[0], r.recv1.at[ch, q, d],
                          peer(q, SIGN[d], 0))

        def second_copy(ch, q, d, h):
            js = pl.ds(CORES * h, CORES)
            return remote(r.acc.at[ch, q, 1 + d, js], r.in2.at[ch, q, d, js], r.rs_send.at[1], r.recv2.at[ch, q],
                          peer(q, SIGN[d], 0))

        def half_rows(d):
            return pl.ds(d * (rows // 2), rows // 2)

        def third_copy(ch, q, d):
            return remote(r.acc.at[ch, q, LAST, 0, half_rows(d)], r.in3.at[ch, q, d], r.rs_send.at[2], r.recv3.at[ch, q, d],
                          peer(q, 0, SIGN[d]))

        def fourth_copy(ch, q, d):
            return remote(r.acc.at[ch, q, LAST, 1 + d], r.in4.at[ch, q, d], r.rs_send.at[LAST], r.recv4.at[ch, q],
                          peer(q, 0, SIGN[d]))

        n_blk = r.wov.shape[3]

        def plane_of(ch, q):
            if l:
                return turn(z, q if ch else 2 + q)
            return turn(z, LAST - q if ch else q)

        def slot_off(s):
            return lax.rem(2 + 3 * s + 3 * (s // 2) + 2 * (s // 3), RING)

        def tile(ch, q, s):
            off = slot_off(s)
            for cc in BOTH:
                for j in RINGS:
                    oy = off * (1 - q) + SLOT_OFF[j] * q
                    ox = SLOT_OFF[j] * (1 - q) + off * q
                    core = c if cc else 1 - c
                    at = pl.multiple_of((turn(x, ox) * CORES + core) * rows, rows)
                    r.lhs[pl.ds((cc * RING + j) * rows, rows), :] = r.joined[turn(y, oy), pl.ds(at, rows), :]
            left = r.lhs[...]
            zz = plane_of(ch, q)
            for n in RINGS:
                res = jnp.dot(left, r.wov[zz, n], preferred_element_type=F32).astype(BF)
                res = res.reshape(CORES, RING, rows, n_blk)
                r.away[q, :, :, n * n_blk:(n + 1) * n_blk] = res[0]
                r.acc[ch, q, s, :, :, n * n_blk:(n + 1) * n_blk] = res[1]

        def pair_sum(ch, q, s):
            die_copy(ch, q, s).wait_recv()

            @pl.loop(0, RING)
            def _(j):
                r.acc[ch, q, s, j] = r.acc[ch, q, s, j] + r.die_in[ch, q, s, j]

        def stage_a(ch):
            @pl.loop(0, CORES * RING)
            def _(t):
                s = t // CORES
                q = lax.rem(t, CORES)

                @pl.when(s >= 1)
                def _():
                    die_copy(ch, q, s - 1).wait_send()

                if ch:
                    @pl.when(s == 0)
                    def _():
                        die_copy(ch - 1, q, LAST).wait_send()

                tile(ch, q, s)
                die_copy(ch, q, s).start()

                @pl.when(s >= 1)
                def _():
                    pair_sum(ch, q, s - 1)

                @pl.when(s == 1)
                def _():
                    for d in BOTH:
                        first_copy(ch, q, d).start()

                for d in BOTH:
                    @pl.when(s == 2 + d)
                    def _(d=d):
                        second_copy(ch, q, d, 1 - d).start()

                for n in RINGS:
                    name = f"a{ch}s{n}"
                    if pump(name, False):
                        @pl.when(t == CORES * n + 1)
                        def _(name=name):
                            hook(pump, name)

        def stage_b(ch):
            for q in BOTH:
                pair_sum(ch, q, LAST)
            for q in BOTH:
                for d in BOTH:
                    first_copy(ch, q, d).wait_recv()
                    for j in BOTH:
                        at = CORES * d + j
                        r.acc[ch, q, 1 + d, at] = r.acc[ch, q, 1 + d, at] + r.in1[ch, q, d, j]
                    second_copy(ch, q, d, d).start()

        def total(ch, q, j):
            val = r.acc[ch, q, LAST, j].astype(F32)
            for d in BOTH:
                val += r.in2[ch, q, d, j].astype(F32)
            r.acc[ch, q, LAST, j] = val.astype(BF)

        def stage_c(ch):
            for q in BOTH:
                ref = r.in2.at[ch, q]
                remote(ref, ref, r.rs_send.at[1], r.recv2.at[ch, q], here).wait_recv()
                total(ch, q, 0)
                for d in BOTH:
                    third_copy(ch, q, d).start()
                for j in RINGS[1:]:
                    total(ch, q, j)

        def stage_d(ch):
            for q in BOTH:
                for d in BOTH:
                    third_copy(ch, q, d).wait_recv()
                    rws = half_rows(d)
                    r.acc[ch, q, LAST, 1 + d, rws] = r.acc[ch, q, LAST, 1 + d, rws] + r.in3[ch, q, d]
                    fourth_copy(ch, q, d).start()

        def stage_e(ch):
            for q in BOTH:
                ref = r.in4.at[ch, q]
                remote(ref, ref, r.rs_send.at[LAST], r.recv4.at[ch, q], here).wait_recv()
                cols = pl.ds(pl.multiple_of(plane_of(ch, q) * width, width), width)
                upd = r.acc[ch, q, LAST, LAST].astype(F32)
                for d in BOTH:
                    upd += r.in4[ch, q, d].astype(F32)
                upd = upd.astype(BF)
                r.hid[:, cols] = (r.hid[:, cols].astype(F32) + upd.astype(F32)).astype(BF)

        stages = {"a": stage_a, "b": stage_b, "c": stage_c, "d": stage_d, "e": stage_e, "f": leave_a, "g": leave_b, "h": leave_c}
        for step in LAST_ORDER if l else FIRST_ORDER:
            with jax.named_scope(step):
                stages[step[0]](int(step[1]))
            hook(pump, step)
        for q in BOTH:
            die_copy(1, q, LAST).wait_send()
        for n, ref in enumerate((r.in1, r.in2, r.in3, r.in4)):
            remote(ref, ref, r.rs_send.at[n], r.drecv.at[0, 0, 0], here).wait_send()

    def near(fn, t):
        for j in (LAST, 1):
            fn(t, j)

    def far(fn, t):
        fn(t, 2)

    def z_all(t):
        near(z_direct, t)
        far(z_direct, t)

    def peers_of(fn, op="start"):
        for k in range(len(OTHERS)):
            getattr(fn(k), op)()

    def start(pump):
        peers_of(gain_z)
        kv_z()
        peers_of(x_z)
        x_own().start()
        pump("s0")
        with jax.named_scope("gain_a"):
            peers_of(gain_z, "wait_recv")
            peers_of(gain_y)
            kv_y1()
        pump("s1")
        with jax.named_scope("gain_b"):
            peers_of(gain_y, "wait_recv")
            peers_of(gain_x)
            gain_die(x, LAST).start()
        pump("s2")
        with jax.named_scope("x_z"):
            three_planes().wait_recv()
            x_own().wait()
        for oy in RINGS:
            for ox in RINGS:
                if oy or ox:
                    x_plane(oy, ox).start()
        r.xp[c, y, x] = r.xz[:, y, :, pos(x)]
        pump("s3")
        with jax.named_scope("kv_b"):
            kv_y2()
        with jax.named_scope("gain_c"):
            for k, o in enumerate(OTHERS):
                gain_x(k).wait_recv()
                gain_die(turn(x, -o), k).start()
        pump("s4")
        for oy in (OWN, BEFORE, AFTER, FAR):
            with jax.named_scope(f"row_{oy}"):
                x_row(oy)
            pump(f"r{oy}")
        pump("s5")
        kv_y3()
        pump("s6")
        with jax.named_scope("gain_sum"):
            for k in RINGS:
                gain_die(x, k).wait_recv()
            gain_sum()
            for fill in fills[1:]:
                fill.wait()
        with jax.named_scope("turn"):
            x_turn()
        pump("s7")

    def when(i, n, *fns):
        @pl.when(i == n)
        def _():
            for fn in fns:
                fn()

    def plan(steps):
        def pump(step, run=True):
            if not isinstance(step, str):
                for n in RINGS:
                    if (step[0], n) in steps:
                        when(step[1], n, lambda n=n: run_steps(steps[step[0], n]))
                return True
            found = steps.get(step, ())
            if run:
                run_steps(found)
            return found
        return pump

    def run_steps(steps):
        for fn, *args in steps:
            with jax.named_scope(f"{fn.__name__}_{args[-1] if args else 0}"):
                fn(*args)

    first_entry = plan({
        "s0": [(z_own, UP0)],
        "s1": [(y_send, QG0)],
        "s3": [(z_own, QG0)],
        "r0": [(y_relay, QG0), (z_forward, UP0, OWN), (z_direct, QG0, AFTER), (z_forward, QG0, OWN), (z_direct, QG0, BEFORE)],
        "s6": [(kv_x1, 0)],
    })
    first_front = plan({
        "begin": [(kv_x2, 0), (y_send, UP0), (z_forward, QG0, AFTER), (z_direct, QG0, FAR)],
        "k0": [(y_relay, UP0), (kv_x3, 0), (z_forward, QG0, BEFORE), (z_forward, QG0, FAR), (z_direct, UP0, AFTER), (z_direct, UP0, BEFORE)],
        "first_on": [(y_send, WO0)],
        "ready": [(load_near, QG0), (load_far, QG0), (kv_load, 0), (loaded, QG0), (kv_loaded,)],
        "k1": [(z_direct, UP0, FAR), (z_forward, UP0, AFTER)],
        "k2": [
            (z_forward, UP0, BEFORE), (y_relay, WO0), (z_forward, UP0, FAR), (y_send, QG1), (z_own, WO0), (z_direct, WO0, BEFORE),
            (kv_x1, 1),
        ],
        ("seq", 1): [(y_send, WO1), (z_direct, WO0, AFTER), (x_sent,)],
        "up": [(y_send, UP1), (z_direct, WO0, FAR), (load_near, UP0), (load_far, UP0)],
        ("two", 0): [(y_relay, QG1), (z_forward, WO0, OWN)],
        ("seq", 2): [(kv_x2, 1)],
        ("two", 1): [(kv_x3, 1), (z_direct, QG1, AFTER), (z_forward, WO0, BEFORE)],
        ("seq", 3): [(y_relay, WO1), (z_forward, WO0, AFTER)],
        ("two", 2): [(z_forward, WO0, FAR), (z_own, QG1), (y_relay, UP1)],
        "near": [(load_near, WO0)],
    })
    first_scatter = plan({
        "a0s0": [(z_forward, QG1, AFTER)],
        "a0s2": [(z_direct, QG1, BEFORE)],
        "b0": [(load_far, WO0), (far_loaded, WO0)],
        "a1s0": [(z_direct, QG1, FAR)],
        "a1s1": [(z_forward, QG1, OWN)],
        "a1": [(z_direct, UP1, FAR)],
        "b1": [(z_direct, UP1, BEFORE)],
        "c1": [(z_forward, QG1, FAR), (z_direct, UP1, AFTER), (z_own, UP1), (z_forward, QG1, BEFORE)],
        "e0": [(z_forward, UP1, FAR)],
    })
    second_front = plan({
        "begin": [(z_forward, UP1, BEFORE), (kv_load, 1)],
        "first": [(z_forward, UP1, AFTER)],
        "k0": [(z_forward, UP1, OWN), (z_direct, WO1, FAR)],
        "ready": [(load_near, QG1), (load_far, QG1), (loaded, QG1), (kv_loaded,)],
        ("seq", 0): [(z_own, WO1)],
        "k1": [(z_direct, WO1, BEFORE)],
        "up": [(load_near, UP1), (load_far, UP1)],
        "k2": [(z_direct, WO1, AFTER)],
        ("seq", 1): [(z_forward, WO1, FAR)],
        ("two", 1): [(z_forward, WO1, OWN)],
        ("two", 2): [(z_forward, WO1, BEFORE), (z_forward, WO1, AFTER)],
        "near": [(load_near, WO1), (load_far, WO1)],
    })
    second_scatter = plan({
    })

    with jax.named_scope("start"):
        start(first_entry)
    with jax.named_scope("front_0"):
        gather_norm(0, rows // RING, first_front)
    with jax.named_scope("near_0"):
        kv_share(0)
        first_front("near")
        near_loaded(WO0)
    with jax.named_scope("scatter_0"):
        out_scatter(0, first_scatter)
    with jax.named_scope("front_1"):
        gather_norm(1, rows // 2, second_front)
    with jax.named_scope("near_1"):
        kv_share(1)
        second_front("near")
        loaded(WO1)
    with jax.named_scope("scatter_1"):
        out_scatter(1, second_scatter)
    with jax.named_scope("drain"):
        left()
        for t in range(WO1 + 1):
            drain(t)
        for l in range(n_layers):
            kv_shared(l)
            kv_sent(l)


def run_model(xt, gain, wkv_t, w_in, w_out, cos_full, sin_full):
    batch, d_local, seq_len = xt.shape
    n_layers, d_row, e_block = w_in.shape
    r_block, d_col = w_out.shape[1:]
    head_dim = cos_full.shape[1]
    d_model = d_row * RING * RING
    seqs = batch // RING
    rows = seqs * seq_len // (RING * RING * CORES)
    e_loc, r_loc = e_block // RING, r_block // RING
    kc = wkv_t.shape[1]
    width = d_model // RING
    n_t = 3 * n_layers
    n_o = len(OTHERS)

    def dma(*shape):
        return pltpu.SemaphoreType.DMA(shape)

    def vm(*shape):
        return pltpu.VMEM(shape, BF)

    def out(*shape):
        return jax.ShapeDtypeStruct(shape, BF)

    any_spec = pl.BlockSpec(memory_space=pl.ANY)
    out_shape = [
        out(batch, d_local, seq_len),
        out(n_layers, 2, seqs, seq_len, head_dim),
        out(n_layers, RING, RING, CORES, rows, d_model),
        out(n_layers, RING, RING * d_row, e_loc),
        out(n_layers, RING, RING, r_loc, d_col),
        out(RING, CORES, n_layers, RING, RING, kc, d_row),
        out(n_layers, RING, 2, seqs, CORES * (seq_len // (CORES * RING * RING * RING)), head_dim),
        out(n_layers, 2, d_row // 2, e_loc),
        out(n_layers, 2, r_loc // 2, d_col),
    ]
    pair = (2, 2, 2)
    scratch = [
        pltpu.VMEM(cos_full.shape, F32), pltpu.VMEM(cos_full.shape, F32), vm(n_layers, d_local),
        vm(rows, d_model), vm(rows, d_model), pltpu.VMEM((n_layers, d_model), F32),
        vm(RING, CORES, RING, RING, G_ROWS, d_row),
        vm(RING, seqs, d_local, seq_len),
        vm(CORES, RING, RING, RING, d_local, CORES * rows),
        vm(RING, RING * d_row, e_loc), vm(RING, RING, 2 * head_dim, d_row), vm(RING, RING, r_loc, d_col),
        vm(H_SLOTS, RING, CORES, rows, d_model), vm(RING, seq_len, r_loc), vm(2, 2, seq_len, head_dim), vm(seq_len, head_dim),
        vm(CORES * RING * rows, r_loc), vm(2, RING, rows, width), vm(2, 2, RING, RING, rows, width), vm(2, 2, RING, RING, rows, width),
        vm(*pair, 2, rows, width), vm(*pair, RING, rows, width), vm(*pair, rows // 2, width), vm(*pair, rows, width),
        pltpu.SemaphoreType.DMA, pltpu.SemaphoreType.DMA, dma(RING), dma(RING), pltpu.SemaphoreType.DMA, pltpu.SemaphoreType.DMA,
        pltpu.SemaphoreType.DMA,
        dma(3 * n_o), dma(3 * n_o), dma(RING), dma(RING),
        dma(RING), dma(RING), dma(2, RING), dma(2, RING), dma(RING), dma(RING), pltpu.SemaphoreType.DMA,
        dma(RING), dma(40), pltpu.SemaphoreType.DMA, dma(RING), pltpu.SemaphoreType.DMA, dma(H_SLOTS), dma(2, 2), dma(3), dma(3),
        dma(n_t, RING), dma(n_t, 2), dma(3, RING, 2), dma(3), dma(n_t),
        dma(n_o), dma(n_o), pltpu.SemaphoreType.DMA, dma(n_o), dma(n_layers), dma(n_layers, n_o), dma(n_layers), dma(n_layers), dma(2),
        dma(2), dma(2, 2, RING), dma(RING), dma(*pair), dma(2, 2), dma(*pair), dma(2, 2),
        dma(3), dma(n_layers, n_o), dma(n_layers, n_o), dma(n_layers),
    ]
    res = pl.pallas_call(
        model_kernel,
        out_shape=out_shape,
        in_specs=[any_spec] * 7,
        out_specs=[any_spec] * len(out_shape),
        scratch_shapes=scratch,
        compiler_params=pltpu.CompilerParams(collective_id=0, has_side_effects=True, vmem_limit_bytes=VMEM_LIMIT),
        name="two_layers",
    )(xt, gain, wkv_t, w_in, w_out, cos_full, sin_full)
    return res[0], res[6]


def solution(mesh):
    row_size = mesh.shape["row"]
    n_col = mesh.shape["col"]
    n_z = row_size // RING
    n_y = RING
    n_x = n_col // CORES
    n_tp = n_y * n_col
    n_dev = row_size * n_col
    mesh4 = Mesh(mesh.devices.reshape(n_z, n_y, n_x, CORES), ("z", "y", "x", "core"))
    every = ("z", "y", "x", "core")
    col = ("x", "core")
    act_spec = P(NIL, NIL, every)
    w_spec = P(NIL, ("z", "y"), col)

    def device_fn(x_loc, gain_loc, w_in_loc, w_kv_loc, w_out_loc):
        n_layers = w_in_loc.shape[0]
        n_batch, seq_len, d_local = x_loc.shape
        head_dim = w_kv_loc.shape[2] * n_col // 2
        batch_loc = n_batch // n_z
        seq_local = seq_len // n_dev
        steps = np.arange(head_dim // 2, dtype=np.float32)
        inv_freq = (1.0 / 10000.0 ** (steps * 2 / head_dim)).astype(np.float32)
        angles = np.arange(seq_len, dtype=np.float32)[:, NIL] * inv_freq[NIL, :]
        cos_tab, sin_tab = np.cos(angles), np.sin(angles)
        cos_full = jnp.asarray(np.concatenate([cos_tab, cos_tab], axis=1))
        sin_full = jnp.asarray(np.concatenate([-sin_tab, sin_tab], axis=1))
        y_loc, kv = run_model(x_loc.transpose(0, 2, 1), gain_loc, w_kv_loc.transpose(0, 2, 1), w_in_loc, w_out_loc, cos_full, sin_full)
        y_loc = y_loc.transpose(0, 2, 1)
        kv = kv.reshape(n_layers, n_z, 2, batch_loc, CORES, seq_local, head_dim)
        kv = lax.dynamic_index_in_dim(kv, lax.axis_index("core"), axis=4, keepdims=False)
        kv = kv.transpose(0, 2, 1, 3, 4, 5).reshape(n_layers, 2, n_batch, seq_local, head_dim)
        return y_loc, kv

    return jax.shard_map(device_fn, mesh=mesh4, in_specs=(act_spec, P(NIL, every), w_spec, w_spec, P(NIL, col, ("z", "y"))), out_specs=(act_spec, P(NIL, NIL, NIL, every, NIL)), check_vma=False)
```

```python
import typing

import jax
import jax.numpy as jnp
import numpy as np
from jax import lax
from jax.experimental import pallas as pl
from jax.experimental.pallas import tpu as pltpu
from jax.sharding import Mesh
from jax.sharding import PartitionSpec as P

LN_EPS = 1e-6
RING = 4
CORES = 2
VMEM_LIMIT = 67_000_000
BF = jnp.bfloat16
F32 = jnp.float32
SLOT_OFF = (2, 1, 3, 0)
SIGN = (1, -1)
NIL = None
BOTH = range(CORES)
RINGS = range(RING)
OTHERS = (1, 3, 2)
LAST = RING - 1
G_ROWS = 8
H_SLOTS = 3
QG0, UP0, WO0, QG1, UP1, WO1 = range(6)
OWN, AFTER, FAR, BEFORE = RINGS
FIRST_ORDER = ("a0", "b0", "a1", "b1", "c0", "c1", "d0", "d1", "e0", "e1")
LAST_ORDER = FIRST_ORDER[:-1] + ("f1", "e1", "g1", "f0", "g0", "h1", "h0")
KINDS = ("first", "second", "first_on", "second_on")


class Refs(typing.NamedTuple):
    xt: typing.Any
    gain_in: typing.Any
    wkv: typing.Any
    w_in: typing.Any
    w_out: typing.Any
    cos_in: typing.Any
    sin_in: typing.Any
    y_out: typing.Any
    kv_out: typing.Any
    h_all: typing.Any
    wi: typing.Any
    wo: typing.Any
    kvh: typing.Any
    kvx: typing.Any
    rwi: typing.Any
    rwo: typing.Any
    cos: typing.Any
    sin: typing.Any
    gain_own: typing.Any
    h_ref: typing.Any
    hid: typing.Any
    gain: typing.Any
    gbuf: typing.Any
    xz: typing.Any
    xp: typing.Any
    wv: typing.Any
    kvb: typing.Any
    wov: typing.Any
    hb: typing.Any
    joined: typing.Any
    qkv: typing.Any
    stage: typing.Any
    lhs: typing.Any
    away: typing.Any
    acc: typing.Any
    die_in: typing.Any
    in1: typing.Any
    in2: typing.Any
    in3: typing.Any
    in4: typing.Any
    xz_send: typing.Any
    xz_recv: typing.Any
    xp_send: typing.Any
    xp_recv: typing.Any
    xd_send: typing.Any
    xd_recv: typing.Any
    x_loc: typing.Any
    g_send: typing.Any
    g_recv: typing.Any
    gd_send: typing.Any
    gd_recv: typing.Any
    yd_send: typing.Any
    yd_recv: typing.Any
    yp_send: typing.Any
    yp_recv: typing.Any
    yz_send: typing.Any
    yz_recv: typing.Any
    y_loc: typing.Any
    ag_send: typing.Any
    ag_recv: typing.Any
    ag_dsend: typing.Any
    ag_drecv: typing.Any
    ag_loc: typing.Any
    h_sem: typing.Any
    kvo_sem: typing.Any
    w_load: typing.Any
    far_load: typing.Any
    y_recv: typing.Any
    ry_recv: typing.Any
    zb_recv: typing.Any
    zc_recv: typing.Any
    w_send: typing.Any
    kz_send: typing.Any
    kz_recv: typing.Any
    ky_send: typing.Any
    ky_recv: typing.Any
    kx_send: typing.Any
    kx_recv: typing.Any
    kd_send: typing.Any
    kd_recv: typing.Any
    k_loc: typing.Any
    dsend: typing.Any
    drecv: typing.Any
    rs_send: typing.Any
    recv1: typing.Any
    recv2: typing.Any
    recv3: typing.Any
    recv4: typing.Any
    small: typing.Any
    kvx_send: typing.Any
    kvx_recv: typing.Any
    kvx_loc: typing.Any


def model_kernel(*refs):
    r = Refs(*refs)
    z, y, x, c = (lax.axis_index(a) for a in ("z", "y", "x", "core"))
    n_layers = r.wkv.shape[0]
    rows, d_model = r.hid.shape
    batch, d_local = r.xt.shape[:2]
    seqs = batch // RING
    seq_len, head_dim = r.cos.shape
    d_row = r.w_in.shape[1]
    e_loc = r.wi.shape[3]
    depth = r.wo.shape[3]
    f_loc = depth - head_dim
    quarter = rows // 4
    width = d_model // RING
    q_block = head_dim * RING
    f_block = f_loc * RING

    turned = {id(v): [lax.rem(v + o, RING) for o in RINGS] for v in (z, y, x)}

    def turn(base, off):
        if isinstance(off, int):
            return turned[id(base)][off % RING]
        return lax.rem(base + off + RING, RING)

    def remote(src, dst, ssem, rsem, dev):
        return pltpu.make_async_remote_copy(
            src_ref=src, dst_ref=dst, send_sem=ssem, recv_sem=rsem, device_id=dev, device_id_type=pl.DeviceIdType.MESH)

    partner = (z, y, x, 1 - c)

    peers = [(turn(z, o), y, x, c) for o in OTHERS]
    peers += [(z, turn(y, oy), turn(x, ox), c) for oy in RINGS for ox in RINGS if oy or ox]
    peers.append(partner)
    here = (z, y, x, c)
    gate_sem = pltpu.get_barrier_semaphore()
    for dev in peers:
        pl.semaphore_signal(gate_sem, inc=1, device_id=dev, device_id_type=pl.DeviceIdType.MESH)
    fills = [pltpu.make_async_copy(src, dst, r.small.at[n]) for n, (src, dst) in enumerate(
        ((r.gain_in, r.gain_own), (r.cos_in, r.cos), (r.sin_in, r.sin)))]
    for fill in fills:
        fill.start()
    fills[0].wait()

    src_id = lax.broadcasted_iota(jnp.int32, (d_local, d_row), 0) + (x * CORES + c) * d_local
    dst_id = lax.broadcasted_iota(jnp.int32, (d_local, d_row), 1)
    spread = jnp.where(src_id == dst_id, 1.0, 0.0).astype(BF)
    r.gbuf[x, c, y, z] = jnp.zeros((G_ROWS, d_row), BF)
    r.gbuf[x, c, y, z, :n_layers] = jnp.dot(r.gain_own[...], spread, preferred_element_type=F32).astype(BF)
    pl.semaphore_wait(gate_sem, len(peers))

    def hook(pump, i):
        with jax.named_scope(f"hook_{i}"):
            pump(i)

    def w_cols(kind):
        return pl.ds(0, head_dim + f_loc) if kind == 0 else pl.ds(head_dim + f_loc, f_loc)

    def piece(t, zz, yy):
        l, kind = t // 3, t % 3
        if kind == 2:
            return r.wo.at[l, zz, yy]
        return r.wi.at[l, zz, pl.ds(pl.multiple_of(yy * d_row, d_row), d_row), w_cols(kind)]

    def piece_half(t, zz, yy, h):
        l, kind = t // 3, t % 3
        if kind == 2:
            return r.wo.at[l, zz, yy, pl.ds(h * (depth // 2), depth // 2)]
        return r.wi.at[l, zz, pl.ds(pl.multiple_of(yy * d_row + h * (d_row // 2), d_row // 2), d_row // 2), w_cols(kind)]

    def own_parts(t, owner, zz, yy):
        l, kind = t // 3, t % 3
        hq = pl.ds(pl.multiple_of(owner * head_dim, head_dim), head_dim)
        if kind == 2:
            return [
                (r.w_out.at[l, hq], r.wo.at[l, zz, yy, pl.ds(0, head_dim)]),
                (r.w_out.at[l, pl.ds(pl.multiple_of(q_block + owner * f_loc, head_dim), f_loc)], r.wo.at[l, zz, yy, pl.ds(head_dim, f_loc)]),
            ]
        rws = pl.ds(pl.multiple_of(yy * d_row, d_row), d_row)
        if kind == 0:
            return [
                (r.w_in.at[l, :, hq], r.wi.at[l, zz, rws, pl.ds(0, head_dim)]),
                (r.w_in.at[l, :, pl.ds(pl.multiple_of(q_block + owner * f_loc, head_dim), f_loc)], r.wi.at[l, zz, rws, pl.ds(head_dim, f_loc)]),
            ]
        return [(r.w_in.at[l, :, pl.ds(pl.multiple_of(q_block + f_block + owner * f_loc, head_dim), f_loc)],
                 r.wi.at[l, zz, rws, pl.ds(head_dim + f_loc, f_loc)])]

    def relay_ref(t, d):
        l, kind = t // 3, t % 3
        return r.rwo.at[l, d] if kind == 2 else r.rwi.at[l, d, :, w_cols(kind)]

    def far_parts(t, d):
        l, kind = t // 3, t % 3
        owner = turn(y, 2)
        hq = pl.ds(pl.multiple_of(owner * head_dim, head_dim), head_dim)
        if kind == 2:
            n = depth // 2
            base = q_block + owner * f_loc
            if d:
                return [(r.w_out.at[l, pl.ds(pl.multiple_of(base + n - head_dim, G_ROWS), n)], r.rwo.at[l, d])]
            return [
                (r.w_out.at[l, hq], r.rwo.at[l, d, pl.ds(0, head_dim)]),
                (r.w_out.at[l, pl.ds(pl.multiple_of(base, head_dim), n - head_dim)], r.rwo.at[l, d, pl.ds(head_dim, n - head_dim)]),
            ]
        rws = pl.ds(d * (d_row // 2), d_row // 2)
        if kind == 0:
            return [
                (r.w_in.at[l, rws, hq], r.rwi.at[l, d, :, pl.ds(0, head_dim)]),
                (r.w_in.at[l, rws, pl.ds(pl.multiple_of(q_block + owner * f_loc, head_dim), f_loc)], r.rwi.at[l, d, :, pl.ds(head_dim, f_loc)]),
            ]
        return [(r.w_in.at[l, rws, pl.ds(pl.multiple_of(q_block + f_block + owner * f_loc, head_dim), f_loc)], relay_ref(t, d))]

    def y_send(t):
        for d in BOTH:
            owner = turn(y, SIGN[d])
            dev = (z, owner, x, c)
            for src, dst in far_parts(t, d):
                remote(src, dst, r.w_send.at[t], r.ry_recv.at[t, d], dev).start()
            for src, dst in own_parts(t, owner, z, y):
                remote(src, dst, r.w_send.at[t], r.y_recv.at[t, -SIGN[d] % RING], dev).start()

    def y_relay(t):
        for d in BOTH:
            ref = relay_ref(t, d)
            remote(ref, ref, r.w_send.at[t], r.ry_recv.at[t, d], here).wait_recv()
            dst = piece_half(t, z, turn(y, -SIGN[d]), d)
            remote(ref, dst, r.w_send.at[t], r.y_recv.at[t, 2], (z, turn(y, SIGN[d]), x, c)).start()

    def z_own(t):
        for d in BOTH:
            for src, dst in own_parts(t, y, z, y):
                remote(src, dst, r.w_send.at[t], r.zb_recv.at[t % 3, 0, d], (turn(z, SIGN[d]), y, x, c)).start()

    def z_direct(t, j):
        yy = turn(y, j)
        ref = piece(t, z, yy)
        remote(ref, ref, r.w_send.at[t], r.y_recv.at[t, j], here).wait_recv()
        for d in BOTH:
            remote(ref, ref, r.w_send.at[t], r.zb_recv.at[t % 3, j, d], (turn(z, SIGN[d]), y, x, c)).start()

    def z_forward(t, j):
        yy = turn(y, j)
        for d in BOTH:
            zz = turn(z, -SIGN[d])
            ref = piece(t, zz, yy)
            remote(ref, ref, r.w_send.at[t], r.zb_recv.at[t % 3, j, d], here).wait_recv()
            part = piece_half(t, zz, yy, d)
            remote(part, part, r.w_send.at[t], r.zc_recv.at[t % 3], (turn(z, SIGN[d]), y, x, c)).start()

    def place(t, zz):
        l, kind = t // 3, t % 3
        if kind == 2:
            return r.wo.at[l, zz], r.wov.at[zz]
        return r.wi.at[l, zz, :, w_cols(kind)], r.wv.at[zz, :, w_cols(kind)]

    def load_near(t):
        kind = t % 3
        for d in BOTH:
            src, dst = place(t, turn(z, SIGN[d]))
            pltpu.make_async_copy(src, dst, r.w_load.at[kind]).start()
        for j in OTHERS:
            yy = turn(y, j)
            dst = r.wov.at[z, yy] if kind == 2 else r.wv.at[z, pl.ds(pl.multiple_of(yy * d_row, d_row), d_row), w_cols(kind)]
            pltpu.make_async_copy(piece(t, z, yy), dst, r.w_load.at[kind]).start()
        for src, dst in own_parts(t, y, z, y):
            pltpu.make_async_copy(src, own_place(t, dst, src), r.w_load.at[kind]).start()

    def load_far(t):
        src, dst = place(t, turn(z, 2))
        remote(src, src, r.w_send.at[t], r.zc_recv.at[t % 3], here).wait_recv()
        pltpu.make_async_copy(src, dst, r.far_load.at[t % 3]).start()

    def own_place(t, dst, src):
        kind = t % 3
        if kind == 2:
            n = src.shape[0]
            return r.wov.at[z, y, pl.ds(0 if n == head_dim and f_loc != head_dim else head_dim, n)]
        n = src.shape[1]
        rws = pl.ds(pl.multiple_of(y * d_row, d_row), d_row)
        if kind == 0:
            return r.wv.at[z, rws, pl.ds(0 if n == head_dim and f_loc != head_dim else head_dim, n)]
        return r.wv.at[z, rws, pl.ds(head_dim + f_loc, f_loc)]

    def near_loaded(t):
        kind = t % 3
        dst = r.wov.at[pl.ds(0, LAST)] if kind == 2 else r.wv.at[pl.ds(0, LAST), :, w_cols(kind)]
        pltpu.make_async_copy(dst, dst, r.w_load.at[kind]).wait()

    def far_loaded(t):
        kind = t % 3
        dst = r.wov.at[0] if kind == 2 else r.wv.at[0, :, w_cols(kind)]
        pltpu.make_async_copy(dst, dst, r.far_load.at[kind]).wait()

    def loaded(t):
        near_loaded(t)
        far_loaded(t)

    def drain(t):
        l, kind = t // 3, t % 3
        ref = r.wo.at[l] if kind == 2 else r.wi.at[l, :, :, w_cols(kind)]
        remote(ref, ref, r.w_send.at[t], r.y_recv.at[t, 0], here).wait_send()

    def kv_z_copy(k):
        return remote(r.wkv, r.kvh.at[x, c, :, y, z], r.kz_send.at[k], r.kz_recv.at[k], (turn(z, OTHERS[k]), y, x, c))

    def kv_own():
        return pltpu.make_async_copy(r.wkv, r.kvh.at[x, c, :, y, z], r.k_loc.at[0])

    def kv_z():
        for k in range(len(OTHERS)):
            kv_z_copy(k).start()
        kv_own().start()

    def kv_y_copy(ref, k, d):
        return remote(ref, ref, r.ky_send, r.ky_recv.at[k], (z, turn(y, SIGN[d]), x, c))

    def kv_y1():
        kv_own().wait()
        for k in range(len(OTHERS)):
            kv_z_copy(k).wait()
        for d in BOTH:
            kv_y_copy(r.kvh.at[x, c, :, y], d, d).start()

    def kv_y2():
        for d in BOTH:
            yy = turn(y, -SIGN[d])
            kv_y_copy(r.kvh.at[x, c, :, yy], d, d).wait_recv()
            kv_y_copy(r.kvh.at[x, c, :, yy, pl.ds(2 * d, 2)], 2, d).start()

    def kv_y3():
        kv_y_copy(r.kvh.at[x, c, :, turn(y, 2)], 2, 0).wait_recv()
        kv_y_copy(r.kvh.at[x, c, :, pl.ds(0, LAST)], 0, 0).wait_send()

    def kv_x_copy(l, ref, k, d):
        return remote(ref, ref, r.kx_send.at[l], r.kx_recv.at[l, k], (z, y, turn(x, SIGN[d]), c))

    def kv_die(l, ref):
        return remote(ref, ref, r.kd_send.at[l], r.kd_recv.at[l], partner)

    def kv_x1(l):
        ref = r.kvh.at[x, c, l]
        for d in BOTH:
            kv_x_copy(l, ref, d, d).start()
        kv_die(l, ref).start()

    def kv_x2(l):
        for d in BOTH:
            xx = turn(x, -SIGN[d])
            ref = r.kvh.at[xx, c, l]
            kv_x_copy(l, ref, d, d).wait_recv()
            kv_x_copy(l, r.kvh.at[xx, c, l, pl.ds(2 * d, 2)], 2, d).start()
            kv_die(l, ref).start()

    def kv_x3(l):
        ref = r.kvh.at[turn(x, 2), c, l]
        kv_x_copy(l, ref, 2, 0).wait_recv()
        kv_die(l, ref).start()

    def kv_load(l):
        kv_die(l, r.kvh.at[:, 1 - c, l]).wait_recv()
        kc = r.wkv.shape[1]
        for xx in RINGS:
            for cc in BOTH:
                pltpu.make_async_copy(r.kvh.at[xx, cc, l], r.kvb.at[:, :, pl.ds((xx * CORES + cc) * kc, kc)], r.k_loc.at[1]).start()

    def kv_sent(l):
        kv_x_copy(l, r.kvh.at[pl.ds(0, LAST), c, l], 0, 0).wait_send()
        kv_die(l, r.kvh.at[:, c, l]).wait_send()

    def kv_loaded():
        pltpu.make_async_copy(r.kvb, r.kvb, r.k_loc.at[1]).wait()

    def gain_move(i, src, dst, dev):
        return remote(src, dst, r.g_send.at[i], r.g_recv.at[i], dev)

    def gain_z(k):
        dev = (turn(z, OTHERS[k]), y, x, c)
        return gain_move(k, r.gbuf.at[x, c, y, z], r.gbuf.at[x, c, y, z], dev)

    def gain_y(k):
        dev = (z, turn(y, OTHERS[k]), x, c)
        return gain_move(len(OTHERS) + k, r.gbuf.at[x, c, y], r.gbuf.at[x, c, y], dev)

    def gain_x(k):
        dev = (z, y, turn(x, OTHERS[k]), c)
        return gain_move(CORES * len(OTHERS) + k, r.gbuf.at[x, c], r.gbuf.at[x, c], dev)

    def gain_die(xx, k):
        ref = r.gbuf.at[xx, c]
        return remote(ref, ref, r.gd_send.at[k], r.gd_recv.at[k], partner)

    def gain_sum():
        for zz in RINGS:
            for yy in RINGS:
                tot = jnp.zeros((n_layers, d_row), F32)
                for xx in RINGS:
                    for cc in BOTH:
                        tot += r.gbuf[xx, cc, yy, zz, :n_layers].astype(F32)
                at = (zz * RING + yy) * d_row
                r.gain[:, at:at + d_row] = tot

    tok_pair = CORES * rows

    def x_z(k):
        zz = turn(z, OTHERS[k])
        src = r.xt.at[pl.ds(zz * seqs, seqs)]
        return remote(src, r.xz.at[z], r.xz_send, r.xz_recv, (zz, y, x, c))

    def three_planes():
        ref = r.xz.at[pl.ds(0, LAST)]
        return remote(ref, ref, r.xz_send, r.xz_recv, here)

    def x_own():
        return pltpu.make_async_copy(r.xt.at[pl.ds(z * seqs, seqs)], r.xz.at[z], r.x_loc)

    def pos(xx):
        return pl.ds(pl.multiple_of(xx * tok_pair, tok_pair), tok_pair)

    def x_plane(oy, ox):
        yy, xx = turn(y, oy), turn(x, ox)
        return remote(r.xz.at[:, yy, :, pos(xx)], r.xp.at[c, y, x], r.xp_send.at[oy], r.xp_recv.at[(RING - oy) % RING], (z, yy, xx, c))

    def row_bytes(oy):
        return r.xp.at[c, 0] if oy else r.xp.at[c, 0, pl.ds(0, RING - 1)]

    def x_row(oy):
        yy = turn(y, oy)
        got = row_bytes(oy)
        remote(got, got, r.xp_send.at[oy], r.xp_recv.at[oy], partner).wait_recv()
        row = r.xp.at[c, yy]
        remote(row, row, r.xd_send, r.xd_recv, partner).start()

    def x_turn():
        got = r.xp.at[1 - c]
        remote(got, got, r.xd_send, r.xd_recv, partner).wait_recv()

        @pl.loop(0, RING)
        def _(zz):
            for yy in RINGS:
                for xh in BOTH:
                    blk = [r.xp[cc, yy, CORES * xh + xx, zz] for xx in BOTH for cc in BOTH]
                    blk = jnp.concatenate(blk, axis=0).astype(F32).T.astype(BF)
                    n = blk.shape[1]
                    at = pl.multiple_of(zz * RING * d_row + yy * d_row + xh * n, n)
                    r.hb[0, 0, :, :, pl.ds(at, n)] = blk.reshape(CORES, rows, n)
        r.hid[...] = r.hb[0, 0, c]
        remote(got, got, r.xd_send, r.xd_recv, partner).wait_send()

    def x_sent():
        three_planes().wait_send()
        for fn in (gain_z, gain_y, gain_x):
            peers_of(fn, "wait_send")
        for k in RINGS:
            gain_die(x, k).wait_send()
        for oy in RINGS:
            got = row_bytes(oy)
            remote(got, got, r.xp_send.at[oy], r.xp_recv.at[oy], partner).wait_send()

    def y_die(p):
        cols = pl.ds(pl.multiple_of(turn(z, p) * width, width), width)
        return remote(r.hid.at[:, cols], r.hb.at[0, 0, c, :, cols], r.yd_send.at[p], r.yd_recv.at[p], partner)

    def planes(h):
        return pl.ds(2 * h, 2)

    def y_plane(h, oy, ox):
        yy, xx = turn(y, oy), turn(x, ox)
        return remote(r.xp.at[c, yy, xx, planes(h)], r.xz.at[planes(h), y, :, pos(x)], r.yp_send.at[h, oy], r.yp_recv.at[h, (RING - oy) % RING],
                      (z, yy, xx, c))

    def y_z(p, oy):
        s = turn(y, oy)
        return remote(r.xz.at[p, s], r.y_out.at[z * seqs + s], r.yz_send.at[p], r.yz_recv.at[p], (turn(z, p), y, x, c))

    def y_own(oy):
        s = turn(y, oy)
        return pltpu.make_async_copy(r.xz.at[0, s], r.y_out.at[z * seqs + s], r.y_loc)

    def leave_a(h):
        for p in BOTH:
            p = 2 * h + p
            y_die(p).start()
            cols = pl.ds(pl.multiple_of(turn(z, p) * width, width), width)
            r.hb[0, 0, c, :, cols] = r.hid[:, cols]

    def leave_b(h):
        n = CORES * CORES * d_local
        for p in BOTH:
            p = 2 * h + p
            y_die(p).wait()

            @pl.loop(0, RING)
            def _(yy, p=p):
                for xh in BOTH:
                    at = pl.multiple_of(turn(z, p) * width + yy * d_row + xh * n, n)
                    blk = r.hb[0, 0, :, :, pl.ds(at, n)].reshape(tok_pair, n).astype(F32).T.astype(BF)
                    for xx in BOTH:
                        for cc in BOTH:
                            lo = (xx * CORES + cc) * d_local
                            r.xp[cc, yy, CORES * xh + xx, p] = blk[lo:lo + d_local]

        for oy in OTHERS + (0,):
            for ox in RINGS:
                if oy or ox:
                    y_plane(h, oy, ox).start()
        for p in BOTH:
            p = 2 * h + p
            r.xz[p, y, :, pos(x)] = r.xp[c, y, x, p]

    def plane_bytes(h, oy):
        return r.xp.at[c, 0, :, planes(h)] if oy else r.xp.at[c, 0, pl.ds(0, LAST), planes(h)]

    def leave_c(h):
        for oy in OTHERS + (0,):
            got = plane_bytes(h, oy)
            remote(got, got, r.yp_send.at[h, oy], r.yp_recv.at[h, oy], partner).wait_recv()
            for p in BOTH:
                p = 2 * h + p
                (y_z(p, oy) if p else y_own(oy)).start()

    def left():
        for oy in RINGS:
            for h in BOTH:
                got = plane_bytes(h, oy)
                remote(got, got, r.yp_send.at[h, oy], r.yp_recv.at[h, oy], partner).wait_send()
        for p in OTHERS:
            ref = r.xz.at[p]
            remote(ref, ref, r.yz_send.at[p], r.yz_recv.at[p], here).wait()
        pltpu.make_async_copy(r.xz.at[0], r.xz.at[0], r.y_loc).wait()

    def kv_rows(zz):
        n = CORES * seq_len // (RING * RING * RING * CORES)
        return pl.ds(pl.multiple_of(((zz * RING + y) * RING + x) * n, n), n)

    def kv_trade(l, k):
        zz = turn(z, OTHERS[k])
        return remote(r.kv_out.at[l, :, :, kv_rows(zz)], r.kvx.at[l, :, pl.ds(z * seqs, seqs)], r.kvx_send.at[l, k], r.kvx_recv.at[l, k], (zz, y, x, c))

    def kv_keep(l):
        return pltpu.make_async_copy(r.kv_out.at[l, :, :, kv_rows(z)], r.kvx.at[l, :, pl.ds(z * seqs, seqs)], r.kvx_loc.at[l])

    def kv_share(l):
        for k in range(len(OTHERS)):
            kv_trade(l, k).start()
        kv_keep(l).start()

    def kv_shared(l):
        for k in range(len(OTHERS)):
            kv_trade(l, k).wait()
        kv_keep(l).wait()

    def gather_norm(l, split, pump):
        hid = r.hid
        gain = r.gain[l:l + 1, :]
        for b in range(4):
            blk = hid[b * quarter:(b + 1) * quarter, :].astype(F32)
            mean = jnp.mean(blk, axis=-1, keepdims=True)
            cen = blk - mean
            var = jnp.mean(cen * cen, axis=-1, keepdims=True)
            r.h_ref[b * quarter:(b + 1) * quarter, :] = (cen * lax.rsqrt(var + LN_EPS) * gain).astype(BF)
        out = r.h_all.at[l]

        def spot(q, first, second):
            if q == 0:
                return turn(y, second), turn(x, first)
            return turn(y, first), turn(x, second)

        def span(q, part):
            lo, n = (split, rows - split) if q else (0, split)
            if part is NIL:
                return pl.ds(lo, n)
            return pl.ds(lo + part * (n // 2), n // 2)

        offs = (0, -1, 1, 2)
        plans = {}
        for q in BOTH:
            for d in BOTH:
                plans["first", q, d] = (q, 0, 0, NIL, SIGN[d], 0)
                plans["first_on", q, d] = (q, -SIGN[d], 0, d, SIGN[d], 0)
                for k in RINGS:
                    plans["second", q, k, d] = (q, offs[k], 0, NIL, 0, SIGN[d])
                    plans["second_on", q, k, d] = (q, offs[k], -SIGN[d], d, 0, SIGN[d])
        index = {key: n for n, key in enumerate(plans)}

        def link(*key, own=False):
            idx, (q, first, second, part, to_first, to_second) = index[key], plans[key]
            sy, sx = spot(q, first, second)
            ty, tx = spot(q, to_first, to_second)
            rws = span(q, part)
            dst = out.at[sy, sx, c, rws]
            return remote(r.h_ref.at[rws] if own else dst, dst, r.ag_send.at[KINDS.index(key[0])], r.ag_recv.at[idx], (z, ty, tx, c))

        def arrived(*key):
            for d in BOTH:
                link(*key, d).wait_recv()

        def die(q, first, second, own=False):
            sy, sx = spot(q, first, second)
            rws = span(q, NIL)
            dst = out.at[sy, sx, c, rws]
            off = (first if q else second) % RING
            remote(r.h_ref.at[rws] if own else dst, dst, r.ag_dsend, r.ag_drecv.at[off], partner).start()

        def take(k, q):
            for d in BOTH:
                link("second", q, k, d).wait_recv()
                die(q, offs[k], -SIGN[d])

        def pass_on(k, q):
            for d in BOTH:
                link("second_on", q, k, d).start()

        def second_step(k):
            take(k, 1)
            pass_on(k, 1)
            take(k, 0)

        def far_first(q):
            for e in BOTH:
                link("second", q, LAST, e).start()

        def last_step(q, k):
            arrived("second_on", q, k)
            die(q, offs[k], 2)

        def tail_a():
            second_step(2)
            far_first(1)
            for k in RINGS[:-1]:
                pass_on(k, 0)
            hook(pump, "k2")
            take(LAST, 0)
            pass_on(LAST, 0)
            hook(pump, "k3")
            for k in (1, 2):
                last_step(1, k)

        def tail_b():
            take(LAST, 1)
            pass_on(LAST, 1)

        def tail_c():
            for k in RINGS:
                last_step(0, k)
            last_step(1, LAST)

        for q in BOTH:
            for d in BOTH:
                link("first", q, d, own=True).start()
        for q in BOTH:
            for d in BOTH:
                link("second", q, 0, d, own=True).start()
        for q in BOTH:
            die(q, 0, 0, own=True)
        own = pltpu.make_async_copy(r.h_ref, out.at[y, x, c], r.ag_loc)
        own.start()
        hook(pump, "begin")
        for d in BOTH:
            for q in BOTH:
                link("first", q, d).wait_recv()
                src = -SIGN[d]
                link("first_on", q, d).start()
                die(q, src, 0)
        hook(pump, "first")
        second_step(0)
        for q in reversed(BOTH):
            for d in BOTH:
                for e in BOTH:
                    link("second", q, 1 + d, e).start()
        hook(pump, "k0")
        for q in BOTH:
            arrived("first_on", q)
            die(q, 2, 0)
        far_first(0)
        hook(pump, "first_on")
        last_step(1, 0)
        own.wait()
        hook(pump, "ready")

        def crossed(off):
            got = out.at[turn(y, off), :, 1 - c]
            remote(got, got, r.ag_dsend, r.ag_drecv.at[off], partner).wait_recv()

        def order(i):
            if isinstance(i, int):
                return (OWN, BEFORE, AFTER, FAR)[i]
            return lax.rem(3 * i + 3 * (i // 2) + 2 * (i // 3), RING)

        def fetch(i, slot):
            off = order(i)
            crossed(off)
            h_copy(l, turn(y, off), slot).start()

        def up_ready():
            hook(pump, "up")
            loaded(UP1 if l else UP0)

        crossed(0)
        h_copy(l, y, 0).start()

        def opening():
            second_step(1)
            hook(pump, "k1")

        def turn_of(i):
            slot = lax.rem(i, H_SLOTS)
            s = turn(y, order(i))
            h_copy(l, s, slot).wait()
            pump(("seq", i))
            one(l, s, slot, i)

            @pl.when(i == 1)
            def _():
                tail_b()

            @pl.when(i == 2)
            def _():
                tail_c()
                fetch(LAST, 0)

            return s, slot

        def neighbours():
            tail_a()
            for n in (1, 2):
                fetch(n, n)

        if l:
            @pl.loop(0, RING)
            def _(i):
                s, slot = turn_of(i)

                @pl.when(i == 0)
                def _():
                    opening()
                    up_ready()

                pump(("two", i))
                two(s, slot)

                @pl.when(i == 0)
                def _():
                    neighbours()
        else:
            h_copy(l, y, 0).wait()
            hook(pump, "own")
            one(l, y, 0, 0)
            opening()
            neighbours()

            @pl.loop(1, RING)
            def _(i):
                turn_of(i)

                @pl.when(i == 1)
                def _():
                    up_ready()

                pump(("two", i - 1))
                two(turn(y, order(i - 1)), lax.rem(i - 1, H_SLOTS))

            hook(pump, "two3")
            two(turn(y, FAR), 0)

        for slot in BOTH:
            for i in BOTH:
                kv_out_copy(l, 0, slot, i).wait()
        sent = (out.at[y, x], out.at[y], out.at[y, x, c], out.at[y, pl.ds(0, CORES)])
        for kind, ref in enumerate(sent):
            remote(ref, ref, r.ag_send.at[kind], r.ag_recv.at[kind], partner).wait_send()
        remote(out.at[pl.ds(0, 2)], out.at[pl.ds(0, 2)], r.ag_dsend, r.ag_drecv.at[0], partner).wait_send()

    def h_copy(l, s, slot):
        return pltpu.make_async_copy(r.h_all.at[l, s], r.hb.at[slot], r.h_sem.at[slot])

    def h_tile(slot):
        return r.hb[slot].reshape(seq_len, d_model)

    def project(h, lo, n):
        w = r.wv[:, :, lo:lo + n].reshape(d_model, n)
        return jnp.dot(h, w, preferred_element_type=F32).astype(BF)

    def rope(val):
        val = val.astype(F32)
        return val * r.cos[...] + pltpu.roll(val, head_dim // 2, 1) * r.sin[...]

    n_chunk = min(256, f_loc)

    def kv_out_copy(l, s, slot, i):
        return pltpu.make_async_copy(r.qkv.at[slot, i], r.kv_out.at[l, i, s], r.kvo_sem.at[slot, i])

    def one(l, s, slot, i):
        pair = i % 2 if isinstance(i, int) else lax.rem(i, 2)

        @pl.when(i >= 2)
        def _():
            for k in BOTH:
                kv_out_copy(l, s, pair, k).wait()

        kv = jnp.zeros((seq_len, 2 * head_dim), F32)
        for zz in RINGS:
            for yy in RINGS:
                col = (zz * RING + yy) * d_row
                kv += lax.dot_general(h_cols(slot, col, d_row), r.kvb[yy, zz], (((1,), (1,)), ((), ())), preferred_element_type=F32)
        kv = kv.astype(BF)
        r.qkv[pair, 0] = rope(kv[:, :head_dim]).astype(BF)
        r.qkv[pair, 1] = kv[:, head_dim:]
        for i in BOTH:
            kv_out_copy(l, s, pair, i).start()
        q = project(h_tile(slot), 0, head_dim)
        r.stage[...] = (rope(q) * head_dim ** -0.5).astype(BF)
        for lo in range(0, f_loc, n_chunk):
            r.joined[s, :, head_dim + lo:head_dim + lo + n_chunk] = project(h_tile(slot), head_dim + lo, n_chunk)
        n_tile = seq_len // 2
        for i in BOTH:
            keys = (i + 1) * n_tile
            sc = lax.dot_general(r.stage[i * n_tile:(i + 1) * n_tile, :], r.qkv[pair, 0, :keys, :], (((1,), (1,)), ((), ())), preferred_element_type=F32)
            row_id = lax.broadcasted_iota(jnp.int32, sc.shape, 0) + i * n_tile
            col_id = lax.broadcasted_iota(jnp.int32, sc.shape, 1)
            sc = jnp.where(col_id <= row_id, sc, -1e30)
            top = jnp.max(sc, axis=-1, keepdims=True)
            ex = jnp.exp(sc - top)
            prob = (ex * (1.0 / jnp.sum(ex, axis=-1, keepdims=True))).astype(BF)
            att = jnp.dot(prob, r.qkv[pair, 1, :keys, :], preferred_element_type=F32)
            r.joined[s, i * n_tile:(i + 1) * n_tile, :head_dim] = att.astype(BF)

    def h_cols(slot, col, n):
        return r.hb[slot, :, :, :, col:col + n].reshape(seq_len, n)

    def two(s, slot):
        for lo in range(0, f_loc, n_chunk):
            up = project(h_tile(slot), head_dim + f_loc + lo, n_chunk).astype(F32)
            cols = slice(head_dim + lo, head_dim + lo + n_chunk)
            g = r.joined[s, :, cols].astype(F32)
            r.joined[s, :, cols] = (g * jax.nn.sigmoid(g) * up).astype(BF)

    def out_scatter(l, pump):
        def peer(q, first, second):
            dy = first * (1 - q) + second * q
            dx = first * q + second * (1 - q)
            return (z, turn(y, dy), turn(x, dx), c)

        def die_copy(ch, q, s):
            return remote(r.away.at[q], r.die_in.at[ch, q, s], r.dsend.at[q], r.drecv.at[ch, q, s], partner)

        def first_copy(ch, q, d):
            return remote(r.acc.at[ch, q, 0, pl.ds(CORES * d, CORES)], r.in1.at[ch, q, d], r.rs_send.at[0], r.recv1.at[ch, q, d],
                          peer(q, SIGN[d], 0))

        def second_copy(ch, q, d, h):
            js = pl.ds(CORES * h, CORES)
            return remote(r.acc.at[ch, q, 1 + d, js], r.in2.at[ch, q, d, js], r.rs_send.at[1], r.recv2.at[ch, q],
                          peer(q, SIGN[d], 0))

        def half_rows(d):
            return pl.ds(d * (rows // 2), rows // 2)

        def third_copy(ch, q, d):
            return remote(r.acc.at[ch, q, LAST, 0, half_rows(d)], r.in3.at[ch, q, d], r.rs_send.at[2], r.recv3.at[ch, q, d],
                          peer(q, 0, SIGN[d]))

        def fourth_copy(ch, q, d):
            return remote(r.acc.at[ch, q, LAST, 1 + d], r.in4.at[ch, q, d], r.rs_send.at[LAST], r.recv4.at[ch, q],
                          peer(q, 0, SIGN[d]))

        n_blk = r.wov.shape[3]

        def plane_of(ch, q):
            if l:
                return turn(z, q if ch else 2 + q)
            return turn(z, LAST - q if ch else q)

        def slot_off(s):
            return lax.rem(2 + 3 * s + 3 * (s // 2) + 2 * (s // 3), RING)

        def tile(ch, q, s):
            off = slot_off(s)
            for cc in BOTH:
                for j in RINGS:
                    oy = off * (1 - q) + SLOT_OFF[j] * q
                    ox = SLOT_OFF[j] * (1 - q) + off * q
                    core = c if cc else 1 - c
                    at = pl.multiple_of((turn(x, ox) * CORES + core) * rows, rows)
                    r.lhs[pl.ds((cc * RING + j) * rows, rows), :] = r.joined[turn(y, oy), pl.ds(at, rows), :]
            left = r.lhs[...]
            zz = plane_of(ch, q)
            for n in RINGS:
                res = jnp.dot(left, r.wov[zz, n], preferred_element_type=F32).astype(BF)
                res = res.reshape(CORES, RING, rows, n_blk)
                r.away[q, :, :, n * n_blk:(n + 1) * n_blk] = res[0]
                r.acc[ch, q, s, :, :, n * n_blk:(n + 1) * n_blk] = res[1]

        def pair_sum(ch, q, s):
            die_copy(ch, q, s).wait_recv()

            @pl.loop(0, RING)
            def _(j):
                r.acc[ch, q, s, j] = r.acc[ch, q, s, j] + r.die_in[ch, q, s, j]

        def stage_a(ch):
            @pl.loop(0, CORES * RING)
            def _(t):
                s = t // CORES
                q = lax.rem(t, CORES)

                @pl.when(s >= 1)
                def _():
                    die_copy(ch, q, s - 1).wait_send()

                if ch:
                    @pl.when(s == 0)
                    def _():
                        die_copy(ch - 1, q, LAST).wait_send()

                tile(ch, q, s)
                die_copy(ch, q, s).start()

                @pl.when(s >= 1)
                def _():
                    pair_sum(ch, q, s - 1)

                @pl.when(s == 1)
                def _():
                    for d in BOTH:
                        first_copy(ch, q, d).start()

                for d in BOTH:
                    @pl.when(s == 2 + d)
                    def _(d=d):
                        second_copy(ch, q, d, 1 - d).start()

                for n in RINGS:
                    name = f"a{ch}s{n}"
                    if pump(name, False):
                        @pl.when(t == CORES * n + 1)
                        def _(name=name):
                            hook(pump, name)

        def stage_b(ch):
            for q in BOTH:
                pair_sum(ch, q, LAST)
            for q in BOTH:
                for d in BOTH:
                    first_copy(ch, q, d).wait_recv()
                    for j in BOTH:
                        at = CORES * d + j
                        r.acc[ch, q, 1 + d, at] = r.acc[ch, q, 1 + d, at] + r.in1[ch, q, d, j]
                    second_copy(ch, q, d, d).start()

        def total(ch, q, j):
            val = r.acc[ch, q, LAST, j].astype(F32)
            for d in BOTH:
                val += r.in2[ch, q, d, j].astype(F32)
            r.acc[ch, q, LAST, j] = val.astype(BF)

        def stage_c(ch):
            for q in BOTH:
                ref = r.in2.at[ch, q]
                remote(ref, ref, r.rs_send.at[1], r.recv2.at[ch, q], here).wait_recv()
                total(ch, q, 0)
                for d in BOTH:
                    third_copy(ch, q, d).start()
                for j in RINGS[1:]:
                    total(ch, q, j)

        def stage_d(ch):
            for q in BOTH:
                for d in BOTH:
                    third_copy(ch, q, d).wait_recv()
                    rws = half_rows(d)
                    r.acc[ch, q, LAST, 1 + d, rws] = r.acc[ch, q, LAST, 1 + d, rws] + r.in3[ch, q, d]
                    fourth_copy(ch, q, d).start()

        def stage_e(ch):
            for q in BOTH:
                ref = r.in4.at[ch, q]
                remote(ref, ref, r.rs_send.at[LAST], r.recv4.at[ch, q], here).wait_recv()
                cols = pl.ds(pl.multiple_of(plane_of(ch, q) * width, width), width)
                upd = r.acc[ch, q, LAST, LAST].astype(F32)
                for d in BOTH:
                    upd += r.in4[ch, q, d].astype(F32)
                upd = upd.astype(BF)
                r.hid[:, cols] = (r.hid[:, cols].astype(F32) + upd.astype(F32)).astype(BF)

        stages = {"a": stage_a, "b": stage_b, "c": stage_c, "d": stage_d, "e": stage_e, "f": leave_a, "g": leave_b, "h": leave_c}
        for step in LAST_ORDER if l else FIRST_ORDER:
            with jax.named_scope(step):
                stages[step[0]](int(step[1]))
            hook(pump, step)
        for q in BOTH:
            die_copy(1, q, LAST).wait_send()
        for n, ref in enumerate((r.in1, r.in2, r.in3, r.in4)):
            remote(ref, ref, r.rs_send.at[n], r.drecv.at[0, 0, 0], here).wait_send()

    def near(fn, t):
        for j in (LAST, 1):
            fn(t, j)

    def far(fn, t):
        fn(t, 2)

    def z_all(t):
        near(z_direct, t)
        far(z_direct, t)

    def peers_of(fn, op="start"):
        for k in range(len(OTHERS)):
            getattr(fn(k), op)()

    def start(pump):
        peers_of(gain_z)
        kv_z()
        peers_of(x_z)
        x_own().start()
        pump("s0")
        with jax.named_scope("gain_a"):
            peers_of(gain_z, "wait_recv")
            peers_of(gain_y)
            kv_y1()
        pump("s1")
        with jax.named_scope("gain_b"):
            peers_of(gain_y, "wait_recv")
            peers_of(gain_x)
            gain_die(x, LAST).start()
        pump("s2")
        with jax.named_scope("x_z"):
            three_planes().wait_recv()
            x_own().wait()
        for oy in RINGS:
            for ox in RINGS:
                if oy or ox:
                    x_plane(oy, ox).start()
        r.xp[c, y, x] = r.xz[:, y, :, pos(x)]
        pump("s3")
        with jax.named_scope("kv_b"):
            kv_y2()
        with jax.named_scope("gain_c"):
            for k, o in enumerate(OTHERS):
                gain_x(k).wait_recv()
                gain_die(turn(x, -o), k).start()
        pump("s4")
        for oy in (OWN, BEFORE, AFTER, FAR):
            with jax.named_scope(f"row_{oy}"):
                x_row(oy)
            pump(f"r{oy}")
        pump("s5")
        kv_y3()
        pump("s6")
        with jax.named_scope("gain_sum"):
            for k in RINGS:
                gain_die(x, k).wait_recv()
            gain_sum()
            for fill in fills[1:]:
                fill.wait()
        with jax.named_scope("turn"):
            x_turn()
        pump("s7")

    def when(i, n, *fns):
        @pl.when(i == n)
        def _():
            for fn in fns:
                fn()

    def plan(steps):
        def pump(step, run=True):
            if not isinstance(step, str):
                for n in RINGS:
                    if (step[0], n) in steps:
                        when(step[1], n, lambda n=n: run_steps(steps[step[0], n]))
                return True
            found = steps.get(step, ())
            if run:
                run_steps(found)
            return found
        return pump

    def run_steps(steps):
        for fn, *args in steps:
            with jax.named_scope(f"{fn.__name__}_{args[-1] if args else 0}"):
                fn(*args)

    first_entry = plan({
        "s0": [(z_own, UP0)],
        "s1": [(y_send, QG0)],
        "s3": [(z_own, QG0)],
        "r0": [(y_relay, QG0), (z_forward, UP0, OWN), (z_direct, QG0, AFTER), (z_forward, QG0, OWN), (z_direct, QG0, BEFORE)],
        "s6": [(kv_x1, 0)],
    })
    first_front = plan({
        "begin": [(kv_x2, 0), (y_send, UP0), (z_forward, QG0, AFTER), (z_direct, QG0, FAR)],
        "k0": [(y_relay, UP0), (kv_x3, 0), (z_forward, QG0, BEFORE), (z_forward, QG0, FAR), (z_direct, UP0, AFTER), (z_direct, UP0, BEFORE)],
        "first_on": [(y_send, WO0)],
        "ready": [(load_near, QG0), (load_far, QG0), (kv_load, 0), (loaded, QG0), (kv_loaded,)],
        "k1": [(z_direct, UP0, FAR), (z_forward, UP0, AFTER)],
        "k2": [
            (z_forward, UP0, BEFORE), (y_relay, WO0), (z_forward, UP0, FAR), (y_send, QG1), (z_own, WO0), (z_direct, WO0, BEFORE),
            (kv_x1, 1),
        ],
        ("seq", 1): [(y_send, WO1), (z_direct, WO0, AFTER), (x_sent,)],
        "up": [(y_send, UP1), (z_direct, WO0, FAR), (load_near, UP0), (load_far, UP0)],
        ("two", 0): [(y_relay, QG1), (z_forward, WO0, OWN)],
        ("seq", 2): [(kv_x2, 1)],
        ("two", 1): [(kv_x3, 1), (z_direct, QG1, AFTER), (z_forward, WO0, BEFORE)],
        ("seq", 3): [(y_relay, WO1), (z_forward, WO0, AFTER)],
        ("two", 2): [(z_forward, WO0, FAR), (z_own, QG1), (y_relay, UP1)],
        "near": [(load_near, WO0)],
    })
    first_scatter = plan({
        "a0s0": [(z_forward, QG1, AFTER)],
        "a0s2": [(z_direct, QG1, BEFORE)],
        "b0": [(load_far, WO0), (far_loaded, WO0)],
        "a1s0": [(z_direct, QG1, FAR)],
        "a1s1": [(z_forward, QG1, OWN)],
        "a1": [(z_direct, UP1, FAR)],
        "b1": [(z_direct, UP1, BEFORE)],
        "c1": [(z_forward, QG1, FAR), (z_direct, UP1, AFTER), (z_own, UP1), (z_forward, QG1, BEFORE)],
        "e0": [(z_forward, UP1, FAR)],
    })
    second_front = plan({
        "begin": [(z_forward, UP1, BEFORE), (kv_load, 1)],
        "first": [(z_forward, UP1, AFTER)],
        "k0": [(z_forward, UP1, OWN), (z_direct, WO1, FAR)],
        "ready": [(load_near, QG1), (load_far, QG1), (loaded, QG1), (kv_loaded,)],
        ("seq", 0): [(z_own, WO1)],
        "k1": [(z_direct, WO1, BEFORE)],
        "up": [(load_near, UP1), (load_far, UP1)],
        "k2": [(z_direct, WO1, AFTER)],
        ("seq", 1): [(z_forward, WO1, FAR)],
        ("two", 1): [(z_forward, WO1, OWN)],
        ("two", 2): [(z_forward, WO1, BEFORE), (z_forward, WO1, AFTER)],
        "near": [(load_near, WO1), (load_far, WO1)],
    })
    second_scatter = plan({
    })

    with jax.named_scope("start"):
        start(first_entry)
    with jax.named_scope("front_0"):
        gather_norm(0, rows // RING, first_front)
    with jax.named_scope("near_0"):
        kv_share(0)
        first_front("near")
        near_loaded(WO0)
    with jax.named_scope("scatter_0"):
        out_scatter(0, first_scatter)
    with jax.named_scope("front_1"):
        gather_norm(1, rows // 2, second_front)
    with jax.named_scope("near_1"):
        kv_share(1)
        second_front("near")
        loaded(WO1)
    with jax.named_scope("scatter_1"):
        out_scatter(1, second_scatter)
    with jax.named_scope("drain"):
        left()
        for t in range(WO1 + 1):
            drain(t)
        for l in range(n_layers):
            kv_shared(l)
            kv_sent(l)


def run_model(xt, gain, wkv_t, w_in, w_out, cos_full, sin_full):
    batch, d_local, seq_len = xt.shape
    n_layers, d_row, e_block = w_in.shape
    r_block, d_col = w_out.shape[1:]
    head_dim = cos_full.shape[1]
    d_model = d_row * RING * RING
    seqs = batch // RING
    rows = seqs * seq_len // (RING * RING * CORES)
    e_loc, r_loc = e_block // RING, r_block // RING
    kc = wkv_t.shape[1]
    width = d_model // RING
    n_t = 3 * n_layers
    n_o = len(OTHERS)

    def dma(*shape):
        return pltpu.SemaphoreType.DMA(shape)

    def vm(*shape):
        return pltpu.VMEM(shape, BF)

    def out(*shape):
        return jax.ShapeDtypeStruct(shape, BF)

    any_spec = pl.BlockSpec(memory_space=pl.ANY)
    out_shape = [
        out(batch, d_local, seq_len),
        out(n_layers, 2, seqs, seq_len, head_dim),
        out(n_layers, RING, RING, CORES, rows, d_model),
        out(n_layers, RING, RING * d_row, e_loc),
        out(n_layers, RING, RING, r_loc, d_col),
        out(RING, CORES, n_layers, RING, RING, kc, d_row),
        out(n_layers, 2, batch, CORES * (seq_len // (CORES * RING * RING * RING)), head_dim),
        out(n_layers, 2, d_row // 2, e_loc),
        out(n_layers, 2, r_loc // 2, d_col),
    ]
    pair = (2, 2, 2)
    scratch = [
        pltpu.VMEM(cos_full.shape, F32), pltpu.VMEM(cos_full.shape, F32), vm(n_layers, d_local),
        vm(rows, d_model), vm(rows, d_model), pltpu.VMEM((n_layers, d_model), F32),
        vm(RING, CORES, RING, RING, G_ROWS, d_row),
        vm(RING, seqs, d_local, seq_len),
        vm(CORES, RING, RING, RING, d_local, CORES * rows),
        vm(RING, RING * d_row, e_loc), vm(RING, RING, 2 * head_dim, d_row), vm(RING, RING, r_loc, d_col),
        vm(H_SLOTS, RING, CORES, rows, d_model), vm(RING, seq_len, r_loc), vm(2, 2, seq_len, head_dim), vm(seq_len, head_dim),
        vm(CORES * RING * rows, r_loc), vm(2, RING, rows, width), vm(2, 2, RING, RING, rows, width), vm(2, 2, RING, RING, rows, width),
        vm(*pair, 2, rows, width), vm(*pair, RING, rows, width), vm(*pair, rows // 2, width), vm(*pair, rows, width),
        pltpu.SemaphoreType.DMA, pltpu.SemaphoreType.DMA, dma(RING), dma(RING), pltpu.SemaphoreType.DMA, pltpu.SemaphoreType.DMA,
        pltpu.SemaphoreType.DMA,
        dma(3 * n_o), dma(3 * n_o), dma(RING), dma(RING),
        dma(RING), dma(RING), dma(2, RING), dma(2, RING), dma(RING), dma(RING), pltpu.SemaphoreType.DMA,
        dma(RING), dma(40), pltpu.SemaphoreType.DMA, dma(RING), pltpu.SemaphoreType.DMA, dma(H_SLOTS), dma(2, 2), dma(3), dma(3),
        dma(n_t, RING), dma(n_t, 2), dma(3, RING, 2), dma(3), dma(n_t),
        dma(n_o), dma(n_o), pltpu.SemaphoreType.DMA, dma(n_o), dma(n_layers), dma(n_layers, n_o), dma(n_layers), dma(n_layers), dma(2),
        dma(2), dma(2, 2, RING), dma(RING), dma(*pair), dma(2, 2), dma(*pair), dma(2, 2),
        dma(3), dma(n_layers, n_o), dma(n_layers, n_o), dma(n_layers),
    ]
    res = pl.pallas_call(
        model_kernel,
        out_shape=out_shape,
        in_specs=[any_spec] * 7,
        out_specs=[any_spec] * len(out_shape),
        scratch_shapes=scratch,
        compiler_params=pltpu.CompilerParams(collective_id=0, has_side_effects=True, vmem_limit_bytes=VMEM_LIMIT),
        name="two_layers",
    )(xt, gain, wkv_t, w_in, w_out, cos_full, sin_full)
    return res[0], res[6]


def solution(mesh):
    row_size = mesh.shape["row"]
    n_col = mesh.shape["col"]
    n_z = row_size // RING
    n_y = RING
    n_x = n_col // CORES
    n_tp = n_y * n_col
    n_dev = row_size * n_col
    mesh4 = Mesh(mesh.devices.reshape(n_z, n_y, n_x, CORES), ("z", "y", "x", "core"))
    every = ("z", "y", "x", "core")
    col = ("x", "core")
    act_spec = P(NIL, NIL, every)
    w_spec = P(NIL, ("z", "y"), col)

    def device_fn(x_loc, gain_loc, w_in_loc, w_kv_loc, w_out_loc):
        n_layers = w_in_loc.shape[0]
        n_batch, seq_len, d_local = x_loc.shape
        head_dim = w_kv_loc.shape[2] * n_col // 2
        batch_loc = n_batch // n_z
        seq_local = seq_len // n_dev
        steps = np.arange(head_dim // 2, dtype=np.float32)
        inv_freq = (1.0 / 10000.0 ** (steps * 2 / head_dim)).astype(np.float32)
        angles = np.arange(seq_len, dtype=np.float32)[:, NIL] * inv_freq[NIL, :]
        cos_tab, sin_tab = np.cos(angles), np.sin(angles)
        cos_full = jnp.asarray(np.concatenate([cos_tab, cos_tab], axis=1))
        sin_full = jnp.asarray(np.concatenate([-sin_tab, sin_tab], axis=1))
        y_loc, kv = run_model(x_loc.transpose(0, 2, 1), gain_loc, w_kv_loc.transpose(0, 2, 1), w_in_loc, w_out_loc, cos_full, sin_full)
        y_loc = y_loc.transpose(0, 2, 1)
        kv = kv.reshape(n_layers, 2, n_batch, CORES, seq_local, head_dim)
        kv = lax.dynamic_index_in_dim(kv, lax.axis_index("core"), axis=3, keepdims=False)
        return y_loc, kv

    return jax.shard_map(device_fn, mesh=mesh4, in_specs=(act_spec, P(NIL, every), w_spec, w_spec, P(NIL, col, ("z", "y"))), out_specs=(act_spec, P(NIL, NIL, NIL, every, NIL)), check_vma=False)
```

```python
import typing

import jax
import jax.numpy as jnp
import numpy as np
from jax import lax
from jax.experimental import pallas as pl
from jax.experimental.pallas import tpu as pltpu
from jax.sharding import Mesh
from jax.sharding import PartitionSpec as P

LN_EPS = 1e-6
RING = 4
CORES = 2
VMEM_LIMIT = 67_000_000
BF = jnp.bfloat16
F32 = jnp.float32
SLOT_OFF = (2, 1, 3, 0)
SIGN = (1, -1)
NIL = None
BOTH = range(CORES)
RINGS = range(RING)
OTHERS = (1, 3, 2)
LAST = RING - 1
G_ROWS = 8
H_SLOTS = 3
QG0, UP0, WO0, QG1, UP1, WO1 = range(6)
OWN, AFTER, FAR, BEFORE = RINGS
FIRST_ORDER = ("a0", "b0", "a1", "b1", "c0", "c1", "d0", "d1", "e0", "e1")
LAST_ORDER = FIRST_ORDER[:-1] + ("f1", "e1", "g1", "f0", "g0", "h1", "h0")
KINDS = ("first", "second", "first_on", "second_on")


class Refs(typing.NamedTuple):
    xt: typing.Any
    gain_in: typing.Any
    wkv: typing.Any
    w_in: typing.Any
    w_out: typing.Any
    cos_in: typing.Any
    sin_in: typing.Any
    y_out: typing.Any
    kv_out: typing.Any
    h_all: typing.Any
    wi: typing.Any
    wo: typing.Any
    kvh: typing.Any
    kvx: typing.Any
    rwi: typing.Any
    rwo: typing.Any
    cos: typing.Any
    sin: typing.Any
    gain_own: typing.Any
    h_ref: typing.Any
    hid: typing.Any
    gain: typing.Any
    gbuf: typing.Any
    xz: typing.Any
    xp: typing.Any
    wv: typing.Any
    kvb: typing.Any
    wov: typing.Any
    hb: typing.Any
    joined: typing.Any
    qkv: typing.Any
    stage: typing.Any
    lhs: typing.Any
    away: typing.Any
    acc: typing.Any
    die_in: typing.Any
    in1: typing.Any
    in2: typing.Any
    in3: typing.Any
    in4: typing.Any
    xz_send: typing.Any
    xz_recv: typing.Any
    xp_send: typing.Any
    xp_recv: typing.Any
    xd_send: typing.Any
    xd_recv: typing.Any
    x_loc: typing.Any
    g_send: typing.Any
    g_recv: typing.Any
    gd_send: typing.Any
    gd_recv: typing.Any
    yd_send: typing.Any
    yd_recv: typing.Any
    yp_send: typing.Any
    yp_recv: typing.Any
    yz_send: typing.Any
    yz_recv: typing.Any
    y_loc: typing.Any
    ag_send: typing.Any
    ag_recv: typing.Any
    ag_dsend: typing.Any
    ag_drecv: typing.Any
    ag_loc: typing.Any
    h_sem: typing.Any
    kvo_sem: typing.Any
    w_load: typing.Any
    far_load: typing.Any
    y_recv: typing.Any
    ry_recv: typing.Any
    zb_recv: typing.Any
    zc_recv: typing.Any
    w_send: typing.Any
    kz_send: typing.Any
    kz_recv: typing.Any
    ky_send: typing.Any
    ky_recv: typing.Any
    kx_send: typing.Any
    kx_recv: typing.Any
    kd_send: typing.Any
    kd_recv: typing.Any
    k_loc: typing.Any
    dsend: typing.Any
    drecv: typing.Any
    rs_send: typing.Any
    recv1: typing.Any
    recv2: typing.Any
    recv3: typing.Any
    recv4: typing.Any
    small: typing.Any
    kvx_send: typing.Any
    kvx_recv: typing.Any
    kvx_loc: typing.Any


def model_kernel(*refs):
    r = Refs(*refs)
    z, y, x, c = (lax.axis_index(a) for a in ("z", "y", "x", "core"))
    n_layers = r.wkv.shape[0]
    rows, d_model = r.hid.shape
    batch, d_local = r.xt.shape[:2]
    seqs = batch // RING
    seq_len, head_dim = r.cos.shape
    d_row = r.w_in.shape[1]
    e_loc = r.wi.shape[3]
    depth = r.wo.shape[3]
    f_loc = depth - head_dim
    quarter = rows // 4
    width = d_model // RING
    q_block = head_dim * RING
    f_block = f_loc * RING

    turned = {id(v): [lax.rem(v + o, RING) for o in RINGS] for v in (z, y, x)}

    def turn(base, off):
        if isinstance(off, int):
            return turned[id(base)][off % RING]
        return lax.rem(base + off + RING, RING)

    def remote(src, dst, ssem, rsem, dev):
        return pltpu.make_async_remote_copy(
            src_ref=src, dst_ref=dst, send_sem=ssem, recv_sem=rsem, device_id=dev, device_id_type=pl.DeviceIdType.MESH)

    partner = (z, y, x, 1 - c)

    peers = [(turn(z, o), y, x, c) for o in OTHERS]
    peers += [(z, turn(y, oy), turn(x, ox), c) for oy in RINGS for ox in RINGS if oy or ox]
    peers.append(partner)
    here = (z, y, x, c)
    gate_sem = pltpu.get_barrier_semaphore()
    for dev in peers:
        pl.semaphore_signal(gate_sem, inc=1, device_id=dev, device_id_type=pl.DeviceIdType.MESH)
    fills = [pltpu.make_async_copy(src, dst, r.small.at[n]) for n, (src, dst) in enumerate(
        ((r.gain_in, r.gain_own), (r.cos_in, r.cos), (r.sin_in, r.sin)))]
    for fill in fills:
        fill.start()
    fills[0].wait()

    src_id = lax.broadcasted_iota(jnp.int32, (d_local, d_row), 0) + (x * CORES + c) * d_local
    dst_id = lax.broadcasted_iota(jnp.int32, (d_local, d_row), 1)
    spread = jnp.where(src_id == dst_id, 1.0, 0.0).astype(BF)
    r.gbuf[x, c, y, z] = jnp.zeros((G_ROWS, d_row), BF)
    r.gbuf[x, c, y, z, :n_layers] = jnp.dot(r.gain_own[...], spread, preferred_element_type=F32).astype(BF)
    pl.semaphore_wait(gate_sem, len(peers))

    def hook(pump, i):
        with jax.named_scope(f"hook_{i}"):
            pump(i)

    def w_cols(kind):
        return pl.ds(0, head_dim + f_loc) if kind == 0 else pl.ds(head_dim + f_loc, f_loc)

    def piece(t, zz, yy):
        l, kind = t // 3, t % 3
        if kind == 2:
            return r.wo.at[l, zz, yy]
        return r.wi.at[l, zz, pl.ds(pl.multiple_of(yy * d_row, d_row), d_row), w_cols(kind)]

    def piece_half(t, zz, yy, h):
        l, kind = t // 3, t % 3
        if kind == 2:
            return r.wo.at[l, zz, yy, pl.ds(h * (depth // 2), depth // 2)]
        return r.wi.at[l, zz, pl.ds(pl.multiple_of(yy * d_row + h * (d_row // 2), d_row // 2), d_row // 2), w_cols(kind)]

    def own_parts(t, owner, zz, yy):
        l, kind = t // 3, t % 3
        hq = pl.ds(pl.multiple_of(owner * head_dim, head_dim), head_dim)
        if kind == 2:
            return [
                (r.w_out.at[l, hq], r.wo.at[l, zz, yy, pl.ds(0, head_dim)]),
                (r.w_out.at[l, pl.ds(pl.multiple_of(q_block + owner * f_loc, head_dim), f_loc)], r.wo.at[l, zz, yy, pl.ds(head_dim, f_loc)]),
            ]
        rws = pl.ds(pl.multiple_of(yy * d_row, d_row), d_row)
        if kind == 0:
            return [
                (r.w_in.at[l, :, hq], r.wi.at[l, zz, rws, pl.ds(0, head_dim)]),
                (r.w_in.at[l, :, pl.ds(pl.multiple_of(q_block + owner * f_loc, head_dim), f_loc)], r.wi.at[l, zz, rws, pl.ds(head_dim, f_loc)]),
            ]
        return [(r.w_in.at[l, :, pl.ds(pl.multiple_of(q_block + f_block + owner * f_loc, head_dim), f_loc)],
                 r.wi.at[l, zz, rws, pl.ds(head_dim + f_loc, f_loc)])]

    def relay_ref(t, d):
        l, kind = t // 3, t % 3
        return r.rwo.at[l, d] if kind == 2 else r.rwi.at[l, d, :, w_cols(kind)]

    def far_parts(t, d):
        l, kind = t // 3, t % 3
        owner = turn(y, 2)
        hq = pl.ds(pl.multiple_of(owner * head_dim, head_dim), head_dim)
        if kind == 2:
            n = depth // 2
            base = q_block + owner * f_loc
            if d:
                return [(r.w_out.at[l, pl.ds(pl.multiple_of(base + n - head_dim, G_ROWS), n)], r.rwo.at[l, d])]
            return [
                (r.w_out.at[l, hq], r.rwo.at[l, d, pl.ds(0, head_dim)]),
                (r.w_out.at[l, pl.ds(pl.multiple_of(base, head_dim), n - head_dim)], r.rwo.at[l, d, pl.ds(head_dim, n - head_dim)]),
            ]
        rws = pl.ds(d * (d_row // 2), d_row // 2)
        if kind == 0:
            return [
                (r.w_in.at[l, rws, hq], r.rwi.at[l, d, :, pl.ds(0, head_dim)]),
                (r.w_in.at[l, rws, pl.ds(pl.multiple_of(q_block + owner * f_loc, head_dim), f_loc)], r.rwi.at[l, d, :, pl.ds(head_dim, f_loc)]),
            ]
        return [(r.w_in.at[l, rws, pl.ds(pl.multiple_of(q_block + f_block + owner * f_loc, head_dim), f_loc)], relay_ref(t, d))]

    def y_send(t):
        for d in BOTH:
            owner = turn(y, SIGN[d])
            dev = (z, owner, x, c)
            for src, dst in far_parts(t, d):
                remote(src, dst, r.w_send.at[t], r.ry_recv.at[t, d], dev).start()
            for src, dst in own_parts(t, owner, z, y):
                remote(src, dst, r.w_send.at[t], r.y_recv.at[t, -SIGN[d] % RING], dev).start()

    def y_relay(t):
        for d in BOTH:
            ref = relay_ref(t, d)
            remote(ref, ref, r.w_send.at[t], r.ry_recv.at[t, d], here).wait_recv()
            dst = piece_half(t, z, turn(y, -SIGN[d]), d)
            remote(ref, dst, r.w_send.at[t], r.y_recv.at[t, 2], (z, turn(y, SIGN[d]), x, c)).start()

    def z_own(t):
        for d in BOTH:
            for src, dst in own_parts(t, y, z, y):
                remote(src, dst, r.w_send.at[t], r.zb_recv.at[t % 3, 0, d], (turn(z, SIGN[d]), y, x, c)).start()

    def z_direct(t, j):
        yy = turn(y, j)
        ref = piece(t, z, yy)
        remote(ref, ref, r.w_send.at[t], r.y_recv.at[t, j], here).wait_recv()
        for d in BOTH:
            remote(ref, ref, r.w_send.at[t], r.zb_recv.at[t % 3, j, d], (turn(z, SIGN[d]), y, x, c)).start()

    def z_forward(t, j):
        yy = turn(y, j)
        for d in BOTH:
            zz = turn(z, -SIGN[d])
            ref = piece(t, zz, yy)
            remote(ref, ref, r.w_send.at[t], r.zb_recv.at[t % 3, j, d], here).wait_recv()
            part = piece_half(t, zz, yy, d)
            remote(part, part, r.w_send.at[t], r.zc_recv.at[t % 3], (turn(z, SIGN[d]), y, x, c)).start()

    def place(t, zz):
        l, kind = t // 3, t % 3
        if kind == 2:
            return r.wo.at[l, zz], r.wov.at[zz]
        return r.wi.at[l, zz, :, w_cols(kind)], r.wv.at[zz, :, w_cols(kind)]

    def load_near(t):
        kind = t % 3
        for d in BOTH:
            src, dst = place(t, turn(z, SIGN[d]))
            pltpu.make_async_copy(src, dst, r.w_load.at[kind]).start()
        for j in OTHERS:
            yy = turn(y, j)
            dst = r.wov.at[z, yy] if kind == 2 else r.wv.at[z, pl.ds(pl.multiple_of(yy * d_row, d_row), d_row), w_cols(kind)]
            pltpu.make_async_copy(piece(t, z, yy), dst, r.w_load.at[kind]).start()
        for src, dst in own_parts(t, y, z, y):
            pltpu.make_async_copy(src, own_place(t, dst, src), r.w_load.at[kind]).start()

    def load_far(t):
        src, dst = place(t, turn(z, 2))
        remote(src, src, r.w_send.at[t], r.zc_recv.at[t % 3], here).wait_recv()
        pltpu.make_async_copy(src, dst, r.far_load.at[t % 3]).start()

    def own_place(t, dst, src):
        kind = t % 3
        if kind == 2:
            n = src.shape[0]
            return r.wov.at[z, y, pl.ds(0 if n == head_dim and f_loc != head_dim else head_dim, n)]
        n = src.shape[1]
        rws = pl.ds(pl.multiple_of(y * d_row, d_row), d_row)
        if kind == 0:
            return r.wv.at[z, rws, pl.ds(0 if n == head_dim and f_loc != head_dim else head_dim, n)]
        return r.wv.at[z, rws, pl.ds(head_dim + f_loc, f_loc)]

    def near_loaded(t):
        kind = t % 3
        dst = r.wov.at[pl.ds(0, LAST)] if kind == 2 else r.wv.at[pl.ds(0, LAST), :, w_cols(kind)]
        pltpu.make_async_copy(dst, dst, r.w_load.at[kind]).wait()

    def far_loaded(t):
        kind = t % 3
        dst = r.wov.at[0] if kind == 2 else r.wv.at[0, :, w_cols(kind)]
        pltpu.make_async_copy(dst, dst, r.far_load.at[kind]).wait()

    def loaded(t):
        near_loaded(t)
        far_loaded(t)

    def drain(t):
        l, kind = t // 3, t % 3
        ref = r.wo.at[l] if kind == 2 else r.wi.at[l, :, :, w_cols(kind)]
        remote(ref, ref, r.w_send.at[t], r.y_recv.at[t, 0], here).wait_send()

    def kv_z_copy(k):
        return remote(r.wkv, r.kvh.at[x, c, :, y, z], r.kz_send.at[k], r.kz_recv.at[k], (turn(z, OTHERS[k]), y, x, c))

    def kv_own():
        return pltpu.make_async_copy(r.wkv, r.kvh.at[x, c, :, y, z], r.k_loc.at[0])

    def kv_z():
        for k in range(len(OTHERS)):
            kv_z_copy(k).start()
        kv_own().start()

    def kv_y_copy(ref, k, d):
        return remote(ref, ref, r.ky_send, r.ky_recv.at[k], (z, turn(y, SIGN[d]), x, c))

    def kv_y1():
        kv_own().wait()
        for k in range(len(OTHERS)):
            kv_z_copy(k).wait()
        for d in BOTH:
            kv_y_copy(r.kvh.at[x, c, :, y], d, d).start()

    def kv_y2():
        for d in BOTH:
            yy = turn(y, -SIGN[d])
            kv_y_copy(r.kvh.at[x, c, :, yy], d, d).wait_recv()
            kv_y_copy(r.kvh.at[x, c, :, yy, pl.ds(2 * d, 2)], 2, d).start()

    def kv_y3():
        kv_y_copy(r.kvh.at[x, c, :, turn(y, 2)], 2, 0).wait_recv()
        kv_y_copy(r.kvh.at[x, c, :, pl.ds(0, LAST)], 0, 0).wait_send()

    def kv_x_copy(l, ref, k, d):
        return remote(ref, ref, r.kx_send.at[l], r.kx_recv.at[l, k], (z, y, turn(x, SIGN[d]), c))

    def kv_die(l, ref):
        return remote(ref, ref, r.kd_send.at[l], r.kd_recv.at[l], partner)

    def kv_x1(l):
        ref = r.kvh.at[x, c, l]
        for d in BOTH:
            kv_x_copy(l, ref, d, d).start()
        kv_die(l, ref).start()

    def kv_x2(l):
        for d in BOTH:
            xx = turn(x, -SIGN[d])
            ref = r.kvh.at[xx, c, l]
            kv_x_copy(l, ref, d, d).wait_recv()
            kv_x_copy(l, r.kvh.at[xx, c, l, pl.ds(2 * d, 2)], 2, d).start()
            kv_die(l, ref).start()

    def kv_x3(l):
        ref = r.kvh.at[turn(x, 2), c, l]
        kv_x_copy(l, ref, 2, 0).wait_recv()
        kv_die(l, ref).start()

    def kv_load(l):
        kv_die(l, r.kvh.at[:, 1 - c, l]).wait_recv()
        kc = r.wkv.shape[1]
        for xx in RINGS:
            for cc in BOTH:
                pltpu.make_async_copy(r.kvh.at[xx, cc, l], r.kvb.at[:, :, pl.ds((xx * CORES + cc) * kc, kc)], r.k_loc.at[1]).start()

    def kv_sent(l):
        kv_x_copy(l, r.kvh.at[pl.ds(0, LAST), c, l], 0, 0).wait_send()
        kv_die(l, r.kvh.at[:, c, l]).wait_send()

    def kv_loaded():
        pltpu.make_async_copy(r.kvb, r.kvb, r.k_loc.at[1]).wait()

    def gain_move(i, src, dst, dev):
        return remote(src, dst, r.g_send.at[i], r.g_recv.at[i], dev)

    def gain_z(k):
        dev = (turn(z, OTHERS[k]), y, x, c)
        return gain_move(k, r.gbuf.at[x, c, y, z], r.gbuf.at[x, c, y, z], dev)

    def gain_y(k):
        dev = (z, turn(y, OTHERS[k]), x, c)
        return gain_move(len(OTHERS) + k, r.gbuf.at[x, c, y], r.gbuf.at[x, c, y], dev)

    def gain_x(k):
        dev = (z, y, turn(x, OTHERS[k]), c)
        return gain_move(CORES * len(OTHERS) + k, r.gbuf.at[x, c], r.gbuf.at[x, c], dev)

    def gain_die(xx, k):
        ref = r.gbuf.at[xx, c]
        return remote(ref, ref, r.gd_send, r.gd_recv, partner)

    def gain_sum():
        for zz in RINGS:
            for yy in RINGS:
                tot = jnp.zeros((n_layers, d_row), F32)
                for xx in RINGS:
                    for cc in BOTH:
                        tot += r.gbuf[xx, cc, yy, zz, :n_layers].astype(F32)
                at = (zz * RING + yy) * d_row
                r.gain[:, at:at + d_row] = tot

    tok_pair = CORES * rows

    def x_z(k):
        zz = turn(z, OTHERS[k])
        src = r.xt.at[pl.ds(zz * seqs, seqs)]
        return remote(src, r.xz.at[z], r.xz_send, r.xz_recv, (zz, y, x, c))

    def three_planes():
        ref = r.xz.at[pl.ds(0, LAST)]
        return remote(ref, ref, r.xz_send, r.xz_recv, here)

    def x_own():
        return pltpu.make_async_copy(r.xt.at[pl.ds(z * seqs, seqs)], r.xz.at[z], r.x_loc)

    def pos(xx):
        return pl.ds(pl.multiple_of(xx * tok_pair, tok_pair), tok_pair)

    def x_plane(oy, ox):
        yy, xx = turn(y, oy), turn(x, ox)
        return remote(r.xz.at[:, yy, :, pos(xx)], r.xp.at[c, y, x], r.xp_send.at[oy], r.xp_recv.at[(RING - oy) % RING], (z, yy, xx, c))

    def row_bytes(oy):
        return r.xp.at[c, 0] if oy else r.xp.at[c, 0, pl.ds(0, RING - 1)]

    def x_row(oy):
        yy = turn(y, oy)
        got = row_bytes(oy)
        remote(got, got, r.xp_send.at[oy], r.xp_recv.at[oy], partner).wait_recv()
        row = r.xp.at[c, yy]
        remote(row, row, r.xd_send, r.xd_recv, partner).start()

    def x_turn():
        got = r.xp.at[1 - c]
        remote(got, got, r.xd_send, r.xd_recv, partner).wait_recv()

        @pl.loop(0, RING)
        def _(zz):
            for yy in RINGS:
                for xh in BOTH:
                    blk = [r.xp[cc, yy, CORES * xh + xx, zz] for xx in BOTH for cc in BOTH]
                    blk = jnp.concatenate(blk, axis=0).astype(F32).T.astype(BF)
                    n = blk.shape[1]
                    at = pl.multiple_of(zz * RING * d_row + yy * d_row + xh * n, n)
                    r.hb[0, 0, :, :, pl.ds(at, n)] = blk.reshape(CORES, rows, n)
        r.hid[...] = r.hb[0, 0, c]
        remote(got, got, r.xd_send, r.xd_recv, partner).wait_send()

    def x_sent():
        three_planes().wait_send()
        for fn in (gain_z, gain_y, gain_x):
            peers_of(fn, "wait_send")
        ref = r.gbuf.at[:, c]
        remote(ref, ref, r.gd_send, r.gd_recv, partner).wait_send()
        for oy in RINGS:
            got = row_bytes(oy)
            remote(got, got, r.xp_send.at[oy], r.xp_recv.at[oy], partner).wait_send()

    def y_die(p):
        cols = pl.ds(pl.multiple_of(turn(z, p) * width, width), width)
        return remote(r.hid.at[:, cols], r.hb.at[0, 0, c, :, cols], r.yd_send.at[p], r.yd_recv.at[p], partner)

    def planes(h):
        return pl.ds(2 * h, 2)

    def y_plane(h, oy, ox):
        yy, xx = turn(y, oy), turn(x, ox)
        return remote(r.xp.at[c, yy, xx, planes(h)], r.xz.at[planes(h), y, :, pos(x)], r.yp_send.at[h, oy], r.yp_recv.at[h, (RING - oy) % RING],
                      (z, yy, xx, c))

    def y_z(p, oy):
        s = turn(y, oy)
        return remote(r.xz.at[p, s], r.y_out.at[z * seqs + s], r.yz_send.at[p], r.yz_recv.at[p], (turn(z, p), y, x, c))

    def y_own(oy):
        s = turn(y, oy)
        return pltpu.make_async_copy(r.xz.at[0, s], r.y_out.at[z * seqs + s], r.y_loc)

    def leave_a(h):
        for p in BOTH:
            p = 2 * h + p
            y_die(p).start()
            cols = pl.ds(pl.multiple_of(turn(z, p) * width, width), width)
            r.hb[0, 0, c, :, cols] = r.hid[:, cols]

    def leave_b(h):
        n = CORES * CORES * d_local
        for p in BOTH:
            p = 2 * h + p
            y_die(p).wait()

            @pl.loop(0, RING)
            def _(yy, p=p):
                for xh in BOTH:
                    at = pl.multiple_of(turn(z, p) * width + yy * d_row + xh * n, n)
                    blk = r.hb[0, 0, :, :, pl.ds(at, n)].reshape(tok_pair, n).astype(F32).T.astype(BF)
                    for xx in BOTH:
                        for cc in BOTH:
                            lo = (xx * CORES + cc) * d_local
                            r.xp[cc, yy, CORES * xh + xx, p] = blk[lo:lo + d_local]

        for oy in OTHERS + (0,):
            for ox in RINGS:
                if oy or ox:
                    y_plane(h, oy, ox).start()
        for p in BOTH:
            p = 2 * h + p
            r.xz[p, y, :, pos(x)] = r.xp[c, y, x, p]

    def plane_bytes(h, oy):
        return r.xp.at[c, 0, :, planes(h)] if oy else r.xp.at[c, 0, pl.ds(0, LAST), planes(h)]

    def leave_c(h):
        for oy in OTHERS + (0,):
            got = plane_bytes(h, oy)
            remote(got, got, r.yp_send.at[h, oy], r.yp_recv.at[h, oy], partner).wait_recv()
            for p in BOTH:
                p = 2 * h + p
                (y_z(p, oy) if p else y_own(oy)).start()

    def left():
        for oy in RINGS:
            for h in BOTH:
                got = plane_bytes(h, oy)
                remote(got, got, r.yp_send.at[h, oy], r.yp_recv.at[h, oy], partner).wait_send()
        for p in OTHERS:
            ref = r.xz.at[p]
            remote(ref, ref, r.yz_send.at[p], r.yz_recv.at[p], here).wait()
        pltpu.make_async_copy(r.xz.at[0], r.xz.at[0], r.y_loc).wait()

    def kv_rows(zz):
        n = CORES * seq_len // (RING * RING * RING * CORES)
        return pl.ds(pl.multiple_of(((zz * RING + y) * RING + x) * n, n), n)

    def kv_trade(l, k):
        zz = turn(z, OTHERS[k])
        return remote(r.kv_out.at[l, :, :, kv_rows(zz)], r.kvx.at[l, z], r.kvx_send.at[l], r.kvx_recv.at[l], (zz, y, x, c))

    def kv_keep(l):
        return pltpu.make_async_copy(r.kv_out.at[l, :, :, kv_rows(z)], r.kvx.at[l, z], r.kvx_loc.at[l])

    def kv_share(l):
        for k in range(len(OTHERS)):
            kv_trade(l, k).start()
        kv_keep(l).start()

    def kv_shared(l):
        ref = r.kvx.at[l, pl.ds(0, LAST)]
        remote(ref, ref, r.kvx_send.at[l], r.kvx_recv.at[l], here).wait()
        kv_keep(l).wait()

    def gather_norm(l, split, pump):
        hid = r.hid
        gain = r.gain[l:l + 1, :]
        for b in range(4):
            blk = hid[b * quarter:(b + 1) * quarter, :].astype(F32)
            mean = jnp.mean(blk, axis=-1, keepdims=True)
            cen = blk - mean
            var = jnp.mean(cen * cen, axis=-1, keepdims=True)
            r.h_ref[b * quarter:(b + 1) * quarter, :] = (cen * lax.rsqrt(var + LN_EPS) * gain).astype(BF)
        out = r.h_all.at[l]

        def spot(q, first, second):
            if q == 0:
                return turn(y, second), turn(x, first)
            return turn(y, first), turn(x, second)

        def span(q, part):
            lo, n = (split, rows - split) if q else (0, split)
            if part is NIL:
                return pl.ds(lo, n)
            return pl.ds(lo + part * (n // 2), n // 2)

        offs = (0, -1, 1, 2)
        plans = {}
        for q in BOTH:
            for d in BOTH:
                plans["first", q, d] = (q, 0, 0, NIL, SIGN[d], 0)
                plans["first_on", q, d] = (q, -SIGN[d], 0, d, SIGN[d], 0)
                for k in RINGS:
                    plans["second", q, k, d] = (q, offs[k], 0, NIL, 0, SIGN[d])
                    plans["second_on", q, k, d] = (q, offs[k], -SIGN[d], d, 0, SIGN[d])
        index = {key: n for n, key in enumerate(plans)}

        def link(*key, own=False):
            idx, (q, first, second, part, to_first, to_second) = index[key], plans[key]
            sy, sx = spot(q, first, second)
            ty, tx = spot(q, to_first, to_second)
            rws = span(q, part)
            dst = out.at[sy, sx, c, rws]
            return remote(r.h_ref.at[rws] if own else dst, dst, r.ag_send.at[KINDS.index(key[0])], r.ag_recv.at[idx], (z, ty, tx, c))

        def arrived(*key):
            for d in BOTH:
                link(*key, d).wait_recv()

        def die(q, first, second, own=False):
            sy, sx = spot(q, first, second)
            rws = span(q, NIL)
            dst = out.at[sy, sx, c, rws]
            off = (first if q else second) % RING
            remote(r.h_ref.at[rws] if own else dst, dst, r.ag_dsend, r.ag_drecv.at[off], partner).start()

        def take(k, q):
            for d in BOTH:
                link("second", q, k, d).wait_recv()
                die(q, offs[k], -SIGN[d])

        def pass_on(k, q):
            for d in BOTH:
                link("second_on", q, k, d).start()

        def second_step(k):
            take(k, 1)
            pass_on(k, 1)
            take(k, 0)

        def far_first(q):
            for e in BOTH:
                link("second", q, LAST, e).start()

        def last_step(q, k):
            arrived("second_on", q, k)
            die(q, offs[k], 2)

        def tail_a():
            second_step(2)
            far_first(1)
            for k in RINGS[:-1]:
                pass_on(k, 0)
            hook(pump, "k2")
            take(LAST, 0)
            pass_on(LAST, 0)
            hook(pump, "k3")
            for k in (1, 2):
                last_step(1, k)

        def tail_b():
            take(LAST, 1)
            pass_on(LAST, 1)

        def tail_c():
            for k in RINGS:
                last_step(0, k)
            last_step(1, LAST)

        for q in BOTH:
            for d in BOTH:
                link("first", q, d, own=True).start()
        for q in BOTH:
            for d in BOTH:
                link("second", q, 0, d, own=True).start()
        for q in BOTH:
            die(q, 0, 0, own=True)
        own = pltpu.make_async_copy(r.h_ref, out.at[y, x, c], r.ag_loc)
        own.start()
        hook(pump, "begin")
        for d in BOTH:
            for q in BOTH:
                link("first", q, d).wait_recv()
                src = -SIGN[d]
                link("first_on", q, d).start()
                die(q, src, 0)
        hook(pump, "first")
        second_step(0)
        for q in reversed(BOTH):
            for d in BOTH:
                for e in BOTH:
                    link("second", q, 1 + d, e).start()
        hook(pump, "k0")
        for q in BOTH:
            arrived("first_on", q)
            die(q, 2, 0)
        far_first(0)
        hook(pump, "first_on")
        last_step(1, 0)
        own.wait()
        hook(pump, "ready")

        def crossed(off):
            got = out.at[turn(y, off), :, 1 - c]
            remote(got, got, r.ag_dsend, r.ag_drecv.at[off], partner).wait_recv()

        def order(i):
            if isinstance(i, int):
                return (OWN, BEFORE, AFTER, FAR)[i]
            return lax.rem(3 * i + 3 * (i // 2) + 2 * (i // 3), RING)

        def fetch(i, slot):
            off = order(i)
            crossed(off)
            h_copy(l, turn(y, off), slot).start()

        def up_ready():
            hook(pump, "up")
            loaded(UP1 if l else UP0)

        crossed(0)
        h_copy(l, y, 0).start()

        def opening():
            second_step(1)
            hook(pump, "k1")

        def turn_of(i):
            slot = lax.rem(i, H_SLOTS)
            s = turn(y, order(i))
            h_copy(l, s, slot).wait()
            pump(("seq", i))
            one(l, s, slot, i)

            @pl.when(i == 1)
            def _():
                tail_b()

            @pl.when(i == 2)
            def _():
                tail_c()
                fetch(LAST, 0)

            return s, slot

        def neighbours():
            tail_a()
            for n in (1, 2):
                fetch(n, n)

        if l:
            @pl.loop(0, RING)
            def _(i):
                s, slot = turn_of(i)

                @pl.when(i == 0)
                def _():
                    opening()
                    up_ready()

                pump(("two", i))
                two(s, slot)

                @pl.when(i == 0)
                def _():
                    neighbours()
        else:
            h_copy(l, y, 0).wait()
            hook(pump, "own")
            one(l, y, 0, 0)
            opening()
            neighbours()

            @pl.loop(1, RING)
            def _(i):
                turn_of(i)

                @pl.when(i == 1)
                def _():
                    up_ready()

                pump(("two", i - 1))
                two(turn(y, order(i - 1)), lax.rem(i - 1, H_SLOTS))

            hook(pump, "two3")
            two(turn(y, FAR), 0)

        for slot in BOTH:
            for i in BOTH:
                kv_out_copy(l, 0, slot, i).wait()
        sent = (out.at[y, x], out.at[y], out.at[y, x, c], out.at[y, pl.ds(0, CORES)])
        for kind, ref in enumerate(sent):
            remote(ref, ref, r.ag_send.at[kind], r.ag_recv.at[kind], partner).wait_send()
        remote(out.at[pl.ds(0, 2)], out.at[pl.ds(0, 2)], r.ag_dsend, r.ag_drecv.at[0], partner).wait_send()

    def h_copy(l, s, slot):
        return pltpu.make_async_copy(r.h_all.at[l, s], r.hb.at[slot], r.h_sem.at[slot])

    def h_tile(slot):
        return r.hb[slot].reshape(seq_len, d_model)

    def project(h, lo, n):
        w = r.wv[:, :, lo:lo + n].reshape(d_model, n)
        return jnp.dot(h, w, preferred_element_type=F32).astype(BF)

    def rope(val):
        val = val.astype(F32)
        return val * r.cos[...] + pltpu.roll(val, head_dim // 2, 1) * r.sin[...]

    n_chunk = min(256, f_loc)

    def kv_out_copy(l, s, slot, i):
        return pltpu.make_async_copy(r.qkv.at[slot, i], r.kv_out.at[l, i, s], r.kvo_sem.at[slot, i])

    def one(l, s, slot, i):
        pair = i % 2 if isinstance(i, int) else lax.rem(i, 2)

        @pl.when(i >= 2)
        def _():
            for k in BOTH:
                kv_out_copy(l, s, pair, k).wait()

        kv = jnp.zeros((seq_len, 2 * head_dim), F32)
        for zz in RINGS:
            for yy in RINGS:
                col = (zz * RING + yy) * d_row
                kv += lax.dot_general(h_cols(slot, col, d_row), r.kvb[yy, zz], (((1,), (1,)), ((), ())), preferred_element_type=F32)
        kv = kv.astype(BF)
        r.qkv[pair, 0] = rope(kv[:, :head_dim]).astype(BF)
        r.qkv[pair, 1] = kv[:, head_dim:]
        for i in BOTH:
            kv_out_copy(l, s, pair, i).start()
        q = project(h_tile(slot), 0, head_dim)
        r.stage[...] = (rope(q) * head_dim ** -0.5).astype(BF)
        for lo in range(0, f_loc, n_chunk):
            r.joined[s, :, head_dim + lo:head_dim + lo + n_chunk] = project(h_tile(slot), head_dim + lo, n_chunk)
        n_tile = seq_len // 2
        for i in BOTH:
            keys = (i + 1) * n_tile
            sc = lax.dot_general(r.stage[i * n_tile:(i + 1) * n_tile, :], r.qkv[pair, 0, :keys, :], (((1,), (1,)), ((), ())), preferred_element_type=F32)
            row_id = lax.broadcasted_iota(jnp.int32, sc.shape, 0) + i * n_tile
            col_id = lax.broadcasted_iota(jnp.int32, sc.shape, 1)
            sc = jnp.where(col_id <= row_id, sc, -1e30)
            top = jnp.max(sc, axis=-1, keepdims=True)
            ex = jnp.exp(sc - top)
            prob = (ex * (1.0 / jnp.sum(ex, axis=-1, keepdims=True))).astype(BF)
            att = jnp.dot(prob, r.qkv[pair, 1, :keys, :], preferred_element_type=F32)
            r.joined[s, i * n_tile:(i + 1) * n_tile, :head_dim] = att.astype(BF)

    def h_cols(slot, col, n):
        return r.hb[slot, :, :, :, col:col + n].reshape(seq_len, n)

    def two(s, slot):
        for lo in range(0, f_loc, n_chunk):
            up = project(h_tile(slot), head_dim + f_loc + lo, n_chunk).astype(F32)
            cols = slice(head_dim + lo, head_dim + lo + n_chunk)
            g = r.joined[s, :, cols].astype(F32)
            r.joined[s, :, cols] = (g * jax.nn.sigmoid(g) * up).astype(BF)

    def out_scatter(l, pump):
        def peer(q, first, second):
            dy = first * (1 - q) + second * q
            dx = first * q + second * (1 - q)
            return (z, turn(y, dy), turn(x, dx), c)

        def die_copy(ch, q, s):
            return remote(r.away.at[q], r.die_in.at[ch, q, s], r.dsend.at[q], r.drecv.at[ch, q, s], partner)

        def first_copy(ch, q, d):
            return remote(r.acc.at[ch, q, 0, pl.ds(CORES * d, CORES)], r.in1.at[ch, q, d], r.rs_send.at[0], r.recv1.at[ch, q, d],
                          peer(q, SIGN[d], 0))

        def second_copy(ch, q, d, h):
            js = pl.ds(CORES * h, CORES)
            return remote(r.acc.at[ch, q, 1 + d, js], r.in2.at[ch, q, d, js], r.rs_send.at[1], r.recv2.at[ch, q],
                          peer(q, SIGN[d], 0))

        def half_rows(d):
            return pl.ds(d * (rows // 2), rows // 2)

        def third_copy(ch, q, d):
            return remote(r.acc.at[ch, q, LAST, 0, half_rows(d)], r.in3.at[ch, q, d], r.rs_send.at[2], r.recv3.at[ch, q, d],
                          peer(q, 0, SIGN[d]))

        def fourth_copy(ch, q, d):
            return remote(r.acc.at[ch, q, LAST, 1 + d], r.in4.at[ch, q, d], r.rs_send.at[LAST], r.recv4.at[ch, q],
                          peer(q, 0, SIGN[d]))

        n_blk = r.wov.shape[3]

        def plane_of(ch, q):
            if l:
                return turn(z, q if ch else 2 + q)
            return turn(z, LAST - q if ch else q)

        def slot_off(s):
            return lax.rem(2 + 3 * s + 3 * (s // 2) + 2 * (s // 3), RING)

        def tile(ch, q, s):
            off = slot_off(s)
            for cc in BOTH:
                for j in RINGS:
                    oy = off * (1 - q) + SLOT_OFF[j] * q
                    ox = SLOT_OFF[j] * (1 - q) + off * q
                    core = c if cc else 1 - c
                    at = pl.multiple_of((turn(x, ox) * CORES + core) * rows, rows)
                    r.lhs[pl.ds((cc * RING + j) * rows, rows), :] = r.joined[turn(y, oy), pl.ds(at, rows), :]
            left = r.lhs[...]
            zz = plane_of(ch, q)
            for n in RINGS:
                res = jnp.dot(left, r.wov[zz, n], preferred_element_type=F32).astype(BF)
                res = res.reshape(CORES, RING, rows, n_blk)
                r.away[q, :, :, n * n_blk:(n + 1) * n_blk] = res[0]
                r.acc[ch, q, s, :, :, n * n_blk:(n + 1) * n_blk] = res[1]

        def pair_sum(ch, q, s):
            die_copy(ch, q, s).wait_recv()

            @pl.loop(0, RING)
            def _(j):
                r.acc[ch, q, s, j] = r.acc[ch, q, s, j] + r.die_in[ch, q, s, j]

        def stage_a(ch):
            @pl.loop(0, CORES * RING)
            def _(t):
                s = t // CORES
                q = lax.rem(t, CORES)

                @pl.when(s >= 1)
                def _():
                    die_copy(ch, q, s - 1).wait_send()

                if ch:
                    @pl.when(s == 0)
                    def _():
                        die_copy(ch - 1, q, LAST).wait_send()

                tile(ch, q, s)
                die_copy(ch, q, s).start()

                @pl.when(s >= 1)
                def _():
                    pair_sum(ch, q, s - 1)

                @pl.when(s == 1)
                def _():
                    for d in BOTH:
                        first_copy(ch, q, d).start()

                for d in BOTH:
                    @pl.when(s == 2 + d)
                    def _(d=d):
                        second_copy(ch, q, d, 1 - d).start()

                for n in RINGS:
                    name = f"a{ch}s{n}"
                    if pump(name, False):
                        @pl.when(t == CORES * n + 1)
                        def _(name=name):
                            hook(pump, name)

        def stage_b(ch):
            for q in BOTH:
                pair_sum(ch, q, LAST)
            for q in BOTH:
                for d in BOTH:
                    first_copy(ch, q, d).wait_recv()
                    for j in BOTH:
                        at = CORES * d + j
                        r.acc[ch, q, 1 + d, at] = r.acc[ch, q, 1 + d, at] + r.in1[ch, q, d, j]
                    second_copy(ch, q, d, d).start()

        def total(ch, q, j):
            val = r.acc[ch, q, LAST, j].astype(F32)
            for d in BOTH:
                val += r.in2[ch, q, d, j].astype(F32)
            r.acc[ch, q, LAST, j] = val.astype(BF)

        def stage_c(ch):
            for q in BOTH:
                ref = r.in2.at[ch, q]
                remote(ref, ref, r.rs_send.at[1], r.recv2.at[ch, q], here).wait_recv()
                total(ch, q, 0)
                for d in BOTH:
                    third_copy(ch, q, d).start()
                for j in RINGS[1:]:
                    total(ch, q, j)

        def stage_d(ch):
            for q in BOTH:
                for d in BOTH:
                    third_copy(ch, q, d).wait_recv()
                    rws = half_rows(d)
                    r.acc[ch, q, LAST, 1 + d, rws] = r.acc[ch, q, LAST, 1 + d, rws] + r.in3[ch, q, d]
                    fourth_copy(ch, q, d).start()

        def stage_e(ch):
            for q in BOTH:
                ref = r.in4.at[ch, q]
                remote(ref, ref, r.rs_send.at[LAST], r.recv4.at[ch, q], here).wait_recv()
                cols = pl.ds(pl.multiple_of(plane_of(ch, q) * width, width), width)
                upd = r.acc[ch, q, LAST, LAST].astype(F32)
                for d in BOTH:
                    upd += r.in4[ch, q, d].astype(F32)
                upd = upd.astype(BF)
                r.hid[:, cols] = (r.hid[:, cols].astype(F32) + upd.astype(F32)).astype(BF)

        stages = {"a": stage_a, "b": stage_b, "c": stage_c, "d": stage_d, "e": stage_e, "f": leave_a, "g": leave_b, "h": leave_c}
        for step in LAST_ORDER if l else FIRST_ORDER:
            with jax.named_scope(step):
                stages[step[0]](int(step[1]))
            hook(pump, step)
        for q in BOTH:
            die_copy(1, q, LAST).wait_send()
        for n, ref in enumerate((r.in1, r.in2, r.in3, r.in4)):
            remote(ref, ref, r.rs_send.at[n], r.drecv.at[0, 0, 0], here).wait_send()

    def near(fn, t):
        for j in (LAST, 1):
            fn(t, j)

    def far(fn, t):
        fn(t, 2)

    def z_all(t):
        near(z_direct, t)
        far(z_direct, t)

    def peers_of(fn, op="start"):
        for k in range(len(OTHERS)):
            getattr(fn(k), op)()

    def start(pump):
        peers_of(gain_z)
        kv_z()
        peers_of(x_z)
        x_own().start()
        pump("s0")
        with jax.named_scope("gain_a"):
            peers_of(gain_z, "wait_recv")
            peers_of(gain_y)
            kv_y1()
        pump("s1")
        with jax.named_scope("gain_b"):
            peers_of(gain_y, "wait_recv")
            peers_of(gain_x)
            gain_die(x, LAST).start()
        pump("s2")
        with jax.named_scope("x_z"):
            three_planes().wait_recv()
            x_own().wait()
        for oy in RINGS:
            for ox in RINGS:
                if oy or ox:
                    x_plane(oy, ox).start()
        r.xp[c, y, x] = r.xz[:, y, :, pos(x)]
        pump("s3")
        with jax.named_scope("kv_b"):
            kv_y2()
        with jax.named_scope("gain_c"):
            for k, o in enumerate(OTHERS):
                gain_x(k).wait_recv()
                gain_die(turn(x, -o), k).start()
        pump("s4")
        for oy in (OWN, BEFORE, AFTER, FAR):
            with jax.named_scope(f"row_{oy}"):
                x_row(oy)
            pump(f"r{oy}")
        pump("s5")
        kv_y3()
        pump("s6")
        with jax.named_scope("gain_sum"):
            ref = r.gbuf.at[:, 1 - c]
            remote(ref, ref, r.gd_send, r.gd_recv, partner).wait_recv()
            gain_sum()
            for fill in fills[1:]:
                fill.wait()
        with jax.named_scope("turn"):
            x_turn()
        pump("s7")

    def when(i, n, *fns):
        @pl.when(i == n)
        def _():
            for fn in fns:
                fn()

    def plan(steps):
        def pump(step, run=True):
            if not isinstance(step, str):
                for n in RINGS:
                    if (step[0], n) in steps:
                        when(step[1], n, lambda n=n: run_steps(steps[step[0], n]))
                return True
            found = steps.get(step, ())
            if run:
                run_steps(found)
            return found
        return pump

    def run_steps(steps):
        for fn, *args in steps:
            with jax.named_scope(f"{fn.__name__}_{args[-1] if args else 0}"):
                fn(*args)

    first_entry = plan({
        "s0": [(z_own, UP0)],
        "s1": [(y_send, QG0)],
        "s3": [(z_own, QG0)],
        "r0": [(y_relay, QG0), (z_forward, UP0, OWN), (z_direct, QG0, AFTER), (z_forward, QG0, OWN), (z_direct, QG0, BEFORE)],
        "s6": [(kv_x1, 0)],
    })
    first_front = plan({
        "begin": [(kv_x2, 0), (y_send, UP0), (z_forward, QG0, AFTER), (z_direct, QG0, FAR)],
        "k0": [(y_relay, UP0), (kv_x3, 0), (z_forward, QG0, BEFORE), (z_forward, QG0, FAR), (z_direct, UP0, AFTER), (z_direct, UP0, BEFORE)],
        "first_on": [(y_send, WO0)],
        "ready": [(load_near, QG0), (load_far, QG0), (kv_load, 0), (loaded, QG0), (kv_loaded,)],
        "k1": [(z_direct, UP0, FAR), (z_forward, UP0, AFTER)],
        "k2": [
            (z_forward, UP0, BEFORE), (y_relay, WO0), (z_forward, UP0, FAR), (y_send, QG1), (z_own, WO0), (z_direct, WO0, BEFORE),
            (kv_x1, 1),
        ],
        ("seq", 1): [(y_send, WO1), (z_direct, WO0, AFTER), (x_sent,)],
        "up": [(y_send, UP1), (z_direct, WO0, FAR), (load_near, UP0), (load_far, UP0)],
        ("two", 0): [(y_relay, QG1), (z_forward, WO0, OWN)],
        ("seq", 2): [(kv_x2, 1)],
        ("two", 1): [(kv_x3, 1), (z_direct, QG1, AFTER), (z_forward, WO0, BEFORE)],
        ("seq", 3): [(y_relay, WO1), (z_forward, WO0, AFTER)],
        ("two", 2): [(z_forward, WO0, FAR), (z_own, QG1), (y_relay, UP1)],
        "near": [(load_near, WO0)],
    })
    first_scatter = plan({
        "a0s0": [(z_forward, QG1, AFTER)],
        "a0s2": [(z_direct, QG1, BEFORE)],
        "b0": [(load_far, WO0), (far_loaded, WO0)],
        "a1s0": [(z_direct, QG1, FAR)],
        "a1s1": [(z_forward, QG1, OWN)],
        "a1": [(z_direct, UP1, FAR)],
        "b1": [(z_direct, UP1, BEFORE)],
        "c1": [(z_forward, QG1, FAR), (z_direct, UP1, AFTER), (z_own, UP1), (z_forward, QG1, BEFORE)],
        "e0": [(z_forward, UP1, FAR)],
    })
    second_front = plan({
        "begin": [(z_forward, UP1, BEFORE), (kv_load, 1)],
        "first": [(z_forward, UP1, AFTER)],
        "k0": [(z_forward, UP1, OWN), (z_direct, WO1, FAR)],
        "ready": [(load_near, QG1), (load_far, QG1), (loaded, QG1), (kv_loaded,)],
        ("seq", 0): [(z_own, WO1)],
        "k1": [(z_direct, WO1, BEFORE)],
        "up": [(load_near, UP1), (load_far, UP1)],
        "k2": [(z_direct, WO1, AFTER)],
        ("seq", 1): [(z_forward, WO1, FAR)],
        ("two", 1): [(z_forward, WO1, OWN)],
        ("two", 2): [(z_forward, WO1, BEFORE), (z_forward, WO1, AFTER)],
        "near": [(load_near, WO1), (load_far, WO1)],
    })
    second_scatter = plan({
    })

    with jax.named_scope("start"):
        start(first_entry)
    with jax.named_scope("front_0"):
        gather_norm(0, rows // RING, first_front)
    with jax.named_scope("near_0"):
        kv_share(0)
        first_front("near")
        near_loaded(WO0)
    with jax.named_scope("scatter_0"):
        out_scatter(0, first_scatter)
    with jax.named_scope("front_1"):
        gather_norm(1, rows // 2, second_front)
    with jax.named_scope("near_1"):
        kv_share(1)
        second_front("near")
        loaded(WO1)
    with jax.named_scope("scatter_1"):
        out_scatter(1, second_scatter)
    with jax.named_scope("drain"):
        left()
        for t in range(WO1 + 1):
            drain(t)
        for l in range(n_layers):
            kv_shared(l)
            kv_sent(l)


def run_model(xt, gain, wkv_t, w_in, w_out, cos_full, sin_full):
    batch, d_local, seq_len = xt.shape
    n_layers, d_row, e_block = w_in.shape
    r_block, d_col = w_out.shape[1:]
    head_dim = cos_full.shape[1]
    d_model = d_row * RING * RING
    seqs = batch // RING
    rows = seqs * seq_len // (RING * RING * CORES)
    e_loc, r_loc = e_block // RING, r_block // RING
    kc = wkv_t.shape[1]
    width = d_model // RING
    n_t = 3 * n_layers
    n_o = len(OTHERS)

    def dma(*shape):
        return pltpu.SemaphoreType.DMA(shape)

    def vm(*shape):
        return pltpu.VMEM(shape, BF)

    def out(*shape):
        return jax.ShapeDtypeStruct(shape, BF)

    any_spec = pl.BlockSpec(memory_space=pl.ANY)
    out_shape = [
        out(batch, d_local, seq_len),
        out(n_layers, 2, seqs, seq_len, head_dim),
        out(n_layers, RING, RING, CORES, rows, d_model),
        out(n_layers, RING, RING * d_row, e_loc),
        out(n_layers, RING, RING, r_loc, d_col),
        out(RING, CORES, n_layers, RING, RING, kc, d_row),
        out(n_layers, RING, 2, seqs, CORES * (seq_len // (CORES * RING * RING * RING)), head_dim),
        out(n_layers, 2, d_row // 2, e_loc),
        out(n_layers, 2, r_loc // 2, d_col),
    ]
    pair = (2, 2, 2)
    scratch = [
        pltpu.VMEM(cos_full.shape, F32), pltpu.VMEM(cos_full.shape, F32), vm(n_layers, d_local),
        vm(rows, d_model), vm(rows, d_model), pltpu.VMEM((n_layers, d_model), F32),
        vm(RING, CORES, RING, RING, G_ROWS, d_row),
        vm(RING, seqs, d_local, seq_len),
        vm(CORES, RING, RING, RING, d_local, CORES * rows),
        vm(RING, RING * d_row, e_loc), vm(RING, RING, 2 * head_dim, d_row), vm(RING, RING, r_loc, d_col),
        vm(H_SLOTS, RING, CORES, rows, d_model), vm(RING, seq_len, r_loc), vm(2, 2, seq_len, head_dim), vm(seq_len, head_dim),
        vm(CORES * RING * rows, r_loc), vm(2, RING, rows, width), vm(2, 2, RING, RING, rows, width), vm(2, 2, RING, RING, rows, width),
        vm(*pair, 2, rows, width), vm(*pair, RING, rows, width), vm(*pair, rows // 2, width), vm(*pair, rows, width),
        pltpu.SemaphoreType.DMA, pltpu.SemaphoreType.DMA, dma(RING), dma(RING), pltpu.SemaphoreType.DMA, pltpu.SemaphoreType.DMA,
        pltpu.SemaphoreType.DMA,
        dma(3 * n_o), dma(3 * n_o), pltpu.SemaphoreType.DMA, pltpu.SemaphoreType.DMA,
        dma(RING), dma(RING), dma(2, RING), dma(2, RING), dma(RING), dma(RING), pltpu.SemaphoreType.DMA,
        dma(RING), dma(40), pltpu.SemaphoreType.DMA, dma(RING), pltpu.SemaphoreType.DMA, dma(H_SLOTS), dma(2, 2), dma(3), dma(3),
        dma(n_t, RING), dma(n_t, 2), dma(3, RING, 2), dma(3), dma(n_t),
        dma(n_o), dma(n_o), pltpu.SemaphoreType.DMA, dma(n_o), dma(n_layers), dma(n_layers, n_o), dma(n_layers), dma(n_layers), dma(2),
        dma(2), dma(2, 2, RING), dma(RING), dma(*pair), dma(2, 2), dma(*pair), dma(2, 2),
        dma(3), dma(n_layers), dma(n_layers), dma(n_layers),
    ]
    res = pl.pallas_call(
        model_kernel,
        out_shape=out_shape,
        in_specs=[any_spec] * 7,
        out_specs=[any_spec] * len(out_shape),
        scratch_shapes=scratch,
        compiler_params=pltpu.CompilerParams(collective_id=0, has_side_effects=True, vmem_limit_bytes=VMEM_LIMIT),
        name="two_layers",
    )(xt, gain, wkv_t, w_in, w_out, cos_full, sin_full)
    return res[0], res[6]


def solution(mesh):
    row_size = mesh.shape["row"]
    n_col = mesh.shape["col"]
    n_z = row_size // RING
    n_y = RING
    n_x = n_col // CORES
    n_tp = n_y * n_col
    n_dev = row_size * n_col
    mesh4 = Mesh(mesh.devices.reshape(n_z, n_y, n_x, CORES), ("z", "y", "x", "core"))
    every = ("z", "y", "x", "core")
    col = ("x", "core")
    act_spec = P(NIL, NIL, every)
    w_spec = P(NIL, ("z", "y"), col)

    def device_fn(x_loc, gain_loc, w_in_loc, w_kv_loc, w_out_loc):
        n_layers = w_in_loc.shape[0]
        n_batch, seq_len, d_local = x_loc.shape
        head_dim = w_kv_loc.shape[2] * n_col // 2
        batch_loc = n_batch // n_z
        seq_local = seq_len // n_dev
        steps = np.arange(head_dim // 2, dtype=np.float32)
        inv_freq = (1.0 / 10000.0 ** (steps * 2 / head_dim)).astype(np.float32)
        angles = np.arange(seq_len, dtype=np.float32)[:, NIL] * inv_freq[NIL, :]
        cos_tab, sin_tab = np.cos(angles), np.sin(angles)
        cos_full = jnp.asarray(np.concatenate([cos_tab, cos_tab], axis=1))
        sin_full = jnp.asarray(np.concatenate([-sin_tab, sin_tab], axis=1))
        y_loc, kv = run_model(x_loc.transpose(0, 2, 1), gain_loc, w_kv_loc.transpose(0, 2, 1), w_in_loc, w_out_loc, cos_full, sin_full)
        y_loc = y_loc.transpose(0, 2, 1)
        kv = kv.reshape(n_layers, n_z, 2, batch_loc, CORES, seq_local, head_dim)
        kv = lax.dynamic_index_in_dim(kv, lax.axis_index("core"), axis=4, keepdims=False)
        kv = kv.transpose(0, 2, 1, 3, 4, 5).reshape(n_layers, 2, n_batch, seq_local, head_dim)
        return y_loc, kv

    return jax.shard_map(device_fn, mesh=mesh4, in_specs=(act_spec, P(NIL, every), w_spec, w_spec, P(NIL, col, ("z", "y"))), out_specs=(act_spec, P(NIL, NIL, NIL, every, NIL)), check_vma=False)
```
